16 devices in a mesh: dp: 2 (over y, z), stage: 8 (over x, core).
Axes of the slice: x: 4, y: 2, z: 1, core: 2. Of those that a mesh axis runs over, the one named last changes fastest.
The devices are a block of a 4x4x8 slice.
Arguments:
- tokens: int32 [16, 128], P('dp'), parts along dimension 0
- labels: int32 [16, 128], P('dp'), parts along dimension 0
- emb_table: bfloat16 [32128, 512], replicated
- w_up: bfloat16 [8, 512, 2048], P('stage')
- w_down: bfloat16 [8, 2048, 512], P('stage')
Outputs:
- output 1: float32 [2], P('dp'), parts along dimension 0
- output 2: float32 [16, 512, 2048], P(('dp', 'stage')), parts along dimension 0
- output 3: float32 [16, 2048, 512], P(('dp', 'stage')), parts along dimension 0
- output 4: float32 [64256, 512], P('dp'), parts along dimension 0
There are 2 independent parts. The reference program is written for one: setup_inputs(seed, part) draws one part's arguments, and reference() takes and returns one part's arrays. A program takes and returns all parts, laid end to end along the dimension named above; an argument that names none is the same for every part.
All inputs are finite; a program needn't handle non-finite values.
Results may differ from the reference program's by a relative error of at most 0.02.
Values are sent between devices in bfloat16 or wider.
A program may use at most 768 MiB of HBM per device.

```python
import jax
import jax.numpy as jnp
from jax import lax

VOCAB_SIZE = 32128
MODEL_DIM = 512
FFN_DIM = 2048
NUM_STAGES = 8
NUM_MICRO = 8
SEQ_TOKENS = 128

LOGIT_SCALE = MODEL_DIM ** -0.5
INV_COUNT = 1.0 / (NUM_MICRO * SEQ_TOKENS)


def setup_inputs(seed: int = 0, part: int = 0) -> dict:
    key_part = jax.random.fold_in(jax.random.key(seed), part)
    key_ids, key_shift = jax.random.split(key_part)
    key_emb, key_up, key_down = jax.random.split(jax.random.key(seed + 1), 3)
    raw_ids = jax.random.randint(key_ids, (NUM_MICRO, SEQ_TOKENS + 1), 0, VOCAB_SIZE)
    shifts = jax.random.randint(key_shift, (NUM_MICRO, SEQ_TOKENS + 1), 0, 9)
    sequence = jnp.right_shift(raw_ids, shifts)
    sequence = sequence.at[0, 0].set(VOCAB_SIZE - 1).at[0, 1].set(0)
    emb_table = jax.random.normal(key_emb, (VOCAB_SIZE, MODEL_DIM), jnp.float32)
    w_up = jax.random.normal(key_up, (NUM_STAGES, MODEL_DIM, FFN_DIM), jnp.float32) * MODEL_DIM ** -0.5
    w_down = jax.random.normal(key_down, (NUM_STAGES, FFN_DIM, MODEL_DIM), jnp.float32) * (2.0 / (FFN_DIM * NUM_STAGES)) ** 0.5
    return {"tokens": sequence[:, :-1], "labels": sequence[:, 1:], "emb_table": emb_table.astype(jnp.bfloat16), "w_up": w_up.astype(jnp.bfloat16), "w_down": w_down.astype(jnp.bfloat16)}


def rms_normalize(x_act):
    x_wide = x_act.astype(jnp.float32)
    inv_rms = lax.rsqrt(jnp.mean(x_wide * x_wide, axis=-1, keepdims=True) + 1e-6)
    return (x_wide * inv_rms).astype(jnp.bfloat16)


def micro_loss(table_f32, up_f32, down_f32, tok_row, lab_row):
    x_act = table_f32[tok_row].astype(jnp.bfloat16)

    def layer_step(x_cur, weights):
        x_wide = x_cur.astype(jnp.float32)
        pre_act = jnp.dot(x_wide, weights[0], preferred_element_type=jnp.float32).astype(jnp.bfloat16)
        hidden = jax.nn.gelu(pre_act.astype(jnp.float32)).astype(jnp.bfloat16)
        branch = jnp.dot(hidden.astype(jnp.float32), weights[1], preferred_element_type=jnp.float32)
        return (x_wide + branch).astype(jnp.bfloat16), None

    x_act, _ = lax.scan(layer_step, x_act, (up_f32, down_f32))
    normed = rms_normalize(x_act)
    logits = (jnp.dot(normed.astype(jnp.float32), table_f32.T, preferred_element_type=jnp.float32) * LOGIT_SCALE).astype(jnp.bfloat16)
    logit_f = logits.astype(jnp.float32)
    log_norm = jax.nn.logsumexp(logit_f, axis=-1)
    picked = jnp.take_along_axis(logit_f, lab_row[:, None], axis=-1)[:, 0]
    return jnp.sum(log_norm - picked) * INV_COUNT


def reference(tokens, labels, emb_table, w_up, w_down):
    table_f32 = emb_table.astype(jnp.float32)
    up_f32 = w_up.astype(jnp.float32)
    down_f32 = w_down.astype(jnp.float32)
    grad_fn = jax.value_and_grad(micro_loss, argnums=(0, 1, 2))

    def micro_step(loop_state, micro_rows):
        loss_sum, grad_emb, grad_up, grad_down = loop_state
        loss_val, grad_all = grad_fn(table_f32, up_f32, down_f32, micro_rows[0], micro_rows[1])
        return (loss_sum + loss_val, grad_emb + grad_all[0], grad_up + grad_all[1], grad_down + grad_all[2]), None

    init_carry = (jnp.zeros((), jnp.float32), jnp.zeros_like(table_f32), jnp.zeros_like(up_f32), jnp.zeros_like(down_f32))
    (loss_sum, grad_emb, grad_up, grad_down), _ = lax.scan(micro_step, init_carry, (tokens, labels))
    return loss_sum.reshape(1), grad_up, grad_down, grad_emb
```

```python
import functools
import math

import jax
import jax.numpy as jnp
from jax import lax
from jax.experimental import pallas as pl
from jax.experimental.pallas import tpu as pltpu
from jax.sharding import PartitionSpec as P

MESH = pl.DeviceIdType.MESH
LOG2E = math.log2(math.e)
LN2 = math.log(2.0)
GELU_C = math.sqrt(2.0 / math.pi)
GELU_K = 0.044715
EPS = 1e-6
LANES = 128
F32 = jnp.float32
BF16 = jnp.bfloat16


def gelu_fwd(a):
    return 0.5 * a * (1.0 + jnp.tanh(GELU_C * (a + GELU_K * (a * a * a))))


def gelu_slope(a):
    a2 = a * a
    t = jnp.tanh(GELU_C * (a + GELU_K * (a2 * a)))
    return 0.5 * (1.0 + t) + (0.5 * a) * (1.0 - t * t) * (GELU_C + (3.0 * GELU_C * GELU_K) * a2)


def dot(x, y):
    return jnp.dot(x, y, preferred_element_type=F32)


def dot_t(x, y):
    return lax.dot_general(x, y, (((0,), (0,)), ((), ())), preferred_element_type=F32)


def remote(src, dst, send_sem, recv_sem, dev):
    return pltpu.make_async_remote_copy(src_ref=src, dst_ref=dst, send_sem=send_sem, recv_sem=recv_sem, device_id={"stage": dev}, device_id_type=MESH)


def pipe_kernel(n_stage, half, tile, x0_hbm, emb_hbm, up_hbm, down_hbm, lab_ref,
                n_out, xs_out, hid_out, da_out, g_out, dx0_out, stat_out,
                xbuf, ybuf, abuf, hbuf, nbuf, gbuf, dxbuf, dx0buf, dnbuf, up, down, up_t, down_t,
                emb, zbuf, n_t, dn_acc, dn_send, dn_recv, dn_own, st_send, st_recv, statall,
                w_sem, e_sem, x_sem, f_send, f_recv, n_send, n_recv, ag_send, ag_recv, fw_send,
                st_sems, dp_sems, dn_ssem, dn_rsem, sa_send, sa_recv, b_send, b_recv, d_send, d_recv, r_send, out_sem):
    n_micro, seq, dim = x0_hbm.shape
    ffn = up.shape[1]
    vocab = emb_hbm.shape[0]
    me = lax.axis_index("stage")
    core = lax.rem(me, 2)
    chip = me // 2
    mate = me + 1 - 2 * core
    last_id = n_stage - 1
    first = me == 0
    last = me == last_id
    fblk = 512
    n_fblk = ffn // fblk
    row0 = core * (vocab - half)
    n_tiles = half // tile

    barrier = pltpu.get_barrier_semaphore()
    for d in range(1, n_stage):
        pl.semaphore_signal(barrier, inc=1, device_id={"stage": lax.rem(me + d, n_stage)}, device_id_type=MESH)
    w_copy = [pltpu.make_async_copy(up_hbm, up, w_sem.at[0]), pltpu.make_async_copy(down_hbm, down, w_sem.at[1])]
    for c in w_copy:
        c.start()

    @pl.when(first)
    def _():
        for m in range(n_micro):
            pltpu.make_async_copy(x0_hbm.at[m], xbuf.at[m], x_sem.at[m]).start()

    e_step = half // e_sem.shape[0]

    def e_copy(i):
        src = emb_hbm.at[pl.ds(pl.multiple_of(row0 + i * e_step, LANES), e_step)]
        return pltpu.make_async_copy(src, emb.at[pl.ds(i * e_step, e_step)], e_sem.at[i])

    for i in range(e_sem.shape[0]):
        e_copy(i).start()
    pl.semaphore_wait(barrier, n_stage - 1)
    for c in w_copy:
        c.wait()

    def transpose_weights():
        for j in range(n_fblk):
            up_t[j * fblk:(j + 1) * fblk, :] = up[:, j * fblk:(j + 1) * fblk].T
            down_t[:, j * fblk:(j + 1) * fblk] = down[j * fblk:(j + 1) * fblk, :].T

    @pl.when(chip >= n_stage // 4)
    def _():
        transpose_weights()

    def n_copies(m):
        tgt = 2 * (m // 2)
        return [remote(nbuf.at[m], nbuf.at[m], n_send.at[m, k], n_recv.at[m], tgt + k) for k in range(2)]

    def fwd(m, carry):
        @pl.when(first)
        def _():
            pltpu.make_async_copy(x0_hbm.at[m], xbuf.at[m], x_sem.at[m]).wait()

        @pl.when(jnp.logical_not(first))
        def _():
            remote(xbuf.at[m], xbuf.at[m], f_send.at[m], f_recv.at[m], me).wait_recv()

        x = xbuf[m]
        for j in range(n_fblk):
            cols = slice(j * fblk, (j + 1) * fblk)
            a = dot(x, up[:, cols]).astype(BF16)
            abuf[m, :, cols] = a
            hbuf[m, :, cols] = gelu_fwd(a.astype(F32)).astype(BF16)
        y = (x.astype(F32) + dot(hbuf[m], down[...])).astype(BF16)
        ybuf[m] = y

        @pl.when(jnp.logical_not(last))
        def _():
            remote(ybuf.at[m], xbuf.at[m], f_send.at[m], f_recv.at[m], me + 1).start()

        @pl.when(last)
        def _():
            yf = y.astype(F32)
            inv = lax.rsqrt(jnp.mean(yf * yf, axis=-1, keepdims=True) + EPS)
            nbuf[m] = (yf * inv).astype(BF16)
            copies = n_copies(m)
            copies[0].start()

            @pl.when(m // 2 != last_id // 2)
            def _():
                copies[1].start()

        pltpu.make_async_copy(hbuf.at[m], hid_out.at[m], out_sem.at[0, m]).start()
        pltpu.make_async_copy(xbuf.at[m], xs_out.at[m], out_sem.at[1, m]).start()
        return carry

    lax.fori_loop(0, n_micro, fwd, 0)

    @pl.when(chip < n_stage // 4)
    def _():
        transpose_weights()

    for k in range(2):
        mk = 2 * chip + k

        @pl.when(jnp.logical_not(last))
        def _():
            remote(nbuf.at[mk], nbuf.at[mk], n_send.at[mk, 0], n_recv.at[mk], me).wait_recv()

        n_t[:, k * seq:(k + 1) * seq] = nbuf[mk].T

    peers = [lax.rem(me + 2 * d, n_stage) for d in range(1, n_stage // 2)]
    ag_copies = [remote(nbuf.at[me], nbuf.at[me], ag_send.at[d], ag_recv.at[me], p) for d, p in enumerate(peers)]
    for c, p in zip(ag_copies, peers):
        pl.when(p != last_id)(c.start)
    for i in range(e_sem.shape[0]):
        e_copy(i).wait()

    pair = 2 * seq
    scale = dim ** -0.5
    lab = jnp.concatenate([lab_ref[pl.ds(2 * chip, 1), :], lab_ref[pl.ds(2 * chip + 1, 1), :]], axis=1)
    dup = core * (2 * half - vocab)
    groups = tile // 8

    def logits_step(i, carry):
        top, tot = carry
        rows = pl.ds(pl.multiple_of(i * tile, LANES), tile)
        z = (dot(emb[rows, :], n_t[...]) * scale).astype(BF16)
        local = i * tile + lax.broadcasted_iota(jnp.int32, (tile, pair), 0)
        zf = jnp.where(local >= dup, z.astype(F32), -jnp.inf)
        zbuf[rows, :] = z
        z3 = zf.reshape(groups, 8, pair)
        new_top = jnp.maximum(top, jnp.max(z3, axis=0))
        safe = jnp.where(new_top == -jnp.inf, 0.0, new_top)
        tot = tot * jnp.exp(top - safe) + jnp.sum(jnp.exp(z3 - safe[None]), axis=0)
        return new_top, tot

    top, tot = lax.fori_loop(0, n_tiles, logits_step, (jnp.full((8, pair), -jnp.inf, F32), jnp.zeros((8, pair), F32)))
    row_top = jnp.max(top, axis=0, keepdims=True)
    row_tot = jnp.sum(tot * jnp.exp(top - row_top), axis=0, keepdims=True)
    st_send[0:8, :] = jnp.broadcast_to(row_top, (8, pair))
    st_send[8:16, :] = jnp.broadcast_to(row_tot, (8, pair))
    st_copy = remote(st_send, st_recv, st_sems.at[0], st_sems.at[1], mate)
    st_copy.start()
    st_copy.wait()
    far_top = st_recv[0:1, :]
    far_tot = st_recv[8:9, :]
    all_top = jnp.maximum(row_top, far_top)
    mine = row_tot * jnp.exp(row_top - all_top)
    other = far_tot * jnp.exp(far_top - all_top)
    lse = all_top + jnp.log(jnp.where(core == 0, mine + other, other + mine))
    shift = lse * LOG2E + math.log2(n_micro * seq)
    inv_count = 1.0 / (n_micro * seq)
    dn_acc[...] = jnp.zeros_like(dn_acc)

    def grad_step(i, picked):
        rows = pl.ds(pl.multiple_of(i * tile, LANES), tile)
        zf = zbuf[rows, :].astype(F32)
        local = i * tile + lax.broadcasted_iota(jnp.int32, (tile, pair), 0)
        prob = jnp.exp2(zf * LOG2E - shift)
        hit = local + row0 == lab
        keep = local >= dup
        dz = jnp.where(keep, jnp.where(hit, prob - inv_count, prob), 0.0).astype(BF16)
        dn_acc[...] += dot_t(dz, emb[rows, :])
        got = jnp.where(hit & keep, zf, 0.0).reshape(groups, 8, pair)
        return picked + jnp.sum(got, axis=0)

    picked = lax.fori_loop(0, n_tiles, grad_step, jnp.zeros((8, pair), F32))
    far = pl.ds(pl.multiple_of((1 - core) * seq, seq), seq)
    near = pl.ds(pl.multiple_of(core * seq, seq), seq)
    dn_send[...] = dn_acc[far, :]
    dp_copy = remote(dn_send, dn_recv, dp_sems.at[0], dp_sems.at[1], mate)
    dp_copy.start()
    row_loss = jnp.where(core == 0, lse, 0.0) - jnp.sum(picked, axis=0, keepdims=True)
    pick = lax.broadcasted_iota(jnp.int32, (8, pair), 0)
    statall[me] = jnp.where(pick == 0, lse, jnp.where(pick == 1, row_loss, 0.0))
    sa_copies = [remote(statall.at[me], statall.at[me], sa_send.at[d - 1], sa_recv.at[me], lax.rem(me + d, n_stage)) for d in range(1, n_stage)]
    for c in sa_copies:
        c.start()
    dp_copy.wait()
    dn = ((dn_acc[near, :] + dn_recv[...]) * scale).astype(BF16)
    dn_copy = remote(dn_own, dnbuf.at[me], dn_ssem, dn_rsem.at[me], last_id)

    @pl.when(last)
    def _():
        dnbuf[last_id] = dn

    @pl.when(jnp.logical_not(last))
    def _():
        dn_own[...] = dn
        dn_copy.start()

    for p in peers:
        got = remote(nbuf.at[p], nbuf.at[p], ag_send.at[0], ag_recv.at[p], me)
        pl.when(jnp.logical_not(last))(got.wait_recv)
        pl.when(mate != last_id)(remote(nbuf.at[p], nbuf.at[p], fw_send.at[p], ag_recv.at[p], mate).start)

    dx0_dst = [1] + list(range(2, n_stage, 2))

    def bwd(m, carry):
        @pl.when(jnp.logical_not(last))
        def _():
            remote(gbuf.at[m], gbuf.at[m], b_send.at[m], b_recv.at[m], me).wait_recv()

        @pl.when(last)
        def _():
            @pl.when(m != last_id)
            def _():
                remote(dnbuf.at[m], dnbuf.at[m], dn_ssem, dn_rsem.at[m], me).wait_recv()

            yf = ybuf[m].astype(F32)
            inv = lax.rsqrt(jnp.mean(yf * yf, axis=-1, keepdims=True) + EPS)
            dnf = dnbuf[m].astype(F32)
            proj = jnp.mean(yf * dnf, axis=-1, keepdims=True)
            gbuf[m] = (dnf * inv - yf * (inv * inv * inv * proj)).astype(BF16)

        g = gbuf[m]
        for j in range(n_fblk):
            cols = slice(j * fblk, (j + 1) * fblk)
            dh = dot(g, down_t[:, cols]).astype(BF16).astype(F32)
            abuf[m, :, cols] = (dh * gelu_slope(abuf[m, :, cols].astype(F32))).astype(BF16)
        dxbuf[m] = (g.astype(F32) + dot(abuf[m], up_t[...])).astype(BF16)

        @pl.when(jnp.logical_not(first))
        def _():
            remote(dxbuf.at[m], gbuf.at[m], b_send.at[m], b_recv.at[m], me - 1).start()

        @pl.when(first)
        def _():
            for k, dev in enumerate(dx0_dst):
                remote(dxbuf.at[m], dx0buf.at[m], d_send.at[m, k], d_recv.at[m], dev).start()

        pltpu.make_async_copy(abuf.at[m], da_out.at[m], out_sem.at[2, m]).start()
        pltpu.make_async_copy(gbuf.at[m], g_out.at[m], out_sem.at[3, m]).start()
        return carry

    lax.fori_loop(0, n_micro, bwd, 0)

    def relay(m, carry):
        @pl.when(jnp.logical_not(first))
        def _():
            remote(dx0buf.at[m], dx0buf.at[m], r_send.at[m], d_recv.at[m], me).wait_recv()

            @pl.when(core == 0)
            def _():
                remote(dx0buf.at[m], dx0buf.at[m], r_send.at[m], d_recv.at[m], mate).start()

            pltpu.make_async_copy(dx0buf.at[m], dx0_out.at[m], out_sem.at[4, m]).start()

        @pl.when(first)
        def _():
            pltpu.make_async_copy(dxbuf.at[m], dx0_out.at[m], out_sem.at[4, m]).start()

        return carry

    lax.fori_loop(0, n_micro, relay, 0)

    for d in range(1, n_stage):
        src = lax.rem(me + d, n_stage)
        remote(statall.at[src], statall.at[src], sa_send.at[0], sa_recv.at[src], me).wait_recv()
    for d in range(1, n_stage // 2):
        src = lax.rem(mate + 2 * d, n_stage)
        pl.when(jnp.logical_not(last))(remote(nbuf.at[src], nbuf.at[src], ag_send.at[0], ag_recv.at[src], me).wait_recv)
    outs = [pltpu.make_async_copy(nbuf, n_out, out_sem.at[5, 0]), pltpu.make_async_copy(statall, stat_out, out_sem.at[5, 1])]
    for c in outs:
        c.start()
    for c in sa_copies:
        c.wait_send()
    for c, p in zip(ag_copies, peers):
        pl.when(p != last_id)(c.wait_send)
        pl.when(mate != last_id)(remote(nbuf.at[p], nbuf.at[p], fw_send.at[p], ag_recv.at[p], mate).wait_send)

    @pl.when(jnp.logical_not(last))
    def _():
        dn_copy.wait_send()

    def drain(m, carry):
        @pl.when(jnp.logical_not(last))
        def _():
            remote(ybuf.at[m], xbuf.at[m], f_send.at[m], f_recv.at[m], me).wait_send()

        @pl.when(last)
        def _():
            copies = n_copies(m)
            copies[0].wait_send()

            @pl.when(m // 2 != last_id // 2)
            def _():
                copies[1].wait_send()

        @pl.when(jnp.logical_not(first))
        def _():
            remote(dxbuf.at[m], gbuf.at[m], b_send.at[m], b_recv.at[m], me).wait_send()

            @pl.when(core == 0)
            def _():
                remote(dx0buf.at[m], dx0buf.at[m], r_send.at[m], d_recv.at[m], me).wait_send()

        @pl.when(first)
        def _():
            for k, dev in enumerate(dx0_dst):
                remote(dxbuf.at[m], dx0buf.at[m], d_send.at[m, k], d_recv.at[m], dev).wait_send()

        pltpu.make_async_copy(hbuf.at[m], hid_out.at[m], out_sem.at[0, m]).wait()
        pltpu.make_async_copy(xbuf.at[m], xs_out.at[m], out_sem.at[1, m]).wait()
        pltpu.make_async_copy(abuf.at[m], da_out.at[m], out_sem.at[2, m]).wait()
        pltpu.make_async_copy(gbuf.at[m], g_out.at[m], out_sem.at[3, m]).wait()
        pltpu.make_async_copy(dx0buf.at[m], dx0_out.at[m], out_sem.at[4, m]).wait()
        return carry

    lax.fori_loop(0, n_micro, drain, 0)
    for c in outs:
        c.wait()


def run_pipe(x0, emb, w_up, w_down, labels, n_stage):
    n_micro, seq, dim = x0.shape
    ffn = w_up.shape[1]
    vocab = emb.shape[0]
    half = (vocab // LANES + 1) // 2 * LANES
    tile = next(t for t in (768, 640, 512, 384, 256, 128) if half % t == 0)
    e_parts = next(k for k in (9, 8, 7, 6, 5, 4, 3, 2, 1) if (half // LANES) % k == 0)
    any_spec = pl.BlockSpec(memory_space=pl.ANY)
    act = (n_micro, seq, dim)
    wide = (n_micro, seq, ffn)
    dma = pltpu.SemaphoreType.DMA
    vm = pltpu.VMEM
    pair = 2 * seq
    return pl.pallas_call(
        functools.partial(pipe_kernel, n_stage, half, tile),
        out_shape=[
            jax.ShapeDtypeStruct(act, BF16), jax.ShapeDtypeStruct(act, BF16), jax.ShapeDtypeStruct(wide, BF16),
            jax.ShapeDtypeStruct(wide, BF16), jax.ShapeDtypeStruct(act, BF16), jax.ShapeDtypeStruct(act, BF16),
            jax.ShapeDtypeStruct((n_stage, 8, pair), F32),
        ],
        in_specs=[any_spec] * 4 + [pl.BlockSpec(memory_space=pltpu.VMEM)],
        out_specs=[any_spec] * 7,
        scratch_shapes=[
            vm(act, BF16), vm(act, BF16), vm(wide, BF16), vm(wide, BF16), vm(act, BF16), vm(act, BF16), vm(act, BF16), vm(act, BF16), vm(act, BF16),
            vm((dim, ffn), BF16), vm((ffn, dim), BF16), vm((ffn, dim), BF16), vm((dim, ffn), BF16),
            vm((half, dim), BF16), vm((half, pair), BF16), vm((dim, pair), BF16), vm((pair, dim), F32),
            vm((seq, dim), F32), vm((seq, dim), F32), vm((seq, dim), BF16), vm((16, pair), F32), vm((16, pair), F32), vm((n_stage, 8, pair), F32),
            dma((2,)), dma((e_parts,)), dma((n_micro,)), dma((n_micro,)), dma((n_micro,)), dma((n_micro, 2)), dma((n_micro,)),
            dma((n_stage,)), dma((n_stage,)), dma((n_stage,)),
            dma((2,)), dma((2,)), dma, dma((n_stage,)), dma((n_stage,)), dma((n_stage,)),
            dma((n_micro,)), dma((n_micro,)), dma((n_micro, n_stage // 2)), dma((n_micro,)), dma((n_micro,)), dma((6, n_micro)),
        ],
        compiler_params=pltpu.CompilerParams(collective_id=0, has_side_effects=True, vmem_limit_bytes=66 * 1000 * 1000),
        cost_estimate=pl.CostEstimate(flops=30 * 10**9, bytes_accessed=60 * 10**6, transcendentals=0),
        name="pipe",
    )(x0, emb, w_up, w_down, labels)


def emb_kernel(n_stage, n_tok, bound_ref, e_ref, n_ref, stat_ref, lab_ref, rank_ref, sid_ref, dx0_ref, out_ref, loss_ref, n_t, dx0s, dz, shift):
    i = pl.program_id(0)
    rows, dim = e_ref.shape
    blk = 256
    scale = dim ** -0.5
    inv_count = 1.0 / n_tok

    @pl.when(i == 0)
    def _():
        n_t[...] = n_ref[...].T
        order = lax.broadcasted_iota(jnp.int32, (n_tok, n_tok), 0) == rank_ref[...]
        dx0s[...] = dot(jnp.where(order, 1.0, 0.0).astype(BF16), dx0_ref[...]).astype(BF16)
        pair = stat_ref.shape[2]
        loss = jnp.zeros((1, pair), F32)
        for d in range(n_stage):
            if d % 2 == 0:
                shift[:, (d // 2) * pair:(d // 2 + 1) * pair] = stat_ref[d, 0:1, :] * LOG2E + math.log2(n_tok)
            loss = loss + stat_ref[d, 1:2, :]
        loss_ref[...] = jnp.broadcast_to(jnp.sum(loss, axis=1, keepdims=True) * inv_count, loss_ref.shape)

    e = e_ref[...]
    vid = i * rows + lax.broadcasted_iota(jnp.int32, (rows, blk), 0)
    for j in range(n_tok // blk):
        cols = slice(j * blk, (j + 1) * blk)
        z = (dot(e, n_t[:, cols]) * scale).astype(BF16).astype(F32)
        prob = jnp.exp2(z * LOG2E - shift[:, cols])
        dz[:, cols] = jnp.where(vid == lab_ref[:, cols], prob - inv_count, prob).astype(BF16)
    out_ref[...] = dot(dz[...], n_ref[...]) * scale

    lo = bound_ref[i]
    hi = bound_ref[i + 1]

    def add_rows(c, carry):
        ids = sid_ref[pl.ds(c, 1), :]
        hot = jnp.where(i * rows + lax.broadcasted_iota(jnp.int32, (rows, LANES), 0) == ids, 1.0, 0.0).astype(BF16)
        out_ref[...] += dot(hot, dx0s[pl.ds(pl.multiple_of(c * LANES, LANES), LANES), :])
        return carry

    lax.fori_loop(lo // LANES, jnp.where(hi > lo, (hi + LANES - 1) // LANES, lo // LANES), add_rows, 0)


def run_emb(emb, n_all, stats, labels, tokens, dx0, n_stage):
    vocab, dim = emb.shape
    n_tok = n_all.shape[0]
    rows = 1024
    steps = pl.cdiv(vocab, rows)
    pos = jnp.arange(n_tok, dtype=jnp.int32)
    tc, tr = tokens[:, None], tokens[None, :]
    before = (tr < tc) | ((tr == tc) & (pos[None, :] < pos[:, None]))
    rank = jnp.sum(before.astype(jnp.int32), axis=1)
    sid = jnp.sum(jnp.where(rank[None, :] == pos[:, None], tr, 0), axis=1)
    bounds = jnp.sum((tr < (jnp.arange(steps + 1, dtype=jnp.int32) * rows)[:, None]).astype(jnp.int32), axis=1)
    full = lambda *shape: pl.BlockSpec(shape, lambda i, b: (0,) * len(shape))
    return pl.pallas_call(
        functools.partial(emb_kernel, n_stage, n_tok),
        out_shape=[jax.ShapeDtypeStruct((vocab, dim), F32), jax.ShapeDtypeStruct((8, LANES), F32)],
        grid_spec=pltpu.PrefetchScalarGridSpec(
            num_scalar_prefetch=1,
            grid=(steps,),
            in_specs=[
                pl.BlockSpec((rows, dim), lambda i, b: (i, 0)),
                full(n_tok, dim), full(*stats.shape), full(1, n_tok), full(1, n_tok), full(n_tok // LANES, LANES), full(n_tok, dim),
            ],
            out_specs=[pl.BlockSpec((rows, dim), lambda i, b: (i, 0)), full(8, LANES)],
            scratch_shapes=[pltpu.VMEM((dim, n_tok), BF16), pltpu.VMEM((n_tok, dim), BF16), pltpu.VMEM((rows, n_tok), BF16), pltpu.VMEM((1, n_tok), F32)],
        ),
        compiler_params=pltpu.CompilerParams(vmem_limit_bytes=60 * 1000 * 1000),
        cost_estimate=pl.CostEstimate(flops=4 * n_tok * vocab * dim, bytes_accessed=6 * vocab * dim, transcendentals=0),
        name="emb",
    )(bounds, emb, n_all, stats, labels[None, :], rank[None, :], sid.reshape(n_tok // LANES, LANES), dx0)


def solution(mesh):
    n_stage = mesh.shape["stage"]

    def device_fn(tokens, labels, emb, w_up, w_down):
        n_micro, seq = tokens.shape
        dim = emb.shape[1]
        w_up, w_down = w_up[0], w_down[0]
        ffn = w_up.shape[1]
        n_tok = n_micro * seq
        flat = tokens.reshape(n_tok)
        x0 = jnp.take(emb, flat, axis=0).reshape(n_micro, seq, dim)
        n_all, xs, hid, da, g, dx0, stats = run_pipe(x0, emb, w_up, w_down, labels, n_stage)
        grad_emb, loss = run_emb(emb, n_all.reshape(n_tok, dim), stats, labels.reshape(n_tok), flat, dx0.reshape(n_tok, dim), n_stage)
        over = lambda p, q: lax.dot_general(p.reshape(n_tok, -1), q.reshape(n_tok, -1), (((0,), (0,)), ((), ())), preferred_element_type=F32)
        return loss[0, :1], over(xs, da)[None], over(hid, g)[None], grad_emb

    return jax.shard_map(device_fn, mesh=mesh, in_specs=(P("dp", None), P("dp", None), P(None, None), P("stage", None, None), P("stage", None, None)), out_specs=(P("dp"), P(("dp", "stage"), None, None), P(("dp", "stage"), None, None), P("dp", None)), check_vma=False)
```

```python
import functools
import math

import jax
import jax.numpy as jnp
from jax import lax
from jax.experimental import pallas as pl
from jax.experimental.pallas import tpu as pltpu
from jax.sharding import PartitionSpec as P

MESH = pl.DeviceIdType.MESH
LOG2E = math.log2(math.e)
LN2 = math.log(2.0)
GELU_C = math.sqrt(2.0 / math.pi)
GELU_K = 0.044715
EPS = 1e-6
LANES = 128
F32 = jnp.float32
BF16 = jnp.bfloat16


def gelu_fwd(a):
    return 0.5 * a * (1.0 + jnp.tanh(GELU_C * (a + GELU_K * (a * a * a))))


def gelu_slope(a):
    a2 = a * a
    t = jnp.tanh(GELU_C * (a + GELU_K * (a2 * a)))
    return 0.5 * (1.0 + t) + (0.5 * a) * (1.0 - t * t) * (GELU_C + (3.0 * GELU_C * GELU_K) * a2)


def dot(x, y):
    return jnp.dot(x, y, preferred_element_type=F32)


def dot_t(x, y):
    return lax.dot_general(x, y, (((0,), (0,)), ((), ())), preferred_element_type=F32)


def remote(src, dst, send_sem, recv_sem, dev):
    return pltpu.make_async_remote_copy(src_ref=src, dst_ref=dst, send_sem=send_sem, recv_sem=recv_sem, device_id={"stage": dev}, device_id_type=MESH)


def gather_kernel(n_stage, ids_ref, row_ref, tok_ref, cut_ref, emb_hbm, x0_out, rank_out, sid_out, cnt_out, tiles, sem):
    n_micro, seq = tok_ref.shape
    n_tok = n_micro * seq
    me = lax.axis_index("stage")
    group = tiles.shape[1] // seq
    slots = tiles.shape[0]
    owners = [head_chunk(me, k, n_micro) for k in range(slots)]

    def fetch(k):
        def one(i, carry):
            t = ids_ref[owners[k] * seq + i]
            start = pl.multiple_of(t // group * group, group)
            pltpu.make_async_copy(emb_hbm.at[pl.ds(start, group)], tiles.at[k, pl.ds(pl.multiple_of(i * group, group), group)], sem.at[k]).start()
            return carry

        lax.fori_loop(0, seq, one, 0, unroll=8)

    fetch(0)
    for k in range(1, slots):
        pl.when(me < slots)(functools.partial(fetch, k))

    def column(row):
        return jnp.broadcast_to(row, (LANES, LANES)).T

    sub = lax.broadcasted_iota(jnp.int32, (LANES, LANES), 0)
    lane = lax.broadcasted_iota(jnp.int32, (LANES, LANES), 1)
    tok_row = row_ref[...]
    key_row = tok_row * n_tok + lax.broadcasted_iota(jnp.int32, (1, n_tok), 1)
    n_grp = n_tok // LANES
    cols = [column(tok_row[:, c * LANES:(c + 1) * LANES].astype(F32)) for c in range(n_grp)]
    keys = [cols[c].astype(jnp.int32) * n_tok + (sub + c * LANES) for c in range(n_grp)]
    ranks = []
    for g in range(n_grp):
        mine = key_row[:, g * LANES:(g + 1) * LANES]
        acc = jnp.zeros((LANES, LANES), F32)
        for c in range(n_grp):
            acc = acc + jnp.where(keys[c] < mine, 1.0, 0.0)
        ranks.append(jnp.sum(acc, axis=0, keepdims=True))
        rank_out[:, g * LANES:(g + 1) * LANES] = ranks[g].astype(jnp.int32)
    rank_cols = [column(r) for r in ranks]
    for g in range(n_grp):
        want = (lane + g * LANES).astype(F32)
        acc = jnp.zeros((LANES, LANES), F32)
        for c in range(n_grp):
            acc = acc + jnp.where(rank_cols[c] == want, cols[c], 0.0)
        sid_out[g:g + 1, :] = jnp.sum(acc, axis=0, keepdims=True).astype(jnp.int32)
    cut = cut_ref[...].astype(F32)
    acc = jnp.zeros((LANES, LANES), F32)
    for c in range(n_grp):
        acc = acc + jnp.where(cols[c] < cut, 1.0, 0.0)
    cnt_out[...] = jnp.sum(acc, axis=0, keepdims=True).astype(jnp.int32)

    def select(k):
        pltpu.make_async_copy(emb_hbm.at[pl.ds(0, seq * group)], tiles.at[k], sem.at[k]).wait()
        tok = column(tok_ref[pl.ds(owners[k], 1), :].astype(F32)).astype(jnp.int32)
        want = sub * group + (tok - tok // group * group)
        hot = [jnp.where(lane + b * LANES == want, 1.0, 0.0).astype(BF16) for b in range(seq * group // LANES)]
        x0_out[k] = dot(jnp.concatenate(hot, axis=1), tiles[k]).astype(BF16)

    select(0)
    for k in range(1, slots):
        pl.when(me < slots)(functools.partial(select, k))


def head_chunk(dev, k, n_micro):
    return jnp.minimum(jnp.where(dev < 2, 2 * dev + k, dev + 2), n_micro - 1)


def run_gather(tokens, emb, cuts, n_stage):
    n_micro, seq = tokens.shape
    n_tok = n_micro * seq
    dim = emb.shape[1]
    group = 16
    vspec = pl.BlockSpec(memory_space=pltpu.VMEM)
    return pl.pallas_call(
        functools.partial(gather_kernel, n_stage),
        out_shape=[
            jax.ShapeDtypeStruct((2, seq, dim), BF16), jax.ShapeDtypeStruct((1, n_tok), jnp.int32),
            jax.ShapeDtypeStruct((n_tok // LANES, LANES), jnp.int32), jax.ShapeDtypeStruct((1, LANES), jnp.int32),
        ],
        in_specs=[pl.BlockSpec(memory_space=pltpu.SMEM), vspec, vspec, vspec, pl.BlockSpec(memory_space=pl.ANY)],
        out_specs=[vspec] * 4,
        scratch_shapes=[pltpu.VMEM((2, seq * group, dim), BF16), pltpu.SemaphoreType.DMA((2,))],
        compiler_params=pltpu.CompilerParams(vmem_limit_bytes=32 * 1000 * 1000),
        cost_estimate=pl.CostEstimate(flops=10**9, bytes_accessed=2 * seq * group * dim * 2, transcendentals=0),
        name="gather",
    )(tokens.reshape(n_tok), tokens.reshape(1, n_tok), tokens, cuts, emb)


def logit_grad(e, n_t, shift, lab, first_id, inv_count, scale, dz):
    rows = e.shape[0]
    n_tok = n_t.shape[1]
    blk = 256
    vid = lax.broadcasted_iota(jnp.int32, (rows, blk), 0)
    for j in range(n_tok // blk):
        cols = slice(j * blk, (j + 1) * blk)
        z = (dot(e, n_t[:, cols]) * scale).astype(BF16).astype(F32)
        prob = jnp.exp2(z * LOG2E - shift[:, cols])
        dz[:, cols] = jnp.where(vid == lab[:, cols] - first_id, prob - inv_count, prob).astype(BF16)


def pipe_kernel(n_stage, plan, x0_hbm, emb_hbm, up_hbm, down_hbm, lab_ref,
                n_out, xs_out, hid_out, da_out, g_out, dx0_out, stat_out, tmp_out,
                xbuf, ybuf, abuf, hbuf, nbuf, gbuf, dxbuf, dx0buf, dnbuf, up, down, up_t, down_t,
                emb, zbuf, n_t, dn_acc, dn_send, dn_recv, dn_own, st_send, st_recv, statall, tops, n_all_t, shift, dz, obuf,
                w_sem, e_sem, x_sem, f_send, f_recv, n_send, n_recv, ag_send, ag_recv, fw_send,
                st_sems, dp_sems, dn_ssem, dn_rsem, sa_send, sa_recv, b_send, b_recv, d_send, d_recv, r_send, out_sem, x_send, o_sem, od_send, od_recv):
    n_micro, seq, dim = xbuf.shape
    n_tok = n_micro * seq
    ffn = up.shape[1]
    vocab = emb_hbm.shape[0]
    me = lax.axis_index("stage")
    core = lax.rem(me, 2)
    chip = me // 2
    mate = me + 1 - 2 * core
    last_id = n_stage - 1
    first = me == 0
    last = me == last_id
    fblk = 512
    n_fblk = ffn // fblk
    base, extra, tile = plan.base, plan.extra, plan.head_tile
    row0 = core * (base + extra)
    n_tiles = base // tile

    barrier = pltpu.get_barrier_semaphore()
    for d in range(1, n_stage):
        pl.semaphore_signal(barrier, inc=1, device_id={"stage": lax.rem(me + d, n_stage)}, device_id_type=MESH)
    w_copy = [pltpu.make_async_copy(up_hbm, up, w_sem.at[0]), pltpu.make_async_copy(down_hbm, down, w_sem.at[1])]
    for c in w_copy:
        c.start()
    x_slots = x0_hbm.shape[0]
    x_mine = [head_chunk(me, k, n_micro) for k in range(x_slots)]

    @pl.when(first)
    def _():
        for k in range(x_slots):
            pltpu.make_async_copy(x0_hbm.at[k], xbuf.at[k], x_sem.at[k]).start()

    e_parts = e_sem.shape[0] - 1
    e_step = base // e_parts

    def e_copy(i):
        src = emb_hbm.at[pl.ds(pl.multiple_of(row0 + i * e_step, 16), e_step)]
        return pltpu.make_async_copy(src, emb.at[pl.ds(i * e_step, e_step)], e_sem.at[i])

    e_more = pltpu.make_async_copy(emb_hbm.at[pl.ds(base, extra)], emb.at[pl.ds(base, extra)], e_sem.at[e_parts])
    for i in range(e_parts):
        e_copy(i).start()
    pl.when(core == 0)(e_more.start)
    pl.semaphore_wait(barrier, n_stage - 1)

    def x_copy(k):
        return remote(x0_hbm.at[k], xbuf.at[x_mine[k]], x_send.at[k], f_recv.at[x_mine[k]], 0)

    @pl.when(jnp.logical_not(first) & (me + 2 < n_micro))
    def _():
        x_copy(0).start()

        @pl.when(me < 2)
        def _():
            x_copy(1).start()

    for c in w_copy:
        c.wait()

    def transpose_weights():
        for j in range(n_fblk):
            up_t[j * fblk:(j + 1) * fblk, :] = up[:, j * fblk:(j + 1) * fblk].T
            down_t[:, j * fblk:(j + 1) * fblk] = down[j * fblk:(j + 1) * fblk, :].T

    @pl.when(chip >= n_stage // 4)
    def _():
        transpose_weights()

    def n_copies(m):
        tgt = 2 * (m // 2)
        return [remote(nbuf.at[m], nbuf.at[m], n_send.at[m, k], n_recv.at[m], tgt + k) for k in range(2)]

    def fwd(m, carry):
        local = first & (m < x_slots)

        @pl.when(local)
        def _():
            pltpu.make_async_copy(x0_hbm.at[m], xbuf.at[m], x_sem.at[m]).wait()

        @pl.when(jnp.logical_not(local))
        def _():
            remote(xbuf.at[m], xbuf.at[m], f_send.at[m], f_recv.at[m], me).wait_recv()

        x = xbuf[m]
        for j in range(n_fblk):
            cols = slice(j * fblk, (j + 1) * fblk)
            a = dot(x, up[:, cols]).astype(BF16)
            abuf[m, :, cols] = a
            hbuf[m, :, cols] = gelu_fwd(a.astype(F32)).astype(BF16)
        y = (x.astype(F32) + dot(hbuf[m], down[...])).astype(BF16)
        ybuf[m] = y

        @pl.when(jnp.logical_not(last))
        def _():
            remote(ybuf.at[m], xbuf.at[m], f_send.at[m], f_recv.at[m], me + 1).start()

        @pl.when(last)
        def _():
            yf = y.astype(F32)
            inv = lax.rsqrt(jnp.mean(yf * yf, axis=-1, keepdims=True) + EPS)
            nbuf[m] = (yf * inv).astype(BF16)
            copies = n_copies(m)
            copies[0].start()

            @pl.when(m // 2 != last_id // 2)
            def _():
                copies[1].start()

        pltpu.make_async_copy(hbuf.at[m], hid_out.at[m], out_sem.at[0, m]).start()
        pltpu.make_async_copy(xbuf.at[m], xs_out.at[m], out_sem.at[1, m]).start()
        return carry

    lax.fori_loop(0, n_micro, fwd, 0)

    @pl.when(chip < n_stage // 4)
    def _():
        transpose_weights()

    for k in range(2):
        mk = 2 * chip + k

        @pl.when(jnp.logical_not(last))
        def _():
            remote(nbuf.at[mk], nbuf.at[mk], n_send.at[mk, 0], n_recv.at[mk], me).wait_recv()

        n_t[:, k * seq:(k + 1) * seq] = nbuf[mk].T

    peers = [lax.rem(me + 2 * d, n_stage) for d in range(1, n_stage // 2)]
    ag_copies = [remote(nbuf.at[me], nbuf.at[me], ag_send.at[d], ag_recv.at[me], p) for d, p in enumerate(peers)]
    for c, p in zip(ag_copies, peers):
        pl.when(p != last_id)(c.start)
    for i in range(e_parts):
        e_copy(i).wait()
    pl.when(core == 0)(e_more.wait)

    pair = 2 * seq
    scale = dim ** -0.5
    inv_count = 1.0 / n_tok
    log_count = math.log2(n_tok)
    lab = lab_ref[:, pl.ds(pl.multiple_of(chip * pair, pair), pair)]

    def logits(rows, size, top, tot):
        z = (dot(emb[rows, :], n_t[...]) * scale).astype(BF16)
        zbuf[rows, :] = z
        z3 = z.astype(F32).reshape(size // 8, 8, pair)
        new_top = jnp.maximum(top, jnp.max(z3, axis=0))
        off = new_top * LOG2E
        return new_top, tot * jnp.exp2(top * LOG2E - off) + jnp.sum(jnp.exp2(z3 * LOG2E - off[None]), axis=0)

    tops[0] = jnp.full((8, pair), -jnp.inf, F32)
    tops[1] = jnp.zeros((8, pair), F32)

    @pl.when(core == 0)
    def _():
        tops[0], tops[1] = logits(pl.ds(base, extra), extra, tops[0], tops[1])

    top, tot = lax.fori_loop(0, n_tiles, lambda i, c: logits(pl.ds(pl.multiple_of(i * tile, 16), tile), tile, *c), (tops[0], tops[1]))
    row_top = jnp.max(top, axis=0, keepdims=True)
    row_tot = jnp.sum(tot * jnp.exp2((top - row_top) * LOG2E), axis=0, keepdims=True)
    st_send[0:8, :] = jnp.broadcast_to(row_top, (8, pair))
    st_send[8:16, :] = jnp.broadcast_to(row_tot, (8, pair))
    st_copy = remote(st_send, st_recv, st_sems.at[0], st_sems.at[1], mate)
    st_copy.start()
    st_copy.wait()
    far_top = st_recv[0:1, :]
    far_tot = st_recv[8:9, :]
    all_top = jnp.maximum(row_top, far_top)
    mine = row_tot * jnp.exp(row_top - all_top)
    other = far_tot * jnp.exp(far_top - all_top)
    lse = all_top + jnp.log(jnp.where(core == 0, mine + other, other + mine))
    my_shift = lse * LOG2E + log_count

    def grads(rows, size, first_row, picked):
        zf = zbuf[rows, :].astype(F32)
        prob = jnp.exp2(zf * LOG2E - my_shift)
        hit = lax.broadcasted_iota(jnp.int32, (size, pair), 0) == lab - (row0 + first_row)
        dz_t = jnp.where(hit, prob - inv_count, prob).astype(BF16)
        got = jnp.where(hit, zf, 0.0).reshape(size // 8, 8, pair)
        return dot_t(dz_t, emb[rows, :]), picked + jnp.sum(got, axis=0)

    tops[0] = jnp.zeros((8, pair), F32)
    dn_acc[...] = jnp.zeros_like(dn_acc)

    @pl.when(core == 0)
    def _():
        dn_acc[...], tops[0] = grads(pl.ds(base, extra), extra, base, tops[0])

    def grad_step(i, picked):
        part, picked = grads(pl.ds(pl.multiple_of(i * tile, 16), tile), tile, i * tile, picked)
        dn_acc[...] += part
        return picked

    picked = lax.fori_loop(0, n_tiles, grad_step, tops[0])
    far = pl.ds(pl.multiple_of((1 - core) * seq, seq), seq)
    near = pl.ds(pl.multiple_of(core * seq, seq), seq)
    dn_send[...] = dn_acc[far, :]
    dp_copy = remote(dn_send, dn_recv, dp_sems.at[0], dp_sems.at[1], mate)
    dp_copy.start()
    row_loss = jnp.where(core == 0, lse, 0.0) - jnp.sum(picked, axis=0, keepdims=True)
    pick = lax.broadcasted_iota(jnp.int32, (8, pair), 0)
    statall[me] = jnp.where(pick == 0, lse, jnp.where(pick == 1, row_loss, 0.0))
    sa_copies = [remote(statall.at[me], statall.at[me], sa_send.at[d - 1], sa_recv.at[me], lax.rem(me + d, n_stage)) for d in range(1, n_stage)]
    for c in sa_copies:
        c.start()
    dp_copy.wait()
    dn = ((dn_acc[near, :] + dn_recv[...]) * scale).astype(BF16)
    dn_copy = remote(dn_own, dnbuf.at[me], dn_ssem, dn_rsem.at[me], last_id)

    @pl.when(last)
    def _():
        dnbuf[last_id] = dn

    @pl.when(jnp.logical_not(last))
    def _():
        dn_own[...] = dn
        dn_copy.start()

    for p in peers:
        got = remote(nbuf.at[p], nbuf.at[p], ag_send.at[0], ag_recv.at[p], me)
        pl.when(jnp.logical_not(last))(got.wait_recv)
        pl.when(mate != last_id)(remote(nbuf.at[p], nbuf.at[p], fw_send.at[p], ag_recv.at[p], mate).start)

    dx0_dst = [1] + list(range(2, n_stage, 2))

    def bwd(m):
        @pl.when(jnp.logical_not(last))
        def _():
            remote(gbuf.at[m], gbuf.at[m], b_send.at[m], b_recv.at[m], me).wait_recv()

        @pl.when(last)
        def _():
            @pl.when(m != last_id)
            def _():
                remote(dnbuf.at[m], dnbuf.at[m], dn_ssem, dn_rsem.at[m], me).wait_recv()

            yf = ybuf[m].astype(F32)
            inv = lax.rsqrt(jnp.mean(yf * yf, axis=-1, keepdims=True) + EPS)
            dnf = dnbuf[m].astype(F32)
            proj = jnp.mean(yf * dnf, axis=-1, keepdims=True)
            gbuf[m] = (dnf * inv - yf * (inv * inv * inv * proj)).astype(BF16)

        g = gbuf[m]
        for j in range(n_fblk):
            cols = slice(j * fblk, (j + 1) * fblk)
            dh = dot(g, down_t[:, cols]).astype(BF16).astype(F32)
            abuf[m, :, cols] = (dh * gelu_slope(abuf[m, :, cols].astype(F32))).astype(BF16)
        dxbuf[m] = (g.astype(F32) + dot(abuf[m], up_t[...])).astype(BF16)

        @pl.when(jnp.logical_not(first))
        def _():
            remote(dxbuf.at[m], gbuf.at[m], b_send.at[m], b_recv.at[m], me - 1).start()

        @pl.when(first)
        def _():
            for k, dev in enumerate(dx0_dst):
                remote(dxbuf.at[m], dx0buf.at[m], d_send.at[m, k], d_recv.at[m], dev).start()

        pltpu.make_async_copy(abuf.at[m], da_out.at[m], out_sem.at[2, m]).start()
        pltpu.make_async_copy(gbuf.at[m], g_out.at[m], out_sem.at[3, m]).start()

    def tile_copies(k, slot):
        rows = pl.ds(pl.multiple_of(k * plan.rows, plan.rows), plan.rows)
        own = pltpu.make_async_copy(obuf.at[slot], tmp_out.at[core, rows], o_sem.at[slot])
        return own, remote(obuf.at[slot], tmp_out.at[core, rows], od_send.at[k], od_recv.at[k], mate)

    def emb_tile(k):
        @pl.when(k == 0)
        def _():
            for d in range(1, n_stage):
                src = lax.rem(me + d, n_stage)
                remote(statall.at[src], statall.at[src], sa_send.at[0], sa_recv.at[src], me).wait_recv()
            for d in range(1, n_stage // 2):
                src = lax.rem(mate + 2 * d, n_stage)
                pl.when(jnp.logical_not(last))(remote(nbuf.at[src], nbuf.at[src], ag_send.at[0], ag_recv.at[src], me).wait_recv)
            for m in range(n_micro):
                n_all_t[:, m * seq:(m + 1) * seq] = nbuf[m].T
            for c in range(n_stage // 2):
                shift[:, c * pair:(c + 1) * pair] = statall[2 * c, 0:1, :] * LOG2E + log_count

        slot = lax.rem(k, 2)

        @pl.when(k >= 2)
        def _():
            own, far_copy = tile_copies(k - 2, slot)
            own.wait()
            far_copy.wait_send()

        rows = pl.ds(pl.multiple_of(k * plan.rows, plan.rows), plan.rows)
        logit_grad(emb[rows, :], n_all_t, shift, lab_ref, row0 + k * plan.rows, inv_count, scale, dz)
        obuf[slot] = dot(dz[...], nbuf[...].reshape(n_tok, dim)) * scale
        own, far_copy = tile_copies(k, slot)
        own.start()
        far_copy.start()

    before = sum(jnp.where(me == s, plan.before[s], 0) for s in range(n_stage))

    def work(i, carry):
        chunk = (i >= before) & (i < before + n_micro)
        pl.when(chunk)(lambda: bwd(i - before))
        pl.when(jnp.logical_not(chunk))(lambda: emb_tile(jnp.where(i < before, i, i - n_micro)))
        return carry

    lax.fori_loop(0, plan.tiles + n_micro, work, 0)
    outs = [pltpu.make_async_copy(nbuf, n_out, out_sem.at[5, 0]), pltpu.make_async_copy(statall, stat_out, out_sem.at[5, 1])]
    for c in outs:
        c.start()

    def relay(m, carry):
        @pl.when(jnp.logical_not(first))
        def _():
            remote(dx0buf.at[m], dx0buf.at[m], r_send.at[m], d_recv.at[m], me).wait_recv()

            @pl.when(core == 0)
            def _():
                remote(dx0buf.at[m], dx0buf.at[m], r_send.at[m], d_recv.at[m], mate).start()

            pltpu.make_async_copy(dx0buf.at[m], dx0_out.at[m], out_sem.at[4, m]).start()

        @pl.when(first)
        def _():
            pltpu.make_async_copy(dxbuf.at[m], dx0_out.at[m], out_sem.at[4, m]).start()

        return carry

    lax.fori_loop(0, n_micro, relay, 0)

    for k in range(max(plan.tiles - 2, 0), plan.tiles):
        own, far_copy = tile_copies(k, k % 2)
        own.wait()
        far_copy.wait_send()
    for k in range(plan.tiles):
        rows = pl.ds(k * plan.rows, plan.rows)
        remote(obuf.at[0], tmp_out.at[1 - core, rows], od_send.at[k], od_recv.at[k], me).wait_recv()
    for c in sa_copies:
        c.wait_send()
    for c, p in zip(ag_copies, peers):
        pl.when(p != last_id)(c.wait_send)
        pl.when(mate != last_id)(remote(nbuf.at[p], nbuf.at[p], fw_send.at[p], ag_recv.at[p], mate).wait_send)

    @pl.when(jnp.logical_not(last))
    def _():
        dn_copy.wait_send()

    @pl.when(jnp.logical_not(first) & (me + 2 < n_micro))
    def _():
        x_copy(0).wait_send()

        @pl.when(me < 2)
        def _():
            x_copy(1).wait_send()

    def drain(m, carry):
        @pl.when(jnp.logical_not(last))
        def _():
            remote(ybuf.at[m], xbuf.at[m], f_send.at[m], f_recv.at[m], me).wait_send()

        @pl.when(last)
        def _():
            copies = n_copies(m)
            copies[0].wait_send()

            @pl.when(m // 2 != last_id // 2)
            def _():
                copies[1].wait_send()

        @pl.when(jnp.logical_not(first))
        def _():
            remote(dxbuf.at[m], gbuf.at[m], b_send.at[m], b_recv.at[m], me).wait_send()

            @pl.when(core == 0)
            def _():
                remote(dx0buf.at[m], dx0buf.at[m], r_send.at[m], d_recv.at[m], me).wait_send()

        @pl.when(first)
        def _():
            for k, dev in enumerate(dx0_dst):
                remote(dxbuf.at[m], dx0buf.at[m], d_send.at[m, k], d_recv.at[m], dev).wait_send()

        pltpu.make_async_copy(hbuf.at[m], hid_out.at[m], out_sem.at[0, m]).wait()
        pltpu.make_async_copy(xbuf.at[m], xs_out.at[m], out_sem.at[1, m]).wait()
        pltpu.make_async_copy(abuf.at[m], da_out.at[m], out_sem.at[2, m]).wait()
        pltpu.make_async_copy(gbuf.at[m], g_out.at[m], out_sem.at[3, m]).wait()
        pltpu.make_async_copy(dx0buf.at[m], dx0_out.at[m], out_sem.at[4, m]).wait()
        return carry

    lax.fori_loop(0, n_micro, drain, 0)
    for c in outs:
        c.wait()


class Plan:
    def __init__(self, vocab, n_stage):
        units = vocab // LANES
        self.base = units // 2 * LANES
        self.extra = vocab - 2 * self.base
        self.head_tile = next(t for t in (1600, 1536, 1280, 1024, 768, 640, 512, 256, 128) if self.base % t == 0)
        self.rows = 1024
        self.tiles = 9
        self.steps = 12
        arrive, self.before = 0.0, [0] * n_stage
        for s in reversed(range(n_stage)):
            self.before[s] = min(max(int((arrive - 4.5) / 2.6 + 0.3), 0), self.tiles)
            arrive += 2.3 if s % 2 else 4.6
        early = self.tiles * self.rows
        self.half_steps = self.steps // 2
        self.copy_rows = early // self.half_steps
        mid = self.base + self.extra
        self.spans = [(early, mid), (mid + early, vocab)]
        longest = max(b - a for a, b in self.spans)
        self.calc_rows = -(-longest // (16 * self.half_steps)) * 16
        self.over = [self.half_steps * self.calc_rows - (b - a) for a, b in self.spans]
        self.head = max(self.over)

    def calc_start(self, s):
        h, i = s // self.half_steps, s % self.half_steps
        return min(self.spans[h][0] + i * self.calc_rows, self.spans[h][1] - self.calc_rows)

    def copy_start(self, s):
        h, i = s // self.half_steps, s % self.half_steps
        return h * (self.base + self.extra) + i * self.copy_rows


def run_pipe(x0, emb, w_up, w_down, labels, n_stage, plan):
    n_micro, seq = labels.shape
    dim, ffn = w_up.shape
    n_tok = n_micro * seq
    base = plan.base
    e_parts = next(k for k in (10, 8, 5, 4, 2, 1) if base % (16 * k) == 0)
    any_spec = pl.BlockSpec(memory_space=pl.ANY)
    act = (n_micro, seq, dim)
    wide = (n_micro, seq, ffn)
    dma = pltpu.SemaphoreType.DMA
    vm = pltpu.VMEM
    pair = 2 * seq
    return pl.pallas_call(
        functools.partial(pipe_kernel, n_stage, plan),
        out_shape=[
            jax.ShapeDtypeStruct(act, BF16), jax.ShapeDtypeStruct(act, BF16), jax.ShapeDtypeStruct(wide, BF16),
            jax.ShapeDtypeStruct(wide, BF16), jax.ShapeDtypeStruct(act, BF16), jax.ShapeDtypeStruct(act, BF16),
            jax.ShapeDtypeStruct((n_stage, 8, pair), F32), jax.ShapeDtypeStruct((2, plan.tiles * plan.rows, dim), F32),
        ],
        in_specs=[any_spec] * 4 + [pl.BlockSpec(memory_space=pltpu.VMEM)],
        out_specs=[any_spec] * 8,
        scratch_shapes=[
            vm(act, BF16), vm(act, BF16), vm(wide, BF16), vm(wide, BF16), vm(act, BF16), vm(act, BF16), vm(act, BF16), vm(act, BF16), vm(act, BF16),
            vm((dim, ffn), BF16), vm((ffn, dim), BF16), vm((ffn, dim), BF16), vm((dim, ffn), BF16),
            vm((base + plan.extra, dim), BF16), vm((base + plan.extra, pair), BF16), vm((dim, pair), BF16), vm((pair, dim), F32),
            vm((seq, dim), F32), vm((seq, dim), F32), vm((seq, dim), BF16), vm((16, pair), F32), vm((16, pair), F32), vm((n_stage, 8, pair), F32),
            vm((2, 8, pair), F32), vm((dim, n_tok), BF16), vm((1, n_tok), F32), vm((plan.rows, n_tok), BF16), vm((2, plan.rows, dim), F32),
            dma((2,)), dma((e_parts + 1,)), dma((n_micro,)), dma((n_micro,)), dma((n_micro,)), dma((n_micro, 2)), dma((n_micro,)),
            dma((n_stage,)), dma((n_stage,)), dma((n_stage,)),
            dma((2,)), dma((2,)), dma, dma((n_stage,)), dma((n_stage,)), dma((n_stage,)),
            dma((n_micro,)), dma((n_micro,)), dma((n_micro, n_stage // 2)), dma((n_micro,)), dma((n_micro,)), dma((6, n_micro)),
            dma((2,)), dma((2,)), dma((plan.tiles,)), dma((plan.tiles,)),
        ],
        compiler_params=pltpu.CompilerParams(collective_id=0, has_side_effects=True, vmem_limit_bytes=67_000_000),
        cost_estimate=pl.CostEstimate(flops=60 * 10**9, bytes_accessed=100 * 10**6, transcendentals=0),
        name="pipe",
    )(x0, emb, w_up, w_down, labels.reshape(1, n_tok))


def fin_kernel(n_stage, n_tok, plan, cnt_ref, emb_hbm, tmp_hbm, n_hbm, stat_ref, lab_ref, rank_ref, sid_ref, dx0_hbm, xs_hbm, hid_hbm, da_hbm, g_hbm,
               out_hbm, loss_ref, gup_hbm, gdown_hbm,
               n_all, dx0, xs, hid, da, g, n_t, x_t, dx0s, dz, shift, e_in, c_out, cp, gup, gdown,
               ld_sem, e_sem, t_sem, co_sem, po_sem, gu_sem, gd_sem):
    dim = n_all.shape[1]
    ffn = da.shape[1]
    scale = dim ** -0.5
    inv_count = 1.0 / n_tok
    steps, half, crows, prows = plan.steps, plan.half_steps, plan.calc_rows, plan.copy_rows
    mid = plan.base + plan.extra
    wblk = 256
    n_wblk = ffn // wblk

    def calc_start(s):
        h, i = s // half, lax.rem(s, half)
        lo = jnp.where(h == 0, plan.spans[0][0], plan.spans[1][0]) + i * crows
        return pl.multiple_of(jnp.minimum(lo, jnp.where(h == 0, plan.spans[0][1], plan.spans[1][1]) - crows), 16)

    def copy_start(s):
        return pl.multiple_of(s // half * mid + lax.rem(s, half) * prows, 16)

    def e_copy(s):
        return pltpu.make_async_copy(emb_hbm.at[pl.ds(calc_start(s), crows)], e_in.at[lax.rem(s, 2)], e_sem.at[lax.rem(s, 2)])

    def t_copy(s):
        return pltpu.make_async_copy(tmp_hbm.at[pl.ds(pl.multiple_of(s * prows, 16), prows)], cp.at[lax.rem(s, 3)], t_sem.at[lax.rem(s, 3)])

    def p_out(s):
        return pltpu.make_async_copy(cp.at[lax.rem(s, 3)], out_hbm.at[pl.ds(copy_start(s), prows)], po_sem.at[lax.rem(s, 3)])

    def c_outs(s):
        slot = lax.rem(s, 2)
        start = calc_start(s)
        return (
            pltpu.make_async_copy(c_out.at[slot, pl.ds(plan.head, crows - plan.head)], out_hbm.at[pl.ds(start + plan.head, crows - plan.head)], co_sem.at[slot, 0]),
            pltpu.make_async_copy(c_out.at[slot, pl.ds(0, plan.head)], out_hbm.at[pl.ds(start, plan.head)], co_sem.at[slot, 1]),
        )

    def has_head(s):
        skip = False
        for h in range(2):
            if plan.over[h] > 0:
                skip = skip | (s == h * half + half - 1)
        return jnp.logical_not(skip)

    def c_start(s):
        a, b = c_outs(s)
        a.start()
        if plan.head:
            pl.when(has_head(s))(b.start)

    def c_wait(s):
        a, b = c_outs(s)
        a.wait()
        if plan.head:
            pl.when(has_head(s))(b.wait)

    loads = [pltpu.make_async_copy(s, d, ld_sem.at[i]) for i, (s, d) in enumerate(((n_hbm, n_all), (dx0_hbm, dx0), (xs_hbm, xs), (da_hbm, da), (hid_hbm, hid), (g_hbm, g)))]
    loads[0].start()
    loads[1].start()
    e_copy(0).start()
    t_copy(0).start()
    for c in loads[2:]:
        c.start()
    pair = stat_ref.shape[2]
    loss = jnp.zeros((1, pair), F32)
    for d in range(n_stage):
        if d % 2 == 0:
            shift[:, (d // 2) * pair:(d // 2 + 1) * pair] = stat_ref[d, 0:1, :] * LOG2E + math.log2(n_tok)
        loss = loss + stat_ref[d, 1:2, :]
    loss_ref[0] = jnp.sum(loss) * inv_count
    loads[0].wait()
    n_t[...] = n_all[...].T
    loads[1].wait()
    order = lax.broadcasted_iota(jnp.int32, (n_tok, n_tok), 0) == rank_ref[...]
    dx0s[...] = dot(jnp.where(order, 1.0, 0.0).astype(BF16), dx0[...]).astype(BF16)

    def rows_of(c, start, rows):
        hot = lax.broadcasted_iota(jnp.int32, (rows, LANES), 0) == sid_ref[pl.ds(c, 1), :] - start
        return dot(jnp.where(hot, 1.0, 0.0).astype(BF16), dx0s[pl.ds(pl.multiple_of(c * LANES, LANES), LANES), :])

    def first_blk(k):
        return jnp.minimum(cnt_ref[k] // LANES, n_tok // LANES - 1)

    def more(k, start, ref):
        def add(c, carry):
            ref[...] += rows_of(c, start, ref.shape[0])
            return carry

        lax.fori_loop(first_blk(k) + 1, (cnt_ref[k + 1] + LANES - 1) // LANES, add, 0)

    def step(s, carry):
        e_copy(s).wait()
        t_copy(s).wait()

        @pl.when(s + 1 < steps)
        def _():
            e_copy(s + 1).start()

            @pl.when(s >= 2)
            def _():
                p_out(s - 2).wait()

            t_copy(s + 1).start()

        @pl.when(s >= 2)
        def _():
            c_wait(s - 2)

        slot = lax.rem(s, 2)
        pslot = lax.rem(s, 3)
        start = calc_start(s)
        logit_grad(e_in[slot], n_t, shift, lab_ref, start, inv_count, scale, dz)
        c_out[slot] = dot(dz[...], n_all[...]) * scale + rows_of(first_blk(4 * s), start, crows)
        cp[pslot] += rows_of(first_blk(4 * s + 2), copy_start(s), prows)
        more(4 * s, start, c_out.at[slot])
        more(4 * s + 2, copy_start(s), cp.at[pslot])
        c_start(s)
        p_out(s).start()

        w = s - 2

        @pl.when(w == 0)
        def _():
            for c in loads[2:]:
                c.wait()
            x_t[...] = xs[...].T

        @pl.when((w >= 0) & (w < n_wblk))
        def _():
            cols = pl.ds(pl.multiple_of(w * wblk, wblk), wblk)
            wslot = lax.rem(w, 2)
            up_copy, down_copy = w_outs(w)

            @pl.when(w >= 2)
            def _():
                for c in w_outs(w - 2):
                    c.wait()

            gup[wslot] = dot(x_t[...], da[:, cols])
            gdown[wslot] = dot_t(hid[:, cols], g[...])
            up_copy.start()
            down_copy.start()

        return carry

    def w_outs(w):
        cols = pl.ds(pl.multiple_of(w * wblk, wblk), wblk)
        wslot = lax.rem(w, 2)
        return (pltpu.make_async_copy(gup.at[wslot], gup_hbm.at[:, cols], gu_sem.at[wslot]), pltpu.make_async_copy(gdown.at[wslot], gdown_hbm.at[cols], gd_sem.at[wslot]))

    lax.fori_loop(0, steps, step, 0)
    for w in range(n_wblk - 2, n_wblk):
        for c in w_outs(w):
            c.wait()
    for s in range(steps - 2, steps):
        c_wait(s)
    for s in range(steps - 3, steps):
        p_out(s).wait()


def run_fin(emb, tmp, n_all, stats, labels, rank, sid, cnt, dx0, xs, hid, da, g, n_stage, plan):
    vocab, dim = emb.shape
    n_tok, ffn = hid.shape
    vm = pltpu.VMEM
    dma = pltpu.SemaphoreType.DMA
    any_spec = pl.BlockSpec(memory_space=pl.ANY)
    vspec = pl.BlockSpec(memory_space=pltpu.VMEM)
    smem = pl.BlockSpec(memory_space=pltpu.SMEM)
    wblk = 256
    return pl.pallas_call(
        functools.partial(fin_kernel, n_stage, n_tok, plan),
        out_shape=[jax.ShapeDtypeStruct((vocab, dim), F32), jax.ShapeDtypeStruct((1,), F32), jax.ShapeDtypeStruct((dim, ffn), F32), jax.ShapeDtypeStruct((ffn, dim), F32)],
        in_specs=[smem, any_spec, any_spec, any_spec, vspec, vspec, vspec, vspec] + [any_spec] * 5,
        out_specs=[any_spec, smem, any_spec, any_spec],
        scratch_shapes=[
            vm((n_tok, dim), BF16), vm((n_tok, dim), BF16), vm((n_tok, dim), BF16), vm((n_tok, ffn), BF16), vm((n_tok, ffn), BF16), vm((n_tok, dim), BF16),
            vm((dim, n_tok), BF16), vm((dim, n_tok), BF16), vm((n_tok, dim), BF16), vm((plan.calc_rows, n_tok), BF16), vm((1, n_tok), F32),
            vm((2, plan.calc_rows, dim), BF16), vm((2, plan.calc_rows, dim), F32), vm((3, plan.copy_rows, dim), F32),
            vm((2, dim, wblk), F32), vm((2, wblk, dim), F32),
            dma((6,)), dma((2,)), dma((3,)), dma((2, 2)), dma((3,)), dma((2,)), dma((2,)),
        ],
        compiler_params=pltpu.CompilerParams(vmem_limit_bytes=67_000_000),
        cost_estimate=pl.CostEstimate(flops=2 * n_tok * vocab * dim, bytes_accessed=5 * vocab * dim, transcendentals=0),
        name="fin",
    )(cnt, emb, tmp, n_all, stats, labels.reshape(1, n_tok), rank, sid, dx0, xs, hid, da, g)


def solution(mesh):
    n_stage = mesh.shape["stage"]

    def device_fn(tokens, labels, emb, w_up, w_down):
        n_micro, seq = tokens.shape
        vocab, dim = emb.shape
        w_up, w_down = w_up[0], w_down[0]
        n_tok = n_micro * seq
        plan = Plan(vocab, n_stage)
        cuts = []
        for s in range(plan.steps):
            for lo, rows in ((plan.calc_start(s), plan.calc_rows), (plan.copy_start(s), plan.copy_rows)):
                cuts += [lo, lo + rows]
        cuts = jnp.array(cuts + [vocab] * (LANES - len(cuts)), jnp.int32).reshape(1, LANES)
        x0, rank, sid, cnt = run_gather(tokens, emb, cuts, n_stage)
        n_all, xs, hid, da, g, dx0, stats, tmp = run_pipe(x0, emb, w_up, w_down, labels, n_stage, plan)
        flat = lambda p: p.reshape(n_tok, -1)
        grad_emb, loss, grad_up, grad_down = run_fin(
            emb, tmp.reshape(-1, dim), flat(n_all), stats, labels, rank, sid, cnt.reshape(LANES), flat(dx0), flat(xs), flat(hid), flat(da), flat(g), n_stage, plan
        )
        return loss, grad_up[None], grad_down[None], grad_emb

    return jax.shard_map(device_fn, mesh=mesh, in_specs=(P("dp", None), P("dp", None), P(None, None), P("stage", None, None), P("stage", None, None)), out_specs=(P("dp"), P(("dp", "stage"), None, None), P(("dp", "stage"), None, None), P("dp", None)), check_vma=False)
```

```python
import functools
import math

import jax
import jax.numpy as jnp
from jax import lax
from jax.experimental import pallas as pl
from jax.experimental.pallas import tpu as pltpu
from jax.sharding import PartitionSpec as P

MESH = pl.DeviceIdType.MESH
LOG2E = math.log2(math.e)
LN2 = math.log(2.0)
GELU_C = math.sqrt(2.0 / math.pi)
GELU_K = 0.044715
EPS = 1e-6
LANES = 128
F32 = jnp.float32
BF16 = jnp.bfloat16


def gelu_fwd(a):
    return 0.5 * a * (1.0 + jnp.tanh(GELU_C * (a + GELU_K * (a * a * a))))


def gelu_slope(a):
    a2 = a * a
    t = jnp.tanh(GELU_C * (a + GELU_K * (a2 * a)))
    return 0.5 * (1.0 + t) + (0.5 * a) * (1.0 - t * t) * (GELU_C + (3.0 * GELU_C * GELU_K) * a2)


def dot(x, y):
    return jnp.dot(x, y, preferred_element_type=F32)


def dot_t(x, y):
    return lax.dot_general(x, y, (((0,), (0,)), ((), ())), preferred_element_type=F32)


def remote(src, dst, send_sem, recv_sem, dev):
    return pltpu.make_async_remote_copy(src_ref=src, dst_ref=dst, send_sem=send_sem, recv_sem=recv_sem, device_id={"stage": dev}, device_id_type=MESH)


def column(row):
    return jnp.broadcast_to(row, (LANES, LANES)).T


def gather_kernel(ids_ref, tok_ref, emb_hbm, x0_hbm, tiles, picked, sem, out_sem):
    n_micro, seq = tok_ref.shape
    me = lax.axis_index("stage")
    group = tiles.shape[1] // seq
    slots = tiles.shape[0]
    owners = [head_chunk(me, k, n_micro) for k in range(slots)]

    def fetch(k):
        def one(i, carry):
            t = ids_ref[owners[k] * seq + i]
            start = pl.multiple_of(t // group * group, group)
            pltpu.make_async_copy(emb_hbm.at[pl.ds(start, group)], tiles.at[k, pl.ds(pl.multiple_of(i * group, group), group)], sem.at[k]).start()
            return carry

        lax.fori_loop(0, seq, one, 0, unroll=8)

    def select(k):
        sub = lax.broadcasted_iota(jnp.int32, (LANES, LANES), 0)
        lane = lax.broadcasted_iota(jnp.int32, (LANES, LANES), 1)
        tok = column(tok_ref[pl.ds(owners[k], 1), :].astype(F32)).astype(jnp.int32)
        want = sub * group + (tok - tok // group * group)
        hot = jnp.concatenate([jnp.where(lane + b * LANES == want, 1.0, 0.0).astype(BF16) for b in range(seq * group // LANES)], axis=1)
        pltpu.make_async_copy(emb_hbm.at[pl.ds(0, seq * group)], tiles.at[k], sem.at[k]).wait()
        picked[k] = dot(hot, tiles[k]).astype(BF16)
        pltpu.make_async_copy(picked.at[k], x0_hbm.at[k], out_sem.at[k]).start()

    def finish(k):
        pltpu.make_async_copy(picked.at[k], x0_hbm.at[k], out_sem.at[k]).wait()

    for work in (fetch, select, finish):
        work(0)
        for k in range(1, slots):
            pl.when(me < slots)(functools.partial(work, k))


def head_chunk(dev, k, n_micro):
    return jnp.minimum(jnp.where(dev < 2, 2 * dev + k, dev + 2), n_micro - 1)


def run_gather(tokens, emb):
    n_micro, seq = tokens.shape
    dim = emb.shape[1]
    group = 16
    return pl.pallas_call(
        gather_kernel,
        out_shape=jax.ShapeDtypeStruct((2, seq, dim), BF16),
        in_specs=[pl.BlockSpec(memory_space=pltpu.SMEM), pl.BlockSpec(memory_space=pltpu.VMEM), pl.BlockSpec(memory_space=pl.ANY)],
        out_specs=pl.BlockSpec(memory_space=pl.ANY),
        scratch_shapes=[pltpu.VMEM((2, seq * group, dim), BF16), pltpu.VMEM((2, seq, dim), BF16), pltpu.SemaphoreType.DMA((2,)), pltpu.SemaphoreType.DMA((2,))],
        cost_estimate=pl.CostEstimate(flops=10**9, bytes_accessed=2 * seq * group * dim * 2, transcendentals=0),
        name="gather",
    )(tokens.reshape(n_micro * seq), tokens, emb)


def token_table(row_ref, cut_ref, meta):
    n_tok = row_ref.shape[1]
    n_grp = n_tok // LANES
    lane = lax.broadcasted_iota(jnp.int32, (LANES, LANES), 1).astype(F32)
    sub = lax.broadcasted_iota(jnp.int32, (LANES, LANES), 0)
    row = lambda g: row_ref[:, g * LANES:(g + 1) * LANES].astype(F32)
    zero = jnp.zeros((LANES, LANES), F32)
    fold = lambda acc: jnp.sum(acc, axis=0, keepdims=True)
    cols = [column(row(c)) for c in range(n_grp)]
    firsts = []
    for g in range(n_grp):
        acc = zero
        for c in range(g + 1):
            same = cols[c] == row(g)
            if c == g:
                same = same & (sub < lane.astype(jnp.int32))
            acc = acc + jnp.where(same, 1.0, 0.0)
        firsts.append(column(jnp.where(fold(acc) == 0.0, 1.0, 0.0)))
    ranks = []
    for g in range(n_grp):
        acc = zero
        for c in range(n_grp):
            acc = acc + jnp.where(cols[c] < row(g), firsts[c], 0.0)
        ranks.append(fold(acc))
        meta[g:g + 1, :] = ranks[g].astype(jnp.int32)
    rank_cols = [column(r) for r in ranks]
    for g in range(n_grp):
        acc = zero
        for c in range(n_grp):
            acc = acc + jnp.where(rank_cols[c] == lane + g * LANES, firsts[c] * cols[c], 0.0)
        meta[n_grp + g:n_grp + g + 1, :] = fold(acc).astype(jnp.int32)
    cut = cut_ref[...].astype(F32)
    acc = zero
    for c in range(n_grp):
        acc = acc + jnp.where(cols[c] < cut, firsts[c], 0.0)
    meta[2 * n_grp:3 * n_grp, :] = jnp.broadcast_to(fold(acc), (n_grp, LANES)).astype(jnp.int32)


def logit_grad(e, n_t, shift, lab, first_id, inv_count, scale, dz):
    rows = e.shape[0]
    n_tok = n_t.shape[1]
    blk = 256
    vid = lax.broadcasted_iota(jnp.int32, (rows, blk), 0)
    for j in range(n_tok // blk):
        cols = slice(j * blk, (j + 1) * blk)
        z = (dot(e, n_t[:, cols]) * scale).astype(BF16).astype(F32)
        prob = jnp.exp2(z * LOG2E - shift[:, cols])
        dz[:, cols] = jnp.where(vid == lab[:, cols] - first_id, prob - inv_count, prob).astype(BF16)


def pipe_kernel(n_stage, plan, x0_hbm, emb_hbm, up_hbm, down_hbm, lab_ref, row_ref, cut_ref,
                n_out, xs_out, hid_out, da_out, g_out, dx0_out, stat_out, tmp_out, meta_out,
                xbuf, ybuf, abuf, hbuf, nbuf, gbuf, dxbuf, dx0buf, dnbuf, up, down, up_t, down_t,
                emb, zbuf, n_t, dn_acc, dn_send, dn_recv, dn_own, st_send, st_recv, statall, tops, n_all_t, shift, dz, obuf, z_pair, meta,
                w_sem, e_sem, x_sem, f_send, f_recv, n_send, n_recv, ag_send, ag_recv, fw_send,
                st_sems, dp_sems, dn_ssem, dn_rsem, sa_send, sa_recv, b_send, b_recv, d_send, d_recv, r_send, rf_send, out_sem, x_send, o_sem, od_send, od_recv):
    n_micro, seq, dim = xbuf.shape
    n_tok = n_micro * seq
    ffn = up.shape[1]
    vocab = emb_hbm.shape[0]
    me = lax.axis_index("stage")
    core = lax.rem(me, 2)
    chip = me // 2
    mate = me + 1 - 2 * core
    last_id = n_stage - 1
    first = me == 0
    last = me == last_id
    fblk = 512
    n_fblk = ffn // fblk
    base, extra, tile = plan.base, plan.extra, plan.head_tile
    row0 = core * (base + extra)
    n_tiles = base // tile

    barrier = pltpu.get_barrier_semaphore()
    for d in range(1, n_stage):
        pl.semaphore_signal(barrier, inc=1, device_id={"stage": lax.rem(me + d, n_stage)}, device_id_type=MESH)
    w_copy = [pltpu.make_async_copy(up_hbm, up, w_sem.at[0]), pltpu.make_async_copy(down_hbm, down, w_sem.at[1])]
    for c in w_copy:
        c.start()
    x_slots = x0_hbm.shape[0]
    x_mine = [head_chunk(me, k, n_micro) for k in range(x_slots)]

    @pl.when(first)
    def _():
        for k in range(x_slots):
            pltpu.make_async_copy(x0_hbm.at[k], xbuf.at[k], x_sem.at[k]).start()

    e_parts = e_sem.shape[0] - 1
    e_step = base // e_parts

    def e_copy(i):
        src = emb_hbm.at[pl.ds(pl.multiple_of(row0 + i * e_step, 16), e_step)]
        return pltpu.make_async_copy(src, emb.at[pl.ds(i * e_step, e_step)], e_sem.at[i])

    e_more = pltpu.make_async_copy(emb_hbm.at[pl.ds(base, extra)], emb.at[pl.ds(base, extra)], e_sem.at[e_parts])
    pl.semaphore_wait(barrier, n_stage - 1)

    def x_copy(k):
        return remote(x0_hbm.at[k], xbuf.at[x_mine[k]], x_send.at[k], f_recv.at[x_mine[k]], 0)

    @pl.when(jnp.logical_not(first) & (me + 2 < n_micro))
    def _():
        x_copy(0).start()

        @pl.when(me < 2)
        def _():
            x_copy(1).start()

    for c in w_copy:
        c.wait()
    for i in range(e_parts):
        e_copy(i).start()
    pl.when(core == 0)(e_more.start)

    def transpose_weights():
        for j in range(n_fblk):
            up_t[j * fblk:(j + 1) * fblk, :] = up[:, j * fblk:(j + 1) * fblk].T
            down_t[:, j * fblk:(j + 1) * fblk] = down[j * fblk:(j + 1) * fblk, :].T

    @pl.when(chip >= n_stage // 4)
    def _():
        transpose_weights()

    def n_copies(m):
        tgt = 2 * (m // 2)
        return [remote(nbuf.at[m], nbuf.at[m], n_send.at[m, k], n_recv.at[m], tgt + k) for k in range(2)]

    def fwd(m, carry):
        local = first & (m < x_slots)

        @pl.when(local)
        def _():
            pltpu.make_async_copy(x0_hbm.at[m], xbuf.at[m], x_sem.at[m]).wait()

        @pl.when(jnp.logical_not(local))
        def _():
            remote(xbuf.at[m], xbuf.at[m], f_send.at[m], f_recv.at[m], me).wait_recv()

        x = xbuf[m]
        for j in range(n_fblk):
            cols = slice(j * fblk, (j + 1) * fblk)
            a = dot(x, up[:, cols]).astype(BF16)
            abuf[m, :, cols] = a
            hbuf[m, :, cols] = gelu_fwd(a.astype(F32)).astype(BF16)
        y = (x.astype(F32) + dot(hbuf[m], down[...])).astype(BF16)
        ybuf[m] = y

        @pl.when(jnp.logical_not(last))
        def _():
            remote(ybuf.at[m], xbuf.at[m], f_send.at[m], f_recv.at[m], me + 1).start()

        @pl.when(last)
        def _():
            yf = y.astype(F32)
            inv = lax.rsqrt(jnp.mean(yf * yf, axis=-1, keepdims=True) + EPS)
            nbuf[m] = (yf * inv).astype(BF16)
            copies = n_copies(m)
            copies[0].start()

            @pl.when(m // 2 != last_id // 2)
            def _():
                copies[1].start()

        pltpu.make_async_copy(hbuf.at[m], hid_out.at[m], out_sem.at[0, m]).start()
        pltpu.make_async_copy(xbuf.at[m], xs_out.at[m], out_sem.at[1, m]).start()
        return carry

    lax.fori_loop(0, n_micro, fwd, 0)

    @pl.when(chip < n_stage // 4)
    def _():
        transpose_weights()

    for k in range(2):
        mk = 2 * chip + k

        @pl.when(jnp.logical_not(last))
        def _():
            remote(nbuf.at[mk], nbuf.at[mk], n_send.at[mk, 0], n_recv.at[mk], me).wait_recv()

        n_t[:, k * seq:(k + 1) * seq] = nbuf[mk].T

    peers = [lax.rem(me + 2 * d, n_stage) for d in range(1, n_stage // 2)]
    ag_copies = [remote(nbuf.at[me], nbuf.at[me], ag_send.at[d], ag_recv.at[me], p) for d, p in enumerate(peers)]
    for c, p in zip(ag_copies, peers):
        pl.when(p != last_id)(c.start)
    for i in range(e_parts):
        e_copy(i).wait()
    pl.when(core == 0)(e_more.wait)

    pair = 2 * seq
    scale = dim ** -0.5
    inv_count = 1.0 / n_tok
    log_count = math.log2(n_tok)
    lab = lab_ref[:, pl.ds(pl.multiple_of(chip * pair, pair), pair)]

    def logits(rows, size):
        e = emb[rows, :]
        parts = [dot(e[k * size // 2:(k + 1) * size // 2], n_t[...]) for k in range(2)]
        z = jnp.concatenate([(p * scale).astype(BF16) for p in parts], axis=0)
        zbuf[rows, :] = z
        return z

    def peak(z, size, top):
        best = jnp.max(z.reshape(size // 16, 16, pair), axis=0).astype(F32)
        return jnp.maximum(top, jnp.maximum(best[:8], best[8:]))

    def total(z, size, old, top, tot):
        off = top * LOG2E
        return tot * jnp.exp2(old * LOG2E - off) + jnp.sum(jnp.exp2(z.astype(F32).reshape(size // 8, 8, pair) * LOG2E - off[None]), axis=0)

    tops[0] = jnp.full((8, pair), -jnp.inf, F32)
    tops[1] = jnp.zeros((8, pair), F32)

    @pl.when(core == 0)
    def _():
        z = logits(pl.ds(base, extra), extra)
        top = peak(z, extra, tops[0])
        tops[1] = total(z, extra, tops[0], top, tops[1])
        tops[0] = top

    def logits_step(i, slot, old, top, tot):
        z = logits(pl.ds(pl.multiple_of(i * tile, 16), tile), tile)
        tot = total(z_pair[1 - slot], tile, old, top, tot)
        z_pair[slot] = z
        return top, peak(z, tile, top), tot

    z = logits(pl.ds(0, tile), tile)
    z_pair[0] = z
    state = (tops[0], peak(z, tile, tops[0]), tops[1])
    state = lax.fori_loop(0, (n_tiles - 1) // 2, lambda i, c: logits_step(2 * i + 2, 0, *logits_step(2 * i + 1, 1, *c)), state)
    if n_tiles % 2 == 0:
        state = logits_step(n_tiles - 1, 1, *state)
    old, top, tot = state
    tot = total(z_pair[(n_tiles - 1) % 2], tile, old, top, tot)
    row_top = jnp.max(top, axis=0, keepdims=True)
    row_tot = jnp.sum(tot * jnp.exp2((top - row_top) * LOG2E), axis=0, keepdims=True)
    st_send[0:8, :] = jnp.broadcast_to(row_top, (8, pair))
    st_send[8:16, :] = jnp.broadcast_to(row_tot, (8, pair))
    st_copy = remote(st_send, st_recv, st_sems.at[0], st_sems.at[1], mate)
    st_copy.start()
    st_copy.wait()
    far_top = st_recv[0:1, :]
    far_tot = st_recv[8:9, :]
    all_top = jnp.maximum(row_top, far_top)
    mine = row_tot * jnp.exp(row_top - all_top)
    other = far_tot * jnp.exp(far_top - all_top)
    lse = all_top + jnp.log(jnp.where(core == 0, mine + other, other + mine))
    my_shift = lse * LOG2E + log_count

    def grads(rows, size, first_row, picked):
        zf = zbuf[rows, :].astype(F32)
        prob = jnp.exp2(zf * LOG2E - my_shift)
        hit = lax.broadcasted_iota(jnp.int32, (size, pair), 0) == lab - (row0 + first_row)
        dz_t = jnp.where(hit, prob - inv_count, prob).astype(BF16)
        got = jnp.where(hit, zf, 0.0).reshape(size // 8, 8, pair)
        return dot_t(dz_t, emb[rows, :]), picked + jnp.sum(got, axis=0)

    tops[0] = jnp.zeros((8, pair), F32)
    dn_acc[...] = jnp.zeros_like(dn_acc)

    @pl.when(core == 0)
    def _():
        dn_acc[...], tops[0] = grads(pl.ds(base, extra), extra, base, tops[0])

    def grad_step(i, picked):
        part, picked = grads(pl.ds(pl.multiple_of(i * tile, 16), tile), tile, i * tile, picked)
        dn_acc[...] += part
        return picked

    picked = lax.fori_loop(0, n_tiles, grad_step, tops[0])
    far = pl.ds(pl.multiple_of((1 - core) * seq, seq), seq)
    near = pl.ds(pl.multiple_of(core * seq, seq), seq)
    dn_send[...] = dn_acc[far, :]
    dp_copy = remote(dn_send, dn_recv, dp_sems.at[0], dp_sems.at[1], mate)
    dp_copy.start()
    row_loss = jnp.where(core == 0, lse, 0.0) - jnp.sum(picked, axis=0, keepdims=True)
    pick = lax.broadcasted_iota(jnp.int32, (8, pair), 0)
    statall[me] = jnp.where(pick == 0, lse, jnp.where(pick == 1, row_loss, 0.0))
    sa_copies = [remote(statall.at[me], statall.at[me], sa_send.at[d - 1], sa_recv.at[me], lax.rem(me + d, n_stage)) for d in range(1, n_stage)]
    for c in sa_copies:
        c.start()
    dp_copy.wait()
    dn = ((dn_acc[near, :] + dn_recv[...]) * scale).astype(BF16)
    dn_copy = remote(dn_own, dnbuf.at[me], dn_ssem, dn_rsem.at[me], last_id)

    @pl.when(last)
    def _():
        dnbuf[last_id] = dn

    @pl.when(jnp.logical_not(last))
    def _():
        dn_own[...] = dn
        dn_copy.start()

    for p in peers:
        got = remote(nbuf.at[p], nbuf.at[p], ag_send.at[0], ag_recv.at[p], me)
        pl.when(jnp.logical_not(last))(got.wait_recv)
        pl.when(mate != last_id)(remote(nbuf.at[p], nbuf.at[p], fw_send.at[p], ag_recv.at[p], mate).start)

    near_dst = [1, 2, n_stage - 2]
    far_dst = n_stage // 2
    n_relay = (n_micro - 2) // 2

    def dx0_copies(m):
        return [remote(dxbuf.at[m], dx0buf.at[m], d_send.at[m, k], d_recv.at[m], dev) for k, dev in enumerate(near_dst + [far_dst])]

    def relay_far(j):
        m = 2 * j + jnp.where(me == 2, 0, 1)
        return remote(dx0buf.at[m], dx0buf.at[m], rf_send.at[j], d_recv.at[m], far_dst)

    def bwd(m):
        @pl.when(jnp.logical_not(last))
        def _():
            remote(gbuf.at[m], gbuf.at[m], b_send.at[m], b_recv.at[m], me).wait_recv()

        @pl.when(last)
        def _():
            @pl.when(m != last_id)
            def _():
                remote(dnbuf.at[m], dnbuf.at[m], dn_ssem, dn_rsem.at[m], me).wait_recv()

            yf = ybuf[m].astype(F32)
            inv = lax.rsqrt(jnp.mean(yf * yf, axis=-1, keepdims=True) + EPS)
            dnf = dnbuf[m].astype(F32)
            proj = jnp.mean(yf * dnf, axis=-1, keepdims=True)
            gbuf[m] = (dnf * inv - yf * (inv * inv * inv * proj)).astype(BF16)

        g = gbuf[m]
        for j in range(n_fblk):
            cols = slice(j * fblk, (j + 1) * fblk)
            dh = dot(g, down_t[:, cols]).astype(BF16).astype(F32)
            abuf[m, :, cols] = (dh * gelu_slope(abuf[m, :, cols].astype(F32))).astype(BF16)
        dxbuf[m] = (g.astype(F32) + dot(abuf[m], up_t[...])).astype(BF16)

        @pl.when(jnp.logical_not(first))
        def _():
            remote(dxbuf.at[m], gbuf.at[m], b_send.at[m], b_recv.at[m], me - 1).start()

        @pl.when(first)
        def _():
            copies = dx0_copies(m)
            for c in copies[:-1]:
                c.start()
            pl.when(m >= 2 * n_relay)(copies[-1].start)

        pltpu.make_async_copy(abuf.at[m], da_out.at[m], out_sem.at[2, m]).start()
        pltpu.make_async_copy(gbuf.at[m], g_out.at[m], out_sem.at[3, m]).start()

    def tile_copies(k, slot):
        rows = pl.ds(pl.multiple_of(k * plan.rows, plan.rows), plan.rows)
        own = pltpu.make_async_copy(obuf.at[slot], tmp_out.at[core, rows], o_sem.at[slot])
        return own, remote(obuf.at[slot], tmp_out.at[core, rows], od_send.at[k], od_recv.at[k], mate)

    def emb_tile(k):
        @pl.when(k == 0)
        def _():
            for d in range(1, n_stage):
                src = lax.rem(me + d, n_stage)
                remote(statall.at[src], statall.at[src], sa_send.at[0], sa_recv.at[src], me).wait_recv()
            for d in range(1, n_stage // 2):
                src = lax.rem(mate + 2 * d, n_stage)
                pl.when(jnp.logical_not(last))(remote(nbuf.at[src], nbuf.at[src], ag_send.at[0], ag_recv.at[src], me).wait_recv)
            token_table(row_ref, cut_ref, meta)
            for m in range(n_micro):
                n_all_t[:, m * seq:(m + 1) * seq] = nbuf[m].T
            for c in range(n_stage // 2):
                shift[:, c * pair:(c + 1) * pair] = statall[2 * c, 0:1, :] * LOG2E + log_count

        slot = lax.rem(k, 2)

        @pl.when(k >= 2)
        def _():
            own, far_copy = tile_copies(k - 2, slot)
            own.wait()
            far_copy.wait_send()

        rows = pl.ds(pl.multiple_of(k * plan.rows, plan.rows), plan.rows)
        logit_grad(emb[rows, :], n_all_t, shift, lab_ref, row0 + k * plan.rows, inv_count, scale, dz)
        obuf[slot] = dot(dz[...], nbuf[...].reshape(n_tok, dim)) * scale
        own, far_copy = tile_copies(k, slot)
        own.start()
        far_copy.start()

    relays = (me == 2) | (me == n_stage - 2)
    before = sum(jnp.where(me == s, plan.before[s], 0) for s in range(n_stage))

    def work(i, carry):
        chunk = (i >= before) & (i < before + n_micro)
        pl.when(chunk)(lambda: bwd(i - before))
        pl.when(jnp.logical_not(chunk))(lambda: emb_tile(jnp.where(i < before, i, i - n_micro)))
        j = i - n_micro - jnp.where(me == 2, before, plan.tiles - n_relay)

        @pl.when(relays & (j >= 0) & (j < n_relay))
        def _():
            copy = relay_far(j)
            copy.wait_recv()
            copy.start()

        return carry

    lax.fori_loop(0, plan.tiles + n_micro, work, 0)
    outs = [pltpu.make_async_copy(nbuf, n_out, out_sem.at[5, 0]), pltpu.make_async_copy(statall, stat_out, out_sem.at[5, 1]), pltpu.make_async_copy(meta, meta_out, out_sem.at[5, 2])]
    for c in outs:
        c.start()

    def relay(m, carry):
        @pl.when(jnp.logical_not(first))
        def _():
            relayed = relays & (m < 2 * n_relay) & (lax.rem(m, 2) == jnp.where(me == 2, 0, 1))
            pl.when(jnp.logical_not(relayed))(remote(dx0buf.at[m], dx0buf.at[m], r_send.at[m], d_recv.at[m], me).wait_recv)

            @pl.when(core == 0)
            def _():
                remote(dx0buf.at[m], dx0buf.at[m], r_send.at[m], d_recv.at[m], mate).start()

            pltpu.make_async_copy(dx0buf.at[m], dx0_out.at[m], out_sem.at[4, m]).start()

        @pl.when(first)
        def _():
            pltpu.make_async_copy(dxbuf.at[m], dx0_out.at[m], out_sem.at[4, m]).start()

        return carry

    lax.fori_loop(0, n_micro, relay, 0)

    for k in range(max(plan.tiles - 2, 0), plan.tiles):
        own, far_copy = tile_copies(k, k % 2)
        own.wait()
        far_copy.wait_send()
    for k in range(plan.tiles):
        rows = pl.ds(k * plan.rows, plan.rows)
        remote(obuf.at[0], tmp_out.at[1 - core, rows], od_send.at[k], od_recv.at[k], me).wait_recv()
    for j in range(n_relay):
        pl.when(relays)(relay_far(j).wait_send)
    for c in sa_copies:
        c.wait_send()
    for c, p in zip(ag_copies, peers):
        pl.when(p != last_id)(c.wait_send)
        pl.when(mate != last_id)(remote(nbuf.at[p], nbuf.at[p], fw_send.at[p], ag_recv.at[p], mate).wait_send)

    @pl.when(jnp.logical_not(last))
    def _():
        dn_copy.wait_send()

    @pl.when(jnp.logical_not(first) & (me + 2 < n_micro))
    def _():
        x_copy(0).wait_send()

        @pl.when(me < 2)
        def _():
            x_copy(1).wait_send()

    def drain(m, carry):
        @pl.when(jnp.logical_not(last))
        def _():
            remote(ybuf.at[m], xbuf.at[m], f_send.at[m], f_recv.at[m], me).wait_send()

        @pl.when(last)
        def _():
            copies = n_copies(m)
            copies[0].wait_send()

            @pl.when(m // 2 != last_id // 2)
            def _():
                copies[1].wait_send()

        @pl.when(jnp.logical_not(first))
        def _():
            remote(dxbuf.at[m], gbuf.at[m], b_send.at[m], b_recv.at[m], me).wait_send()

            @pl.when(core == 0)
            def _():
                remote(dx0buf.at[m], dx0buf.at[m], r_send.at[m], d_recv.at[m], me).wait_send()

        @pl.when(first)
        def _():
            copies = dx0_copies(m)
            for c in copies[:-1]:
                c.wait_send()
            pl.when(m >= 2 * n_relay)(copies[-1].wait_send)

        pltpu.make_async_copy(hbuf.at[m], hid_out.at[m], out_sem.at[0, m]).wait()
        pltpu.make_async_copy(xbuf.at[m], xs_out.at[m], out_sem.at[1, m]).wait()
        pltpu.make_async_copy(abuf.at[m], da_out.at[m], out_sem.at[2, m]).wait()
        pltpu.make_async_copy(gbuf.at[m], g_out.at[m], out_sem.at[3, m]).wait()
        pltpu.make_async_copy(dx0buf.at[m], dx0_out.at[m], out_sem.at[4, m]).wait()
        return carry

    lax.fori_loop(0, n_micro, drain, 0)
    for c in outs:
        c.wait()


class Plan:
    def __init__(self, vocab, n_stage):
        units = vocab // LANES
        self.base = units // 2 * LANES
        self.extra = vocab - 2 * self.base
        self.head_tile = next(t for t in (1600, 1536, 1280, 1024, 768, 640, 512, 256, 128) if self.base % t == 0)
        self.rows = 1024
        self.tiles = 9
        self.steps = 12
        arrive, self.before = 0.0, [0] * n_stage
        for s in reversed(range(n_stage)):
            self.before[s] = min(max(int((arrive - 4.5) / 2.6 + 0.3), 0), self.tiles)
            arrive += 2.3 if s % 2 else 4.6
        early = self.tiles * self.rows
        self.half_steps = self.steps // 2
        self.copy_rows = early // self.half_steps
        mid = self.base + self.extra
        self.spans = [(early, mid), (mid + early, vocab)]
        longest = max(b - a for a, b in self.spans)
        self.calc_rows = -(-longest // (16 * self.half_steps)) * 16
        self.over = [self.half_steps * self.calc_rows - (b - a) for a, b in self.spans]
        self.head = max(self.over)

    def calc_start(self, s):
        h, i = s // self.half_steps, s % self.half_steps
        return min(self.spans[h][0] + i * self.calc_rows, self.spans[h][1] - self.calc_rows)

    def copy_start(self, s):
        h, i = s // self.half_steps, s % self.half_steps
        return h * (self.base + self.extra) + i * self.copy_rows


def run_pipe(x0, emb, w_up, w_down, labels, tokens, cuts, n_stage, plan):
    n_micro, seq = labels.shape
    dim, ffn = w_up.shape
    n_tok = n_micro * seq
    base = plan.base
    e_parts = next(k for k in (10, 8, 5, 4, 2, 1) if base % (16 * k) == 0)
    any_spec = pl.BlockSpec(memory_space=pl.ANY)
    act = (n_micro, seq, dim)
    wide = (n_micro, seq, ffn)
    dma = pltpu.SemaphoreType.DMA
    vm = pltpu.VMEM
    pair = 2 * seq
    return pl.pallas_call(
        functools.partial(pipe_kernel, n_stage, plan),
        out_shape=[
            jax.ShapeDtypeStruct(act, BF16), jax.ShapeDtypeStruct(act, BF16), jax.ShapeDtypeStruct(wide, BF16),
            jax.ShapeDtypeStruct(wide, BF16), jax.ShapeDtypeStruct(act, BF16), jax.ShapeDtypeStruct(act, BF16),
            jax.ShapeDtypeStruct((n_stage, 8, pair), F32), jax.ShapeDtypeStruct((2, plan.tiles * plan.rows, dim), F32),
            jax.ShapeDtypeStruct((3 * n_tok // LANES, LANES), jnp.int32),
        ],
        in_specs=[any_spec] * 4 + [pl.BlockSpec(memory_space=pltpu.VMEM)] * 3,
        out_specs=[any_spec] * 9,
        scratch_shapes=[
            vm(act, BF16), vm(act, BF16), vm(wide, BF16), vm(wide, BF16), vm(act, BF16), vm(act, BF16), vm(act, BF16), vm(act, BF16), vm(act, BF16),
            vm((dim, ffn), BF16), vm((ffn, dim), BF16), vm((ffn, dim), BF16), vm((dim, ffn), BF16),
            vm((base + plan.extra, dim), BF16), vm((base + plan.extra, pair), BF16), vm((dim, pair), BF16), vm((pair, dim), F32),
            vm((seq, dim), F32), vm((seq, dim), F32), vm((seq, dim), BF16), vm((16, pair), F32), vm((16, pair), F32), vm((n_stage, 8, pair), F32),
            vm((2, 8, pair), F32), vm((dim, n_tok), BF16), vm((1, n_tok), F32), vm((plan.rows, n_tok), BF16), vm((2, plan.rows, dim), F32),
            vm((2, plan.head_tile, pair), BF16), vm((3 * n_tok // LANES, LANES), jnp.int32),
            dma((2,)), dma((e_parts + 1,)), dma((n_micro,)), dma((n_micro,)), dma((n_micro,)), dma((n_micro, 2)), dma((n_micro,)),
            dma((n_stage,)), dma((n_stage,)), dma((n_stage,)),
            dma((2,)), dma((2,)), dma, dma((n_stage,)), dma((n_stage,)), dma((n_stage,)),
            dma((n_micro,)), dma((n_micro,)), dma((n_micro, 4)), dma((n_micro,)), dma((n_micro,)), dma((n_micro,)), dma((6, n_micro)),
            dma((2,)), dma((2,)), dma((plan.tiles,)), dma((plan.tiles,)),
        ],
        compiler_params=pltpu.CompilerParams(collective_id=0, has_side_effects=True, vmem_limit_bytes=67_000_000),
        cost_estimate=pl.CostEstimate(flops=60 * 10**9, bytes_accessed=100 * 10**6, transcendentals=0),
        name="pipe",
    )(x0, emb, w_up, w_down, labels.reshape(1, n_tok), tokens.reshape(1, n_tok), cuts)


def fin_kernel(n_stage, n_tok, plan, ids_ref, emb_hbm, tmp_hbm, n_hbm, stat_ref, lab_ref, meta_ref, dx0_hbm, xs_hbm, hid_hbm, da_hbm, g_hbm,
               out_hbm, loss_ref, gup_hbm, gdown_hbm,
               n_all, dx0, xs, hid, da, g, n_t, x_t, dx0s, dz, shift, e_in, c_out, cp, gup, gdown,
               ld_sem, e_sem, t_sem, co_sem, po_sem, gu_sem, gd_sem):
    dim = n_all.shape[1]
    ffn = da.shape[1]
    scale = dim ** -0.5
    inv_count = 1.0 / n_tok
    steps, half, crows, prows = plan.steps, plan.half_steps, plan.calc_rows, plan.copy_rows
    mid = plan.base + plan.extra
    wblk = 256
    n_wblk = ffn // wblk

    def calc_start(s):
        h, i = s // half, lax.rem(s, half)
        lo = jnp.where(h == 0, plan.spans[0][0], plan.spans[1][0]) + i * crows
        return pl.multiple_of(jnp.minimum(lo, jnp.where(h == 0, plan.spans[0][1], plan.spans[1][1]) - crows), 16)

    def copy_start(s):
        return pl.multiple_of(s // half * mid + lax.rem(s, half) * prows, 16)

    def e_copy(s):
        return pltpu.make_async_copy(emb_hbm.at[pl.ds(calc_start(s), crows)], e_in.at[lax.rem(s, 2)], e_sem.at[lax.rem(s, 2)])

    def t_copy(s):
        return pltpu.make_async_copy(tmp_hbm.at[pl.ds(pl.multiple_of(s * prows, 16), prows)], cp.at[lax.rem(s, 3)], t_sem.at[lax.rem(s, 3)])

    def p_out(s):
        return pltpu.make_async_copy(cp.at[lax.rem(s, 3)], out_hbm.at[pl.ds(copy_start(s), prows)], po_sem.at[lax.rem(s, 3)])

    def c_outs(s):
        slot = lax.rem(s, 2)
        start = calc_start(s)
        return (
            pltpu.make_async_copy(c_out.at[slot, pl.ds(plan.head, crows - plan.head)], out_hbm.at[pl.ds(start + plan.head, crows - plan.head)], co_sem.at[slot, 0]),
            pltpu.make_async_copy(c_out.at[slot, pl.ds(0, plan.head)], out_hbm.at[pl.ds(start, plan.head)], co_sem.at[slot, 1]),
        )

    def has_head(s):
        skip = False
        for h in range(2):
            if plan.over[h] > 0:
                skip = skip | (s == h * half + half - 1)
        return jnp.logical_not(skip)

    def c_start(s):
        a, b = c_outs(s)
        a.start()
        if plan.head:
            pl.when(has_head(s))(b.start)

    def c_wait(s):
        a, b = c_outs(s)
        a.wait()
        if plan.head:
            pl.when(has_head(s))(b.wait)

    loads = [pltpu.make_async_copy(s, d, ld_sem.at[i]) for i, (s, d) in enumerate(((n_hbm, n_all), (dx0_hbm, dx0), (xs_hbm, xs), (da_hbm, da), (hid_hbm, hid), (g_hbm, g)))]
    loads[0].start()
    loads[1].start()
    e_copy(0).start()
    t_copy(0).start()
    for c in loads[2:]:
        c.start()
    pair = stat_ref.shape[2]
    loss = jnp.zeros((1, pair), F32)
    for d in range(n_stage):
        if d % 2 == 0:
            shift[:, (d // 2) * pair:(d // 2 + 1) * pair] = stat_ref[d, 0:1, :] * LOG2E + math.log2(n_tok)
        loss = loss + stat_ref[d, 1:2, :]
    loss_ref[0] = jnp.sum(loss) * inv_count
    loads[0].wait()
    n_t[...] = n_all[...].T
    loads[1].wait()
    dense = jnp.concatenate([meta_ref[g:g + 1, :] for g in range(n_tok // LANES)], axis=1)
    order = lax.broadcasted_iota(jnp.int32, (n_tok, n_tok), 0) == dense
    dx0s[...] = dot(jnp.where(order, 1.0, 0.0).astype(BF16), dx0[...])

    def add_rows(k, start, ref):
        lo, hi = ids_ref[2 * n_tok + k], ids_ref[2 * n_tok + k + 1]
        wide = 8

        def some(p, width):
            at = [pl.ds(ids_ref[n_tok + p + u] - start, 1) for u in range(width)]
            new = [ref[at[u], :] + dx0s[pl.ds(p + u, 1), :] for u in range(width)]
            for u in range(width):
                ref[at[u], :] = new[u]

        def group(g, carry):
            some(lo + g * wide, wide)
            return carry

        def single(p, carry):
            some(p, 1)
            return carry

        n_grp = (hi - lo) // wide
        lax.fori_loop(0, n_grp, group, 0)
        lax.fori_loop(lo + n_grp * wide, hi, single, 0)

    def step(s, carry):
        e_copy(s).wait()
        t_copy(s).wait()

        @pl.when(s + 1 < steps)
        def _():
            e_copy(s + 1).start()

            @pl.when(s >= 2)
            def _():
                p_out(s - 2).wait()

            t_copy(s + 1).start()

        @pl.when(s >= 2)
        def _():
            c_wait(s - 2)

        slot = lax.rem(s, 2)
        pslot = lax.rem(s, 3)
        start = calc_start(s)
        add_rows(4 * s + 2, copy_start(s), cp.at[pslot])
        p_out(s).start()
        logit_grad(e_in[slot], n_t, shift, lab_ref, start, inv_count, scale, dz)
        c_out[slot] = dot(dz[...], n_all[...]) * scale
        add_rows(4 * s, start, c_out.at[slot])
        c_start(s)

        w = s - 2

        @pl.when(w == 0)
        def _():
            for c in loads[2:]:
                c.wait()
            x_t[...] = xs[...].T

        @pl.when((w >= 0) & (w < n_wblk))
        def _():
            cols = pl.ds(pl.multiple_of(w * wblk, wblk), wblk)
            wslot = lax.rem(w, 2)
            up_copy, down_copy = w_outs(w)

            @pl.when(w >= 2)
            def _():
                for c in w_outs(w - 2):
                    c.wait()

            gup[wslot] = dot(x_t[...], da[:, cols])
            gdown[wslot] = dot_t(hid[:, cols], g[...])
            up_copy.start()
            down_copy.start()

        return carry

    def w_outs(w):
        cols = pl.ds(pl.multiple_of(w * wblk, wblk), wblk)
        wslot = lax.rem(w, 2)
        return (pltpu.make_async_copy(gup.at[wslot], gup_hbm.at[:, cols], gu_sem.at[wslot]), pltpu.make_async_copy(gdown.at[wslot], gdown_hbm.at[cols], gd_sem.at[wslot]))

    lax.fori_loop(0, steps, step, 0)
    for w in range(n_wblk - 2, n_wblk):
        for c in w_outs(w):
            c.wait()
    for s in range(steps - 2, steps):
        c_wait(s)
    for s in range(steps - 3, steps):
        p_out(s).wait()


def run_fin(emb, tmp, n_all, stats, labels, meta, dx0, xs, hid, da, g, n_stage, plan):
    vocab, dim = emb.shape
    n_tok, ffn = hid.shape
    vm = pltpu.VMEM
    dma = pltpu.SemaphoreType.DMA
    any_spec = pl.BlockSpec(memory_space=pl.ANY)
    vspec = pl.BlockSpec(memory_space=pltpu.VMEM)
    smem = pl.BlockSpec(memory_space=pltpu.SMEM)
    wblk = 256
    return pl.pallas_call(
        functools.partial(fin_kernel, n_stage, n_tok, plan),
        out_shape=[jax.ShapeDtypeStruct((vocab, dim), F32), jax.ShapeDtypeStruct((1,), F32), jax.ShapeDtypeStruct((dim, ffn), F32), jax.ShapeDtypeStruct((ffn, dim), F32)],
        in_specs=[smem, any_spec, any_spec, any_spec, vspec, vspec, vspec] + [any_spec] * 5,
        out_specs=[any_spec, smem, any_spec, any_spec],
        scratch_shapes=[
            vm((n_tok, dim), BF16), vm((n_tok, dim), BF16), vm((n_tok, dim), BF16), vm((n_tok, ffn), BF16), vm((n_tok, ffn), BF16), vm((n_tok, dim), BF16),
            vm((dim, n_tok), BF16), vm((dim, n_tok), BF16), vm((n_tok, dim), F32), vm((plan.calc_rows, n_tok), BF16), vm((1, n_tok), F32),
            vm((2, plan.calc_rows, dim), BF16), vm((2, plan.calc_rows, dim), F32), vm((3, plan.copy_rows, dim), F32),
            vm((2, dim, wblk), F32), vm((2, wblk, dim), F32),
            dma((6,)), dma((2,)), dma((3,)), dma((2, 2)), dma((3,)), dma((2,)), dma((2,)),
        ],
        compiler_params=pltpu.CompilerParams(vmem_limit_bytes=67_000_000),
        cost_estimate=pl.CostEstimate(flops=2 * n_tok * vocab * dim, bytes_accessed=5 * vocab * dim, transcendentals=0),
        name="fin",
    )(meta.reshape(-1), emb, tmp, n_all, stats, labels.reshape(1, n_tok), meta, dx0, xs, hid, da, g)


def solution(mesh):
    n_stage = mesh.shape["stage"]

    def device_fn(tokens, labels, emb, w_up, w_down):
        n_micro, seq = tokens.shape
        vocab, dim = emb.shape
        w_up, w_down = w_up[0], w_down[0]
        n_tok = n_micro * seq
        plan = Plan(vocab, n_stage)
        cuts = []
        for s in range(plan.steps):
            for lo, rows in ((plan.calc_start(s), plan.calc_rows), (plan.copy_start(s), plan.copy_rows)):
                cuts += [lo, lo + rows]
        cuts = jnp.array(cuts + [vocab] * (LANES - len(cuts)), jnp.int32).reshape(1, LANES)
        x0 = run_gather(tokens, emb)
        n_all, xs, hid, da, g, dx0, stats, tmp, meta = run_pipe(x0, emb, w_up, w_down, labels, tokens, cuts, n_stage, plan)
        flat = lambda p: p.reshape(n_tok, -1)
        grad_emb, loss, grad_up, grad_down = run_fin(
            emb, tmp.reshape(-1, dim), flat(n_all), stats, labels, meta, flat(dx0), flat(xs), flat(hid), flat(da), flat(g), n_stage, plan
        )
        return loss, grad_up[None], grad_down[None], grad_emb

    return jax.shard_map(device_fn, mesh=mesh, in_specs=(P("dp", None), P("dp", None), P(None, None), P("stage", None, None), P("stage", None, None)), out_specs=(P("dp"), P(("dp", "stage"), None, None), P(("dp", "stage"), None, None), P("dp", None)), check_vma=False)
```

```python
import functools
import math

import jax
import jax.numpy as jnp
from jax import lax
from jax.experimental import pallas as pl
from jax.experimental.pallas import tpu as pltpu
from jax.sharding import PartitionSpec as P


MESH = pl.DeviceIdType.MESH
LOG2E = math.log2(math.e)
LN2 = math.log(2.0)
GELU_C = math.sqrt(2.0 / math.pi)
GELU_K = 0.044715
EPS = 1e-6
LANES = 128
F32 = jnp.float32
BF16 = jnp.bfloat16


def gelu_fwd(a):
    return 0.5 * a * (1.0 + jnp.tanh(GELU_C * (a + GELU_K * (a * a * a))))


def gelu_slope(a):
    a2 = a * a
    t = jnp.tanh(GELU_C * (a + GELU_K * (a2 * a)))
    return 0.5 * (1.0 + t) + (0.5 * a) * (1.0 - t * t) * (GELU_C + (3.0 * GELU_C * GELU_K) * a2)


def dot(x, y):
    return jnp.dot(x, y, preferred_element_type=F32)


def dot_t(x, y):
    return lax.dot_general(x, y, (((0,), (0,)), ((), ())), preferred_element_type=F32)


def remote(src, dst, send_sem, recv_sem, dev):
    return pltpu.make_async_remote_copy(src_ref=src, dst_ref=dst, send_sem=send_sem, recv_sem=recv_sem, device_id={"stage": dev}, device_id_type=MESH)


def column(row):
    return jnp.broadcast_to(row, (LANES, LANES)).T


def gather_kernel(ids_ref, tok_ref, emb_hbm, x0_hbm, tiles, picked, sem, out_sem):
    n_micro, seq = tok_ref.shape
    me = lax.axis_index("stage")
    group = tiles.shape[1] // seq
    slots = tiles.shape[0]
    owners = [head_chunk(me, k, n_micro) for k in range(slots)]

    def fetch(k):
        def one(i, carry):
            t = ids_ref[owners[k] * seq + i]
            start = pl.multiple_of(t // group * group, group)
            pltpu.make_async_copy(emb_hbm.at[pl.ds(start, group)], tiles.at[k, pl.ds(pl.multiple_of(i * group, group), group)], sem.at[k]).start()
            return carry

        lax.fori_loop(0, seq, one, 0, unroll=8)

    def select(k):
        sub = lax.broadcasted_iota(jnp.int32, (LANES, LANES), 0)
        lane = lax.broadcasted_iota(jnp.int32, (LANES, LANES), 1)
        tok = column(tok_ref[pl.ds(owners[k], 1), :].astype(F32)).astype(jnp.int32)
        want = sub * group + (tok - tok // group * group)
        hot = jnp.concatenate([jnp.where(lane + b * LANES == want, 1.0, 0.0).astype(BF16) for b in range(seq * group // LANES)], axis=1)
        pltpu.make_async_copy(emb_hbm.at[pl.ds(0, seq * group)], tiles.at[k], sem.at[k]).wait()
        picked[k] = dot(hot, tiles[k]).astype(BF16)
        pltpu.make_async_copy(picked.at[k], x0_hbm.at[k], out_sem.at[k]).start()

    def finish(k):
        pltpu.make_async_copy(picked.at[k], x0_hbm.at[k], out_sem.at[k]).wait()

    for work in (fetch, select, finish):
        work(0)
        for k in range(1, slots):
            pl.when(me < slots)(functools.partial(work, k))


def head_chunk(dev, k, n_micro):
    return jnp.minimum(jnp.where(dev < 2, 2 * dev + k, dev + 2), n_micro - 1)


def run_gather(tokens, emb):
    n_micro, seq = tokens.shape
    dim = emb.shape[1]
    group = 16
    return pl.pallas_call(
        gather_kernel,
        out_shape=jax.ShapeDtypeStruct((2, seq, dim), BF16),
        in_specs=[pl.BlockSpec(memory_space=pltpu.SMEM), pl.BlockSpec(memory_space=pltpu.VMEM), pl.BlockSpec(memory_space=pl.ANY)],
        out_specs=pl.BlockSpec(memory_space=pl.ANY),
        scratch_shapes=[pltpu.VMEM((2, seq * group, dim), BF16), pltpu.VMEM((2, seq, dim), BF16), pltpu.SemaphoreType.DMA((2,)), pltpu.SemaphoreType.DMA((2,))],
        cost_estimate=pl.CostEstimate(flops=10**9, bytes_accessed=2 * seq * group * dim * 2, transcendentals=0),
        name="gather",
    )(tokens.reshape(n_micro * seq), tokens, emb)


def token_table(row_ref, cut_ref, meta):
    n_tok = row_ref.shape[1]
    n_grp = n_tok // LANES
    lane = lax.broadcasted_iota(jnp.int32, (LANES, LANES), 1).astype(F32)
    sub = lax.broadcasted_iota(jnp.int32, (LANES, LANES), 0)
    row = lambda g: row_ref[:, g * LANES:(g + 1) * LANES].astype(F32)
    zero = jnp.zeros((LANES, LANES), F32)
    fold = lambda acc: jnp.sum(acc, axis=0, keepdims=True)
    cols = [column(row(c)) for c in range(n_grp)]
    firsts = []
    for g in range(n_grp):
        acc = zero
        for c in range(g + 1):
            same = cols[c] == row(g)
            if c == g:
                same = same & (sub < lane.astype(jnp.int32))
            acc = acc + jnp.where(same, 1.0, 0.0)
        firsts.append(column(jnp.where(fold(acc) == 0.0, 1.0, 0.0)))
    ranks = []
    for g in range(n_grp):
        acc = zero
        for c in range(n_grp):
            acc = acc + jnp.where(cols[c] < row(g), firsts[c], 0.0)
        ranks.append(fold(acc))
        meta[g:g + 1, :] = ranks[g].astype(jnp.int32)
    rank_cols = [column(r) for r in ranks]
    for g in range(n_grp):
        acc = zero
        for c in range(n_grp):
            acc = acc + jnp.where(rank_cols[c] == lane + g * LANES, firsts[c] * cols[c], 0.0)
        meta[n_grp + g:n_grp + g + 1, :] = fold(acc).astype(jnp.int32)
    cut = cut_ref[...].astype(F32)
    acc = zero
    for c in range(n_grp):
        acc = acc + jnp.where(cols[c] < cut, firsts[c], 0.0)
    meta[2 * n_grp:3 * n_grp, :] = jnp.broadcast_to(fold(acc), (n_grp, LANES)).astype(jnp.int32)


def logit_grad(e, n_t, shift, lab, first_id, inv_count, scale, dz, own=None, known=None):
    rows = e.shape[0]
    n_tok = n_t.shape[1]
    blk = 256
    n_blk = n_tok // blk
    vid = lax.broadcasted_iota(jnp.int32, (rows, blk), 0)
    for j in range(n_blk):
        cols = slice(j * blk, (j + 1) * blk) if own is None else pl.ds(pl.multiple_of(lax.rem(own + j, n_blk) * blk, blk), blk)
        if own is not None and j == 0:
            z = known.astype(F32)
        else:
            z = (dot(e, n_t[:, cols]) * scale).astype(BF16).astype(F32)
        prob = jnp.exp2(z * LOG2E - shift[:, cols])
        dz[:, cols] = jnp.where(vid == lab[:, cols] - first_id, prob - inv_count, prob).astype(BF16)


def pipe_kernel(n_stage, plan, x0_hbm, emb_hbm, up_hbm, down_hbm, lab_ref, row_ref, cut_ref,
                n_out, xs_out, hid_out, da_out, g_out, dx0_out, stat_out, tmp_out, meta_out,
                xbuf, ybuf, abuf, hbuf, nbuf, gbuf, dxbuf, dx0buf, dnbuf, up, down, up_t, down_t,
                emb, zbuf, n_t, dn_acc, dn_send, dn_recv, dn_own, st_send, st_recv, statall, tops, n_all_t, shift, dz, obuf, z_pair, meta,
                w_sem, e_sem, x_sem, f_send, f_recv, n_send, n_recv, nf_send, ag_send, ag_recv, fw_send,
                st_sems, dp_sems, dn_ssem, dn_rsem, sa_send, sa_recv, b_send, b_recv, d_send, d_recv, r_send, rf_send, out_sem, x_send, o_sem, od_send, od_recv):
    n_micro, seq, dim = xbuf.shape
    n_tok = n_micro * seq
    ffn = up.shape[1]
    vocab = emb_hbm.shape[0]
    me = lax.axis_index("stage")
    core = lax.rem(me, 2)
    chip = me // 2
    mate = me + 1 - 2 * core
    last_id = n_stage - 1
    first = me == 0
    last = me == last_id
    fblk = 512
    n_fblk = ffn // fblk
    base, extra, tile = plan.base, plan.extra, plan.head_tile
    row0 = core * (base + extra)
    n_tiles = base // tile

    barrier = pltpu.get_barrier_semaphore()
    for d in range(1, n_stage):
        pl.semaphore_signal(barrier, inc=1, device_id={"stage": lax.rem(me + d, n_stage)}, device_id_type=MESH)
    w_copy = [pltpu.make_async_copy(up_hbm, up, w_sem.at[0]), pltpu.make_async_copy(down_hbm, down, w_sem.at[1])]
    for c in w_copy:
        c.start()
    x_slots = x0_hbm.shape[0]
    x_mine = [head_chunk(me, k, n_micro) for k in range(x_slots)]

    @pl.when(first)
    def _():
        for k in range(x_slots):
            pltpu.make_async_copy(x0_hbm.at[k], xbuf.at[k], x_sem.at[k]).start()

    e_parts = e_sem.shape[0] - 1
    e_step = base // e_parts

    def e_copy(i):
        src = emb_hbm.at[pl.ds(pl.multiple_of(row0 + i * e_step, 16), e_step)]
        return pltpu.make_async_copy(src, emb.at[pl.ds(i * e_step, e_step)], e_sem.at[i])

    e_more = pltpu.make_async_copy(emb_hbm.at[pl.ds(base, extra)], emb.at[pl.ds(base, extra)], e_sem.at[e_parts])
    with jax.named_scope("entry"):
        pl.semaphore_wait(barrier, n_stage - 1)

    def x_copy(k):
        return remote(x0_hbm.at[k], xbuf.at[x_mine[k]], x_send.at[k], f_recv.at[x_mine[k]], 0)

    @pl.when(jnp.logical_not(first) & (me + 2 < n_micro))
    def _():
        x_copy(0).start()

        @pl.when(me < 2)
        def _():
            x_copy(1).start()

    with jax.named_scope("w_wait"):
        for c in w_copy:
            c.wait()
        for i in range(e_parts):
            e_copy(i).start()
        pl.when(core == 0)(e_more.start)

    def transpose_weights():
        for j in range(n_fblk):
            up_t[j * fblk:(j + 1) * fblk, :] = up[:, j * fblk:(j + 1) * fblk].T
            down_t[:, j * fblk:(j + 1) * fblk] = down[j * fblk:(j + 1) * fblk, :].T

    @pl.when(chip >= n_stage // 4)
    def _():
        transpose_weights()

    def n_copy(m):
        return remote(nbuf.at[m], nbuf.at[m], n_send.at[m], n_recv.at[m], jnp.where(m == last_id, last_id - 1, m))

    def fwd(m, carry):
        local = first & (m < x_slots)

        with jax.named_scope("fwd_wait"):
            @pl.when(local)
            def _():
                pltpu.make_async_copy(x0_hbm.at[m], xbuf.at[m], x_sem.at[m]).wait()

            @pl.when(jnp.logical_not(local))
            def _():
                remote(xbuf.at[m], xbuf.at[m], f_send.at[m], f_recv.at[m], me).wait_recv()

        with jax.named_scope("fwd_comp"):
            x = xbuf[m]
            for j in range(n_fblk):
                cols = slice(j * fblk, (j + 1) * fblk)
                a = dot(x, up[:, cols]).astype(BF16)
                abuf[m, :, cols] = a
                hbuf[m, :, cols] = gelu_fwd(a.astype(F32)).astype(BF16)
            y = (x.astype(F32) + dot(hbuf[m], down[...])).astype(BF16)
            ybuf[m] = y

        @pl.when(jnp.logical_not(last))
        def _():
            remote(ybuf.at[m], xbuf.at[m], f_send.at[m], f_recv.at[m], me + 1).start()

        @pl.when(last)
        def _():
            yf = y.astype(F32)
            inv = lax.rsqrt(jnp.mean(yf * yf, axis=-1, keepdims=True) + EPS)
            nbuf[m] = (yf * inv).astype(BF16)
            n_copy(m).start()

        pltpu.make_async_copy(hbuf.at[m], hid_out.at[m], out_sem.at[0, m]).start()
        pltpu.make_async_copy(xbuf.at[m], xs_out.at[m], out_sem.at[1, m]).start()
        return carry

    lax.fori_loop(0, n_micro, fwd, 0)

    @pl.when(chip < n_stage // 4)
    def _():
        transpose_weights()

    n_forward = remote(nbuf.at[me], nbuf.at[me], nf_send, n_recv.at[me], mate)
    with jax.named_scope("n_wait"):

        @pl.when(jnp.logical_not(last))
        def _():
            remote(nbuf.at[me], nbuf.at[me], n_send.at[me], n_recv.at[me], me).wait_recv()
            pl.when(mate != last_id)(n_forward.start)
            remote(nbuf.at[mate], nbuf.at[mate], n_send.at[mate], n_recv.at[mate], me).wait_recv()

        for k in range(2):
            n_t[:, k * seq:(k + 1) * seq] = nbuf[2 * chip + k].T

    peers = [lax.rem(me + 2 * d, n_stage) for d in range(1, n_stage // 2)]
    ag_copies = [remote(nbuf.at[me], nbuf.at[me], ag_send.at[d], ag_recv.at[me], p) for d, p in enumerate(peers)]
    for c, p in zip(ag_copies, peers):
        pl.when(p != last_id)(c.start)
    with jax.named_scope("e_wait"):
        for i in range(e_parts):
            e_copy(i).wait()
        pl.when(core == 0)(e_more.wait)

    pair = 2 * seq
    scale = dim ** -0.5
    inv_count = 1.0 / n_tok
    log_count = math.log2(n_tok)
    lab = lab_ref[:, pl.ds(pl.multiple_of(chip * pair, pair), pair)]

    def logits(rows, size):
        e = emb[rows, :]
        parts = [dot(e[k * size // 2:(k + 1) * size // 2], n_t[...]) for k in range(2)]
        z = jnp.concatenate([(p * scale).astype(BF16) for p in parts], axis=0)
        zbuf[rows, :] = z
        return z

    def peak(z, size, top):
        best = jnp.max(z.reshape(size // 16, 16, pair), axis=0).astype(F32)
        return jnp.maximum(top, jnp.maximum(best[:8], best[8:]))

    def total(z, size, old, top, tot):
        off = top * LOG2E
        return tot * jnp.exp2(old * LOG2E - off) + jnp.sum(jnp.exp2(z.astype(F32).reshape(size // 8, 8, pair) * LOG2E - off[None]), axis=0)

    tops[0] = jnp.full((8, pair), -jnp.inf, F32)
    tops[1] = jnp.zeros((8, pair), F32)

    @pl.when(core == 0)
    def _():
        z = logits(pl.ds(base, extra), extra)
        top = peak(z, extra, tops[0])
        tops[1] = total(z, extra, tops[0], top, tops[1])
        tops[0] = top

    def logits_step(i, slot, old, top, tot):
        z = logits(pl.ds(pl.multiple_of(i * tile, 16), tile), tile)
        tot = total(z_pair[1 - slot], tile, old, top, tot)
        z_pair[slot] = z
        return top, peak(z, tile, top), tot

    with jax.named_scope("logits"):
        z = logits(pl.ds(0, tile), tile)
        z_pair[0] = z
        state = (tops[0], peak(z, tile, tops[0]), tops[1])
        state = lax.fori_loop(0, (n_tiles - 1) // 2, lambda i, c: logits_step(2 * i + 2, 0, *logits_step(2 * i + 1, 1, *c)), state)
        if n_tiles % 2 == 0:
            state = logits_step(n_tiles - 1, 1, *state)
        old, top, tot = state
        tot = total(z_pair[(n_tiles - 1) % 2], tile, old, top, tot)
    row_top = jnp.max(top, axis=0, keepdims=True)
    row_tot = jnp.sum(tot * jnp.exp2((top - row_top) * LOG2E), axis=0, keepdims=True)
    st_send[0:8, :] = jnp.broadcast_to(row_top, (8, pair))
    st_send[8:16, :] = jnp.broadcast_to(row_tot, (8, pair))
    st_copy = remote(st_send, st_recv, st_sems.at[0], st_sems.at[1], mate)
    with jax.named_scope("stat_x"):
        st_copy.start()
        st_copy.wait()
    far_top = st_recv[0:1, :]
    far_tot = st_recv[8:9, :]
    all_top = jnp.maximum(row_top, far_top)
    mine = row_tot * jnp.exp(row_top - all_top)
    other = far_tot * jnp.exp(far_top - all_top)
    lse = all_top + jnp.log(jnp.where(core == 0, mine + other, other + mine))
    my_shift = lse * LOG2E + log_count

    def grads(rows, size, first_row, picked):
        zf = zbuf[rows, :].astype(F32)
        prob = jnp.exp2(zf * LOG2E - my_shift)
        hit = lax.broadcasted_iota(jnp.int32, (size, pair), 0) == lab - (row0 + first_row)
        dz_t = jnp.where(hit, prob - inv_count, prob).astype(BF16)
        got = jnp.where(hit, zf, 0.0).reshape(size // 8, 8, pair)
        return dot_t(dz_t, emb[rows, :]), picked + jnp.sum(got, axis=0)

    tops[0] = jnp.zeros((8, pair), F32)
    dn_acc[...] = jnp.zeros_like(dn_acc)

    @pl.when(core == 0)
    def _():
        dn_acc[...], tops[0] = grads(pl.ds(base, extra), extra, base, tops[0])

    def grad_step(i, picked):
        part, picked = grads(pl.ds(pl.multiple_of(i * tile, 16), tile), tile, i * tile, picked)
        dn_acc[...] += part
        return picked

    with jax.named_scope("grads"):
        picked = lax.fori_loop(0, n_tiles, grad_step, tops[0])
    far = pl.ds(pl.multiple_of((1 - core) * seq, seq), seq)
    near = pl.ds(pl.multiple_of(core * seq, seq), seq)
    dn_send[...] = dn_acc[far, :]
    dp_copy = remote(dn_send, dn_recv, dp_sems.at[0], dp_sems.at[1], mate)
    dp_copy.start()
    row_loss = jnp.where(core == 0, lse, 0.0) - jnp.sum(picked, axis=0, keepdims=True)
    pick = lax.broadcasted_iota(jnp.int32, (8, pair), 0)
    statall[me] = jnp.where(pick == 0, lse, jnp.where(pick == 1, row_loss, 0.0))
    sa_copies = [remote(statall.at[me], statall.at[me], sa_send.at[d - 1], sa_recv.at[me], lax.rem(me + d, n_stage)) for d in range(1, n_stage)]
    for c in sa_copies:
        c.start()
    with jax.named_scope("dn_x"):
        dp_copy.wait()
        dn = ((dn_acc[near, :] + dn_recv[...]) * scale).astype(BF16)
    dn_copy = remote(dn_own, dnbuf.at[me], dn_ssem, dn_rsem.at[me], last_id)

    @pl.when(last)
    def _():
        dnbuf[last_id] = dn

    @pl.when(jnp.logical_not(last))
    def _():
        dn_own[...] = dn
        dn_copy.start()

    with jax.named_scope("ag_wait"):
        for p in peers:
            got = remote(nbuf.at[p], nbuf.at[p], ag_send.at[0], ag_recv.at[p], me)
            pl.when(jnp.logical_not(last))(got.wait_recv)
            pl.when(mate != last_id)(remote(nbuf.at[p], nbuf.at[p], fw_send.at[p], ag_recv.at[p], mate).start)

    near_dst = [1, 2, n_stage - 2]
    far_dst = n_stage // 2
    n_relay = (n_micro - 2) // 2

    def dx0_copies(m):
        return [remote(dxbuf.at[m], dx0buf.at[m], d_send.at[m, k], d_recv.at[m], dev) for k, dev in enumerate(near_dst + [far_dst])]

    def relay_far(j):
        m = 2 * j + jnp.where(me == 2, 0, 1)
        return remote(dx0buf.at[m], dx0buf.at[m], rf_send.at[j], d_recv.at[m], far_dst)

    def bwd(m):
        with jax.named_scope("bwd_wait"):
            @pl.when(jnp.logical_not(last))
            def _():
                remote(gbuf.at[m], gbuf.at[m], b_send.at[m], b_recv.at[m], me).wait_recv()

            @pl.when(last)
            def _():
                @pl.when(m != last_id)
                def _():
                    remote(dnbuf.at[m], dnbuf.at[m], dn_ssem, dn_rsem.at[m], me).wait_recv()

                yf = ybuf[m].astype(F32)
                inv = lax.rsqrt(jnp.mean(yf * yf, axis=-1, keepdims=True) + EPS)
                dnf = dnbuf[m].astype(F32)
                proj = jnp.mean(yf * dnf, axis=-1, keepdims=True)
                gbuf[m] = (dnf * inv - yf * (inv * inv * inv * proj)).astype(BF16)

        with jax.named_scope("bwd_comp"):
            g = gbuf[m]
            for j in range(n_fblk):
                cols = slice(j * fblk, (j + 1) * fblk)
                dh = dot(g, down_t[:, cols]).astype(BF16).astype(F32)
                abuf[m, :, cols] = (dh * gelu_slope(abuf[m, :, cols].astype(F32))).astype(BF16)
            dxbuf[m] = (g.astype(F32) + dot(abuf[m], up_t[...])).astype(BF16)

        @pl.when(jnp.logical_not(first))
        def _():
            remote(dxbuf.at[m], gbuf.at[m], b_send.at[m], b_recv.at[m], me - 1).start()

        @pl.when(first)
        def _():
            copies = dx0_copies(m)
            for c in copies[:-1]:
                c.start()
            pl.when(m >= 2 * n_relay)(copies[-1].start)

        pltpu.make_async_copy(abuf.at[m], da_out.at[m], out_sem.at[2, m]).start()
        pltpu.make_async_copy(gbuf.at[m], g_out.at[m], out_sem.at[3, m]).start()

    def tile_copies(k, slot):
        rows = pl.ds(pl.multiple_of(k * plan.rows, plan.rows), plan.rows)
        own = pltpu.make_async_copy(obuf.at[slot], tmp_out.at[core, rows], o_sem.at[slot])
        return own, remote(obuf.at[slot], tmp_out.at[core, rows], od_send.at[k], od_recv.at[k], mate)

    def emb_tile(k):
        with jax.named_scope("tile_prep"):
            @pl.when(k == 0)
            def _():
                for d in range(1, n_stage):
                    src = lax.rem(me + d, n_stage)
                    remote(statall.at[src], statall.at[src], sa_send.at[0], sa_recv.at[src], me).wait_recv()
                for d in range(1, n_stage // 2):
                    src = lax.rem(mate + 2 * d, n_stage)
                    pl.when(jnp.logical_not(last))(remote(nbuf.at[src], nbuf.at[src], ag_send.at[0], ag_recv.at[src], me).wait_recv)
                token_table(row_ref, cut_ref, meta)
                for m in range(n_micro):
                    n_all_t[:, m * seq:(m + 1) * seq] = nbuf[m].T
                for c in range(n_stage // 2):
                    shift[:, c * pair:(c + 1) * pair] = statall[2 * c, 0:1, :] * LOG2E + log_count

        slot = lax.rem(k, 2)

        with jax.named_scope("tile_wait"):
            @pl.when(k >= 2)
            def _():
                own, far_copy = tile_copies(k - 2, slot)
                own.wait()
                far_copy.wait_send()

        with jax.named_scope("tile"):
            rows = pl.ds(pl.multiple_of(k * plan.rows, plan.rows), plan.rows)
            logit_grad(emb[rows, :], n_all_t, shift, lab_ref, row0 + k * plan.rows, inv_count, scale, dz, chip, zbuf[rows, :])
            obuf[slot] = dot(dz[...], nbuf[...].reshape(n_tok, dim)) * scale
        own, far_copy = tile_copies(k, slot)
        own.start()
        far_copy.start()

    relays = (me == 2) | (me == n_stage - 2)
    before = sum(jnp.where(me == s, plan.before[s], 0) for s in range(n_stage))

    def work(i, carry):
        chunk = (i >= before) & (i < before + n_micro)
        pl.when(chunk)(lambda: bwd(i - before))
        pl.when(jnp.logical_not(chunk))(lambda: emb_tile(jnp.where(i < before, i, i - n_micro)))
        j = i - n_micro - jnp.where(me == 2, before, plan.tiles - n_relay)

        @pl.when(relays & (j >= 0) & (j < n_relay))
        def _():
            with jax.named_scope("relay"):
                copy = relay_far(j)
                copy.wait_recv()
            copy.start()

        return carry

    lax.fori_loop(0, plan.tiles + n_micro, work, 0)
    outs = [pltpu.make_async_copy(nbuf, n_out, out_sem.at[5, 0]), pltpu.make_async_copy(statall, stat_out, out_sem.at[5, 1]), pltpu.make_async_copy(meta, meta_out, out_sem.at[5, 2])]
    for c in outs:
        c.start()

    def relay(m, carry):
        @pl.when(jnp.logical_not(first))
        def _():
            relayed = relays & (m < 2 * n_relay) & (lax.rem(m, 2) == jnp.where(me == 2, 0, 1))
            pl.when(jnp.logical_not(relayed))(remote(dx0buf.at[m], dx0buf.at[m], r_send.at[m], d_recv.at[m], me).wait_recv)

            @pl.when(core == 0)
            def _():
                remote(dx0buf.at[m], dx0buf.at[m], r_send.at[m], d_recv.at[m], mate).start()

            pltpu.make_async_copy(dx0buf.at[m], dx0_out.at[m], out_sem.at[4, m]).start()

        @pl.when(first)
        def _():
            pltpu.make_async_copy(dxbuf.at[m], dx0_out.at[m], out_sem.at[4, m]).start()

        return carry

    with jax.named_scope("relay_all"):
        lax.fori_loop(0, n_micro, relay, 0)

    with jax.named_scope("drain"):
        for k in range(max(plan.tiles - 2, 0), plan.tiles):
            own, far_copy = tile_copies(k, k % 2)
            own.wait()
            far_copy.wait_send()
        for k in range(plan.tiles):
            rows = pl.ds(k * plan.rows, plan.rows)
            remote(obuf.at[0], tmp_out.at[1 - core, rows], od_send.at[k], od_recv.at[k], me).wait_recv()
        for j in range(n_relay):
            pl.when(relays)(relay_far(j).wait_send)
        for c in sa_copies:
            c.wait_send()
        for c, p in zip(ag_copies, peers):
            pl.when(p != last_id)(c.wait_send)
            pl.when(mate != last_id)(remote(nbuf.at[p], nbuf.at[p], fw_send.at[p], ag_recv.at[p], mate).wait_send)

        @pl.when(jnp.logical_not(last))
        def _():
            dn_copy.wait_send()
            pl.when(mate != last_id)(n_forward.wait_send)

        @pl.when(jnp.logical_not(first) & (me + 2 < n_micro))
        def _():
            x_copy(0).wait_send()

            @pl.when(me < 2)
            def _():
                x_copy(1).wait_send()

        def drain(m, carry):
            @pl.when(jnp.logical_not(last))
            def _():
                remote(ybuf.at[m], xbuf.at[m], f_send.at[m], f_recv.at[m], me).wait_send()

            @pl.when(last)
            def _():
                n_copy(m).wait_send()

            @pl.when(jnp.logical_not(first))
            def _():
                remote(dxbuf.at[m], gbuf.at[m], b_send.at[m], b_recv.at[m], me).wait_send()

                @pl.when(core == 0)
                def _():
                    remote(dx0buf.at[m], dx0buf.at[m], r_send.at[m], d_recv.at[m], me).wait_send()

            @pl.when(first)
            def _():
                copies = dx0_copies(m)
                for c in copies[:-1]:
                    c.wait_send()
                pl.when(m >= 2 * n_relay)(copies[-1].wait_send)

            pltpu.make_async_copy(hbuf.at[m], hid_out.at[m], out_sem.at[0, m]).wait()
            pltpu.make_async_copy(xbuf.at[m], xs_out.at[m], out_sem.at[1, m]).wait()
            pltpu.make_async_copy(abuf.at[m], da_out.at[m], out_sem.at[2, m]).wait()
            pltpu.make_async_copy(gbuf.at[m], g_out.at[m], out_sem.at[3, m]).wait()
            pltpu.make_async_copy(dx0buf.at[m], dx0_out.at[m], out_sem.at[4, m]).wait()
            return carry

        lax.fori_loop(0, n_micro, drain, 0)
        for c in outs:
            c.wait()


class Plan:
    def __init__(self, vocab, n_stage):
        units = vocab // LANES
        self.base = units // 2 * LANES
        self.extra = vocab - 2 * self.base
        self.head_tile = next(t for t in (1600, 1536, 1280, 1024, 768, 640, 512, 256, 128) if self.base % t == 0)
        self.rows = 1024
        self.tiles = 9
        self.steps = 12
        arrive, self.before = 0.0, [0] * n_stage
        for s in reversed(range(n_stage)):
            self.before[s] = min(max(int((arrive - 4.5) / 2.6 + 0.3), 0), self.tiles)
            arrive += 2.3 if s % 2 else 4.6
        early = self.tiles * self.rows
        self.half_steps = self.steps // 2
        self.copy_rows = early // self.half_steps
        mid = self.base + self.extra
        self.spans = [(early, mid), (mid + early, vocab)]
        longest = max(b - a for a, b in self.spans)
        self.calc_rows = -(-longest // (16 * self.half_steps)) * 16
        self.over = [self.half_steps * self.calc_rows - (b - a) for a, b in self.spans]
        self.head = max(self.over)

    def calc_start(self, s):
        h, i = s // self.half_steps, s % self.half_steps
        return min(self.spans[h][0] + i * self.calc_rows, self.spans[h][1] - self.calc_rows)

    def copy_start(self, s):
        h, i = s // self.half_steps, s % self.half_steps
        return h * (self.base + self.extra) + i * self.copy_rows


def run_pipe(x0, emb, w_up, w_down, labels, tokens, cuts, n_stage, plan):
    n_micro, seq = labels.shape
    dim, ffn = w_up.shape
    n_tok = n_micro * seq
    base = plan.base
    e_parts = next(k for k in (10, 8, 5, 4, 2, 1) if base % (16 * k) == 0)
    any_spec = pl.BlockSpec(memory_space=pl.ANY)
    act = (n_micro, seq, dim)
    wide = (n_micro, seq, ffn)
    dma = pltpu.SemaphoreType.DMA
    vm = pltpu.VMEM
    pair = 2 * seq
    return pl.pallas_call(
        functools.partial(pipe_kernel, n_stage, plan),
        out_shape=[
            jax.ShapeDtypeStruct(act, BF16), jax.ShapeDtypeStruct(act, BF16), jax.ShapeDtypeStruct(wide, BF16),
            jax.ShapeDtypeStruct(wide, BF16), jax.ShapeDtypeStruct(act, BF16), jax.ShapeDtypeStruct(act, BF16),
            jax.ShapeDtypeStruct((n_stage, 8, pair), F32), jax.ShapeDtypeStruct((2, plan.tiles * plan.rows, dim), F32),
            jax.ShapeDtypeStruct((3 * n_tok // LANES, LANES), jnp.int32),
        ],
        in_specs=[any_spec] * 4 + [pl.BlockSpec(memory_space=pltpu.VMEM)] * 3,
        out_specs=[any_spec] * 9,
        scratch_shapes=[
            vm(act, BF16), vm(act, BF16), vm(wide, BF16), vm(wide, BF16), vm(act, BF16), vm(act, BF16), vm(act, BF16), vm(act, BF16), vm(act, BF16),
            vm((dim, ffn), BF16), vm((ffn, dim), BF16), vm((ffn, dim), BF16), vm((dim, ffn), BF16),
            vm((base + plan.extra, dim), BF16), vm((base + plan.extra, pair), BF16), vm((dim, pair), BF16), vm((pair, dim), F32),
            vm((seq, dim), F32), vm((seq, dim), F32), vm((seq, dim), BF16), vm((16, pair), F32), vm((16, pair), F32), vm((n_stage, 8, pair), F32),
            vm((2, 8, pair), F32), vm((dim, n_tok), BF16), vm((1, n_tok), F32), vm((plan.rows, n_tok), BF16), vm((2, plan.rows, dim), F32),
            vm((2, plan.head_tile, pair), BF16), vm((3 * n_tok // LANES, LANES), jnp.int32),
            dma((2,)), dma((e_parts + 1,)), dma((n_micro,)), dma((n_micro,)), dma((n_micro,)), dma((n_micro,)), dma((n_micro,)), dma,
            dma((n_stage,)), dma((n_stage,)), dma((n_stage,)),
            dma((2,)), dma((2,)), dma, dma((n_stage,)), dma((n_stage,)), dma((n_stage,)),
            dma((n_micro,)), dma((n_micro,)), dma((n_micro, 4)), dma((n_micro,)), dma((n_micro,)), dma((n_micro,)), dma((6, n_micro)),
            dma((2,)), dma((2,)), dma((plan.tiles,)), dma((plan.tiles,)),
        ],
        compiler_params=pltpu.CompilerParams(collective_id=0, has_side_effects=True, vmem_limit_bytes=67_000_000),
        cost_estimate=pl.CostEstimate(flops=60 * 10**9, bytes_accessed=100 * 10**6, transcendentals=0),
        name="pipe",
    )(x0, emb, w_up, w_down, labels.reshape(1, n_tok), tokens.reshape(1, n_tok), cuts)


def fin_kernel(n_stage, n_tok, plan, ids_ref, emb_hbm, tmp_hbm, n_hbm, stat_ref, lab_ref, meta_ref, dx0_hbm, xs_hbm, hid_hbm, da_hbm, g_hbm,
               out_hbm, loss_ref, gup_hbm, gdown_hbm,
               n_all, dx0, xs, hid, da, g, n_t, x_t, dx0s, dz, shift, e_in, c_out, cp, gup, gdown,
               ld_sem, e_sem, t_sem, co_sem, po_sem, gu_sem, gd_sem):
    dim = n_all.shape[1]
    ffn = da.shape[1]
    scale = dim ** -0.5
    inv_count = 1.0 / n_tok
    steps, half, crows, prows = plan.steps, plan.half_steps, plan.calc_rows, plan.copy_rows
    mid = plan.base + plan.extra
    wblk = 256
    n_wblk = ffn // wblk

    def calc_start(s):
        h, i = s // half, lax.rem(s, half)
        lo = jnp.where(h == 0, plan.spans[0][0], plan.spans[1][0]) + i * crows
        return pl.multiple_of(jnp.minimum(lo, jnp.where(h == 0, plan.spans[0][1], plan.spans[1][1]) - crows), 16)

    def copy_start(s):
        return pl.multiple_of(s // half * mid + lax.rem(s, half) * prows, 16)

    def e_copy(s):
        return pltpu.make_async_copy(emb_hbm.at[pl.ds(calc_start(s), crows)], e_in.at[lax.rem(s, 2)], e_sem.at[lax.rem(s, 2)])

    def t_copy(s):
        return pltpu.make_async_copy(tmp_hbm.at[pl.ds(pl.multiple_of(s * prows, 16), prows)], cp.at[lax.rem(s, 3)], t_sem.at[lax.rem(s, 3)])

    def p_out(s):
        return pltpu.make_async_copy(cp.at[lax.rem(s, 3)], out_hbm.at[pl.ds(copy_start(s), prows)], po_sem.at[lax.rem(s, 3)])

    def c_outs(s):
        slot = lax.rem(s, 2)
        start = calc_start(s)
        return (
            pltpu.make_async_copy(c_out.at[slot, pl.ds(plan.head, crows - plan.head)], out_hbm.at[pl.ds(start + plan.head, crows - plan.head)], co_sem.at[slot, 0]),
            pltpu.make_async_copy(c_out.at[slot, pl.ds(0, plan.head)], out_hbm.at[pl.ds(start, plan.head)], co_sem.at[slot, 1]),
        )

    def has_head(s):
        skip = False
        for h in range(2):
            if plan.over[h] > 0:
                skip = skip | (s == h * half + half - 1)
        return jnp.logical_not(skip)

    def c_start(s):
        a, b = c_outs(s)
        a.start()
        if plan.head:
            pl.when(has_head(s))(b.start)

    def c_wait(s):
        a, b = c_outs(s)
        a.wait()
        if plan.head:
            pl.when(has_head(s))(b.wait)

    loads = [pltpu.make_async_copy(s, d, ld_sem.at[i]) for i, (s, d) in enumerate(((n_hbm, n_all), (dx0_hbm, dx0), (xs_hbm, xs), (da_hbm, da), (hid_hbm, hid), (g_hbm, g)))]
    loads[0].start()
    loads[1].start()
    e_copy(0).start()
    t_copy(0).start()
    pair = stat_ref.shape[2]
    loss = jnp.zeros((1, pair), F32)
    for d in range(n_stage):
        if d % 2 == 0:
            shift[:, (d // 2) * pair:(d // 2 + 1) * pair] = stat_ref[d, 0:1, :] * LOG2E + math.log2(n_tok)
        loss = loss + stat_ref[d, 1:2, :]
    loss_ref[0] = jnp.sum(loss) * inv_count
    with jax.named_scope("fin_pre"):
        loads[0].wait()
        n_t[...] = n_all[...].T
        loads[1].wait()
        dense = jnp.concatenate([meta_ref[g:g + 1, :] for g in range(n_tok // LANES)], axis=1)
        order = lax.broadcasted_iota(jnp.int32, (n_tok, n_tok), 0) == dense
        dx0s[...] = dot(jnp.where(order, 1.0, 0.0).astype(BF16), dx0[...])

    def add_rows(k, start, ref):
        lo, hi = ids_ref[2 * n_tok + k], ids_ref[2 * n_tok + k + 1]
        wide = 8

        def some(p, width):
            at = [pl.ds(ids_ref[n_tok + p + u] - start, 1) for u in range(width)]
            new = [ref[at[u], :] + dx0s[pl.ds(p + u, 1), :] for u in range(width)]
            for u in range(width):
                ref[at[u], :] = new[u]

        def group(g, carry):
            some(lo + g * wide, wide)
            return carry

        def single(p, carry):
            some(p, 1)
            return carry

        n_grp = (hi - lo) // wide
        lax.fori_loop(0, n_grp, group, 0)
        lax.fori_loop(lo + n_grp * wide, hi, single, 0)

    def step(s, carry):
        with jax.named_scope("fin_wait"):
            e_copy(s).wait()
            t_copy(s).wait()

            @pl.when(s + 1 < steps)
            def _():
                e_copy(s + 1).start()

                @pl.when(s >= 2)
                def _():
                    p_out(s - 2).wait()

                t_copy(s + 1).start()

            @pl.when(s >= 2)
            def _():
                c_wait(s - 2)

        slot = lax.rem(s, 2)
        pslot = lax.rem(s, 3)
        start = calc_start(s)
        with jax.named_scope("add_p"):
            add_rows(4 * s + 2, copy_start(s), cp.at[pslot])
        p_out(s).start()
        with jax.named_scope("calc"):
            logit_grad(e_in[slot], n_t, shift, lab_ref, start, inv_count, scale, dz)
            c_out[slot] = dot(dz[...], n_all[...]) * scale
        with jax.named_scope("add_c"):
            add_rows(4 * s, start, c_out.at[slot])
        c_start(s)

        @pl.when(s == 0)
        def _():
            for c in loads[2:]:
                c.start()

        w = s - 2

        @pl.when(w == 0)
        def _():
            for c in loads[2:]:
                c.wait()
            x_t[...] = xs[...].T

        @pl.when((w >= 0) & (w < n_wblk))
        def _():
            cols = pl.ds(pl.multiple_of(w * wblk, wblk), wblk)
            wslot = lax.rem(w, 2)
            up_copy, down_copy = w_outs(w)

            @pl.when(w >= 2)
            def _():
                for c in w_outs(w - 2):
                    c.wait()

            with jax.named_scope("dw"):
                gup[wslot] = dot(x_t[...], da[:, cols])
                gdown[wslot] = dot_t(hid[:, cols], g[...])
            up_copy.start()
            down_copy.start()

        return carry

    def w_outs(w):
        cols = pl.ds(pl.multiple_of(w * wblk, wblk), wblk)
        wslot = lax.rem(w, 2)
        return (pltpu.make_async_copy(gup.at[wslot], gup_hbm.at[:, cols], gu_sem.at[wslot]), pltpu.make_async_copy(gdown.at[wslot], gdown_hbm.at[cols], gd_sem.at[wslot]))

    lax.fori_loop(0, steps, step, 0)
    with jax.named_scope("fin_drain"):
        for w in range(n_wblk - 2, n_wblk):
            for c in w_outs(w):
                c.wait()
        for s in range(steps - 2, steps):
            c_wait(s)
        for s in range(steps - 3, steps):
            p_out(s).wait()


def run_fin(emb, tmp, n_all, stats, labels, meta, dx0, xs, hid, da, g, n_stage, plan):
    vocab, dim = emb.shape
    n_tok, ffn = hid.shape
    vm = pltpu.VMEM
    dma = pltpu.SemaphoreType.DMA
    any_spec = pl.BlockSpec(memory_space=pl.ANY)
    vspec = pl.BlockSpec(memory_space=pltpu.VMEM)
    smem = pl.BlockSpec(memory_space=pltpu.SMEM)
    wblk = 256
    return pl.pallas_call(
        functools.partial(fin_kernel, n_stage, n_tok, plan),
        out_shape=[jax.ShapeDtypeStruct((vocab, dim), F32), jax.ShapeDtypeStruct((1,), F32), jax.ShapeDtypeStruct((dim, ffn), F32), jax.ShapeDtypeStruct((ffn, dim), F32)],
        in_specs=[smem, any_spec, any_spec, any_spec, vspec, vspec, vspec] + [any_spec] * 5,
        out_specs=[any_spec, smem, any_spec, any_spec],
        scratch_shapes=[
            vm((n_tok, dim), BF16), vm((n_tok, dim), BF16), vm((n_tok, dim), BF16), vm((n_tok, ffn), BF16), vm((n_tok, ffn), BF16), vm((n_tok, dim), BF16),
            vm((dim, n_tok), BF16), vm((dim, n_tok), BF16), vm((n_tok, dim), F32), vm((plan.calc_rows, n_tok), BF16), vm((1, n_tok), F32),
            vm((2, plan.calc_rows, dim), BF16), vm((2, plan.calc_rows, dim), F32), vm((3, plan.copy_rows, dim), F32),
            vm((2, dim, wblk), F32), vm((2, wblk, dim), F32),
            dma((6,)), dma((2,)), dma((3,)), dma((2, 2)), dma((3,)), dma((2,)), dma((2,)),
        ],
        compiler_params=pltpu.CompilerParams(vmem_limit_bytes=67_000_000),
        cost_estimate=pl.CostEstimate(flops=2 * n_tok * vocab * dim, bytes_accessed=5 * vocab * dim, transcendentals=0),
        name="fin",
    )(meta.reshape(-1), emb, tmp, n_all, stats, labels.reshape(1, n_tok), meta, dx0, xs, hid, da, g)


def solution(mesh):
    n_stage = mesh.shape["stage"]

    def device_fn(tokens, labels, emb, w_up, w_down):
        n_micro, seq = tokens.shape
        vocab, dim = emb.shape
        w_up, w_down = w_up[0], w_down[0]
        n_tok = n_micro * seq
        plan = Plan(vocab, n_stage)
        cuts = []
        for s in range(plan.steps):
            for lo, rows in ((plan.calc_start(s), plan.calc_rows), (plan.copy_start(s), plan.copy_rows)):
                cuts += [lo, lo + rows]
        cuts = jnp.array(cuts + [vocab] * (LANES - len(cuts)), jnp.int32).reshape(1, LANES)
        x0 = run_gather(tokens, emb)
        n_all, xs, hid, da, g, dx0, stats, tmp, meta = run_pipe(x0, emb, w_up, w_down, labels, tokens, cuts, n_stage, plan)
        flat = lambda p: p.reshape(n_tok, -1)
        grad_emb, loss, grad_up, grad_down = run_fin(
            emb, tmp.reshape(-1, dim), flat(n_all), stats, labels, meta, flat(dx0), flat(xs), flat(hid), flat(da), flat(g), n_stage, plan
        )
        return loss, grad_up[None], grad_down[None], grad_emb

    return jax.shard_map(device_fn, mesh=mesh, in_specs=(P("dp", None), P("dp", None), P(None, None), P("stage", None, None), P("stage", None, None)), out_specs=(P("dp"), P(("dp", "stage"), None, None), P(("dp", "stage"), None, None), P("dp", None)), check_vma=False)
```

```python
import functools
import math

import jax
import jax.numpy as jnp
from jax import lax
from jax.experimental import pallas as pl
from jax.experimental.pallas import tpu as pltpu
from jax.sharding import PartitionSpec as P


MESH = pl.DeviceIdType.MESH
LOG2E = math.log2(math.e)
LN2 = math.log(2.0)
GELU_C = math.sqrt(2.0 / math.pi)
GELU_K = 0.044715
EPS = 1e-6
LANES = 128
F32 = jnp.float32
BF16 = jnp.bfloat16


def gelu_fwd(a):
    return 0.5 * a * (1.0 + jnp.tanh(GELU_C * (a + GELU_K * (a * a * a))))


def gelu_slope(a):
    a2 = a * a
    t = jnp.tanh(GELU_C * (a + GELU_K * (a2 * a)))
    return 0.5 * (1.0 + t) + (0.5 * a) * (1.0 - t * t) * (GELU_C + (3.0 * GELU_C * GELU_K) * a2)


def dot(x, y):
    return jnp.dot(x, y, preferred_element_type=F32)


def dot_t(x, y):
    return lax.dot_general(x, y, (((0,), (0,)), ((), ())), preferred_element_type=F32)


def remote(src, dst, send_sem, recv_sem, dev):
    return pltpu.make_async_remote_copy(src_ref=src, dst_ref=dst, send_sem=send_sem, recv_sem=recv_sem, device_id={"stage": dev}, device_id_type=MESH)


def column(row):
    return jnp.broadcast_to(row, (LANES, LANES)).T


def gather_kernel(ids_ref, tok_ref, emb_hbm, x0_hbm, tiles, picked, sem, out_sem):
    n_micro, seq = tok_ref.shape
    me = lax.axis_index("stage")
    group = tiles.shape[1] // seq
    slots = tiles.shape[0]
    owners = [head_chunk(me, k, n_micro) for k in range(slots)]

    def fetch(k):
        def one(i, carry):
            t = ids_ref[owners[k] * seq + i]
            start = pl.multiple_of(t // group * group, group)
            pltpu.make_async_copy(emb_hbm.at[pl.ds(start, group)], tiles.at[k, pl.ds(pl.multiple_of(i * group, group), group)], sem.at[k]).start()
            return carry

        lax.fori_loop(0, seq, one, 0, unroll=8)

    def select(k):
        sub = lax.broadcasted_iota(jnp.int32, (LANES, LANES), 0)
        lane = lax.broadcasted_iota(jnp.int32, (LANES, LANES), 1)
        tok = column(tok_ref[pl.ds(owners[k], 1), :].astype(F32)).astype(jnp.int32)
        want = sub * group + (tok - tok // group * group)
        hot = jnp.concatenate([jnp.where(lane + b * LANES == want, 1.0, 0.0).astype(BF16) for b in range(seq * group // LANES)], axis=1)
        pltpu.make_async_copy(emb_hbm.at[pl.ds(0, seq * group)], tiles.at[k], sem.at[k]).wait()
        picked[k] = dot(hot, tiles[k]).astype(BF16)
        pltpu.make_async_copy(picked.at[k], x0_hbm.at[k], out_sem.at[k]).start()

    def finish(k):
        pltpu.make_async_copy(picked.at[k], x0_hbm.at[k], out_sem.at[k]).wait()

    for work in (fetch, select, finish):
        work(0)
        for k in range(1, slots):
            pl.when(me < slots)(functools.partial(work, k))


def head_chunk(dev, k, n_micro):
    return jnp.minimum(jnp.where(dev < 2, 2 * dev + k, dev + 2), n_micro - 1)


def run_gather(tokens, emb):
    n_micro, seq = tokens.shape
    dim = emb.shape[1]
    group = 16
    return pl.pallas_call(
        gather_kernel,
        out_shape=jax.ShapeDtypeStruct((2, seq, dim), BF16),
        in_specs=[pl.BlockSpec(memory_space=pltpu.SMEM), pl.BlockSpec(memory_space=pltpu.VMEM), pl.BlockSpec(memory_space=pl.ANY)],
        out_specs=pl.BlockSpec(memory_space=pl.ANY),
        scratch_shapes=[pltpu.VMEM((2, seq * group, dim), BF16), pltpu.VMEM((2, seq, dim), BF16), pltpu.SemaphoreType.DMA((2,)), pltpu.SemaphoreType.DMA((2,))],
        cost_estimate=pl.CostEstimate(flops=10**9, bytes_accessed=2 * seq * group * dim * 2, transcendentals=0),
        name="gather",
    )(tokens.reshape(n_micro * seq), tokens, emb)


def token_table(row_ref, cut_ref, meta):
    n_tok = row_ref.shape[1]
    n_grp = n_tok // LANES
    lane = lax.broadcasted_iota(jnp.int32, (LANES, LANES), 1).astype(F32)
    sub = lax.broadcasted_iota(jnp.int32, (LANES, LANES), 0)
    row = lambda g: row_ref[:, g * LANES:(g + 1) * LANES].astype(F32)
    zero = jnp.zeros((LANES, LANES), F32)
    fold = lambda acc: jnp.sum(acc, axis=0, keepdims=True)
    cols = [column(row(c)) for c in range(n_grp)]
    firsts = []
    for g in range(n_grp):
        acc = zero
        for c in range(g + 1):
            same = cols[c] == row(g)
            if c == g:
                same = same & (sub < lane.astype(jnp.int32))
            acc = acc + jnp.where(same, 1.0, 0.0)
        firsts.append(column(jnp.where(fold(acc) == 0.0, 1.0, 0.0)))
    ranks = []
    for g in range(n_grp):
        acc = zero
        for c in range(n_grp):
            acc = acc + jnp.where(cols[c] < row(g), firsts[c], 0.0)
        ranks.append(fold(acc))
        meta[g:g + 1, :] = ranks[g].astype(jnp.int32)
    rank_cols = [column(r) for r in ranks]
    for g in range(n_grp):
        acc = zero
        for c in range(n_grp):
            acc = acc + jnp.where(rank_cols[c] == lane + g * LANES, firsts[c] * cols[c], 0.0)
        meta[n_grp + g:n_grp + g + 1, :] = fold(acc).astype(jnp.int32)
    cut = cut_ref[...].astype(F32)
    acc = zero
    for c in range(n_grp):
        acc = acc + jnp.where(cols[c] < cut, firsts[c], 0.0)
    meta[2 * n_grp:3 * n_grp, :] = jnp.broadcast_to(fold(acc), (n_grp, LANES)).astype(jnp.int32)


def logit_grad(e, n_t, shift, lab, first_id, inv_count, scale, dz):
    rows = e.shape[0]
    n_tok = n_t.shape[1]
    blk = 256
    vid = lax.broadcasted_iota(jnp.int32, (rows, blk), 0)
    for j in range(n_tok // blk):
        cols = slice(j * blk, (j + 1) * blk)
        z = (dot(e, n_t[:, cols]) * scale).astype(BF16).astype(F32)
        prob = jnp.exp2(z * LOG2E - shift[:, cols])
        dz[:, cols] = jnp.where(vid == lab[:, cols] - first_id, prob - inv_count, prob).astype(BF16)


def pipe_kernel(n_stage, plan, x0_hbm, emb_hbm, up_hbm, down_hbm, lab_ref, row_ref, cut_ref,
                n_out, xs_out, hid_out, da_out, g_out, dx0_out, stat_out, tmp_out, meta_out,
                xbuf, ybuf, abuf, hbuf, nbuf, gbuf, dxbuf, dx0buf, dnbuf, up, down, up_t, down_t,
                emb, zbuf, n_t, dn_acc, dn_send, dn_recv, dn_own, st_send, st_recv, statall, tops, n_all_t, shift, dz, obuf, z_pair, meta,
                w_sem, e_sem, x_sem, f_send, f_recv, n_send, n_recv, nf_send, ag_send, ag_recv, fw_send,
                st_sems, dp_sems, dn_ssem, dn_rsem, sa_send, sa_recv, b_send, b_recv, d_send, d_recv, r_send, rf_send, out_sem, x_send, o_sem, od_send, od_recv):
    n_micro, seq, dim = xbuf.shape
    n_tok = n_micro * seq
    ffn = up.shape[1]
    vocab = emb_hbm.shape[0]
    me = lax.axis_index("stage")
    core = lax.rem(me, 2)
    chip = me // 2
    mate = me + 1 - 2 * core
    last_id = n_stage - 1
    first = me == 0
    last = me == last_id
    fblk = 512
    n_fblk = ffn // fblk
    base, extra, tile = plan.base, plan.extra, plan.head_tile
    row0 = core * (base + extra)
    n_tiles = base // tile

    barrier = pltpu.get_barrier_semaphore()
    for d in range(1, n_stage):
        pl.semaphore_signal(barrier, inc=1, device_id={"stage": lax.rem(me + d, n_stage)}, device_id_type=MESH)
    w_copy = [pltpu.make_async_copy(up_hbm, up, w_sem.at[0]), pltpu.make_async_copy(down_hbm, down, w_sem.at[1])]
    for c in w_copy:
        c.start()
    x_slots = x0_hbm.shape[0]
    x_mine = [head_chunk(me, k, n_micro) for k in range(x_slots)]

    @pl.when(first)
    def _():
        for k in range(x_slots):
            pltpu.make_async_copy(x0_hbm.at[k], xbuf.at[k], x_sem.at[k]).start()

    e_parts = e_sem.shape[0] - 1
    e_step = base // e_parts

    def e_copy(i):
        src = emb_hbm.at[pl.ds(pl.multiple_of(row0 + i * e_step, 16), e_step)]
        return pltpu.make_async_copy(src, emb.at[pl.ds(i * e_step, e_step)], e_sem.at[i])

    e_more = pltpu.make_async_copy(emb_hbm.at[pl.ds(base, extra)], emb.at[pl.ds(base, extra)], e_sem.at[e_parts])
    with jax.named_scope("entry"):
        pl.semaphore_wait(barrier, n_stage - 1)

    def x_copy(k):
        return remote(x0_hbm.at[k], xbuf.at[x_mine[k]], x_send.at[k], f_recv.at[x_mine[k]], 0)

    @pl.when(jnp.logical_not(first) & (me + 2 < n_micro))
    def _():
        x_copy(0).start()

        @pl.when(me < 2)
        def _():
            x_copy(1).start()

    with jax.named_scope("w_wait"):
        for c in w_copy:
            c.wait()
        for i in range(e_parts):
            e_copy(i).start()
        pl.when(core == 0)(e_more.start)

    def transpose_weights():
        for j in range(n_fblk):
            up_t[j * fblk:(j + 1) * fblk, :] = up[:, j * fblk:(j + 1) * fblk].T
            down_t[:, j * fblk:(j + 1) * fblk] = down[j * fblk:(j + 1) * fblk, :].T

    @pl.when(chip >= n_stage // 4)
    def _():
        transpose_weights()

    def n_copy(m):
        return remote(nbuf.at[m], nbuf.at[m], n_send.at[m], n_recv.at[m], jnp.where(m == last_id, last_id - 1, m))

    def fwd(m, carry):
        local = first & (m < x_slots)

        with jax.named_scope("fwd_wait"):
            @pl.when(local)
            def _():
                pltpu.make_async_copy(x0_hbm.at[m], xbuf.at[m], x_sem.at[m]).wait()

            @pl.when(jnp.logical_not(local))
            def _():
                remote(xbuf.at[m], xbuf.at[m], f_send.at[m], f_recv.at[m], me).wait_recv()

        with jax.named_scope("fwd_comp"):
            x = xbuf[m]
            for j in range(n_fblk):
                cols = slice(j * fblk, (j + 1) * fblk)
                a = dot(x, up[:, cols]).astype(BF16)
                abuf[m, :, cols] = a
                hbuf[m, :, cols] = gelu_fwd(a.astype(F32)).astype(BF16)
            y = (x.astype(F32) + dot(hbuf[m], down[...])).astype(BF16)
            ybuf[m] = y

        @pl.when(jnp.logical_not(last))
        def _():
            remote(ybuf.at[m], xbuf.at[m], f_send.at[m], f_recv.at[m], me + 1).start()

        @pl.when(last)
        def _():
            yf = y.astype(F32)
            inv = lax.rsqrt(jnp.mean(yf * yf, axis=-1, keepdims=True) + EPS)
            nbuf[m] = (yf * inv).astype(BF16)
            n_copy(m).start()

        pltpu.make_async_copy(hbuf.at[m], hid_out.at[m], out_sem.at[0, m]).start()
        pltpu.make_async_copy(xbuf.at[m], xs_out.at[m], out_sem.at[1, m]).start()
        return carry

    lax.fori_loop(0, n_micro, fwd, 0)

    @pl.when(chip < n_stage // 4)
    def _():
        transpose_weights()

    n_forward = remote(nbuf.at[me], nbuf.at[me], nf_send, n_recv.at[me], mate)
    with jax.named_scope("n_wait"):

        @pl.when(jnp.logical_not(last))
        def _():
            remote(nbuf.at[me], nbuf.at[me], n_send.at[me], n_recv.at[me], me).wait_recv()
            pl.when(mate != last_id)(n_forward.start)
            remote(nbuf.at[mate], nbuf.at[mate], n_send.at[mate], n_recv.at[mate], me).wait_recv()

        for k in range(2):
            n_t[:, k * seq:(k + 1) * seq] = nbuf[2 * chip + k].T

    peers = [lax.rem(me + 2 * d, n_stage) for d in range(1, n_stage // 2)]
    ag_copies = [remote(nbuf.at[me], nbuf.at[me], ag_send.at[d], ag_recv.at[me], p) for d, p in enumerate(peers)]
    for c, p in zip(ag_copies, peers):
        pl.when(p != last_id)(c.start)
    with jax.named_scope("e_wait"):
        for i in range(e_parts):
            e_copy(i).wait()
        pl.when(core == 0)(e_more.wait)

    pair = 2 * seq
    scale = dim ** -0.5
    inv_count = 1.0 / n_tok
    log_count = math.log2(n_tok)
    lab = lab_ref[:, pl.ds(pl.multiple_of(chip * pair, pair), pair)]

    def logits(rows, size):
        e = emb[rows, :]
        parts = [dot(e[k * size // 2:(k + 1) * size // 2], n_t[...]) for k in range(2)]
        z = jnp.concatenate([(p * scale).astype(BF16) for p in parts], axis=0)
        zbuf[rows, :] = z
        return z

    def peak(z, size, top):
        best = jnp.max(z.reshape(size // 16, 16, pair), axis=0).astype(F32)
        return jnp.maximum(top, jnp.maximum(best[:8], best[8:]))

    def total(z, size, old, top, tot):
        off = top * LOG2E
        return tot * jnp.exp2(old * LOG2E - off) + jnp.sum(jnp.exp2(z.astype(F32).reshape(size // 8, 8, pair) * LOG2E - off[None]), axis=0)

    tops[0] = jnp.full((8, pair), -jnp.inf, F32)
    tops[1] = jnp.zeros((8, pair), F32)

    @pl.when(core == 0)
    def _():
        z = logits(pl.ds(base, extra), extra)
        top = peak(z, extra, tops[0])
        tops[1] = total(z, extra, tops[0], top, tops[1])
        tops[0] = top

    def logits_step(i, slot, old, top, tot):
        z = logits(pl.ds(pl.multiple_of(i * tile, 16), tile), tile)
        tot = total(z_pair[1 - slot], tile, old, top, tot)
        z_pair[slot] = z
        return top, peak(z, tile, top), tot

    with jax.named_scope("logits"):
        z = logits(pl.ds(0, tile), tile)
        z_pair[0] = z
        state = (tops[0], peak(z, tile, tops[0]), tops[1])
        state = lax.fori_loop(0, (n_tiles - 1) // 2, lambda i, c: logits_step(2 * i + 2, 0, *logits_step(2 * i + 1, 1, *c)), state)
        if n_tiles % 2 == 0:
            state = logits_step(n_tiles - 1, 1, *state)
        old, top, tot = state
        tot = total(z_pair[(n_tiles - 1) % 2], tile, old, top, tot)
    row_top = jnp.max(top, axis=0, keepdims=True)
    row_tot = jnp.sum(tot * jnp.exp2((top - row_top) * LOG2E), axis=0, keepdims=True)
    st_send[0:8, :] = jnp.broadcast_to(row_top, (8, pair))
    st_send[8:16, :] = jnp.broadcast_to(row_tot, (8, pair))
    st_copy = remote(st_send, st_recv, st_sems.at[0], st_sems.at[1], mate)
    with jax.named_scope("stat_x"):
        st_copy.start()
        st_copy.wait()
    far_top = st_recv[0:1, :]
    far_tot = st_recv[8:9, :]
    all_top = jnp.maximum(row_top, far_top)
    mine = row_tot * jnp.exp(row_top - all_top)
    other = far_tot * jnp.exp(far_top - all_top)
    lse = all_top + jnp.log(jnp.where(core == 0, mine + other, other + mine))
    my_shift = lse * LOG2E + log_count

    def grads(rows, size, first_row, picked):
        zf = zbuf[rows, :].astype(F32)
        prob = jnp.exp2(zf * LOG2E - my_shift)
        hit = lax.broadcasted_iota(jnp.int32, (size, pair), 0) == lab - (row0 + first_row)
        dz_t = jnp.where(hit, prob - inv_count, prob).astype(BF16)
        got = jnp.where(hit, zf, 0.0).reshape(size // 8, 8, pair)
        return dot_t(dz_t, emb[rows, :]), picked + jnp.sum(got, axis=0)

    tops[0] = jnp.zeros((8, pair), F32)
    dn_acc[...] = jnp.zeros_like(dn_acc)

    @pl.when(core == 0)
    def _():
        dn_acc[...], tops[0] = grads(pl.ds(base, extra), extra, base, tops[0])

    def grad_step(i, picked):
        part, picked = grads(pl.ds(pl.multiple_of(i * tile, 16), tile), tile, i * tile, picked)
        dn_acc[...] += part
        return picked

    with jax.named_scope("grads"):
        picked = lax.fori_loop(0, n_tiles, grad_step, tops[0])
    far = pl.ds(pl.multiple_of((1 - core) * seq, seq), seq)
    near = pl.ds(pl.multiple_of(core * seq, seq), seq)
    dn_send[...] = dn_acc[far, :]
    dp_copy = remote(dn_send, dn_recv, dp_sems.at[0], dp_sems.at[1], mate)
    dp_copy.start()
    row_loss = jnp.where(core == 0, lse, 0.0) - jnp.sum(picked, axis=0, keepdims=True)
    pick = lax.broadcasted_iota(jnp.int32, (8, pair), 0)
    statall[me] = jnp.where(pick == 0, lse, jnp.where(pick == 1, row_loss, 0.0))
    sa_copies = [remote(statall.at[me], statall.at[me], sa_send.at[d - 1], sa_recv.at[me], lax.rem(me + d, n_stage)) for d in range(1, n_stage)]
    for c in sa_copies:
        c.start()
    with jax.named_scope("dn_x"):
        dp_copy.wait()
        dn = ((dn_acc[near, :] + dn_recv[...]) * scale).astype(BF16)
    dn_copy = remote(dn_own, dnbuf.at[me], dn_ssem, dn_rsem.at[me], last_id)

    @pl.when(last)
    def _():
        dnbuf[last_id] = dn

    @pl.when(jnp.logical_not(last))
    def _():
        dn_own[...] = dn
        dn_copy.start()

    with jax.named_scope("ag_wait"):
        for p in peers:
            got = remote(nbuf.at[p], nbuf.at[p], ag_send.at[0], ag_recv.at[p], me)
            pl.when(jnp.logical_not(last))(got.wait_recv)
            pl.when(mate != last_id)(remote(nbuf.at[p], nbuf.at[p], fw_send.at[p], ag_recv.at[p], mate).start)

    near_dst = [1, 2, n_stage - 2]
    far_dst = n_stage // 2
    n_relay = (n_micro - 2) // 2

    def dx0_copies(m):
        return [remote(dxbuf.at[m], dx0buf.at[m], d_send.at[m, k], d_recv.at[m], dev) for k, dev in enumerate(near_dst + [far_dst])]

    def relay_far(j):
        m = 2 * j + jnp.where(me == 2, 0, 1)
        return remote(dx0buf.at[m], dx0buf.at[m], rf_send.at[j], d_recv.at[m], far_dst)

    def bwd(m):
        with jax.named_scope("bwd_wait"):
            @pl.when(jnp.logical_not(last))
            def _():
                remote(gbuf.at[m], gbuf.at[m], b_send.at[m], b_recv.at[m], me).wait_recv()

            @pl.when(last)
            def _():
                @pl.when(m != last_id)
                def _():
                    remote(dnbuf.at[m], dnbuf.at[m], dn_ssem, dn_rsem.at[m], me).wait_recv()

                yf = ybuf[m].astype(F32)
                inv = lax.rsqrt(jnp.mean(yf * yf, axis=-1, keepdims=True) + EPS)
                dnf = dnbuf[m].astype(F32)
                proj = jnp.mean(yf * dnf, axis=-1, keepdims=True)
                gbuf[m] = (dnf * inv - yf * (inv * inv * inv * proj)).astype(BF16)

        with jax.named_scope("bwd_comp"):
            g = gbuf[m]
            for j in range(n_fblk):
                cols = slice(j * fblk, (j + 1) * fblk)
                dh = dot(g, down_t[:, cols]).astype(BF16).astype(F32)
                abuf[m, :, cols] = (dh * gelu_slope(abuf[m, :, cols].astype(F32))).astype(BF16)
            dxbuf[m] = (g.astype(F32) + dot(abuf[m], up_t[...])).astype(BF16)

        @pl.when(jnp.logical_not(first))
        def _():
            remote(dxbuf.at[m], gbuf.at[m], b_send.at[m], b_recv.at[m], me - 1).start()

        @pl.when(first)
        def _():
            copies = dx0_copies(m)
            for c in copies[:-1]:
                c.start()
            pl.when(m >= 2 * n_relay)(copies[-1].start)

        pltpu.make_async_copy(abuf.at[m], da_out.at[m], out_sem.at[2, m]).start()
        pltpu.make_async_copy(gbuf.at[m], g_out.at[m], out_sem.at[3, m]).start()

    def tile_copy(k):
        rows = pl.ds(pl.multiple_of(k * plan.rows, plan.rows), plan.rows)
        slot = lax.rem(k, 2)
        return pltpu.make_async_copy(obuf.at[slot], tmp_out.at[core, rows], o_sem.at[slot])

    def piece(p):
        rows = pl.ds(pl.multiple_of(p * plan.piece, plan.piece), plan.piece)
        return remote(tmp_out.at[core, rows], tmp_out.at[core, rows], od_send.at[p], od_recv.at[p], mate)

    def piece_in(p):
        rows = pl.ds(pl.multiple_of(p * plan.piece, plan.piece), plan.piece)
        return remote(tmp_out.at[1 - core, rows], tmp_out.at[1 - core, rows], od_send.at[p], od_recv.at[p], me)

    def emb_tile(k):
        with jax.named_scope("tile_prep"):

            @pl.when(k == 0)
            def _():
                for d in range(1, n_stage // 2):
                    src = lax.rem(mate + 2 * d, n_stage)
                    pl.when(jnp.logical_not(last))(remote(nbuf.at[src], nbuf.at[src], ag_send.at[0], ag_recv.at[src], me).wait_recv)
                token_table(row_ref, jnp.where(core == 0, cut_ref[0:1, :], cut_ref[1:2, :]), meta)
                for m in range(n_micro):
                    n_all_t[:, m * seq:(m + 1) * seq] = nbuf[m].T
                for d in range(1, n_stage):
                    src = lax.rem(me + d, n_stage)
                    remote(statall.at[src], statall.at[src], sa_send.at[0], sa_recv.at[src], me).wait_recv()
                for c in range(n_stage // 2):
                    shift[:, c * pair:(c + 1) * pair] = statall[2 * c, 0:1, :] * LOG2E + log_count

        slot = lax.rem(k, 2)
        with jax.named_scope("tile"):
            rows = pl.ds(pl.multiple_of(k * plan.rows, plan.rows), plan.rows)
            logit_grad(emb[rows, :], n_all_t, shift, lab_ref, row0 + k * plan.rows, inv_count, scale, dz)
            obuf[slot] = dot(dz[...], nbuf[...].reshape(n_tok, dim)) * scale

        @pl.when(k >= 1)
        def _():
            tile_copy(k - 1).wait()

        tile_copy(k).start()

    def send_pieces(done, until):
        lax.fori_loop(done, until, lambda p, c: (piece(p).start(), c)[1], 0)
        return jnp.maximum(done, until)

    relays = (me == 2) | (me == n_stage - 2)
    before = sum(jnp.where(me == s, plan.before[s], 0) for s in range(n_stage))

    def work(i, carry):
        chunk = (i >= before) & (i < before + n_micro)
        pl.when(chunk)(lambda: bwd(i - before))
        k = jnp.where(i < before, i, i - n_micro)
        pl.when(jnp.logical_not(chunk))(lambda: emb_tile(k))
        j = i - n_micro - jnp.where(me == 2, before, plan.tiles - n_relay)

        @pl.when(relays & (j >= 0) & (j < n_relay))
        def _():
            with jax.named_scope("relay"):
                copy = relay_far(j)
                copy.wait_recv()
            copy.start()

        ready = jnp.where(i < before, i, jnp.where(chunk, before - 1, i - n_micro)) * plan.per_tile
        near_chunks = chunk | ((i < before) & (i + 1 >= before))
        until = jnp.minimum(jnp.minimum(ready, plan.shared * plan.per_tile), carry + jnp.where(near_chunks, 1, 2 * plan.per_tile))
        return send_pieces(carry, until)

    sent = lax.fori_loop(0, plan.tiles + n_micro, work, 0)
    with jax.named_scope("last_tile"):
        tile_copy(plan.tiles - 1).wait()
        send_pieces(sent, plan.shared * plan.per_tile)
    outs = [pltpu.make_async_copy(nbuf, n_out, out_sem.at[5, 0]), pltpu.make_async_copy(statall, stat_out, out_sem.at[5, 1]), pltpu.make_async_copy(meta, meta_out, out_sem.at[5, 2])]
    for c in outs:
        c.start()

    def relay(m, carry):
        @pl.when(jnp.logical_not(first))
        def _():
            relayed = relays & (m < 2 * n_relay) & (lax.rem(m, 2) == jnp.where(me == 2, 0, 1))
            pl.when(jnp.logical_not(relayed))(remote(dx0buf.at[m], dx0buf.at[m], r_send.at[m], d_recv.at[m], me).wait_recv)

            @pl.when(core == 0)
            def _():
                remote(dx0buf.at[m], dx0buf.at[m], r_send.at[m], d_recv.at[m], mate).start()

            pltpu.make_async_copy(dx0buf.at[m], dx0_out.at[m], out_sem.at[4, m]).start()

        @pl.when(first)
        def _():
            pltpu.make_async_copy(dxbuf.at[m], dx0_out.at[m], out_sem.at[4, m]).start()

        return carry

    with jax.named_scope("relay_all"):
        lax.fori_loop(0, n_micro, relay, 0)

    with jax.named_scope("drain"):
        for p in range(plan.shared * plan.per_tile):
            piece(p).wait_send()
            piece_in(p).wait_recv()
        for j in range(n_relay):
            pl.when(relays)(relay_far(j).wait_send)
        for c in sa_copies:
            c.wait_send()
        for c, p in zip(ag_copies, peers):
            pl.when(p != last_id)(c.wait_send)
            pl.when(mate != last_id)(remote(nbuf.at[p], nbuf.at[p], fw_send.at[p], ag_recv.at[p], mate).wait_send)

        @pl.when(jnp.logical_not(last))
        def _():
            dn_copy.wait_send()
            pl.when(mate != last_id)(n_forward.wait_send)

        @pl.when(jnp.logical_not(first) & (me + 2 < n_micro))
        def _():
            x_copy(0).wait_send()

            @pl.when(me < 2)
            def _():
                x_copy(1).wait_send()

        def drain(m, carry):
            @pl.when(jnp.logical_not(last))
            def _():
                remote(ybuf.at[m], xbuf.at[m], f_send.at[m], f_recv.at[m], me).wait_send()

            @pl.when(last)
            def _():
                n_copy(m).wait_send()

            @pl.when(jnp.logical_not(first))
            def _():
                remote(dxbuf.at[m], gbuf.at[m], b_send.at[m], b_recv.at[m], me).wait_send()

                @pl.when(core == 0)
                def _():
                    remote(dx0buf.at[m], dx0buf.at[m], r_send.at[m], d_recv.at[m], me).wait_send()

            @pl.when(first)
            def _():
                copies = dx0_copies(m)
                for c in copies[:-1]:
                    c.wait_send()
                pl.when(m >= 2 * n_relay)(copies[-1].wait_send)

            pltpu.make_async_copy(hbuf.at[m], hid_out.at[m], out_sem.at[0, m]).wait()
            pltpu.make_async_copy(xbuf.at[m], xs_out.at[m], out_sem.at[1, m]).wait()
            pltpu.make_async_copy(abuf.at[m], da_out.at[m], out_sem.at[2, m]).wait()
            pltpu.make_async_copy(gbuf.at[m], g_out.at[m], out_sem.at[3, m]).wait()
            pltpu.make_async_copy(dx0buf.at[m], dx0_out.at[m], out_sem.at[4, m]).wait()
            return carry

        lax.fori_loop(0, n_micro, drain, 0)
        for c in outs:
            c.wait()


class Plan:
    def __init__(self, vocab, n_stage):
        units = vocab // LANES
        self.base = units // 2 * LANES
        self.extra = vocab - 2 * self.base
        self.head_tile = next(t for t in (1600, 1536, 1280, 1024, 768, 640, 512, 256, 128) if self.base % t == 0)
        self.rows = 1024
        self.tiles, self.shared = 10, 8
        self.piece = 256
        self.per_tile = self.rows // self.piece
        arrive, self.before = -3.0, [0] * n_stage
        for s in reversed(range(n_stage)):
            self.before[s] = min(max(int(arrive / 2.6 + 0.05), 0), self.tiles)
            arrive += 2.1 if s % 2 else 4.6
        mid = self.base + self.extra
        ends = [(0, mid), (mid, vocab)]
        early = (self.tiles * self.rows, self.shared * self.rows)
        self.spans = [[(ends[h][0] + early[0 if h == c else 1], ends[h][1]) for h in (c, 1 - c)] for c in range(2)]
        self.longest = [max(self.spans[c][k][1] - self.spans[c][k][0] for c in range(2)) for k in range(2)]
        best = min(range(16, 1281, 16), key=lambda r: (sum(-(-n // r) for n in self.longest)) * (r + 40))
        self.calc_rows = best
        self.calc_steps = [-(-n // best) for n in self.longest]
        self.steps = sum(self.calc_steps)
        self.copy_rows = self.rows
        self.copies = self.tiles + self.shared
        self.starts = ends

    def calc_start(self, core, s):
        k = 0 if s < self.calc_steps[0] else 1
        lo, hi = self.spans[core][k]
        return min(lo + (s - k * self.calc_steps[0]) * self.calc_rows, hi - self.calc_rows)

    def copy_start(self, core, c):
        own = c < self.tiles
        h = core if own else 1 - core
        return self.starts[h][0] + (c if own else c - self.tiles) * self.copy_rows

    def cuts(self, core):
        firsts = [(self.calc_start(core, s), self.calc_rows) for s in range(self.steps)] + [(self.copy_start(core, c), self.copy_rows) for c in range(self.copies)]
        flat = [v for lo, rows in firsts for v in (lo, lo + rows)]
        return flat + [0] * (LANES - len(flat))


def run_pipe(x0, emb, w_up, w_down, labels, tokens, cuts, n_stage, plan):
    n_micro, seq = labels.shape
    dim, ffn = w_up.shape
    n_tok = n_micro * seq
    base = plan.base
    e_parts = next(k for k in (10, 8, 5, 4, 2, 1) if base % (16 * k) == 0)
    any_spec = pl.BlockSpec(memory_space=pl.ANY)
    act = (n_micro, seq, dim)
    wide = (n_micro, seq, ffn)
    dma = pltpu.SemaphoreType.DMA
    vm = pltpu.VMEM
    pair = 2 * seq
    return pl.pallas_call(
        functools.partial(pipe_kernel, n_stage, plan),
        out_shape=[
            jax.ShapeDtypeStruct(act, BF16), jax.ShapeDtypeStruct(act, BF16), jax.ShapeDtypeStruct(wide, BF16),
            jax.ShapeDtypeStruct(wide, BF16), jax.ShapeDtypeStruct(act, BF16), jax.ShapeDtypeStruct(act, BF16),
            jax.ShapeDtypeStruct((n_stage, 8, pair), F32), jax.ShapeDtypeStruct((2, plan.tiles * plan.rows, dim), F32),
            jax.ShapeDtypeStruct((3 * n_tok // LANES, LANES), jnp.int32),
        ],
        in_specs=[any_spec] * 4 + [pl.BlockSpec(memory_space=pltpu.VMEM)] * 3,
        out_specs=[any_spec] * 9,
        scratch_shapes=[
            vm(act, BF16), vm(act, BF16), vm(wide, BF16), vm(wide, BF16), vm(act, BF16), vm(act, BF16), vm(act, BF16), vm(act, BF16), vm(act, BF16),
            vm((dim, ffn), BF16), vm((ffn, dim), BF16), vm((ffn, dim), BF16), vm((dim, ffn), BF16),
            vm((base + plan.extra, dim), BF16), vm((base + plan.extra, pair), BF16), vm((dim, pair), BF16), vm((pair, dim), F32),
            vm((seq, dim), F32), vm((seq, dim), F32), vm((seq, dim), BF16), vm((16, pair), F32), vm((16, pair), F32), vm((n_stage, 8, pair), F32),
            vm((2, 8, pair), F32), vm((dim, n_tok), BF16), vm((1, n_tok), F32), vm((plan.rows, n_tok), BF16), vm((2, plan.rows, dim), F32),
            vm((2, plan.head_tile, pair), BF16), vm((3 * n_tok // LANES, LANES), jnp.int32),
            dma((2,)), dma((e_parts + 1,)), dma((n_micro,)), dma((n_micro,)), dma((n_micro,)), dma((n_micro,)), dma((n_micro,)), dma,
            dma((n_stage,)), dma((n_stage,)), dma((n_stage,)),
            dma((2,)), dma((2,)), dma, dma((n_stage,)), dma((n_stage,)), dma((n_stage,)),
            dma((n_micro,)), dma((n_micro,)), dma((n_micro, 4)), dma((n_micro,)), dma((n_micro,)), dma((n_micro,)), dma((6, n_micro)),
            dma((2,)), dma((2,)), dma((plan.shared * plan.per_tile,)), dma((plan.shared * plan.per_tile,)),
        ],
        compiler_params=pltpu.CompilerParams(collective_id=0, has_side_effects=True, vmem_limit_bytes=67_000_000),
        cost_estimate=pl.CostEstimate(flops=60 * 10**9, bytes_accessed=100 * 10**6, transcendentals=0),
        name="pipe",
    )(x0, emb, w_up, w_down, labels.reshape(1, n_tok), tokens.reshape(1, n_tok), cuts)


def fin_kernel(n_stage, n_tok, plan, ids_ref, emb_hbm, tmp_hbm, n_hbm, stat_ref, lab_ref, meta_ref, dx0_hbm, xs_hbm, hid_hbm, da_hbm, g_hbm,
               out_hbm, loss_ref, gup_hbm, gdown_hbm,
               n_all, dx0, xs, hid, da, g, n_t, x_t, dx0s, dz, shift, e_in, c_out, cp, gup, gdown,
               ld_sem, e_sem, t_sem, co_sem, po_sem, gu_sem, gd_sem, wi_sem):
    dim, ffn = gup_hbm.shape
    scale = dim ** -0.5
    inv_count = 1.0 / n_tok
    steps, crows, prows = plan.steps, plan.calc_rows, plan.copy_rows
    core = lax.rem(lax.axis_index("stage"), 2)
    early = plan.tiles * prows
    wblk = gup.shape[2]
    n_wblk = ffn // wblk
    turn = plan.calc_steps[0]

    def pick(pair):
        return jnp.where(core == 0, pair[0], pair[1])

    def calc_start(s):
        own = s < turn
        lo, hi = [jnp.where(own, pick([plan.spans[c][0][e] for c in range(2)]), pick([plan.spans[c][1][e] for c in range(2)])) for e in range(2)]
        return pl.multiple_of(jnp.minimum(lo + (s - jnp.where(own, 0, turn)) * crows, hi - crows), 16)

    def copy_start(c):
        own = c < plan.tiles
        first = jnp.where(own, pick([plan.starts[0][0], plan.starts[1][0]]), pick([plan.starts[1][0], plan.starts[0][0]]))
        return pl.multiple_of(first + (c - jnp.where(own, 0, plan.tiles)) * prows, 16)

    def e_copy(s):
        return pltpu.make_async_copy(emb_hbm.at[pl.ds(calc_start(s), crows)], e_in.at[lax.rem(s, 2)], e_sem.at[lax.rem(s, 2)])

    n_slot = cp.shape[0]

    def t_copy(c):
        own = c < plan.tiles
        row = jnp.where(own, core, 1 - core) * early + (c - jnp.where(own, 0, plan.tiles)) * prows
        slot = lax.rem(c, n_slot)
        return pltpu.make_async_copy(tmp_hbm.at[pl.ds(pl.multiple_of(row, 16), prows)], cp.at[slot], t_sem.at[slot])

    def p_out(c):
        slot = lax.rem(c, n_slot)
        return pltpu.make_async_copy(cp.at[slot], out_hbm.at[pl.ds(copy_start(c), prows)], po_sem.at[slot])

    def c_outs(s):
        slot = lax.rem(s, 2)
        return pltpu.make_async_copy(c_out.at[slot], out_hbm.at[pl.ds(calc_start(s), crows)], co_sem.at[slot])

    loads = [pltpu.make_async_copy(s, d, ld_sem.at[i]) for i, (s, d) in enumerate(((n_hbm, n_all), (dx0_hbm, dx0), (xs_hbm, xs), (g_hbm, g)))]
    loads[0].start()
    e_copy(0).start()
    loads[1].start()
    for c in range(2):
        t_copy(c).start()
    pair = stat_ref.shape[2]
    loss = jnp.zeros((1, pair), F32)
    for d in range(n_stage):
        if d % 2 == 0:
            shift[:, (d // 2) * pair:(d // 2 + 1) * pair] = stat_ref[d, 0:1, :] * LOG2E + math.log2(n_tok)
        loss = loss + stat_ref[d, 1:2, :]
    loss_ref[0] = jnp.sum(loss) * inv_count
    with jax.named_scope("fin_pre"):
        loads[0].wait()
        n_t[...] = n_all[...].T
        loads[1].wait()
        dense = jnp.concatenate([meta_ref[g:g + 1, :] for g in range(n_tok // LANES)], axis=1)
        order = lax.broadcasted_iota(jnp.int32, (n_tok, n_tok), 0) == dense
        dx0s[...] = dot(jnp.where(order, 1.0, 0.0).astype(BF16), dx0[...])

    def add_rows(k, start, ref):
        lo, hi = ids_ref[2 * n_tok + k], ids_ref[2 * n_tok + k + 1]
        wide = 8

        def some(p, width):
            at = [pl.ds(ids_ref[n_tok + p + u] - start, 1) for u in range(width)]
            new = [ref[at[u], :] + dx0s[pl.ds(p + u, 1), :] for u in range(width)]
            for u in range(width):
                ref[at[u], :] = new[u]

        def group(g, carry):
            some(lo + g * wide, wide)
            return carry

        def single(p, carry):
            some(p, 1)
            return carry

        n_grp = (hi - lo) // wide
        lax.fori_loop(0, n_grp, group, 0)
        lax.fori_loop(lo + n_grp * wide, hi, single, 0)

    def w_ins(w):
        cols = pl.ds(pl.multiple_of(w * wblk, wblk), wblk)
        wslot = lax.rem(w, 2)
        return (pltpu.make_async_copy(da_hbm.at[:, cols], da.at[wslot], wi_sem.at[0, wslot]), pltpu.make_async_copy(hid_hbm.at[:, cols], hid.at[wslot], wi_sem.at[1, wslot]))

    def w_outs(w):
        cols = pl.ds(pl.multiple_of(w * wblk, wblk), wblk)
        wslot = lax.rem(w, 2)
        return (pltpu.make_async_copy(gup.at[wslot], gup_hbm.at[:, cols], gu_sem.at[wslot]), pltpu.make_async_copy(gdown.at[wslot], gdown_hbm.at[cols], gd_sem.at[wslot]))

    def copy_tile(c, carry):
        with jax.named_scope("copy_wait"):
            t_copy(c).wait()
        with jax.named_scope("add_p"):
            add_rows(2 * steps + 2 * c, copy_start(c), cp.at[lax.rem(c, n_slot)])
        p_out(c).start()

        @pl.when(c + 2 < plan.copies)
        def _():
            pl.when(c + 2 >= n_slot)(lambda: p_out(c + 2 - n_slot).wait())
            t_copy(c + 2).start()

        return carry

    w_first = 2
    tails = [turn - 1, steps - 1]

    def tail(s):
        return (s == tails[0]) | (s == tails[1])

    def step(s, carry):
        lax.fori_loop(s * plan.copies // steps, (s + 1) * plan.copies // steps, copy_tile, 0)
        with jax.named_scope("fin_wait"):
            e_copy(s).wait()

        pl.when(s + 1 < steps)(lambda: e_copy(s + 1).start())

        @pl.when(s == 0)
        def _():
            for c in loads[2:]:
                c.start()

        w = s - w_first

        @pl.when((w + 1 >= 0) & (w + 1 < n_wblk))
        def _():
            for c in w_ins(w + 1):
                c.start()

        pl.when((s >= 2) & jnp.logical_not(tail(s - 1)))(lambda: c_outs(s - 2).wait())
        slot = lax.rem(s, 2)
        start = calc_start(s)
        with jax.named_scope("calc"):
            logit_grad(e_in[slot], n_t, shift, lab_ref, start, inv_count, scale, dz)
            c_out[slot] = dot(dz[...], n_all[...]) * scale
        with jax.named_scope("add_c"):
            add_rows(2 * s, start, c_out.at[slot])
        pl.when(tail(s))(lambda: c_outs(s - 1).wait())
        c_outs(s).start()

        @pl.when(w == 0)
        def _():
            for c in loads[2:]:
                c.wait()
            x_t[...] = xs[...].T

        @pl.when((w >= 0) & (w < n_wblk))
        def _():
            wslot = lax.rem(w, 2)
            with jax.named_scope("dw_wait"):
                for c in w_ins(w):
                    c.wait()

                @pl.when(w >= 2)
                def _():
                    for c in w_outs(w - 2):
                        c.wait()

            with jax.named_scope("dw"):
                gup[wslot] = dot(x_t[...], da[wslot])
                gdown[wslot] = dot_t(hid[wslot], g[...])
            for c in w_outs(w):
                c.start()

        return carry

    lax.fori_loop(0, steps, step, 0)
    with jax.named_scope("fin_drain"):
        for w in range(n_wblk - 2, n_wblk):
            for c in w_outs(w):
                c.wait()
        c_outs(steps - 1).wait()
        for c in range(plan.copies - n_slot, plan.copies):
            p_out(c).wait()


def run_fin(emb, tmp, n_all, stats, labels, meta, dx0, xs, hid, da, g, n_stage, plan):
    vocab, dim = emb.shape
    n_tok, ffn = hid.shape
    vm = pltpu.VMEM
    dma = pltpu.SemaphoreType.DMA
    any_spec = pl.BlockSpec(memory_space=pl.ANY)
    vspec = pl.BlockSpec(memory_space=pltpu.VMEM)
    smem = pl.BlockSpec(memory_space=pltpu.SMEM)
    wblk = 256
    return pl.pallas_call(
        functools.partial(fin_kernel, n_stage, n_tok, plan),
        out_shape=[jax.ShapeDtypeStruct((vocab, dim), F32), jax.ShapeDtypeStruct((1,), F32), jax.ShapeDtypeStruct((dim, ffn), F32), jax.ShapeDtypeStruct((ffn, dim), F32)],
        in_specs=[smem, any_spec, any_spec, any_spec, vspec, vspec, vspec] + [any_spec] * 5,
        out_specs=[any_spec, smem, any_spec, any_spec],
        scratch_shapes=[
            vm((n_tok, dim), BF16), vm((n_tok, dim), BF16), vm((n_tok, dim), BF16), vm((2, n_tok, wblk), BF16), vm((2, n_tok, wblk), BF16), vm((n_tok, dim), BF16),
            vm((dim, n_tok), BF16), vm((dim, n_tok), BF16), vm((n_tok, dim), F32), vm((plan.calc_rows, n_tok), BF16), vm((1, n_tok), F32),
            vm((2, plan.calc_rows, dim), BF16), vm((2, plan.calc_rows, dim), F32), vm((4, plan.copy_rows, dim), F32),
            vm((2, dim, wblk), F32), vm((2, wblk, dim), F32),
            dma((4,)), dma((2,)), dma((4,)), dma((2,)), dma((4,)), dma((2,)), dma((2,)), dma((2, 2)),
        ],
        compiler_params=pltpu.CompilerParams(vmem_limit_bytes=67_000_000),
        cost_estimate=pl.CostEstimate(flops=2 * n_tok * vocab * dim, bytes_accessed=5 * vocab * dim, transcendentals=0),
        name="fin",
    )(meta.reshape(-1), emb, tmp, n_all, stats, labels.reshape(1, n_tok), meta, dx0, xs, hid, da, g)


def solution(mesh):
    n_stage = mesh.shape["stage"]

    def device_fn(tokens, labels, emb, w_up, w_down):
        n_micro, seq = tokens.shape
        vocab, dim = emb.shape
        w_up, w_down = w_up[0], w_down[0]
        n_tok = n_micro * seq
        plan = Plan(vocab, n_stage)
        cuts = jnp.array([plan.cuts(0), plan.cuts(1)], jnp.int32)
        x0 = run_gather(tokens, emb)
        n_all, xs, hid, da, g, dx0, stats, tmp, meta = run_pipe(x0, emb, w_up, w_down, labels, tokens, cuts, n_stage, plan)
        flat = lambda p: p.reshape(n_tok, -1)
        grad_emb, loss, grad_up, grad_down = run_fin(
            emb, tmp.reshape(-1, dim), flat(n_all), stats, labels, meta, flat(dx0), flat(xs), flat(hid), flat(da), flat(g), n_stage, plan
        )
        return loss, grad_up[None], grad_down[None], grad_emb

    return jax.shard_map(device_fn, mesh=mesh, in_specs=(P("dp", None), P("dp", None), P(None, None), P("stage", None, None), P("stage", None, None)), out_specs=(P("dp"), P(("dp", "stage"), None, None), P(("dp", "stage"), None, None), P("dp", None)), check_vma=False)
```

```python
import functools
import math

import jax
import jax.numpy as jnp
from jax import lax
from jax.experimental import pallas as pl
from jax.experimental.pallas import tpu as pltpu
from jax.sharding import PartitionSpec as P


MESH = pl.DeviceIdType.MESH
LOG2E = math.log2(math.e)
LN2 = math.log(2.0)
GELU_C = math.sqrt(2.0 / math.pi)
GELU_K = 0.044715
EPS = 1e-6
LANES = 128
F32 = jnp.float32
BF16 = jnp.bfloat16


def gelu_fwd(a):
    return 0.5 * a * (1.0 + jnp.tanh(GELU_C * (a + GELU_K * (a * a * a))))


def gelu_slope(a):
    a2 = a * a
    t = jnp.tanh(GELU_C * (a + GELU_K * (a2 * a)))
    return 0.5 * (1.0 + t) + (0.5 * a) * (1.0 - t * t) * (GELU_C + (3.0 * GELU_C * GELU_K) * a2)


def dot(x, y):
    return jnp.dot(x, y, preferred_element_type=F32)


def dot_t(x, y):
    return lax.dot_general(x, y, (((0,), (0,)), ((), ())), preferred_element_type=F32)


def remote(src, dst, send_sem, recv_sem, dev):
    return pltpu.make_async_remote_copy(src_ref=src, dst_ref=dst, send_sem=send_sem, recv_sem=recv_sem, device_id={"stage": dev}, device_id_type=MESH)


def column(row):
    return jnp.broadcast_to(row, (LANES, LANES)).T


def gather_kernel(ids_ref, tok_ref, emb_hbm, x0_hbm, tiles, picked, sem, out_sem):
    n_micro, seq = tok_ref.shape
    me = lax.axis_index("stage")
    group = tiles.shape[1] // seq
    slots = tiles.shape[0]
    owners = [head_chunk(me, k, n_micro) for k in range(slots)]

    def fetch(k):
        def one(i, carry):
            t = ids_ref[owners[k] * seq + i]
            start = pl.multiple_of(t // group * group, group)
            pltpu.make_async_copy(emb_hbm.at[pl.ds(start, group)], tiles.at[k, pl.ds(pl.multiple_of(i * group, group), group)], sem.at[k]).start()
            return carry

        lax.fori_loop(0, seq, one, 0, unroll=8)

    def select(k):
        sub = lax.broadcasted_iota(jnp.int32, (LANES, LANES), 0)
        lane = lax.broadcasted_iota(jnp.int32, (LANES, LANES), 1)
        tok = column(tok_ref[pl.ds(owners[k], 1), :].astype(F32)).astype(jnp.int32)
        want = sub * group + (tok - tok // group * group)
        hot = jnp.concatenate([jnp.where(lane + b * LANES == want, 1.0, 0.0).astype(BF16) for b in range(seq * group // LANES)], axis=1)
        pltpu.make_async_copy(emb_hbm.at[pl.ds(0, seq * group)], tiles.at[k], sem.at[k]).wait()
        picked[k] = dot(hot, tiles[k]).astype(BF16)
        pltpu.make_async_copy(picked.at[k], x0_hbm.at[k], out_sem.at[k]).start()

    def finish(k):
        pltpu.make_async_copy(picked.at[k], x0_hbm.at[k], out_sem.at[k]).wait()

    for work in (fetch, select, finish):
        work(0)
        for k in range(1, slots):
            pl.when(me < slots)(functools.partial(work, k))


def head_chunk(dev, k, n_micro):
    return jnp.minimum(jnp.where(dev < 2, 2 * dev + k, dev + 2), n_micro - 1)


def run_gather(tokens, emb):
    n_micro, seq = tokens.shape
    dim = emb.shape[1]
    group = 16
    return pl.pallas_call(
        gather_kernel,
        out_shape=jax.ShapeDtypeStruct((2, seq, dim), BF16),
        in_specs=[pl.BlockSpec(memory_space=pltpu.SMEM), pl.BlockSpec(memory_space=pltpu.VMEM), pl.BlockSpec(memory_space=pl.ANY)],
        out_specs=pl.BlockSpec(memory_space=pl.ANY),
        scratch_shapes=[pltpu.VMEM((2, seq * group, dim), BF16), pltpu.VMEM((2, seq, dim), BF16), pltpu.SemaphoreType.DMA((2,)), pltpu.SemaphoreType.DMA((2,))],
        cost_estimate=pl.CostEstimate(flops=10**9, bytes_accessed=2 * seq * group * dim * 2, transcendentals=0),
        name="gather",
    )(tokens.reshape(n_micro * seq), tokens, emb)


def token_table(row_ref, cut_ref, meta):
    n_tok = row_ref.shape[1]
    n_grp = n_tok // LANES
    lane = lax.broadcasted_iota(jnp.int32, (LANES, LANES), 1).astype(F32)
    sub = lax.broadcasted_iota(jnp.int32, (LANES, LANES), 0)
    row = lambda g: row_ref[:, g * LANES:(g + 1) * LANES].astype(F32)
    zero = jnp.zeros((LANES, LANES), F32)
    fold = lambda acc: jnp.sum(acc, axis=0, keepdims=True)
    cols = [column(row(c)) for c in range(n_grp)]
    firsts = []
    for g in range(n_grp):
        acc = zero
        for c in range(g + 1):
            same = cols[c] == row(g)
            if c == g:
                same = same & (sub < lane.astype(jnp.int32))
            acc = acc + jnp.where(same, 1.0, 0.0)
        firsts.append(column(jnp.where(fold(acc) == 0.0, 1.0, 0.0)))
    ranks = []
    for g in range(n_grp):
        acc = zero
        for c in range(n_grp):
            acc = acc + jnp.where(cols[c] < row(g), firsts[c], 0.0)
        ranks.append(fold(acc))
        meta[g:g + 1, :] = ranks[g].astype(jnp.int32)
    rank_cols = [column(r) for r in ranks]
    for g in range(n_grp):
        acc = zero
        for c in range(n_grp):
            acc = acc + jnp.where(rank_cols[c] == lane + g * LANES, firsts[c] * cols[c], 0.0)
        meta[n_grp + g:n_grp + g + 1, :] = fold(acc).astype(jnp.int32)
    cut = cut_ref[...].astype(F32)
    acc = zero
    for c in range(n_grp):
        acc = acc + jnp.where(cols[c] < cut, firsts[c], 0.0)
    meta[2 * n_grp:3 * n_grp, :] = jnp.broadcast_to(fold(acc), (n_grp, LANES)).astype(jnp.int32)


def logit_grad(e, n_t, shift, lab, first_id, inv_count, scale, dz):
    rows = e.shape[0]
    n_tok = n_t.shape[1]
    blk = 256
    vid = lax.broadcasted_iota(jnp.int32, (rows, blk), 0)
    for j in range(n_tok // blk):
        cols = slice(j * blk, (j + 1) * blk)
        z = (dot(e, n_t[:, cols]) * scale).astype(BF16).astype(F32)
        prob = jnp.exp2(z * LOG2E - shift[:, cols])
        dz[:, cols] = jnp.where(vid == lab[:, cols] - first_id, prob - inv_count, prob).astype(BF16)


def pipe_kernel(n_stage, plan, x0_hbm, emb_hbm, up_hbm, down_hbm, lab_ref, row_ref, cut_ref,
                n_out, xs_out, hid_out, da_out, g_out, dx0_out, stat_out, tmp_out, meta_out,
                xbuf, ybuf, abuf, hbuf, nbuf, gbuf, dxbuf, dx0buf, dnbuf, up, down, up_t, down_t,
                emb, zbuf, n_t, dn_acc, dn_send, dn_recv, dn_own, st_send, st_recv, statall, tops, n_all_t, shift, dz, obuf, z_pair, meta,
                w_sem, e_sem, x_sem, f_send, f_recv, n_send, n_recv, nf_send, ag_send, ag_recv, fw_send,
                st_sems, dp_sems, dn_ssem, dn_rsem, sa_send, sa_recv, b_send, b_recv, d_send, d_recv, r_send, rf_send, out_sem, x_send, o_sem, od_send, od_recv):
    n_micro, seq, dim = xbuf.shape
    n_tok = n_micro * seq
    ffn = up.shape[1]
    vocab = emb_hbm.shape[0]
    me = lax.axis_index("stage")
    core = lax.rem(me, 2)
    chip = me // 2
    mate = me + 1 - 2 * core
    last_id = n_stage - 1
    first = me == 0
    last = me == last_id
    fblk = 512
    n_fblk = ffn // fblk
    base, extra, tile = plan.base, plan.extra, plan.head_tile
    row0 = core * (base + extra)
    n_tiles = base // tile

    barrier = pltpu.get_barrier_semaphore()
    for d in range(1, n_stage):
        pl.semaphore_signal(barrier, inc=1, device_id={"stage": lax.rem(me + d, n_stage)}, device_id_type=MESH)
    w_copy = [pltpu.make_async_copy(up_hbm, up, w_sem.at[0]), pltpu.make_async_copy(down_hbm, down, w_sem.at[1])]
    for c in w_copy:
        c.start()
    x_slots = x0_hbm.shape[0]
    x_mine = [head_chunk(me, k, n_micro) for k in range(x_slots)]

    @pl.when(first)
    def _():
        for k in range(x_slots):
            pltpu.make_async_copy(x0_hbm.at[k], xbuf.at[k], x_sem.at[k]).start()

    e_parts = e_sem.shape[0] - 1
    e_step = base // e_parts

    def e_copy(i):
        src = emb_hbm.at[pl.ds(pl.multiple_of(row0 + i * e_step, 16), e_step)]
        return pltpu.make_async_copy(src, emb.at[pl.ds(i * e_step, e_step)], e_sem.at[i])

    e_more = pltpu.make_async_copy(emb_hbm.at[pl.ds(base, extra)], emb.at[pl.ds(base, extra)], e_sem.at[e_parts])
    with jax.named_scope("entry"):
        pl.semaphore_wait(barrier, n_stage - 1)

    def x_copy(k):
        return remote(x0_hbm.at[k], xbuf.at[x_mine[k]], x_send.at[k], f_recv.at[x_mine[k]], 0)

    @pl.when(jnp.logical_not(first) & (me + 2 < n_micro))
    def _():
        x_copy(0).start()

        @pl.when(me < 2)
        def _():
            x_copy(1).start()

    with jax.named_scope("w_wait"):
        for c in w_copy:
            c.wait()
        for i in range(e_parts):
            e_copy(i).start()
        pl.when(core == 0)(e_more.start)

    def transpose_weights():
        for j in range(n_fblk):
            up_t[j * fblk:(j + 1) * fblk, :] = up[:, j * fblk:(j + 1) * fblk].T
            down_t[:, j * fblk:(j + 1) * fblk] = down[j * fblk:(j + 1) * fblk, :].T

    @pl.when(chip >= n_stage // 4)
    def _():
        transpose_weights()

    def n_copy(m):
        return remote(nbuf.at[m], nbuf.at[m], n_send.at[m], n_recv.at[m], jnp.where(m == last_id, last_id - 1, m))

    def fwd(m, carry):
        local = first & (m < x_slots)

        with jax.named_scope("fwd_wait"):
            @pl.when(local)
            def _():
                pltpu.make_async_copy(x0_hbm.at[m], xbuf.at[m], x_sem.at[m]).wait()

            @pl.when(jnp.logical_not(local))
            def _():
                remote(xbuf.at[m], xbuf.at[m], f_send.at[m], f_recv.at[m], me).wait_recv()

        with jax.named_scope("fwd_comp"):
            x = xbuf[m]
            for j in range(n_fblk):
                cols = slice(j * fblk, (j + 1) * fblk)
                a = dot(x, up[:, cols]).astype(BF16)
                abuf[m, :, cols] = a
                hbuf[m, :, cols] = gelu_fwd(a.astype(F32)).astype(BF16)
            y = (x.astype(F32) + dot(hbuf[m], down[...])).astype(BF16)
            ybuf[m] = y

        @pl.when(jnp.logical_not(last))
        def _():
            remote(ybuf.at[m], xbuf.at[m], f_send.at[m], f_recv.at[m], me + 1).start()

        @pl.when(last)
        def _():
            yf = y.astype(F32)
            inv = lax.rsqrt(jnp.mean(yf * yf, axis=-1, keepdims=True) + EPS)
            nbuf[m] = (yf * inv).astype(BF16)
            n_copy(m).start()

        pltpu.make_async_copy(hbuf.at[m], hid_out.at[m], out_sem.at[0, m]).start()
        pltpu.make_async_copy(xbuf.at[m], xs_out.at[m], out_sem.at[1, m]).start()
        return carry

    lax.fori_loop(0, n_micro, fwd, 0)

    @pl.when(chip < n_stage // 4)
    def _():
        transpose_weights()

    n_forward = remote(nbuf.at[me], nbuf.at[me], nf_send, n_recv.at[me], mate)
    with jax.named_scope("n_wait"):

        @pl.when(jnp.logical_not(last))
        def _():
            remote(nbuf.at[me], nbuf.at[me], n_send.at[me], n_recv.at[me], me).wait_recv()
            pl.when(mate != last_id)(n_forward.start)
            remote(nbuf.at[mate], nbuf.at[mate], n_send.at[mate], n_recv.at[mate], me).wait_recv()

        for k in range(2):
            n_t[:, k * seq:(k + 1) * seq] = nbuf[2 * chip + k].T

    peers = [lax.rem(me + 2 * d, n_stage) for d in range(1, n_stage // 2)]
    ag_copies = [remote(nbuf.at[me], nbuf.at[me], ag_send.at[d], ag_recv.at[me], p) for d, p in enumerate(peers)]
    for c, p in zip(ag_copies, peers):
        pl.when(p != last_id)(c.start)
    with jax.named_scope("e_wait"):
        for i in range(e_parts):
            e_copy(i).wait()
        pl.when(core == 0)(e_more.wait)

    pair = 2 * seq
    scale = dim ** -0.5
    inv_count = 1.0 / n_tok
    log_count = math.log2(n_tok)
    lab = lab_ref[:, pl.ds(pl.multiple_of(chip * pair, pair), pair)]

    def logits(rows, size):
        e = emb[rows, :]
        parts = [dot(e[k * size // 2:(k + 1) * size // 2], n_t[...]) for k in range(2)]
        z = jnp.concatenate([(p * scale).astype(BF16) for p in parts], axis=0)
        zbuf[rows, :] = z
        return z

    def peak(z, size, top):
        best = jnp.max(z.reshape(size // 16, 16, pair), axis=0).astype(F32)
        return jnp.maximum(top, jnp.maximum(best[:8], best[8:]))

    def total(z, size, old, top, tot):
        off = top * LOG2E
        return tot * jnp.exp2(old * LOG2E - off) + jnp.sum(jnp.exp2(z.astype(F32).reshape(size // 8, 8, pair) * LOG2E - off[None]), axis=0)

    tops[0] = jnp.full((8, pair), -jnp.inf, F32)
    tops[1] = jnp.zeros((8, pair), F32)

    @pl.when(core == 0)
    def _():
        z = logits(pl.ds(base, extra), extra)
        top = peak(z, extra, tops[0])
        tops[1] = total(z, extra, tops[0], top, tops[1])
        tops[0] = top

    def logits_step(i, slot, old, top, tot):
        z = logits(pl.ds(pl.multiple_of(i * tile, 16), tile), tile)
        tot = total(z_pair[1 - slot], tile, old, top, tot)
        z_pair[slot] = z
        return top, peak(z, tile, top), tot

    with jax.named_scope("logits"):
        z = logits(pl.ds(0, tile), tile)
        z_pair[0] = z
        state = (tops[0], peak(z, tile, tops[0]), tops[1])
        state = lax.fori_loop(0, (n_tiles - 1) // 2, lambda i, c: logits_step(2 * i + 2, 0, *logits_step(2 * i + 1, 1, *c)), state)
        if n_tiles % 2 == 0:
            state = logits_step(n_tiles - 1, 1, *state)
        old, top, tot = state
        tot = total(z_pair[(n_tiles - 1) % 2], tile, old, top, tot)
    row_top = jnp.max(top, axis=0, keepdims=True)
    row_tot = jnp.sum(tot * jnp.exp2((top - row_top) * LOG2E), axis=0, keepdims=True)
    st_send[0:8, :] = jnp.broadcast_to(row_top, (8, pair))
    st_send[8:16, :] = jnp.broadcast_to(row_tot, (8, pair))
    st_copy = remote(st_send, st_recv, st_sems.at[0], st_sems.at[1], mate)
    with jax.named_scope("stat_x"):
        st_copy.start()
        st_copy.wait()
    far_top = st_recv[0:1, :]
    far_tot = st_recv[8:9, :]
    all_top = jnp.maximum(row_top, far_top)
    mine = row_tot * jnp.exp(row_top - all_top)
    other = far_tot * jnp.exp(far_top - all_top)
    lse = all_top + jnp.log(jnp.where(core == 0, mine + other, other + mine))
    my_shift = lse * LOG2E + log_count

    def grads(rows, size, first_row, picked):
        zf = zbuf[rows, :].astype(F32)
        prob = jnp.exp2(zf * LOG2E - my_shift)
        hit = lax.broadcasted_iota(jnp.int32, (size, pair), 0) == lab - (row0 + first_row)
        dz_t = jnp.where(hit, prob - inv_count, prob).astype(BF16)
        got = jnp.where(hit, zf, 0.0).reshape(size // 8, 8, pair)
        return dot_t(dz_t, emb[rows, :]), picked + jnp.sum(got, axis=0)

    tops[0] = jnp.zeros((8, pair), F32)
    dn_acc[...] = jnp.zeros_like(dn_acc)

    @pl.when(core == 0)
    def _():
        dn_acc[...], tops[0] = grads(pl.ds(base, extra), extra, base, tops[0])

    def grad_step(i, picked):
        part, picked = grads(pl.ds(pl.multiple_of(i * tile, 16), tile), tile, i * tile, picked)
        dn_acc[...] += part
        return picked

    with jax.named_scope("grads"):
        picked = lax.fori_loop(0, n_tiles, grad_step, tops[0])
    far = pl.ds(pl.multiple_of((1 - core) * seq, seq), seq)
    near = pl.ds(pl.multiple_of(core * seq, seq), seq)
    dn_send[...] = dn_acc[far, :]
    dp_copy = remote(dn_send, dn_recv, dp_sems.at[0], dp_sems.at[1], mate)
    dp_copy.start()
    row_loss = jnp.where(core == 0, lse, 0.0) - jnp.sum(picked, axis=0, keepdims=True)
    pick = lax.broadcasted_iota(jnp.int32, (8, pair), 0)
    statall[me] = jnp.where(pick == 0, lse, jnp.where(pick == 1, row_loss, 0.0))
    sa_copies = [remote(statall.at[me], statall.at[me], sa_send.at[d - 1], sa_recv.at[me], lax.rem(me + d, n_stage)) for d in range(1, n_stage)]
    for c in sa_copies:
        c.start()
    with jax.named_scope("dn_x"):
        dp_copy.wait()
        dn = ((dn_acc[near, :] + dn_recv[...]) * scale).astype(BF16)
    dn_copy = remote(dn_own, dnbuf.at[me], dn_ssem, dn_rsem.at[me], last_id)

    @pl.when(last)
    def _():
        dnbuf[last_id] = dn

    @pl.when(jnp.logical_not(last))
    def _():
        dn_own[...] = dn
        dn_copy.start()

    with jax.named_scope("ag_wait"):
        for p in peers:
            got = remote(nbuf.at[p], nbuf.at[p], ag_send.at[0], ag_recv.at[p], me)
            pl.when(jnp.logical_not(last))(got.wait_recv)
            pl.when(mate != last_id)(remote(nbuf.at[p], nbuf.at[p], fw_send.at[p], ag_recv.at[p], mate).start)

    near_dst = [1, 2, n_stage - 2]
    far_dst = n_stage // 2
    n_relay = (n_micro - 2) // 2

    def dx0_copies(m):
        return [remote(dxbuf.at[m], dx0buf.at[m], d_send.at[m, k], d_recv.at[m], dev) for k, dev in enumerate(near_dst + [far_dst])]

    def relayed(m):
        return (m < 2 * n_relay) & (((me == 2) & (lax.rem(m, 2) == 0)) | ((me == n_stage - 2) & (lax.rem(m, 2) == 1)))

    def relay_far(m):
        return remote(dx0buf.at[m], dx0buf.at[m], rf_send.at[m], d_recv.at[m], far_dst)

    def bwd(m):
        with jax.named_scope("bwd_wait"):
            @pl.when(jnp.logical_not(last))
            def _():
                remote(gbuf.at[m], gbuf.at[m], b_send.at[m], b_recv.at[m], me).wait_recv()

            @pl.when(last)
            def _():
                @pl.when(m != last_id)
                def _():
                    remote(dnbuf.at[m], dnbuf.at[m], dn_ssem, dn_rsem.at[m], me).wait_recv()

                yf = ybuf[m].astype(F32)
                inv = lax.rsqrt(jnp.mean(yf * yf, axis=-1, keepdims=True) + EPS)
                dnf = dnbuf[m].astype(F32)
                proj = jnp.mean(yf * dnf, axis=-1, keepdims=True)
                gbuf[m] = (dnf * inv - yf * (inv * inv * inv * proj)).astype(BF16)

        with jax.named_scope("bwd_comp"):
            g = gbuf[m]
            for j in range(n_fblk):
                cols = slice(j * fblk, (j + 1) * fblk)
                dh = dot(g, down_t[:, cols]).astype(BF16).astype(F32)
                abuf[m, :, cols] = (dh * gelu_slope(abuf[m, :, cols].astype(F32))).astype(BF16)
            dxbuf[m] = (g.astype(F32) + dot(abuf[m], up_t[...])).astype(BF16)

        @pl.when(jnp.logical_not(first))
        def _():
            remote(dxbuf.at[m], gbuf.at[m], b_send.at[m], b_recv.at[m], me - 1).start()

        @pl.when(first)
        def _():
            copies = dx0_copies(m)
            for c in copies[:-1]:
                c.start()
            pl.when(m >= 2 * n_relay)(copies[-1].start)

        pltpu.make_async_copy(abuf.at[m], da_out.at[m], out_sem.at[2, m]).start()
        pltpu.make_async_copy(gbuf.at[m], g_out.at[m], out_sem.at[3, m]).start()

    def tile_copy(k):
        rows = pl.ds(pl.multiple_of(k * plan.rows, plan.rows), plan.rows)
        slot = lax.rem(k, 2)
        return pltpu.make_async_copy(obuf.at[slot], tmp_out.at[core, rows], o_sem.at[slot])

    def piece(p):
        rows = pl.ds(pl.multiple_of(p * plan.piece, plan.piece), plan.piece)
        return remote(tmp_out.at[core, rows], tmp_out.at[core, rows], od_send.at[p], od_recv.at[p], mate)

    def piece_in(p):
        rows = pl.ds(pl.multiple_of(p * plan.piece, plan.piece), plan.piece)
        return remote(tmp_out.at[1 - core, rows], tmp_out.at[1 - core, rows], od_send.at[p], od_recv.at[p], me)

    def emb_tile(k):
        with jax.named_scope("tile_prep"):

            @pl.when(k == 0)
            def _():
                for d in range(1, n_stage // 2):
                    src = lax.rem(mate + 2 * d, n_stage)
                    pl.when(jnp.logical_not(last))(remote(nbuf.at[src], nbuf.at[src], ag_send.at[0], ag_recv.at[src], me).wait_recv)
                token_table(row_ref, jnp.where(core == 0, cut_ref[0:1, :], cut_ref[1:2, :]), meta)
                for m in range(n_micro):
                    n_all_t[:, m * seq:(m + 1) * seq] = nbuf[m].T
                for d in range(1, n_stage):
                    src = lax.rem(me + d, n_stage)
                    remote(statall.at[src], statall.at[src], sa_send.at[0], sa_recv.at[src], me).wait_recv()
                for c in range(n_stage // 2):
                    shift[:, c * pair:(c + 1) * pair] = statall[2 * c, 0:1, :] * LOG2E + log_count

        slot = lax.rem(k, 2)
        with jax.named_scope("tile"):
            rows = pl.ds(pl.multiple_of(k * plan.rows, plan.rows), plan.rows)
            logit_grad(emb[rows, :], n_all_t, shift, lab_ref, row0 + k * plan.rows, inv_count, scale, dz)
            obuf[slot] = dot(dz[...], nbuf[...].reshape(n_tok, dim)) * scale

        @pl.when(k >= 1)
        def _():
            tile_copy(k - 1).wait()

        tile_copy(k).start()

    def send_pieces(done, until):
        lax.fori_loop(done, until, lambda p, c: (piece(p).start(), c)[1], 0)
        return jnp.maximum(done, until)

    before = sum(jnp.where(me == s, plan.before[s], 0) for s in range(n_stage))

    def pass_dx0(m, carry):
        @pl.when(jnp.logical_not(first))
        def _():
            remote(dx0buf.at[m], dx0buf.at[m], r_send.at[m], d_recv.at[m], me).wait_recv()

            @pl.when(core == 0)
            def _():
                remote(dx0buf.at[m], dx0buf.at[m], r_send.at[m], d_recv.at[m], mate).start()

            @pl.when(relayed(m))
            def _():
                relay_far(m).start()

            pltpu.make_async_copy(dx0buf.at[m], dx0_out.at[m], out_sem.at[4, m]).start()

        @pl.when(first)
        def _():
            pltpu.make_async_copy(dxbuf.at[m], dx0_out.at[m], out_sem.at[4, m]).start()

        return carry

    lead = jnp.where(me == 2, -150, jnp.where(me == n_stage - 2, -1500, jnp.where(me == far_dst, -1550, -10**6)))

    def work(i, carry):
        sent, passed = carry
        chunk = (i >= before) & (i < before + n_micro)
        pl.when(chunk)(lambda: bwd(i - before))
        k = jnp.where(i < before, i, i - n_micro)
        pl.when(jnp.logical_not(chunk))(lambda: emb_tile(k))
        after = i - before - n_micro + 1
        here = jnp.where(after > 0, jnp.clip((after * 257 + lead) // 146, 0, n_micro), 0)
        lax.fori_loop(passed, here, pass_dx0, 0)
        ready = jnp.where(i < before, i, jnp.where(chunk, before - 1, i - n_micro)) * plan.per_tile
        near_chunks = chunk | ((i < before) & (i + 1 >= before))
        until = jnp.minimum(jnp.minimum(ready, plan.shared * plan.per_tile), sent + jnp.where(near_chunks, 1, 3))
        return send_pieces(sent, until), jnp.maximum(passed, here)

    sent, passed = lax.fori_loop(0, plan.tiles + n_micro, work, (0, 0))
    outs = [pltpu.make_async_copy(nbuf, n_out, out_sem.at[5, 0]), pltpu.make_async_copy(statall, stat_out, out_sem.at[5, 1]), pltpu.make_async_copy(meta, meta_out, out_sem.at[5, 2])]
    for c in outs:
        c.start()
    with jax.named_scope("relay_all"):
        lax.fori_loop(passed, n_micro, pass_dx0, 0)

    with jax.named_scope("last_tile"):
        tile_copy(plan.tiles - 1).wait()
        send_pieces(sent, plan.shared * plan.per_tile)

    with jax.named_scope("drain"):
        for p in range(plan.shared * plan.per_tile):
            piece(p).wait_send()
            piece_in(p).wait_recv()
        for m in range(2 * n_relay):
            pl.when(relayed(m))(relay_far(m).wait_send)
        for c in sa_copies:
            c.wait_send()
        for c, p in zip(ag_copies, peers):
            pl.when(p != last_id)(c.wait_send)
            pl.when(mate != last_id)(remote(nbuf.at[p], nbuf.at[p], fw_send.at[p], ag_recv.at[p], mate).wait_send)

        @pl.when(jnp.logical_not(last))
        def _():
            dn_copy.wait_send()
            pl.when(mate != last_id)(n_forward.wait_send)

        @pl.when(jnp.logical_not(first) & (me + 2 < n_micro))
        def _():
            x_copy(0).wait_send()

            @pl.when(me < 2)
            def _():
                x_copy(1).wait_send()

        def drain(m, carry):
            @pl.when(jnp.logical_not(last))
            def _():
                remote(ybuf.at[m], xbuf.at[m], f_send.at[m], f_recv.at[m], me).wait_send()

            @pl.when(last)
            def _():
                n_copy(m).wait_send()

            @pl.when(jnp.logical_not(first))
            def _():
                remote(dxbuf.at[m], gbuf.at[m], b_send.at[m], b_recv.at[m], me).wait_send()

                @pl.when(core == 0)
                def _():
                    remote(dx0buf.at[m], dx0buf.at[m], r_send.at[m], d_recv.at[m], me).wait_send()

            @pl.when(first)
            def _():
                copies = dx0_copies(m)
                for c in copies[:-1]:
                    c.wait_send()
                pl.when(m >= 2 * n_relay)(copies[-1].wait_send)

            pltpu.make_async_copy(hbuf.at[m], hid_out.at[m], out_sem.at[0, m]).wait()
            pltpu.make_async_copy(xbuf.at[m], xs_out.at[m], out_sem.at[1, m]).wait()
            pltpu.make_async_copy(abuf.at[m], da_out.at[m], out_sem.at[2, m]).wait()
            pltpu.make_async_copy(gbuf.at[m], g_out.at[m], out_sem.at[3, m]).wait()
            pltpu.make_async_copy(dx0buf.at[m], dx0_out.at[m], out_sem.at[4, m]).wait()
            return carry

        lax.fori_loop(0, n_micro, drain, 0)
        for c in outs:
            c.wait()


class Plan:
    def __init__(self, vocab, n_stage):
        units = vocab // LANES
        self.base = units // 2 * LANES
        self.extra = vocab - 2 * self.base
        self.head_tile = next(t for t in (1600, 1536, 1280, 1024, 768, 640, 512, 256, 128) if self.base % t == 0)
        self.rows = 1024
        self.tiles, self.shared = 10, 7
        self.piece = 256
        self.per_tile = self.rows // self.piece
        measured = [8, 7, 6, 5, 2, 1, 0, 0]
        self.before = (measured + [0] * n_stage)[:n_stage]
        mid = self.base + self.extra
        ends = [(0, mid), (mid, vocab)]
        early = (self.tiles * self.rows, self.shared * self.rows)
        self.spans = [[(ends[h][0] + early[0 if h == c else 1], ends[h][1]) for h in (c, 1 - c)] for c in range(2)]
        self.longest = [max(self.spans[c][k][1] - self.spans[c][k][0] for c in range(2)) for k in range(2)]
        best = min(range(16, 1281, 16), key=lambda r: (sum(-(-n // r) for n in self.longest)) * (r + 40))
        self.calc_rows = best
        self.calc_steps = [-(-n // best) for n in self.longest]
        self.steps = sum(self.calc_steps)
        self.copy_rows = self.rows
        self.copies = self.tiles + self.shared
        self.starts = ends

    def calc_start(self, core, s):
        k = 0 if s < self.calc_steps[0] else 1
        lo, hi = self.spans[core][k]
        return min(lo + (s - k * self.calc_steps[0]) * self.calc_rows, hi - self.calc_rows)

    def copy_start(self, core, c):
        own = c < self.tiles
        h = core if own else 1 - core
        return self.starts[h][0] + (c if own else c - self.tiles) * self.copy_rows

    def cuts(self, core):
        firsts = [(self.calc_start(core, s), self.calc_rows) for s in range(self.steps)] + [(self.copy_start(core, c), self.copy_rows) for c in range(self.copies)]
        flat = [v for lo, rows in firsts for v in (lo, lo + rows)]
        return flat + [0] * (LANES - len(flat))


def run_pipe(x0, emb, w_up, w_down, labels, tokens, cuts, n_stage, plan):
    n_micro, seq = labels.shape
    dim, ffn = w_up.shape
    n_tok = n_micro * seq
    base = plan.base
    e_parts = next(k for k in (10, 8, 5, 4, 2, 1) if base % (16 * k) == 0)
    any_spec = pl.BlockSpec(memory_space=pl.ANY)
    act = (n_micro, seq, dim)
    wide = (n_micro, seq, ffn)
    dma = pltpu.SemaphoreType.DMA
    vm = pltpu.VMEM
    pair = 2 * seq
    return pl.pallas_call(
        functools.partial(pipe_kernel, n_stage, plan),
        out_shape=[
            jax.ShapeDtypeStruct(act, BF16), jax.ShapeDtypeStruct(act, BF16), jax.ShapeDtypeStruct(wide, BF16),
            jax.ShapeDtypeStruct(wide, BF16), jax.ShapeDtypeStruct(act, BF16), jax.ShapeDtypeStruct(act, BF16),
            jax.ShapeDtypeStruct((n_stage, 8, pair), F32), jax.ShapeDtypeStruct((2, plan.tiles * plan.rows, dim), F32),
            jax.ShapeDtypeStruct((3 * n_tok // LANES, LANES), jnp.int32),
        ],
        in_specs=[any_spec] * 4 + [pl.BlockSpec(memory_space=pltpu.VMEM)] * 3,
        out_specs=[any_spec] * 9,
        scratch_shapes=[
            vm(act, BF16), vm(act, BF16), vm(wide, BF16), vm(wide, BF16), vm(act, BF16), vm(act, BF16), vm(act, BF16), vm(act, BF16), vm(act, BF16),
            vm((dim, ffn), BF16), vm((ffn, dim), BF16), vm((ffn, dim), BF16), vm((dim, ffn), BF16),
            vm((base + plan.extra, dim), BF16), vm((base + plan.extra, pair), BF16), vm((dim, pair), BF16), vm((pair, dim), F32),
            vm((seq, dim), F32), vm((seq, dim), F32), vm((seq, dim), BF16), vm((16, pair), F32), vm((16, pair), F32), vm((n_stage, 8, pair), F32),
            vm((2, 8, pair), F32), vm((dim, n_tok), BF16), vm((1, n_tok), F32), vm((plan.rows, n_tok), BF16), vm((2, plan.rows, dim), F32),
            vm((2, plan.head_tile, pair), BF16), vm((3 * n_tok // LANES, LANES), jnp.int32),
            dma((2,)), dma((e_parts + 1,)), dma((n_micro,)), dma((n_micro,)), dma((n_micro,)), dma((n_micro,)), dma((n_micro,)), dma,
            dma((n_stage,)), dma((n_stage,)), dma((n_stage,)),
            dma((2,)), dma((2,)), dma, dma((n_stage,)), dma((n_stage,)), dma((n_stage,)),
            dma((n_micro,)), dma((n_micro,)), dma((n_micro, 4)), dma((n_micro,)), dma((n_micro,)), dma((n_micro,)), dma((6, n_micro)),
            dma((2,)), dma((2,)), dma((plan.shared * plan.per_tile,)), dma((plan.shared * plan.per_tile,)),
        ],
        compiler_params=pltpu.CompilerParams(collective_id=0, has_side_effects=True, vmem_limit_bytes=67_000_000),
        cost_estimate=pl.CostEstimate(flops=60 * 10**9, bytes_accessed=100 * 10**6, transcendentals=0),
        name="pipe",
    )(x0, emb, w_up, w_down, labels.reshape(1, n_tok), tokens.reshape(1, n_tok), cuts)


def fin_kernel(n_stage, n_tok, plan, ids_ref, emb_hbm, tmp_hbm, n_hbm, stat_ref, lab_ref, meta_ref, dx0_hbm, xs_hbm, hid_hbm, da_hbm, g_hbm,
               out_hbm, loss_ref, gup_hbm, gdown_hbm,
               n_all, dx0, xs, hid, da, g, n_t, x_t, dx0s, dz, shift, e_in, c_out, cp, gup, gdown,
               ld_sem, e_sem, t_sem, co_sem, po_sem, gu_sem, gd_sem, wi_sem):
    dim, ffn = gup_hbm.shape
    scale = dim ** -0.5
    inv_count = 1.0 / n_tok
    steps, crows, prows = plan.steps, plan.calc_rows, plan.copy_rows
    core = lax.rem(lax.axis_index("stage"), 2)
    early = plan.tiles * prows
    wblk = gup.shape[2]
    n_wblk = ffn // wblk
    turn = plan.calc_steps[0]

    def pick(pair):
        return jnp.where(core == 0, pair[0], pair[1])

    def calc_start(s):
        own = s < turn
        lo, hi = [jnp.where(own, pick([plan.spans[c][0][e] for c in range(2)]), pick([plan.spans[c][1][e] for c in range(2)])) for e in range(2)]
        return pl.multiple_of(jnp.minimum(lo + (s - jnp.where(own, 0, turn)) * crows, hi - crows), 16)

    def copy_start(c):
        own = c < plan.tiles
        first = jnp.where(own, pick([plan.starts[0][0], plan.starts[1][0]]), pick([plan.starts[1][0], plan.starts[0][0]]))
        return pl.multiple_of(first + (c - jnp.where(own, 0, plan.tiles)) * prows, 16)

    def e_copy(s):
        return pltpu.make_async_copy(emb_hbm.at[pl.ds(calc_start(s), crows)], e_in.at[lax.rem(s, 2)], e_sem.at[lax.rem(s, 2)])

    n_slot = cp.shape[0]
    ahead = 3

    def t_copy(c):
        own = c < plan.tiles
        row = jnp.where(own, core, 1 - core) * early + (c - jnp.where(own, 0, plan.tiles)) * prows
        slot = lax.rem(c, n_slot)
        return pltpu.make_async_copy(tmp_hbm.at[pl.ds(pl.multiple_of(row, 16), prows)], cp.at[slot], t_sem.at[slot])

    def p_out(c):
        slot = lax.rem(c, n_slot)
        return pltpu.make_async_copy(cp.at[slot], out_hbm.at[pl.ds(copy_start(c), prows)], po_sem.at[slot])

    def c_outs(s):
        slot = lax.rem(s, 2)
        return pltpu.make_async_copy(c_out.at[slot], out_hbm.at[pl.ds(calc_start(s), crows)], co_sem.at[slot])

    loads = [pltpu.make_async_copy(s, d, ld_sem.at[i]) for i, (s, d) in enumerate(((n_hbm, n_all), (dx0_hbm, dx0), (xs_hbm, xs), (g_hbm, g)))]
    loads[0].start()
    loads[1].start()
    e_copy(0).start()
    for c in range(ahead):
        t_copy(c).start(priority=1)
    pair = stat_ref.shape[2]
    loss = jnp.zeros((1, pair), F32)
    for d in range(n_stage):
        if d % 2 == 0:
            shift[:, (d // 2) * pair:(d // 2 + 1) * pair] = stat_ref[d, 0:1, :] * LOG2E + math.log2(n_tok)
        loss = loss + stat_ref[d, 1:2, :]
    loss_ref[0] = jnp.sum(loss) * inv_count
    with jax.named_scope("fin_pre"):
        loads[0].wait()
        n_t[...] = n_all[...].T
        loads[1].wait()
        dense = jnp.concatenate([meta_ref[g:g + 1, :] for g in range(n_tok // LANES)], axis=1)
        order = lax.broadcasted_iota(jnp.int32, (n_tok, n_tok), 0) == dense
        dx0s[...] = dot(jnp.where(order, 1.0, 0.0).astype(BF16), dx0[...])

    def add_rows(k, start, ref):
        lo, hi = ids_ref[2 * n_tok + k], ids_ref[2 * n_tok + k + 1]
        wide = 8

        def some(p, width):
            at = [pl.ds(ids_ref[n_tok + p + u] - start, 1) for u in range(width)]
            new = [ref[at[u], :] + dx0s[pl.ds(p + u, 1), :] for u in range(width)]
            for u in range(width):
                ref[at[u], :] = new[u]

        def group(g, carry):
            some(lo + g * wide, wide)
            return carry

        def single(p, carry):
            some(p, 1)
            return carry

        n_grp = (hi - lo) // wide
        lax.fori_loop(0, n_grp, group, 0)
        lax.fori_loop(lo + n_grp * wide, hi, single, 0)

    def w_ins(w):
        cols = pl.ds(pl.multiple_of(w * wblk, wblk), wblk)
        wslot = lax.rem(w, 2)
        return (pltpu.make_async_copy(da_hbm.at[:, cols], da.at[wslot], wi_sem.at[0, wslot]), pltpu.make_async_copy(hid_hbm.at[:, cols], hid.at[wslot], wi_sem.at[1, wslot]))

    def w_outs(w):
        cols = pl.ds(pl.multiple_of(w * wblk, wblk), wblk)
        wslot = lax.rem(w, 2)
        return (pltpu.make_async_copy(gup.at[wslot], gup_hbm.at[:, cols], gu_sem.at[wslot]), pltpu.make_async_copy(gdown.at[wslot], gdown_hbm.at[cols], gd_sem.at[wslot]))

    def copy_tile(c, carry):
        with jax.named_scope("copy_wait"):
            t_copy(c).wait()
        with jax.named_scope("add_p"):
            add_rows(2 * steps + 2 * c, copy_start(c), cp.at[lax.rem(c, n_slot)])
        p_out(c).start()

        @pl.when(c + ahead < plan.copies)
        def _():
            pl.when(c + ahead >= n_slot)(lambda: p_out(c + ahead - n_slot).wait())
            t_copy(c + ahead).start(priority=1)

        return carry

    w_first = 2
    tails = [turn - 1, steps - 1]

    def tail(s):
        return (s == tails[0]) | (s == tails[1])

    def step(s, carry):
        pl.when(s + 1 < steps)(lambda: e_copy(s + 1).start())
        lax.fori_loop(s * plan.copies // steps, (s + 1) * plan.copies // steps, copy_tile, 0)
        with jax.named_scope("fin_wait"):
            e_copy(s).wait()

        @pl.when(s == 0)
        def _():
            for c in loads[2:]:
                c.start()

        w = s - w_first

        @pl.when((w + 1 >= 0) & (w + 1 < n_wblk))
        def _():
            for c in w_ins(w + 1):
                c.start()

        pl.when((s >= 2) & jnp.logical_not(tail(s - 1)))(lambda: c_outs(s - 2).wait())
        slot = lax.rem(s, 2)
        start = calc_start(s)
        with jax.named_scope("calc"):
            logit_grad(e_in[slot], n_t, shift, lab_ref, start, inv_count, scale, dz)
            c_out[slot] = dot(dz[...], n_all[...]) * scale
        with jax.named_scope("add_c"):
            add_rows(2 * s, start, c_out.at[slot])
        pl.when(tail(s))(lambda: c_outs(s - 1).wait())
        c_outs(s).start()

        @pl.when(w == 0)
        def _():
            for c in loads[2:]:
                c.wait()
            x_t[...] = xs[...].T

        @pl.when((w >= 0) & (w < n_wblk))
        def _():
            wslot = lax.rem(w, 2)
            with jax.named_scope("dw_wait"):
                for c in w_ins(w):
                    c.wait()

                @pl.when(w >= 2)
                def _():
                    for c in w_outs(w - 2):
                        c.wait()

            with jax.named_scope("dw"):
                gup[wslot] = dot(x_t[...], da[wslot])
                gdown[wslot] = dot_t(hid[wslot], g[...])
            for c in w_outs(w):
                c.start()

        return carry

    lax.fori_loop(0, steps, step, 0)
    with jax.named_scope("fin_drain"):
        for w in range(n_wblk - 2, n_wblk):
            for c in w_outs(w):
                c.wait()
        c_outs(steps - 1).wait()
        for c in range(plan.copies - n_slot, plan.copies):
            p_out(c).wait()


def run_fin(emb, tmp, n_all, stats, labels, meta, dx0, xs, hid, da, g, n_stage, plan):
    vocab, dim = emb.shape
    n_tok, ffn = hid.shape
    vm = pltpu.VMEM
    dma = pltpu.SemaphoreType.DMA
    any_spec = pl.BlockSpec(memory_space=pl.ANY)
    vspec = pl.BlockSpec(memory_space=pltpu.VMEM)
    smem = pl.BlockSpec(memory_space=pltpu.SMEM)
    wblk = 256
    return pl.pallas_call(
        functools.partial(fin_kernel, n_stage, n_tok, plan),
        out_shape=[jax.ShapeDtypeStruct((vocab, dim), F32), jax.ShapeDtypeStruct((1,), F32), jax.ShapeDtypeStruct((dim, ffn), F32), jax.ShapeDtypeStruct((ffn, dim), F32)],
        in_specs=[smem, any_spec, any_spec, any_spec, vspec, vspec, vspec] + [any_spec] * 5,
        out_specs=[any_spec, smem, any_spec, any_spec],
        scratch_shapes=[
            vm((n_tok, dim), BF16), vm((n_tok, dim), BF16), vm((n_tok, dim), BF16), vm((2, n_tok, wblk), BF16), vm((2, n_tok, wblk), BF16), vm((n_tok, dim), BF16),
            vm((dim, n_tok), BF16), vm((dim, n_tok), BF16), vm((n_tok, dim), F32), vm((plan.calc_rows, n_tok), BF16), vm((1, n_tok), F32),
            vm((2, plan.calc_rows, dim), BF16), vm((2, plan.calc_rows, dim), F32), vm((5, plan.copy_rows, dim), F32),
            vm((2, dim, wblk), F32), vm((2, wblk, dim), F32),
            dma((4,)), dma((2,)), dma((5,)), dma((2,)), dma((5,)), dma((2,)), dma((2,)), dma((2, 2)),
        ],
        compiler_params=pltpu.CompilerParams(vmem_limit_bytes=67_000_000),
        cost_estimate=pl.CostEstimate(flops=2 * n_tok * vocab * dim, bytes_accessed=5 * vocab * dim, transcendentals=0),
        name="fin",
    )(meta.reshape(-1), emb, tmp, n_all, stats, labels.reshape(1, n_tok), meta, dx0, xs, hid, da, g)


def solution(mesh):
    n_stage = mesh.shape["stage"]

    def device_fn(tokens, labels, emb, w_up, w_down):
        n_micro, seq = tokens.shape
        vocab, dim = emb.shape
        w_up, w_down = w_up[0], w_down[0]
        n_tok = n_micro * seq
        plan = Plan(vocab, n_stage)
        cuts = jnp.array([plan.cuts(0), plan.cuts(1)], jnp.int32)
        x0 = run_gather(tokens, emb)
        n_all, xs, hid, da, g, dx0, stats, tmp, meta = run_pipe(x0, emb, w_up, w_down, labels, tokens, cuts, n_stage, plan)
        flat = lambda p: p.reshape(n_tok, -1)
        grad_emb, loss, grad_up, grad_down = run_fin(
            emb, tmp.reshape(-1, dim), flat(n_all), stats, labels, meta, flat(dx0), flat(xs), flat(hid), flat(da), flat(g), n_stage, plan
        )
        return loss, grad_up[None], grad_down[None], grad_emb

    return jax.shard_map(device_fn, mesh=mesh, in_specs=(P("dp", None), P("dp", None), P(None, None), P("stage", None, None), P("stage", None, None)), out_specs=(P("dp"), P(("dp", "stage"), None, None), P(("dp", "stage"), None, None), P("dp", None)), check_vma=False)
```

```python
import functools
import math

import jax
import jax.numpy as jnp
from jax import lax
from jax.experimental import pallas as pl
from jax.experimental.pallas import tpu as pltpu
from jax.sharding import PartitionSpec as P


MESH = pl.DeviceIdType.MESH
LOG2E = math.log2(math.e)
LN2 = math.log(2.0)
GELU_C = math.sqrt(2.0 / math.pi)
GELU_K = 0.044715
EPS = 1e-6
LANES = 128
F32 = jnp.float32
BF16 = jnp.bfloat16


def gelu_fwd(a):
    return 0.5 * a * (1.0 + jnp.tanh(GELU_C * (a + GELU_K * (a * a * a))))


def gelu_slope(a):
    a2 = a * a
    t = jnp.tanh(GELU_C * (a + GELU_K * (a2 * a)))
    return 0.5 * (1.0 + t) + (0.5 * a) * (1.0 - t * t) * (GELU_C + (3.0 * GELU_C * GELU_K) * a2)


def dot(x, y):
    return jnp.dot(x, y, preferred_element_type=F32)


def dot_t(x, y):
    return lax.dot_general(x, y, (((0,), (0,)), ((), ())), preferred_element_type=F32)


def remote(src, dst, send_sem, recv_sem, dev):
    return pltpu.make_async_remote_copy(src_ref=src, dst_ref=dst, send_sem=send_sem, recv_sem=recv_sem, device_id={"stage": dev}, device_id_type=MESH)


def column(row):
    return jnp.broadcast_to(row, (LANES, LANES)).T


def gather_kernel(ids_ref, tok_ref, emb_hbm, x0_hbm, tiles, picked, sem, out_sem):
    n_micro, seq = tok_ref.shape
    me = lax.axis_index("stage")
    group = tiles.shape[1] // seq
    slots = tiles.shape[0]
    owners = [head_chunk(me, k, n_micro) for k in range(slots)]

    def fetch(k):
        def one(i, carry):
            t = ids_ref[owners[k] * seq + i]
            start = pl.multiple_of(t // group * group, group)
            pltpu.make_async_copy(emb_hbm.at[pl.ds(start, group)], tiles.at[k, pl.ds(pl.multiple_of(i * group, group), group)], sem.at[k]).start()
            return carry

        lax.fori_loop(0, seq, one, 0, unroll=8)

    def select(k):
        sub = lax.broadcasted_iota(jnp.int32, (LANES, LANES), 0)
        lane = lax.broadcasted_iota(jnp.int32, (LANES, LANES), 1)
        tok = column(tok_ref[pl.ds(owners[k], 1), :].astype(F32)).astype(jnp.int32)
        want = sub * group + (tok - tok // group * group)
        hot = jnp.concatenate([jnp.where(lane + b * LANES == want, 1.0, 0.0).astype(BF16) for b in range(seq * group // LANES)], axis=1)
        pltpu.make_async_copy(emb_hbm.at[pl.ds(0, seq * group)], tiles.at[k], sem.at[k]).wait()
        picked[k] = dot(hot, tiles[k]).astype(BF16)
        pltpu.make_async_copy(picked.at[k], x0_hbm.at[k], out_sem.at[k]).start()

    def finish(k):
        pltpu.make_async_copy(picked.at[k], x0_hbm.at[k], out_sem.at[k]).wait()

    for work in (fetch, select, finish):
        work(0)
        for k in range(1, slots):
            pl.when(me < slots)(functools.partial(work, k))


def head_chunk(dev, k, n_micro):
    return jnp.minimum(jnp.where(dev < 2, 2 * dev + k, dev + 2), n_micro - 1)


def run_gather(tokens, emb):
    n_micro, seq = tokens.shape
    dim = emb.shape[1]
    group = 16
    return pl.pallas_call(
        gather_kernel,
        out_shape=jax.ShapeDtypeStruct((2, seq, dim), BF16),
        in_specs=[pl.BlockSpec(memory_space=pltpu.SMEM), pl.BlockSpec(memory_space=pltpu.VMEM), pl.BlockSpec(memory_space=pl.ANY)],
        out_specs=pl.BlockSpec(memory_space=pl.ANY),
        scratch_shapes=[pltpu.VMEM((2, seq * group, dim), BF16), pltpu.VMEM((2, seq, dim), BF16), pltpu.SemaphoreType.DMA((2,)), pltpu.SemaphoreType.DMA((2,))],
        cost_estimate=pl.CostEstimate(flops=10**9, bytes_accessed=2 * seq * group * dim * 2, transcendentals=0),
        name="gather",
    )(tokens.reshape(n_micro * seq), tokens, emb)


def token_table(row_ref, cut_ref, meta):
    n_tok = row_ref.shape[1]
    n_grp = n_tok // LANES
    lane = lax.broadcasted_iota(jnp.int32, (LANES, LANES), 1).astype(F32)
    sub = lax.broadcasted_iota(jnp.int32, (LANES, LANES), 0)
    row = lambda g: row_ref[:, g * LANES:(g + 1) * LANES].astype(F32)
    zero = jnp.zeros((LANES, LANES), F32)
    fold = lambda acc: jnp.sum(acc, axis=0, keepdims=True)
    cols = [column(row(c)) for c in range(n_grp)]
    firsts = []
    for g in range(n_grp):
        acc = zero
        for c in range(g + 1):
            same = cols[c] == row(g)
            if c == g:
                same = same & (sub < lane.astype(jnp.int32))
            acc = acc + jnp.where(same, 1.0, 0.0)
        firsts.append(column(jnp.where(fold(acc) == 0.0, 1.0, 0.0)))
    ranks = []
    for g in range(n_grp):
        acc = zero
        for c in range(n_grp):
            acc = acc + jnp.where(cols[c] < row(g), firsts[c], 0.0)
        ranks.append(fold(acc))
        meta[g:g + 1, :] = ranks[g].astype(jnp.int32)
    rank_cols = [column(r) for r in ranks]
    for g in range(n_grp):
        acc = zero
        for c in range(n_grp):
            acc = acc + jnp.where(rank_cols[c] == lane + g * LANES, firsts[c] * cols[c], 0.0)
        meta[n_grp + g:n_grp + g + 1, :] = fold(acc).astype(jnp.int32)
    cut = cut_ref[...].astype(F32)
    acc = zero
    for c in range(n_grp):
        acc = acc + jnp.where(cols[c] < cut, firsts[c], 0.0)
    meta[2 * n_grp:3 * n_grp, :] = jnp.broadcast_to(fold(acc), (n_grp, LANES)).astype(jnp.int32)


def logit_grad(e, n_t, shift, lab, first_id, inv_count, scale, dz):
    rows = e.shape[0]
    n_tok = n_t.shape[1]
    blk = 256
    vid = lax.broadcasted_iota(jnp.int32, (rows, blk), 0)
    for j in range(n_tok // blk):
        cols = slice(j * blk, (j + 1) * blk)
        z = (dot(e, n_t[:, cols]) * scale).astype(BF16).astype(F32)
        prob = jnp.exp2(z * LOG2E - shift[:, cols])
        dz[:, cols] = jnp.where(vid == lab[:, cols] - first_id, prob - inv_count, prob).astype(BF16)


def pipe_kernel(n_stage, plan, x0_hbm, emb_hbm, up_hbm, down_hbm, lab_ref, row_ref, cut_ref,
                n_out, xs_out, hid_out, da_out, g_out, dx0_out, stat_out, tmp_out, meta_out,
                xbuf, ybuf, abuf, hbuf, nbuf, gbuf, dxbuf, dx0buf, dnbuf, up, down, up_t, down_t,
                emb, zbuf, n_t, dn_acc, dn_send, dn_recv, dn_own, st_send, st_recv, statall, tops, n_all_t, shift, dz, obuf, z_pair, meta,
                w_sem, e_sem, x_sem, x_send, x_recv, f_send, f_recv, n_send, n_recv, nf_send, ag_send, ag_recv, fw_send,
                st_sems, dp_sems, dn_ssem, dn_rsem, sa_sems, b_send, b_recv, d_send, d_recv, r_sems, out_sem, o_sem, od_send, od_recv):
    n_micro, seq, dim = gbuf.shape
    part = xbuf.shape[1]
    n_part = xbuf.shape[0]
    per = seq // part
    n_tok = n_micro * seq
    ffn = up.shape[1]
    vocab = emb_hbm.shape[0]
    me = lax.axis_index("stage")
    core = lax.rem(me, 2)
    chip = me // 2
    mate = me + 1 - 2 * core
    last_id = n_stage - 1
    first = me == 0
    last = me == last_id
    fblk = 512
    n_fblk = ffn // fblk
    base, extra, tile = plan.base, plan.extra, plan.head_tile
    row0 = core * (base + extra)
    n_tiles = base // tile

    barrier = pltpu.get_barrier_semaphore()
    for d in range(1, n_stage):
        pl.semaphore_signal(barrier, inc=1, device_id={"stage": lax.rem(me + d, n_stage)}, device_id_type=MESH)
    w_copy = [pltpu.make_async_copy(up_hbm, up, w_sem.at[0]), pltpu.make_async_copy(down_hbm, down, w_sem.at[1])]
    for c in w_copy:
        c.start()
    x_slots = x0_hbm.shape[0]
    x_mine = [head_chunk(me, k, n_micro) for k in range(x_slots)]

    def x_rows(m):
        return xbuf.at[pl.ds(m * per, per)]

    def x_local(k):
        return pltpu.make_async_copy(x0_hbm.at[k], x_rows(k), x_sem.at[k])

    @pl.when(first)
    def _():
        for k in range(x_slots):
            x_local(k).start()

    e_parts = plan.e_parts
    e_step = base // e_parts

    def e_copy(i):
        src = emb_hbm.at[pl.ds(pl.multiple_of(row0 + i * e_step, 16), e_step)]
        return pltpu.make_async_copy(src, emb.at[pl.ds(i * e_step, e_step)], e_sem.at[0])

    e_more = pltpu.make_async_copy(emb_hbm.at[pl.ds(base, extra)], emb.at[pl.ds(base, extra)], e_sem.at[1])
    with jax.named_scope("entry"):
        pl.semaphore_wait(barrier, n_stage - 1)

    def x_copy(k):
        return remote(x0_hbm.at[k], x_rows(x_mine[k]), x_send.at[k], x_recv.at[x_mine[k]], 0)

    @pl.when(jnp.logical_not(first) & (me + 2 < n_micro))
    def _():
        x_copy(0).start()

        @pl.when(me < 2)
        def _():
            x_copy(1).start()

    with jax.named_scope("w_wait"):
        for c in w_copy:
            c.wait()
        for i in range(e_parts):
            e_copy(i).start()
        pl.when(core == 0)(e_more.start)

    def transpose_weights():
        for j in range(n_fblk):
            up_t[j * fblk:(j + 1) * fblk, :] = up[:, j * fblk:(j + 1) * fblk].T
            down_t[:, j * fblk:(j + 1) * fblk] = down[j * fblk:(j + 1) * fblk, :].T

    def idle_work():
        transpose_weights()
        token_table(row_ref, jnp.where(core == 0, cut_ref[0:1, :], cut_ref[1:2, :]), meta)

    @pl.when(chip >= n_stage // 4)
    def _():
        idle_work()

    def n_copy(m):
        return remote(nbuf.at[m], nbuf.at[m], n_send, n_recv.at[m], jnp.where(m == last_id, last_id - 1, m))

    def y_copy(h):
        return remote(ybuf.at[h], xbuf.at[h], f_send, f_recv.at[h], me + 1)

    def fwd(h, carry):
        m = h // per
        sub = lax.rem(h, per)
        rows = pl.ds(pl.multiple_of(sub * part, part), part)
        with jax.named_scope("fwd_wait"):

            @pl.when(first & (sub == 0))
            def _():
                @pl.when(m < x_slots)
                def _():
                    x_local(m).wait()

                @pl.when(m >= x_slots)
                def _():
                    remote(x_rows(m), x_rows(m), x_send.at[0], x_recv.at[m], me).wait_recv()

            @pl.when(jnp.logical_not(first))
            def _():
                remote(xbuf.at[h], xbuf.at[h], f_send, f_recv.at[h], me).wait_recv()

        with jax.named_scope("fwd_comp"):
            x = xbuf[h]
            for j in range(n_fblk):
                cols = slice(j * fblk, (j + 1) * fblk)
                a = dot(x, up[:, cols]).astype(BF16)
                abuf[m, rows, cols] = a
                hbuf[m, rows, cols] = gelu_fwd(a.astype(F32)).astype(BF16)
            y = (x.astype(F32) + dot(hbuf[m, rows, :], down[...])).astype(BF16)
            ybuf[h] = y

        @pl.when(jnp.logical_not(last))
        def _():
            y_copy(h).start()

        @pl.when(last)
        def _():
            yf = y.astype(F32)
            inv = lax.rsqrt(jnp.mean(yf * yf, axis=-1, keepdims=True) + EPS)
            nbuf[m, rows, :] = (yf * inv).astype(BF16)
            pl.when(sub == per - 1)(n_copy(m).start)

        @pl.when(sub == per - 1)
        def _():
            pltpu.make_async_copy(hbuf.at[m], hid_out.at[m], out_sem.at[0]).start()
            pltpu.make_async_copy(x_rows(m), xs_out.at[pl.ds(m * per, per)], out_sem.at[1]).start()

        return carry

    lax.fori_loop(0, n_part, fwd, 0)

    @pl.when(chip < n_stage // 4)
    def _():
        idle_work()

    n_forward = remote(nbuf.at[me], nbuf.at[me], nf_send, n_recv.at[me], mate)
    with jax.named_scope("n_wait"):

        @pl.when(jnp.logical_not(last))
        def _():
            remote(nbuf.at[me], nbuf.at[me], n_send, n_recv.at[me], me).wait_recv()
            pl.when(mate != last_id)(n_forward.start)
            remote(nbuf.at[mate], nbuf.at[mate], n_send, n_recv.at[mate], me).wait_recv()

        for k in range(2):
            n_t[:, k * seq:(k + 1) * seq] = nbuf[2 * chip + k].T

    peers = [lax.rem(me + 2 * d, n_stage) for d in range(1, n_stage // 2)]
    ag_copies = [remote(nbuf.at[me], nbuf.at[me], ag_send.at[d], ag_recv.at[me], p) for d, p in enumerate(peers)]
    for c, p in zip(ag_copies, peers):
        pl.when(p != last_id)(c.start)
    with jax.named_scope("e_wait"):
        pltpu.make_async_copy(emb_hbm.at[pl.ds(0, base)], emb.at[pl.ds(0, base)], e_sem.at[0]).wait()
        pl.when(core == 0)(e_more.wait)

    pair = 2 * seq
    scale = dim ** -0.5
    inv_count = 1.0 / n_tok
    log_count = math.log2(n_tok)
    lab = lab_ref[:, pl.ds(pl.multiple_of(chip * pair, pair), pair)]

    def logits(rows, size):
        e = emb[rows, :]
        parts = [dot(e[k * size // 2:(k + 1) * size // 2], n_t[...]) for k in range(2)]
        z = jnp.concatenate([(p * scale).astype(BF16) for p in parts], axis=0)
        zbuf[rows, :] = z
        return z

    def peak(z, size, top):
        best = jnp.max(z.reshape(size // 16, 16, pair), axis=0).astype(F32)
        return jnp.maximum(top, jnp.maximum(best[:8], best[8:]))

    def total(z, size, old, top, tot):
        off = top * LOG2E
        return tot * jnp.exp2(old * LOG2E - off) + jnp.sum(jnp.exp2(z.astype(F32).reshape(size // 8, 8, pair) * LOG2E - off[None]), axis=0)

    tops[0] = jnp.full((8, pair), -jnp.inf, F32)
    tops[1] = jnp.zeros((8, pair), F32)

    @pl.when(core == 0)
    def _():
        z = logits(pl.ds(base, extra), extra)
        top = peak(z, extra, tops[0])
        tops[1] = total(z, extra, tops[0], top, tops[1])
        tops[0] = top

    def logits_step(i, slot, old, top, tot):
        z = logits(pl.ds(pl.multiple_of(i * tile, 16), tile), tile)
        tot = total(z_pair[1 - slot], tile, old, top, tot)
        z_pair[slot] = z
        return top, peak(z, tile, top), tot

    with jax.named_scope("logits"):
        z = logits(pl.ds(0, tile), tile)
        z_pair[0] = z
        state = (tops[0], peak(z, tile, tops[0]), tops[1])
        state = lax.fori_loop(0, (n_tiles - 1) // 2, lambda i, c: logits_step(2 * i + 2, 0, *logits_step(2 * i + 1, 1, *c)), state)
        if n_tiles % 2 == 0:
            state = logits_step(n_tiles - 1, 1, *state)
        old, top, tot = state
        tot = total(z_pair[(n_tiles - 1) % 2], tile, old, top, tot)
    row_top = jnp.max(top, axis=0, keepdims=True)
    row_tot = jnp.sum(tot * jnp.exp2((top - row_top) * LOG2E), axis=0, keepdims=True)
    st_send[0:8, :] = jnp.broadcast_to(row_top, (8, pair))
    st_send[8:16, :] = jnp.broadcast_to(row_tot, (8, pair))
    st_copy = remote(st_send, st_recv, st_sems.at[0], st_sems.at[1], mate)
    with jax.named_scope("stat_x"):
        st_copy.start()
        st_copy.wait()
    far_top = st_recv[0:1, :]
    far_tot = st_recv[8:9, :]
    all_top = jnp.maximum(row_top, far_top)
    mine = row_tot * jnp.exp(row_top - all_top)
    other = far_tot * jnp.exp(far_top - all_top)
    lse = all_top + jnp.log(jnp.where(core == 0, mine + other, other + mine))
    my_shift = lse * LOG2E + log_count

    def grads(rows, size, first_row, picked):
        zf = zbuf[rows, :].astype(F32)
        prob = jnp.exp2(zf * LOG2E - my_shift)
        hit = lax.broadcasted_iota(jnp.int32, (size, pair), 0) == lab - (row0 + first_row)
        dz_t = jnp.where(hit, prob - inv_count, prob).astype(BF16)
        got = jnp.where(hit, zf, 0.0).reshape(size // 8, 8, pair)
        return dot_t(dz_t, emb[rows, :]), picked + jnp.sum(got, axis=0)

    tops[0] = jnp.zeros((8, pair), F32)
    dn_acc[...] = jnp.zeros_like(dn_acc)

    @pl.when(core == 0)
    def _():
        dn_acc[...], tops[0] = grads(pl.ds(base, extra), extra, base, tops[0])

    def grad_step(i, picked):
        part, picked = grads(pl.ds(pl.multiple_of(i * tile, 16), tile), tile, i * tile, picked)
        dn_acc[...] += part
        return picked

    with jax.named_scope("grads"):
        picked = lax.fori_loop(0, n_tiles, grad_step, tops[0])
    far = pl.ds(pl.multiple_of((1 - core) * seq, seq), seq)
    near = pl.ds(pl.multiple_of(core * seq, seq), seq)
    dn_send[...] = dn_acc[far, :]
    dp_copy = remote(dn_send, dn_recv, dp_sems.at[0], dp_sems.at[1], mate)
    dp_copy.start()
    row_loss = jnp.where(core == 0, lse, 0.0) - jnp.sum(picked, axis=0, keepdims=True)
    pick = lax.broadcasted_iota(jnp.int32, (8, pair), 0)
    statall[me] = jnp.where(pick == 0, lse, jnp.where(pick == 1, row_loss, 0.0))
    sa_copies = [remote(statall.at[me], statall.at[me], sa_sems.at[0], sa_sems.at[1], lax.rem(me + d, n_stage)) for d in range(1, n_stage)]
    for c in sa_copies:
        c.start()
    sa_all = remote(statall.at[pl.ds(0, n_stage - 1)], statall.at[pl.ds(0, n_stage - 1)], sa_sems.at[0], sa_sems.at[1], me)
    with jax.named_scope("dn_x"):
        dp_copy.wait()
        dn = ((dn_acc[near, :] + dn_recv[...]) * scale).astype(BF16)
    dn_copy = remote(dn_own, dnbuf.at[me], dn_ssem, dn_rsem.at[me], last_id)

    @pl.when(last)
    def _():
        dnbuf[last_id] = dn

    @pl.when(jnp.logical_not(last))
    def _():
        dn_own[...] = dn
        dn_copy.start()

    with jax.named_scope("ag_wait"):
        for p in peers:
            got = remote(nbuf.at[p], nbuf.at[p], ag_send.at[0], ag_recv.at[p], me)
            pl.when(jnp.logical_not(last))(got.wait_recv)
            pl.when(mate != last_id)(remote(nbuf.at[p], nbuf.at[p], fw_send, ag_recv.at[p], mate).start)

    near_dst = [1, 2, n_stage - 2]
    far_dst = n_stage // 2
    n_relay = (n_micro - 2) // 2

    def dx0_copies(m):
        return [remote(dxbuf.at[m], dx0buf.at[m], d_send.at[k], d_recv.at[m], dev) for k, dev in enumerate(near_dst + [far_dst])]

    def relayed(m):
        return (m < 2 * n_relay) & (((me == 2) & (lax.rem(m, 2) == 0)) | ((me == n_stage - 2) & (lax.rem(m, 2) == 1)))

    def relay_far(m):
        return remote(dx0buf.at[m], dx0buf.at[m], r_sems.at[1], d_recv.at[m], far_dst)

    def bwd(m):
        with jax.named_scope("bwd_wait"):
            @pl.when(jnp.logical_not(last))
            def _():
                remote(gbuf.at[m], gbuf.at[m], b_send, b_recv.at[m], me).wait_recv()

            @pl.when(last)
            def _():
                @pl.when(m != last_id)
                def _():
                    remote(dnbuf.at[m], dnbuf.at[m], dn_ssem, dn_rsem.at[m], me).wait_recv()

                yf = ybuf[pl.ds(m * per, per)].reshape(seq, dim).astype(F32)
                inv = lax.rsqrt(jnp.mean(yf * yf, axis=-1, keepdims=True) + EPS)
                dnf = dnbuf[m].astype(F32)
                proj = jnp.mean(yf * dnf, axis=-1, keepdims=True)
                gbuf[m] = (dnf * inv - yf * (inv * inv * inv * proj)).astype(BF16)

        with jax.named_scope("bwd_comp"):
            g = gbuf[m]
            for j in range(n_fblk):
                cols = slice(j * fblk, (j + 1) * fblk)
                dh = dot(g, down_t[:, cols]).astype(BF16).astype(F32)
                abuf[m, :, cols] = (dh * gelu_slope(abuf[m, :, cols].astype(F32))).astype(BF16)
            dxbuf[m] = (g.astype(F32) + dot(abuf[m], up_t[...])).astype(BF16)

        @pl.when(jnp.logical_not(first))
        def _():
            remote(dxbuf.at[m], gbuf.at[m], b_send, b_recv.at[m], me - 1).start()

        @pl.when(first)
        def _():
            copies = dx0_copies(m)
            for c in copies[:-1]:
                c.start()
            pl.when(m >= 2 * n_relay)(copies[-1].start)

        pltpu.make_async_copy(abuf.at[m], da_out.at[m], out_sem.at[2]).start()
        pltpu.make_async_copy(gbuf.at[m], g_out.at[m], out_sem.at[3]).start()

    n_slot = obuf.shape[0]

    def tile_copy(k):
        rows = pl.ds(pl.multiple_of(k * plan.rows, plan.rows), plan.rows)
        slot = lax.rem(k, n_slot)
        return pltpu.make_async_copy(obuf.at[slot], tmp_out.at[core, rows], o_sem.at[slot])

    def piece(p):
        k = p // plan.per_tile
        rows = pl.ds(pl.multiple_of(p * plan.piece, plan.piece), plan.piece)
        here = pl.ds(pl.multiple_of(lax.rem(p, plan.per_tile) * plan.piece, plan.piece), plan.piece)
        return remote(obuf.at[lax.rem(k, n_slot), here], tmp_out.at[core, rows], od_send.at[k], od_recv, mate)

    def tile_sent(k):
        slot = lax.rem(k, n_slot)
        return remote(obuf.at[slot], tmp_out.at[core, pl.ds(0, plan.rows)], od_send.at[k], od_recv, mate)

    def emb_tile(k):
        with jax.named_scope("tile_prep"):

            @pl.when(k == 0)
            def _():
                for d in range(1, n_stage // 2):
                    src = lax.rem(mate + 2 * d, n_stage)
                    pl.when(jnp.logical_not(last))(remote(nbuf.at[src], nbuf.at[src], ag_send.at[0], ag_recv.at[src], me).wait_recv)
                for m in range(n_micro):
                    n_all_t[:, m * seq:(m + 1) * seq] = nbuf[m].T
                sa_all.wait_recv()
                for c in range(n_stage // 2):
                    shift[:, c * pair:(c + 1) * pair] = statall[2 * c, 0:1, :] * LOG2E + log_count

        slot = lax.rem(k, n_slot)
        with jax.named_scope("tile_wait"):
            pl.when(k >= n_slot)(lambda: tile_copy(k - n_slot).wait())
            pl.when((k >= n_slot) & (k - n_slot < plan.shared))(lambda: tile_sent(k - n_slot).wait_send())

        with jax.named_scope("tile"):
            rows = pl.ds(pl.multiple_of(k * plan.rows, plan.rows), plan.rows)
            logit_grad(emb[rows, :], n_all_t, shift, lab_ref, row0 + k * plan.rows, inv_count, scale, dz)
            obuf[slot] = dot(dz[...], nbuf[...].reshape(n_tok, dim)) * scale

        tile_copy(k).start()

    def send_pieces(done, until):
        lax.fori_loop(done, until, lambda p, c: (piece(p).start(), c)[1], 0)
        return jnp.maximum(done, until)

    before = sum(jnp.where(me == s, plan.before[s], 0) for s in range(n_stage))

    def pass_dx0(m, carry):
        @pl.when(jnp.logical_not(first))
        def _():
            remote(dx0buf.at[m], dx0buf.at[m], r_sems.at[0], d_recv.at[m], me).wait_recv()

            @pl.when(core == 0)
            def _():
                remote(dx0buf.at[m], dx0buf.at[m], r_sems.at[0], d_recv.at[m], mate).start()

            @pl.when(relayed(m))
            def _():
                relay_far(m).start()

            pltpu.make_async_copy(dx0buf.at[m], dx0_out.at[m], out_sem.at[4]).start()

        @pl.when(first)
        def _():
            pltpu.make_async_copy(dxbuf.at[m], dx0_out.at[m], out_sem.at[4]).start()

        return carry

    lead = jnp.where(me == 2, -150, jnp.where(me == n_stage - 2, -1500, jnp.where(me == far_dst, -1550, -10**6)))

    def work(i, carry):
        sent, passed = carry
        chunk = (i >= before) & (i < before + n_micro)
        pl.when(chunk)(lambda: bwd(i - before))
        k = jnp.where(i < before, i, i - n_micro)
        pl.when(jnp.logical_not(chunk))(lambda: emb_tile(k))
        after = i - before - n_micro + 1
        here = jnp.where(after > 0, jnp.clip((after * 257 + lead) // 146, 0, n_micro), 0)
        lax.fori_loop(passed, here, pass_dx0, 0)
        ready = jnp.where(i < before, i + 1, jnp.where(chunk, before, i + 1 - n_micro)) * plan.per_tile
        near_chunks = chunk | ((i < before) & (i + 1 >= before))
        until = jnp.minimum(jnp.minimum(ready, plan.shared * plan.per_tile), sent + jnp.where(near_chunks, 1, plan.per_tile + 1))
        return send_pieces(sent, until), jnp.maximum(passed, here)

    sent, passed = lax.fori_loop(0, plan.tiles + n_micro, work, (0, 0))
    outs = [pltpu.make_async_copy(nbuf, n_out, out_sem.at[5]), pltpu.make_async_copy(statall, stat_out, out_sem.at[6]), pltpu.make_async_copy(meta, meta_out, out_sem.at[7])]
    for c in outs:
        c.start()
    with jax.named_scope("relay_all"):
        lax.fori_loop(passed, n_micro, pass_dx0, 0)

    with jax.named_scope("drain"):
        send_pieces(sent, plan.shared * plan.per_tile)
        for k in range(max(plan.tiles - n_slot, 0), plan.tiles):
            tile_copy(k).wait()
            if k < plan.shared:
                tile_sent(k).wait_send()
        all_rows = pl.ds(0, plan.shared * plan.rows)
        remote(tmp_out.at[1 - core, all_rows], tmp_out.at[1 - core, all_rows], od_send.at[0], od_recv, me).wait_recv()
        sa_all.wait_send()
        for c, p in zip(ag_copies, peers):
            pl.when(p != last_id)(c.wait_send)

        @pl.when(jnp.logical_not(last))
        def _():
            dn_copy.wait_send()
            pl.when(mate != last_id)(n_forward.wait_send)
            remote(ybuf, xbuf, f_send, f_recv.at[0], me + 1).wait_send()

        @pl.when(last)
        def _():
            remote(nbuf, nbuf, n_send, n_recv.at[0], me).wait_send()

        @pl.when(mate != last_id)
        def _():
            some = nbuf.at[pl.ds(0, len(peers))]
            remote(some, some, fw_send, ag_recv.at[0], mate).wait_send()

        @pl.when(jnp.logical_not(first) & (me + 2 < n_micro))
        def _():
            x_copy(0).wait_send()

            @pl.when(me < 2)
            def _():
                x_copy(1).wait_send()

        @pl.when(jnp.logical_not(first))
        def _():
            remote(dxbuf, gbuf, b_send, b_recv.at[0], me).wait_send()
            pl.when(core == 0)(remote(dx0buf, dx0buf, r_sems.at[0], d_recv.at[0], mate).wait_send)

        @pl.when(first)
        def _():
            for k in range(len(near_dst)):
                remote(dxbuf, dx0buf, d_send.at[k], d_recv.at[0], me).wait_send()
            direct = pl.ds(0, n_micro - 2 * n_relay)
            remote(dxbuf.at[direct], dx0buf.at[direct], d_send.at[len(near_dst)], d_recv.at[0], me).wait_send()

        @pl.when((me == 2) | (me == n_stage - 2))
        def _():
            some = dx0buf.at[pl.ds(0, n_relay)]
            remote(some, some, r_sems.at[1], d_recv.at[0], me).wait_send()

        pltpu.make_async_copy(hbuf, hid_out, out_sem.at[0]).wait()
        pltpu.make_async_copy(xbuf, xs_out, out_sem.at[1]).wait()
        pltpu.make_async_copy(abuf, da_out, out_sem.at[2]).wait()
        pltpu.make_async_copy(gbuf, g_out, out_sem.at[3]).wait()
        pltpu.make_async_copy(dx0buf, dx0_out, out_sem.at[4]).wait()
        for c in outs:
            c.wait()


class Plan:
    def __init__(self, vocab, n_stage):
        units = vocab // LANES
        self.base = units // 2 * LANES
        self.extra = vocab - 2 * self.base
        self.head_tile = next(t for t in (1600, 1536, 1280, 1024, 768, 640, 512, 256, 128) if self.base % t == 0)
        self.rows = 1024
        self.tiles, self.shared = 10, 7
        self.e_parts = next(k for k in (10, 8, 5, 4, 2, 1) if self.base % (16 * k) == 0)
        self.part = 64
        self.slots = 4
        self.piece = 256
        self.per_tile = self.rows // self.piece
        measured = [8, 7, 6, 5, 2, 1, 0, 0]
        self.before = (measured + [0] * n_stage)[:n_stage]
        mid = self.base + self.extra
        ends = [(0, mid), (mid, vocab)]
        early = (self.tiles * self.rows, self.shared * self.rows)
        self.spans = [[(ends[h][0] + early[0 if h == c else 1], ends[h][1]) for h in (c, 1 - c)] for c in range(2)]
        self.longest = [max(self.spans[c][k][1] - self.spans[c][k][0] for c in range(2)) for k in range(2)]
        best = min(range(16, 1281, 16), key=lambda r: (sum(-(-n // r) for n in self.longest)) * (r + 40))
        self.calc_rows = best
        self.calc_steps = [-(-n // best) for n in self.longest]
        self.steps = sum(self.calc_steps)
        self.copy_rows = self.rows
        self.copies = self.tiles + self.shared
        self.starts = ends

    def calc_start(self, core, s):
        k = 0 if s < self.calc_steps[0] else 1
        lo, hi = self.spans[core][k]
        return min(lo + (s - k * self.calc_steps[0]) * self.calc_rows, hi - self.calc_rows)

    def copy_start(self, core, c):
        own = c < self.tiles
        h = core if own else 1 - core
        return self.starts[h][0] + (c if own else c - self.tiles) * self.copy_rows

    def cuts(self, core):
        firsts = [(self.calc_start(core, s), self.calc_rows) for s in range(self.steps)] + [(self.copy_start(core, c), self.copy_rows) for c in range(self.copies)]
        flat = [v for lo, rows in firsts for v in (lo, lo + rows)]
        return flat + [0] * (LANES - len(flat))


def run_pipe(x0, emb, w_up, w_down, labels, tokens, cuts, n_stage, plan):
    n_micro, seq = labels.shape
    dim, ffn = w_up.shape
    n_tok = n_micro * seq
    base = plan.base
    any_spec = pl.BlockSpec(memory_space=pl.ANY)
    act = (n_micro, seq, dim)
    fine = (n_tok // plan.part, plan.part, dim)
    wide = (n_micro, seq, ffn)
    dma = pltpu.SemaphoreType.DMA
    vm = pltpu.VMEM
    pair = 2 * seq
    return pl.pallas_call(
        functools.partial(pipe_kernel, n_stage, plan),
        out_shape=[
            jax.ShapeDtypeStruct(act, BF16), jax.ShapeDtypeStruct(fine, BF16), jax.ShapeDtypeStruct(wide, BF16),
            jax.ShapeDtypeStruct(wide, BF16), jax.ShapeDtypeStruct(act, BF16), jax.ShapeDtypeStruct(act, BF16),
            jax.ShapeDtypeStruct((n_stage, 8, pair), F32), jax.ShapeDtypeStruct((2, plan.tiles * plan.rows, dim), F32),
            jax.ShapeDtypeStruct((3 * n_tok // LANES, LANES), jnp.int32),
        ],
        in_specs=[any_spec] * 4 + [pl.BlockSpec(memory_space=pltpu.VMEM)] * 3,
        out_specs=[any_spec] * 9,
        scratch_shapes=[
            vm(fine, BF16), vm(fine, BF16), vm(wide, BF16), vm(wide, BF16), vm(act, BF16), vm(act, BF16), vm(act, BF16), vm(act, BF16), vm(act, BF16),
            vm((dim, ffn), BF16), vm((ffn, dim), BF16), vm((ffn, dim), BF16), vm((dim, ffn), BF16),
            vm((base + plan.extra, dim), BF16), vm((base + plan.extra, pair), BF16), vm((dim, pair), BF16), vm((pair, dim), F32),
            vm((seq, dim), F32), vm((seq, dim), F32), vm((seq, dim), BF16), vm((16, pair), F32), vm((16, pair), F32), vm((n_stage, 8, pair), F32),
            vm((2, 8, pair), F32), vm((dim, n_tok), BF16), vm((1, n_tok), F32), vm((plan.rows, n_tok), BF16), vm((plan.slots, plan.rows, dim), F32),
            vm((2, plan.head_tile, pair), BF16), vm((3 * n_tok // LANES, LANES), jnp.int32),
            dma((2,)), dma((2,)), dma((2,)), dma((2,)), dma((n_micro,)), dma, dma((n_tok // plan.part,)), dma, dma((n_micro,)), dma,
            dma((n_stage // 2,)), dma((n_micro,)), dma,
            dma((2,)), dma((2,)), dma, dma((n_stage,)), dma((2,)), dma, dma((n_micro,)), dma((4,)), dma((n_micro,)), dma((2,)), dma((8,)),
            dma((plan.slots,)), dma((plan.shared,)), dma,
        ],
        compiler_params=pltpu.CompilerParams(collective_id=0, has_side_effects=True, vmem_limit_bytes=67_000_000),
        cost_estimate=pl.CostEstimate(flops=60 * 10**9, bytes_accessed=100 * 10**6, transcendentals=0),
        name="pipe",
    )(x0.reshape(x0.shape[0], seq // plan.part, plan.part, dim), emb, w_up, w_down, labels.reshape(1, n_tok), tokens.reshape(1, n_tok), cuts)


def fin_kernel(n_stage, n_tok, plan, ids_ref, emb_hbm, tmp_hbm, n_hbm, stat_ref, lab_ref, meta_ref, dx0_hbm, xs_hbm, hid_hbm, da_hbm, g_hbm,
               out_hbm, loss_ref, gup_hbm, gdown_hbm,
               n_all, dx0, xs, hid, da, g, n_t, x_t, dx0s, dz, shift, e_in, c_out, cp, gup, gdown,
               ld_sem, e_sem, t_sem, co_sem, po_sem, gu_sem, gd_sem, wi_sem):
    dim, ffn = gup_hbm.shape
    scale = dim ** -0.5
    inv_count = 1.0 / n_tok
    steps, crows, prows = plan.steps, plan.calc_rows, plan.copy_rows
    core = lax.rem(lax.axis_index("stage"), 2)
    early = plan.tiles * prows
    wblk = gup.shape[2]
    n_wblk = ffn // wblk
    turn = plan.calc_steps[0]

    def pick(pair):
        return jnp.where(core == 0, pair[0], pair[1])

    def calc_start(s):
        own = s < turn
        lo, hi = [jnp.where(own, pick([plan.spans[c][0][e] for c in range(2)]), pick([plan.spans[c][1][e] for c in range(2)])) for e in range(2)]
        return pl.multiple_of(jnp.minimum(lo + (s - jnp.where(own, 0, turn)) * crows, hi - crows), 16)

    def copy_start(c):
        own = c < plan.tiles
        first = jnp.where(own, pick([plan.starts[0][0], plan.starts[1][0]]), pick([plan.starts[1][0], plan.starts[0][0]]))
        return pl.multiple_of(first + (c - jnp.where(own, 0, plan.tiles)) * prows, 16)

    def e_copy(s):
        return pltpu.make_async_copy(emb_hbm.at[pl.ds(calc_start(s), crows)], e_in.at[lax.rem(s, 2)], e_sem.at[lax.rem(s, 2)])

    n_slot = cp.shape[0]
    ahead = 3

    def t_copy(c):
        own = c < plan.tiles
        row = jnp.where(own, core, 1 - core) * early + (c - jnp.where(own, 0, plan.tiles)) * prows
        slot = lax.rem(c, n_slot)
        return pltpu.make_async_copy(tmp_hbm.at[pl.ds(pl.multiple_of(row, 16), prows)], cp.at[slot], t_sem.at[slot])

    def p_out(c):
        slot = lax.rem(c, n_slot)
        return pltpu.make_async_copy(cp.at[slot], out_hbm.at[pl.ds(copy_start(c), prows)], po_sem.at[slot])

    def c_outs(s):
        slot = lax.rem(s, 2)
        return pltpu.make_async_copy(c_out.at[slot], out_hbm.at[pl.ds(calc_start(s), crows)], co_sem.at[slot])

    loads = [pltpu.make_async_copy(s, d, ld_sem.at[i]) for i, (s, d) in enumerate(((n_hbm, n_all), (dx0_hbm, dx0), (xs_hbm, xs), (g_hbm, g)))]
    loads[0].start()
    loads[1].start()
    e_copy(0).start()
    for c in range(ahead):
        t_copy(c).start(priority=1)
    pair = stat_ref.shape[2]
    loss = jnp.zeros((1, pair), F32)
    for d in range(n_stage):
        if d % 2 == 0:
            shift[:, (d // 2) * pair:(d // 2 + 1) * pair] = stat_ref[d, 0:1, :] * LOG2E + math.log2(n_tok)
        loss = loss + stat_ref[d, 1:2, :]
    loss_ref[0] = jnp.sum(loss) * inv_count
    with jax.named_scope("fin_pre"):
        loads[0].wait()
        n_t[...] = n_all[...].T
        loads[1].wait()
        dense = jnp.concatenate([meta_ref[g:g + 1, :] for g in range(n_tok // LANES)], axis=1)
        order = lax.broadcasted_iota(jnp.int32, (n_tok, n_tok), 0) == dense
        dx0s[...] = dot(jnp.where(order, 1.0, 0.0).astype(BF16), dx0[...])

    def add_rows(k, start, ref):
        lo, hi = ids_ref[2 * n_tok + k], ids_ref[2 * n_tok + k + 1]
        wide = 8

        def some(p, width):
            at = [pl.ds(ids_ref[n_tok + p + u] - start, 1) for u in range(width)]
            new = [ref[at[u], :] + dx0s[pl.ds(p + u, 1), :] for u in range(width)]
            for u in range(width):
                ref[at[u], :] = new[u]

        def group(g, carry):
            some(lo + g * wide, wide)
            return carry

        def single(p, carry):
            some(p, 1)
            return carry

        n_grp = (hi - lo) // wide
        lax.fori_loop(0, n_grp, group, 0)
        lax.fori_loop(lo + n_grp * wide, hi, single, 0)

    def w_ins(w):
        cols = pl.ds(pl.multiple_of(w * wblk, wblk), wblk)
        wslot = lax.rem(w, 2)
        return (pltpu.make_async_copy(da_hbm.at[:, cols], da.at[wslot], wi_sem.at[0, wslot]), pltpu.make_async_copy(hid_hbm.at[:, cols], hid.at[wslot], wi_sem.at[1, wslot]))

    def w_outs(w):
        cols = pl.ds(pl.multiple_of(w * wblk, wblk), wblk)
        wslot = lax.rem(w, 2)
        return (pltpu.make_async_copy(gup.at[wslot], gup_hbm.at[:, cols], gu_sem.at[wslot]), pltpu.make_async_copy(gdown.at[wslot], gdown_hbm.at[cols], gd_sem.at[wslot]))

    def copy_tile(c, carry):
        with jax.named_scope("copy_wait"):
            t_copy(c).wait()
        with jax.named_scope("add_p"):
            add_rows(2 * steps + 2 * c, copy_start(c), cp.at[lax.rem(c, n_slot)])
        p_out(c).start()

        @pl.when(c + ahead < plan.copies)
        def _():
            pl.when(c + ahead >= n_slot)(lambda: p_out(c + ahead - n_slot).wait())
            t_copy(c + ahead).start(priority=1)

        return carry

    w_first = 2
    tails = [turn - 1, steps - 1]

    def tail(s):
        return (s == tails[0]) | (s == tails[1])

    def step(s, carry):
        pl.when(s + 1 < steps)(lambda: e_copy(s + 1).start())
        lax.fori_loop(s * plan.copies // steps, (s + 1) * plan.copies // steps, copy_tile, 0)
        with jax.named_scope("fin_wait"):
            e_copy(s).wait()

        @pl.when(s == 0)
        def _():
            for c in loads[2:]:
                c.start()

        w = s - w_first

        @pl.when((w + 1 >= 0) & (w + 1 < n_wblk))
        def _():
            for c in w_ins(w + 1):
                c.start()

        pl.when((s >= 2) & jnp.logical_not(tail(s - 1)))(lambda: c_outs(s - 2).wait())
        slot = lax.rem(s, 2)
        start = calc_start(s)
        with jax.named_scope("calc"):
            logit_grad(e_in[slot], n_t, shift, lab_ref, start, inv_count, scale, dz)
            c_out[slot] = dot(dz[...], n_all[...]) * scale
        with jax.named_scope("add_c"):
            add_rows(2 * s, start, c_out.at[slot])
        pl.when(tail(s))(lambda: c_outs(s - 1).wait())
        c_outs(s).start()

        @pl.when(w == 0)
        def _():
            for c in loads[2:]:
                c.wait()
            x_t[...] = xs[...].T

        @pl.when((w >= 0) & (w < n_wblk))
        def _():
            wslot = lax.rem(w, 2)
            with jax.named_scope("dw_wait"):
                for c in w_ins(w):
                    c.wait()

                @pl.when(w >= 2)
                def _():
                    for c in w_outs(w - 2):
                        c.wait()

            with jax.named_scope("dw"):
                gup[wslot] = dot(x_t[...], da[wslot])
                gdown[wslot] = dot_t(hid[wslot], g[...])
            for c in w_outs(w):
                c.start()

        return carry

    lax.fori_loop(0, steps, step, 0)
    with jax.named_scope("fin_drain"):
        for w in range(n_wblk - 2, n_wblk):
            for c in w_outs(w):
                c.wait()
        c_outs(steps - 1).wait()
        for c in range(plan.copies - n_slot, plan.copies):
            p_out(c).wait()


def run_fin(emb, tmp, n_all, stats, labels, meta, dx0, xs, hid, da, g, n_stage, plan):
    vocab, dim = emb.shape
    n_tok, ffn = hid.shape
    vm = pltpu.VMEM
    dma = pltpu.SemaphoreType.DMA
    any_spec = pl.BlockSpec(memory_space=pl.ANY)
    vspec = pl.BlockSpec(memory_space=pltpu.VMEM)
    smem = pl.BlockSpec(memory_space=pltpu.SMEM)
    wblk = 256
    return pl.pallas_call(
        functools.partial(fin_kernel, n_stage, n_tok, plan),
        out_shape=[jax.ShapeDtypeStruct((vocab, dim), F32), jax.ShapeDtypeStruct((1,), F32), jax.ShapeDtypeStruct((dim, ffn), F32), jax.ShapeDtypeStruct((ffn, dim), F32)],
        in_specs=[smem, any_spec, any_spec, any_spec, vspec, vspec, vspec] + [any_spec] * 5,
        out_specs=[any_spec, smem, any_spec, any_spec],
        scratch_shapes=[
            vm((n_tok, dim), BF16), vm((n_tok, dim), BF16), vm((n_tok, dim), BF16), vm((2, n_tok, wblk), BF16), vm((2, n_tok, wblk), BF16), vm((n_tok, dim), BF16),
            vm((dim, n_tok), BF16), vm((dim, n_tok), BF16), vm((n_tok, dim), F32), vm((plan.calc_rows, n_tok), BF16), vm((1, n_tok), F32),
            vm((2, plan.calc_rows, dim), BF16), vm((2, plan.calc_rows, dim), F32), vm((5, plan.copy_rows, dim), F32),
            vm((2, dim, wblk), F32), vm((2, wblk, dim), F32),
            dma((4,)), dma((2,)), dma((5,)), dma((2,)), dma((5,)), dma((2,)), dma((2,)), dma((2, 2)),
        ],
        compiler_params=pltpu.CompilerParams(vmem_limit_bytes=67_000_000),
        cost_estimate=pl.CostEstimate(flops=2 * n_tok * vocab * dim, bytes_accessed=5 * vocab * dim, transcendentals=0),
        name="fin",
    )(meta.reshape(-1), emb, tmp, n_all, stats, labels.reshape(1, n_tok), meta, dx0, xs, hid, da, g)


def solution(mesh):
    n_stage = mesh.shape["stage"]

    def device_fn(tokens, labels, emb, w_up, w_down):
        n_micro, seq = tokens.shape
        vocab, dim = emb.shape
        w_up, w_down = w_up[0], w_down[0]
        n_tok = n_micro * seq
        plan = Plan(vocab, n_stage)
        cuts = jnp.array([plan.cuts(0), plan.cuts(1)], jnp.int32)
        x0 = run_gather(tokens, emb)
        n_all, xs, hid, da, g, dx0, stats, tmp, meta = run_pipe(x0, emb, w_up, w_down, labels, tokens, cuts, n_stage, plan)
        flat = lambda p: p.reshape(n_tok, -1)
        grad_emb, loss, grad_up, grad_down = run_fin(
            emb, tmp.reshape(-1, dim), flat(n_all), stats, labels, meta, flat(dx0), flat(xs), flat(hid), flat(da), flat(g), n_stage, plan
        )
        return loss, grad_up[None], grad_down[None], grad_emb

    return jax.shard_map(device_fn, mesh=mesh, in_specs=(P("dp", None), P("dp", None), P(None, None), P("stage", None, None), P("stage", None, None)), out_specs=(P("dp"), P(("dp", "stage"), None, None), P(("dp", "stage"), None, None), P("dp", None)), check_vma=False)
```

```python
import functools
import math

import jax
import jax.numpy as jnp
from jax import lax
from jax.experimental import pallas as pl
from jax.experimental.pallas import tpu as pltpu
from jax.sharding import PartitionSpec as P


MESH = pl.DeviceIdType.MESH
LOG2E = math.log2(math.e)
LN2 = math.log(2.0)
GELU_C = math.sqrt(2.0 / math.pi)
GELU_K = 0.044715
EPS = 1e-6
LANES = 128
F32 = jnp.float32
BF16 = jnp.bfloat16


def gelu_fwd(a):
    return 0.5 * a * (1.0 + jnp.tanh(GELU_C * (a + GELU_K * (a * a * a))))


def gelu_slope(a):
    a2 = a * a
    t = jnp.tanh(GELU_C * (a + GELU_K * (a2 * a)))
    return 0.5 * (1.0 + t) + (0.5 * a) * (1.0 - t * t) * (GELU_C + (3.0 * GELU_C * GELU_K) * a2)


def dot(x, y):
    return jnp.dot(x, y, preferred_element_type=F32)


def dot_t(x, y):
    return lax.dot_general(x, y, (((0,), (0,)), ((), ())), preferred_element_type=F32)


def remote(src, dst, send_sem, recv_sem, dev):
    return pltpu.make_async_remote_copy(src_ref=src, dst_ref=dst, send_sem=send_sem, recv_sem=recv_sem, device_id={"stage": dev}, device_id_type=MESH)


def column(row):
    return jnp.broadcast_to(row, (LANES, LANES)).T


def gather_kernel(ids_ref, tok_ref, emb_hbm, x0_hbm, tiles, picked, sem, out_sem):
    n_micro, seq = tok_ref.shape
    me = lax.axis_index("stage")
    group = tiles.shape[1] // seq
    slots = tiles.shape[0]
    owners = [head_chunk(me, k, n_micro) for k in range(slots)]

    def fetch(k):
        def one(i, carry):
            t = ids_ref[owners[k] * seq + i]
            start = pl.multiple_of(t // group * group, group)
            pltpu.make_async_copy(emb_hbm.at[pl.ds(start, group)], tiles.at[k, pl.ds(pl.multiple_of(i * group, group), group)], sem.at[k]).start()
            return carry

        lax.fori_loop(0, seq, one, 0, unroll=8)

    def select(k):
        sub = lax.broadcasted_iota(jnp.int32, (LANES, LANES), 0)
        lane = lax.broadcasted_iota(jnp.int32, (LANES, LANES), 1)
        tok = column(tok_ref[pl.ds(owners[k], 1), :].astype(F32)).astype(jnp.int32)
        want = sub * group + (tok - tok // group * group)
        hot = jnp.concatenate([jnp.where(lane + b * LANES == want, 1.0, 0.0).astype(BF16) for b in range(seq * group // LANES)], axis=1)
        pltpu.make_async_copy(emb_hbm.at[pl.ds(0, seq * group)], tiles.at[k], sem.at[k]).wait()
        picked[k] = dot(hot, tiles[k]).astype(BF16)
        pltpu.make_async_copy(picked.at[k], x0_hbm.at[k], out_sem.at[k]).start()

    def finish(k):
        pltpu.make_async_copy(picked.at[k], x0_hbm.at[k], out_sem.at[k]).wait()

    for work in (fetch, select, finish):
        work(0)
        for k in range(1, slots):
            pl.when(me < slots)(functools.partial(work, k))


def head_chunk(dev, k, n_micro):
    return jnp.minimum(jnp.where(dev < 2, 2 * dev + k, dev + 2), n_micro - 1)


def run_gather(tokens, emb):
    n_micro, seq = tokens.shape
    dim = emb.shape[1]
    group = 16
    return pl.pallas_call(
        gather_kernel,
        out_shape=jax.ShapeDtypeStruct((2, seq, dim), BF16),
        in_specs=[pl.BlockSpec(memory_space=pltpu.SMEM), pl.BlockSpec(memory_space=pltpu.VMEM), pl.BlockSpec(memory_space=pl.ANY)],
        out_specs=pl.BlockSpec(memory_space=pl.ANY),
        scratch_shapes=[pltpu.VMEM((2, seq * group, dim), BF16), pltpu.VMEM((2, seq, dim), BF16), pltpu.SemaphoreType.DMA((2,)), pltpu.SemaphoreType.DMA((2,))],
        cost_estimate=pl.CostEstimate(flops=10**9, bytes_accessed=2 * seq * group * dim * 2, transcendentals=0),
        name="gather",
    )(tokens.reshape(n_micro * seq), tokens, emb)


def token_table(row_ref, cut_ref, meta):
    n_tok = row_ref.shape[1]
    n_grp = n_tok // LANES
    lane = lax.broadcasted_iota(jnp.int32, (LANES, LANES), 1).astype(F32)
    sub = lax.broadcasted_iota(jnp.int32, (LANES, LANES), 0)
    row = lambda g: row_ref[:, g * LANES:(g + 1) * LANES].astype(F32)
    zero = jnp.zeros((LANES, LANES), F32)
    fold = lambda acc: jnp.sum(acc, axis=0, keepdims=True)
    cols = [column(row(c)) for c in range(n_grp)]
    firsts = []
    for g in range(n_grp):
        acc = zero
        for c in range(g + 1):
            same = cols[c] == row(g)
            if c == g:
                same = same & (sub < lane.astype(jnp.int32))
            acc = acc + jnp.where(same, 1.0, 0.0)
        firsts.append(column(jnp.where(fold(acc) == 0.0, 1.0, 0.0)))
    ranks = []
    for g in range(n_grp):
        acc = zero
        for c in range(n_grp):
            acc = acc + jnp.where(cols[c] < row(g), firsts[c], 0.0)
        ranks.append(fold(acc))
        meta[g:g + 1, :] = ranks[g].astype(jnp.int32)
    rank_cols = [column(r) for r in ranks]
    for g in range(n_grp):
        acc = zero
        for c in range(n_grp):
            acc = acc + jnp.where(rank_cols[c] == lane + g * LANES, firsts[c] * cols[c], 0.0)
        meta[n_grp + g:n_grp + g + 1, :] = fold(acc).astype(jnp.int32)
    cut = cut_ref[...].astype(F32)
    acc = zero
    for c in range(n_grp):
        acc = acc + jnp.where(cols[c] < cut, firsts[c], 0.0)
    meta[2 * n_grp:3 * n_grp, :] = jnp.broadcast_to(fold(acc), (n_grp, LANES)).astype(jnp.int32)


def logit_grad(e, n_t, shift, lab, first_id, inv_count, scale, dz):
    rows = e.shape[0]
    n_tok = n_t.shape[1]
    blk = 256
    vid = lax.broadcasted_iota(jnp.int32, (rows, blk), 0)
    for j in range(n_tok // blk):
        cols = slice(j * blk, (j + 1) * blk)
        z = (dot(e, n_t[:, cols]) * scale).astype(BF16).astype(F32)
        prob = jnp.exp2(z * LOG2E - shift[:, cols])
        dz[:, cols] = jnp.where(vid == lab[:, cols] - first_id, prob - inv_count, prob).astype(BF16)


def pipe_kernel(n_stage, plan, x0_hbm, emb_hbm, up_hbm, down_hbm, lab_ref, row_ref, cut_ref,
                n_out, xs_out, hid_out, da_out, g_out, dx0_out, stat_out, loss_out, tmp_out, meta_out,
                xbuf, ybuf, abuf, hbuf, nbuf, gbuf, dxbuf, dx0buf, dnbuf, up, down, up_t, down_t,
                emb, zbuf, n_t, dn_acc, dn_send, dn_recv, dn_own, st_send, st_recv, statall, lossall, tops, n_all_t, shift, dz, obuf, z_pair, meta,
                w_sem, e_sem, x_sem, x_send, x_recv, f_send, f_recv, n_send, n_recv, nf_send, ag_send, ag_recv, fw_send,
                st_sems, dp_sems, dn_ssem, dn_rsem, sa_sems, lo_sems, b_send, b_recv, d_send, d_recv, r_sems, out_sem, o_sem, od_send, od_recv, ic_send):
    n_micro, seq, dim = gbuf.shape
    part = xbuf.shape[1]
    n_part = xbuf.shape[0]
    per = seq // part
    n_tok = n_micro * seq
    ffn = up.shape[1]
    vocab = emb_hbm.shape[0]
    me = lax.axis_index("stage")
    core = lax.rem(me, 2)
    chip = me // 2
    mate = me + 1 - 2 * core
    last_id = n_stage - 1
    first = me == 0
    last = me == last_id
    fblk = 512
    n_fblk = ffn // fblk
    base, extra, tile = plan.base, plan.extra, plan.head_tile
    row0 = core * (base + extra)
    n_tiles = base // tile
    wide_tile = plan.grad_tile

    barrier = pltpu.get_barrier_semaphore()
    for d in range(1, n_stage):
        pl.semaphore_signal(barrier, inc=1, device_id={"stage": lax.rem(me + d, n_stage)}, device_id_type=MESH)
    w_copy = [pltpu.make_async_copy(up_hbm, up, w_sem.at[0]), pltpu.make_async_copy(down_hbm, down, w_sem.at[1])]
    for c in w_copy:
        c.start()
    x_slots = x0_hbm.shape[0]
    x_mine = [head_chunk(me, k, n_micro) for k in range(x_slots)]

    def x_rows(m):
        return xbuf.at[pl.ds(m * per, per)]

    def x_local(k):
        return pltpu.make_async_copy(x0_hbm.at[k], x_rows(k), x_sem.at[k])

    @pl.when(first)
    def _():
        for k in range(x_slots):
            x_local(k).start()

    e_parts = plan.e_parts
    e_step = base // e_parts

    def e_copy(i):
        src = emb_hbm.at[pl.ds(pl.multiple_of(row0 + i * e_step, 16), e_step)]
        return pltpu.make_async_copy(src, emb.at[pl.ds(i * e_step, e_step)], e_sem.at[0])

    e_more = pltpu.make_async_copy(emb_hbm.at[pl.ds(base, extra)], emb.at[pl.ds(base, extra)], e_sem.at[1])
    with jax.named_scope("entry"):
        pl.semaphore_wait(barrier, n_stage - 1)

    def x_copy(k):
        return remote(x0_hbm.at[k], x_rows(x_mine[k]), x_send.at[k], x_recv.at[x_mine[k]], 0)

    @pl.when(jnp.logical_not(first) & (me + 2 < n_micro))
    def _():
        x_copy(0).start()

        @pl.when(me < 2)
        def _():
            x_copy(1).start()

    with jax.named_scope("w_wait"):
        for c in w_copy:
            c.wait()
        for i in range(e_parts):
            e_copy(i).start()
        pl.when(core == 0)(e_more.start)

    def transpose_weights():
        for j in range(n_fblk):
            up_t[j * fblk:(j + 1) * fblk, :] = up[:, j * fblk:(j + 1) * fblk].T
            down_t[:, j * fblk:(j + 1) * fblk] = down[j * fblk:(j + 1) * fblk, :].T

    def idle_work():
        transpose_weights()
        token_table(row_ref, jnp.where(core == 0, cut_ref[0:1, :], cut_ref[1:2, :]), meta)

    @pl.when(chip >= n_stage // 4)
    def _():
        idle_work()

    def n_copy(m):
        return remote(nbuf.at[m], nbuf.at[m], n_send, n_recv.at[m], jnp.where(m == last_id, last_id - 1, m))

    def y_copy(h):
        return remote(ybuf.at[h], xbuf.at[h], f_send, f_recv.at[h], me + 1)

    def fwd(h, carry):
        m = h // per
        sub = lax.rem(h, per)
        rows = pl.ds(pl.multiple_of(sub * part, part), part)
        with jax.named_scope("fwd_wait"):

            @pl.when(first & (sub == 0))
            def _():
                @pl.when(m < x_slots)
                def _():
                    x_local(m).wait()

                @pl.when(m >= x_slots)
                def _():
                    remote(x_rows(m), x_rows(m), x_send.at[0], x_recv.at[m], me).wait_recv()

            @pl.when(jnp.logical_not(first))
            def _():
                remote(xbuf.at[h], xbuf.at[h], f_send, f_recv.at[h], me).wait_recv()

        with jax.named_scope("fwd_comp"):
            x = xbuf[h]
            for j in range(n_fblk):
                cols = slice(j * fblk, (j + 1) * fblk)
                a = dot(x, up[:, cols]).astype(BF16)
                abuf[m, rows, cols] = a
                hbuf[m, rows, cols] = gelu_fwd(a.astype(F32)).astype(BF16)
            y = (x.astype(F32) + dot(hbuf[m, rows, :], down[...])).astype(BF16)
            ybuf[h] = y

        @pl.when(jnp.logical_not(last))
        def _():
            y_copy(h).start()

        @pl.when(last)
        def _():
            yf = y.astype(F32)
            inv = lax.rsqrt(jnp.mean(yf * yf, axis=-1, keepdims=True) + EPS)
            nbuf[m, rows, :] = (yf * inv).astype(BF16)
            pl.when(sub == per - 1)(n_copy(m).start)

        @pl.when(sub == per - 1)
        def _():
            pltpu.make_async_copy(hbuf.at[m], hid_out.at[m], out_sem.at[0]).start()
            pltpu.make_async_copy(x_rows(m), xs_out.at[pl.ds(m * per, per)], out_sem.at[1]).start()

        return carry

    lax.fori_loop(0, n_part, fwd, 0)

    @pl.when(chip < n_stage // 4)
    def _():
        idle_work()

    n_forward = remote(nbuf.at[me], nbuf.at[me], nf_send, n_recv.at[me], mate)
    with jax.named_scope("n_wait"):

        @pl.when(jnp.logical_not(last))
        def _():
            remote(nbuf.at[me], nbuf.at[me], n_send, n_recv.at[me], me).wait_recv()
            pl.when(mate != last_id)(n_forward.start)
            remote(nbuf.at[mate], nbuf.at[mate], n_send, n_recv.at[mate], me).wait_recv()

        for k in range(2):
            n_t[:, k * seq:(k + 1) * seq] = nbuf[2 * chip + k].T

    peers = [lax.rem(me + 2 * d, n_stage) for d in range(1, n_stage // 2)]
    ag_copies = [remote(nbuf.at[me], nbuf.at[me], ag_send.at[d], ag_recv.at[me], p) for d, p in enumerate(peers)]
    for c, p in zip(ag_copies, peers):
        pl.when(p != last_id)(c.start)
    with jax.named_scope("e_wait"):
        pltpu.make_async_copy(emb_hbm.at[pl.ds(0, base)], emb.at[pl.ds(0, base)], e_sem.at[0]).wait()
        pl.when(core == 0)(e_more.wait)

    pair = 2 * seq
    scale = dim ** -0.5
    inv_count = 1.0 / n_tok
    log_count = math.log2(n_tok)
    lab = lab_ref[:, pl.ds(pl.multiple_of(chip * pair, pair), pair)]

    def logits(rows, size):
        e = emb[rows, :]
        parts = [dot(e[k * size // 2:(k + 1) * size // 2], n_t[...]) for k in range(2)]
        z = jnp.concatenate([(p * scale).astype(BF16) for p in parts], axis=0)
        zbuf[rows, :] = z
        return z

    def peak(z, size, top):
        best = jnp.max(z.reshape(size // 16, 16, pair), axis=0).astype(F32)
        return jnp.maximum(top, jnp.maximum(best[:8], best[8:]))

    def total(z, size, old, top, tot):
        off = top * LOG2E
        return tot * jnp.exp2(old * LOG2E - off) + jnp.sum(jnp.exp2(z.astype(F32).reshape(size // 8, 8, pair) * LOG2E - off[None]), axis=0)

    tops[0] = jnp.full((8, pair), -jnp.inf, F32)
    tops[1] = jnp.zeros((8, pair), F32)

    @pl.when(core == 0)
    def _():
        z = logits(pl.ds(base, extra), extra)
        top = peak(z, extra, tops[0])
        tops[1] = total(z, extra, tops[0], top, tops[1])
        tops[0] = top

    def logits_step(i, slot, old, top, tot):
        z = logits(pl.ds(pl.multiple_of(i * tile, 16), tile), tile)
        tot = total(z_pair[1 - slot], tile, old, top, tot)
        z_pair[slot] = z
        return top, peak(z, tile, top), tot

    with jax.named_scope("logits"):
        z = logits(pl.ds(0, tile), tile)
        z_pair[0] = z
        state = (tops[0], peak(z, tile, tops[0]), tops[1])
        state = lax.fori_loop(0, (n_tiles - 1) // 2, lambda i, c: logits_step(2 * i + 2, 0, *logits_step(2 * i + 1, 1, *c)), state)
        if n_tiles % 2 == 0:
            state = logits_step(n_tiles - 1, 1, *state)
        old, top, tot = state
        tot = total(z_pair[(n_tiles - 1) % 2], tile, old, top, tot)
    row_top = jnp.max(top, axis=0, keepdims=True)
    row_tot = jnp.sum(tot * jnp.exp2((top - row_top) * LOG2E), axis=0, keepdims=True)
    st_send[0:8, :] = jnp.broadcast_to(row_top, (8, pair))
    st_send[8:16, :] = jnp.broadcast_to(row_tot, (8, pair))
    st_copy = remote(st_send, st_recv, st_sems.at[0], st_sems.at[1], mate)
    with jax.named_scope("stat_x"):
        st_copy.start()
        st_copy.wait()
    far_top = st_recv[0:1, :]
    far_tot = st_recv[8:9, :]
    all_top = jnp.maximum(row_top, far_top)
    mine = row_tot * jnp.exp(row_top - all_top)
    other = far_tot * jnp.exp(far_top - all_top)
    lse = all_top + jnp.log(jnp.where(core == 0, mine + other, other + mine))
    my_shift = lse * LOG2E + log_count
    others = [lax.rem(me + d, n_stage) for d in range(1, n_stage)]

    def spread(buf, sems):
        whole = buf.at[pl.ds(0, n_stage - 1)]
        return [remote(buf.at[me], buf.at[me], sems.at[0], sems.at[1], p) for p in others], remote(whole, whole, sems.at[0], sems.at[1], me)

    statall[me] = jnp.broadcast_to(lse, (8, pair))
    sa_copies, sa_all = spread(statall, sa_sems)
    for c in sa_copies:
        c.start()

    def grads(rows, size, first_row, picked):
        zf = zbuf[rows, :].astype(F32)
        prob = jnp.exp2(zf * LOG2E - my_shift)
        hit = lax.broadcasted_iota(jnp.int32, (size, pair), 0) == lab - (row0 + first_row)
        dz_t = jnp.where(hit, prob - inv_count, prob).astype(BF16)
        got = jnp.where(hit, zf, 0.0).reshape(size // 8, 8, pair)
        return dot_t(dz_t, emb[rows, :]), picked + jnp.sum(got, axis=0)

    tops[0] = jnp.zeros((8, pair), F32)
    dn_acc[...] = jnp.zeros_like(dn_acc)

    @pl.when(core == 0)
    def _():
        dn_acc[...], tops[0] = grads(pl.ds(base, extra), extra, base, tops[0])

    def grad_step(i, picked):
        part, picked = grads(pl.ds(pl.multiple_of(i * wide_tile, 16), wide_tile), wide_tile, i * wide_tile, picked)
        dn_acc[...] += part
        return picked

    with jax.named_scope("grads"):
        picked = lax.fori_loop(0, base // wide_tile, grad_step, tops[0])
    far = pl.ds(pl.multiple_of((1 - core) * seq, seq), seq)
    near = pl.ds(pl.multiple_of(core * seq, seq), seq)
    dn_send[...] = dn_acc[far, :]
    dp_copy = remote(dn_send, dn_recv, dp_sems.at[0], dp_sems.at[1], mate)
    dp_copy.start()
    row_loss = jnp.where(core == 0, lse, 0.0) - jnp.sum(picked, axis=0, keepdims=True)
    lossall[me] = jnp.broadcast_to(row_loss, (8, pair))
    lo_copies, lo_all = spread(lossall, lo_sems)
    for c in lo_copies:
        c.start()
    with jax.named_scope("dn_x"):
        dp_copy.wait()
        dn = ((dn_acc[near, :] + dn_recv[...]) * scale).astype(BF16)
    dn_copy = remote(dn_own, dnbuf.at[me], dn_ssem, dn_rsem.at[me], last_id)

    @pl.when(last)
    def _():
        dnbuf[last_id] = dn

    @pl.when(jnp.logical_not(last))
    def _():
        dn_own[...] = dn
        dn_copy.start()

    with jax.named_scope("ag_wait"):
        for p in peers:
            got = remote(nbuf.at[p], nbuf.at[p], ag_send.at[0], ag_recv.at[p], me)
            pl.when(jnp.logical_not(last))(got.wait_recv)
            pl.when(mate != last_id)(remote(nbuf.at[p], nbuf.at[p], fw_send, ag_recv.at[p], mate).start)

    near_dst = [1, 2, n_stage - 2]
    far_dst = n_stage // 2
    n_relay = (n_micro - 2) // 2

    def dx0_copies(m):
        return [remote(dxbuf.at[m], dx0buf.at[m], d_send.at[k], d_recv.at[m], dev) for k, dev in enumerate(near_dst + [far_dst])]

    def relayed(m):
        return (m < 2 * n_relay) & (((me == 2) & (lax.rem(m, 2) == 0)) | ((me == n_stage - 2) & (lax.rem(m, 2) == 1)))

    def relay_far(m):
        return remote(dx0buf.at[m], dx0buf.at[m], r_sems.at[1], d_recv.at[m], far_dst)

    def bwd(m):
        with jax.named_scope("bwd_wait"):
            @pl.when(jnp.logical_not(last))
            def _():
                remote(gbuf.at[m], gbuf.at[m], b_send, b_recv.at[m], me).wait_recv()

            @pl.when(last)
            def _():
                @pl.when(m != last_id)
                def _():
                    remote(dnbuf.at[m], dnbuf.at[m], dn_ssem, dn_rsem.at[m], me).wait_recv()

                yf = ybuf[pl.ds(m * per, per)].reshape(seq, dim).astype(F32)
                inv = lax.rsqrt(jnp.mean(yf * yf, axis=-1, keepdims=True) + EPS)
                dnf = dnbuf[m].astype(F32)
                proj = jnp.mean(yf * dnf, axis=-1, keepdims=True)
                gbuf[m] = (dnf * inv - yf * (inv * inv * inv * proj)).astype(BF16)

        with jax.named_scope("bwd_comp"):
            g = gbuf[m]
            for j in range(n_fblk):
                cols = slice(j * fblk, (j + 1) * fblk)
                dh = dot(g, down_t[:, cols]).astype(BF16).astype(F32)
                abuf[m, :, cols] = (dh * gelu_slope(abuf[m, :, cols].astype(F32))).astype(BF16)
            dxbuf[m] = (g.astype(F32) + dot(abuf[m], up_t[...])).astype(BF16)

        @pl.when(jnp.logical_not(first))
        def _():
            remote(dxbuf.at[m], gbuf.at[m], b_send, b_recv.at[m], me - 1).start()

        @pl.when(first)
        def _():
            copies = dx0_copies(m)
            for c in copies[:-1]:
                c.start()
            pl.when(m >= 2 * n_relay)(copies[-1].start)

        pltpu.make_async_copy(abuf.at[m], da_out.at[m], out_sem.at[2]).start()
        pltpu.make_async_copy(gbuf.at[m], g_out.at[m], out_sem.at[3]).start()

    n_slot = obuf.shape[0]
    busy = chip == last_id // 2
    far_tile = remote(tmp_out.at[core, pl.ds(0, plan.rows)], tmp_out.at[core, pl.ds(0, plan.rows)], ic_send, od_recv, jnp.where(first, last_id, last_id - 1))
    sends_far = first | (me == last_id - 2)

    def tile_copy(k):
        rows = pl.ds(pl.multiple_of(k * plan.rows, plan.rows), plan.rows)
        slot = lax.rem(k, n_slot)
        return pltpu.make_async_copy(obuf.at[slot], tmp_out.at[core, rows], o_sem.at[slot])

    def piece(p):
        k = p // plan.per_tile
        rows = pl.ds(pl.multiple_of(p * plan.piece, plan.piece), plan.piece)
        here = pl.ds(pl.multiple_of(lax.rem(p, plan.per_tile) * plan.piece, plan.piece), plan.piece)
        return remote(obuf.at[lax.rem(k, n_slot), here], tmp_out.at[core, rows], od_send.at[k], od_recv, mate)

    def tile_sent(k):
        slot = lax.rem(k, n_slot)
        return remote(obuf.at[slot], tmp_out.at[core, pl.ds(0, plan.rows)], od_send.at[k], od_recv, mate)

    def emb_tile(k):
        with jax.named_scope("tile_prep"):

            @pl.when(k == 0)
            def _():
                for d in range(1, n_stage // 2):
                    src = lax.rem(mate + 2 * d, n_stage)
                    pl.when(jnp.logical_not(last))(remote(nbuf.at[src], nbuf.at[src], ag_send.at[0], ag_recv.at[src], me).wait_recv)
                for m in range(n_micro):
                    n_all_t[:, m * seq:(m + 1) * seq] = nbuf[m].T
                sa_all.wait_recv()
                for c in range(n_stage // 2):
                    shift[:, c * pair:(c + 1) * pair] = statall[2 * c, 0:1, :] * LOG2E + log_count

        slot = lax.rem(k, n_slot)
        with jax.named_scope("tile_wait"):
            @pl.when(k == 1)
            def _():
                tile_copy(0).wait()
                pl.when(sends_far)(far_tile.start)

            pl.when(k > n_slot)(lambda: tile_copy(k - n_slot).wait())
            pl.when((k >= n_slot) & (k - n_slot < plan.shared) & jnp.logical_not(busy & (k == n_slot)))(lambda: tile_sent(k - n_slot).wait_send())

        with jax.named_scope("tile"):
            rows = pl.ds(pl.multiple_of(k * plan.rows, plan.rows), plan.rows)
            logit_grad(emb[rows, :], n_all_t, shift, lab_ref, row0 + k * plan.rows, inv_count, scale, dz)
            obuf[slot] = dot(dz[...], nbuf[...].reshape(n_tok, dim)) * scale

        tile_copy(k).start()

    def send_pieces(done, until):
        lax.fori_loop(done, until, lambda p, c: (piece(p).start(), c)[1], 0)
        return jnp.maximum(done, until)

    before = sum(jnp.where(me == s, plan.before[s], 0) for s in range(n_stage))

    def pass_dx0(m, carry):
        @pl.when(jnp.logical_not(first))
        def _():
            remote(dx0buf.at[m], dx0buf.at[m], r_sems.at[0], d_recv.at[m], me).wait_recv()

            @pl.when(core == 0)
            def _():
                remote(dx0buf.at[m], dx0buf.at[m], r_sems.at[0], d_recv.at[m], mate).start()

            @pl.when(relayed(m))
            def _():
                relay_far(m).start()

            pltpu.make_async_copy(dx0buf.at[m], dx0_out.at[m], out_sem.at[4]).start()

        @pl.when(first)
        def _():
            pltpu.make_async_copy(dxbuf.at[m], dx0_out.at[m], out_sem.at[4]).start()

        return carry

    lead = jnp.where(me == 2, 40, jnp.where(me == n_stage - 2, -1437, jnp.where(me == far_dst, -1150, -10**6)))

    def work(i, carry):
        sent, passed = carry
        chunk = (i >= before) & (i < before + n_micro)
        pl.when(chunk)(lambda: bwd(i - before))
        k = jnp.where(i < before, i, i - n_micro)
        pl.when(jnp.logical_not(chunk))(lambda: emb_tile(k))
        after = i - before - n_micro + 1
        here = jnp.where(after > 0, jnp.clip((after * 257 + lead) // 146, 0, n_micro), 0)
        lax.fori_loop(passed, here, pass_dx0, 0)
        ready = jnp.where(i < before, i + 1, jnp.where(chunk, before, i + 1 - n_micro)) * plan.per_tile
        near_chunks = chunk | ((i < before) & (i + 1 >= before))
        until = jnp.minimum(jnp.minimum(ready, plan.shared * plan.per_tile), sent + jnp.where(near_chunks, 1, plan.per_tile + 1))
        return send_pieces(sent, until), jnp.maximum(passed, here)

    sent, passed = lax.fori_loop(0, plan.tiles + n_micro, work, (jnp.where(busy, plan.per_tile, 0), 0))
    outs = [pltpu.make_async_copy(nbuf, n_out, out_sem.at[5]), pltpu.make_async_copy(lossall, loss_out, out_sem.at[6]), pltpu.make_async_copy(meta, meta_out, out_sem.at[7])]
    lo_all.wait_recv()
    for c in outs:
        c.start()
    pltpu.make_async_copy(statall, stat_out, out_sem.at[8]).start()
    with jax.named_scope("relay_all"):
        lax.fori_loop(passed, n_micro, pass_dx0, 0)

    with jax.named_scope("drain"):
        send_pieces(sent, plan.shared * plan.per_tile)
        for k in range(max(plan.tiles - n_slot, 0), plan.tiles):
            tile_copy(k).wait()
            if k < plan.shared:
                tile_sent(k).wait_send()
        pl.when(sends_far)(far_tile.wait_send)
        all_rows = pl.ds(0, plan.shared * plan.rows)
        remote(tmp_out.at[1 - core, all_rows], tmp_out.at[1 - core, all_rows], od_send.at[0], od_recv, me).wait_recv()
        sa_all.wait_send()
        lo_all.wait_send()
        pltpu.make_async_copy(statall, stat_out, out_sem.at[8]).wait()
        for c, p in zip(ag_copies, peers):
            pl.when(p != last_id)(c.wait_send)

        @pl.when(jnp.logical_not(last))
        def _():
            dn_copy.wait_send()
            pl.when(mate != last_id)(n_forward.wait_send)
            remote(ybuf, xbuf, f_send, f_recv.at[0], me + 1).wait_send()

        @pl.when(last)
        def _():
            remote(nbuf, nbuf, n_send, n_recv.at[0], me).wait_send()

        @pl.when(mate != last_id)
        def _():
            some = nbuf.at[pl.ds(0, len(peers))]
            remote(some, some, fw_send, ag_recv.at[0], mate).wait_send()

        @pl.when(jnp.logical_not(first) & (me + 2 < n_micro))
        def _():
            x_copy(0).wait_send()

            @pl.when(me < 2)
            def _():
                x_copy(1).wait_send()

        @pl.when(jnp.logical_not(first))
        def _():
            remote(dxbuf, gbuf, b_send, b_recv.at[0], me).wait_send()
            pl.when(core == 0)(remote(dx0buf, dx0buf, r_sems.at[0], d_recv.at[0], mate).wait_send)

        @pl.when(first)
        def _():
            for k in range(len(near_dst)):
                remote(dxbuf, dx0buf, d_send.at[k], d_recv.at[0], me).wait_send()
            direct = pl.ds(0, n_micro - 2 * n_relay)
            remote(dxbuf.at[direct], dx0buf.at[direct], d_send.at[len(near_dst)], d_recv.at[0], me).wait_send()

        @pl.when((me == 2) | (me == n_stage - 2))
        def _():
            some = dx0buf.at[pl.ds(0, n_relay)]
            remote(some, some, r_sems.at[1], d_recv.at[0], me).wait_send()

        pltpu.make_async_copy(hbuf, hid_out, out_sem.at[0]).wait()
        pltpu.make_async_copy(xbuf, xs_out, out_sem.at[1]).wait()
        pltpu.make_async_copy(abuf, da_out, out_sem.at[2]).wait()
        pltpu.make_async_copy(gbuf, g_out, out_sem.at[3]).wait()
        pltpu.make_async_copy(dx0buf, dx0_out, out_sem.at[4]).wait()
        for c in outs:
            c.wait()


class Plan:
    def __init__(self, vocab, n_stage):
        units = vocab // LANES
        self.base = units // 2 * LANES
        self.extra = vocab - 2 * self.base
        self.head_tile = next(t for t in (1600, 1536, 1280, 1024, 768, 640, 512, 256, 128) if self.base % t == 0)
        self.rows = 1024
        self.tiles, self.shared = 10, 8
        self.grad_tile = next(t for t in (3200, 1600, 1280, 640, 256, 128) if self.base % t == 0)
        self.e_parts = next(k for k in (10, 8, 5, 4, 2, 1) if self.base % (16 * k) == 0)
        self.part = 128
        self.slots = 4
        self.piece = 256
        self.per_tile = self.rows // self.piece
        measured = [10, 10, 7, 6, 3, 2, 0, 0]
        self.before = (measured + [0] * n_stage)[:n_stage]
        mid = self.base + self.extra
        ends = [(0, mid), (mid, vocab)]
        early = (self.tiles * self.rows, self.shared * self.rows)
        self.spans = [[(ends[h][0] + early[0 if h == c else 1], ends[h][1]) for h in (c, 1 - c)] for c in range(2)]
        self.longest = [max(self.spans[c][k][1] - self.spans[c][k][0] for c in range(2)) for k in range(2)]
        best = min(range(16, 1281, 16), key=lambda r: (sum(-(-n // r) for n in self.longest)) * (r + 40))
        self.calc_rows = best
        self.calc_steps = [-(-n // best) for n in self.longest]
        self.steps = sum(self.calc_steps)
        self.copy_rows = self.rows
        self.copies = self.tiles + self.shared
        self.starts = ends

    def calc_start(self, core, s):
        k = 0 if s < self.calc_steps[0] else 1
        lo, hi = self.spans[core][k]
        return min(lo + (s - k * self.calc_steps[0]) * self.calc_rows, hi - self.calc_rows)

    def copy_start(self, core, c):
        own = c < self.tiles
        h = core if own else 1 - core
        return self.starts[h][0] + (c if own else c - self.tiles) * self.copy_rows

    def cuts(self, core):
        firsts = [(self.calc_start(core, s), self.calc_rows) for s in range(self.steps)] + [(self.copy_start(core, c), self.copy_rows) for c in range(self.copies)]
        flat = [v for lo, rows in firsts for v in (lo, lo + rows)]
        return flat + [0] * (LANES - len(flat))


def run_pipe(x0, emb, w_up, w_down, labels, tokens, cuts, n_stage, plan):
    n_micro, seq = labels.shape
    dim, ffn = w_up.shape
    n_tok = n_micro * seq
    base = plan.base
    any_spec = pl.BlockSpec(memory_space=pl.ANY)
    act = (n_micro, seq, dim)
    fine = (n_tok // plan.part, plan.part, dim)
    wide = (n_micro, seq, ffn)
    dma = pltpu.SemaphoreType.DMA
    vm = pltpu.VMEM
    pair = 2 * seq
    return pl.pallas_call(
        functools.partial(pipe_kernel, n_stage, plan),
        out_shape=[
            jax.ShapeDtypeStruct(act, BF16), jax.ShapeDtypeStruct(fine, BF16), jax.ShapeDtypeStruct(wide, BF16),
            jax.ShapeDtypeStruct(wide, BF16), jax.ShapeDtypeStruct(act, BF16), jax.ShapeDtypeStruct(act, BF16),
            jax.ShapeDtypeStruct((n_stage, 8, pair), F32), jax.ShapeDtypeStruct((n_stage, 8, pair), F32), jax.ShapeDtypeStruct((2, plan.tiles * plan.rows, dim), F32),
            jax.ShapeDtypeStruct((3 * n_tok // LANES, LANES), jnp.int32),
        ],
        in_specs=[any_spec] * 4 + [pl.BlockSpec(memory_space=pltpu.VMEM)] * 3,
        out_specs=[any_spec] * 10,
        scratch_shapes=[
            vm(fine, BF16), vm(fine, BF16), vm(wide, BF16), vm(wide, BF16), vm(act, BF16), vm(act, BF16), vm(act, BF16), vm(act, BF16), vm(act, BF16),
            vm((dim, ffn), BF16), vm((ffn, dim), BF16), vm((ffn, dim), BF16), vm((dim, ffn), BF16),
            vm((base + plan.extra, dim), BF16), vm((base + plan.extra, pair), BF16), vm((dim, pair), BF16), vm((pair, dim), F32),
            vm((seq, dim), F32), vm((seq, dim), F32), vm((seq, dim), BF16), vm((16, pair), F32), vm((16, pair), F32), vm((n_stage, 8, pair), F32), vm((n_stage, 8, pair), F32),
            vm((2, 8, pair), F32), vm((dim, n_tok), BF16), vm((1, n_tok), F32), vm((plan.rows, n_tok), BF16), vm((plan.slots, plan.rows, dim), F32),
            vm((2, plan.head_tile, pair), BF16), vm((3 * n_tok // LANES, LANES), jnp.int32),
            dma((2,)), dma((2,)), dma((2,)), dma((2,)), dma((n_micro,)), dma, dma((n_tok // plan.part,)), dma, dma((n_micro,)), dma,
            dma((n_stage // 2,)), dma((n_micro,)), dma,
            dma((2,)), dma((2,)), dma, dma((n_stage,)), dma((2,)), dma((2,)), dma, dma((n_micro,)), dma((4,)), dma((n_micro,)), dma((2,)), dma((9,)),
            dma((plan.slots,)), dma((plan.shared,)), dma, dma,
        ],
        compiler_params=pltpu.CompilerParams(collective_id=0, has_side_effects=True, vmem_limit_bytes=67_000_000),
        cost_estimate=pl.CostEstimate(flops=60 * 10**9, bytes_accessed=100 * 10**6, transcendentals=0),
        name="pipe",
    )(x0.reshape(x0.shape[0], seq // plan.part, plan.part, dim), emb, w_up, w_down, labels.reshape(1, n_tok), tokens.reshape(1, n_tok), cuts)


def fin_kernel(n_stage, n_tok, plan, ids_ref, emb_hbm, tmp_hbm, n_hbm, stat_ref, part_ref, lab_ref, meta_ref, dx0_hbm, xs_hbm, hid_hbm, da_hbm, g_hbm,
               out_hbm, loss_ref, gup_hbm, gdown_hbm,
               n_all, dx0, xs, hid, da, g, n_t, x_t, dx0s, dz, shift, e_in, c_out, cp, gup, gdown,
               ld_sem, e_sem, t_sem, co_sem, po_sem, gu_sem, gd_sem, wi_sem):
    dim, ffn = gup_hbm.shape
    scale = dim ** -0.5
    inv_count = 1.0 / n_tok
    steps, crows, prows = plan.steps, plan.calc_rows, plan.copy_rows
    core = lax.rem(lax.axis_index("stage"), 2)
    early = plan.tiles * prows
    wblk = gup.shape[2]
    n_wblk = ffn // wblk
    turn = plan.calc_steps[0]

    def pick(pair):
        return jnp.where(core == 0, pair[0], pair[1])

    def calc_start(s):
        own = s < turn
        lo, hi = [jnp.where(own, pick([plan.spans[c][0][e] for c in range(2)]), pick([plan.spans[c][1][e] for c in range(2)])) for e in range(2)]
        return pl.multiple_of(jnp.minimum(lo + (s - jnp.where(own, 0, turn)) * crows, hi - crows), 16)

    def copy_start(c):
        own = c < plan.tiles
        first = jnp.where(own, pick([plan.starts[0][0], plan.starts[1][0]]), pick([plan.starts[1][0], plan.starts[0][0]]))
        return pl.multiple_of(first + (c - jnp.where(own, 0, plan.tiles)) * prows, 16)

    def e_copy(s):
        return pltpu.make_async_copy(emb_hbm.at[pl.ds(calc_start(s), crows)], e_in.at[lax.rem(s, 2)], e_sem.at[lax.rem(s, 2)])

    n_slot = cp.shape[0]
    ahead = 3

    def t_copy(c):
        own = c < plan.tiles
        row = jnp.where(own, core, 1 - core) * early + (c - jnp.where(own, 0, plan.tiles)) * prows
        slot = lax.rem(c, n_slot)
        return pltpu.make_async_copy(tmp_hbm.at[pl.ds(pl.multiple_of(row, 16), prows)], cp.at[slot], t_sem.at[slot])

    def p_out(c):
        slot = lax.rem(c, n_slot)
        return pltpu.make_async_copy(cp.at[slot], out_hbm.at[pl.ds(copy_start(c), prows)], po_sem.at[slot])

    def c_outs(s):
        slot = lax.rem(s, 2)
        return pltpu.make_async_copy(c_out.at[slot], out_hbm.at[pl.ds(calc_start(s), crows)], co_sem.at[slot])

    loads = [pltpu.make_async_copy(s, d, ld_sem.at[i]) for i, (s, d) in enumerate(((n_hbm, n_all), (dx0_hbm, dx0), (xs_hbm, xs), (g_hbm, g)))]
    loads[0].start()
    loads[1].start()
    e_copy(0).start()
    for c in range(ahead):
        t_copy(c).start(priority=1)
    pair = stat_ref.shape[2]
    loss = jnp.zeros((1, pair), F32)
    for d in range(n_stage):
        if d % 2 == 0:
            shift[:, (d // 2) * pair:(d // 2 + 1) * pair] = stat_ref[d, 0:1, :] * LOG2E + math.log2(n_tok)
        loss = loss + part_ref[d, 0:1, :]
    loss_ref[0] = jnp.sum(loss) * inv_count
    with jax.named_scope("fin_pre"):
        loads[0].wait()
        n_t[...] = n_all[...].T

    def sum_rows():
        loads[1].wait()
        dense = jnp.concatenate([meta_ref[g:g + 1, :] for g in range(n_tok // LANES)], axis=1)
        order = lax.broadcasted_iota(jnp.int32, (n_tok, n_tok), 0) == dense
        dx0s[...] = dot(jnp.where(order, 1.0, 0.0).astype(BF16), dx0[...])

    def add_rows(k, start, ref):
        lo, hi = ids_ref[2 * n_tok + k], ids_ref[2 * n_tok + k + 1]
        wide = 8

        def some(p, width):
            at = [pl.ds(ids_ref[n_tok + p + u] - start, 1) for u in range(width)]
            new = [ref[at[u], :] + dx0s[pl.ds(p + u, 1), :] for u in range(width)]
            for u in range(width):
                ref[at[u], :] = new[u]

        def group(g, carry):
            some(lo + g * wide, wide)
            return carry

        def single(p, carry):
            some(p, 1)
            return carry

        n_grp = (hi - lo) // wide
        lax.fori_loop(0, n_grp, group, 0)
        lax.fori_loop(lo + n_grp * wide, hi, single, 0)

    def w_ins(w):
        cols = pl.ds(pl.multiple_of(w * wblk, wblk), wblk)
        wslot = lax.rem(w, 2)
        return (pltpu.make_async_copy(da_hbm.at[:, cols], da.at[wslot], wi_sem.at[0, wslot]), pltpu.make_async_copy(hid_hbm.at[:, cols], hid.at[wslot], wi_sem.at[1, wslot]))

    def w_outs(w):
        cols = pl.ds(pl.multiple_of(w * wblk, wblk), wblk)
        wslot = lax.rem(w, 2)
        return (pltpu.make_async_copy(gup.at[wslot], gup_hbm.at[:, cols], gu_sem.at[wslot]), pltpu.make_async_copy(gdown.at[wslot], gdown_hbm.at[cols], gd_sem.at[wslot]))

    def copy_tile(c, carry):
        with jax.named_scope("copy_wait"):
            t_copy(c).wait()
        with jax.named_scope("add_p"):
            add_rows(2 * steps + 2 * c, copy_start(c), cp.at[lax.rem(c, n_slot)])
        p_out(c).start()

        @pl.when(c + ahead < plan.copies)
        def _():
            pl.when(c + ahead >= n_slot)(lambda: p_out(c + ahead - n_slot).wait())
            t_copy(c + ahead).start(priority=1)

        return carry

    w_first = 2
    tails = [turn - 1, steps - 1]

    def tail(s):
        return (s == tails[0]) | (s == tails[1])

    def step(s, carry):
        pl.when(s + 1 < steps)(lambda: e_copy(s + 1).start())
        with jax.named_scope("fin_wait"):
            e_copy(s).wait()

        @pl.when(s == 0)
        def _():
            for c in loads[2:]:
                c.start()

        w = s - w_first

        @pl.when((w + 1 >= 0) & (w + 1 < n_wblk))
        def _():
            for c in w_ins(w + 1):
                c.start()

        pl.when((s >= 2) & jnp.logical_not(tail(s - 1)))(lambda: c_outs(s - 2).wait())
        slot = lax.rem(s, 2)
        start = calc_start(s)
        with jax.named_scope("calc"):
            logit_grad(e_in[slot], n_t, shift, lab_ref, start, inv_count, scale, dz)
            c_out[slot] = dot(dz[...], n_all[...]) * scale
        pl.when(s == 0)(sum_rows)
        with jax.named_scope("add_c"):
            add_rows(2 * s, start, c_out.at[slot])
        pl.when(tail(s))(lambda: c_outs(s - 1).wait())
        c_outs(s).start()
        lax.fori_loop(s * plan.copies // (steps - 1), jnp.minimum((s + 1) * plan.copies // (steps - 1), plan.copies), copy_tile, 0)

        @pl.when(w == 0)
        def _():
            for c in loads[2:]:
                c.wait()
            x_t[...] = xs[...].T

        @pl.when((w >= 0) & (w < n_wblk))
        def _():
            wslot = lax.rem(w, 2)
            with jax.named_scope("dw_wait"):
                for c in w_ins(w):
                    c.wait()

                @pl.when(w >= 2)
                def _():
                    for c in w_outs(w - 2):
                        c.wait()

            with jax.named_scope("dw"):
                gup[wslot] = dot(x_t[...], da[wslot])
                gdown[wslot] = dot_t(hid[wslot], g[...])
            for c in w_outs(w):
                c.start()

        return carry

    lax.fori_loop(0, steps, step, 0)
    with jax.named_scope("fin_drain"):
        for w in range(n_wblk - 2, n_wblk):
            for c in w_outs(w):
                c.wait()
        c_outs(steps - 1).wait()
        for c in range(plan.copies - n_slot, plan.copies):
            p_out(c).wait()


def run_fin(emb, tmp, n_all, stats, losses, labels, meta, dx0, xs, hid, da, g, n_stage, plan):
    vocab, dim = emb.shape
    n_tok, ffn = hid.shape
    vm = pltpu.VMEM
    dma = pltpu.SemaphoreType.DMA
    any_spec = pl.BlockSpec(memory_space=pl.ANY)
    vspec = pl.BlockSpec(memory_space=pltpu.VMEM)
    smem = pl.BlockSpec(memory_space=pltpu.SMEM)
    wblk = 256
    return pl.pallas_call(
        functools.partial(fin_kernel, n_stage, n_tok, plan),
        out_shape=[jax.ShapeDtypeStruct((vocab, dim), F32), jax.ShapeDtypeStruct((1,), F32), jax.ShapeDtypeStruct((dim, ffn), F32), jax.ShapeDtypeStruct((ffn, dim), F32)],
        in_specs=[smem, any_spec, any_spec, any_spec, vspec, vspec, vspec, vspec] + [any_spec] * 5,
        out_specs=[any_spec, smem, any_spec, any_spec],
        scratch_shapes=[
            vm((n_tok, dim), BF16), vm((n_tok, dim), BF16), vm((n_tok, dim), BF16), vm((2, n_tok, wblk), BF16), vm((2, n_tok, wblk), BF16), vm((n_tok, dim), BF16),
            vm((dim, n_tok), BF16), vm((dim, n_tok), BF16), vm((n_tok, dim), F32), vm((plan.calc_rows, n_tok), BF16), vm((1, n_tok), F32),
            vm((2, plan.calc_rows, dim), BF16), vm((2, plan.calc_rows, dim), F32), vm((5, plan.copy_rows, dim), F32),
            vm((2, dim, wblk), F32), vm((2, wblk, dim), F32),
            dma((4,)), dma((2,)), dma((5,)), dma((2,)), dma((5,)), dma((2,)), dma((2,)), dma((2, 2)),
        ],
        compiler_params=pltpu.CompilerParams(vmem_limit_bytes=67_000_000),
        cost_estimate=pl.CostEstimate(flops=2 * n_tok * vocab * dim, bytes_accessed=5 * vocab * dim, transcendentals=0),
        name="fin",
    )(meta.reshape(-1), emb, tmp, n_all, stats, losses, labels.reshape(1, n_tok), meta, dx0, xs, hid, da, g)


def solution(mesh):
    n_stage = mesh.shape["stage"]

    def device_fn(tokens, labels, emb, w_up, w_down):
        n_micro, seq = tokens.shape
        vocab, dim = emb.shape
        w_up, w_down = w_up[0], w_down[0]
        n_tok = n_micro * seq
        plan = Plan(vocab, n_stage)
        cuts = jnp.array([plan.cuts(0), plan.cuts(1)], jnp.int32)
        x0 = run_gather(tokens, emb)
        n_all, xs, hid, da, g, dx0, stats, losses, tmp, meta = run_pipe(x0, emb, w_up, w_down, labels, tokens, cuts, n_stage, plan)
        flat = lambda p: p.reshape(n_tok, -1)
        grad_emb, loss, grad_up, grad_down = run_fin(
            emb, tmp.reshape(-1, dim), flat(n_all), stats, losses, labels, meta, flat(dx0), flat(xs), flat(hid), flat(da), flat(g), n_stage, plan
        )
        return loss, grad_up[None], grad_down[None], grad_emb

    return jax.shard_map(device_fn, mesh=mesh, in_specs=(P("dp", None), P("dp", None), P(None, None), P("stage", None, None), P("stage", None, None)), out_specs=(P("dp"), P(("dp", "stage"), None, None), P(("dp", "stage"), None, None), P("dp", None)), check_vma=False)
```

```python
import functools
import math

import jax
import jax.numpy as jnp
from jax import lax
from jax.experimental import pallas as pl
from jax.experimental.pallas import tpu as pltpu
from jax.sharding import PartitionSpec as P


MESH = pl.DeviceIdType.MESH
LOG2E = math.log2(math.e)
LN2 = math.log(2.0)
GELU_C = math.sqrt(2.0 / math.pi)
GELU_K = 0.044715
EPS = 1e-6
LANES = 128
F32 = jnp.float32
BF16 = jnp.bfloat16


def gelu_fwd(a):
    return 0.5 * a * (1.0 + jnp.tanh(GELU_C * (a + GELU_K * (a * a * a))))


def gelu_slope(a):
    a2 = a * a
    t = jnp.tanh(GELU_C * (a + GELU_K * (a2 * a)))
    return 0.5 * (1.0 + t) + (0.5 * a) * (1.0 - t * t) * (GELU_C + (3.0 * GELU_C * GELU_K) * a2)


def dot(x, y):
    return jnp.dot(x, y, preferred_element_type=F32)


def dot_t(x, y):
    return lax.dot_general(x, y, (((0,), (0,)), ((), ())), preferred_element_type=F32)


def remote(src, dst, send_sem, recv_sem, dev):
    return pltpu.make_async_remote_copy(src_ref=src, dst_ref=dst, send_sem=send_sem, recv_sem=recv_sem, device_id={"stage": dev}, device_id_type=MESH)


def column(row):
    return jnp.broadcast_to(row, (LANES, LANES)).T


def gather_kernel(ids_ref, tok_ref, emb_hbm, x0_hbm, tiles, picked, sem, out_sem):
    n_micro, seq = tok_ref.shape
    me = lax.axis_index("stage")
    group = tiles.shape[1] // seq
    slots = tiles.shape[0]
    owners = [head_chunk(me, k, n_micro) for k in range(slots)]

    def fetch(k):
        def one(i, carry):
            t = ids_ref[owners[k] * seq + i]
            start = pl.multiple_of(t // group * group, group)
            pltpu.make_async_copy(emb_hbm.at[pl.ds(start, group)], tiles.at[k, pl.ds(pl.multiple_of(i * group, group), group)], sem.at[k]).start()
            return carry

        lax.fori_loop(0, seq, one, 0, unroll=8)

    def select(k):
        sub = lax.broadcasted_iota(jnp.int32, (LANES, LANES), 0)
        lane = lax.broadcasted_iota(jnp.int32, (LANES, LANES), 1)
        tok = column(tok_ref[pl.ds(owners[k], 1), :].astype(F32)).astype(jnp.int32)
        want = sub * group + (tok - tok // group * group)
        hot = jnp.concatenate([jnp.where(lane + b * LANES == want, 1.0, 0.0).astype(BF16) for b in range(seq * group // LANES)], axis=1)
        pltpu.make_async_copy(emb_hbm.at[pl.ds(0, seq * group)], tiles.at[k], sem.at[k]).wait()
        picked[k] = dot(hot, tiles[k]).astype(BF16)
        pltpu.make_async_copy(picked.at[k], x0_hbm.at[k], out_sem.at[k]).start()

    def finish(k):
        pltpu.make_async_copy(picked.at[k], x0_hbm.at[k], out_sem.at[k]).wait()

    for work in (fetch, select, finish):
        work(0)
        for k in range(1, slots):
            pl.when(me < slots)(functools.partial(work, k))


def head_chunk(dev, k, n_micro):
    return jnp.minimum(jnp.where(dev < 2, 2 * dev + k, dev + 2), n_micro - 1)


def run_gather(tokens, emb):
    n_micro, seq = tokens.shape
    dim = emb.shape[1]
    group = 16
    return pl.pallas_call(
        gather_kernel,
        out_shape=jax.ShapeDtypeStruct((2, seq, dim), BF16),
        in_specs=[pl.BlockSpec(memory_space=pltpu.SMEM), pl.BlockSpec(memory_space=pltpu.VMEM), pl.BlockSpec(memory_space=pl.ANY)],
        out_specs=pl.BlockSpec(memory_space=pl.ANY),
        scratch_shapes=[pltpu.VMEM((2, seq * group, dim), BF16), pltpu.VMEM((2, seq, dim), BF16), pltpu.SemaphoreType.DMA((2,)), pltpu.SemaphoreType.DMA((2,))],
        cost_estimate=pl.CostEstimate(flops=10**9, bytes_accessed=2 * seq * group * dim * 2, transcendentals=0),
        name="gather",
    )(tokens.reshape(n_micro * seq), tokens, emb)


def token_table(row_ref, cut_ref, meta):
    n_tok = row_ref.shape[1]
    n_grp = n_tok // LANES
    lane = lax.broadcasted_iota(jnp.int32, (LANES, LANES), 1).astype(F32)
    sub = lax.broadcasted_iota(jnp.int32, (LANES, LANES), 0)
    row = lambda g: row_ref[:, g * LANES:(g + 1) * LANES].astype(F32)
    zero = jnp.zeros((LANES, LANES), F32)
    fold = lambda acc: jnp.sum(acc, axis=0, keepdims=True)
    cols = [column(row(c)) for c in range(n_grp)]
    firsts = []
    for g in range(n_grp):
        acc = zero
        for c in range(g + 1):
            same = cols[c] == row(g)
            if c == g:
                same = same & (sub < lane.astype(jnp.int32))
            acc = acc + jnp.where(same, 1.0, 0.0)
        firsts.append(column(jnp.where(fold(acc) == 0.0, 1.0, 0.0)))
    ranks = []
    for g in range(n_grp):
        acc = zero
        for c in range(n_grp):
            acc = acc + jnp.where(cols[c] < row(g), firsts[c], 0.0)
        ranks.append(fold(acc))
        meta[g:g + 1, :] = ranks[g].astype(jnp.int32)
    rank_cols = [column(r) for r in ranks]
    for g in range(n_grp):
        acc = zero
        for c in range(n_grp):
            acc = acc + jnp.where(rank_cols[c] == lane + g * LANES, firsts[c] * cols[c], 0.0)
        meta[n_grp + g:n_grp + g + 1, :] = fold(acc).astype(jnp.int32)
    cut = cut_ref[...].astype(F32)
    acc = zero
    for c in range(n_grp):
        acc = acc + jnp.where(cols[c] < cut, firsts[c], 0.0)
    meta[2 * n_grp:3 * n_grp, :] = jnp.broadcast_to(fold(acc), (n_grp, LANES)).astype(jnp.int32)


def logit_grad(e, n_t, shift, lab, first_id, inv_count, scale, dz):
    rows = e.shape[0]
    n_tok = n_t.shape[1]
    blk = 256
    vid = lax.broadcasted_iota(jnp.int32, (rows, blk), 0)
    for j in range(n_tok // blk):
        cols = slice(j * blk, (j + 1) * blk)
        z = (dot(e, n_t[:, cols]) * scale).astype(BF16).astype(F32)
        prob = jnp.exp2(z * LOG2E - shift[:, cols])
        dz[:, cols] = jnp.where(vid == lab[:, cols] - first_id, prob - inv_count, prob).astype(BF16)


def pipe_kernel(n_stage, plan, x0_hbm, emb_hbm, up_hbm, down_hbm, lab_ref, row_ref, cut_ref,
                n_out, xs_out, hid_out, da_out, g_out, dx0_out, stat_out, loss_out, tmp_out, meta_out,
                xbuf, ybuf, abuf, hbuf, nbuf, gbuf, dxbuf, dx0buf, dnbuf, up, down, up_t, down_t,
                emb, zbuf, n_t, dn_acc, dn_send, dn_recv, dn_own, st_send, st_recv, statall, lossall, tops, n_all_t, shift, dz, obuf, z_pair, meta,
                w_sem, e_sem, x_sem, x_send, x_recv, f_send, f_recv, n_send, n_recv, nf_send, ag_send, ag_recv, fw_send,
                st_sems, dp_sems, dn_ssem, dn_rsem, sa_sems, lo_sems, b_send, b_recv, d_send, d_recv, r_sems, out_sem, o_sem, od_send, od_recv, ic_send):
    n_micro, seq, dim = gbuf.shape
    part = xbuf.shape[1]
    n_part = xbuf.shape[0]
    per = seq // part
    n_tok = n_micro * seq
    ffn = up.shape[1]
    vocab = emb_hbm.shape[0]
    me = lax.axis_index("stage")
    core = lax.rem(me, 2)
    chip = me // 2
    mate = me + 1 - 2 * core
    last_id = n_stage - 1
    first = me == 0
    last = me == last_id
    fblk = 512
    n_fblk = ffn // fblk
    base, extra, tile = plan.base, plan.extra, plan.head_tile
    row0 = core * (base + extra)
    n_tiles = base // tile
    wide_tile = plan.grad_tile

    barrier = pltpu.get_barrier_semaphore()
    for d in range(1, n_stage):
        pl.semaphore_signal(barrier, inc=1, device_id={"stage": lax.rem(me + d, n_stage)}, device_id_type=MESH)
    w_copy = [pltpu.make_async_copy(up_hbm, up, w_sem.at[0]), pltpu.make_async_copy(down_hbm, down, w_sem.at[1])]
    for c in w_copy:
        c.start()
    x_slots = x0_hbm.shape[0]
    x_mine = [head_chunk(me, k, n_micro) for k in range(x_slots)]

    def x_rows(m):
        return xbuf.at[pl.ds(m * per, per)]

    def x_local(k):
        return pltpu.make_async_copy(x0_hbm.at[k], x_rows(k), x_sem.at[k])

    @pl.when(first)
    def _():
        for k in range(x_slots):
            x_local(k).start()

    e_parts = plan.e_parts
    e_step = base // e_parts

    def e_copy(i):
        src = emb_hbm.at[pl.ds(pl.multiple_of(row0 + i * e_step, 16), e_step)]
        return pltpu.make_async_copy(src, emb.at[pl.ds(i * e_step, e_step)], e_sem.at[0])

    e_more = pltpu.make_async_copy(emb_hbm.at[pl.ds(base, extra)], emb.at[pl.ds(base, extra)], e_sem.at[1])
    with jax.named_scope("entry"):
        pl.semaphore_wait(barrier, n_stage - 1)

    def x_copy(k):
        return remote(x0_hbm.at[k], x_rows(x_mine[k]), x_send.at[k], x_recv.at[x_mine[k]], 0)

    @pl.when(jnp.logical_not(first) & (me + 2 < n_micro))
    def _():
        x_copy(0).start()

        @pl.when(me < 2)
        def _():
            x_copy(1).start()

    with jax.named_scope("w_wait"):
        for c in w_copy:
            c.wait()
        for i in range(e_parts):
            e_copy(i).start()
        pl.when(core == 0)(e_more.start)

    def transpose_weights():
        for j in range(n_fblk):
            up_t[j * fblk:(j + 1) * fblk, :] = up[:, j * fblk:(j + 1) * fblk].T
            down_t[:, j * fblk:(j + 1) * fblk] = down[j * fblk:(j + 1) * fblk, :].T

    def idle_work():
        transpose_weights()
        token_table(row_ref, jnp.where(core == 0, cut_ref[0:1, :], cut_ref[1:2, :]), meta)

    @pl.when(chip >= n_stage // 4)
    def _():
        idle_work()

    def n_copy(m):
        return remote(nbuf.at[m], nbuf.at[m], n_send, n_recv.at[m], jnp.where(m == last_id, last_id - 1, m))

    def y_copy(h):
        return remote(ybuf.at[h], xbuf.at[h], f_send, f_recv.at[h], me + 1)

    def fwd(h, carry):
        m = h // per
        sub = lax.rem(h, per)
        rows = pl.ds(pl.multiple_of(sub * part, part), part)
        with jax.named_scope("fwd_wait"):

            @pl.when(first & (sub == 0))
            def _():
                @pl.when(m < x_slots)
                def _():
                    x_local(m).wait()

                @pl.when(m >= x_slots)
                def _():
                    remote(x_rows(m), x_rows(m), x_send.at[0], x_recv.at[m], me).wait_recv()

            @pl.when(jnp.logical_not(first))
            def _():
                remote(xbuf.at[h], xbuf.at[h], f_send, f_recv.at[h], me).wait_recv()

        with jax.named_scope("fwd_comp"):
            x = xbuf[h]
            for j in range(n_fblk):
                cols = slice(j * fblk, (j + 1) * fblk)
                a = dot(x, up[:, cols]).astype(BF16)
                abuf[m, rows, cols] = a
                hbuf[m, rows, cols] = gelu_fwd(a.astype(F32)).astype(BF16)
            y = (x.astype(F32) + dot(hbuf[m, rows, :], down[...])).astype(BF16)
            ybuf[h] = y

        @pl.when(jnp.logical_not(last))
        def _():
            y_copy(h).start()

        @pl.when(last)
        def _():
            yf = y.astype(F32)
            inv = lax.rsqrt(jnp.mean(yf * yf, axis=-1, keepdims=True) + EPS)
            nbuf[m, rows, :] = (yf * inv).astype(BF16)
            pl.when(sub == per - 1)(n_copy(m).start)

        @pl.when(sub == per - 1)
        def _():
            pltpu.make_async_copy(hbuf.at[m], hid_out.at[m], out_sem.at[0]).start()
            pltpu.make_async_copy(x_rows(m), xs_out.at[pl.ds(m * per, per)], out_sem.at[1]).start()

        return carry

    lax.fori_loop(0, n_part, fwd, 0)

    @pl.when(chip < n_stage // 4)
    def _():
        idle_work()

    n_forward = remote(nbuf.at[me], nbuf.at[me], nf_send, n_recv.at[me], mate)
    with jax.named_scope("n_wait"):

        @pl.when(jnp.logical_not(last))
        def _():
            remote(nbuf.at[me], nbuf.at[me], n_send, n_recv.at[me], me).wait_recv()
            pl.when(mate != last_id)(n_forward.start)
            remote(nbuf.at[mate], nbuf.at[mate], n_send, n_recv.at[mate], me).wait_recv()

        for k in range(2):
            n_t[:, k * seq:(k + 1) * seq] = nbuf[2 * chip + k].T

    peers = [lax.rem(me + 2 * d, n_stage) for d in range(1, n_stage // 2)]
    ag_copies = [remote(nbuf.at[me], nbuf.at[me], ag_send.at[d], ag_recv.at[me], p) for d, p in enumerate(peers)]
    for c, p in zip(ag_copies, peers):
        pl.when(p != last_id)(c.start)
    with jax.named_scope("e_wait"):
        pltpu.make_async_copy(emb_hbm.at[pl.ds(0, base)], emb.at[pl.ds(0, base)], e_sem.at[0]).wait()
        pl.when(core == 0)(e_more.wait)

    pair = 2 * seq
    scale = dim ** -0.5
    inv_count = 1.0 / n_tok
    log_count = math.log2(n_tok)
    lab = lab_ref[:, pl.ds(pl.multiple_of(chip * pair, pair), pair)]

    def logits(rows, size):
        e = emb[rows, :]
        parts = [dot(e[k * size // 2:(k + 1) * size // 2], n_t[...]) for k in range(2)]
        z = jnp.concatenate([(p * scale).astype(BF16) for p in parts], axis=0)
        zbuf[rows, :] = z
        return z

    def peak(z, size, top):
        best = jnp.max(z.reshape(size // 16, 16, pair), axis=0).astype(F32)
        return jnp.maximum(top, jnp.maximum(best[:8], best[8:]))

    def total(z, size, old, top, tot):
        off = top * LOG2E
        return tot * jnp.exp2(old * LOG2E - off) + jnp.sum(jnp.exp2(z.astype(F32).reshape(size // 8, 8, pair) * LOG2E - off[None]), axis=0)

    tops[0] = jnp.full((8, pair), -jnp.inf, F32)
    tops[1] = jnp.zeros((8, pair), F32)

    @pl.when(core == 0)
    def _():
        z = logits(pl.ds(base, extra), extra)
        top = peak(z, extra, tops[0])
        tops[1] = total(z, extra, tops[0], top, tops[1])
        tops[0] = top

    def logits_step(i, slot, old, top, tot):
        z = logits(pl.ds(pl.multiple_of(i * tile, 16), tile), tile)
        tot = total(z_pair[1 - slot], tile, old, top, tot)
        z_pair[slot] = z
        return top, peak(z, tile, top), tot

    with jax.named_scope("logits"):
        z = logits(pl.ds(0, tile), tile)
        z_pair[0] = z
        state = (tops[0], peak(z, tile, tops[0]), tops[1])
        state = lax.fori_loop(0, (n_tiles - 1) // 2, lambda i, c: logits_step(2 * i + 2, 0, *logits_step(2 * i + 1, 1, *c)), state)
        if n_tiles % 2 == 0:
            state = logits_step(n_tiles - 1, 1, *state)
        old, top, tot = state
        tot = total(z_pair[(n_tiles - 1) % 2], tile, old, top, tot)
    row_top = jnp.max(top, axis=0, keepdims=True)
    row_tot = jnp.sum(tot * jnp.exp2((top - row_top) * LOG2E), axis=0, keepdims=True)
    st_send[0:8, :] = jnp.broadcast_to(row_top, (8, pair))
    st_send[8:16, :] = jnp.broadcast_to(row_tot, (8, pair))
    st_copy = remote(st_send, st_recv, st_sems.at[0], st_sems.at[1], mate)
    with jax.named_scope("stat_x"):
        st_copy.start()
        st_copy.wait()
    far_top = st_recv[0:1, :]
    far_tot = st_recv[8:9, :]
    all_top = jnp.maximum(row_top, far_top)
    mine = row_tot * jnp.exp(row_top - all_top)
    other = far_tot * jnp.exp(far_top - all_top)
    lse = all_top + jnp.log(jnp.where(core == 0, mine + other, other + mine))
    my_shift = lse * LOG2E + log_count
    others = [lax.rem(me + d, n_stage) for d in range(1, n_stage)]

    def spread(buf, sems):
        whole = buf.at[pl.ds(0, n_stage - 1)]
        return [remote(buf.at[me], buf.at[me], sems.at[0], sems.at[1], p) for p in others], remote(whole, whole, sems.at[0], sems.at[1], me)

    statall[me] = jnp.broadcast_to(lse, (8, pair))
    sa_copies, sa_all = spread(statall, sa_sems)
    for c in sa_copies:
        c.start()

    def grads(rows, size, first_row, picked):
        zf = zbuf[rows, :].astype(F32)
        prob = jnp.exp2(zf * LOG2E - my_shift)
        hit = lax.broadcasted_iota(jnp.int32, (size, pair), 0) == lab - (row0 + first_row)
        dz_t = jnp.where(hit, prob - inv_count, prob).astype(BF16)
        got = jnp.where(hit, zf, 0.0).reshape(size // 8, 8, pair)
        return dot_t(dz_t, emb[rows, :]), picked + jnp.sum(got, axis=0)

    tops[0] = jnp.zeros((8, pair), F32)
    dn_acc[...] = jnp.zeros_like(dn_acc)

    @pl.when(core == 0)
    def _():
        dn_acc[...], tops[0] = grads(pl.ds(base, extra), extra, base, tops[0])

    def grad_step(i, picked):
        part, picked = grads(pl.ds(pl.multiple_of(i * wide_tile, 16), wide_tile), wide_tile, i * wide_tile, picked)
        dn_acc[...] += part
        return picked

    with jax.named_scope("grads"):
        picked = lax.fori_loop(0, base // wide_tile, grad_step, tops[0])
    far = pl.ds(pl.multiple_of((1 - core) * seq, seq), seq)
    near = pl.ds(pl.multiple_of(core * seq, seq), seq)
    dn_send[...] = dn_acc[far, :]
    dp_copy = remote(dn_send, dn_recv, dp_sems.at[0], dp_sems.at[1], mate)
    dp_copy.start()
    row_loss = jnp.where(core == 0, lse, 0.0) - jnp.sum(picked, axis=0, keepdims=True)
    lossall[me] = jnp.broadcast_to(row_loss, (8, pair))
    lo_copies, lo_all = spread(lossall, lo_sems)
    for c in lo_copies:
        c.start()
    with jax.named_scope("dn_x"):
        dp_copy.wait()
        dn = ((dn_acc[near, :] + dn_recv[...]) * scale).astype(BF16)
    dn_copy = remote(dn_own, dnbuf.at[me], dn_ssem, dn_rsem.at[me], last_id)

    @pl.when(last)
    def _():
        dnbuf[last_id] = dn

    @pl.when(jnp.logical_not(last))
    def _():
        dn_own[...] = dn
        dn_copy.start()

    with jax.named_scope("ag_wait"):
        for p in peers:
            got = remote(nbuf.at[p], nbuf.at[p], ag_send.at[0], ag_recv.at[p], me)
            pl.when(jnp.logical_not(last))(got.wait_recv)
            pl.when(mate != last_id)(remote(nbuf.at[p], nbuf.at[p], fw_send, ag_recv.at[p], mate).start)

    near_dst = [1, 2, n_stage - 2]
    far_dst = n_stage // 2
    n_relay = (n_micro - 2) // 2

    def dx0_copies(m):
        return [remote(dxbuf.at[m], dx0buf.at[m], d_send.at[k], d_recv.at[m], dev) for k, dev in enumerate(near_dst + [far_dst])]

    def relayed(m):
        return (m < 2 * n_relay) & (((me == 2) & (lax.rem(m, 2) == 0)) | ((me == n_stage - 2) & (lax.rem(m, 2) == 1)))

    def relay_far(m):
        return remote(dx0buf.at[m], dx0buf.at[m], r_sems.at[1], d_recv.at[m], far_dst)

    def bwd(m):
        with jax.named_scope("bwd_wait"):
            @pl.when(jnp.logical_not(last))
            def _():
                remote(gbuf.at[m], gbuf.at[m], b_send, b_recv.at[m], me).wait_recv()

            @pl.when(last)
            def _():
                @pl.when(m != last_id)
                def _():
                    remote(dnbuf.at[m], dnbuf.at[m], dn_ssem, dn_rsem.at[m], me).wait_recv()

                yf = ybuf[pl.ds(m * per, per)].reshape(seq, dim).astype(F32)
                inv = lax.rsqrt(jnp.mean(yf * yf, axis=-1, keepdims=True) + EPS)
                dnf = dnbuf[m].astype(F32)
                proj = jnp.mean(yf * dnf, axis=-1, keepdims=True)
                gbuf[m] = (dnf * inv - yf * (inv * inv * inv * proj)).astype(BF16)

        with jax.named_scope("bwd_comp"):
            g = gbuf[m]
            for j in range(n_fblk):
                cols = slice(j * fblk, (j + 1) * fblk)
                dh = dot(g, down_t[:, cols]).astype(BF16).astype(F32)
                abuf[m, :, cols] = (dh * gelu_slope(abuf[m, :, cols].astype(F32))).astype(BF16)
            dxbuf[m] = (g.astype(F32) + dot(abuf[m], up_t[...])).astype(BF16)

        @pl.when(jnp.logical_not(first))
        def _():
            remote(dxbuf.at[m], gbuf.at[m], b_send, b_recv.at[m], me - 1).start()

        @pl.when(first)
        def _():
            copies = dx0_copies(m)
            for c in copies[:-1]:
                c.start()
            pl.when(m >= 2 * n_relay)(copies[-1].start)

        pltpu.make_async_copy(abuf.at[m], da_out.at[m], out_sem.at[2]).start()
        pltpu.make_async_copy(gbuf.at[m], g_out.at[m], out_sem.at[3]).start()

    n_slot = obuf.shape[0]
    busy = chip == last_id // 2
    far_tile = remote(tmp_out.at[core, pl.ds(0, plan.rows)], tmp_out.at[core, pl.ds(0, plan.rows)], ic_send, od_recv, jnp.where(first, last_id, last_id - 1))
    sends_far = first | (me == last_id - 2)

    def tile_copy(k):
        rows = pl.ds(pl.multiple_of(k * plan.rows, plan.rows), plan.rows)
        slot = lax.rem(k, n_slot)
        return pltpu.make_async_copy(obuf.at[slot], tmp_out.at[core, rows], o_sem.at[slot])

    def piece(p):
        k = p // plan.per_tile
        rows = pl.ds(pl.multiple_of(p * plan.piece, plan.piece), plan.piece)
        here = pl.ds(pl.multiple_of(lax.rem(p, plan.per_tile) * plan.piece, plan.piece), plan.piece)
        return remote(obuf.at[lax.rem(k, n_slot), here], tmp_out.at[core, rows], od_send.at[k], od_recv, mate)

    def tile_sent(k):
        slot = lax.rem(k, n_slot)
        return remote(obuf.at[slot], tmp_out.at[core, pl.ds(0, plan.rows)], od_send.at[k], od_recv, mate)

    def emb_tile(k):
        with jax.named_scope("tile_prep"):

            @pl.when(k == 0)
            def _():
                for d in range(1, n_stage // 2):
                    src = lax.rem(mate + 2 * d, n_stage)
                    pl.when(jnp.logical_not(last))(remote(nbuf.at[src], nbuf.at[src], ag_send.at[0], ag_recv.at[src], me).wait_recv)
                for m in range(n_micro):
                    n_all_t[:, m * seq:(m + 1) * seq] = nbuf[m].T
                sa_all.wait_recv()
                for c in range(n_stage // 2):
                    shift[:, c * pair:(c + 1) * pair] = statall[2 * c, 0:1, :] * LOG2E + log_count

        slot = lax.rem(k, n_slot)
        with jax.named_scope("tile_wait"):
            @pl.when(k == 1)
            def _():
                tile_copy(0).wait()
                pl.when(sends_far)(far_tile.start)

            pl.when(k > n_slot)(lambda: tile_copy(k - n_slot).wait())
            pl.when((k >= n_slot) & (k - n_slot < plan.shared) & jnp.logical_not(busy & (k == n_slot)))(lambda: tile_sent(k - n_slot).wait_send())

        with jax.named_scope("tile"):
            rows = pl.ds(pl.multiple_of(k * plan.rows, plan.rows), plan.rows)
            logit_grad(emb[rows, :], n_all_t, shift, lab_ref, row0 + k * plan.rows, inv_count, scale, dz)
            obuf[slot] = dot(dz[...], nbuf[...].reshape(n_tok, dim)) * scale

        tile_copy(k).start()

    def send_pieces(done, until):
        lax.fori_loop(done, until, lambda p, c: (piece(p).start(), c)[1], 0)
        return jnp.maximum(done, until)

    before = sum(jnp.where(me == s, plan.before[s], 0) for s in range(n_stage))

    def pass_dx0(m, carry):
        @pl.when(jnp.logical_not(first))
        def _():
            remote(dx0buf.at[m], dx0buf.at[m], r_sems.at[0], d_recv.at[m], me).wait_recv()

            @pl.when(core == 0)
            def _():
                remote(dx0buf.at[m], dx0buf.at[m], r_sems.at[0], d_recv.at[m], mate).start()

            @pl.when(relayed(m))
            def _():
                relay_far(m).start()

            pltpu.make_async_copy(dx0buf.at[m], dx0_out.at[m], out_sem.at[4]).start()

        @pl.when(first)
        def _():
            pltpu.make_async_copy(dxbuf.at[m], dx0_out.at[m], out_sem.at[4]).start()

        return carry

    lead = jnp.where(me == 2, 40, jnp.where(me == n_stage - 2, -1437, jnp.where(me == far_dst, -1150, -10**6)))

    def work(i, carry):
        sent, passed = carry
        chunk = (i >= before) & (i < before + n_micro)
        pl.when(chunk)(lambda: bwd(i - before))
        k = jnp.where(i < before, i, i - n_micro)
        pl.when(jnp.logical_not(chunk))(lambda: emb_tile(k))
        after = i - before - n_micro + 1
        here = jnp.where(after > 0, jnp.clip((after * 257 + lead) // 146, 0, n_micro), 0)
        lax.fori_loop(passed, here, pass_dx0, 0)
        ready = jnp.where(i < before, i + 1, jnp.where(chunk, before, i + 1 - n_micro)) * plan.per_tile
        near_chunks = chunk | ((i < before) & (i + 1 >= before))
        until = jnp.minimum(jnp.minimum(ready, plan.shared * plan.per_tile), sent + jnp.where(near_chunks, 1, plan.per_tile + 1))
        return send_pieces(sent, until), jnp.maximum(passed, here)

    sent, passed = lax.fori_loop(0, plan.tiles + n_micro, work, (jnp.where(busy, plan.per_tile, 0), 0))
    outs = [pltpu.make_async_copy(nbuf, n_out, out_sem.at[5]), pltpu.make_async_copy(lossall, loss_out, out_sem.at[6]), pltpu.make_async_copy(meta, meta_out, out_sem.at[7])]
    lo_all.wait_recv()
    for c in outs:
        c.start()
    pltpu.make_async_copy(statall, stat_out, out_sem.at[8]).start()
    with jax.named_scope("relay_all"):
        lax.fori_loop(passed, n_micro, pass_dx0, 0)

    with jax.named_scope("drain"):
        send_pieces(sent, plan.shared * plan.per_tile)
        for k in range(max(plan.tiles - n_slot, 0), plan.tiles):
            tile_copy(k).wait()
            if k < plan.shared:
                tile_sent(k).wait_send()
        pl.when(sends_far)(far_tile.wait_send)
        all_rows = pl.ds(0, plan.shared * plan.rows)
        remote(tmp_out.at[1 - core, all_rows], tmp_out.at[1 - core, all_rows], od_send.at[0], od_recv, me).wait_recv()
        sa_all.wait_send()
        lo_all.wait_send()
        pltpu.make_async_copy(statall, stat_out, out_sem.at[8]).wait()
        for c, p in zip(ag_copies, peers):
            pl.when(p != last_id)(c.wait_send)

        @pl.when(jnp.logical_not(last))
        def _():
            dn_copy.wait_send()
            pl.when(mate != last_id)(n_forward.wait_send)
            remote(ybuf, xbuf, f_send, f_recv.at[0], me + 1).wait_send()

        @pl.when(last)
        def _():
            remote(nbuf, nbuf, n_send, n_recv.at[0], me).wait_send()

        @pl.when(mate != last_id)
        def _():
            some = nbuf.at[pl.ds(0, len(peers))]
            remote(some, some, fw_send, ag_recv.at[0], mate).wait_send()

        @pl.when(jnp.logical_not(first) & (me + 2 < n_micro))
        def _():
            x_copy(0).wait_send()

            @pl.when(me < 2)
            def _():
                x_copy(1).wait_send()

        @pl.when(jnp.logical_not(first))
        def _():
            remote(dxbuf, gbuf, b_send, b_recv.at[0], me).wait_send()
            pl.when(core == 0)(remote(dx0buf, dx0buf, r_sems.at[0], d_recv.at[0], mate).wait_send)

        @pl.when(first)
        def _():
            for k in range(len(near_dst)):
                remote(dxbuf, dx0buf, d_send.at[k], d_recv.at[0], me).wait_send()
            direct = pl.ds(0, n_micro - 2 * n_relay)
            remote(dxbuf.at[direct], dx0buf.at[direct], d_send.at[len(near_dst)], d_recv.at[0], me).wait_send()

        @pl.when((me == 2) | (me == n_stage - 2))
        def _():
            some = dx0buf.at[pl.ds(0, n_relay)]
            remote(some, some, r_sems.at[1], d_recv.at[0], me).wait_send()

        pltpu.make_async_copy(hbuf, hid_out, out_sem.at[0]).wait()
        pltpu.make_async_copy(xbuf, xs_out, out_sem.at[1]).wait()
        pltpu.make_async_copy(abuf, da_out, out_sem.at[2]).wait()
        pltpu.make_async_copy(gbuf, g_out, out_sem.at[3]).wait()
        pltpu.make_async_copy(dx0buf, dx0_out, out_sem.at[4]).wait()
        for c in outs:
            c.wait()


class Plan:
    def __init__(self, vocab, n_stage):
        units = vocab // LANES
        self.base = units // 2 * LANES
        self.extra = vocab - 2 * self.base
        self.head_tile = next(t for t in (1600, 1536, 1280, 1024, 768, 640, 512, 256, 128) if self.base % t == 0)
        self.rows = 1024
        self.tiles, self.shared = 10, 8
        self.grad_tile = next(t for t in (3200, 1600, 1280, 640, 256, 128) if self.base % t == 0)
        self.e_parts = next(k for k in (10, 8, 5, 4, 2, 1) if self.base % (16 * k) == 0)
        self.part = 128
        self.slots = 4
        self.piece = 256
        self.per_tile = self.rows // self.piece
        measured = [10, 9, 6, 5, 2, 2, 0, 0]
        self.before = (measured + [0] * n_stage)[:n_stage]
        mid = self.base + self.extra
        ends = [(0, mid), (mid, vocab)]
        early = (self.tiles * self.rows, self.shared * self.rows)
        self.spans = [[(ends[h][0] + early[0 if h == c else 1], ends[h][1]) for h in (c, 1 - c)] for c in range(2)]
        self.longest = [max(self.spans[c][k][1] - self.spans[c][k][0] for c in range(2)) for k in range(2)]
        best = min(range(16, 1281, 16), key=lambda r: (sum(-(-n // r) for n in self.longest)) * (r + 40))
        self.calc_rows = best
        self.calc_steps = [-(-n // best) for n in self.longest]
        self.steps = sum(self.calc_steps)
        self.copy_rows = self.rows
        self.copies = self.tiles + self.shared
        self.starts = ends

    def calc_start(self, core, s):
        k = 0 if s < self.calc_steps[0] else 1
        lo, hi = self.spans[core][k]
        return min(lo + (s - k * self.calc_steps[0]) * self.calc_rows, hi - self.calc_rows)

    def copy_start(self, core, c):
        own = c < self.tiles
        h = core if own else 1 - core
        return self.starts[h][0] + (c if own else c - self.tiles) * self.copy_rows

    def cuts(self, core):
        firsts = [(self.calc_start(core, s), self.calc_rows) for s in range(self.steps)] + [(self.copy_start(core, c), self.copy_rows) for c in range(self.copies)]
        flat = [v for lo, rows in firsts for v in (lo, lo + rows)]
        return flat + [0] * (LANES - len(flat))


def run_pipe(x0, emb, w_up, w_down, labels, tokens, cuts, n_stage, plan):
    n_micro, seq = labels.shape
    dim, ffn = w_up.shape
    n_tok = n_micro * seq
    base = plan.base
    any_spec = pl.BlockSpec(memory_space=pl.ANY)
    act = (n_micro, seq, dim)
    fine = (n_tok // plan.part, plan.part, dim)
    wide = (n_micro, seq, ffn)
    dma = pltpu.SemaphoreType.DMA
    vm = pltpu.VMEM
    pair = 2 * seq
    return pl.pallas_call(
        functools.partial(pipe_kernel, n_stage, plan),
        out_shape=[
            jax.ShapeDtypeStruct(act, BF16), jax.ShapeDtypeStruct(fine, BF16), jax.ShapeDtypeStruct(wide, BF16),
            jax.ShapeDtypeStruct(wide, BF16), jax.ShapeDtypeStruct(act, BF16), jax.ShapeDtypeStruct(act, BF16),
            jax.ShapeDtypeStruct((n_stage, 8, pair), F32), jax.ShapeDtypeStruct((n_stage, 8, pair), F32), jax.ShapeDtypeStruct((2, plan.tiles * plan.rows, dim), F32),
            jax.ShapeDtypeStruct((3 * n_tok // LANES, LANES), jnp.int32),
        ],
        in_specs=[any_spec] * 4 + [pl.BlockSpec(memory_space=pltpu.VMEM)] * 3,
        out_specs=[any_spec] * 10,
        scratch_shapes=[
            vm(fine, BF16), vm(fine, BF16), vm(wide, BF16), vm(wide, BF16), vm(act, BF16), vm(act, BF16), vm(act, BF16), vm(act, BF16), vm(act, BF16),
            vm((dim, ffn), BF16), vm((ffn, dim), BF16), vm((ffn, dim), BF16), vm((dim, ffn), BF16),
            vm((base + plan.extra, dim), BF16), vm((base + plan.extra, pair), BF16), vm((dim, pair), BF16), vm((pair, dim), F32),
            vm((seq, dim), F32), vm((seq, dim), F32), vm((seq, dim), BF16), vm((16, pair), F32), vm((16, pair), F32), vm((n_stage, 8, pair), F32), vm((n_stage, 8, pair), F32),
            vm((2, 8, pair), F32), vm((dim, n_tok), BF16), vm((1, n_tok), F32), vm((plan.rows, n_tok), BF16), vm((plan.slots, plan.rows, dim), F32),
            vm((2, plan.head_tile, pair), BF16), vm((3 * n_tok // LANES, LANES), jnp.int32),
            dma((2,)), dma((2,)), dma((2,)), dma((2,)), dma((n_micro,)), dma, dma((n_tok // plan.part,)), dma, dma((n_micro,)), dma,
            dma((n_stage // 2,)), dma((n_micro,)), dma,
            dma((2,)), dma((2,)), dma, dma((n_stage,)), dma((2,)), dma((2,)), dma, dma((n_micro,)), dma((4,)), dma((n_micro,)), dma((2,)), dma((9,)),
            dma((plan.slots,)), dma((plan.shared,)), dma, dma,
        ],
        compiler_params=pltpu.CompilerParams(collective_id=0, has_side_effects=True, vmem_limit_bytes=67_000_000),
        cost_estimate=pl.CostEstimate(flops=60 * 10**9, bytes_accessed=100 * 10**6, transcendentals=0),
        name="pipe",
    )(x0.reshape(x0.shape[0], seq // plan.part, plan.part, dim), emb, w_up, w_down, labels.reshape(1, n_tok), tokens.reshape(1, n_tok), cuts)


def fin_kernel(n_stage, n_tok, plan, ids_ref, emb_hbm, tmp_hbm, n_hbm, stat_ref, part_ref, lab_ref, meta_ref, dx0_hbm, xs_hbm, hid_hbm, da_hbm, g_hbm,
               out_hbm, loss_ref, gup_hbm, gdown_hbm,
               n_all, dx0, xs, hid, da, g, n_t, x_t, dx0s, dz, shift, e_in, c_out, cp, gup, gdown,
               ld_sem, e_sem, t_sem, co_sem, po_sem, gu_sem, gd_sem, wi_sem):
    dim, ffn = gup_hbm.shape
    scale = dim ** -0.5
    inv_count = 1.0 / n_tok
    steps, crows, prows = plan.steps, plan.calc_rows, plan.copy_rows
    core = lax.rem(lax.axis_index("stage"), 2)
    early = plan.tiles * prows
    wblk = gup.shape[2]
    n_wblk = ffn // wblk
    turn = plan.calc_steps[0]

    def pick(pair):
        return jnp.where(core == 0, pair[0], pair[1])

    def calc_start(s):
        own = s < turn
        lo, hi = [jnp.where(own, pick([plan.spans[c][0][e] for c in range(2)]), pick([plan.spans[c][1][e] for c in range(2)])) for e in range(2)]
        return pl.multiple_of(jnp.minimum(lo + (s - jnp.where(own, 0, turn)) * crows, hi - crows), 16)

    def copy_start(c):
        own = c < plan.tiles
        first = jnp.where(own, pick([plan.starts[0][0], plan.starts[1][0]]), pick([plan.starts[1][0], plan.starts[0][0]]))
        return pl.multiple_of(first + (c - jnp.where(own, 0, plan.tiles)) * prows, 16)

    def e_copy(s):
        return pltpu.make_async_copy(emb_hbm.at[pl.ds(calc_start(s), crows)], e_in.at[lax.rem(s, 2)], e_sem.at[lax.rem(s, 2)])

    n_slot = cp.shape[0]
    ahead = 3

    def t_copy(c):
        own = c < plan.tiles
        row = jnp.where(own, core, 1 - core) * early + (c - jnp.where(own, 0, plan.tiles)) * prows
        slot = lax.rem(c, n_slot)
        return pltpu.make_async_copy(tmp_hbm.at[pl.ds(pl.multiple_of(row, 16), prows)], cp.at[slot], t_sem.at[slot])

    def p_out(c):
        slot = lax.rem(c, n_slot)
        return pltpu.make_async_copy(cp.at[slot], out_hbm.at[pl.ds(copy_start(c), prows)], po_sem.at[slot])

    def c_outs(s):
        slot = lax.rem(s, 2)
        return pltpu.make_async_copy(c_out.at[slot], out_hbm.at[pl.ds(calc_start(s), crows)], co_sem.at[slot])

    loads = [pltpu.make_async_copy(s, d, ld_sem.at[i]) for i, (s, d) in enumerate(((n_hbm, n_all), (dx0_hbm, dx0), (xs_hbm, xs), (g_hbm, g)))]
    loads[0].start()
    loads[1].start()
    e_copy(0).start()
    for c in range(ahead):
        t_copy(c).start(priority=1)
    pair = stat_ref.shape[2]
    loss = jnp.zeros((1, pair), F32)
    for d in range(n_stage):
        if d % 2 == 0:
            shift[:, (d // 2) * pair:(d // 2 + 1) * pair] = stat_ref[d, 0:1, :] * LOG2E + math.log2(n_tok)
        loss = loss + part_ref[d, 0:1, :]
    loss_ref[0] = jnp.sum(loss) * inv_count
    with jax.named_scope("fin_pre"):
        loads[0].wait()
        n_t[...] = n_all[...].T

    def sum_rows():
        loads[1].wait()
        dense = jnp.concatenate([meta_ref[g:g + 1, :] for g in range(n_tok // LANES)], axis=1)
        order = lax.broadcasted_iota(jnp.int32, (n_tok, n_tok), 0) == dense
        dx0s[...] = dot(jnp.where(order, 1.0, 0.0).astype(BF16), dx0[...])

    def add_rows(k, start, ref):
        lo, hi = ids_ref[2 * n_tok + k], ids_ref[2 * n_tok + k + 1]
        wide = 8

        def some(p, width):
            at = [pl.ds(ids_ref[n_tok + p + u] - start, 1) for u in range(width)]
            new = [ref[at[u], :] + dx0s[pl.ds(p + u, 1), :] for u in range(width)]
            for u in range(width):
                ref[at[u], :] = new[u]

        def group(g, carry):
            some(lo + g * wide, wide)
            return carry

        def single(p, carry):
            some(p, 1)
            return carry

        n_grp = (hi - lo) // wide
        lax.fori_loop(0, n_grp, group, 0)
        lax.fori_loop(lo + n_grp * wide, hi, single, 0)

    def w_ins(w):
        cols = pl.ds(pl.multiple_of(w * wblk, wblk), wblk)
        wslot = lax.rem(w, 2)
        return (pltpu.make_async_copy(da_hbm.at[:, cols], da.at[wslot], wi_sem.at[0, wslot]), pltpu.make_async_copy(hid_hbm.at[:, cols], hid.at[wslot], wi_sem.at[1, wslot]))

    def w_outs(w):
        cols = pl.ds(pl.multiple_of(w * wblk, wblk), wblk)
        wslot = lax.rem(w, 2)
        return (pltpu.make_async_copy(gup.at[wslot], gup_hbm.at[:, cols], gu_sem.at[wslot]), pltpu.make_async_copy(gdown.at[wslot], gdown_hbm.at[cols], gd_sem.at[wslot]))

    def copy_tile(c, carry):
        with jax.named_scope("copy_wait"):
            t_copy(c).wait()
        with jax.named_scope("add_p"):
            add_rows(2 * steps + 2 * c, copy_start(c), cp.at[lax.rem(c, n_slot)])
        p_out(c).start()

        @pl.when(c + ahead < plan.copies)
        def _():
            pl.when(c + ahead >= n_slot)(lambda: p_out(c + ahead - n_slot).wait())
            t_copy(c + ahead).start(priority=1)

        return carry

    w_first = 2
    tails = [turn - 1, steps - 1]

    def tail(s):
        return (s == tails[0]) | (s == tails[1])

    def step(s, carry):
        pl.when(s + 1 < steps)(lambda: e_copy(s + 1).start())
        with jax.named_scope("fin_wait"):
            e_copy(s).wait()

        @pl.when(s == 0)
        def _():
            for c in loads[2:]:
                c.start()

        w = s - w_first

        @pl.when((w + 1 >= 0) & (w + 1 < n_wblk))
        def _():
            for c in w_ins(w + 1):
                c.start()

        pl.when((s >= 2) & jnp.logical_not(tail(s - 1)))(lambda: c_outs(s - 2).wait())
        slot = lax.rem(s, 2)
        start = calc_start(s)
        with jax.named_scope("calc"):
            logit_grad(e_in[slot], n_t, shift, lab_ref, start, inv_count, scale, dz)
            c_out[slot] = dot(dz[...], n_all[...]) * scale
        pl.when(s == 0)(sum_rows)
        with jax.named_scope("add_c"):
            add_rows(2 * s, start, c_out.at[slot])
        pl.when(tail(s))(lambda: c_outs(s - 1).wait())
        c_outs(s).start()
        lax.fori_loop(s * plan.copies // (steps - 1), jnp.minimum((s + 1) * plan.copies // (steps - 1), plan.copies), copy_tile, 0)

        @pl.when(w == 0)
        def _():
            for c in loads[2:]:
                c.wait()
            x_t[...] = xs[...].T

        @pl.when((w >= 0) & (w < n_wblk))
        def _():
            wslot = lax.rem(w, 2)
            with jax.named_scope("dw_wait"):
                for c in w_ins(w):
                    c.wait()

                @pl.when(w >= 2)
                def _():
                    for c in w_outs(w - 2):
                        c.wait()

            with jax.named_scope("dw"):
                gup[wslot] = dot(x_t[...], da[wslot])
                gdown[wslot] = dot_t(hid[wslot], g[...])
            for c in w_outs(w):
                c.start()

        return carry

    lax.fori_loop(0, steps, step, 0)
    with jax.named_scope("fin_drain"):
        for w in range(n_wblk - 2, n_wblk):
            for c in w_outs(w):
                c.wait()
        c_outs(steps - 1).wait()
        for c in range(plan.copies - n_slot, plan.copies):
            p_out(c).wait()


def run_fin(emb, tmp, n_all, stats, losses, labels, meta, dx0, xs, hid, da, g, n_stage, plan):
    vocab, dim = emb.shape
    n_tok, ffn = hid.shape
    vm = pltpu.VMEM
    dma = pltpu.SemaphoreType.DMA
    any_spec = pl.BlockSpec(memory_space=pl.ANY)
    vspec = pl.BlockSpec(memory_space=pltpu.VMEM)
    smem = pl.BlockSpec(memory_space=pltpu.SMEM)
    wblk = 512
    return pl.pallas_call(
        functools.partial(fin_kernel, n_stage, n_tok, plan),
        out_shape=[jax.ShapeDtypeStruct((vocab, dim), F32), jax.ShapeDtypeStruct((1,), F32), jax.ShapeDtypeStruct((dim, ffn), F32), jax.ShapeDtypeStruct((ffn, dim), F32)],
        in_specs=[smem, any_spec, any_spec, any_spec, vspec, vspec, vspec, vspec] + [any_spec] * 5,
        out_specs=[any_spec, smem, any_spec, any_spec],
        scratch_shapes=[
            vm((n_tok, dim), BF16), vm((n_tok, dim), BF16), vm((n_tok, dim), BF16), vm((2, n_tok, wblk), BF16), vm((2, n_tok, wblk), BF16), vm((n_tok, dim), BF16),
            vm((dim, n_tok), BF16), vm((dim, n_tok), BF16), vm((n_tok, dim), F32), vm((plan.calc_rows, n_tok), BF16), vm((1, n_tok), F32),
            vm((2, plan.calc_rows, dim), BF16), vm((2, plan.calc_rows, dim), F32), vm((5, plan.copy_rows, dim), F32),
            vm((2, dim, wblk), F32), vm((2, wblk, dim), F32),
            dma((4,)), dma((2,)), dma((5,)), dma((2,)), dma((5,)), dma((2,)), dma((2,)), dma((2, 2)),
        ],
        compiler_params=pltpu.CompilerParams(vmem_limit_bytes=67_000_000),
        cost_estimate=pl.CostEstimate(flops=2 * n_tok * vocab * dim, bytes_accessed=5 * vocab * dim, transcendentals=0),
        name="fin",
    )(meta.reshape(-1), emb, tmp, n_all, stats, losses, labels.reshape(1, n_tok), meta, dx0, xs, hid, da, g)


def solution(mesh):
    n_stage = mesh.shape["stage"]

    def device_fn(tokens, labels, emb, w_up, w_down):
        n_micro, seq = tokens.shape
        vocab, dim = emb.shape
        w_up, w_down = w_up[0], w_down[0]
        n_tok = n_micro * seq
        plan = Plan(vocab, n_stage)
        cuts = jnp.array([plan.cuts(0), plan.cuts(1)], jnp.int32)
        x0 = run_gather(tokens, emb)
        n_all, xs, hid, da, g, dx0, stats, losses, tmp, meta = run_pipe(x0, emb, w_up, w_down, labels, tokens, cuts, n_stage, plan)
        flat = lambda p: p.reshape(n_tok, -1)
        grad_emb, loss, grad_up, grad_down = run_fin(
            emb, tmp.reshape(-1, dim), flat(n_all), stats, losses, labels, meta, flat(dx0), flat(xs), flat(hid), flat(da), flat(g), n_stage, plan
        )
        return loss, grad_up[None], grad_down[None], grad_emb

    return jax.shard_map(device_fn, mesh=mesh, in_specs=(P("dp", None), P("dp", None), P(None, None), P("stage", None, None), P("stage", None, None)), out_specs=(P("dp"), P(("dp", "stage"), None, None), P(("dp", "stage"), None, None), P("dp", None)), check_vma=False)
```

```python
import functools
import math

import jax
import jax.numpy as jnp
from jax import lax
from jax.experimental import pallas as pl
from jax.experimental.pallas import tpu as pltpu
from jax.sharding import PartitionSpec as P


MESH = pl.DeviceIdType.MESH
LOG2E = math.log2(math.e)
LN2 = math.log(2.0)
GELU_C = math.sqrt(2.0 / math.pi)
GELU_K = 0.044715
EPS = 1e-6
LANES = 128
F32 = jnp.float32
BF16 = jnp.bfloat16


def gelu_fwd(a):
    return (0.5 * a) * (1.0 + jnp.tanh(a * (GELU_C + (GELU_C * GELU_K) * (a * a))))


def gelu_slope(a):
    a2 = a * a
    half = 0.5 * jnp.tanh(a * (GELU_C + (GELU_C * GELU_K) * a2))
    up, down = 0.5 + half, 0.5 - half
    return up + (up * down) * (a * (2.0 * GELU_C + (6.0 * GELU_C * GELU_K) * a2))


def dot(x, y):
    return jnp.dot(x, y, preferred_element_type=F32)


def dot_t(x, y):
    return lax.dot_general(x, y, (((0,), (0,)), ((), ())), preferred_element_type=F32)


def remote(src, dst, send_sem, recv_sem, dev):
    return pltpu.make_async_remote_copy(src_ref=src, dst_ref=dst, send_sem=send_sem, recv_sem=recv_sem, device_id={"stage": dev}, device_id_type=MESH)


def column(row):
    return jnp.broadcast_to(row, (LANES, LANES)).T


def gather_kernel(ids_ref, tok_ref, emb_hbm, x0_hbm, tiles, picked, sem, out_sem):
    n_micro, seq = tok_ref.shape
    me = lax.axis_index("stage")
    group = tiles.shape[1] // seq
    slots = tiles.shape[0]
    owners = [head_chunk(me, k, n_micro) for k in range(slots)]

    def fetch(k):
        def one(i, carry):
            t = ids_ref[owners[k] * seq + i]
            start = pl.multiple_of(t // group * group, group)
            pltpu.make_async_copy(emb_hbm.at[pl.ds(start, group)], tiles.at[k, pl.ds(pl.multiple_of(i * group, group), group)], sem.at[k]).start()
            return carry

        lax.fori_loop(0, seq, one, 0, unroll=8)

    def select(k):
        sub = lax.broadcasted_iota(jnp.int32, (LANES, LANES), 0)
        lane = lax.broadcasted_iota(jnp.int32, (LANES, LANES), 1)
        tok = column(tok_ref[pl.ds(owners[k], 1), :].astype(F32)).astype(jnp.int32)
        want = sub * group + (tok - tok // group * group)
        hot = jnp.concatenate([jnp.where(lane + b * LANES == want, 1.0, 0.0).astype(BF16) for b in range(seq * group // LANES)], axis=1)
        pltpu.make_async_copy(emb_hbm.at[pl.ds(0, seq * group)], tiles.at[k], sem.at[k]).wait()
        picked[k] = dot(hot, tiles[k]).astype(BF16)
        pltpu.make_async_copy(picked.at[k], x0_hbm.at[k], out_sem.at[k]).start()

    def finish(k):
        pltpu.make_async_copy(picked.at[k], x0_hbm.at[k], out_sem.at[k]).wait()

    for work in (fetch, select, finish):
        work(0)
        for k in range(1, slots):
            pl.when(me < slots)(functools.partial(work, k))


def head_chunk(dev, k, n_micro):
    return jnp.minimum(jnp.where(dev < 2, 2 * dev + k, dev + 2), n_micro - 1)


def run_gather(tokens, emb):
    n_micro, seq = tokens.shape
    dim = emb.shape[1]
    group = 16
    return pl.pallas_call(
        gather_kernel,
        out_shape=jax.ShapeDtypeStruct((2, seq, dim), BF16),
        in_specs=[pl.BlockSpec(memory_space=pltpu.SMEM), pl.BlockSpec(memory_space=pltpu.VMEM), pl.BlockSpec(memory_space=pl.ANY)],
        out_specs=pl.BlockSpec(memory_space=pl.ANY),
        scratch_shapes=[pltpu.VMEM((2, seq * group, dim), BF16), pltpu.VMEM((2, seq, dim), BF16), pltpu.SemaphoreType.DMA((2,)), pltpu.SemaphoreType.DMA((2,))],
        cost_estimate=pl.CostEstimate(flops=10**9, bytes_accessed=2 * seq * group * dim * 2, transcendentals=0),
        name="gather",
    )(tokens.reshape(n_micro * seq), tokens, emb)


def token_table(row_ref, cut_ref, meta):
    n_tok = row_ref.shape[1]
    n_grp = n_tok // LANES
    lane = lax.broadcasted_iota(jnp.int32, (LANES, LANES), 1).astype(F32)
    sub = lax.broadcasted_iota(jnp.int32, (LANES, LANES), 0)
    row = lambda g: row_ref[:, g * LANES:(g + 1) * LANES].astype(F32)
    zero = jnp.zeros((LANES, LANES), F32)
    fold = lambda acc: jnp.sum(acc, axis=0, keepdims=True)
    cols = [column(row(c)) for c in range(n_grp)]
    firsts = []
    for g in range(n_grp):
        acc = zero
        for c in range(g + 1):
            same = cols[c] == row(g)
            if c == g:
                same = same & (sub < lane.astype(jnp.int32))
            acc = acc + jnp.where(same, 1.0, 0.0)
        firsts.append(column(jnp.where(fold(acc) == 0.0, 1.0, 0.0)))
    ranks = []
    for g in range(n_grp):
        acc = zero
        for c in range(n_grp):
            acc = acc + jnp.where(cols[c] < row(g), firsts[c], 0.0)
        ranks.append(fold(acc))
        meta[g:g + 1, :] = ranks[g].astype(jnp.int32)
    rank_cols = [column(r) for r in ranks]
    for g in range(n_grp):
        acc = zero
        for c in range(n_grp):
            acc = acc + jnp.where(rank_cols[c] == lane + g * LANES, firsts[c] * cols[c], 0.0)
        meta[n_grp + g:n_grp + g + 1, :] = fold(acc).astype(jnp.int32)
    cut = cut_ref[...].astype(F32)
    acc = zero
    for c in range(n_grp):
        acc = acc + jnp.where(cols[c] < cut, firsts[c], 0.0)
    meta[2 * n_grp:3 * n_grp, :] = jnp.broadcast_to(fold(acc), (n_grp, LANES)).astype(jnp.int32)


def logit_grad(e, n_t, shift, lab, first_id, inv_count, scale, dz):
    rows = e.shape[0]
    n_tok = n_t.shape[1]
    blk = 256
    vid = lax.broadcasted_iota(jnp.int32, (rows, blk), 0)
    for j in range(n_tok // blk):
        cols = slice(j * blk, (j + 1) * blk)
        z = (dot(e, n_t[:, cols]) * scale).astype(BF16).astype(F32)
        prob = jnp.exp2(z * LOG2E - shift[:, cols])
        dz[:, cols] = jnp.where(vid == lab[:, cols] - first_id, prob - inv_count, prob).astype(BF16)


def pipe_kernel(n_stage, plan, x0_hbm, emb_hbm, up_hbm, down_hbm, lab_ref, row_ref, cut_ref,
                n_out, xs_out, hid_out, da_out, g_out, dx0_out, stat_out, loss_out, tmp_out, meta_out,
                xbuf, ybuf, abuf, hbuf, nbuf, gbuf, dxbuf, dx0buf, dnbuf, up, down, up_t, down_t,
                emb, zbuf, n_t, dn_acc, dn_send, dn_recv, dn_own, st_send, st_recv, statall, lossall, tops, n_all_t, shift, dz, obuf, z_pair, meta,
                w_sem, e_sem, x_sem, x_send, x_recv, f_send, f_recv, n_send, n_recv, nf_send, ag_send, ag_recv, fw_send,
                st_sems, dp_sems, dn_ssem, dn_rsem, sa_sems, lo_sems, b_send, b_recv, d_send, d_recv, r_sems, out_sem, o_sem, od_send, od_recv, ic_send):
    n_micro, seq, dim = gbuf.shape
    part = xbuf.shape[1]
    n_part = xbuf.shape[0]
    per = seq // part
    n_tok = n_micro * seq
    ffn = up.shape[1]
    vocab = emb_hbm.shape[0]
    me = lax.axis_index("stage")
    core = lax.rem(me, 2)
    chip = me // 2
    mate = me + 1 - 2 * core
    last_id = n_stage - 1
    first = me == 0
    last = me == last_id
    fblk = 512
    n_fblk = ffn // fblk
    base, extra, tile = plan.base, plan.extra, plan.head_tile
    row0 = core * (base + extra)
    n_tiles = base // tile
    wide_tile = plan.grad_tile

    barrier = pltpu.get_barrier_semaphore()
    for d in range(1, n_stage):
        pl.semaphore_signal(barrier, inc=1, device_id={"stage": lax.rem(me + d, n_stage)}, device_id_type=MESH)
    w_copy = [pltpu.make_async_copy(up_hbm, up, w_sem.at[0]), pltpu.make_async_copy(down_hbm, down, w_sem.at[1])]
    for c in w_copy:
        c.start()
    x_slots = x0_hbm.shape[0]
    x_mine = [head_chunk(me, k, n_micro) for k in range(x_slots)]

    def x_rows(m):
        return xbuf.at[pl.ds(m * per, per)]

    def x_local(k):
        return pltpu.make_async_copy(x0_hbm.at[k], x_rows(k), x_sem.at[k])

    @pl.when(first)
    def _():
        for k in range(x_slots):
            x_local(k).start()

    e_parts = plan.e_parts
    e_step = base // e_parts

    def e_copy(i):
        src = emb_hbm.at[pl.ds(pl.multiple_of(row0 + i * e_step, 16), e_step)]
        return pltpu.make_async_copy(src, emb.at[pl.ds(i * e_step, e_step)], e_sem.at[0])

    e_more = pltpu.make_async_copy(emb_hbm.at[pl.ds(base, extra)], emb.at[pl.ds(base, extra)], e_sem.at[1])
    with jax.named_scope("entry"):
        pl.semaphore_wait(barrier, n_stage - 1)

    def x_copy(k):
        return remote(x0_hbm.at[k], x_rows(x_mine[k]), x_send.at[k], x_recv.at[x_mine[k]], 0)

    @pl.when(jnp.logical_not(first) & (me + 2 < n_micro))
    def _():
        x_copy(0).start()

        @pl.when(me < 2)
        def _():
            x_copy(1).start()

    with jax.named_scope("w_wait"):
        for c in w_copy:
            c.wait()
        for i in range(e_parts):
            e_copy(i).start()
        pl.when(core == 0)(e_more.start)

    def transpose_weights():
        for j in range(n_fblk):
            up_t[j * fblk:(j + 1) * fblk, :] = up[:, j * fblk:(j + 1) * fblk].T
            down_t[:, j * fblk:(j + 1) * fblk] = down[j * fblk:(j + 1) * fblk, :].T

    def idle_work():
        transpose_weights()
        token_table(row_ref, jnp.where(core == 0, cut_ref[0:1, :], cut_ref[1:2, :]), meta)

    @pl.when(chip >= n_stage // 4)
    def _():
        idle_work()

    def n_copy(m):
        return remote(nbuf.at[m], nbuf.at[m], n_send, n_recv.at[m], jnp.where(m == last_id, last_id - 1, m))

    def y_copy(h):
        return remote(ybuf.at[h], xbuf.at[h], f_send, f_recv.at[h], me + 1)

    def fwd(h, carry):
        m = h // per
        sub = lax.rem(h, per)
        rows = pl.ds(pl.multiple_of(sub * part, part), part)
        with jax.named_scope("fwd_wait"):

            @pl.when(first & (sub == 0))
            def _():
                @pl.when(m < x_slots)
                def _():
                    x_local(m).wait()

                @pl.when(m >= x_slots)
                def _():
                    remote(x_rows(m), x_rows(m), x_send.at[0], x_recv.at[m], me).wait_recv()

            @pl.when(jnp.logical_not(first))
            def _():
                remote(xbuf.at[h], xbuf.at[h], f_send, f_recv.at[h], me).wait_recv()

        with jax.named_scope("fwd_comp"):
            x = xbuf[h]
            for j in range(n_fblk):
                cols = slice(j * fblk, (j + 1) * fblk)
                a = dot(x, up[:, cols]).astype(BF16)
                abuf[m, rows, cols] = a
                hbuf[m, rows, cols] = gelu_fwd(a.astype(F32)).astype(BF16)
            y = (x.astype(F32) + dot(hbuf[m, rows, :], down[...])).astype(BF16)
            ybuf[h] = y

        @pl.when(jnp.logical_not(last))
        def _():
            y_copy(h).start()

        @pl.when(last)
        def _():
            yf = y.astype(F32)
            inv = lax.rsqrt(jnp.mean(yf * yf, axis=-1, keepdims=True) + EPS)
            nbuf[m, rows, :] = (yf * inv).astype(BF16)
            pl.when(sub == per - 1)(n_copy(m).start)

        @pl.when(sub == per - 1)
        def _():
            pltpu.make_async_copy(hbuf.at[m], hid_out.at[m], out_sem.at[0]).start()
            pltpu.make_async_copy(x_rows(m), xs_out.at[pl.ds(m * per, per)], out_sem.at[1]).start()

        return carry

    lax.fori_loop(0, n_part, fwd, 0)

    @pl.when(chip < n_stage // 4)
    def _():
        idle_work()

    n_forward = remote(nbuf.at[me], nbuf.at[me], nf_send, n_recv.at[me], mate)
    with jax.named_scope("n_wait"):

        @pl.when(jnp.logical_not(last))
        def _():
            remote(nbuf.at[me], nbuf.at[me], n_send, n_recv.at[me], me).wait_recv()
            pl.when(mate != last_id)(n_forward.start)
            remote(nbuf.at[mate], nbuf.at[mate], n_send, n_recv.at[mate], me).wait_recv()

        for k in range(2):
            n_t[:, k * seq:(k + 1) * seq] = nbuf[2 * chip + k].T

    peers = [lax.rem(me + 2 * d, n_stage) for d in range(1, n_stage // 2)]
    ag_copies = [remote(nbuf.at[me], nbuf.at[me], ag_send.at[d], ag_recv.at[me], p) for d, p in enumerate(peers)]
    for c, p in zip(ag_copies, peers):
        pl.when(p != last_id)(c.start)
    with jax.named_scope("e_wait"):
        pltpu.make_async_copy(emb_hbm.at[pl.ds(0, base)], emb.at[pl.ds(0, base)], e_sem.at[0]).wait()
        pl.when(core == 0)(e_more.wait)

    pair = 2 * seq
    scale = dim ** -0.5
    inv_count = 1.0 / n_tok
    log_count = math.log2(n_tok)
    lab = lab_ref[:, pl.ds(pl.multiple_of(chip * pair, pair), pair)]

    def logits(rows, size):
        e = emb[rows, :]
        parts = [dot(e[k * size // 2:(k + 1) * size // 2], n_t[...]) for k in range(2)]
        z = jnp.concatenate([(p * scale).astype(BF16) for p in parts], axis=0)
        zbuf[rows, :] = z
        return z

    def peak(z, size, top):
        best = jnp.max(z.reshape(size // 16, 16, pair), axis=0).astype(F32)
        return jnp.maximum(top, jnp.maximum(best[:8], best[8:]))

    def total(z, size, old, top, tot):
        off = top * LOG2E
        return tot * jnp.exp2(old * LOG2E - off) + jnp.sum(jnp.exp2(z.astype(F32).reshape(size // 8, 8, pair) * LOG2E - off[None]), axis=0)

    tops[0] = jnp.full((8, pair), -jnp.inf, F32)
    tops[1] = jnp.zeros((8, pair), F32)

    @pl.when(core == 0)
    def _():
        z = logits(pl.ds(base, extra), extra)
        top = peak(z, extra, tops[0])
        tops[1] = total(z, extra, tops[0], top, tops[1])
        tops[0] = top

    def logits_step(i, slot, old, top, tot):
        z = logits(pl.ds(pl.multiple_of(i * tile, 16), tile), tile)
        tot = total(z_pair[1 - slot], tile, old, top, tot)
        z_pair[slot] = z
        return top, peak(z, tile, top), tot

    with jax.named_scope("logits"):
        z = logits(pl.ds(0, tile), tile)
        z_pair[0] = z
        state = (tops[0], peak(z, tile, tops[0]), tops[1])
        state = lax.fori_loop(0, (n_tiles - 1) // 2, lambda i, c: logits_step(2 * i + 2, 0, *logits_step(2 * i + 1, 1, *c)), state)
        if n_tiles % 2 == 0:
            state = logits_step(n_tiles - 1, 1, *state)
        old, top, tot = state
        tot = total(z_pair[(n_tiles - 1) % 2], tile, old, top, tot)
    row_top = jnp.max(top, axis=0, keepdims=True)
    row_tot = jnp.sum(tot * jnp.exp2((top - row_top) * LOG2E), axis=0, keepdims=True)
    st_send[0:8, :] = jnp.broadcast_to(row_top, (8, pair))
    st_send[8:16, :] = jnp.broadcast_to(row_tot, (8, pair))
    st_copy = remote(st_send, st_recv, st_sems.at[0], st_sems.at[1], mate)
    with jax.named_scope("stat_x"):
        st_copy.start()
        st_copy.wait()
    far_top = st_recv[0:1, :]
    far_tot = st_recv[8:9, :]
    all_top = jnp.maximum(row_top, far_top)
    mine = row_tot * jnp.exp(row_top - all_top)
    other = far_tot * jnp.exp(far_top - all_top)
    lse = all_top + jnp.log(jnp.where(core == 0, mine + other, other + mine))
    my_shift = lse * LOG2E + log_count
    others = [lax.rem(me + d, n_stage) for d in range(1, n_stage)]

    def spread(buf, sems):
        whole = buf.at[pl.ds(0, n_stage - 1)]
        return [remote(buf.at[me], buf.at[me], sems.at[0], sems.at[1], p) for p in others], remote(whole, whole, sems.at[0], sems.at[1], me)

    statall[me] = jnp.broadcast_to(lse, (8, pair))
    sa_copies, sa_all = spread(statall, sa_sems)
    for c in sa_copies:
        c.start()

    def grads(rows, size, first_row, picked):
        zf = zbuf[rows, :].astype(F32)
        prob = jnp.exp2(zf * LOG2E - my_shift)
        hit = lax.broadcasted_iota(jnp.int32, (size, pair), 0) == lab - (row0 + first_row)
        dz_t = jnp.where(hit, prob - inv_count, prob).astype(BF16)
        got = jnp.where(hit, zf, 0.0).reshape(size // 8, 8, pair)
        return dot_t(dz_t, emb[rows, :]), picked + jnp.sum(got, axis=0)

    tops[0] = jnp.zeros((8, pair), F32)
    dn_acc[...] = jnp.zeros_like(dn_acc)

    @pl.when(core == 0)
    def _():
        dn_acc[...], tops[0] = grads(pl.ds(base, extra), extra, base, tops[0])

    def grad_step(i, picked):
        part, picked = grads(pl.ds(pl.multiple_of(i * wide_tile, 16), wide_tile), wide_tile, i * wide_tile, picked)
        dn_acc[...] += part
        return picked

    with jax.named_scope("grads"):
        picked = lax.fori_loop(0, base // wide_tile, grad_step, tops[0])
    far = pl.ds(pl.multiple_of((1 - core) * seq, seq), seq)
    near = pl.ds(pl.multiple_of(core * seq, seq), seq)
    dn_send[...] = dn_acc[far, :]
    dp_copy = remote(dn_send, dn_recv, dp_sems.at[0], dp_sems.at[1], mate)
    dp_copy.start()
    row_loss = jnp.where(core == 0, lse, 0.0) - jnp.sum(picked, axis=0, keepdims=True)
    lossall[me] = jnp.broadcast_to(row_loss, (8, pair))
    lo_copies, lo_all = spread(lossall, lo_sems)
    for c in lo_copies:
        c.start()
    with jax.named_scope("dn_x"):
        dp_copy.wait()
        dn = ((dn_acc[near, :] + dn_recv[...]) * scale).astype(BF16)
    dn_copy = remote(dn_own, dnbuf.at[me], dn_ssem, dn_rsem.at[me], last_id)

    @pl.when(last)
    def _():
        dnbuf[last_id] = dn

    @pl.when(jnp.logical_not(last))
    def _():
        dn_own[...] = dn
        dn_copy.start()

    with jax.named_scope("ag_wait"):
        for p in peers:
            got = remote(nbuf.at[p], nbuf.at[p], ag_send.at[0], ag_recv.at[p], me)
            pl.when(jnp.logical_not(last))(got.wait_recv)
            pl.when(mate != last_id)(remote(nbuf.at[p], nbuf.at[p], fw_send, ag_recv.at[p], mate).start)

    near_dst = [1, 2, n_stage - 2]
    far_dst = n_stage // 2
    direct = n_micro - 1
    by_next = [m for m in range(direct) if m % 2 == 0 or m >= n_micro - 3]
    by_prev = [m for m in range(direct) if m not in by_next]

    def dx0_copies(m):
        return [remote(dxbuf.at[m], dx0buf.at[m], d_send.at[k], d_recv.at[m], dev) for k, dev in enumerate(near_dst + [far_dst])]

    def relayed(m):
        next_one = (lax.rem(m, 2) == 0) | (m >= n_micro - 3)
        return (m < direct) & (((me == 2) & next_one) | ((me == n_stage - 2) & jnp.logical_not(next_one)))

    def relay_far(m):
        return remote(dx0buf.at[m], dx0buf.at[m], r_sems.at[1], d_recv.at[m], far_dst)

    def bwd(m):
        with jax.named_scope("bwd_wait"):
            @pl.when(jnp.logical_not(last))
            def _():
                remote(gbuf.at[m], gbuf.at[m], b_send, b_recv.at[m], me).wait_recv()

            @pl.when(last)
            def _():
                @pl.when(m != last_id)
                def _():
                    remote(dnbuf.at[m], dnbuf.at[m], dn_ssem, dn_rsem.at[m], me).wait_recv()

                yf = ybuf[pl.ds(m * per, per)].reshape(seq, dim).astype(F32)
                inv = lax.rsqrt(jnp.mean(yf * yf, axis=-1, keepdims=True) + EPS)
                dnf = dnbuf[m].astype(F32)
                proj = jnp.mean(yf * dnf, axis=-1, keepdims=True)
                gbuf[m] = (dnf * inv - yf * (inv * inv * inv * proj)).astype(BF16)

        with jax.named_scope("bwd_comp"):
            g = gbuf[m]
            for j in range(n_fblk):
                cols = slice(j * fblk, (j + 1) * fblk)
                dh = dot(g, down_t[:, cols]).astype(BF16).astype(F32)
                abuf[m, :, cols] = (dh * gelu_slope(abuf[m, :, cols].astype(F32))).astype(BF16)
            dxbuf[m] = (g.astype(F32) + dot(abuf[m], up_t[...])).astype(BF16)

        @pl.when(jnp.logical_not(first))
        def _():
            remote(dxbuf.at[m], gbuf.at[m], b_send, b_recv.at[m], me - 1).start()

        @pl.when(first)
        def _():
            copies = dx0_copies(m)
            pl.when(m >= direct)(copies[-1].start)
            for c in copies[:-1]:
                c.start()

        pltpu.make_async_copy(abuf.at[m], da_out.at[m], out_sem.at[2]).start()
        pltpu.make_async_copy(gbuf.at[m], g_out.at[m], out_sem.at[3]).start()

    n_slot = obuf.shape[0]
    busy = chip == last_id // 2
    far_tile = remote(tmp_out.at[core, pl.ds(0, plan.rows)], tmp_out.at[core, pl.ds(0, plan.rows)], ic_send, od_recv, jnp.where(first, last_id, last_id - 1))
    sends_far = first | (me == last_id - 2)

    def tile_copy(k):
        rows = pl.ds(pl.multiple_of(k * plan.rows, plan.rows), plan.rows)
        slot = lax.rem(k, n_slot)
        return pltpu.make_async_copy(obuf.at[slot], tmp_out.at[core, rows], o_sem.at[slot])

    def piece(p):
        k = p // plan.per_tile
        rows = pl.ds(pl.multiple_of(p * plan.piece, plan.piece), plan.piece)
        here = pl.ds(pl.multiple_of(lax.rem(p, plan.per_tile) * plan.piece, plan.piece), plan.piece)
        return remote(obuf.at[lax.rem(k, n_slot), here], tmp_out.at[core, rows], od_send.at[k], od_recv, mate)

    def tile_sent(k):
        slot = lax.rem(k, n_slot)
        return remote(obuf.at[slot], tmp_out.at[core, pl.ds(0, plan.rows)], od_send.at[k], od_recv, mate)

    def emb_tile(k):
        with jax.named_scope("tile_prep"):

            @pl.when(k == 0)
            def _():
                for d in range(1, n_stage // 2):
                    src = lax.rem(mate + 2 * d, n_stage)
                    pl.when(jnp.logical_not(last))(remote(nbuf.at[src], nbuf.at[src], ag_send.at[0], ag_recv.at[src], me).wait_recv)
                for m in range(n_micro):
                    n_all_t[:, m * seq:(m + 1) * seq] = nbuf[m].T
                sa_all.wait_recv()
                for c in range(n_stage // 2):
                    shift[:, c * pair:(c + 1) * pair] = statall[2 * c, 0:1, :] * LOG2E + log_count

        slot = lax.rem(k, n_slot)
        with jax.named_scope("tile_wait"):
            @pl.when(k == 2)
            def _():
                tile_copy(0).wait()
                pl.when(sends_far)(far_tile.start)

            pl.when(k > n_slot)(lambda: tile_copy(k - n_slot).wait())
            pl.when((k >= n_slot) & (k - n_slot < plan.shared) & jnp.logical_not(busy & (k == n_slot)))(lambda: tile_sent(k - n_slot).wait_send())

        with jax.named_scope("tile"):
            rows = pl.ds(pl.multiple_of(k * plan.rows, plan.rows), plan.rows)
            logit_grad(emb[rows, :], n_all_t, shift, lab_ref, row0 + k * plan.rows, inv_count, scale, dz)
            obuf[slot] = dot(dz[...], nbuf[...].reshape(n_tok, dim)) * scale

        tile_copy(k).start()

    def send_pieces(done, until):
        lax.fori_loop(done, until, lambda p, c: (piece(p).start(), c)[1], 0)
        return jnp.maximum(done, until)

    before = sum(jnp.where(me == s, plan.before[s], 0) for s in range(n_stage))

    def pass_dx0(m, carry):
        @pl.when(jnp.logical_not(first))
        def _():
            remote(dx0buf.at[m], dx0buf.at[m], r_sems.at[0], d_recv.at[m], me).wait_recv()

            @pl.when(core == 0)
            def _():
                remote(dx0buf.at[m], dx0buf.at[m], r_sems.at[0], d_recv.at[m], mate).start()

            @pl.when(relayed(m))
            def _():
                relay_far(m).start()

            pltpu.make_async_copy(dx0buf.at[m], dx0_out.at[m], out_sem.at[4]).start()

        @pl.when(first)
        def _():
            pltpu.make_async_copy(dxbuf.at[m], dx0_out.at[m], out_sem.at[4]).start()

        return carry

    lead = jnp.where(me == 2, 40, jnp.where(me == n_stage - 2, -1460, jnp.where(me == far_dst, -1300, -10**6)))

    def work(i, carry):
        sent, passed = carry
        chunk = (i >= before) & (i < before + n_micro)
        pl.when(chunk)(lambda: bwd(i - before))
        k = jnp.where(i < before, i, i - n_micro)
        pl.when(jnp.logical_not(chunk))(lambda: emb_tile(k))
        after = i - before - n_micro + 1
        here = jnp.where(after > 0, jnp.clip((after * 257 + lead) // 146, 0, n_micro), 0)
        lax.fori_loop(passed, here, pass_dx0, 0)
        ready = jnp.where(i < before, i + 1, jnp.where(chunk, before, i + 1 - n_micro)) * plan.per_tile
        near_chunks = chunk | ((i < before) & (i + 1 >= before))
        until = jnp.minimum(jnp.minimum(ready, plan.shared * plan.per_tile), sent + jnp.where(near_chunks, 1, plan.per_tile + 1))
        return send_pieces(sent, until), jnp.maximum(passed, here)

    sent, passed = lax.fori_loop(0, plan.tiles + n_micro, work, (jnp.where(busy, plan.per_tile, 0), 0))
    outs = [pltpu.make_async_copy(nbuf, n_out, out_sem.at[5]), pltpu.make_async_copy(lossall, loss_out, out_sem.at[6]), pltpu.make_async_copy(meta, meta_out, out_sem.at[7])]
    lo_all.wait_recv()
    for c in outs:
        c.start()
    pltpu.make_async_copy(statall, stat_out, out_sem.at[8]).start()
    with jax.named_scope("relay_all"):
        lax.fori_loop(passed, n_micro, pass_dx0, 0)

    with jax.named_scope("drain"):
        send_pieces(sent, plan.shared * plan.per_tile)
        for k in range(max(plan.tiles - n_slot, 0), plan.tiles):
            tile_copy(k).wait()
            if k < plan.shared:
                tile_sent(k).wait_send()
        pl.when(sends_far)(far_tile.wait_send)
        all_rows = pl.ds(0, plan.shared * plan.rows)
        remote(tmp_out.at[1 - core, all_rows], tmp_out.at[1 - core, all_rows], od_send.at[0], od_recv, me).wait_recv()
        sa_all.wait_send()
        lo_all.wait_send()
        pltpu.make_async_copy(statall, stat_out, out_sem.at[8]).wait()
        for c, p in zip(ag_copies, peers):
            pl.when(p != last_id)(c.wait_send)

        @pl.when(jnp.logical_not(last))
        def _():
            dn_copy.wait_send()
            pl.when(mate != last_id)(n_forward.wait_send)
            remote(ybuf, xbuf, f_send, f_recv.at[0], me + 1).wait_send()

        @pl.when(last)
        def _():
            remote(nbuf, nbuf, n_send, n_recv.at[0], me).wait_send()

        @pl.when(mate != last_id)
        def _():
            some = nbuf.at[pl.ds(0, len(peers))]
            remote(some, some, fw_send, ag_recv.at[0], mate).wait_send()

        @pl.when(jnp.logical_not(first) & (me + 2 < n_micro))
        def _():
            x_copy(0).wait_send()

            @pl.when(me < 2)
            def _():
                x_copy(1).wait_send()

        @pl.when(jnp.logical_not(first))
        def _():
            remote(dxbuf, gbuf, b_send, b_recv.at[0], me).wait_send()
            pl.when(core == 0)(remote(dx0buf, dx0buf, r_sems.at[0], d_recv.at[0], mate).wait_send)

        @pl.when(first)
        def _():
            for k in range(len(near_dst)):
                remote(dxbuf, dx0buf, d_send.at[k], d_recv.at[0], me).wait_send()
            rest = pl.ds(0, n_micro - direct)
            remote(dxbuf.at[rest], dx0buf.at[rest], d_send.at[len(near_dst)], d_recv.at[0], me).wait_send()

        for dev, kept in ((2, by_next), (n_stage - 2, by_prev)):
            some = dx0buf.at[pl.ds(0, len(kept))]
            pl.when(me == dev)(remote(some, some, r_sems.at[1], d_recv.at[0], me).wait_send)

        pltpu.make_async_copy(hbuf, hid_out, out_sem.at[0]).wait()
        pltpu.make_async_copy(xbuf, xs_out, out_sem.at[1]).wait()
        pltpu.make_async_copy(abuf, da_out, out_sem.at[2]).wait()
        pltpu.make_async_copy(gbuf, g_out, out_sem.at[3]).wait()
        pltpu.make_async_copy(dx0buf, dx0_out, out_sem.at[4]).wait()
        for c in outs:
            c.wait()


class Plan:
    def __init__(self, vocab, n_stage):
        units = vocab // LANES
        self.base = units // 2 * LANES
        self.extra = vocab - 2 * self.base
        self.head_tile = next(t for t in (1600, 1536, 1280, 1024, 768, 640, 512, 256, 128) if self.base % t == 0)
        self.rows = 1024
        self.tiles, self.shared = 10, 8
        self.grad_tile = next(t for t in (4000, 3200, 1600, 1280, 640, 256, 128) if self.base % t == 0)
        self.e_parts = next(k for k in (10, 8, 5, 4, 2, 1) if self.base % (16 * k) == 0)
        self.part = 128
        self.slots = 4
        self.piece = 256
        self.per_tile = self.rows // self.piece
        measured = [10, 10, 7, 6, 3, 2, 0, 0]
        self.before = (measured + [0] * n_stage)[:n_stage]
        mid = self.base + self.extra
        ends = [(0, mid), (mid, vocab)]
        early = (self.tiles * self.rows, self.shared * self.rows)
        self.spans = [[(ends[h][0] + early[0 if h == c else 1], ends[h][1]) for h in (c, 1 - c)] for c in range(2)]
        self.longest = [max(self.spans[c][k][1] - self.spans[c][k][0] for c in range(2)) for k in range(2)]
        best = min(range(16, 1281, 16), key=lambda r: (sum(-(-n // r) for n in self.longest)) * (r + 40))
        self.calc_rows = best
        self.calc_steps = [-(-n // best) for n in self.longest]
        self.steps = sum(self.calc_steps)
        self.copy_rows = self.rows
        self.copies = self.tiles + self.shared
        self.starts = ends

    def calc_start(self, core, s):
        k = 0 if s < self.calc_steps[0] else 1
        lo, hi = self.spans[core][k]
        return min(lo + (s - k * self.calc_steps[0]) * self.calc_rows, hi - self.calc_rows)

    def copy_start(self, core, c):
        own = c < self.tiles
        h = core if own else 1 - core
        return self.starts[h][0] + (c if own else c - self.tiles) * self.copy_rows

    def cuts(self, core):
        firsts = [(self.calc_start(core, s), self.calc_rows) for s in range(self.steps)] + [(self.copy_start(core, c), self.copy_rows) for c in range(self.copies)]
        flat = [v for lo, rows in firsts for v in (lo, lo + rows)]
        return flat + [0] * (LANES - len(flat))


def run_pipe(x0, emb, w_up, w_down, labels, tokens, cuts, n_stage, plan):
    n_micro, seq = labels.shape
    dim, ffn = w_up.shape
    n_tok = n_micro * seq
    base = plan.base
    any_spec = pl.BlockSpec(memory_space=pl.ANY)
    act = (n_micro, seq, dim)
    fine = (n_tok // plan.part, plan.part, dim)
    wide = (n_micro, seq, ffn)
    dma = pltpu.SemaphoreType.DMA
    vm = pltpu.VMEM
    pair = 2 * seq
    return pl.pallas_call(
        functools.partial(pipe_kernel, n_stage, plan),
        out_shape=[
            jax.ShapeDtypeStruct(act, BF16), jax.ShapeDtypeStruct(fine, BF16), jax.ShapeDtypeStruct(wide, BF16),
            jax.ShapeDtypeStruct(wide, BF16), jax.ShapeDtypeStruct(act, BF16), jax.ShapeDtypeStruct(act, BF16),
            jax.ShapeDtypeStruct((n_stage, 8, pair), F32), jax.ShapeDtypeStruct((n_stage, 8, pair), F32), jax.ShapeDtypeStruct((2, plan.tiles * plan.rows, dim), F32),
            jax.ShapeDtypeStruct((3 * n_tok // LANES, LANES), jnp.int32),
        ],
        in_specs=[any_spec] * 4 + [pl.BlockSpec(memory_space=pltpu.VMEM)] * 3,
        out_specs=[any_spec] * 10,
        scratch_shapes=[
            vm(fine, BF16), vm(fine, BF16), vm(wide, BF16), vm(wide, BF16), vm(act, BF16), vm(act, BF16), vm(act, BF16), vm(act, BF16), vm(act, BF16),
            vm((dim, ffn), BF16), vm((ffn, dim), BF16), vm((ffn, dim), BF16), vm((dim, ffn), BF16),
            vm((base + plan.extra, dim), BF16), vm((base + plan.extra, pair), BF16), vm((dim, pair), BF16), vm((pair, dim), F32),
            vm((seq, dim), F32), vm((seq, dim), F32), vm((seq, dim), BF16), vm((16, pair), F32), vm((16, pair), F32), vm((n_stage, 8, pair), F32), vm((n_stage, 8, pair), F32),
            vm((2, 8, pair), F32), vm((dim, n_tok), BF16), vm((1, n_tok), F32), vm((plan.rows, n_tok), BF16), vm((plan.slots, plan.rows, dim), F32),
            vm((2, plan.head_tile, pair), BF16), vm((3 * n_tok // LANES, LANES), jnp.int32),
            dma((2,)), dma((2,)), dma((2,)), dma((2,)), dma((n_micro,)), dma, dma((n_tok // plan.part,)), dma, dma((n_micro,)), dma,
            dma((n_stage // 2,)), dma((n_micro,)), dma,
            dma((2,)), dma((2,)), dma, dma((n_stage,)), dma((2,)), dma((2,)), dma, dma((n_micro,)), dma((4,)), dma((n_micro,)), dma((2,)), dma((9,)),
            dma((plan.slots,)), dma((plan.shared,)), dma, dma,
        ],
        compiler_params=pltpu.CompilerParams(collective_id=0, has_side_effects=True, vmem_limit_bytes=67_000_000),
        cost_estimate=pl.CostEstimate(flops=60 * 10**9, bytes_accessed=100 * 10**6, transcendentals=0),
        name="pipe",
    )(x0.reshape(x0.shape[0], seq // plan.part, plan.part, dim), emb, w_up, w_down, labels.reshape(1, n_tok), tokens.reshape(1, n_tok), cuts)


def fin_kernel(n_stage, n_tok, plan, ids_ref, emb_hbm, tmp_hbm, n_hbm, stat_ref, part_ref, lab_ref, meta_ref, dx0_hbm, xs_hbm, hid_hbm, da_hbm, g_hbm,
               out_hbm, loss_ref, gup_hbm, gdown_hbm,
               n_all, dx0, xs, hid, da, g, n_t, x_t, dx0s, dz, shift, e_in, c_out, cp, gup, gdown,
               ld_sem, e_sem, t_sem, co_sem, po_sem, gu_sem, gd_sem, wi_sem):
    dim, ffn = gup_hbm.shape
    scale = dim ** -0.5
    inv_count = 1.0 / n_tok
    steps, crows, prows = plan.steps, plan.calc_rows, plan.copy_rows
    core = lax.rem(lax.axis_index("stage"), 2)
    early = plan.tiles * prows
    wblk = gup.shape[2]
    n_wblk = ffn // wblk
    turn = plan.calc_steps[0]

    def pick(pair):
        return jnp.where(core == 0, pair[0], pair[1])

    def calc_start(s):
        own = s < turn
        lo, hi = [jnp.where(own, pick([plan.spans[c][0][e] for c in range(2)]), pick([plan.spans[c][1][e] for c in range(2)])) for e in range(2)]
        return pl.multiple_of(jnp.minimum(lo + (s - jnp.where(own, 0, turn)) * crows, hi - crows), 16)

    def copy_start(c):
        own = c < plan.tiles
        first = jnp.where(own, pick([plan.starts[0][0], plan.starts[1][0]]), pick([plan.starts[1][0], plan.starts[0][0]]))
        return pl.multiple_of(first + (c - jnp.where(own, 0, plan.tiles)) * prows, 16)

    def e_copy(s):
        return pltpu.make_async_copy(emb_hbm.at[pl.ds(calc_start(s), crows)], e_in.at[lax.rem(s, 2)], e_sem.at[lax.rem(s, 2)])

    n_slot = cp.shape[0]
    ahead = 3

    def t_copy(c):
        own = c < plan.tiles
        row = jnp.where(own, core, 1 - core) * early + (c - jnp.where(own, 0, plan.tiles)) * prows
        slot = lax.rem(c, n_slot)
        return pltpu.make_async_copy(tmp_hbm.at[pl.ds(pl.multiple_of(row, 16), prows)], cp.at[slot], t_sem.at[slot])

    def p_out(c):
        slot = lax.rem(c, n_slot)
        return pltpu.make_async_copy(cp.at[slot], out_hbm.at[pl.ds(copy_start(c), prows)], po_sem.at[slot])

    def c_outs(s):
        slot = lax.rem(s, 2)
        return pltpu.make_async_copy(c_out.at[slot], out_hbm.at[pl.ds(calc_start(s), crows)], co_sem.at[slot])

    loads = [pltpu.make_async_copy(s, d, ld_sem.at[i]) for i, (s, d) in enumerate(((n_hbm, n_all), (dx0_hbm, dx0), (xs_hbm, xs), (g_hbm, g)))]
    loads[0].start()
    loads[1].start()
    e_copy(0).start()
    for c in range(ahead):
        t_copy(c).start(priority=1)
    pair = stat_ref.shape[2]
    loss = jnp.zeros((1, pair), F32)
    for d in range(n_stage):
        if d % 2 == 0:
            shift[:, (d // 2) * pair:(d // 2 + 1) * pair] = stat_ref[d, 0:1, :] * LOG2E + math.log2(n_tok)
        loss = loss + part_ref[d, 0:1, :]
    loss_ref[0] = jnp.sum(loss) * inv_count
    with jax.named_scope("fin_pre"):
        loads[0].wait()
        n_t[...] = n_all[...].T

    def sum_rows():
        loads[1].wait()
        dense = jnp.concatenate([meta_ref[g:g + 1, :] for g in range(n_tok // LANES)], axis=1)
        order = lax.broadcasted_iota(jnp.int32, (n_tok, n_tok), 0) == dense
        dx0s[...] = dot(jnp.where(order, 1.0, 0.0).astype(BF16), dx0[...])

    def add_rows(k, start, ref):
        lo, hi = ids_ref[2 * n_tok + k], ids_ref[2 * n_tok + k + 1]
        wide = 8

        def some(p, width):
            at = [pl.ds(ids_ref[n_tok + p + u] - start, 1) for u in range(width)]
            new = [ref[at[u], :] + dx0s[pl.ds(p + u, 1), :] for u in range(width)]
            for u in range(width):
                ref[at[u], :] = new[u]

        def group(g, carry):
            some(lo + g * wide, wide)
            return carry

        def single(p, carry):
            some(p, 1)
            return carry

        n_grp = (hi - lo) // wide
        lax.fori_loop(0, n_grp, group, 0)
        lax.fori_loop(lo + n_grp * wide, hi, single, 0)

    def w_ins(w):
        cols = pl.ds(pl.multiple_of(w * wblk, wblk), wblk)
        wslot = lax.rem(w, 2)
        return (pltpu.make_async_copy(da_hbm.at[:, cols], da.at[wslot], wi_sem.at[0, wslot]), pltpu.make_async_copy(hid_hbm.at[:, cols], hid.at[wslot], wi_sem.at[1, wslot]))

    def w_outs(w):
        cols = pl.ds(pl.multiple_of(w * wblk, wblk), wblk)
        wslot = lax.rem(w, 2)
        return (pltpu.make_async_copy(gup.at[wslot], gup_hbm.at[:, cols], gu_sem.at[wslot]), pltpu.make_async_copy(gdown.at[wslot], gdown_hbm.at[cols], gd_sem.at[wslot]))

    def copy_tile(c, carry):
        with jax.named_scope("copy_wait"):
            t_copy(c).wait()
        with jax.named_scope("add_p"):
            add_rows(2 * steps + 2 * c, copy_start(c), cp.at[lax.rem(c, n_slot)])
        p_out(c).start()

        @pl.when(c + ahead < plan.copies)
        def _():
            pl.when(c + ahead >= n_slot)(lambda: p_out(c + ahead - n_slot).wait())
            t_copy(c + ahead).start(priority=1)

        return carry

    w_first = 2
    tails = [turn - 1, steps - 1]

    def tail(s):
        return (s == tails[0]) | (s == tails[1])

    def step(s, carry):
        pl.when(s + 1 < steps)(lambda: e_copy(s + 1).start())
        with jax.named_scope("fin_wait"):
            e_copy(s).wait()

        @pl.when(s == 0)
        def _():
            for c in loads[2:]:
                c.start()

        w = s - w_first

        @pl.when((w + 1 >= 0) & (w + 1 < n_wblk))
        def _():
            for c in w_ins(w + 1):
                c.start()

        pl.when((s >= 2) & jnp.logical_not(tail(s - 1)))(lambda: c_outs(s - 2).wait())
        slot = lax.rem(s, 2)
        start = calc_start(s)
        with jax.named_scope("calc"):
            logit_grad(e_in[slot], n_t, shift, lab_ref, start, inv_count, scale, dz)
            c_out[slot] = dot(dz[...], n_all[...]) * scale
        pl.when(s == 0)(sum_rows)
        with jax.named_scope("add_c"):
            add_rows(2 * s, start, c_out.at[slot])
        pl.when(tail(s))(lambda: c_outs(s - 1).wait())
        c_outs(s).start()
        lax.fori_loop(s * plan.copies // (steps - 1), jnp.minimum((s + 1) * plan.copies // (steps - 1), plan.copies), copy_tile, 0)

        @pl.when(w == 0)
        def _():
            for c in loads[2:]:
                c.wait()
            x_t[...] = xs[...].T

        @pl.when((w >= 0) & (w < n_wblk))
        def _():
            wslot = lax.rem(w, 2)
            with jax.named_scope("dw_wait"):
                for c in w_ins(w):
                    c.wait()

                @pl.when(w >= 2)
                def _():
                    for c in w_outs(w - 2):
                        c.wait()

            with jax.named_scope("dw"):
                gup[wslot] = dot(x_t[...], da[wslot])
                gdown[wslot] = dot_t(hid[wslot], g[...])
            for c in w_outs(w):
                c.start()

        return carry

    lax.fori_loop(0, steps, step, 0)
    with jax.named_scope("fin_drain"):
        for w in range(n_wblk - 2, n_wblk):
            for c in w_outs(w):
                c.wait()
        c_outs(steps - 1).wait()
        for c in range(plan.copies - n_slot, plan.copies):
            p_out(c).wait()


def run_fin(emb, tmp, n_all, stats, losses, labels, meta, dx0, xs, hid, da, g, n_stage, plan):
    vocab, dim = emb.shape
    n_tok, ffn = hid.shape
    vm = pltpu.VMEM
    dma = pltpu.SemaphoreType.DMA
    any_spec = pl.BlockSpec(memory_space=pl.ANY)
    vspec = pl.BlockSpec(memory_space=pltpu.VMEM)
    smem = pl.BlockSpec(memory_space=pltpu.SMEM)
    wblk = 512
    return pl.pallas_call(
        functools.partial(fin_kernel, n_stage, n_tok, plan),
        out_shape=[jax.ShapeDtypeStruct((vocab, dim), F32), jax.ShapeDtypeStruct((1,), F32), jax.ShapeDtypeStruct((dim, ffn), F32), jax.ShapeDtypeStruct((ffn, dim), F32)],
        in_specs=[smem, any_spec, any_spec, any_spec, vspec, vspec, vspec, vspec] + [any_spec] * 5,
        out_specs=[any_spec, smem, any_spec, any_spec],
        scratch_shapes=[
            vm((n_tok, dim), BF16), vm((n_tok, dim), BF16), vm((n_tok, dim), BF16), vm((2, n_tok, wblk), BF16), vm((2, n_tok, wblk), BF16), vm((n_tok, dim), BF16),
            vm((dim, n_tok), BF16), vm((dim, n_tok), BF16), vm((n_tok, dim), F32), vm((plan.calc_rows, n_tok), BF16), vm((1, n_tok), F32),
            vm((2, plan.calc_rows, dim), BF16), vm((2, plan.calc_rows, dim), F32), vm((5, plan.copy_rows, dim), F32),
            vm((2, dim, wblk), F32), vm((2, wblk, dim), F32),
            dma((4,)), dma((2,)), dma((5,)), dma((2,)), dma((5,)), dma((2,)), dma((2,)), dma((2, 2)),
        ],
        compiler_params=pltpu.CompilerParams(vmem_limit_bytes=67_000_000),
        cost_estimate=pl.CostEstimate(flops=2 * n_tok * vocab * dim, bytes_accessed=5 * vocab * dim, transcendentals=0),
        name="fin",
    )(meta.reshape(-1), emb, tmp, n_all, stats, losses, labels.reshape(1, n_tok), meta, dx0, xs, hid, da, g)


def solution(mesh):
    n_stage = mesh.shape["stage"]

    def device_fn(tokens, labels, emb, w_up, w_down):
        n_micro, seq = tokens.shape
        vocab, dim = emb.shape
        w_up, w_down = w_up[0], w_down[0]
        n_tok = n_micro * seq
        plan = Plan(vocab, n_stage)
        cuts = jnp.array([plan.cuts(0), plan.cuts(1)], jnp.int32)
        x0 = run_gather(tokens, emb)
        n_all, xs, hid, da, g, dx0, stats, losses, tmp, meta = run_pipe(x0, emb, w_up, w_down, labels, tokens, cuts, n_stage, plan)
        flat = lambda p: p.reshape(n_tok, -1)
        grad_emb, loss, grad_up, grad_down = run_fin(
            emb, tmp.reshape(-1, dim), flat(n_all), stats, losses, labels, meta, flat(dx0), flat(xs), flat(hid), flat(da), flat(g), n_stage, plan
        )
        return loss, grad_up[None], grad_down[None], grad_emb

    return jax.shard_map(device_fn, mesh=mesh, in_specs=(P("dp", None), P("dp", None), P(None, None), P("stage", None, None), P("stage", None, None)), out_specs=(P("dp"), P(("dp", "stage"), None, None), P(("dp", "stage"), None, None), P("dp", None)), check_vma=False)
```

```python
import functools
import math

import jax
import jax.numpy as jnp
from jax import lax
from jax.experimental import pallas as pl
from jax.experimental.pallas import tpu as pltpu
from jax.sharding import PartitionSpec as P


MESH = pl.DeviceIdType.MESH
LOG2E = math.log2(math.e)
LN2 = math.log(2.0)
GELU_C = math.sqrt(2.0 / math.pi)
GELU_K = 0.044715
EPS = 1e-6
LANES = 128
F32 = jnp.float32
BF16 = jnp.bfloat16


def gelu_fwd(a):
    return (0.5 * a) * (1.0 + jnp.tanh(a * (GELU_C + (GELU_C * GELU_K) * (a * a))))


def gelu_slope(a):
    a2 = a * a
    half = 0.5 * jnp.tanh(a * (GELU_C + (GELU_C * GELU_K) * a2))
    up, down = 0.5 + half, 0.5 - half
    return up + (up * down) * (a * (2.0 * GELU_C + (6.0 * GELU_C * GELU_K) * a2))


def dot(x, y):
    return jnp.dot(x, y, preferred_element_type=F32)


def dot_t(x, y):
    return lax.dot_general(x, y, (((0,), (0,)), ((), ())), preferred_element_type=F32)


def remote(src, dst, send_sem, recv_sem, dev):
    return pltpu.make_async_remote_copy(src_ref=src, dst_ref=dst, send_sem=send_sem, recv_sem=recv_sem, device_id={"stage": dev}, device_id_type=MESH)


def send_halves(src, dst, send_sem, recv_sem, dev, halves=2):
    rows = src.shape[0] // halves
    for k in range(halves):
        part = pl.ds(k * rows, rows)
        remote(src.at[part], dst.at[part], send_sem, recv_sem, dev).start()


def column(row):
    return jnp.broadcast_to(row, (LANES, LANES)).T


def gather_kernel(ids_ref, tok_ref, emb_hbm, x0_hbm, tiles, picked, sem, out_sem):
    n_micro, seq = tok_ref.shape
    me = lax.axis_index("stage")
    group = tiles.shape[1] // seq
    slots = tiles.shape[0]
    owners = [head_chunk(me, k, n_micro) for k in range(slots)]

    def fetch(k):
        def one(i, carry):
            t = ids_ref[owners[k] * seq + i]
            start = pl.multiple_of(t // group * group, group)
            pltpu.make_async_copy(emb_hbm.at[pl.ds(start, group)], tiles.at[k, pl.ds(pl.multiple_of(i * group, group), group)], sem.at[k]).start()
            return carry

        lax.fori_loop(0, seq, one, 0, unroll=8)

    def select(k):
        sub = lax.broadcasted_iota(jnp.int32, (LANES, LANES), 0)
        lane = lax.broadcasted_iota(jnp.int32, (LANES, LANES), 1)
        tok = column(tok_ref[pl.ds(owners[k], 1), :].astype(F32)).astype(jnp.int32)
        want = sub * group + (tok - tok // group * group)
        hot = jnp.concatenate([jnp.where(lane + b * LANES == want, 1.0, 0.0).astype(BF16) for b in range(seq * group // LANES)], axis=1)
        pltpu.make_async_copy(emb_hbm.at[pl.ds(0, seq * group)], tiles.at[k], sem.at[k]).wait()
        picked[k] = dot(hot, tiles[k]).astype(BF16)
        pltpu.make_async_copy(picked.at[k], x0_hbm.at[k], out_sem.at[k]).start()

    def finish(k):
        pltpu.make_async_copy(picked.at[k], x0_hbm.at[k], out_sem.at[k]).wait()

    for work in (fetch, select, finish):
        work(0)
        for k in range(1, slots):
            pl.when(me < slots)(functools.partial(work, k))


def head_chunk(dev, k, n_micro):
    return jnp.minimum(jnp.where(dev < 2, 2 * dev + k, dev + 2), n_micro - 1)


def run_gather(tokens, emb):
    n_micro, seq = tokens.shape
    dim = emb.shape[1]
    group = 16
    return pl.pallas_call(
        gather_kernel,
        out_shape=jax.ShapeDtypeStruct((2, seq, dim), BF16),
        in_specs=[pl.BlockSpec(memory_space=pltpu.SMEM), pl.BlockSpec(memory_space=pltpu.VMEM), pl.BlockSpec(memory_space=pl.ANY)],
        out_specs=pl.BlockSpec(memory_space=pl.ANY),
        scratch_shapes=[pltpu.VMEM((2, seq * group, dim), BF16), pltpu.VMEM((2, seq, dim), BF16), pltpu.SemaphoreType.DMA((2,)), pltpu.SemaphoreType.DMA((2,))],
        cost_estimate=pl.CostEstimate(flops=10**9, bytes_accessed=2 * seq * group * dim * 2, transcendentals=0),
        name="gather",
    )(tokens.reshape(n_micro * seq), tokens, emb)


def token_table(row_ref, cut_ref, meta):
    n_tok = row_ref.shape[1]
    n_grp = n_tok // LANES
    lane = lax.broadcasted_iota(jnp.int32, (LANES, LANES), 1).astype(F32)
    sub = lax.broadcasted_iota(jnp.int32, (LANES, LANES), 0)
    row = lambda g: row_ref[:, g * LANES:(g + 1) * LANES].astype(F32)
    zero = jnp.zeros((LANES, LANES), F32)
    fold = lambda acc: jnp.sum(acc, axis=0, keepdims=True)
    cols = [column(row(c)) for c in range(n_grp)]
    firsts = []
    for g in range(n_grp):
        acc = zero
        for c in range(g + 1):
            same = cols[c] == row(g)
            if c == g:
                same = same & (sub < lane.astype(jnp.int32))
            acc = acc + jnp.where(same, 1.0, 0.0)
        firsts.append(column(jnp.where(fold(acc) == 0.0, 1.0, 0.0)))
    ranks = []
    for g in range(n_grp):
        acc = zero
        for c in range(n_grp):
            acc = acc + jnp.where(cols[c] < row(g), firsts[c], 0.0)
        ranks.append(fold(acc))
        meta[g:g + 1, :] = ranks[g].astype(jnp.int32)
    rank_cols = [column(r) for r in ranks]
    for g in range(n_grp):
        acc = zero
        for c in range(n_grp):
            acc = acc + jnp.where(rank_cols[c] == lane + g * LANES, firsts[c] * cols[c], 0.0)
        meta[n_grp + g:n_grp + g + 1, :] = fold(acc).astype(jnp.int32)
    cut = cut_ref[...].astype(F32)
    acc = zero
    for c in range(n_grp):
        acc = acc + jnp.where(cols[c] < cut, firsts[c], 0.0)
    meta[2 * n_grp:3 * n_grp, :] = jnp.broadcast_to(fold(acc), (n_grp, LANES)).astype(jnp.int32)


def logit_grad(e, n_t, shift, lab, first_id, inv_count, scale, dz):
    rows = e.shape[0]
    n_tok = n_t.shape[1]
    blk = 256
    vid = lax.broadcasted_iota(jnp.int32, (rows, blk), 0)
    for j in range(n_tok // blk):
        cols = slice(j * blk, (j + 1) * blk)
        z = (dot(e, n_t[:, cols]) * scale).astype(BF16).astype(F32)
        prob = jnp.exp2(z * LOG2E - shift[:, cols])
        dz[:, cols] = jnp.where(vid == lab[:, cols] - first_id, prob - inv_count, prob).astype(BF16)


def pipe_kernel(n_stage, plan, x0_hbm, emb_hbm, up_hbm, down_hbm, lab_ref, row_ref, cut_ref,
                n_out, xs_out, hid_out, da_out, g_out, dx0_out, stat_out, loss_out, tmp_out, meta_out,
                xbuf, ybuf, abuf, hbuf, nbuf, gbuf, dxbuf, dx0buf, dnbuf, up, down, up_t, down_t,
                emb, zbuf, n_t, dn_acc, dn_send, dn_recv, dn_own, st_send, st_recv, statall, lossall, tops, n_all_t, shift, dz, obuf, z_pair, meta,
                w_sem, e_sem, x_sem, x_send, x_recv, f_send, f_recv, n_send, n_recv, nf_send, ag_send, ag_recv, fw_send,
                st_sems, dp_sems, dn_ssem, dn_rsem, sa_sems, lo_sems, b_send, b_recv, d_send, d_recv, r_sems, out_sem, o_sem, od_send, od_recv, ic_send):
    n_micro, seq, dim = gbuf.shape
    part = xbuf.shape[1]
    n_part = xbuf.shape[0]
    per = seq // part
    n_tok = n_micro * seq
    ffn = up.shape[1]
    vocab = emb_hbm.shape[0]
    me = lax.axis_index("stage")
    core = lax.rem(me, 2)
    chip = me // 2
    mate = me + 1 - 2 * core
    last_id = n_stage - 1
    first = me == 0
    last = me == last_id
    fblk = 512
    n_fblk = ffn // fblk
    base, extra, tile = plan.base, plan.extra, plan.head_tile
    row0 = core * (base + extra)
    n_tiles = base // tile
    wide_tile = plan.grad_tile

    barrier = pltpu.get_barrier_semaphore()
    for d in range(1, n_stage):
        pl.semaphore_signal(barrier, inc=1, device_id={"stage": lax.rem(me + d, n_stage)}, device_id_type=MESH)
    w_copy = [pltpu.make_async_copy(up_hbm, up, w_sem.at[0]), pltpu.make_async_copy(down_hbm, down, w_sem.at[1])]
    for c in w_copy:
        c.start()
    x_slots = x0_hbm.shape[0]
    x_mine = [head_chunk(me, k, n_micro) for k in range(x_slots)]

    def x_rows(m):
        return xbuf.at[pl.ds(m * per, per)]

    def x_local(k):
        return pltpu.make_async_copy(x0_hbm.at[k], x_rows(k), x_sem.at[k])

    @pl.when(first)
    def _():
        for k in range(x_slots):
            x_local(k).start()

    e_parts = plan.e_parts
    e_step = base // e_parts

    def e_copy(i):
        src = emb_hbm.at[pl.ds(pl.multiple_of(row0 + i * e_step, 16), e_step)]
        return pltpu.make_async_copy(src, emb.at[pl.ds(i * e_step, e_step)], e_sem.at[0])

    e_more = pltpu.make_async_copy(emb_hbm.at[pl.ds(base, extra)], emb.at[pl.ds(base, extra)], e_sem.at[1])
    with jax.named_scope("entry"):
        pl.semaphore_wait(barrier, n_stage - 1)

    def x_copy(k):
        return remote(x0_hbm.at[k], x_rows(x_mine[k]), x_send.at[k], x_recv.at[x_mine[k]], 0)

    @pl.when(jnp.logical_not(first) & (me + 2 < n_micro))
    def _():
        x_copy(0).start()

        @pl.when(me < 2)
        def _():
            x_copy(1).start()

    with jax.named_scope("w_wait"):
        for c in w_copy:
            c.wait()
        for i in range(e_parts):
            e_copy(i).start()
        pl.when(core == 0)(e_more.start)

    def transpose_weights():
        for j in range(n_fblk):
            up_t[j * fblk:(j + 1) * fblk, :] = up[:, j * fblk:(j + 1) * fblk].T
            down_t[:, j * fblk:(j + 1) * fblk] = down[j * fblk:(j + 1) * fblk, :].T

    def idle_work():
        transpose_weights()
        token_table(row_ref, jnp.where(core == 0, cut_ref[0:1, :], cut_ref[1:2, :]), meta)

    @pl.when(chip >= n_stage // 4)
    def _():
        idle_work()

    def n_start(m):
        send_halves(nbuf.at[m], nbuf.at[m], n_send, n_recv.at[m], jnp.where(m == last_id, last_id - 1, m))

    def fwd(h, carry):
        m = h // per
        sub = lax.rem(h, per)
        rows = pl.ds(pl.multiple_of(sub * part, part), part)
        with jax.named_scope("fwd_wait"):

            @pl.when(first & (sub == 0))
            def _():
                @pl.when(m < x_slots)
                def _():
                    x_local(m).wait()

                @pl.when(m >= x_slots)
                def _():
                    remote(x_rows(m), x_rows(m), x_send.at[0], x_recv.at[m], me).wait_recv()

            @pl.when(jnp.logical_not(first))
            def _():
                remote(xbuf.at[h], xbuf.at[h], f_send, f_recv.at[h], me).wait_recv()

        with jax.named_scope("fwd_comp"):
            x = xbuf[h]
            for j in range(n_fblk):
                cols = slice(j * fblk, (j + 1) * fblk)
                a = dot(x, up[:, cols]).astype(BF16)
                abuf[m, rows, cols] = a
                hbuf[m, rows, cols] = gelu_fwd(a.astype(F32)).astype(BF16)
            y = (x.astype(F32) + dot(hbuf[m, rows, :], down[...])).astype(BF16)
            ybuf[h] = y

        @pl.when(jnp.logical_not(last))
        def _():
            send_halves(ybuf.at[h], xbuf.at[h], f_send, f_recv.at[h], me + 1)

        @pl.when(last)
        def _():
            yf = y.astype(F32)
            inv = lax.rsqrt(jnp.mean(yf * yf, axis=-1, keepdims=True) + EPS)
            nbuf[m, rows, :] = (yf * inv).astype(BF16)
            pl.when(sub == per - 1)(lambda: n_start(m))

        @pl.when(sub == per - 1)
        def _():
            pltpu.make_async_copy(hbuf.at[m], hid_out.at[m], out_sem.at[0]).start()
            pltpu.make_async_copy(x_rows(m), xs_out.at[pl.ds(m * per, per)], out_sem.at[1]).start()

        return carry

    lax.fori_loop(0, n_part, fwd, 0)

    @pl.when(chip < n_stage // 4)
    def _():
        idle_work()

    n_forward = remote(nbuf.at[me], nbuf.at[me], nf_send, n_recv.at[me], mate)
    with jax.named_scope("n_wait"):

        @pl.when(jnp.logical_not(last))
        def _():
            remote(nbuf.at[me], nbuf.at[me], n_send, n_recv.at[me], me).wait_recv()
            pl.when(mate != last_id)(n_forward.start)
            remote(nbuf.at[mate], nbuf.at[mate], n_send, n_recv.at[mate], me).wait_recv()

        for k in range(2):
            n_t[:, k * seq:(k + 1) * seq] = nbuf[2 * chip + k].T

    peers = [lax.rem(me + 2 * d, n_stage) for d in range(1, n_stage // 2)]
    ag_copies = [remote(nbuf.at[me], nbuf.at[me], ag_send.at[d], ag_recv.at[me], p) for d, p in enumerate(peers)]
    for c, p in zip(ag_copies, peers):
        pl.when(p != last_id)(c.start)
    with jax.named_scope("e_wait"):
        pltpu.make_async_copy(emb_hbm.at[pl.ds(0, base)], emb.at[pl.ds(0, base)], e_sem.at[0]).wait()
        pl.when(core == 0)(e_more.wait)

    pair = 2 * seq
    scale = dim ** -0.5
    inv_count = 1.0 / n_tok
    log_count = math.log2(n_tok)
    lab = lab_ref[:, pl.ds(pl.multiple_of(chip * pair, pair), pair)]

    def logits(rows, size):
        e = emb[rows, :]
        parts = [dot(e[k * size // 2:(k + 1) * size // 2], n_t[...]) for k in range(2)]
        z = jnp.concatenate([(p * scale).astype(BF16) for p in parts], axis=0)
        zbuf[rows, :] = z
        return z

    def peak(z, size, top):
        best = jnp.max(z.reshape(size // 16, 16, pair), axis=0).astype(F32)
        return jnp.maximum(top, jnp.maximum(best[:8], best[8:]))

    def total(z, size, old, top, tot):
        off = top * LOG2E
        return tot * jnp.exp2(old * LOG2E - off) + jnp.sum(jnp.exp2(z.astype(F32).reshape(size // 8, 8, pair) * LOG2E - off[None]), axis=0)

    tops[0] = jnp.full((8, pair), -jnp.inf, F32)
    tops[1] = jnp.zeros((8, pair), F32)

    @pl.when(core == 0)
    def _():
        z = logits(pl.ds(base, extra), extra)
        top = peak(z, extra, tops[0])
        tops[1] = total(z, extra, tops[0], top, tops[1])
        tops[0] = top

    def logits_step(i, slot, old, top, tot):
        z = logits(pl.ds(pl.multiple_of(i * tile, 16), tile), tile)
        tot = total(z_pair[1 - slot], tile, old, top, tot)
        z_pair[slot] = z
        return top, peak(z, tile, top), tot

    with jax.named_scope("logits"):
        z = logits(pl.ds(0, tile), tile)
        z_pair[0] = z
        state = (tops[0], peak(z, tile, tops[0]), tops[1])
        state = lax.fori_loop(0, (n_tiles - 1) // 2, lambda i, c: logits_step(2 * i + 2, 0, *logits_step(2 * i + 1, 1, *c)), state)
        if n_tiles % 2 == 0:
            state = logits_step(n_tiles - 1, 1, *state)
        old, top, tot = state
        tot = total(z_pair[(n_tiles - 1) % 2], tile, old, top, tot)
    row_top = jnp.max(top, axis=0, keepdims=True)
    row_tot = jnp.sum(tot * jnp.exp2((top - row_top) * LOG2E), axis=0, keepdims=True)
    st_send[0:8, :] = jnp.broadcast_to(row_top, (8, pair))
    st_send[8:16, :] = jnp.broadcast_to(row_tot, (8, pair))
    st_copy = remote(st_send, st_recv, st_sems.at[0], st_sems.at[1], mate)
    with jax.named_scope("stat_x"):
        st_copy.start()
        st_copy.wait()
    far_top = st_recv[0:1, :]
    far_tot = st_recv[8:9, :]
    all_top = jnp.maximum(row_top, far_top)
    mine = row_tot * jnp.exp(row_top - all_top)
    other = far_tot * jnp.exp(far_top - all_top)
    lse = all_top + jnp.log(jnp.where(core == 0, mine + other, other + mine))
    my_shift = lse * LOG2E + log_count
    others = [lax.rem(me + d, n_stage) for d in range(1, n_stage)]

    def spread(buf, sems):
        whole = buf.at[pl.ds(0, n_stage - 1)]
        return [remote(buf.at[me], buf.at[me], sems.at[0], sems.at[1], p) for p in others], remote(whole, whole, sems.at[0], sems.at[1], me)

    statall[me] = jnp.broadcast_to(lse, (8, pair))
    sa_copies, sa_all = spread(statall, sa_sems)
    for c in sa_copies:
        c.start()

    def grads(rows, size, first_row, picked):
        zf = zbuf[rows, :].astype(F32)
        prob = jnp.exp2(zf * LOG2E - my_shift)
        hit = lax.broadcasted_iota(jnp.int32, (size, pair), 0) == lab - (row0 + first_row)
        dz_t = jnp.where(hit, prob - inv_count, prob).astype(BF16)
        got = jnp.where(hit, zf, 0.0).reshape(size // 8, 8, pair)
        return dot_t(dz_t, emb[rows, :]), picked + jnp.sum(got, axis=0)

    tops[0] = jnp.zeros((8, pair), F32)
    dn_acc[...] = jnp.zeros_like(dn_acc)

    @pl.when(core == 0)
    def _():
        dn_acc[...], tops[0] = grads(pl.ds(base, extra), extra, base, tops[0])

    def grad_step(i, picked):
        part, picked = grads(pl.ds(pl.multiple_of(i * wide_tile, 16), wide_tile), wide_tile, i * wide_tile, picked)
        dn_acc[...] += part
        return picked

    with jax.named_scope("grads"):
        picked = lax.fori_loop(0, base // wide_tile, grad_step, tops[0])
    far = pl.ds(pl.multiple_of((1 - core) * seq, seq), seq)
    near = pl.ds(pl.multiple_of(core * seq, seq), seq)
    dn_send[...] = dn_acc[far, :]
    dp_copy = remote(dn_send, dn_recv, dp_sems.at[0], dp_sems.at[1], mate)
    dp_copy.start()
    row_loss = jnp.where(core == 0, lse, 0.0) - jnp.sum(picked, axis=0, keepdims=True)
    lossall[me] = jnp.broadcast_to(row_loss, (8, pair))
    lo_copies, lo_all = spread(lossall, lo_sems)
    for c in lo_copies:
        c.start()
    with jax.named_scope("dn_x"):
        dp_copy.wait()
        dn = ((dn_acc[near, :] + dn_recv[...]) * scale).astype(BF16)
    dn_copy = remote(dn_own, dnbuf.at[me], dn_ssem, dn_rsem.at[me], last_id)

    @pl.when(last)
    def _():
        dnbuf[last_id] = dn

    @pl.when(jnp.logical_not(last))
    def _():
        dn_own[...] = dn
        send_halves(dn_own, dnbuf.at[me], dn_ssem, dn_rsem.at[me], last_id)

    with jax.named_scope("ag_wait"):
        for p in peers:
            got = remote(nbuf.at[p], nbuf.at[p], ag_send.at[0], ag_recv.at[p], me)
            pl.when(jnp.logical_not(last))(got.wait_recv)
            pl.when(mate != last_id)(remote(nbuf.at[p], nbuf.at[p], fw_send, ag_recv.at[p], mate).start)

    near_dst = [1, 2, n_stage - 2]
    far_dst = n_stage // 2
    direct = n_micro - 1
    by_next = [m for m in range(direct) if m % 2 == 0 or m >= n_micro - 3]
    by_prev = [m for m in range(direct) if m not in by_next]

    def dx0_start(m, k, dev):
        send_halves(dxbuf.at[m], dx0buf.at[m], d_send.at[k], d_recv.at[m], dev)

    def relayed(m):
        next_one = (lax.rem(m, 2) == 0) | (m >= n_micro - 3)
        return (m < direct) & (((me == 2) & next_one) | ((me == n_stage - 2) & jnp.logical_not(next_one)))

    def relay_far(m):
        send_halves(dx0buf.at[m], dx0buf.at[m], r_sems.at[1], d_recv.at[m], far_dst)

    def bwd(m):
        with jax.named_scope("bwd_wait"):
            @pl.when(jnp.logical_not(last))
            def _():
                remote(gbuf.at[m], gbuf.at[m], b_send, b_recv.at[m], me).wait_recv()

            @pl.when(last)
            def _():
                @pl.when(m != last_id)
                def _():
                    remote(dnbuf.at[m], dnbuf.at[m], dn_ssem, dn_rsem.at[m], me).wait_recv()

                yf = ybuf[pl.ds(m * per, per)].reshape(seq, dim).astype(F32)
                inv = lax.rsqrt(jnp.mean(yf * yf, axis=-1, keepdims=True) + EPS)
                dnf = dnbuf[m].astype(F32)
                proj = jnp.mean(yf * dnf, axis=-1, keepdims=True)
                gbuf[m] = (dnf * inv - yf * (inv * inv * inv * proj)).astype(BF16)

        with jax.named_scope("bwd_comp"):
            g = gbuf[m]
            for j in range(n_fblk):
                cols = slice(j * fblk, (j + 1) * fblk)
                dh = dot(g, down_t[:, cols]).astype(BF16).astype(F32)
                abuf[m, :, cols] = (dh * gelu_slope(abuf[m, :, cols].astype(F32))).astype(BF16)
            dxbuf[m] = (g.astype(F32) + dot(abuf[m], up_t[...])).astype(BF16)

        @pl.when(jnp.logical_not(first))
        def _():
            send_halves(dxbuf.at[m], gbuf.at[m], b_send, b_recv.at[m], me - 1)

        @pl.when(first)
        def _():
            pl.when(m >= direct)(lambda: dx0_start(m, len(near_dst), far_dst))
            for k, dev in enumerate(near_dst):
                dx0_start(m, k, dev)

        pltpu.make_async_copy(abuf.at[m], da_out.at[m], out_sem.at[2]).start()
        pltpu.make_async_copy(gbuf.at[m], g_out.at[m], out_sem.at[3]).start()

    n_slot = obuf.shape[0]
    busy = chip == last_id // 2
    far_tile = remote(tmp_out.at[core, pl.ds(0, plan.rows)], tmp_out.at[core, pl.ds(0, plan.rows)], ic_send, od_recv, jnp.where(first, last_id, last_id - 1))
    sends_far = first | (me == last_id - 2)

    def tile_copy(k):
        rows = pl.ds(pl.multiple_of(k * plan.rows, plan.rows), plan.rows)
        slot = lax.rem(k, n_slot)
        return pltpu.make_async_copy(obuf.at[slot], tmp_out.at[core, rows], o_sem.at[slot])

    def piece(p):
        k = p // plan.per_tile
        rows = pl.ds(pl.multiple_of(p * plan.piece, plan.piece), plan.piece)
        here = pl.ds(pl.multiple_of(lax.rem(p, plan.per_tile) * plan.piece, plan.piece), plan.piece)
        return remote(obuf.at[lax.rem(k, n_slot), here], tmp_out.at[core, rows], od_send.at[k], od_recv, mate)

    def tile_sent(k):
        slot = lax.rem(k, n_slot)
        return remote(obuf.at[slot], tmp_out.at[core, pl.ds(0, plan.rows)], od_send.at[k], od_recv, mate)

    def emb_tile(k):
        with jax.named_scope("tile_prep"):

            @pl.when(k == 0)
            def _():
                for d in range(1, n_stage // 2):
                    src = lax.rem(mate + 2 * d, n_stage)
                    pl.when(jnp.logical_not(last))(remote(nbuf.at[src], nbuf.at[src], ag_send.at[0], ag_recv.at[src], me).wait_recv)
                for m in range(n_micro):
                    n_all_t[:, m * seq:(m + 1) * seq] = nbuf[m].T
                sa_all.wait_recv()
                for c in range(n_stage // 2):
                    shift[:, c * pair:(c + 1) * pair] = statall[2 * c, 0:1, :] * LOG2E + log_count

        slot = lax.rem(k, n_slot)
        with jax.named_scope("tile_wait"):
            @pl.when(k == 2)
            def _():
                tile_copy(0).wait()
                pl.when(sends_far)(far_tile.start)

            pl.when(k > n_slot)(lambda: tile_copy(k - n_slot).wait())
            pl.when((k >= n_slot) & (k - n_slot < plan.shared) & jnp.logical_not(busy & (k == n_slot)))(lambda: tile_sent(k - n_slot).wait_send())

        with jax.named_scope("tile"):
            rows = pl.ds(pl.multiple_of(k * plan.rows, plan.rows), plan.rows)
            logit_grad(emb[rows, :], n_all_t, shift, lab_ref, row0 + k * plan.rows, inv_count, scale, dz)
            obuf[slot] = dot(dz[...], nbuf[...].reshape(n_tok, dim)) * scale

        tile_copy(k).start()

    def send_pieces(done, until):
        lax.fori_loop(done, until, lambda p, c: (piece(p).start(), c)[1], 0)
        return jnp.maximum(done, until)

    before = sum(jnp.where(me == s, plan.before[s], 0) for s in range(n_stage))

    def pass_dx0(m, carry):
        @pl.when(jnp.logical_not(first))
        def _():
            remote(dx0buf.at[m], dx0buf.at[m], r_sems.at[0], d_recv.at[m], me).wait_recv()

            @pl.when(core == 0)
            def _():
                remote(dx0buf.at[m], dx0buf.at[m], r_sems.at[0], d_recv.at[m], mate).start()

            @pl.when(relayed(m))
            def _():
                relay_far(m)

            pltpu.make_async_copy(dx0buf.at[m], dx0_out.at[m], out_sem.at[4]).start()

        @pl.when(first)
        def _():
            pltpu.make_async_copy(dxbuf.at[m], dx0_out.at[m], out_sem.at[4]).start()

        return carry

    lead = jnp.where(me == 2, 40, jnp.where(me == n_stage - 2, -1460, jnp.where(me == far_dst, -1300, -10**6)))

    def work(i, carry):
        sent, passed = carry
        chunk = (i >= before) & (i < before + n_micro)
        pl.when(chunk)(lambda: bwd(i - before))
        k = jnp.where(i < before, i, i - n_micro)
        pl.when(jnp.logical_not(chunk))(lambda: emb_tile(k))
        after = i - before - n_micro + 1
        here = jnp.where(after > 0, jnp.clip((after * 257 + lead) // 146, 0, n_micro), 0)
        lax.fori_loop(passed, here, pass_dx0, 0)
        ready = jnp.where(i < before, i + 1, jnp.where(chunk, before, i + 1 - n_micro)) * plan.per_tile
        near_chunks = chunk | ((i < before) & (i + 1 >= before))
        until = jnp.minimum(jnp.minimum(ready, plan.shared * plan.per_tile), sent + jnp.where(near_chunks, 1, plan.per_tile + 1))
        return send_pieces(sent, until), jnp.maximum(passed, here)

    sent, passed = lax.fori_loop(0, plan.tiles + n_micro, work, (jnp.where(busy, plan.per_tile, 0), 0))
    outs = [pltpu.make_async_copy(nbuf, n_out, out_sem.at[5]), pltpu.make_async_copy(lossall, loss_out, out_sem.at[6]), pltpu.make_async_copy(meta, meta_out, out_sem.at[7])]
    lo_all.wait_recv()
    for c in outs:
        c.start()
    pltpu.make_async_copy(statall, stat_out, out_sem.at[8]).start()
    with jax.named_scope("relay_all"):
        lax.fori_loop(passed, n_micro, pass_dx0, 0)

    with jax.named_scope("drain"):
        send_pieces(sent, plan.shared * plan.per_tile)
        for k in range(max(plan.tiles - n_slot, 0), plan.tiles):
            tile_copy(k).wait()
            if k < plan.shared:
                tile_sent(k).wait_send()
        pl.when(sends_far)(far_tile.wait_send)
        all_rows = pl.ds(0, plan.shared * plan.rows)
        remote(tmp_out.at[1 - core, all_rows], tmp_out.at[1 - core, all_rows], od_send.at[0], od_recv, me).wait_recv()
        sa_all.wait_send()
        lo_all.wait_send()
        pltpu.make_async_copy(statall, stat_out, out_sem.at[8]).wait()
        for c, p in zip(ag_copies, peers):
            pl.when(p != last_id)(c.wait_send)

        @pl.when(jnp.logical_not(last))
        def _():
            dn_copy.wait_send()
            pl.when(mate != last_id)(n_forward.wait_send)
            remote(ybuf, xbuf, f_send, f_recv.at[0], me + 1).wait_send()

        @pl.when(last)
        def _():
            remote(nbuf, nbuf, n_send, n_recv.at[0], me).wait_send()

        @pl.when(mate != last_id)
        def _():
            some = nbuf.at[pl.ds(0, len(peers))]
            remote(some, some, fw_send, ag_recv.at[0], mate).wait_send()

        @pl.when(jnp.logical_not(first) & (me + 2 < n_micro))
        def _():
            x_copy(0).wait_send()

            @pl.when(me < 2)
            def _():
                x_copy(1).wait_send()

        @pl.when(jnp.logical_not(first))
        def _():
            remote(dxbuf, gbuf, b_send, b_recv.at[0], me).wait_send()
            pl.when(core == 0)(remote(dx0buf, dx0buf, r_sems.at[0], d_recv.at[0], mate).wait_send)

        @pl.when(first)
        def _():
            for k in range(len(near_dst)):
                remote(dxbuf, dx0buf, d_send.at[k], d_recv.at[0], me).wait_send()
            rest = pl.ds(0, n_micro - direct)
            remote(dxbuf.at[rest], dx0buf.at[rest], d_send.at[len(near_dst)], d_recv.at[0], me).wait_send()

        for dev, kept in ((2, by_next), (n_stage - 2, by_prev)):
            some = dx0buf.at[pl.ds(0, len(kept))]
            pl.when(me == dev)(remote(some, some, r_sems.at[1], d_recv.at[0], me).wait_send)

        pltpu.make_async_copy(hbuf, hid_out, out_sem.at[0]).wait()
        pltpu.make_async_copy(xbuf, xs_out, out_sem.at[1]).wait()
        pltpu.make_async_copy(abuf, da_out, out_sem.at[2]).wait()
        pltpu.make_async_copy(gbuf, g_out, out_sem.at[3]).wait()
        pltpu.make_async_copy(dx0buf, dx0_out, out_sem.at[4]).wait()
        for c in outs:
            c.wait()


class Plan:
    def __init__(self, vocab, n_stage):
        units = vocab // LANES
        self.base = units // 2 * LANES
        self.extra = vocab - 2 * self.base
        self.head_tile = next(t for t in (1600, 1536, 1280, 1024, 768, 640, 512, 256, 128) if self.base % t == 0)
        self.rows = 1024
        self.tiles, self.shared = 10, 8
        self.grad_tile = next(t for t in (4000, 3200, 1600, 1280, 640, 256, 128) if self.base % t == 0)
        self.e_parts = next(k for k in (10, 8, 5, 4, 2, 1) if self.base % (16 * k) == 0)
        self.part = 128
        self.slots = 4
        self.piece = 256
        self.per_tile = self.rows // self.piece
        measured = [10, 9, 6, 5, 3, 2, 0, 0]
        self.before = (measured + [0] * n_stage)[:n_stage]
        mid = self.base + self.extra
        ends = [(0, mid), (mid, vocab)]
        early = (self.tiles * self.rows, self.shared * self.rows)
        self.spans = [[(ends[h][0] + early[0 if h == c else 1], ends[h][1]) for h in (c, 1 - c)] for c in range(2)]
        self.longest = [max(self.spans[c][k][1] - self.spans[c][k][0] for c in range(2)) for k in range(2)]
        best = min(range(16, 1281, 16), key=lambda r: (sum(-(-n // r) for n in self.longest)) * (r + 40))
        self.calc_rows = best
        self.calc_steps = [-(-n // best) for n in self.longest]
        self.steps = sum(self.calc_steps)
        self.copy_rows = self.rows
        self.copies = self.tiles + self.shared
        self.starts = ends

    def calc_start(self, core, s):
        k = 0 if s < self.calc_steps[0] else 1
        lo, hi = self.spans[core][k]
        return min(lo + (s - k * self.calc_steps[0]) * self.calc_rows, hi - self.calc_rows)

    def copy_start(self, core, c):
        own = c < self.tiles
        h = core if own else 1 - core
        return self.starts[h][0] + (c if own else c - self.tiles) * self.copy_rows

    def cuts(self, core):
        firsts = [(self.calc_start(core, s), self.calc_rows) for s in range(self.steps)] + [(self.copy_start(core, c), self.copy_rows) for c in range(self.copies)]
        flat = [v for lo, rows in firsts for v in (lo, lo + rows)]
        return flat + [0] * (LANES - len(flat))


def run_pipe(x0, emb, w_up, w_down, labels, tokens, cuts, n_stage, plan):
    n_micro, seq = labels.shape
    dim, ffn = w_up.shape
    n_tok = n_micro * seq
    base = plan.base
    any_spec = pl.BlockSpec(memory_space=pl.ANY)
    act = (n_micro, seq, dim)
    fine = (n_tok // plan.part, plan.part, dim)
    wide = (n_micro, seq, ffn)
    dma = pltpu.SemaphoreType.DMA
    vm = pltpu.VMEM
    pair = 2 * seq
    return pl.pallas_call(
        functools.partial(pipe_kernel, n_stage, plan),
        out_shape=[
            jax.ShapeDtypeStruct(act, BF16), jax.ShapeDtypeStruct(fine, BF16), jax.ShapeDtypeStruct(wide, BF16),
            jax.ShapeDtypeStruct(wide, BF16), jax.ShapeDtypeStruct(act, BF16), jax.ShapeDtypeStruct(act, BF16),
            jax.ShapeDtypeStruct((n_stage, 8, pair), F32), jax.ShapeDtypeStruct((n_stage, 8, pair), F32), jax.ShapeDtypeStruct((2, plan.tiles * plan.rows, dim), F32),
            jax.ShapeDtypeStruct((3 * n_tok // LANES, LANES), jnp.int32),
        ],
        in_specs=[any_spec] * 4 + [pl.BlockSpec(memory_space=pltpu.VMEM)] * 3,
        out_specs=[any_spec] * 10,
        scratch_shapes=[
            vm(fine, BF16), vm(fine, BF16), vm(wide, BF16), vm(wide, BF16), vm(act, BF16), vm(act, BF16), vm(act, BF16), vm(act, BF16), vm(act, BF16),
            vm((dim, ffn), BF16), vm((ffn, dim), BF16), vm((ffn, dim), BF16), vm((dim, ffn), BF16),
            vm((base + plan.extra, dim), BF16), vm((base + plan.extra, pair), BF16), vm((dim, pair), BF16), vm((pair, dim), F32),
            vm((seq, dim), F32), vm((seq, dim), F32), vm((seq, dim), BF16), vm((16, pair), F32), vm((16, pair), F32), vm((n_stage, 8, pair), F32), vm((n_stage, 8, pair), F32),
            vm((2, 8, pair), F32), vm((dim, n_tok), BF16), vm((1, n_tok), F32), vm((plan.rows, n_tok), BF16), vm((plan.slots, plan.rows, dim), F32),
            vm((2, plan.head_tile, pair), BF16), vm((3 * n_tok // LANES, LANES), jnp.int32),
            dma((2,)), dma((2,)), dma((2,)), dma((2,)), dma((n_micro,)), dma, dma((n_tok // plan.part,)), dma, dma((n_micro,)), dma,
            dma((n_stage // 2,)), dma((n_micro,)), dma,
            dma((2,)), dma((2,)), dma, dma((n_stage,)), dma((2,)), dma((2,)), dma, dma((n_micro,)), dma((4,)), dma((n_micro,)), dma((2,)), dma((9,)),
            dma((plan.slots,)), dma((plan.shared,)), dma, dma,
        ],
        compiler_params=pltpu.CompilerParams(collective_id=0, has_side_effects=True, vmem_limit_bytes=67_000_000),
        cost_estimate=pl.CostEstimate(flops=60 * 10**9, bytes_accessed=100 * 10**6, transcendentals=0),
        name="pipe",
    )(x0.reshape(x0.shape[0], seq // plan.part, plan.part, dim), emb, w_up, w_down, labels.reshape(1, n_tok), tokens.reshape(1, n_tok), cuts)


def fin_kernel(n_stage, n_tok, plan, ids_ref, emb_hbm, tmp_hbm, n_hbm, stat_ref, part_ref, lab_ref, meta_ref, dx0_hbm, xs_hbm, hid_hbm, da_hbm, g_hbm,
               out_hbm, loss_ref, gup_hbm, gdown_hbm,
               n_all, dx0, xs, hid, da, g, n_t, x_t, dx0s, dz, shift, e_in, c_out, cp, gup, gdown,
               ld_sem, e_sem, t_sem, co_sem, po_sem, gu_sem, gd_sem, wi_sem):
    dim, ffn = gup_hbm.shape
    scale = dim ** -0.5
    inv_count = 1.0 / n_tok
    steps, crows, prows = plan.steps, plan.calc_rows, plan.copy_rows
    core = lax.rem(lax.axis_index("stage"), 2)
    early = plan.tiles * prows
    wblk = gup.shape[2]
    n_wblk = ffn // wblk
    turn = plan.calc_steps[0]

    def pick(pair):
        return jnp.where(core == 0, pair[0], pair[1])

    def calc_start(s):
        own = s < turn
        lo, hi = [jnp.where(own, pick([plan.spans[c][0][e] for c in range(2)]), pick([plan.spans[c][1][e] for c in range(2)])) for e in range(2)]
        return pl.multiple_of(jnp.minimum(lo + (s - jnp.where(own, 0, turn)) * crows, hi - crows), 16)

    def copy_start(c):
        own = c < plan.tiles
        first = jnp.where(own, pick([plan.starts[0][0], plan.starts[1][0]]), pick([plan.starts[1][0], plan.starts[0][0]]))
        return pl.multiple_of(first + (c - jnp.where(own, 0, plan.tiles)) * prows, 16)

    def e_copy(s):
        return pltpu.make_async_copy(emb_hbm.at[pl.ds(calc_start(s), crows)], e_in.at[lax.rem(s, 2)], e_sem.at[lax.rem(s, 2)])

    n_slot = cp.shape[0]
    ahead = 3

    def t_copy(c):
        own = c < plan.tiles
        row = jnp.where(own, core, 1 - core) * early + (c - jnp.where(own, 0, plan.tiles)) * prows
        slot = lax.rem(c, n_slot)
        return pltpu.make_async_copy(tmp_hbm.at[pl.ds(pl.multiple_of(row, 16), prows)], cp.at[slot], t_sem.at[slot])

    def p_out(c):
        slot = lax.rem(c, n_slot)
        return pltpu.make_async_copy(cp.at[slot], out_hbm.at[pl.ds(copy_start(c), prows)], po_sem.at[slot])

    def c_outs(s):
        slot = lax.rem(s, 2)
        return pltpu.make_async_copy(c_out.at[slot], out_hbm.at[pl.ds(calc_start(s), crows)], co_sem.at[slot])

    loads = [pltpu.make_async_copy(s, d, ld_sem.at[i]) for i, (s, d) in enumerate(((n_hbm, n_all), (dx0_hbm, dx0), (xs_hbm, xs), (g_hbm, g)))]
    loads[0].start()
    loads[1].start()
    e_copy(0).start()
    for c in range(ahead):
        t_copy(c).start(priority=1)
    pair = stat_ref.shape[2]
    loss = jnp.zeros((1, pair), F32)
    for d in range(n_stage):
        if d % 2 == 0:
            shift[:, (d // 2) * pair:(d // 2 + 1) * pair] = stat_ref[d, 0:1, :] * LOG2E + math.log2(n_tok)
        loss = loss + part_ref[d, 0:1, :]
    loss_ref[0] = jnp.sum(loss) * inv_count
    with jax.named_scope("fin_pre"):
        loads[0].wait()
        n_t[...] = n_all[...].T

    def sum_rows():
        loads[1].wait()
        dense = jnp.concatenate([meta_ref[g:g + 1, :] for g in range(n_tok // LANES)], axis=1)
        order = lax.broadcasted_iota(jnp.int32, (n_tok, n_tok), 0) == dense
        dx0s[...] = dot(jnp.where(order, 1.0, 0.0).astype(BF16), dx0[...])

    def add_rows(k, start, ref):
        lo, hi = ids_ref[2 * n_tok + k], ids_ref[2 * n_tok + k + 1]
        wide = 8

        def some(p, width):
            at = [pl.ds(ids_ref[n_tok + p + u] - start, 1) for u in range(width)]
            new = [ref[at[u], :] + dx0s[pl.ds(p + u, 1), :] for u in range(width)]
            for u in range(width):
                ref[at[u], :] = new[u]

        def group(g, carry):
            some(lo + g * wide, wide)
            return carry

        def single(p, carry):
            some(p, 1)
            return carry

        n_grp = (hi - lo) // wide
        lax.fori_loop(0, n_grp, group, 0)
        lax.fori_loop(lo + n_grp * wide, hi, single, 0)

    def w_ins(w):
        cols = pl.ds(pl.multiple_of(w * wblk, wblk), wblk)
        wslot = lax.rem(w, 2)
        return (pltpu.make_async_copy(da_hbm.at[:, cols], da.at[wslot], wi_sem.at[0, wslot]), pltpu.make_async_copy(hid_hbm.at[:, cols], hid.at[wslot], wi_sem.at[1, wslot]))

    def w_outs(w):
        cols = pl.ds(pl.multiple_of(w * wblk, wblk), wblk)
        wslot = lax.rem(w, 2)
        return (pltpu.make_async_copy(gup.at[wslot], gup_hbm.at[:, cols], gu_sem.at[wslot]), pltpu.make_async_copy(gdown.at[wslot], gdown_hbm.at[cols], gd_sem.at[wslot]))

    def copy_tile(c, carry):
        with jax.named_scope("copy_wait"):
            t_copy(c).wait()
        with jax.named_scope("add_p"):
            add_rows(2 * steps + 2 * c, copy_start(c), cp.at[lax.rem(c, n_slot)])
        p_out(c).start()

        @pl.when(c + ahead < plan.copies)
        def _():
            pl.when(c + ahead >= n_slot)(lambda: p_out(c + ahead - n_slot).wait())
            t_copy(c + ahead).start(priority=1)

        return carry

    w_first = 2
    tails = [turn - 1, steps - 1]

    def tail(s):
        return (s == tails[0]) | (s == tails[1])

    def step(s, carry):
        pl.when(s + 1 < steps)(lambda: e_copy(s + 1).start())
        with jax.named_scope("fin_wait"):
            e_copy(s).wait()

        @pl.when(s == 0)
        def _():
            for c in loads[2:]:
                c.start()

        w = s - w_first

        @pl.when((w + 1 >= 0) & (w + 1 < n_wblk))
        def _():
            for c in w_ins(w + 1):
                c.start()

        pl.when((s >= 2) & jnp.logical_not(tail(s - 1)))(lambda: c_outs(s - 2).wait())
        slot = lax.rem(s, 2)
        start = calc_start(s)
        with jax.named_scope("calc"):
            logit_grad(e_in[slot], n_t, shift, lab_ref, start, inv_count, scale, dz)
            c_out[slot] = dot(dz[...], n_all[...]) * scale
        pl.when(s == 0)(sum_rows)
        with jax.named_scope("add_c"):
            add_rows(2 * s, start, c_out.at[slot])
        pl.when(tail(s))(lambda: c_outs(s - 1).wait())
        c_outs(s).start()
        lax.fori_loop(s * plan.copies // (steps - 1), jnp.minimum((s + 1) * plan.copies // (steps - 1), plan.copies), copy_tile, 0)

        @pl.when(w == 0)
        def _():
            for c in loads[2:]:
                c.wait()
            x_t[...] = xs[...].T

        @pl.when((w >= 0) & (w < n_wblk))
        def _():
            wslot = lax.rem(w, 2)
            with jax.named_scope("dw_wait"):
                for c in w_ins(w):
                    c.wait()

                @pl.when(w >= 2)
                def _():
                    for c in w_outs(w - 2):
                        c.wait()

            with jax.named_scope("dw"):
                gup[wslot] = dot(x_t[...], da[wslot])
                gdown[wslot] = dot_t(hid[wslot], g[...])
            for c in w_outs(w):
                c.start()

        return carry

    lax.fori_loop(0, steps, step, 0)
    with jax.named_scope("fin_drain"):
        for w in range(n_wblk - 2, n_wblk):
            for c in w_outs(w):
                c.wait()
        c_outs(steps - 1).wait()
        for c in range(plan.copies - n_slot, plan.copies):
            p_out(c).wait()


def run_fin(emb, tmp, n_all, stats, losses, labels, meta, dx0, xs, hid, da, g, n_stage, plan):
    vocab, dim = emb.shape
    n_tok, ffn = hid.shape
    vm = pltpu.VMEM
    dma = pltpu.SemaphoreType.DMA
    any_spec = pl.BlockSpec(memory_space=pl.ANY)
    vspec = pl.BlockSpec(memory_space=pltpu.VMEM)
    smem = pl.BlockSpec(memory_space=pltpu.SMEM)
    wblk = 512
    return pl.pallas_call(
        functools.partial(fin_kernel, n_stage, n_tok, plan),
        out_shape=[jax.ShapeDtypeStruct((vocab, dim), F32), jax.ShapeDtypeStruct((1,), F32), jax.ShapeDtypeStruct((dim, ffn), F32), jax.ShapeDtypeStruct((ffn, dim), F32)],
        in_specs=[smem, any_spec, any_spec, any_spec, vspec, vspec, vspec, vspec] + [any_spec] * 5,
        out_specs=[any_spec, smem, any_spec, any_spec],
        scratch_shapes=[
            vm((n_tok, dim), BF16), vm((n_tok, dim), BF16), vm((n_tok, dim), BF16), vm((2, n_tok, wblk), BF16), vm((2, n_tok, wblk), BF16), vm((n_tok, dim), BF16),
            vm((dim, n_tok), BF16), vm((dim, n_tok), BF16), vm((n_tok, dim), F32), vm((plan.calc_rows, n_tok), BF16), vm((1, n_tok), F32),
            vm((2, plan.calc_rows, dim), BF16), vm((2, plan.calc_rows, dim), F32), vm((5, plan.copy_rows, dim), F32),
            vm((2, dim, wblk), F32), vm((2, wblk, dim), F32),
            dma((4,)), dma((2,)), dma((5,)), dma((2,)), dma((5,)), dma((2,)), dma((2,)), dma((2, 2)),
        ],
        compiler_params=pltpu.CompilerParams(vmem_limit_bytes=67_000_000),
        cost_estimate=pl.CostEstimate(flops=2 * n_tok * vocab * dim, bytes_accessed=5 * vocab * dim, transcendentals=0),
        name="fin",
    )(meta.reshape(-1), emb, tmp, n_all, stats, losses, labels.reshape(1, n_tok), meta, dx0, xs, hid, da, g)


def solution(mesh):
    n_stage = mesh.shape["stage"]

    def device_fn(tokens, labels, emb, w_up, w_down):
        n_micro, seq = tokens.shape
        vocab, dim = emb.shape
        w_up, w_down = w_up[0], w_down[0]
        n_tok = n_micro * seq
        plan = Plan(vocab, n_stage)
        cuts = jnp.array([plan.cuts(0), plan.cuts(1)], jnp.int32)
        x0 = run_gather(tokens, emb)
        n_all, xs, hid, da, g, dx0, stats, losses, tmp, meta = run_pipe(x0, emb, w_up, w_down, labels, tokens, cuts, n_stage, plan)
        flat = lambda p: p.reshape(n_tok, -1)
        grad_emb, loss, grad_up, grad_down = run_fin(
            emb, tmp.reshape(-1, dim), flat(n_all), stats, losses, labels, meta, flat(dx0), flat(xs), flat(hid), flat(da), flat(g), n_stage, plan
        )
        return loss, grad_up[None], grad_down[None], grad_emb

    return jax.shard_map(device_fn, mesh=mesh, in_specs=(P("dp", None), P("dp", None), P(None, None), P("stage", None, None), P("stage", None, None)), out_specs=(P("dp"), P(("dp", "stage"), None, None), P(("dp", "stage"), None, None), P("dp", None)), check_vma=False)
```

```python
import functools
import math

import jax
import jax.numpy as jnp
from jax import lax
from jax.experimental import pallas as pl
from jax.experimental.pallas import tpu as pltpu
from jax.sharding import PartitionSpec as P


MESH = pl.DeviceIdType.MESH
LOG2E = math.log2(math.e)
LN2 = math.log(2.0)
GELU_C = math.sqrt(2.0 / math.pi)
GELU_K = 0.044715
EPS = 1e-6
LANES = 128
F32 = jnp.float32
BF16 = jnp.bfloat16


def gelu_fwd(a):
    return (0.5 * a) * (1.0 + jnp.tanh(a * (GELU_C + (GELU_C * GELU_K) * (a * a))))


def gelu_slope(a):
    a2 = a * a
    half = 0.5 * jnp.tanh(a * (GELU_C + (GELU_C * GELU_K) * a2))
    up, down = 0.5 + half, 0.5 - half
    return up + (up * down) * (a * (2.0 * GELU_C + (6.0 * GELU_C * GELU_K) * a2))


def dot(x, y):
    return jnp.dot(x, y, preferred_element_type=F32)


def dot_t(x, y):
    return lax.dot_general(x, y, (((0,), (0,)), ((), ())), preferred_element_type=F32)


def remote(src, dst, send_sem, recv_sem, dev):
    return pltpu.make_async_remote_copy(src_ref=src, dst_ref=dst, send_sem=send_sem, recv_sem=recv_sem, device_id={"stage": dev}, device_id_type=MESH)


def send_halves(src, dst, send_sem, recv_sem, dev, halves=2):
    rows = src.shape[0] // halves
    for k in range(halves):
        part = pl.ds(k * rows, rows)
        remote(src.at[part], dst.at[part], send_sem, recv_sem, dev).start()


def column(row):
    return jnp.broadcast_to(row, (LANES, LANES)).T


def gather_kernel(ids_ref, tok_ref, emb_hbm, x0_hbm, tiles, picked, sem, out_sem):
    n_micro, seq = tok_ref.shape
    me = lax.axis_index("stage")
    group = tiles.shape[1] // seq
    slots = tiles.shape[0]
    owners = [head_chunk(me, k, n_micro) for k in range(slots)]

    def fetch(k):
        def one(i, carry):
            t = ids_ref[owners[k] * seq + i]
            start = pl.multiple_of(t // group * group, group)
            pltpu.make_async_copy(emb_hbm.at[pl.ds(start, group)], tiles.at[k, pl.ds(pl.multiple_of(i * group, group), group)], sem.at[k]).start()
            return carry

        lax.fori_loop(0, seq, one, 0, unroll=8)

    def select(k):
        sub = lax.broadcasted_iota(jnp.int32, (LANES, LANES), 0)
        lane = lax.broadcasted_iota(jnp.int32, (LANES, LANES), 1)
        tok = column(tok_ref[pl.ds(owners[k], 1), :].astype(F32)).astype(jnp.int32)
        want = sub * group + (tok - tok // group * group)
        hot = jnp.concatenate([jnp.where(lane + b * LANES == want, 1.0, 0.0).astype(BF16) for b in range(seq * group // LANES)], axis=1)
        pltpu.make_async_copy(emb_hbm.at[pl.ds(0, seq * group)], tiles.at[k], sem.at[k]).wait()
        picked[k] = dot(hot, tiles[k]).astype(BF16)
        pltpu.make_async_copy(picked.at[k], x0_hbm.at[k], out_sem.at[k]).start()

    def finish(k):
        pltpu.make_async_copy(picked.at[k], x0_hbm.at[k], out_sem.at[k]).wait()

    for work in (fetch, select, finish):
        work(0)
        for k in range(1, slots):
            pl.when(me < slots)(functools.partial(work, k))


def head_chunk(dev, k, n_micro):
    return jnp.minimum(jnp.where(dev < 2, 2 * dev + k, dev + 2), n_micro - 1)


def run_gather(tokens, emb):
    n_micro, seq = tokens.shape
    dim = emb.shape[1]
    group = 16
    return pl.pallas_call(
        gather_kernel,
        out_shape=jax.ShapeDtypeStruct((2, seq, dim), BF16),
        in_specs=[pl.BlockSpec(memory_space=pltpu.SMEM), pl.BlockSpec(memory_space=pltpu.VMEM), pl.BlockSpec(memory_space=pl.ANY)],
        out_specs=pl.BlockSpec(memory_space=pl.ANY),
        scratch_shapes=[pltpu.VMEM((2, seq * group, dim), BF16), pltpu.VMEM((2, seq, dim), BF16), pltpu.SemaphoreType.DMA((2,)), pltpu.SemaphoreType.DMA((2,))],
        cost_estimate=pl.CostEstimate(flops=10**9, bytes_accessed=2 * seq * group * dim * 2, transcendentals=0),
        name="gather",
    )(tokens.reshape(n_micro * seq), tokens, emb)


def token_table(row_ref, cut_ref, meta):
    n_tok = row_ref.shape[1]
    n_grp = n_tok // LANES
    lane = lax.broadcasted_iota(jnp.int32, (LANES, LANES), 1).astype(F32)
    sub = lax.broadcasted_iota(jnp.int32, (LANES, LANES), 0)
    row = lambda g: row_ref[:, g * LANES:(g + 1) * LANES].astype(F32)
    zero = jnp.zeros((LANES, LANES), F32)
    fold = lambda acc: jnp.sum(acc, axis=0, keepdims=True)
    cols = [column(row(c)) for c in range(n_grp)]
    firsts = []
    for g in range(n_grp):
        acc = zero
        for c in range(g + 1):
            same = cols[c] == row(g)
            if c == g:
                same = same & (sub < lane.astype(jnp.int32))
            acc = acc + jnp.where(same, 1.0, 0.0)
        firsts.append(column(jnp.where(fold(acc) == 0.0, 1.0, 0.0)))
    ranks = []
    for g in range(n_grp):
        acc = zero
        for c in range(n_grp):
            acc = acc + jnp.where(cols[c] < row(g), firsts[c], 0.0)
        ranks.append(fold(acc))
        meta[g:g + 1, :] = ranks[g].astype(jnp.int32)
    rank_cols = [column(r) for r in ranks]
    for g in range(n_grp):
        acc = zero
        for c in range(n_grp):
            acc = acc + jnp.where(rank_cols[c] == lane + g * LANES, firsts[c] * cols[c], 0.0)
        meta[n_grp + g:n_grp + g + 1, :] = fold(acc).astype(jnp.int32)
    cut = cut_ref[...].astype(F32)
    acc = zero
    for c in range(n_grp):
        acc = acc + jnp.where(cols[c] < cut, firsts[c], 0.0)
    meta[2 * n_grp:3 * n_grp, :] = jnp.broadcast_to(fold(acc), (n_grp, LANES)).astype(jnp.int32)


def logit_grad(e, n_t, shift, lab, first_id, inv_count, scale, dz):
    rows = e.shape[0]
    n_tok = n_t.shape[1]
    blk = 256
    vid = lax.broadcasted_iota(jnp.int32, (rows, blk), 0)
    for j in range(n_tok // blk):
        cols = slice(j * blk, (j + 1) * blk)
        z = (dot(e, n_t[:, cols]) * scale).astype(BF16).astype(F32)
        prob = jnp.exp2(z * LOG2E - shift[:, cols])
        dz[:, cols] = jnp.where(vid == lab[:, cols] - first_id, prob - inv_count, prob).astype(BF16)


def pipe_kernel(n_stage, plan, x0_hbm, emb_hbm, up_hbm, down_hbm, lab_ref, row_ref, cut_ref,
                n_out, xs_out, hid_out, da_out, g_out, dx0_out, stat_out, loss_out, tmp_out, meta_out,
                xbuf, ybuf, abuf, hbuf, nbuf, gbuf, dxbuf, dx0buf, dnbuf, up, down, up_t, down_t,
                emb, zbuf, n_t, dn_acc, dn_send, dn_recv, dn_own, st_send, st_recv, statall, lossall, tops, n_all_t, shift, dz, obuf, z_pair, meta,
                w_sem, e_sem, x_sem, x_send, x_recv, f_send, f_recv, n_send, n_recv, nf_send, ag_send, ag_recv, fw_send,
                st_sems, dp_sems, dn_ssem, dn_rsem, sa_sems, lo_sems, b_send, b_recv, d_send, d_recv, r_sems, out_sem, o_sem, od_send, od_recv, ic_send):
    n_micro, seq, dim = gbuf.shape
    part = xbuf.shape[1]
    n_part = xbuf.shape[0]
    per = seq // part
    n_tok = n_micro * seq
    ffn = up.shape[1]
    vocab = emb_hbm.shape[0]
    me = lax.axis_index("stage")
    core = lax.rem(me, 2)
    chip = me // 2
    mate = me + 1 - 2 * core
    last_id = n_stage - 1
    first = me == 0
    last = me == last_id
    fblk = 512
    n_fblk = ffn // fblk
    base, extra, tile = plan.base, plan.extra, plan.head_tile
    row0 = core * (base + extra)
    n_tiles = base // tile
    wide_tile = plan.grad_tile

    barrier = pltpu.get_barrier_semaphore()
    for d in range(1, n_stage):
        pl.semaphore_signal(barrier, inc=1, device_id={"stage": lax.rem(me + d, n_stage)}, device_id_type=MESH)
    w_copy = [pltpu.make_async_copy(up_hbm, up, w_sem.at[0]), pltpu.make_async_copy(down_hbm, down, w_sem.at[1])]
    for c in w_copy:
        c.start()
    x_slots = x0_hbm.shape[0]
    x_mine = [head_chunk(me, k, n_micro) for k in range(x_slots)]

    def x_rows(m):
        return xbuf.at[pl.ds(m * per, per)]

    def x_local(k):
        return pltpu.make_async_copy(x0_hbm.at[k], x_rows(k), x_sem.at[k])

    @pl.when(first)
    def _():
        for k in range(x_slots):
            x_local(k).start()

    e_parts = plan.e_parts
    e_step = base // e_parts

    def e_copy(i):
        src = emb_hbm.at[pl.ds(pl.multiple_of(row0 + i * e_step, 16), e_step)]
        return pltpu.make_async_copy(src, emb.at[pl.ds(i * e_step, e_step)], e_sem.at[0])

    e_more = pltpu.make_async_copy(emb_hbm.at[pl.ds(base, extra)], emb.at[pl.ds(base, extra)], e_sem.at[1])
    with jax.named_scope("entry"):
        pl.semaphore_wait(barrier, n_stage - 1)

    def x_copy(k):
        return remote(x0_hbm.at[k], x_rows(x_mine[k]), x_send.at[k], x_recv.at[x_mine[k]], 0)

    @pl.when(jnp.logical_not(first) & (me + 2 < n_micro))
    def _():
        x_copy(0).start()

        @pl.when(me < 2)
        def _():
            x_copy(1).start()

    with jax.named_scope("w_wait"):
        for c in w_copy:
            c.wait()
        for i in range(e_parts):
            e_copy(i).start()
        pl.when(core == 0)(e_more.start)

    def transpose_weights():
        for j in range(n_fblk):
            up_t[j * fblk:(j + 1) * fblk, :] = up[:, j * fblk:(j + 1) * fblk].T
            down_t[:, j * fblk:(j + 1) * fblk] = down[j * fblk:(j + 1) * fblk, :].T

    def idle_work():
        transpose_weights()
        token_table(row_ref, jnp.where(core == 0, cut_ref[0:1, :], cut_ref[1:2, :]), meta)

    @pl.when(chip >= n_stage // 4)
    def _():
        idle_work()

    def n_start(m):
        send_halves(nbuf.at[m], nbuf.at[m], n_send, n_recv.at[m], jnp.where(m == last_id, last_id - 1, m))

    def fwd(h, carry):
        m = h // per
        sub = lax.rem(h, per)
        rows = pl.ds(pl.multiple_of(sub * part, part), part)
        with jax.named_scope("fwd_wait"):

            @pl.when(first & (sub == 0))
            def _():
                @pl.when(m < x_slots)
                def _():
                    x_local(m).wait()

                @pl.when(m >= x_slots)
                def _():
                    remote(x_rows(m), x_rows(m), x_send.at[0], x_recv.at[m], me).wait_recv()

            @pl.when(jnp.logical_not(first))
            def _():
                remote(xbuf.at[h], xbuf.at[h], f_send, f_recv.at[h], me).wait_recv()

        with jax.named_scope("fwd_comp"):
            x = xbuf[h]
            for j in range(n_fblk):
                cols = slice(j * fblk, (j + 1) * fblk)
                a = dot(x, up[:, cols]).astype(BF16)
                abuf[m, rows, cols] = a
                hbuf[m, rows, cols] = gelu_fwd(a.astype(F32)).astype(BF16)
            y = (x.astype(F32) + dot(hbuf[m, rows, :], down[...])).astype(BF16)
            ybuf[h] = y

        @pl.when(jnp.logical_not(last))
        def _():
            send_halves(ybuf.at[h], xbuf.at[h], f_send, f_recv.at[h], me + 1)

        @pl.when(last)
        def _():
            yf = y.astype(F32)
            inv = lax.rsqrt(jnp.mean(yf * yf, axis=-1, keepdims=True) + EPS)
            nbuf[m, rows, :] = (yf * inv).astype(BF16)
            pl.when(sub == per - 1)(lambda: n_start(m))

        @pl.when(sub == per - 1)
        def _():
            pltpu.make_async_copy(hbuf.at[m], hid_out.at[m], out_sem.at[0]).start()
            pltpu.make_async_copy(x_rows(m), xs_out.at[pl.ds(m * per, per)], out_sem.at[1]).start()

        return carry

    lax.fori_loop(0, n_part, fwd, 0)

    @pl.when(chip < n_stage // 4)
    def _():
        idle_work()

    n_forward = remote(nbuf.at[me], nbuf.at[me], nf_send, n_recv.at[me], mate)
    with jax.named_scope("n_wait"):

        @pl.when(jnp.logical_not(last))
        def _():
            remote(nbuf.at[me], nbuf.at[me], n_send, n_recv.at[me], me).wait_recv()
            pl.when(mate != last_id)(n_forward.start)
            remote(nbuf.at[mate], nbuf.at[mate], n_send, n_recv.at[mate], me).wait_recv()

        for k in range(2):
            n_t[:, k * seq:(k + 1) * seq] = nbuf[2 * chip + k].T

    peers = [lax.rem(me + 2 * d, n_stage) for d in range(1, n_stage // 2)]
    ag_copies = [remote(nbuf.at[me], nbuf.at[me], ag_send.at[d], ag_recv.at[me], p) for d, p in enumerate(peers)]
    for c, p in zip(ag_copies, peers):
        pl.when(p != last_id)(c.start)
    with jax.named_scope("e_wait"):
        pltpu.make_async_copy(emb_hbm.at[pl.ds(0, base)], emb.at[pl.ds(0, base)], e_sem.at[0]).wait()
        pl.when(core == 0)(e_more.wait)

    pair = 2 * seq
    scale = dim ** -0.5
    inv_count = 1.0 / n_tok
    log_count = math.log2(n_tok)
    lab = lab_ref[:, pl.ds(pl.multiple_of(chip * pair, pair), pair)]

    def logits(rows, size):
        e = emb[rows, :]
        parts = [dot(e[k * size // 2:(k + 1) * size // 2], n_t[...]) for k in range(2)]
        z = jnp.concatenate([(p * scale).astype(BF16) for p in parts], axis=0)
        zbuf[rows, :] = z
        return z

    def peak(z, size, top):
        best = jnp.max(z.reshape(size // 16, 16, pair), axis=0).astype(F32)
        return jnp.maximum(top, jnp.maximum(best[:8], best[8:]))

    def total(z, size, old, top, tot):
        off = top * LOG2E
        return tot * jnp.exp2(old * LOG2E - off) + jnp.sum(jnp.exp2(z.astype(F32).reshape(size // 8, 8, pair) * LOG2E - off[None]), axis=0)

    tops[0] = jnp.full((8, pair), -jnp.inf, F32)
    tops[1] = jnp.zeros((8, pair), F32)

    @pl.when(core == 0)
    def _():
        z = logits(pl.ds(base, extra), extra)
        top = peak(z, extra, tops[0])
        tops[1] = total(z, extra, tops[0], top, tops[1])
        tops[0] = top

    def logits_step(i, slot, old, top, tot):
        z = logits(pl.ds(pl.multiple_of(i * tile, 16), tile), tile)
        tot = total(z_pair[1 - slot], tile, old, top, tot)
        z_pair[slot] = z
        return top, peak(z, tile, top), tot

    with jax.named_scope("logits"):
        z = logits(pl.ds(0, tile), tile)
        z_pair[0] = z
        state = (tops[0], peak(z, tile, tops[0]), tops[1])
        state = lax.fori_loop(0, (n_tiles - 1) // 2, lambda i, c: logits_step(2 * i + 2, 0, *logits_step(2 * i + 1, 1, *c)), state)
        if n_tiles % 2 == 0:
            state = logits_step(n_tiles - 1, 1, *state)
        old, top, tot = state
        tot = total(z_pair[(n_tiles - 1) % 2], tile, old, top, tot)
    row_top = jnp.max(top, axis=0, keepdims=True)
    row_tot = jnp.sum(tot * jnp.exp2((top - row_top) * LOG2E), axis=0, keepdims=True)
    st_send[0:8, :] = jnp.broadcast_to(row_top, (8, pair))
    st_send[8:16, :] = jnp.broadcast_to(row_tot, (8, pair))
    st_copy = remote(st_send, st_recv, st_sems.at[0], st_sems.at[1], mate)
    with jax.named_scope("stat_x"):
        st_copy.start()
        st_copy.wait()
    far_top = st_recv[0:1, :]
    far_tot = st_recv[8:9, :]
    all_top = jnp.maximum(row_top, far_top)
    mine = row_tot * jnp.exp(row_top - all_top)
    other = far_tot * jnp.exp(far_top - all_top)
    lse = all_top + jnp.log(jnp.where(core == 0, mine + other, other + mine))
    my_shift = lse * LOG2E + log_count
    others = [lax.rem(me + d, n_stage) for d in range(1, n_stage)]

    def spread(buf, sems):
        whole = buf.at[pl.ds(0, n_stage - 1)]
        return [remote(buf.at[me], buf.at[me], sems.at[0], sems.at[1], p) for p in others], remote(whole, whole, sems.at[0], sems.at[1], me)

    statall[me] = jnp.broadcast_to(lse, (8, pair))
    sa_copies, sa_all = spread(statall, sa_sems)
    for c in sa_copies:
        c.start()

    def grads(rows, size, first_row, picked):
        zf = zbuf[rows, :].astype(F32)
        prob = jnp.exp2(zf * LOG2E - my_shift)
        hit = lax.broadcasted_iota(jnp.int32, (size, pair), 0) == lab - (row0 + first_row)
        dz_t = jnp.where(hit, prob - inv_count, prob).astype(BF16)
        got = jnp.where(hit, zf, 0.0).reshape(size // 8, 8, pair)
        return dot_t(dz_t, emb[rows, :]), picked + jnp.sum(got, axis=0)

    tops[0] = jnp.zeros((8, pair), F32)
    dn_acc[...] = jnp.zeros_like(dn_acc)

    @pl.when(core == 0)
    def _():
        dn_acc[...], tops[0] = grads(pl.ds(base, extra), extra, base, tops[0])

    def grad_step(i, picked):
        part, picked = grads(pl.ds(pl.multiple_of(i * wide_tile, 16), wide_tile), wide_tile, i * wide_tile, picked)
        dn_acc[...] += part
        return picked

    with jax.named_scope("grads"):
        picked = lax.fori_loop(0, base // wide_tile, grad_step, tops[0])
    far = pl.ds(pl.multiple_of((1 - core) * seq, seq), seq)
    near = pl.ds(pl.multiple_of(core * seq, seq), seq)
    dn_send[...] = dn_acc[far, :]
    dp_copy = remote(dn_send, dn_recv, dp_sems.at[0], dp_sems.at[1], mate)
    dp_copy.start()
    row_loss = jnp.where(core == 0, lse, 0.0) - jnp.sum(picked, axis=0, keepdims=True)
    lossall[me] = jnp.broadcast_to(row_loss, (8, pair))
    lo_copies, lo_all = spread(lossall, lo_sems)
    for c in lo_copies:
        c.start()
    with jax.named_scope("dn_x"):
        dp_copy.wait()
        dn = ((dn_acc[near, :] + dn_recv[...]) * scale).astype(BF16)
    dn_copy = remote(dn_own, dnbuf.at[me], dn_ssem, dn_rsem.at[me], last_id)

    @pl.when(last)
    def _():
        dnbuf[last_id] = dn

    @pl.when(jnp.logical_not(last))
    def _():
        dn_own[...] = dn
        send_halves(dn_own, dnbuf.at[me], dn_ssem, dn_rsem.at[me], last_id)

    with jax.named_scope("ag_wait"):
        for p in peers:
            got = remote(nbuf.at[p], nbuf.at[p], ag_send.at[0], ag_recv.at[p], me)
            pl.when(jnp.logical_not(last))(got.wait_recv)
            pl.when(mate != last_id)(remote(nbuf.at[p], nbuf.at[p], fw_send, ag_recv.at[p], mate).start)

    near_dst = [1, 3, last_id]
    far_dst = n_stage // 2 + 1
    direct = n_micro - 1
    by_prev = [m for m in range(direct) if m >= n_micro - 3]
    by_next = [m for m in range(direct) if m < n_micro - 3]
    hands_on = (core == 1) & (me != 1)

    def dx0_start(m, k, dev):
        send_halves(dxbuf.at[m], dx0buf.at[m], d_send.at[k], d_recv.at[m], dev)

    def relayed(m):
        late = m >= n_micro - 3
        return (m < direct) & (((me == 3) & jnp.logical_not(late)) | (last & late))

    def relay_far(m):
        send_halves(dx0buf.at[m], dx0buf.at[m], r_sems.at[1], d_recv.at[m], far_dst)

    def bwd(m):
        with jax.named_scope("bwd_wait"):
            @pl.when(jnp.logical_not(last))
            def _():
                remote(gbuf.at[m], gbuf.at[m], b_send, b_recv.at[m], me).wait_recv()

            @pl.when(last)
            def _():
                @pl.when(m != last_id)
                def _():
                    remote(dnbuf.at[m], dnbuf.at[m], dn_ssem, dn_rsem.at[m], me).wait_recv()

                yf = ybuf[pl.ds(m * per, per)].reshape(seq, dim).astype(F32)
                inv = lax.rsqrt(jnp.mean(yf * yf, axis=-1, keepdims=True) + EPS)
                dnf = dnbuf[m].astype(F32)
                proj = jnp.mean(yf * dnf, axis=-1, keepdims=True)
                gbuf[m] = (dnf * inv - yf * (inv * inv * inv * proj)).astype(BF16)

        with jax.named_scope("bwd_comp"):
            g = gbuf[m]
            for j in range(n_fblk):
                cols = slice(j * fblk, (j + 1) * fblk)
                dh = dot(g, down_t[:, cols]).astype(BF16).astype(F32)
                abuf[m, :, cols] = (dh * gelu_slope(abuf[m, :, cols].astype(F32))).astype(BF16)
            dxbuf[m] = (g.astype(F32) + dot(abuf[m], up_t[...])).astype(BF16)

        @pl.when(jnp.logical_not(first))
        def _():
            send_halves(dxbuf.at[m], gbuf.at[m], b_send, b_recv.at[m], me - 1)

        @pl.when(first)
        def _():
            pl.when(m >= direct)(lambda: dx0_start(m, len(near_dst), far_dst))
            for k, dev in enumerate(near_dst):
                dx0_start(m, k, dev)

        pltpu.make_async_copy(abuf.at[m], da_out.at[m], out_sem.at[2]).start()
        pltpu.make_async_copy(gbuf.at[m], g_out.at[m], out_sem.at[3]).start()

    n_slot = obuf.shape[0]
    busy = chip == last_id // 2
    far_tile = remote(tmp_out.at[core, pl.ds(0, plan.rows)], tmp_out.at[core, pl.ds(0, plan.rows)], ic_send, od_recv, jnp.where(first, last_id, last_id - 1))
    sends_far = first | (me == last_id - 2)

    def tile_copy(k):
        rows = pl.ds(pl.multiple_of(k * plan.rows, plan.rows), plan.rows)
        slot = lax.rem(k, n_slot)
        return pltpu.make_async_copy(obuf.at[slot], tmp_out.at[core, rows], o_sem.at[slot])

    def piece(p):
        k = p // plan.per_tile
        rows = pl.ds(pl.multiple_of(p * plan.piece, plan.piece), plan.piece)
        here = pl.ds(pl.multiple_of(lax.rem(p, plan.per_tile) * plan.piece, plan.piece), plan.piece)
        return remote(obuf.at[lax.rem(k, n_slot), here], tmp_out.at[core, rows], od_send.at[k], od_recv, mate)

    def tile_sent(k):
        slot = lax.rem(k, n_slot)
        return remote(obuf.at[slot], tmp_out.at[core, pl.ds(0, plan.rows)], od_send.at[k], od_recv, mate)

    def emb_tile(k):
        with jax.named_scope("tile_prep"):

            @pl.when(k == 0)
            def _():
                for d in range(1, n_stage // 2):
                    src = lax.rem(mate + 2 * d, n_stage)
                    pl.when(jnp.logical_not(last))(remote(nbuf.at[src], nbuf.at[src], ag_send.at[0], ag_recv.at[src], me).wait_recv)
                for m in range(n_micro):
                    n_all_t[:, m * seq:(m + 1) * seq] = nbuf[m].T
                sa_all.wait_recv()
                for c in range(n_stage // 2):
                    shift[:, c * pair:(c + 1) * pair] = statall[2 * c, 0:1, :] * LOG2E + log_count

        slot = lax.rem(k, n_slot)
        with jax.named_scope("tile_wait"):
            @pl.when(k == 2)
            def _():
                tile_copy(0).wait()
                pl.when(sends_far)(far_tile.start)

            pl.when(k > n_slot)(lambda: tile_copy(k - n_slot).wait())
            pl.when((k >= n_slot) & (k - n_slot < plan.shared) & jnp.logical_not(busy & (k == n_slot)))(lambda: tile_sent(k - n_slot).wait_send())

        with jax.named_scope("tile"):
            rows = pl.ds(pl.multiple_of(k * plan.rows, plan.rows), plan.rows)
            logit_grad(emb[rows, :], n_all_t, shift, lab_ref, row0 + k * plan.rows, inv_count, scale, dz)
            obuf[slot] = dot(dz[...], nbuf[...].reshape(n_tok, dim)) * scale

        tile_copy(k).start()

    def send_pieces(done, until):
        lax.fori_loop(done, until, lambda p, c: (piece(p).start(), c)[1], 0)
        return jnp.maximum(done, until)

    before = sum(jnp.where(me == s, plan.before[s], 0) for s in range(n_stage))

    def pass_dx0(m, carry):
        @pl.when(jnp.logical_not(first))
        def _():
            remote(dx0buf.at[m], dx0buf.at[m], r_sems.at[0], d_recv.at[m], me).wait_recv()

            @pl.when(hands_on)
            def _():
                remote(dx0buf.at[m], dx0buf.at[m], r_sems.at[0], d_recv.at[m], mate).start()

            @pl.when(relayed(m))
            def _():
                relay_far(m)

            pltpu.make_async_copy(dx0buf.at[m], dx0_out.at[m], out_sem.at[4]).start()

        @pl.when(first)
        def _():
            pltpu.make_async_copy(dxbuf.at[m], dx0_out.at[m], out_sem.at[4]).start()

        return carry

    lead = jnp.where(me == 3, -250, jnp.where(last, -1800, jnp.where(me == far_dst, -1600, -10**6)))

    def work(i, carry):
        sent, passed = carry
        chunk = (i >= before) & (i < before + n_micro)
        pl.when(chunk)(lambda: bwd(i - before))
        k = jnp.where(i < before, i, i - n_micro)
        pl.when(jnp.logical_not(chunk))(lambda: emb_tile(k))
        after = i - before - n_micro + 1
        here = jnp.where(after > 0, jnp.clip((after * 257 + lead) // 146, 0, n_micro), 0)
        lax.fori_loop(passed, here, pass_dx0, 0)
        ready = jnp.where(i < before, i + 1, jnp.where(chunk, before, i + 1 - n_micro)) * plan.per_tile
        near_chunks = chunk | ((i < before) & (i + 1 >= before))
        until = jnp.minimum(jnp.minimum(ready, plan.shared * plan.per_tile), sent + jnp.where(near_chunks, 1, plan.per_tile + 1))
        return send_pieces(sent, until), jnp.maximum(passed, here)

    sent, passed = lax.fori_loop(0, plan.tiles + n_micro, work, (jnp.where(busy, plan.per_tile, 0), 0))
    outs = [pltpu.make_async_copy(nbuf, n_out, out_sem.at[5]), pltpu.make_async_copy(lossall, loss_out, out_sem.at[6]), pltpu.make_async_copy(meta, meta_out, out_sem.at[7])]
    lo_all.wait_recv()
    for c in outs:
        c.start()
    pltpu.make_async_copy(statall, stat_out, out_sem.at[8]).start()
    with jax.named_scope("relay_all"):
        lax.fori_loop(passed, n_micro, pass_dx0, 0)

    with jax.named_scope("drain"):
        send_pieces(sent, plan.shared * plan.per_tile)
        for k in range(max(plan.tiles - n_slot, 0), plan.tiles):
            tile_copy(k).wait()
            if k < plan.shared:
                tile_sent(k).wait_send()
        pl.when(sends_far)(far_tile.wait_send)
        all_rows = pl.ds(0, plan.shared * plan.rows)
        remote(tmp_out.at[1 - core, all_rows], tmp_out.at[1 - core, all_rows], od_send.at[0], od_recv, me).wait_recv()
        sa_all.wait_send()
        lo_all.wait_send()
        pltpu.make_async_copy(statall, stat_out, out_sem.at[8]).wait()
        for c, p in zip(ag_copies, peers):
            pl.when(p != last_id)(c.wait_send)

        @pl.when(jnp.logical_not(last))
        def _():
            dn_copy.wait_send()
            pl.when(mate != last_id)(n_forward.wait_send)
            remote(ybuf, xbuf, f_send, f_recv.at[0], me + 1).wait_send()

        @pl.when(last)
        def _():
            remote(nbuf, nbuf, n_send, n_recv.at[0], me).wait_send()

        @pl.when(mate != last_id)
        def _():
            some = nbuf.at[pl.ds(0, len(peers))]
            remote(some, some, fw_send, ag_recv.at[0], mate).wait_send()

        @pl.when(jnp.logical_not(first) & (me + 2 < n_micro))
        def _():
            x_copy(0).wait_send()

            @pl.when(me < 2)
            def _():
                x_copy(1).wait_send()

        @pl.when(jnp.logical_not(first))
        def _():
            remote(dxbuf, gbuf, b_send, b_recv.at[0], me).wait_send()
            pl.when(hands_on)(remote(dx0buf, dx0buf, r_sems.at[0], d_recv.at[0], mate).wait_send)

        @pl.when(first)
        def _():
            for k in range(len(near_dst)):
                remote(dxbuf, dx0buf, d_send.at[k], d_recv.at[0], me).wait_send()
            rest = pl.ds(0, n_micro - direct)
            remote(dxbuf.at[rest], dx0buf.at[rest], d_send.at[len(near_dst)], d_recv.at[0], me).wait_send()

        for dev, kept in ((3, by_next), (last_id, by_prev)):
            some = dx0buf.at[pl.ds(0, len(kept))]
            pl.when(me == dev)(remote(some, some, r_sems.at[1], d_recv.at[0], me).wait_send)

        pltpu.make_async_copy(hbuf, hid_out, out_sem.at[0]).wait()
        pltpu.make_async_copy(xbuf, xs_out, out_sem.at[1]).wait()
        pltpu.make_async_copy(abuf, da_out, out_sem.at[2]).wait()
        pltpu.make_async_copy(gbuf, g_out, out_sem.at[3]).wait()
        pltpu.make_async_copy(dx0buf, dx0_out, out_sem.at[4]).wait()
        for c in outs:
            c.wait()


class Plan:
    def __init__(self, vocab, n_stage):
        units = vocab // LANES
        self.base = units // 2 * LANES
        self.extra = vocab - 2 * self.base
        self.head_tile = next(t for t in (1600, 1536, 1280, 1024, 768, 640, 512, 256, 128) if self.base % t == 0)
        self.rows = 1024
        self.tiles, self.shared = 10, 8
        self.grad_tile = next(t for t in (4000, 3200, 1600, 1280, 640, 256, 128) if self.base % t == 0)
        self.e_parts = next(k for k in (10, 8, 5, 4, 2, 1) if self.base % (16 * k) == 0)
        self.part = 128
        self.slots = 4
        self.piece = 256
        self.per_tile = self.rows // self.piece
        measured = [10, 9, 6, 5, 3, 2, 0, 0]
        self.before = (measured + [0] * n_stage)[:n_stage]
        mid = self.base + self.extra
        ends = [(0, mid), (mid, vocab)]
        early = (self.tiles * self.rows, self.shared * self.rows)
        self.spans = [[(ends[h][0] + early[0 if h == c else 1], ends[h][1]) for h in (c, 1 - c)] for c in range(2)]
        self.longest = [max(self.spans[c][k][1] - self.spans[c][k][0] for c in range(2)) for k in range(2)]
        best = min(range(16, 1281, 16), key=lambda r: (sum(-(-n // r) for n in self.longest)) * (r + 40))
        self.calc_rows = best
        self.calc_steps = [-(-n // best) for n in self.longest]
        self.steps = sum(self.calc_steps)
        self.copy_rows = self.rows
        self.copies = self.tiles + self.shared
        self.starts = ends

    def calc_start(self, core, s):
        k = 0 if s < self.calc_steps[0] else 1
        lo, hi = self.spans[core][k]
        return min(lo + (s - k * self.calc_steps[0]) * self.calc_rows, hi - self.calc_rows)

    def copy_start(self, core, c):
        own = c < self.tiles
        h = core if own else 1 - core
        return self.starts[h][0] + (c if own else c - self.tiles) * self.copy_rows

    def cuts(self, core):
        firsts = [(self.calc_start(core, s), self.calc_rows) for s in range(self.steps)] + [(self.copy_start(core, c), self.copy_rows) for c in range(self.copies)]
        flat = [v for lo, rows in firsts for v in (lo, lo + rows)]
        return flat + [0] * (LANES - len(flat))


def run_pipe(x0, emb, w_up, w_down, labels, tokens, cuts, n_stage, plan):
    n_micro, seq = labels.shape
    dim, ffn = w_up.shape
    n_tok = n_micro * seq
    base = plan.base
    any_spec = pl.BlockSpec(memory_space=pl.ANY)
    act = (n_micro, seq, dim)
    fine = (n_tok // plan.part, plan.part, dim)
    wide = (n_micro, seq, ffn)
    dma = pltpu.SemaphoreType.DMA
    vm = pltpu.VMEM
    pair = 2 * seq
    return pl.pallas_call(
        functools.partial(pipe_kernel, n_stage, plan),
        out_shape=[
            jax.ShapeDtypeStruct(act, BF16), jax.ShapeDtypeStruct(fine, BF16), jax.ShapeDtypeStruct(wide, BF16),
            jax.ShapeDtypeStruct(wide, BF16), jax.ShapeDtypeStruct(act, BF16), jax.ShapeDtypeStruct(act, BF16),
            jax.ShapeDtypeStruct((n_stage, 8, pair), F32), jax.ShapeDtypeStruct((n_stage, 8, pair), F32), jax.ShapeDtypeStruct((2, plan.tiles * plan.rows, dim), F32),
            jax.ShapeDtypeStruct((3 * n_tok // LANES, LANES), jnp.int32),
        ],
        in_specs=[any_spec] * 4 + [pl.BlockSpec(memory_space=pltpu.VMEM)] * 3,
        out_specs=[any_spec] * 10,
        scratch_shapes=[
            vm(fine, BF16), vm(fine, BF16), vm(wide, BF16), vm(wide, BF16), vm(act, BF16), vm(act, BF16), vm(act, BF16), vm(act, BF16), vm(act, BF16),
            vm((dim, ffn), BF16), vm((ffn, dim), BF16), vm((ffn, dim), BF16), vm((dim, ffn), BF16),
            vm((base + plan.extra, dim), BF16), vm((base + plan.extra, pair), BF16), vm((dim, pair), BF16), vm((pair, dim), F32),
            vm((seq, dim), F32), vm((seq, dim), F32), vm((seq, dim), BF16), vm((16, pair), F32), vm((16, pair), F32), vm((n_stage, 8, pair), F32), vm((n_stage, 8, pair), F32),
            vm((2, 8, pair), F32), vm((dim, n_tok), BF16), vm((1, n_tok), F32), vm((plan.rows, n_tok), BF16), vm((plan.slots, plan.rows, dim), F32),
            vm((2, plan.head_tile, pair), BF16), vm((3 * n_tok // LANES, LANES), jnp.int32),
            dma((2,)), dma((2,)), dma((2,)), dma((2,)), dma((n_micro,)), dma, dma((n_tok // plan.part,)), dma, dma((n_micro,)), dma,
            dma((n_stage // 2,)), dma((n_micro,)), dma,
            dma((2,)), dma((2,)), dma, dma((n_stage,)), dma((2,)), dma((2,)), dma, dma((n_micro,)), dma((4,)), dma((n_micro,)), dma((2,)), dma((9,)),
            dma((plan.slots,)), dma((plan.shared,)), dma, dma,
        ],
        compiler_params=pltpu.CompilerParams(collective_id=0, has_side_effects=True, vmem_limit_bytes=67_000_000),
        cost_estimate=pl.CostEstimate(flops=60 * 10**9, bytes_accessed=100 * 10**6, transcendentals=0),
        name="pipe",
    )(x0.reshape(x0.shape[0], seq // plan.part, plan.part, dim), emb, w_up, w_down, labels.reshape(1, n_tok), tokens.reshape(1, n_tok), cuts)


def fin_kernel(n_stage, n_tok, plan, ids_ref, emb_hbm, tmp_hbm, n_hbm, stat_ref, part_ref, lab_ref, meta_ref, dx0_hbm, xs_hbm, hid_hbm, da_hbm, g_hbm,
               out_hbm, loss_ref, gup_hbm, gdown_hbm,
               n_all, dx0, xs, hid, da, g, n_t, x_t, dx0s, dz, shift, e_in, c_out, cp, gup, gdown,
               ld_sem, e_sem, t_sem, co_sem, po_sem, gu_sem, gd_sem, wi_sem):
    dim, ffn = gup_hbm.shape
    scale = dim ** -0.5
    inv_count = 1.0 / n_tok
    steps, crows, prows = plan.steps, plan.calc_rows, plan.copy_rows
    core = lax.rem(lax.axis_index("stage"), 2)
    early = plan.tiles * prows
    wblk = gup.shape[2]
    n_wblk = ffn // wblk
    turn = plan.calc_steps[0]

    def pick(pair):
        return jnp.where(core == 0, pair[0], pair[1])

    def calc_start(s):
        own = s < turn
        lo, hi = [jnp.where(own, pick([plan.spans[c][0][e] for c in range(2)]), pick([plan.spans[c][1][e] for c in range(2)])) for e in range(2)]
        return pl.multiple_of(jnp.minimum(lo + (s - jnp.where(own, 0, turn)) * crows, hi - crows), 16)

    def copy_start(c):
        own = c < plan.tiles
        first = jnp.where(own, pick([plan.starts[0][0], plan.starts[1][0]]), pick([plan.starts[1][0], plan.starts[0][0]]))
        return pl.multiple_of(first + (c - jnp.where(own, 0, plan.tiles)) * prows, 16)

    def e_copy(s):
        return pltpu.make_async_copy(emb_hbm.at[pl.ds(calc_start(s), crows)], e_in.at[lax.rem(s, 2)], e_sem.at[lax.rem(s, 2)])

    n_slot = cp.shape[0]
    ahead = 3

    def t_copy(c):
        own = c < plan.tiles
        row = jnp.where(own, core, 1 - core) * early + (c - jnp.where(own, 0, plan.tiles)) * prows
        slot = lax.rem(c, n_slot)
        return pltpu.make_async_copy(tmp_hbm.at[pl.ds(pl.multiple_of(row, 16), prows)], cp.at[slot], t_sem.at[slot])

    def p_out(c):
        slot = lax.rem(c, n_slot)
        return pltpu.make_async_copy(cp.at[slot], out_hbm.at[pl.ds(copy_start(c), prows)], po_sem.at[slot])

    def c_outs(s):
        slot = lax.rem(s, 2)
        return pltpu.make_async_copy(c_out.at[slot], out_hbm.at[pl.ds(calc_start(s), crows)], co_sem.at[slot])

    loads = [pltpu.make_async_copy(s, d, ld_sem.at[i]) for i, (s, d) in enumerate(((n_hbm, n_all), (dx0_hbm, dx0), (xs_hbm, xs), (g_hbm, g)))]
    loads[0].start()
    loads[1].start()
    e_copy(0).start()
    for c in range(ahead):
        t_copy(c).start(priority=1)
    pair = stat_ref.shape[2]
    loss = jnp.zeros((1, pair), F32)
    for d in range(n_stage):
        if d % 2 == 0:
            shift[:, (d // 2) * pair:(d // 2 + 1) * pair] = stat_ref[d, 0:1, :] * LOG2E + math.log2(n_tok)
        loss = loss + part_ref[d, 0:1, :]
    loss_ref[0] = jnp.sum(loss) * inv_count
    with jax.named_scope("fin_pre"):
        loads[0].wait()
        n_t[...] = n_all[...].T

    def sum_rows():
        loads[1].wait()
        dense = jnp.concatenate([meta_ref[g:g + 1, :] for g in range(n_tok // LANES)], axis=1)
        order = lax.broadcasted_iota(jnp.int32, (n_tok, n_tok), 0) == dense
        dx0s[...] = dot(jnp.where(order, 1.0, 0.0).astype(BF16), dx0[...])

    def add_rows(k, start, ref):
        lo, hi = ids_ref[2 * n_tok + k], ids_ref[2 * n_tok + k + 1]
        wide = 8

        def some(p, width):
            at = [pl.ds(ids_ref[n_tok + p + u] - start, 1) for u in range(width)]
            new = [ref[at[u], :] + dx0s[pl.ds(p + u, 1), :] for u in range(width)]
            for u in range(width):
                ref[at[u], :] = new[u]

        def group(g, carry):
            some(lo + g * wide, wide)
            return carry

        def single(p, carry):
            some(p, 1)
            return carry

        n_grp = (hi - lo) // wide
        lax.fori_loop(0, n_grp, group, 0)
        lax.fori_loop(lo + n_grp * wide, hi, single, 0)

    def w_ins(w):
        cols = pl.ds(pl.multiple_of(w * wblk, wblk), wblk)
        wslot = lax.rem(w, 2)
        return (pltpu.make_async_copy(da_hbm.at[:, cols], da.at[wslot], wi_sem.at[0, wslot]), pltpu.make_async_copy(hid_hbm.at[:, cols], hid.at[wslot], wi_sem.at[1, wslot]))

    def w_outs(w):
        cols = pl.ds(pl.multiple_of(w * wblk, wblk), wblk)
        wslot = lax.rem(w, 2)
        return (pltpu.make_async_copy(gup.at[wslot], gup_hbm.at[:, cols], gu_sem.at[wslot]), pltpu.make_async_copy(gdown.at[wslot], gdown_hbm.at[cols], gd_sem.at[wslot]))

    def copy_tile(c, carry):
        with jax.named_scope("copy_wait"):
            t_copy(c).wait()
        with jax.named_scope("add_p"):
            add_rows(2 * steps + 2 * c, copy_start(c), cp.at[lax.rem(c, n_slot)])
        p_out(c).start()

        @pl.when(c + ahead < plan.copies)
        def _():
            pl.when(c + ahead >= n_slot)(lambda: p_out(c + ahead - n_slot).wait())
            t_copy(c + ahead).start(priority=1)

        return carry

    w_first = 2
    tails = [turn - 1, steps - 1]

    def tail(s):
        return (s == tails[0]) | (s == tails[1])

    def step(s, carry):
        pl.when(s + 1 < steps)(lambda: e_copy(s + 1).start())
        with jax.named_scope("fin_wait"):
            e_copy(s).wait()

        @pl.when(s == 0)
        def _():
            for c in loads[2:]:
                c.start()

        w = s - w_first

        @pl.when((w + 1 >= 0) & (w + 1 < n_wblk))
        def _():
            for c in w_ins(w + 1):
                c.start()

        pl.when((s >= 2) & jnp.logical_not(tail(s - 1)))(lambda: c_outs(s - 2).wait())
        slot = lax.rem(s, 2)
        start = calc_start(s)
        with jax.named_scope("calc"):
            logit_grad(e_in[slot], n_t, shift, lab_ref, start, inv_count, scale, dz)
            c_out[slot] = dot(dz[...], n_all[...]) * scale
        pl.when(s == 0)(sum_rows)
        with jax.named_scope("add_c"):
            add_rows(2 * s, start, c_out.at[slot])
        pl.when(tail(s))(lambda: c_outs(s - 1).wait())
        c_outs(s).start()
        lax.fori_loop(s * plan.copies // (steps - 1), jnp.minimum((s + 1) * plan.copies // (steps - 1), plan.copies), copy_tile, 0)

        @pl.when(w == 0)
        def _():
            for c in loads[2:]:
                c.wait()
            x_t[...] = xs[...].T

        @pl.when((w >= 0) & (w < n_wblk))
        def _():
            wslot = lax.rem(w, 2)
            with jax.named_scope("dw_wait"):
                for c in w_ins(w):
                    c.wait()

                @pl.when(w >= 2)
                def _():
                    for c in w_outs(w - 2):
                        c.wait()

            with jax.named_scope("dw"):
                gup[wslot] = dot(x_t[...], da[wslot])
                gdown[wslot] = dot_t(hid[wslot], g[...])
            for c in w_outs(w):
                c.start()

        return carry

    lax.fori_loop(0, steps, step, 0)
    with jax.named_scope("fin_drain"):
        for w in range(n_wblk - 2, n_wblk):
            for c in w_outs(w):
                c.wait()
        c_outs(steps - 1).wait()
        for c in range(plan.copies - n_slot, plan.copies):
            p_out(c).wait()


def run_fin(emb, tmp, n_all, stats, losses, labels, meta, dx0, xs, hid, da, g, n_stage, plan):
    vocab, dim = emb.shape
    n_tok, ffn = hid.shape
    vm = pltpu.VMEM
    dma = pltpu.SemaphoreType.DMA
    any_spec = pl.BlockSpec(memory_space=pl.ANY)
    vspec = pl.BlockSpec(memory_space=pltpu.VMEM)
    smem = pl.BlockSpec(memory_space=pltpu.SMEM)
    wblk = 512
    return pl.pallas_call(
        functools.partial(fin_kernel, n_stage, n_tok, plan),
        out_shape=[jax.ShapeDtypeStruct((vocab, dim), F32), jax.ShapeDtypeStruct((1,), F32), jax.ShapeDtypeStruct((dim, ffn), F32), jax.ShapeDtypeStruct((ffn, dim), F32)],
        in_specs=[smem, any_spec, any_spec, any_spec, vspec, vspec, vspec, vspec] + [any_spec] * 5,
        out_specs=[any_spec, smem, any_spec, any_spec],
        scratch_shapes=[
            vm((n_tok, dim), BF16), vm((n_tok, dim), BF16), vm((n_tok, dim), BF16), vm((2, n_tok, wblk), BF16), vm((2, n_tok, wblk), BF16), vm((n_tok, dim), BF16),
            vm((dim, n_tok), BF16), vm((dim, n_tok), BF16), vm((n_tok, dim), F32), vm((plan.calc_rows, n_tok), BF16), vm((1, n_tok), F32),
            vm((2, plan.calc_rows, dim), BF16), vm((2, plan.calc_rows, dim), F32), vm((5, plan.copy_rows, dim), F32),
            vm((2, dim, wblk), F32), vm((2, wblk, dim), F32),
            dma((4,)), dma((2,)), dma((5,)), dma((2,)), dma((5,)), dma((2,)), dma((2,)), dma((2, 2)),
        ],
        compiler_params=pltpu.CompilerParams(vmem_limit_bytes=67_000_000),
        cost_estimate=pl.CostEstimate(flops=2 * n_tok * vocab * dim, bytes_accessed=5 * vocab * dim, transcendentals=0),
        name="fin",
    )(meta.reshape(-1), emb, tmp, n_all, stats, losses, labels.reshape(1, n_tok), meta, dx0, xs, hid, da, g)


def solution(mesh):
    n_stage = mesh.shape["stage"]

    def device_fn(tokens, labels, emb, w_up, w_down):
        n_micro, seq = tokens.shape
        vocab, dim = emb.shape
        w_up, w_down = w_up[0], w_down[0]
        n_tok = n_micro * seq
        plan = Plan(vocab, n_stage)
        cuts = jnp.array([plan.cuts(0), plan.cuts(1)], jnp.int32)
        x0 = run_gather(tokens, emb)
        n_all, xs, hid, da, g, dx0, stats, losses, tmp, meta = run_pipe(x0, emb, w_up, w_down, labels, tokens, cuts, n_stage, plan)
        flat = lambda p: p.reshape(n_tok, -1)
        grad_emb, loss, grad_up, grad_down = run_fin(
            emb, tmp.reshape(-1, dim), flat(n_all), stats, losses, labels, meta, flat(dx0), flat(xs), flat(hid), flat(da), flat(g), n_stage, plan
        )
        return loss, grad_up[None], grad_down[None], grad_emb

    return jax.shard_map(device_fn, mesh=mesh, in_specs=(P("dp", None), P("dp", None), P(None, None), P("stage", None, None), P("stage", None, None)), out_specs=(P("dp"), P(("dp", "stage"), None, None), P(("dp", "stage"), None, None), P("dp", None)), check_vma=False)
```

```python
import functools
import math

import jax
import jax.numpy as jnp
from jax import lax
from jax.experimental import pallas as pl
from jax.experimental.pallas import tpu as pltpu
from jax.sharding import PartitionSpec as P


MESH = pl.DeviceIdType.MESH
LOG2E = math.log2(math.e)
LN2 = math.log(2.0)
GELU_C = math.sqrt(2.0 / math.pi)
GELU_K = 0.044715
EPS = 1e-6
LANES = 128
F32 = jnp.float32
BF16 = jnp.bfloat16


def gelu_fwd(a):
    return (0.5 * a) * (1.0 + jnp.tanh(a * (GELU_C + (GELU_C * GELU_K) * (a * a))))


def gelu_slope(a):
    a2 = a * a
    half = 0.5 * jnp.tanh(a * (GELU_C + (GELU_C * GELU_K) * a2))
    up, down = 0.5 + half, 0.5 - half
    return up + (up * down) * (a * (2.0 * GELU_C + (6.0 * GELU_C * GELU_K) * a2))


def dot(x, y):
    return jnp.dot(x, y, preferred_element_type=F32)


def dot_t(x, y):
    return lax.dot_general(x, y, (((0,), (0,)), ((), ())), preferred_element_type=F32)


def remote(src, dst, send_sem, recv_sem, dev):
    return pltpu.make_async_remote_copy(src_ref=src, dst_ref=dst, send_sem=send_sem, recv_sem=recv_sem, device_id={"stage": dev}, device_id_type=MESH)


def column(row):
    return jnp.broadcast_to(row, (LANES, LANES)).T


def gather_kernel(ids_ref, tok_ref, emb_hbm, x0_hbm, tiles, picked, sem, out_sem):
    n_micro, seq = tok_ref.shape
    me = lax.axis_index("stage")
    group = tiles.shape[1] // seq
    slots = tiles.shape[0]
    owners = [head_chunk(me, k, n_micro) for k in range(slots)]

    def fetch(k):
        def one(i, carry):
            t = ids_ref[owners[k] * seq + i]
            start = pl.multiple_of(t // group * group, group)
            pltpu.make_async_copy(emb_hbm.at[pl.ds(start, group)], tiles.at[k, pl.ds(pl.multiple_of(i * group, group), group)], sem.at[k]).start()
            return carry

        lax.fori_loop(0, seq, one, 0, unroll=8)

    def select(k):
        sub = lax.broadcasted_iota(jnp.int32, (LANES, LANES), 0)
        lane = lax.broadcasted_iota(jnp.int32, (LANES, LANES), 1)
        tok = column(tok_ref[pl.ds(owners[k], 1), :].astype(F32)).astype(jnp.int32)
        want = sub * group + (tok - tok // group * group)
        hot = jnp.concatenate([jnp.where(lane + b * LANES == want, 1.0, 0.0).astype(BF16) for b in range(seq * group // LANES)], axis=1)
        pltpu.make_async_copy(emb_hbm.at[pl.ds(0, seq * group)], tiles.at[k], sem.at[k]).wait()
        picked[k] = dot(hot, tiles[k]).astype(BF16)
        pltpu.make_async_copy(picked.at[k], x0_hbm.at[k], out_sem.at[k]).start()

    def finish(k):
        pltpu.make_async_copy(picked.at[k], x0_hbm.at[k], out_sem.at[k]).wait()

    for work in (fetch, select, finish):
        work(0)
        for k in range(1, slots):
            pl.when(me < slots)(functools.partial(work, k))


def head_chunk(dev, k, n_micro):
    return jnp.minimum(jnp.where(dev < 2, 2 * dev + k, dev + 2), n_micro - 1)


def run_gather(tokens, emb):
    n_micro, seq = tokens.shape
    dim = emb.shape[1]
    group = 16
    return pl.pallas_call(
        gather_kernel,
        out_shape=jax.ShapeDtypeStruct((2, seq, dim), BF16),
        in_specs=[pl.BlockSpec(memory_space=pltpu.SMEM), pl.BlockSpec(memory_space=pltpu.VMEM), pl.BlockSpec(memory_space=pl.ANY)],
        out_specs=pl.BlockSpec(memory_space=pl.ANY),
        scratch_shapes=[pltpu.VMEM((2, seq * group, dim), BF16), pltpu.VMEM((2, seq, dim), BF16), pltpu.SemaphoreType.DMA((2,)), pltpu.SemaphoreType.DMA((2,))],
        cost_estimate=pl.CostEstimate(flops=10**9, bytes_accessed=2 * seq * group * dim * 2, transcendentals=0),
        name="gather",
    )(tokens.reshape(n_micro * seq), tokens, emb)


def token_table(row_ref, cut_ref, meta):
    n_tok = row_ref.shape[1]
    n_grp = n_tok // LANES
    lane = lax.broadcasted_iota(jnp.int32, (LANES, LANES), 1).astype(F32)
    sub = lax.broadcasted_iota(jnp.int32, (LANES, LANES), 0)
    row = lambda g: row_ref[:, g * LANES:(g + 1) * LANES].astype(F32)
    zero = jnp.zeros((LANES, LANES), F32)
    fold = lambda acc: jnp.sum(acc, axis=0, keepdims=True)
    cols = [column(row(c)) for c in range(n_grp)]
    firsts = []
    for g in range(n_grp):
        acc = zero
        for c in range(g + 1):
            same = cols[c] == row(g)
            if c == g:
                same = same & (sub < lane.astype(jnp.int32))
            acc = acc + jnp.where(same, 1.0, 0.0)
        firsts.append(column(jnp.where(fold(acc) == 0.0, 1.0, 0.0)))
    ranks = []
    for g in range(n_grp):
        acc = zero
        for c in range(n_grp):
            acc = acc + jnp.where(cols[c] < row(g), firsts[c], 0.0)
        ranks.append(fold(acc))
        meta[g:g + 1, :] = ranks[g].astype(jnp.int32)
    rank_cols = [column(r) for r in ranks]
    for g in range(n_grp):
        acc = zero
        for c in range(n_grp):
            acc = acc + jnp.where(rank_cols[c] == lane + g * LANES, firsts[c] * cols[c], 0.0)
        meta[n_grp + g:n_grp + g + 1, :] = fold(acc).astype(jnp.int32)
    cut = cut_ref[...].astype(F32)
    acc = zero
    for c in range(n_grp):
        acc = acc + jnp.where(cols[c] < cut, firsts[c], 0.0)
    meta[2 * n_grp:3 * n_grp, :] = jnp.broadcast_to(fold(acc), (n_grp, LANES)).astype(jnp.int32)


def logit_grad(e, n_t, shift, lab, first_id, inv_count, scale, dz):
    rows = e.shape[0]
    n_tok = n_t.shape[1]
    blk = 256
    vid = lax.broadcasted_iota(jnp.int32, (rows, blk), 0)
    for j in range(n_tok // blk):
        cols = slice(j * blk, (j + 1) * blk)
        z = (dot(e, n_t[:, cols]) * scale).astype(BF16).astype(F32)
        prob = jnp.exp2(z * LOG2E - shift[:, cols])
        dz[:, cols] = jnp.where(vid == lab[:, cols] - first_id, prob - inv_count, prob).astype(BF16)


def pipe_kernel(n_stage, plan, x0_hbm, emb_hbm, up_hbm, down_hbm, lab_ref, row_ref, cut_ref,
                n_out, xs_out, hid_out, da_out, g_out, dx0_out, stat_out, loss_out, tmp_out, meta_out,
                xbuf, ybuf, abuf, hbuf, nbuf, gbuf, dxbuf, dx0buf, dnbuf, up, down, up_t, down_t,
                emb, zbuf, n_t, dn_acc, dn_send, dn_recv, dn_own, st_send, st_recv, statall, lossall, tops, n_all_t, shift, dz, obuf, z_pair, meta,
                w_sem, e_sem, x_sem, x_send, x_recv, f_send, f_recv, n_send, n_recv, nf_send, ag_send, ag_recv, fw_send,
                st_sems, dp_sems, dn_ssem, dn_rsem, sa_sems, lo_sems, b_send, b_recv, d_send, d_recv, r_sems, out_sem, o_sem, od_send, od_recv, ic_send):
    n_micro, seq, dim = gbuf.shape
    part = xbuf.shape[1]
    n_part = xbuf.shape[0]
    per = seq // part
    n_tok = n_micro * seq
    ffn = up.shape[1]
    vocab = emb_hbm.shape[0]
    me = lax.axis_index("stage")
    core = lax.rem(me, 2)
    chip = me // 2
    mate = me + 1 - 2 * core
    last_id = n_stage - 1
    first = me == 0
    last = me == last_id
    fblk = 512
    n_fblk = ffn // fblk
    base, extra, tile = plan.base, plan.extra, plan.head_tile
    row0 = core * (base + extra)
    n_tiles = base // tile
    wide_tile = plan.grad_tile

    barrier = pltpu.get_barrier_semaphore()
    for d in range(1, n_stage):
        pl.semaphore_signal(barrier, inc=1, device_id={"stage": lax.rem(me + d, n_stage)}, device_id_type=MESH)
    w_copy = [pltpu.make_async_copy(up_hbm, up, w_sem.at[0]), pltpu.make_async_copy(down_hbm, down, w_sem.at[1])]
    for c in w_copy:
        c.start()
    x_slots = x0_hbm.shape[0]
    x_mine = [head_chunk(me, k, n_micro) for k in range(x_slots)]

    def x_rows(m):
        return xbuf.at[pl.ds(m * per, per)]

    def x_local(k):
        return pltpu.make_async_copy(x0_hbm.at[k], x_rows(k), x_sem.at[k])

    @pl.when(first)
    def _():
        for k in range(x_slots):
            x_local(k).start()

    e_parts = plan.e_parts
    e_step = base // e_parts

    def e_copy(i):
        src = emb_hbm.at[pl.ds(pl.multiple_of(row0 + i * e_step, 16), e_step)]
        return pltpu.make_async_copy(src, emb.at[pl.ds(i * e_step, e_step)], e_sem.at[0])

    e_more = pltpu.make_async_copy(emb_hbm.at[pl.ds(base, extra)], emb.at[pl.ds(base, extra)], e_sem.at[1])
    with jax.named_scope("entry"):
        pl.semaphore_wait(barrier, n_stage - 1)

    def x_copy(k):
        return remote(x0_hbm.at[k], x_rows(x_mine[k]), x_send.at[k], x_recv.at[x_mine[k]], 0)

    @pl.when(jnp.logical_not(first) & (me + 2 < n_micro))
    def _():
        x_copy(0).start()

        @pl.when(me < 2)
        def _():
            x_copy(1).start()

    with jax.named_scope("w_wait"):
        for c in w_copy:
            c.wait()
        for i in range(e_parts):
            e_copy(i).start()
        pl.when(core == 0)(e_more.start)

    def transpose_weights():
        for j in range(n_fblk):
            up_t[j * fblk:(j + 1) * fblk, :] = up[:, j * fblk:(j + 1) * fblk].T
            down_t[:, j * fblk:(j + 1) * fblk] = down[j * fblk:(j + 1) * fblk, :].T

    def idle_work():
        transpose_weights()
        token_table(row_ref, jnp.where(core == 0, cut_ref[0:1, :], cut_ref[1:2, :]), meta)

    @pl.when(chip >= n_stage // 4)
    def _():
        idle_work()

    def n_start(m):
        remote(nbuf.at[m], nbuf.at[m], n_send, n_recv.at[m], jnp.where(m == last_id, last_id - 1, m)).start()

    def fwd(h, carry):
        m = h // per
        sub = lax.rem(h, per)
        rows = pl.ds(pl.multiple_of(sub * part, part), part)
        with jax.named_scope("fwd_wait"):

            @pl.when(first & (sub == 0))
            def _():
                @pl.when(m < x_slots)
                def _():
                    x_local(m).wait()

                @pl.when(m >= x_slots)
                def _():
                    remote(x_rows(m), x_rows(m), x_send.at[0], x_recv.at[m], me).wait_recv()

            @pl.when(jnp.logical_not(first))
            def _():
                remote(xbuf.at[h], xbuf.at[h], f_send, f_recv.at[h], me).wait_recv()

        with jax.named_scope("fwd_comp"):
            x = xbuf[h]
            for j in range(n_fblk):
                cols = slice(j * fblk, (j + 1) * fblk)
                a = dot(x, up[:, cols]).astype(BF16)
                abuf[m, rows, cols] = a
                hbuf[m, rows, cols] = gelu_fwd(a.astype(F32)).astype(BF16)
            y = (x.astype(F32) + dot(hbuf[m, rows, :], down[...])).astype(BF16)
            ybuf[h] = y

        @pl.when(jnp.logical_not(last))
        def _():
            remote(ybuf.at[h], xbuf.at[h], f_send, f_recv.at[h], me + 1).start()

        @pl.when(last)
        def _():
            yf = y.astype(F32)
            inv = lax.rsqrt(jnp.mean(yf * yf, axis=-1, keepdims=True) + EPS)
            nbuf[m, rows, :] = (yf * inv).astype(BF16)
            pl.when(sub == per - 1)(lambda: n_start(m))

        @pl.when(sub == per - 1)
        def _():
            pltpu.make_async_copy(hbuf.at[m], hid_out.at[m], out_sem.at[0]).start()
            pltpu.make_async_copy(x_rows(m), xs_out.at[pl.ds(m * per, per)], out_sem.at[1]).start()

        return carry

    lax.fori_loop(0, n_part, fwd, 0)

    @pl.when(chip < n_stage // 4)
    def _():
        idle_work()

    n_forward = remote(nbuf.at[me], nbuf.at[me], nf_send, n_recv.at[me], mate)
    with jax.named_scope("n_wait"):

        @pl.when(jnp.logical_not(last))
        def _():
            remote(nbuf.at[me], nbuf.at[me], n_send, n_recv.at[me], me).wait_recv()
            pl.when(mate != last_id)(n_forward.start)
            remote(nbuf.at[mate], nbuf.at[mate], n_send, n_recv.at[mate], me).wait_recv()

        for k in range(2):
            n_t[:, k * seq:(k + 1) * seq] = nbuf[2 * chip + k].T

    peers = [lax.rem(me + 2 * d, n_stage) for d in range(1, n_stage // 2)]
    ag_copies = [remote(nbuf.at[me], nbuf.at[me], ag_send.at[d], ag_recv.at[me], p) for d, p in enumerate(peers)]
    for c, p in zip(ag_copies, peers):
        pl.when(p != last_id)(c.start)
    with jax.named_scope("e_wait"):
        pltpu.make_async_copy(emb_hbm.at[pl.ds(0, base)], emb.at[pl.ds(0, base)], e_sem.at[0]).wait()
        pl.when(core == 0)(e_more.wait)

    pair = 2 * seq
    scale = dim ** -0.5
    inv_count = 1.0 / n_tok
    log_count = math.log2(n_tok)
    lab = lab_ref[:, pl.ds(pl.multiple_of(chip * pair, pair), pair)]

    def logits(rows, size):
        e = emb[rows, :]
        parts = [dot(e[k * size // 2:(k + 1) * size // 2], n_t[...]) for k in range(2)]
        z = jnp.concatenate([(p * scale).astype(BF16) for p in parts], axis=0)
        zbuf[rows, :] = z
        return z

    def peak(z, size, top):
        best = jnp.max(z.reshape(size // 16, 16, pair), axis=0).astype(F32)
        return jnp.maximum(top, jnp.maximum(best[:8], best[8:]))

    def total(z, size, old, top, tot):
        off = top * LOG2E
        return tot * jnp.exp2(old * LOG2E - off) + jnp.sum(jnp.exp2(z.astype(F32).reshape(size // 8, 8, pair) * LOG2E - off[None]), axis=0)

    tops[0] = jnp.full((8, pair), -jnp.inf, F32)
    tops[1] = jnp.zeros((8, pair), F32)

    @pl.when(core == 0)
    def _():
        z = logits(pl.ds(base, extra), extra)
        top = peak(z, extra, tops[0])
        tops[1] = total(z, extra, tops[0], top, tops[1])
        tops[0] = top

    def logits_step(i, slot, old, top, tot):
        z = logits(pl.ds(pl.multiple_of(i * tile, 16), tile), tile)
        tot = total(z_pair[1 - slot], tile, old, top, tot)
        z_pair[slot] = z
        return top, peak(z, tile, top), tot

    with jax.named_scope("logits"):
        z = logits(pl.ds(0, tile), tile)
        z_pair[0] = z
        state = (tops[0], peak(z, tile, tops[0]), tops[1])
        state = lax.fori_loop(0, (n_tiles - 1) // 2, lambda i, c: logits_step(2 * i + 2, 0, *logits_step(2 * i + 1, 1, *c)), state)
        if n_tiles % 2 == 0:
            state = logits_step(n_tiles - 1, 1, *state)
        old, top, tot = state
        tot = total(z_pair[(n_tiles - 1) % 2], tile, old, top, tot)
    row_top = jnp.max(top, axis=0, keepdims=True)
    row_tot = jnp.sum(tot * jnp.exp2((top - row_top) * LOG2E), axis=0, keepdims=True)
    st_send[0:8, :] = jnp.broadcast_to(row_top, (8, pair))
    st_send[8:16, :] = jnp.broadcast_to(row_tot, (8, pair))
    st_copy = remote(st_send, st_recv, st_sems.at[0], st_sems.at[1], mate)
    with jax.named_scope("stat_x"):
        st_copy.start()
        st_copy.wait()
    far_top = st_recv[0:1, :]
    far_tot = st_recv[8:9, :]
    all_top = jnp.maximum(row_top, far_top)
    mine = row_tot * jnp.exp(row_top - all_top)
    other = far_tot * jnp.exp(far_top - all_top)
    lse = all_top + jnp.log(jnp.where(core == 0, mine + other, other + mine))
    my_shift = lse * LOG2E + log_count
    others = [lax.rem(me + d, n_stage) for d in range(1, n_stage)]

    def spread(buf, sems):
        whole = buf.at[pl.ds(0, n_stage - 1)]
        return [remote(buf.at[me], buf.at[me], sems.at[0], sems.at[1], p) for p in others], remote(whole, whole, sems.at[0], sems.at[1], me)

    statall[me] = jnp.broadcast_to(lse, (8, pair))
    sa_copies, sa_all = spread(statall, sa_sems)
    for c in sa_copies:
        c.start()

    def grads(rows, size, first_row, picked):
        zf = zbuf[rows, :].astype(F32)
        prob = jnp.exp2(zf * LOG2E - my_shift)
        hit = lax.broadcasted_iota(jnp.int32, (size, pair), 0) == lab - (row0 + first_row)
        dz_t = jnp.where(hit, prob - inv_count, prob).astype(BF16)
        got = jnp.where(hit, zf, 0.0).reshape(size // 8, 8, pair)
        return dot_t(dz_t, emb[rows, :]), picked + jnp.sum(got, axis=0)

    tops[0] = jnp.zeros((8, pair), F32)
    dn_acc[...] = jnp.zeros_like(dn_acc)

    @pl.when(core == 0)
    def _():
        dn_acc[...], tops[0] = grads(pl.ds(base, extra), extra, base, tops[0])

    def grad_step(i, picked):
        part, picked = grads(pl.ds(pl.multiple_of(i * wide_tile, 16), wide_tile), wide_tile, i * wide_tile, picked)
        dn_acc[...] += part
        return picked

    with jax.named_scope("grads"):
        picked = lax.fori_loop(0, base // wide_tile, grad_step, tops[0])
    far = pl.ds(pl.multiple_of((1 - core) * seq, seq), seq)
    near = pl.ds(pl.multiple_of(core * seq, seq), seq)
    dn_send[...] = dn_acc[far, :]
    dp_copy = remote(dn_send, dn_recv, dp_sems.at[0], dp_sems.at[1], mate)
    dp_copy.start()
    row_loss = jnp.where(core == 0, lse, 0.0) - jnp.sum(picked, axis=0, keepdims=True)
    lossall[me] = jnp.broadcast_to(row_loss, (8, pair))
    lo_copies, lo_all = spread(lossall, lo_sems)
    for c in lo_copies:
        c.start()
    with jax.named_scope("dn_x"):
        dp_copy.wait()
        dn = ((dn_acc[near, :] + dn_recv[...]) * scale).astype(BF16)
    dn_copy = remote(dn_own, dnbuf.at[me], dn_ssem, dn_rsem.at[me], last_id)

    @pl.when(last)
    def _():
        dnbuf[last_id] = dn

    @pl.when(jnp.logical_not(last))
    def _():
        dn_own[...] = dn
        remote(dn_own, dnbuf.at[me], dn_ssem, dn_rsem.at[me], last_id).start()

    with jax.named_scope("ag_wait"):
        for p in peers:
            got = remote(nbuf.at[p], nbuf.at[p], ag_send.at[0], ag_recv.at[p], me)
            pl.when(jnp.logical_not(last))(got.wait_recv)
            pl.when(mate != last_id)(remote(nbuf.at[p], nbuf.at[p], fw_send, ag_recv.at[p], mate).start)

    near_dst = [1, 3, last_id]
    far_dst = n_stage // 2 + 1
    direct = n_micro - 1
    by_prev = [m for m in range(direct) if m >= n_micro - 3]
    by_next = [m for m in range(direct) if m < n_micro - 3]
    hands_on = (core == 1) & (me != 1)

    def dx0_start(m, k, dev):
        remote(dxbuf.at[m], dx0buf.at[m], d_send.at[k], d_recv.at[m], dev).start()

    def relayed(m):
        late = m >= n_micro - 3
        return (m < direct) & (((me == 3) & jnp.logical_not(late)) | (last & late))

    def relay_far(m):
        remote(dx0buf.at[m], dx0buf.at[m], r_sems.at[1], d_recv.at[m], far_dst).start()

    def bwd(m):
        with jax.named_scope("bwd_wait"):
            @pl.when(jnp.logical_not(last))
            def _():
                remote(gbuf.at[m], gbuf.at[m], b_send, b_recv.at[m], me).wait_recv()

            @pl.when(last)
            def _():
                @pl.when(m != last_id)
                def _():
                    remote(dnbuf.at[m], dnbuf.at[m], dn_ssem, dn_rsem.at[m], me).wait_recv()

                yf = ybuf[pl.ds(m * per, per)].reshape(seq, dim).astype(F32)
                inv = lax.rsqrt(jnp.mean(yf * yf, axis=-1, keepdims=True) + EPS)
                dnf = dnbuf[m].astype(F32)
                proj = jnp.mean(yf * dnf, axis=-1, keepdims=True)
                gbuf[m] = (dnf * inv - yf * (inv * inv * inv * proj)).astype(BF16)

        with jax.named_scope("bwd_comp"):
            g = gbuf[m]
            for j in range(n_fblk):
                cols = slice(j * fblk, (j + 1) * fblk)
                dh = dot(g, down_t[:, cols]).astype(BF16).astype(F32)
                abuf[m, :, cols] = (dh * gelu_slope(abuf[m, :, cols].astype(F32))).astype(BF16)
            dxbuf[m] = (g.astype(F32) + dot(abuf[m], up_t[...])).astype(BF16)

        @pl.when(jnp.logical_not(first))
        def _():
            remote(dxbuf.at[m], gbuf.at[m], b_send, b_recv.at[m], me - 1).start()

        @pl.when(first)
        def _():
            pl.when(m >= direct)(lambda: dx0_start(m, len(near_dst), far_dst))
            for k, dev in enumerate(near_dst):
                dx0_start(m, k, dev)

        pltpu.make_async_copy(abuf.at[m], da_out.at[m], out_sem.at[2]).start()
        pltpu.make_async_copy(gbuf.at[m], g_out.at[m], out_sem.at[3]).start()

    n_slot = obuf.shape[0]
    busy = chip == last_id // 2
    far_tile = remote(tmp_out.at[core, pl.ds(0, plan.rows)], tmp_out.at[core, pl.ds(0, plan.rows)], ic_send, od_recv, jnp.where(first, last_id, last_id - 1))
    sends_far = first | (me == last_id - 2)

    def tile_copy(k):
        rows = pl.ds(pl.multiple_of(k * plan.rows, plan.rows), plan.rows)
        slot = lax.rem(k, n_slot)
        return pltpu.make_async_copy(obuf.at[slot], tmp_out.at[core, rows], o_sem.at[slot])

    def piece(p):
        k = p // plan.per_tile
        rows = pl.ds(pl.multiple_of(p * plan.piece, plan.piece), plan.piece)
        here = pl.ds(pl.multiple_of(lax.rem(p, plan.per_tile) * plan.piece, plan.piece), plan.piece)
        return remote(obuf.at[lax.rem(k, n_slot), here], tmp_out.at[core, rows], od_send.at[k], od_recv, mate)

    def tile_sent(k):
        slot = lax.rem(k, n_slot)
        return remote(obuf.at[slot], tmp_out.at[core, pl.ds(0, plan.rows)], od_send.at[k], od_recv, mate)

    def emb_tile(k):
        with jax.named_scope("tile_prep"):

            @pl.when(k == 0)
            def _():
                for d in range(1, n_stage // 2):
                    src = lax.rem(mate + 2 * d, n_stage)
                    pl.when(jnp.logical_not(last))(remote(nbuf.at[src], nbuf.at[src], ag_send.at[0], ag_recv.at[src], me).wait_recv)
                for m in range(n_micro):
                    n_all_t[:, m * seq:(m + 1) * seq] = nbuf[m].T
                sa_all.wait_recv()
                for c in range(n_stage // 2):
                    shift[:, c * pair:(c + 1) * pair] = statall[2 * c, 0:1, :] * LOG2E + log_count

        slot = lax.rem(k, n_slot)
        with jax.named_scope("tile_wait"):
            @pl.when(k == 2)
            def _():
                tile_copy(0).wait()
                pl.when(sends_far)(far_tile.start)

            pl.when(k > n_slot)(lambda: tile_copy(k - n_slot).wait())
            pl.when((k >= n_slot) & (k - n_slot < plan.shared) & jnp.logical_not(busy & (k == n_slot)))(lambda: tile_sent(k - n_slot).wait_send())

        with jax.named_scope("tile"):
            rows = pl.ds(pl.multiple_of(k * plan.rows, plan.rows), plan.rows)
            logit_grad(emb[rows, :], n_all_t, shift, lab_ref, row0 + k * plan.rows, inv_count, scale, dz)
            obuf[slot] = dot(dz[...], nbuf[...].reshape(n_tok, dim)) * scale

        tile_copy(k).start()

    def send_pieces(done, until):
        lax.fori_loop(done, until, lambda p, c: (piece(p).start(), c)[1], 0)

    def send_tiles(done, until):
        def one(k, carry):
            rows = pl.ds(pl.multiple_of(k * plan.rows, plan.rows), plan.rows)
            remote(obuf.at[lax.rem(k, n_slot)], tmp_out.at[core, rows], od_send.at[k], od_recv, mate).start()
            return carry

        lax.fori_loop(done, until, one, 0)

    before = sum(jnp.where(me == s, plan.before[s], 0) for s in range(n_stage))

    def pass_dx0(m, carry):
        @pl.when(jnp.logical_not(first))
        def _():
            remote(dx0buf.at[m], dx0buf.at[m], r_sems.at[0], d_recv.at[m], me).wait_recv()

            @pl.when(hands_on)
            def _():
                remote(dx0buf.at[m], dx0buf.at[m], r_sems.at[0], d_recv.at[m], mate).start()

            @pl.when(relayed(m))
            def _():
                relay_far(m)

            pltpu.make_async_copy(dx0buf.at[m], dx0_out.at[m], out_sem.at[4]).start()

        @pl.when(first)
        def _():
            pltpu.make_async_copy(dxbuf.at[m], dx0_out.at[m], out_sem.at[4]).start()

        return carry

    lead = jnp.where(me == 3, -250, jnp.where(last, -1800, jnp.where(me == far_dst, -1600, -10**6)))

    def work(i, carry):
        sent, passed = carry
        chunk = (i >= before) & (i < before + n_micro)
        pl.when(chunk)(lambda: bwd(i - before))
        k = jnp.where(i < before, i, i - n_micro)
        pl.when(jnp.logical_not(chunk))(lambda: emb_tile(k))
        after = i - before - n_micro + 1
        here = jnp.where(after > 0, jnp.clip((after * 257 + lead) // 146, 0, n_micro), 0)
        lax.fori_loop(passed, here, pass_dx0, 0)
        ready = jnp.where(i < before, i + 1, jnp.where(chunk, before, i + 1 - n_micro))
        near_chunks = chunk | ((i < before) & (i + 1 >= before))
        whole = (sent + plan.per_tile - 1) // plan.per_tile
        upto = jnp.minimum(jnp.minimum(ready, plan.shared), whole + 1)
        some = jnp.where(near_chunks, jnp.minimum(sent + 1, jnp.minimum(ready, plan.shared) * plan.per_tile), whole * plan.per_tile)
        send_pieces(sent, some)
        send_tiles(whole, jnp.where(near_chunks, 0, upto))
        now = jnp.where(near_chunks, some, jnp.maximum(some, upto * plan.per_tile))
        return jnp.maximum(sent, now), jnp.maximum(passed, here)

    sent, passed = lax.fori_loop(0, plan.tiles + n_micro, work, (jnp.where(busy, plan.per_tile, 0), 0))
    outs = [pltpu.make_async_copy(nbuf, n_out, out_sem.at[5]), pltpu.make_async_copy(lossall, loss_out, out_sem.at[6]), pltpu.make_async_copy(meta, meta_out, out_sem.at[7])]
    lo_all.wait_recv()
    for c in outs:
        c.start()
    pltpu.make_async_copy(statall, stat_out, out_sem.at[8]).start()
    with jax.named_scope("relay_all"):
        lax.fori_loop(passed, n_micro, pass_dx0, 0)

    with jax.named_scope("drain"):
        send_pieces(sent, plan.shared * plan.per_tile)
        for k in range(max(plan.tiles - n_slot, 0), plan.tiles):
            tile_copy(k).wait()
            if k < plan.shared:
                tile_sent(k).wait_send()
        pl.when(sends_far)(far_tile.wait_send)
        all_rows = pl.ds(0, plan.shared * plan.rows)
        remote(tmp_out.at[1 - core, all_rows], tmp_out.at[1 - core, all_rows], od_send.at[0], od_recv, me).wait_recv()
        sa_all.wait_send()
        lo_all.wait_send()
        pltpu.make_async_copy(statall, stat_out, out_sem.at[8]).wait()
        for c, p in zip(ag_copies, peers):
            pl.when(p != last_id)(c.wait_send)

        @pl.when(jnp.logical_not(last))
        def _():
            dn_copy.wait_send()
            pl.when(mate != last_id)(n_forward.wait_send)
            remote(ybuf, xbuf, f_send, f_recv.at[0], me + 1).wait_send()

        @pl.when(last)
        def _():
            remote(nbuf, nbuf, n_send, n_recv.at[0], me).wait_send()

        @pl.when(mate != last_id)
        def _():
            some = nbuf.at[pl.ds(0, len(peers))]
            remote(some, some, fw_send, ag_recv.at[0], mate).wait_send()

        @pl.when(jnp.logical_not(first) & (me + 2 < n_micro))
        def _():
            x_copy(0).wait_send()

            @pl.when(me < 2)
            def _():
                x_copy(1).wait_send()

        @pl.when(jnp.logical_not(first))
        def _():
            remote(dxbuf, gbuf, b_send, b_recv.at[0], me).wait_send()
            pl.when(hands_on)(remote(dx0buf, dx0buf, r_sems.at[0], d_recv.at[0], mate).wait_send)

        @pl.when(first)
        def _():
            for k in range(len(near_dst)):
                remote(dxbuf, dx0buf, d_send.at[k], d_recv.at[0], me).wait_send()
            rest = pl.ds(0, n_micro - direct)
            remote(dxbuf.at[rest], dx0buf.at[rest], d_send.at[len(near_dst)], d_recv.at[0], me).wait_send()

        for dev, kept in ((3, by_next), (last_id, by_prev)):
            some = dx0buf.at[pl.ds(0, len(kept))]
            pl.when(me == dev)(remote(some, some, r_sems.at[1], d_recv.at[0], me).wait_send)

        pltpu.make_async_copy(hbuf, hid_out, out_sem.at[0]).wait()
        pltpu.make_async_copy(xbuf, xs_out, out_sem.at[1]).wait()
        pltpu.make_async_copy(abuf, da_out, out_sem.at[2]).wait()
        pltpu.make_async_copy(gbuf, g_out, out_sem.at[3]).wait()
        pltpu.make_async_copy(dx0buf, dx0_out, out_sem.at[4]).wait()
        for c in outs:
            c.wait()


class Plan:
    def __init__(self, vocab, n_stage):
        units = vocab // LANES
        self.base = units // 2 * LANES
        self.extra = vocab - 2 * self.base
        self.head_tile = next(t for t in (1600, 1536, 1280, 1024, 768, 640, 512, 256, 128) if self.base % t == 0)
        self.rows = 1024
        self.tiles, self.shared = 10, 8
        self.grad_tile = next(t for t in (4000, 3200, 1600, 1280, 640, 256, 128) if self.base % t == 0)
        self.e_parts = next(k for k in (10, 8, 5, 4, 2, 1) if self.base % (16 * k) == 0)
        self.part = 128
        self.slots = 4
        self.piece = 256
        self.per_tile = self.rows // self.piece
        measured = [10, 9, 6, 5, 3, 2, 0, 0]
        self.before = (measured + [0] * n_stage)[:n_stage]
        mid = self.base + self.extra
        ends = [(0, mid), (mid, vocab)]
        early = (self.tiles * self.rows, self.shared * self.rows)
        self.spans = [[(ends[h][0] + early[0 if h == c else 1], ends[h][1]) for h in (c, 1 - c)] for c in range(2)]
        self.longest = [max(self.spans[c][k][1] - self.spans[c][k][0] for c in range(2)) for k in range(2)]
        best = min(range(16, 1281, 16), key=lambda r: (sum(-(-n // r) for n in self.longest)) * (r + 40))
        self.calc_rows = best
        self.calc_steps = [-(-n // best) for n in self.longest]
        self.steps = sum(self.calc_steps)
        self.copy_rows = self.rows
        self.copies = self.tiles + self.shared
        self.starts = ends

    def calc_start(self, core, s):
        k = 0 if s < self.calc_steps[0] else 1
        lo, hi = self.spans[core][k]
        return min(lo + (s - k * self.calc_steps[0]) * self.calc_rows, hi - self.calc_rows)

    def copy_start(self, core, c):
        own = c < self.tiles
        h = core if own else 1 - core
        return self.starts[h][0] + (c if own else c - self.tiles) * self.copy_rows

    def cuts(self, core):
        firsts = [(self.calc_start(core, s), self.calc_rows) for s in range(self.steps)] + [(self.copy_start(core, c), self.copy_rows) for c in range(self.copies)]
        flat = [v for lo, rows in firsts for v in (lo, lo + rows)]
        return flat + [0] * (LANES - len(flat))


def run_pipe(x0, emb, w_up, w_down, labels, tokens, cuts, n_stage, plan):
    n_micro, seq = labels.shape
    dim, ffn = w_up.shape
    n_tok = n_micro * seq
    base = plan.base
    any_spec = pl.BlockSpec(memory_space=pl.ANY)
    act = (n_micro, seq, dim)
    fine = (n_tok // plan.part, plan.part, dim)
    wide = (n_micro, seq, ffn)
    dma = pltpu.SemaphoreType.DMA
    vm = pltpu.VMEM
    pair = 2 * seq
    return pl.pallas_call(
        functools.partial(pipe_kernel, n_stage, plan),
        out_shape=[
            jax.ShapeDtypeStruct(act, BF16), jax.ShapeDtypeStruct(fine, BF16), jax.ShapeDtypeStruct(wide, BF16),
            jax.ShapeDtypeStruct(wide, BF16), jax.ShapeDtypeStruct(act, BF16), jax.ShapeDtypeStruct(act, BF16),
            jax.ShapeDtypeStruct((n_stage, 8, pair), F32), jax.ShapeDtypeStruct((n_stage, 8, pair), F32), jax.ShapeDtypeStruct((2, plan.tiles * plan.rows, dim), F32),
            jax.ShapeDtypeStruct((3 * n_tok // LANES, LANES), jnp.int32),
        ],
        in_specs=[any_spec] * 4 + [pl.BlockSpec(memory_space=pltpu.VMEM)] * 3,
        out_specs=[any_spec] * 10,
        scratch_shapes=[
            vm(fine, BF16), vm(fine, BF16), vm(wide, BF16), vm(wide, BF16), vm(act, BF16), vm(act, BF16), vm(act, BF16), vm(act, BF16), vm(act, BF16),
            vm((dim, ffn), BF16), vm((ffn, dim), BF16), vm((ffn, dim), BF16), vm((dim, ffn), BF16),
            vm((base + plan.extra, dim), BF16), vm((base + plan.extra, pair), BF16), vm((dim, pair), BF16), vm((pair, dim), F32),
            vm((seq, dim), F32), vm((seq, dim), F32), vm((seq, dim), BF16), vm((16, pair), F32), vm((16, pair), F32), vm((n_stage, 8, pair), F32), vm((n_stage, 8, pair), F32),
            vm((2, 8, pair), F32), vm((dim, n_tok), BF16), vm((1, n_tok), F32), vm((plan.rows, n_tok), BF16), vm((plan.slots, plan.rows, dim), F32),
            vm((2, plan.head_tile, pair), BF16), vm((3 * n_tok // LANES, LANES), jnp.int32),
            dma((2,)), dma((2,)), dma((2,)), dma((2,)), dma((n_micro,)), dma, dma((n_tok // plan.part,)), dma, dma((n_micro,)), dma,
            dma((n_stage // 2,)), dma((n_micro,)), dma,
            dma((2,)), dma((2,)), dma, dma((n_stage,)), dma((2,)), dma((2,)), dma, dma((n_micro,)), dma((4,)), dma((n_micro,)), dma((2,)), dma((9,)),
            dma((plan.slots,)), dma((plan.shared,)), dma, dma,
        ],
        compiler_params=pltpu.CompilerParams(collective_id=0, has_side_effects=True, vmem_limit_bytes=67_000_000),
        cost_estimate=pl.CostEstimate(flops=60 * 10**9, bytes_accessed=100 * 10**6, transcendentals=0),
        name="pipe",
    )(x0.reshape(x0.shape[0], seq // plan.part, plan.part, dim), emb, w_up, w_down, labels.reshape(1, n_tok), tokens.reshape(1, n_tok), cuts)


def fin_kernel(n_stage, n_tok, plan, ids_ref, emb_hbm, tmp_hbm, n_hbm, stat_ref, part_ref, lab_ref, meta_ref, dx0_hbm, xs_hbm, hid_hbm, da_hbm, g_hbm,
               out_hbm, loss_ref, gup_hbm, gdown_hbm,
               n_all, dx0, xs, hid, da, g, n_t, x_t, dx0s, dz, shift, e_in, c_out, cp, gup, gdown,
               ld_sem, e_sem, t_sem, co_sem, po_sem, gu_sem, gd_sem, wi_sem):
    dim, ffn = gup_hbm.shape
    scale = dim ** -0.5
    inv_count = 1.0 / n_tok
    steps, crows, prows = plan.steps, plan.calc_rows, plan.copy_rows
    core = lax.rem(lax.axis_index("stage"), 2)
    early = plan.tiles * prows
    wblk = gup.shape[2]
    n_wblk = ffn // wblk
    turn = plan.calc_steps[0]

    def pick(pair):
        return jnp.where(core == 0, pair[0], pair[1])

    def calc_start(s):
        own = s < turn
        lo, hi = [jnp.where(own, pick([plan.spans[c][0][e] for c in range(2)]), pick([plan.spans[c][1][e] for c in range(2)])) for e in range(2)]
        return pl.multiple_of(jnp.minimum(lo + (s - jnp.where(own, 0, turn)) * crows, hi - crows), 16)

    def copy_start(c):
        own = c < plan.tiles
        first = jnp.where(own, pick([plan.starts[0][0], plan.starts[1][0]]), pick([plan.starts[1][0], plan.starts[0][0]]))
        return pl.multiple_of(first + (c - jnp.where(own, 0, plan.tiles)) * prows, 16)

    def e_copy(s):
        return pltpu.make_async_copy(emb_hbm.at[pl.ds(calc_start(s), crows)], e_in.at[lax.rem(s, 2)], e_sem.at[lax.rem(s, 2)])

    n_slot = cp.shape[0]
    ahead = 3

    def t_copy(c):
        own = c < plan.tiles
        row = jnp.where(own, core, 1 - core) * early + (c - jnp.where(own, 0, plan.tiles)) * prows
        slot = lax.rem(c, n_slot)
        return pltpu.make_async_copy(tmp_hbm.at[pl.ds(pl.multiple_of(row, 16), prows)], cp.at[slot], t_sem.at[slot])

    def p_out(c):
        slot = lax.rem(c, n_slot)
        return pltpu.make_async_copy(cp.at[slot], out_hbm.at[pl.ds(copy_start(c), prows)], po_sem.at[slot])

    def c_outs(s):
        slot = lax.rem(s, 2)
        return pltpu.make_async_copy(c_out.at[slot], out_hbm.at[pl.ds(calc_start(s), crows)], co_sem.at[slot])

    loads = [pltpu.make_async_copy(s, d, ld_sem.at[i]) for i, (s, d) in enumerate(((n_hbm, n_all), (dx0_hbm, dx0), (xs_hbm, xs), (g_hbm, g)))]
    loads[0].start()
    loads[1].start()
    e_copy(0).start()
    for c in range(ahead):
        t_copy(c).start(priority=1)
    pair = stat_ref.shape[2]
    loss = jnp.zeros((1, pair), F32)
    for d in range(n_stage):
        if d % 2 == 0:
            shift[:, (d // 2) * pair:(d // 2 + 1) * pair] = stat_ref[d, 0:1, :] * LOG2E + math.log2(n_tok)
        loss = loss + part_ref[d, 0:1, :]
    loss_ref[0] = jnp.sum(loss) * inv_count
    with jax.named_scope("fin_pre"):
        loads[0].wait()
        n_t[...] = n_all[...].T

    def sum_rows():
        loads[1].wait()
        dense = jnp.concatenate([meta_ref[g:g + 1, :] for g in range(n_tok // LANES)], axis=1)
        order = lax.broadcasted_iota(jnp.int32, (n_tok, n_tok), 0) == dense
        dx0s[...] = dot(jnp.where(order, 1.0, 0.0).astype(BF16), dx0[...])

    def add_rows(k, start, ref):
        lo, hi = ids_ref[2 * n_tok + k], ids_ref[2 * n_tok + k + 1]
        wide = 8

        def some(p, width):
            at = [pl.ds(ids_ref[n_tok + p + u] - start, 1) for u in range(width)]
            new = [ref[at[u], :] + dx0s[pl.ds(p + u, 1), :] for u in range(width)]
            for u in range(width):
                ref[at[u], :] = new[u]

        def group(g, carry):
            some(lo + g * wide, wide)
            return carry

        def single(p, carry):
            some(p, 1)
            return carry

        n_grp = (hi - lo) // wide
        lax.fori_loop(0, n_grp, group, 0)
        lax.fori_loop(lo + n_grp * wide, hi, single, 0)

    def w_ins(w):
        cols = pl.ds(pl.multiple_of(w * wblk, wblk), wblk)
        wslot = lax.rem(w, 2)
        return (pltpu.make_async_copy(da_hbm.at[:, cols], da.at[wslot], wi_sem.at[0, wslot]), pltpu.make_async_copy(hid_hbm.at[:, cols], hid.at[wslot], wi_sem.at[1, wslot]))

    def w_outs(w):
        cols = pl.ds(pl.multiple_of(w * wblk, wblk), wblk)
        wslot = lax.rem(w, 2)
        return (pltpu.make_async_copy(gup.at[wslot], gup_hbm.at[:, cols], gu_sem.at[wslot]), pltpu.make_async_copy(gdown.at[wslot], gdown_hbm.at[cols], gd_sem.at[wslot]))

    def copy_tile(c, carry):
        with jax.named_scope("copy_wait"):
            t_copy(c).wait()
        with jax.named_scope("add_p"):
            add_rows(2 * steps + 2 * c, copy_start(c), cp.at[lax.rem(c, n_slot)])
        p_out(c).start()

        @pl.when(c + ahead < plan.copies)
        def _():
            pl.when(c + ahead >= n_slot)(lambda: p_out(c + ahead - n_slot).wait())
            t_copy(c + ahead).start(priority=1)

        return carry

    w_first = 2
    tails = [turn - 1, steps - 1]

    def tail(s):
        return (s == tails[0]) | (s == tails[1])

    def step(s, carry):
        pl.when(s + 1 < steps)(lambda: e_copy(s + 1).start())
        with jax.named_scope("fin_wait"):
            e_copy(s).wait()

        @pl.when(s == 0)
        def _():
            for c in loads[2:]:
                c.start()

        w = s - w_first

        @pl.when((w + 1 >= 0) & (w + 1 < n_wblk))
        def _():
            for c in w_ins(w + 1):
                c.start()

        pl.when((s >= 2) & jnp.logical_not(tail(s - 1)))(lambda: c_outs(s - 2).wait())
        slot = lax.rem(s, 2)
        start = calc_start(s)
        with jax.named_scope("calc"):
            logit_grad(e_in[slot], n_t, shift, lab_ref, start, inv_count, scale, dz)
            c_out[slot] = dot(dz[...], n_all[...]) * scale
        pl.when(s == 0)(sum_rows)
        with jax.named_scope("add_c"):
            add_rows(2 * s, start, c_out.at[slot])
        pl.when(tail(s))(lambda: c_outs(s - 1).wait())
        c_outs(s).start()
        lax.fori_loop(s * plan.copies // (steps - 1), jnp.minimum((s + 1) * plan.copies // (steps - 1), plan.copies), copy_tile, 0)

        @pl.when(w == 0)
        def _():
            for c in loads[2:]:
                c.wait()
            x_t[...] = xs[...].T

        @pl.when((w >= 0) & (w < n_wblk))
        def _():
            wslot = lax.rem(w, 2)
            with jax.named_scope("dw_wait"):
                for c in w_ins(w):
                    c.wait()

                @pl.when(w >= 2)
                def _():
                    for c in w_outs(w - 2):
                        c.wait()

            with jax.named_scope("dw"):
                gup[wslot] = dot(x_t[...], da[wslot])
                gdown[wslot] = dot_t(hid[wslot], g[...])
            for c in w_outs(w):
                c.start()

        return carry

    lax.fori_loop(0, steps, step, 0)
    with jax.named_scope("fin_drain"):
        for w in range(n_wblk - 2, n_wblk):
            for c in w_outs(w):
                c.wait()
        c_outs(steps - 1).wait()
        for c in range(plan.copies - n_slot, plan.copies):
            p_out(c).wait()


def run_fin(emb, tmp, n_all, stats, losses, labels, meta, dx0, xs, hid, da, g, n_stage, plan):
    vocab, dim = emb.shape
    n_tok, ffn = hid.shape
    vm = pltpu.VMEM
    dma = pltpu.SemaphoreType.DMA
    any_spec = pl.BlockSpec(memory_space=pl.ANY)
    vspec = pl.BlockSpec(memory_space=pltpu.VMEM)
    smem = pl.BlockSpec(memory_space=pltpu.SMEM)
    wblk = 512
    return pl.pallas_call(
        functools.partial(fin_kernel, n_stage, n_tok, plan),
        out_shape=[jax.ShapeDtypeStruct((vocab, dim), F32), jax.ShapeDtypeStruct((1,), F32), jax.ShapeDtypeStruct((dim, ffn), F32), jax.ShapeDtypeStruct((ffn, dim), F32)],
        in_specs=[smem, any_spec, any_spec, any_spec, vspec, vspec, vspec, vspec] + [any_spec] * 5,
        out_specs=[any_spec, smem, any_spec, any_spec],
        scratch_shapes=[
            vm((n_tok, dim), BF16), vm((n_tok, dim), BF16), vm((n_tok, dim), BF16), vm((2, n_tok, wblk), BF16), vm((2, n_tok, wblk), BF16), vm((n_tok, dim), BF16),
            vm((dim, n_tok), BF16), vm((dim, n_tok), BF16), vm((n_tok, dim), F32), vm((plan.calc_rows, n_tok), BF16), vm((1, n_tok), F32),
            vm((2, plan.calc_rows, dim), BF16), vm((2, plan.calc_rows, dim), F32), vm((5, plan.copy_rows, dim), F32),
            vm((2, dim, wblk), F32), vm((2, wblk, dim), F32),
            dma((4,)), dma((2,)), dma((5,)), dma((2,)), dma((5,)), dma((2,)), dma((2,)), dma((2, 2)),
        ],
        compiler_params=pltpu.CompilerParams(vmem_limit_bytes=67_000_000),
        cost_estimate=pl.CostEstimate(flops=2 * n_tok * vocab * dim, bytes_accessed=5 * vocab * dim, transcendentals=0),
        name="fin",
    )(meta.reshape(-1), emb, tmp, n_all, stats, losses, labels.reshape(1, n_tok), meta, dx0, xs, hid, da, g)


def solution(mesh):
    n_stage = mesh.shape["stage"]

    def device_fn(tokens, labels, emb, w_up, w_down):
        n_micro, seq = tokens.shape
        vocab, dim = emb.shape
        w_up, w_down = w_up[0], w_down[0]
        n_tok = n_micro * seq
        plan = Plan(vocab, n_stage)
        cuts = jnp.array([plan.cuts(0), plan.cuts(1)], jnp.int32)
        x0 = run_gather(tokens, emb)
        n_all, xs, hid, da, g, dx0, stats, losses, tmp, meta = run_pipe(x0, emb, w_up, w_down, labels, tokens, cuts, n_stage, plan)
        flat = lambda p: p.reshape(n_tok, -1)
        grad_emb, loss, grad_up, grad_down = run_fin(
            emb, tmp.reshape(-1, dim), flat(n_all), stats, losses, labels, meta, flat(dx0), flat(xs), flat(hid), flat(da), flat(g), n_stage, plan
        )
        return loss, grad_up[None], grad_down[None], grad_emb

    return jax.shard_map(device_fn, mesh=mesh, in_specs=(P("dp", None), P("dp", None), P(None, None), P("stage", None, None), P("stage", None, None)), out_specs=(P("dp"), P(("dp", "stage"), None, None), P(("dp", "stage"), None, None), P("dp", None)), check_vma=False)
```

```python
import functools
import math

import jax
import jax.numpy as jnp
from jax import lax
from jax.experimental import pallas as pl
from jax.experimental.pallas import tpu as pltpu
from jax.sharding import PartitionSpec as P


MESH = pl.DeviceIdType.MESH
LOG2E = math.log2(math.e)
LN2 = math.log(2.0)
GELU_C = math.sqrt(2.0 / math.pi)
GELU_K = 0.044715
EPS = 1e-6
LANES = 128
F32 = jnp.float32
BF16 = jnp.bfloat16


def gelu_fwd(a):
    return (0.5 * a) * (1.0 + jnp.tanh(a * (GELU_C + (GELU_C * GELU_K) * (a * a))))


def gelu_slope(a):
    a2 = a * a
    half = 0.5 * jnp.tanh(a * (GELU_C + (GELU_C * GELU_K) * a2))
    up, down = 0.5 + half, 0.5 - half
    return up + (up * down) * (a * (2.0 * GELU_C + (6.0 * GELU_C * GELU_K) * a2))


def dot(x, y):
    return jnp.dot(x, y, preferred_element_type=F32)


def dot_t(x, y):
    return lax.dot_general(x, y, (((0,), (0,)), ((), ())), preferred_element_type=F32)


def remote(src, dst, send_sem, recv_sem, dev):
    return pltpu.make_async_remote_copy(src_ref=src, dst_ref=dst, send_sem=send_sem, recv_sem=recv_sem, device_id={"stage": dev}, device_id_type=MESH)


def column(row):
    return jnp.broadcast_to(row, (LANES, LANES)).T


def gather_kernel(ids_ref, tok_ref, emb_hbm, x0_hbm, tiles, picked, sem, out_sem):
    n_micro, seq = tok_ref.shape
    me = lax.axis_index("stage")
    group = tiles.shape[1] // seq
    slots = tiles.shape[0]
    owners = [head_chunk(me, k, n_micro) for k in range(slots)]

    def fetch(k):
        def one(i, carry):
            t = ids_ref[owners[k] * seq + i]
            start = pl.multiple_of(t // group * group, group)
            pltpu.make_async_copy(emb_hbm.at[pl.ds(start, group)], tiles.at[k, pl.ds(pl.multiple_of(i * group, group), group)], sem.at[k]).start()
            return carry

        lax.fori_loop(0, seq, one, 0, unroll=8)

    def select(k):
        sub = lax.broadcasted_iota(jnp.int32, (LANES, LANES), 0)
        lane = lax.broadcasted_iota(jnp.int32, (LANES, LANES), 1)
        tok = column(tok_ref[pl.ds(owners[k], 1), :].astype(F32)).astype(jnp.int32)
        want = sub * group + (tok - tok // group * group)
        hot = jnp.concatenate([jnp.where(lane + b * LANES == want, 1.0, 0.0).astype(BF16) for b in range(seq * group // LANES)], axis=1)
        pltpu.make_async_copy(emb_hbm.at[pl.ds(0, seq * group)], tiles.at[k], sem.at[k]).wait()
        picked[k] = dot(hot, tiles[k]).astype(BF16)
        pltpu.make_async_copy(picked.at[k], x0_hbm.at[k], out_sem.at[k]).start()

    def finish(k):
        pltpu.make_async_copy(picked.at[k], x0_hbm.at[k], out_sem.at[k]).wait()

    for work in (fetch, select, finish):
        work(0)
        for k in range(1, slots):
            pl.when(me < slots)(functools.partial(work, k))


def head_chunk(dev, k, n_micro):
    return jnp.minimum(jnp.where(dev < 2, 2 * dev + k, dev + 2), n_micro - 1)


def run_gather(tokens, emb):
    n_micro, seq = tokens.shape
    dim = emb.shape[1]
    group = 16
    return pl.pallas_call(
        gather_kernel,
        out_shape=jax.ShapeDtypeStruct((2, seq, dim), BF16),
        in_specs=[pl.BlockSpec(memory_space=pltpu.SMEM), pl.BlockSpec(memory_space=pltpu.VMEM), pl.BlockSpec(memory_space=pl.ANY)],
        out_specs=pl.BlockSpec(memory_space=pl.ANY),
        scratch_shapes=[pltpu.VMEM((2, seq * group, dim), BF16), pltpu.VMEM((2, seq, dim), BF16), pltpu.SemaphoreType.DMA((2,)), pltpu.SemaphoreType.DMA((2,))],
        cost_estimate=pl.CostEstimate(flops=10**9, bytes_accessed=2 * seq * group * dim * 2, transcendentals=0),
        name="gather",
    )(tokens.reshape(n_micro * seq), tokens, emb)


def token_table(row_ref, cut_ref, meta):
    n_tok = row_ref.shape[1]
    n_grp = n_tok // LANES
    lane = lax.broadcasted_iota(jnp.int32, (LANES, LANES), 1).astype(F32)
    sub = lax.broadcasted_iota(jnp.int32, (LANES, LANES), 0)
    row = lambda g: row_ref[:, g * LANES:(g + 1) * LANES].astype(F32)
    zero = jnp.zeros((LANES, LANES), F32)
    fold = lambda acc: jnp.sum(acc, axis=0, keepdims=True)
    cols = [column(row(c)) for c in range(n_grp)]
    firsts = []
    for g in range(n_grp):
        acc = zero
        for c in range(g + 1):
            same = cols[c] == row(g)
            if c == g:
                same = same & (sub < lane.astype(jnp.int32))
            acc = acc + jnp.where(same, 1.0, 0.0)
        firsts.append(column(jnp.where(fold(acc) == 0.0, 1.0, 0.0)))
    ranks = []
    for g in range(n_grp):
        acc = zero
        for c in range(n_grp):
            acc = acc + jnp.where(cols[c] < row(g), firsts[c], 0.0)
        ranks.append(fold(acc))
        meta[g:g + 1, :] = ranks[g].astype(jnp.int32)
    rank_cols = [column(r) for r in ranks]
    for g in range(n_grp):
        acc = zero
        for c in range(n_grp):
            acc = acc + jnp.where(rank_cols[c] == lane + g * LANES, firsts[c] * cols[c], 0.0)
        meta[n_grp + g:n_grp + g + 1, :] = fold(acc).astype(jnp.int32)
    cut = cut_ref[...].astype(F32)
    acc = zero
    for c in range(n_grp):
        acc = acc + jnp.where(cols[c] < cut, firsts[c], 0.0)
    meta[2 * n_grp:3 * n_grp, :] = jnp.broadcast_to(fold(acc), (n_grp, LANES)).astype(jnp.int32)


def logit_grad(e, n_t, shift, lab, first_id, inv_count, scale, dz):
    rows = e.shape[0]
    n_tok = n_t.shape[1]
    blk = 256
    vid = lax.broadcasted_iota(jnp.int32, (rows, blk), 0)
    for j in range(n_tok // blk):
        cols = slice(j * blk, (j + 1) * blk)
        z = (dot(e, n_t[:, cols]) * scale).astype(BF16).astype(F32)
        prob = jnp.exp2(z * LOG2E - shift[:, cols])
        dz[:, cols] = jnp.where(vid == lab[:, cols] - first_id, prob - inv_count, prob).astype(BF16)


def pipe_kernel(n_stage, plan, x0_hbm, emb_hbm, up_hbm, down_hbm, lab_ref, row_ref, cut_ref,
                n_out, xs_out, hid_out, da_out, g_out, dx0_out, stat_out, loss_out, tmp_out, meta_out,
                xbuf, ybuf, abuf, hbuf, nbuf, gbuf, dxbuf, dx0buf, dnbuf, up, down, up_t, down_t,
                emb, zbuf, n_t, dn_acc, dn_send, dn_recv, dn_own, st_send, st_recv, statall, lossall, tops, n_all_t, shift, dz, obuf, z_pair, meta,
                w_sem, e_sem, x_sem, x_send, x_recv, f_send, f_recv, n_send, n_recv, nf_send, ag_send, ag_recv, fw_send,
                st_sems, dp_sems, dn_ssem, dn_rsem, sa_sems, lo_sems, b_send, b_recv, d_send, d_recv, r_sems, out_sem, o_sem, od_send, od_recv, ic_send):
    n_micro, seq, dim = gbuf.shape
    part = xbuf.shape[1]
    n_part = xbuf.shape[0]
    per = seq // part
    n_tok = n_micro * seq
    ffn = up.shape[1]
    vocab = emb_hbm.shape[0]
    me = lax.axis_index("stage")
    core = lax.rem(me, 2)
    chip = me // 2
    mate = me + 1 - 2 * core
    last_id = n_stage - 1
    first = me == 0
    last = me == last_id
    fblk = 512
    n_fblk = ffn // fblk
    base, extra, tile = plan.base, plan.extra, plan.head_tile
    row0 = core * (base + extra)
    n_tiles = base // tile
    wide_tile = plan.grad_tile

    barrier = pltpu.get_barrier_semaphore()
    for d in range(1, n_stage):
        pl.semaphore_signal(barrier, inc=1, device_id={"stage": lax.rem(me + d, n_stage)}, device_id_type=MESH)
    w_copy = [pltpu.make_async_copy(up_hbm, up, w_sem.at[0]), pltpu.make_async_copy(down_hbm, down, w_sem.at[1])]
    for c in w_copy:
        c.start()
    x_slots = x0_hbm.shape[0]
    x_mine = [head_chunk(me, k, n_micro) for k in range(x_slots)]

    def x_rows(m):
        return xbuf.at[pl.ds(m * per, per)]

    def x_local(k):
        return pltpu.make_async_copy(x0_hbm.at[k], x_rows(k), x_sem.at[k])

    @pl.when(first)
    def _():
        for k in range(x_slots):
            x_local(k).start()

    e_parts = plan.e_parts
    e_step = base // e_parts

    def e_copy(i):
        src = emb_hbm.at[pl.ds(pl.multiple_of(row0 + i * e_step, 16), e_step)]
        return pltpu.make_async_copy(src, emb.at[pl.ds(i * e_step, e_step)], e_sem.at[0])

    e_more = pltpu.make_async_copy(emb_hbm.at[pl.ds(base, extra)], emb.at[pl.ds(base, extra)], e_sem.at[1])
    with jax.named_scope("entry"):
        pl.semaphore_wait(barrier, n_stage - 1)

    def x_copy(k):
        return remote(x0_hbm.at[k], x_rows(x_mine[k]), x_send.at[k], x_recv.at[x_mine[k]], 0)

    @pl.when(jnp.logical_not(first) & (me + 2 < n_micro))
    def _():
        x_copy(0).start()

        @pl.when(me < 2)
        def _():
            x_copy(1).start()

    with jax.named_scope("w_wait"):
        for c in w_copy:
            c.wait()
        for i in range(e_parts):
            e_copy(i).start()
        pl.when(core == 0)(e_more.start)

    def transpose_weights():
        for j in range(n_fblk):
            up_t[j * fblk:(j + 1) * fblk, :] = up[:, j * fblk:(j + 1) * fblk].T
            down_t[:, j * fblk:(j + 1) * fblk] = down[j * fblk:(j + 1) * fblk, :].T

    def idle_work():
        transpose_weights()
        token_table(row_ref, jnp.where(core == 0, cut_ref[0:1, :], cut_ref[1:2, :]), meta)

    @pl.when(chip >= n_stage // 4)
    def _():
        idle_work()

    def n_start(m):
        remote(nbuf.at[m], nbuf.at[m], n_send, n_recv.at[m], jnp.where(m == last_id, last_id - 1, m)).start()

    def fwd(h, carry):
        m = h // per
        sub = lax.rem(h, per)
        rows = pl.ds(pl.multiple_of(sub * part, part), part)
        with jax.named_scope("fwd_wait"):

            @pl.when(first & (sub == 0))
            def _():
                @pl.when(m < x_slots)
                def _():
                    x_local(m).wait()

                @pl.when(m >= x_slots)
                def _():
                    remote(x_rows(m), x_rows(m), x_send.at[0], x_recv.at[m], me).wait_recv()

            @pl.when(jnp.logical_not(first))
            def _():
                remote(xbuf.at[h], xbuf.at[h], f_send, f_recv.at[h], me).wait_recv()

        with jax.named_scope("fwd_comp"):
            x = xbuf[h]
            for j in range(n_fblk):
                cols = slice(j * fblk, (j + 1) * fblk)
                a = dot(x, up[:, cols]).astype(BF16)
                abuf[m, rows, cols] = a
                hbuf[m, rows, cols] = gelu_fwd(a.astype(F32)).astype(BF16)
            y = (x.astype(F32) + dot(hbuf[m, rows, :], down[...])).astype(BF16)
            ybuf[h] = y

        @pl.when(jnp.logical_not(last))
        def _():
            remote(ybuf.at[h], xbuf.at[h], f_send, f_recv.at[h], me + 1).start()

        @pl.when(last)
        def _():
            yf = y.astype(F32)
            inv = lax.rsqrt(jnp.mean(yf * yf, axis=-1, keepdims=True) + EPS)
            nbuf[m, rows, :] = (yf * inv).astype(BF16)
            pl.when(sub == per - 1)(lambda: n_start(m))

        @pl.when(sub == per - 1)
        def _():
            pltpu.make_async_copy(hbuf.at[m], hid_out.at[m], out_sem.at[0]).start()
            pltpu.make_async_copy(x_rows(m), xs_out.at[pl.ds(m * per, per)], out_sem.at[1]).start()

        return carry

    lax.fori_loop(0, n_part, fwd, 0)

    @pl.when(chip < n_stage // 4)
    def _():
        idle_work()

    n_forward = remote(nbuf.at[me], nbuf.at[me], nf_send, n_recv.at[me], mate)
    with jax.named_scope("n_wait"):

        @pl.when(jnp.logical_not(last))
        def _():
            remote(nbuf.at[me], nbuf.at[me], n_send, n_recv.at[me], me).wait_recv()
            pl.when(mate != last_id)(n_forward.start)
            remote(nbuf.at[mate], nbuf.at[mate], n_send, n_recv.at[mate], me).wait_recv()

        for k in range(2):
            n_t[:, k * seq:(k + 1) * seq] = nbuf[2 * chip + k].T

    peers = [lax.rem(me + 2 * d, n_stage) for d in range(1, n_stage // 2)]
    ag_copies = [remote(nbuf.at[me], nbuf.at[me], ag_send.at[d], ag_recv.at[me], p) for d, p in enumerate(peers)]
    for c, p in zip(ag_copies, peers):
        pl.when(p != last_id)(c.start)
    with jax.named_scope("e_wait"):
        pltpu.make_async_copy(emb_hbm.at[pl.ds(0, base)], emb.at[pl.ds(0, base)], e_sem.at[0]).wait()
        pl.when(core == 0)(e_more.wait)

    pair = 2 * seq
    scale = dim ** -0.5
    inv_count = 1.0 / n_tok
    log_count = math.log2(n_tok)
    lab = lab_ref[:, pl.ds(pl.multiple_of(chip * pair, pair), pair)]

    def logits(rows, size):
        e = emb[rows, :]
        parts = [dot(e[k * size // 2:(k + 1) * size // 2], n_t[...]) for k in range(2)]
        z = jnp.concatenate([(p * scale).astype(BF16) for p in parts], axis=0)
        zbuf[rows, :] = z
        return z

    def peak(z, size, top):
        best = jnp.max(z.reshape(size // 16, 16, pair), axis=0).astype(F32)
        return jnp.maximum(top, jnp.maximum(best[:8], best[8:]))

    def total(z, size, old, top, tot):
        off = top * LOG2E
        return tot * jnp.exp2(old * LOG2E - off) + jnp.sum(jnp.exp2(z.astype(F32).reshape(size // 8, 8, pair) * LOG2E - off[None]), axis=0)

    tops[0] = jnp.full((8, pair), -jnp.inf, F32)
    tops[1] = jnp.zeros((8, pair), F32)

    @pl.when(core == 0)
    def _():
        z = logits(pl.ds(base, extra), extra)
        top = peak(z, extra, tops[0])
        tops[1] = total(z, extra, tops[0], top, tops[1])
        tops[0] = top

    def logits_step(i, slot, old, top, tot):
        z = logits(pl.ds(pl.multiple_of(i * tile, 16), tile), tile)
        tot = total(z_pair[1 - slot], tile, old, top, tot)
        z_pair[slot] = z
        return top, peak(z, tile, top), tot

    with jax.named_scope("logits"):
        z = logits(pl.ds(0, tile), tile)
        z_pair[0] = z
        state = (tops[0], peak(z, tile, tops[0]), tops[1])
        state = lax.fori_loop(0, (n_tiles - 1) // 2, lambda i, c: logits_step(2 * i + 2, 0, *logits_step(2 * i + 1, 1, *c)), state)
        if n_tiles % 2 == 0:
            state = logits_step(n_tiles - 1, 1, *state)
        old, top, tot = state
        tot = total(z_pair[(n_tiles - 1) % 2], tile, old, top, tot)
    row_top = jnp.max(top, axis=0, keepdims=True)
    row_tot = jnp.sum(tot * jnp.exp2((top - row_top) * LOG2E), axis=0, keepdims=True)
    st_send[0:8, :] = jnp.broadcast_to(row_top, (8, pair))
    st_send[8:16, :] = jnp.broadcast_to(row_tot, (8, pair))
    st_copy = remote(st_send, st_recv, st_sems.at[0], st_sems.at[1], mate)
    with jax.named_scope("stat_x"):
        st_copy.start()
        st_copy.wait()
    far_top = st_recv[0:1, :]
    far_tot = st_recv[8:9, :]
    all_top = jnp.maximum(row_top, far_top)
    mine = row_tot * jnp.exp(row_top - all_top)
    other = far_tot * jnp.exp(far_top - all_top)
    lse = all_top + jnp.log(jnp.where(core == 0, mine + other, other + mine))
    my_shift = lse * LOG2E + log_count
    others = [lax.rem(me + d, n_stage) for d in range(1, n_stage)]

    def spread(buf, sems):
        whole = buf.at[pl.ds(0, n_stage - 1)]
        return [remote(buf.at[me], buf.at[me], sems.at[0], sems.at[1], p) for p in others], remote(whole, whole, sems.at[0], sems.at[1], me)

    statall[me] = jnp.broadcast_to(lse, (8, pair))
    sa_copies, sa_all = spread(statall, sa_sems)
    for c in sa_copies:
        c.start()

    def grads(rows, size, first_row, picked):
        zf = zbuf[rows, :].astype(F32)
        prob = jnp.exp2(zf * LOG2E - my_shift)
        hit = lax.broadcasted_iota(jnp.int32, (size, pair), 0) == lab - (row0 + first_row)
        dz_t = jnp.where(hit, prob - inv_count, prob).astype(BF16)
        got = jnp.where(hit, zf, 0.0).reshape(size // 8, 8, pair)
        return dot_t(dz_t, emb[rows, :]), picked + jnp.sum(got, axis=0)

    tops[0] = jnp.zeros((8, pair), F32)
    dn_acc[...] = jnp.zeros_like(dn_acc)

    @pl.when(core == 0)
    def _():
        dn_acc[...], tops[0] = grads(pl.ds(base, extra), extra, base, tops[0])

    def grad_step(i, picked):
        part, picked = grads(pl.ds(pl.multiple_of(i * wide_tile, 16), wide_tile), wide_tile, i * wide_tile, picked)
        dn_acc[...] += part
        return picked

    with jax.named_scope("grads"):
        picked = lax.fori_loop(0, base // wide_tile, grad_step, tops[0])
    far = pl.ds(pl.multiple_of((1 - core) * seq, seq), seq)
    near = pl.ds(pl.multiple_of(core * seq, seq), seq)
    dn_send[...] = dn_acc[far, :]
    dp_copy = remote(dn_send, dn_recv, dp_sems.at[0], dp_sems.at[1], mate)
    dp_copy.start()
    row_loss = jnp.where(core == 0, lse, 0.0) - jnp.sum(picked, axis=0, keepdims=True)
    lossall[me] = jnp.broadcast_to(row_loss, (8, pair))
    lo_copies, lo_all = spread(lossall, lo_sems)
    for c in lo_copies:
        c.start()
    with jax.named_scope("dn_x"):
        dp_copy.wait()
        dn = ((dn_acc[near, :] + dn_recv[...]) * scale).astype(BF16)
    dn_copy = remote(dn_own, dnbuf.at[me], dn_ssem, dn_rsem.at[me], last_id)

    @pl.when(last)
    def _():
        dnbuf[last_id] = dn

    @pl.when(jnp.logical_not(last))
    def _():
        dn_own[...] = dn
        remote(dn_own, dnbuf.at[me], dn_ssem, dn_rsem.at[me], last_id).start()

    with jax.named_scope("ag_wait"):
        for p in peers:
            got = remote(nbuf.at[p], nbuf.at[p], ag_send.at[0], ag_recv.at[p], me)
            pl.when(jnp.logical_not(last))(got.wait_recv)
            pl.when(mate != last_id)(remote(nbuf.at[p], nbuf.at[p], fw_send, ag_recv.at[p], mate).start)

    near_dst = [1, 3, last_id]
    far_dst = n_stage // 2 + 1
    direct = n_micro - 1
    by_prev = n_micro - 3
    hands_on = (core == 1) & (me != 1)

    def dx0_start(m, k, dev):
        remote(dxbuf.at[m], dx0buf.at[m], d_send.at[k], d_recv.at[m], dev).start()

    def relayed(m):
        return (m < direct) & (((me == 3) & (m != by_prev)) | (last & (m == by_prev)))

    def relay_far(m):
        remote(dx0buf.at[m], dx0buf.at[m], r_sems.at[1], d_recv.at[m], far_dst).start()

    def bwd(m):
        with jax.named_scope("bwd_wait"):
            @pl.when(jnp.logical_not(last))
            def _():
                remote(gbuf.at[m], gbuf.at[m], b_send, b_recv.at[m], me).wait_recv()

            @pl.when(last)
            def _():
                @pl.when(m != last_id)
                def _():
                    remote(dnbuf.at[m], dnbuf.at[m], dn_ssem, dn_rsem.at[m], me).wait_recv()

                yf = ybuf[pl.ds(m * per, per)].reshape(seq, dim).astype(F32)
                inv = lax.rsqrt(jnp.mean(yf * yf, axis=-1, keepdims=True) + EPS)
                dnf = dnbuf[m].astype(F32)
                proj = jnp.mean(yf * dnf, axis=-1, keepdims=True)
                gbuf[m] = (dnf * inv - yf * (inv * inv * inv * proj)).astype(BF16)

        with jax.named_scope("bwd_comp"):
            g = gbuf[m]
            for j in range(n_fblk):
                cols = slice(j * fblk, (j + 1) * fblk)
                dh = dot(g, down_t[:, cols]).astype(BF16).astype(F32)
                abuf[m, :, cols] = (dh * gelu_slope(abuf[m, :, cols].astype(F32))).astype(BF16)
            dxbuf[m] = (g.astype(F32) + dot(abuf[m], up_t[...])).astype(BF16)

        @pl.when(jnp.logical_not(first))
        def _():
            remote(dxbuf.at[m], gbuf.at[m], b_send, b_recv.at[m], me - 1).start()

        @pl.when(first)
        def _():
            pl.when(m >= direct)(lambda: dx0_start(m, len(near_dst), far_dst))
            for k, dev in enumerate(near_dst):
                dx0_start(m, k, dev)

        pltpu.make_async_copy(abuf.at[m], da_out.at[m], out_sem.at[2]).start()
        pltpu.make_async_copy(gbuf.at[m], g_out.at[m], out_sem.at[3]).start()

    n_slot = obuf.shape[0]
    busy = chip == last_id // 2
    far_tile = remote(tmp_out.at[core, pl.ds(0, plan.rows)], tmp_out.at[core, pl.ds(0, plan.rows)], ic_send, od_recv, jnp.where(first, last_id, last_id - 1))
    sends_far = first | (me == last_id - 2)

    def tile_copy(k):
        rows = pl.ds(pl.multiple_of(k * plan.rows, plan.rows), plan.rows)
        slot = lax.rem(k, n_slot)
        return pltpu.make_async_copy(obuf.at[slot], tmp_out.at[core, rows], o_sem.at[slot])

    def piece(p):
        k = p // plan.per_tile
        rows = pl.ds(pl.multiple_of(p * plan.piece, plan.piece), plan.piece)
        here = pl.ds(pl.multiple_of(lax.rem(p, plan.per_tile) * plan.piece, plan.piece), plan.piece)
        return remote(obuf.at[lax.rem(k, n_slot), here], tmp_out.at[core, rows], od_send.at[k], od_recv, mate)

    def tile_sent(k):
        slot = lax.rem(k, n_slot)
        return remote(obuf.at[slot], tmp_out.at[core, pl.ds(0, plan.rows)], od_send.at[k], od_recv, mate)

    def emb_tile(k):
        with jax.named_scope("tile_prep"):

            @pl.when(k == 0)
            def _():
                for d in range(1, n_stage // 2):
                    src = lax.rem(mate + 2 * d, n_stage)
                    pl.when(jnp.logical_not(last))(remote(nbuf.at[src], nbuf.at[src], ag_send.at[0], ag_recv.at[src], me).wait_recv)
                for m in range(n_micro):
                    n_all_t[:, m * seq:(m + 1) * seq] = nbuf[m].T
                sa_all.wait_recv()
                for c in range(n_stage // 2):
                    shift[:, c * pair:(c + 1) * pair] = statall[2 * c, 0:1, :] * LOG2E + log_count

        slot = lax.rem(k, n_slot)
        with jax.named_scope("tile_wait"):
            @pl.when(k == 2)
            def _():
                tile_copy(0).wait()
                pl.when(sends_far)(far_tile.start)

            pl.when(k > n_slot)(lambda: tile_copy(k - n_slot).wait())
            pl.when((k >= n_slot) & (k - n_slot < plan.shared) & jnp.logical_not(busy & (k == n_slot)))(lambda: tile_sent(k - n_slot).wait_send())

        with jax.named_scope("tile"):
            rows = pl.ds(pl.multiple_of(k * plan.rows, plan.rows), plan.rows)
            logit_grad(emb[rows, :], n_all_t, shift, lab_ref, row0 + k * plan.rows, inv_count, scale, dz)
            obuf[slot] = dot(dz[...], nbuf[...].reshape(n_tok, dim)) * scale

        tile_copy(k).start()

    def send_pieces(done, until):
        lax.fori_loop(done, until, lambda p, c: (piece(p).start(), c)[1], 0)

    def send_tiles(done, until):
        def one(k, carry):
            rows = pl.ds(pl.multiple_of(k * plan.rows, plan.rows), plan.rows)
            remote(obuf.at[lax.rem(k, n_slot)], tmp_out.at[core, rows], od_send.at[k], od_recv, mate).start()
            return carry

        lax.fori_loop(done, until, one, 0)

    before = sum(jnp.where(me == s, plan.before[s], 0) for s in range(n_stage))

    def pass_dx0(m, carry):
        @pl.when(jnp.logical_not(first))
        def _():
            remote(dx0buf.at[m], dx0buf.at[m], r_sems.at[0], d_recv.at[m], me).wait_recv()

            @pl.when(hands_on)
            def _():
                remote(dx0buf.at[m], dx0buf.at[m], r_sems.at[0], d_recv.at[m], mate).start()

            @pl.when(relayed(m))
            def _():
                relay_far(m)

            pltpu.make_async_copy(dx0buf.at[m], dx0_out.at[m], out_sem.at[4]).start()

        @pl.when(first)
        def _():
            pltpu.make_async_copy(dxbuf.at[m], dx0_out.at[m], out_sem.at[4]).start()

        return carry

    lead = jnp.where(me == 3, -300, jnp.where(last, -1800, jnp.where(me == far_dst, -1600, -10**6)))

    def work(i, carry):
        sent, passed = carry
        chunk = (i >= before) & (i < before + n_micro)
        pl.when(chunk)(lambda: bwd(i - before))
        k = jnp.where(i < before, i, i - n_micro)
        pl.when(jnp.logical_not(chunk))(lambda: emb_tile(k))
        after = i - before - n_micro + 1
        here = jnp.where(after > 0, jnp.clip((after * 264 + lead) // 138, 0, n_micro), 0)
        lax.fori_loop(passed, here, pass_dx0, 0)
        ready = jnp.where(i < before, i + 1, jnp.where(chunk, before, i + 1 - n_micro))
        near_chunks = chunk | ((i < before) & (i + 1 >= before))
        whole = (sent + plan.per_tile - 1) // plan.per_tile
        upto = jnp.minimum(jnp.minimum(ready, plan.shared), whole + 1)
        some = jnp.where(near_chunks, jnp.minimum(sent + 1, jnp.minimum(ready, plan.shared) * plan.per_tile), whole * plan.per_tile)
        send_pieces(sent, some)
        send_tiles(whole, jnp.where(near_chunks, 0, upto))
        now = jnp.where(near_chunks, some, jnp.maximum(some, upto * plan.per_tile))
        return jnp.maximum(sent, now), jnp.maximum(passed, here)

    sent, passed = lax.fori_loop(0, plan.tiles + n_micro, work, (jnp.where(busy, plan.per_tile, 0), 0))
    outs = [pltpu.make_async_copy(nbuf, n_out, out_sem.at[5]), pltpu.make_async_copy(lossall, loss_out, out_sem.at[6]), pltpu.make_async_copy(meta, meta_out, out_sem.at[7])]
    lo_all.wait_recv()
    for c in outs:
        c.start()
    pltpu.make_async_copy(statall, stat_out, out_sem.at[8]).start()
    with jax.named_scope("relay_all"):
        lax.fori_loop(passed, n_micro, pass_dx0, 0)

    with jax.named_scope("drain"):
        send_pieces(sent, plan.shared * plan.per_tile)
        for k in range(max(plan.tiles - n_slot, 0), plan.tiles):
            tile_copy(k).wait()
            if k < plan.shared:
                tile_sent(k).wait_send()
        pl.when(sends_far)(far_tile.wait_send)
        all_rows = pl.ds(0, plan.shared * plan.rows)
        remote(tmp_out.at[1 - core, all_rows], tmp_out.at[1 - core, all_rows], od_send.at[0], od_recv, me).wait_recv()
        sa_all.wait_send()
        lo_all.wait_send()
        pltpu.make_async_copy(statall, stat_out, out_sem.at[8]).wait()
        for c, p in zip(ag_copies, peers):
            pl.when(p != last_id)(c.wait_send)

        @pl.when(jnp.logical_not(last))
        def _():
            dn_copy.wait_send()
            pl.when(mate != last_id)(n_forward.wait_send)
            remote(ybuf, xbuf, f_send, f_recv.at[0], me + 1).wait_send()

        @pl.when(last)
        def _():
            remote(nbuf, nbuf, n_send, n_recv.at[0], me).wait_send()

        @pl.when(mate != last_id)
        def _():
            some = nbuf.at[pl.ds(0, len(peers))]
            remote(some, some, fw_send, ag_recv.at[0], mate).wait_send()

        @pl.when(jnp.logical_not(first) & (me + 2 < n_micro))
        def _():
            x_copy(0).wait_send()

            @pl.when(me < 2)
            def _():
                x_copy(1).wait_send()

        @pl.when(jnp.logical_not(first))
        def _():
            remote(dxbuf, gbuf, b_send, b_recv.at[0], me).wait_send()
            pl.when(hands_on)(remote(dx0buf, dx0buf, r_sems.at[0], d_recv.at[0], mate).wait_send)

        @pl.when(first)
        def _():
            for k in range(len(near_dst)):
                remote(dxbuf, dx0buf, d_send.at[k], d_recv.at[0], me).wait_send()
            rest = pl.ds(0, n_micro - direct)
            remote(dxbuf.at[rest], dx0buf.at[rest], d_send.at[len(near_dst)], d_recv.at[0], me).wait_send()

        for dev, kept in ((3, direct - 1), (last_id, 1)):
            some = dx0buf.at[pl.ds(0, kept)]
            pl.when(me == dev)(remote(some, some, r_sems.at[1], d_recv.at[0], me).wait_send)

        pltpu.make_async_copy(hbuf, hid_out, out_sem.at[0]).wait()
        pltpu.make_async_copy(xbuf, xs_out, out_sem.at[1]).wait()
        pltpu.make_async_copy(abuf, da_out, out_sem.at[2]).wait()
        pltpu.make_async_copy(gbuf, g_out, out_sem.at[3]).wait()
        pltpu.make_async_copy(dx0buf, dx0_out, out_sem.at[4]).wait()
        for c in outs:
            c.wait()


class Plan:
    def __init__(self, vocab, n_stage):
        units = vocab // LANES
        self.base = units // 2 * LANES
        self.extra = vocab - 2 * self.base
        self.head_tile = next(t for t in (1600, 1536, 1280, 1024, 768, 640, 512, 256, 128) if self.base % t == 0)
        self.rows = 1024
        self.tiles, self.shared = 11, 9
        self.grad_tile = next(t for t in (4000, 3200, 1600, 1280, 640, 256, 128) if self.base % t == 0)
        self.e_parts = next(k for k in (10, 8, 5, 4, 2, 1) if self.base % (16 * k) == 0)
        self.part = 128
        self.slots = 4
        self.piece = 256
        self.per_tile = self.rows // self.piece
        measured = [10, 9, 6, 5, 3, 2, 0, 0]
        self.before = (measured + [0] * n_stage)[:n_stage]
        mid = self.base + self.extra
        ends = [(0, mid), (mid, vocab)]
        early = (self.tiles * self.rows, self.shared * self.rows)
        self.spans = [[(ends[h][0] + early[0 if h == c else 1], ends[h][1]) for h in (c, 1 - c)] for c in range(2)]
        self.longest = [max(self.spans[c][k][1] - self.spans[c][k][0] for c in range(2)) for k in range(2)]
        best = min(range(16, 1281, 16), key=lambda r: (sum(-(-n // r) for n in self.longest)) * (r + 40))
        self.calc_rows = best
        self.calc_steps = [-(-n // best) for n in self.longest]
        self.steps = sum(self.calc_steps)
        self.copy_rows = self.rows
        self.copies = self.tiles + self.shared
        self.starts = ends

    def calc_start(self, core, s):
        k = 0 if s < self.calc_steps[0] else 1
        lo, hi = self.spans[core][k]
        return min(lo + (s - k * self.calc_steps[0]) * self.calc_rows, hi - self.calc_rows)

    def copy_start(self, core, c):
        own = c < self.tiles
        h = core if own else 1 - core
        return self.starts[h][0] + (c if own else c - self.tiles) * self.copy_rows

    def cuts(self, core):
        firsts = [(self.calc_start(core, s), self.calc_rows) for s in range(self.steps)] + [(self.copy_start(core, c), self.copy_rows) for c in range(self.copies)]
        flat = [v for lo, rows in firsts for v in (lo, lo + rows)]
        return flat + [0] * (LANES - len(flat))


def run_pipe(x0, emb, w_up, w_down, labels, tokens, cuts, n_stage, plan):
    n_micro, seq = labels.shape
    dim, ffn = w_up.shape
    n_tok = n_micro * seq
    base = plan.base
    any_spec = pl.BlockSpec(memory_space=pl.ANY)
    act = (n_micro, seq, dim)
    fine = (n_tok // plan.part, plan.part, dim)
    wide = (n_micro, seq, ffn)
    dma = pltpu.SemaphoreType.DMA
    vm = pltpu.VMEM
    pair = 2 * seq
    return pl.pallas_call(
        functools.partial(pipe_kernel, n_stage, plan),
        out_shape=[
            jax.ShapeDtypeStruct(act, BF16), jax.ShapeDtypeStruct(fine, BF16), jax.ShapeDtypeStruct(wide, BF16),
            jax.ShapeDtypeStruct(wide, BF16), jax.ShapeDtypeStruct(act, BF16), jax.ShapeDtypeStruct(act, BF16),
            jax.ShapeDtypeStruct((n_stage, 8, pair), F32), jax.ShapeDtypeStruct((n_stage, 8, pair), F32), jax.ShapeDtypeStruct((2, plan.tiles * plan.rows, dim), F32),
            jax.ShapeDtypeStruct((3 * n_tok // LANES, LANES), jnp.int32),
        ],
        in_specs=[any_spec] * 4 + [pl.BlockSpec(memory_space=pltpu.VMEM)] * 3,
        out_specs=[any_spec] * 10,
        scratch_shapes=[
            vm(fine, BF16), vm(fine, BF16), vm(wide, BF16), vm(wide, BF16), vm(act, BF16), vm(act, BF16), vm(act, BF16), vm(act, BF16), vm(act, BF16),
            vm((dim, ffn), BF16), vm((ffn, dim), BF16), vm((ffn, dim), BF16), vm((dim, ffn), BF16),
            vm((base + plan.extra, dim), BF16), vm((base + plan.extra, pair), BF16), vm((dim, pair), BF16), vm((pair, dim), F32),
            vm((seq, dim), F32), vm((seq, dim), F32), vm((seq, dim), BF16), vm((16, pair), F32), vm((16, pair), F32), vm((n_stage, 8, pair), F32), vm((n_stage, 8, pair), F32),
            vm((2, 8, pair), F32), vm((dim, n_tok), BF16), vm((1, n_tok), F32), vm((plan.rows, n_tok), BF16), vm((plan.slots, plan.rows, dim), F32),
            vm((2, plan.head_tile, pair), BF16), vm((3 * n_tok // LANES, LANES), jnp.int32),
            dma((2,)), dma((2,)), dma((2,)), dma((2,)), dma((n_micro,)), dma, dma((n_tok // plan.part,)), dma, dma((n_micro,)), dma,
            dma((n_stage // 2,)), dma((n_micro,)), dma,
            dma((2,)), dma((2,)), dma, dma((n_stage,)), dma((2,)), dma((2,)), dma, dma((n_micro,)), dma((4,)), dma((n_micro,)), dma((2,)), dma((9,)),
            dma((plan.slots,)), dma((plan.shared,)), dma, dma,
        ],
        compiler_params=pltpu.CompilerParams(collective_id=0, has_side_effects=True, vmem_limit_bytes=67_000_000),
        cost_estimate=pl.CostEstimate(flops=60 * 10**9, bytes_accessed=100 * 10**6, transcendentals=0),
        name="pipe",
    )(x0.reshape(x0.shape[0], seq // plan.part, plan.part, dim), emb, w_up, w_down, labels.reshape(1, n_tok), tokens.reshape(1, n_tok), cuts)


def fin_kernel(n_stage, n_tok, plan, ids_ref, emb_hbm, tmp_hbm, n_hbm, stat_ref, part_ref, lab_ref, meta_ref, dx0_hbm, xs_hbm, hid_hbm, da_hbm, g_hbm,
               out_hbm, loss_ref, gup_hbm, gdown_hbm,
               n_all, dx0, xs, hid, da, g, n_t, x_t, dx0s, dz, shift, e_in, c_out, cp, gup, gdown,
               ld_sem, e_sem, t_sem, co_sem, po_sem, gu_sem, gd_sem, wi_sem):
    dim, ffn = gup_hbm.shape
    scale = dim ** -0.5
    inv_count = 1.0 / n_tok
    steps, crows, prows = plan.steps, plan.calc_rows, plan.copy_rows
    core = lax.rem(lax.axis_index("stage"), 2)
    early = plan.tiles * prows
    wblk = gup.shape[2]
    n_wblk = ffn // wblk
    turn = plan.calc_steps[0]

    def pick(pair):
        return jnp.where(core == 0, pair[0], pair[1])

    def calc_start(s):
        own = s < turn
        lo, hi = [jnp.where(own, pick([plan.spans[c][0][e] for c in range(2)]), pick([plan.spans[c][1][e] for c in range(2)])) for e in range(2)]
        return pl.multiple_of(jnp.minimum(lo + (s - jnp.where(own, 0, turn)) * crows, hi - crows), 16)

    def copy_start(c):
        own = c < plan.tiles
        first = jnp.where(own, pick([plan.starts[0][0], plan.starts[1][0]]), pick([plan.starts[1][0], plan.starts[0][0]]))
        return pl.multiple_of(first + (c - jnp.where(own, 0, plan.tiles)) * prows, 16)

    def e_copy(s):
        return pltpu.make_async_copy(emb_hbm.at[pl.ds(calc_start(s), crows)], e_in.at[lax.rem(s, 2)], e_sem.at[lax.rem(s, 2)])

    n_slot = cp.shape[0]
    ahead = 3

    def t_copy(c):
        own = c < plan.tiles
        row = jnp.where(own, core, 1 - core) * early + (c - jnp.where(own, 0, plan.tiles)) * prows
        slot = lax.rem(c, n_slot)
        return pltpu.make_async_copy(tmp_hbm.at[pl.ds(pl.multiple_of(row, 16), prows)], cp.at[slot], t_sem.at[slot])

    def p_out(c):
        slot = lax.rem(c, n_slot)
        return pltpu.make_async_copy(cp.at[slot], out_hbm.at[pl.ds(copy_start(c), prows)], po_sem.at[slot])

    def c_outs(s):
        slot = lax.rem(s, 2)
        return pltpu.make_async_copy(c_out.at[slot], out_hbm.at[pl.ds(calc_start(s), crows)], co_sem.at[slot])

    loads = [pltpu.make_async_copy(s, d, ld_sem.at[i]) for i, (s, d) in enumerate(((n_hbm, n_all), (dx0_hbm, dx0), (xs_hbm, xs), (g_hbm, g)))]
    loads[0].start()
    loads[1].start()
    e_copy(0).start()
    for c in range(ahead):
        t_copy(c).start(priority=1)
    pair = stat_ref.shape[2]
    loss = jnp.zeros((1, pair), F32)
    for d in range(n_stage):
        if d % 2 == 0:
            shift[:, (d // 2) * pair:(d // 2 + 1) * pair] = stat_ref[d, 0:1, :] * LOG2E + math.log2(n_tok)
        loss = loss + part_ref[d, 0:1, :]
    loss_ref[0] = jnp.sum(loss) * inv_count
    with jax.named_scope("fin_pre"):
        loads[0].wait()
        n_t[...] = n_all[...].T

    def sum_rows():
        loads[1].wait()
        dense = jnp.concatenate([meta_ref[g:g + 1, :] for g in range(n_tok // LANES)], axis=1)
        order = lax.broadcasted_iota(jnp.int32, (n_tok, n_tok), 0) == dense
        dx0s[...] = dot(jnp.where(order, 1.0, 0.0).astype(BF16), dx0[...])

    def add_rows(k, start, ref):
        lo, hi = ids_ref[2 * n_tok + k], ids_ref[2 * n_tok + k + 1]
        wide = 8

        def some(p, width):
            at = [pl.ds(ids_ref[n_tok + p + u] - start, 1) for u in range(width)]
            new = [ref[at[u], :] + dx0s[pl.ds(p + u, 1), :] for u in range(width)]
            for u in range(width):
                ref[at[u], :] = new[u]

        def group(g, carry):
            some(lo + g * wide, wide)
            return carry

        def single(p, carry):
            some(p, 1)
            return carry

        n_grp = (hi - lo) // wide
        lax.fori_loop(0, n_grp, group, 0)
        lax.fori_loop(lo + n_grp * wide, hi, single, 0)

    def w_ins(w):
        cols = pl.ds(pl.multiple_of(w * wblk, wblk), wblk)
        wslot = lax.rem(w, 2)
        return (pltpu.make_async_copy(da_hbm.at[:, cols], da.at[wslot], wi_sem.at[0, wslot]), pltpu.make_async_copy(hid_hbm.at[:, cols], hid.at[wslot], wi_sem.at[1, wslot]))

    def w_outs(w):
        cols = pl.ds(pl.multiple_of(w * wblk, wblk), wblk)
        wslot = lax.rem(w, 2)
        return (pltpu.make_async_copy(gup.at[wslot], gup_hbm.at[:, cols], gu_sem.at[wslot]), pltpu.make_async_copy(gdown.at[wslot], gdown_hbm.at[cols], gd_sem.at[wslot]))

    def copy_tile(c, carry):
        with jax.named_scope("copy_wait"):
            t_copy(c).wait()
        with jax.named_scope("add_p"):
            add_rows(2 * steps + 2 * c, copy_start(c), cp.at[lax.rem(c, n_slot)])
        p_out(c).start()

        @pl.when(c + ahead < plan.copies)
        def _():
            pl.when(c + ahead >= n_slot)(lambda: p_out(c + ahead - n_slot).wait())
            t_copy(c + ahead).start(priority=1)

        return carry

    w_first = 2
    tails = [turn - 1, steps - 1]

    def tail(s):
        return (s == tails[0]) | (s == tails[1])

    def step(s, carry):
        pl.when(s + 1 < steps)(lambda: e_copy(s + 1).start())
        with jax.named_scope("fin_wait"):
            e_copy(s).wait()

        @pl.when(s == 0)
        def _():
            for c in loads[2:]:
                c.start()

        w = s - w_first

        @pl.when((w + 1 >= 0) & (w + 1 < n_wblk))
        def _():
            for c in w_ins(w + 1):
                c.start()

        pl.when((s >= 2) & jnp.logical_not(tail(s - 1)))(lambda: c_outs(s - 2).wait())
        slot = lax.rem(s, 2)
        start = calc_start(s)
        with jax.named_scope("calc"):
            logit_grad(e_in[slot], n_t, shift, lab_ref, start, inv_count, scale, dz)
            c_out[slot] = dot(dz[...], n_all[...]) * scale
        pl.when(s == 0)(sum_rows)
        with jax.named_scope("add_c"):
            add_rows(2 * s, start, c_out.at[slot])
        pl.when(tail(s))(lambda: c_outs(s - 1).wait())
        c_outs(s).start()
        lax.fori_loop(s * plan.copies // (steps - 1), jnp.minimum((s + 1) * plan.copies // (steps - 1), plan.copies), copy_tile, 0)

        @pl.when(w == 0)
        def _():
            for c in loads[2:]:
                c.wait()
            x_t[...] = xs[...].T

        @pl.when((w >= 0) & (w < n_wblk))
        def _():
            wslot = lax.rem(w, 2)
            with jax.named_scope("dw_wait"):
                for c in w_ins(w):
                    c.wait()

                @pl.when(w >= 2)
                def _():
                    for c in w_outs(w - 2):
                        c.wait()

            with jax.named_scope("dw"):
                gup[wslot] = dot(x_t[...], da[wslot])
                gdown[wslot] = dot_t(hid[wslot], g[...])
            for c in w_outs(w):
                c.start()

        return carry

    lax.fori_loop(0, steps, step, 0)
    with jax.named_scope("fin_drain"):
        for w in range(n_wblk - 2, n_wblk):
            for c in w_outs(w):
                c.wait()
        c_outs(steps - 1).wait()
        for c in range(plan.copies - n_slot, plan.copies):
            p_out(c).wait()


def run_fin(emb, tmp, n_all, stats, losses, labels, meta, dx0, xs, hid, da, g, n_stage, plan):
    vocab, dim = emb.shape
    n_tok, ffn = hid.shape
    vm = pltpu.VMEM
    dma = pltpu.SemaphoreType.DMA
    any_spec = pl.BlockSpec(memory_space=pl.ANY)
    vspec = pl.BlockSpec(memory_space=pltpu.VMEM)
    smem = pl.BlockSpec(memory_space=pltpu.SMEM)
    wblk = 512
    return pl.pallas_call(
        functools.partial(fin_kernel, n_stage, n_tok, plan),
        out_shape=[jax.ShapeDtypeStruct((vocab, dim), F32), jax.ShapeDtypeStruct((1,), F32), jax.ShapeDtypeStruct((dim, ffn), F32), jax.ShapeDtypeStruct((ffn, dim), F32)],
        in_specs=[smem, any_spec, any_spec, any_spec, vspec, vspec, vspec, vspec] + [any_spec] * 5,
        out_specs=[any_spec, smem, any_spec, any_spec],
        scratch_shapes=[
            vm((n_tok, dim), BF16), vm((n_tok, dim), BF16), vm((n_tok, dim), BF16), vm((2, n_tok, wblk), BF16), vm((2, n_tok, wblk), BF16), vm((n_tok, dim), BF16),
            vm((dim, n_tok), BF16), vm((dim, n_tok), BF16), vm((n_tok, dim), F32), vm((plan.calc_rows, n_tok), BF16), vm((1, n_tok), F32),
            vm((2, plan.calc_rows, dim), BF16), vm((2, plan.calc_rows, dim), F32), vm((5, plan.copy_rows, dim), F32),
            vm((2, dim, wblk), F32), vm((2, wblk, dim), F32),
            dma((4,)), dma((2,)), dma((5,)), dma((2,)), dma((5,)), dma((2,)), dma((2,)), dma((2, 2)),
        ],
        compiler_params=pltpu.CompilerParams(vmem_limit_bytes=67_000_000),
        cost_estimate=pl.CostEstimate(flops=2 * n_tok * vocab * dim, bytes_accessed=5 * vocab * dim, transcendentals=0),
        name="fin",
    )(meta.reshape(-1), emb, tmp, n_all, stats, losses, labels.reshape(1, n_tok), meta, dx0, xs, hid, da, g)


def solution(mesh):
    n_stage = mesh.shape["stage"]

    def device_fn(tokens, labels, emb, w_up, w_down):
        n_micro, seq = tokens.shape
        vocab, dim = emb.shape
        w_up, w_down = w_up[0], w_down[0]
        n_tok = n_micro * seq
        plan = Plan(vocab, n_stage)
        cuts = jnp.array([plan.cuts(0), plan.cuts(1)], jnp.int32)
        x0 = run_gather(tokens, emb)
        n_all, xs, hid, da, g, dx0, stats, losses, tmp, meta = run_pipe(x0, emb, w_up, w_down, labels, tokens, cuts, n_stage, plan)
        flat = lambda p: p.reshape(n_tok, -1)
        grad_emb, loss, grad_up, grad_down = run_fin(
            emb, tmp.reshape(-1, dim), flat(n_all), stats, losses, labels, meta, flat(dx0), flat(xs), flat(hid), flat(da), flat(g), n_stage, plan
        )
        return loss, grad_up[None], grad_down[None], grad_emb

    return jax.shard_map(device_fn, mesh=mesh, in_specs=(P("dp", None), P("dp", None), P(None, None), P("stage", None, None), P("stage", None, None)), out_specs=(P("dp"), P(("dp", "stage"), None, None), P(("dp", "stage"), None, None), P("dp", None)), check_vma=False)
```

```python
import functools
import math

import jax
import jax.numpy as jnp
from jax import lax
from jax.experimental import pallas as pl
from jax.experimental.pallas import tpu as pltpu
from jax.sharding import PartitionSpec as P


MESH = pl.DeviceIdType.MESH
LOG2E = math.log2(math.e)
LN2 = math.log(2.0)
GELU_C = math.sqrt(2.0 / math.pi)
GELU_K = 0.044715
EPS = 1e-6
LANES = 128
F32 = jnp.float32
BF16 = jnp.bfloat16


def gelu_fwd(a):
    return (0.5 * a) * (1.0 + jnp.tanh(a * (GELU_C + (GELU_C * GELU_K) * (a * a))))


def gelu_slope(a):
    a2 = a * a
    half = 0.5 * jnp.tanh(a * (GELU_C + (GELU_C * GELU_K) * a2))
    up, down = 0.5 + half, 0.5 - half
    return up + (up * down) * (a * (2.0 * GELU_C + (6.0 * GELU_C * GELU_K) * a2))


def dot(x, y):
    return jnp.dot(x, y, preferred_element_type=F32)


def dot_t(x, y):
    return lax.dot_general(x, y, (((0,), (0,)), ((), ())), preferred_element_type=F32)


def remote(src, dst, send_sem, recv_sem, dev):
    return pltpu.make_async_remote_copy(src_ref=src, dst_ref=dst, send_sem=send_sem, recv_sem=recv_sem, device_id={"stage": dev}, device_id_type=MESH)


def column(row):
    return jnp.broadcast_to(row, (LANES, LANES)).T


def gather_kernel(ids_ref, tok_ref, emb_hbm, x0_hbm, tiles, picked, sem, out_sem):
    n_micro, seq = tok_ref.shape
    me = lax.axis_index("stage")
    group = tiles.shape[1] // seq
    slots = tiles.shape[0]
    owners = [head_chunk(me, k, n_micro) for k in range(slots)]

    def fetch(k):
        def one(i, carry):
            t = ids_ref[owners[k] * seq + i]
            start = pl.multiple_of(t // group * group, group)
            pltpu.make_async_copy(emb_hbm.at[pl.ds(start, group)], tiles.at[k, pl.ds(pl.multiple_of(i * group, group), group)], sem.at[k]).start()
            return carry

        lax.fori_loop(0, seq, one, 0, unroll=8)

    def select(k):
        sub = lax.broadcasted_iota(jnp.int32, (LANES, LANES), 0)
        lane = lax.broadcasted_iota(jnp.int32, (LANES, LANES), 1)
        tok = column(tok_ref[pl.ds(owners[k], 1), :].astype(F32)).astype(jnp.int32)
        want = sub * group + (tok - tok // group * group)
        hot = jnp.concatenate([jnp.where(lane + b * LANES == want, 1.0, 0.0).astype(BF16) for b in range(seq * group // LANES)], axis=1)
        pltpu.make_async_copy(emb_hbm.at[pl.ds(0, seq * group)], tiles.at[k], sem.at[k]).wait()
        picked[k] = dot(hot, tiles[k]).astype(BF16)
        pltpu.make_async_copy(picked.at[k], x0_hbm.at[k], out_sem.at[k]).start()

    def finish(k):
        pltpu.make_async_copy(picked.at[k], x0_hbm.at[k], out_sem.at[k]).wait()

    for work in (fetch, select, finish):
        work(0)
        for k in range(1, slots):
            pl.when(me < slots)(functools.partial(work, k))


def head_chunk(dev, k, n_micro):
    return jnp.minimum(jnp.where(dev < 2, 2 * dev + k, dev + 2), n_micro - 1)


def run_gather(tokens, emb):
    n_micro, seq = tokens.shape
    dim = emb.shape[1]
    group = 16
    return pl.pallas_call(
        gather_kernel,
        out_shape=jax.ShapeDtypeStruct((2, seq, dim), BF16),
        in_specs=[pl.BlockSpec(memory_space=pltpu.SMEM), pl.BlockSpec(memory_space=pltpu.VMEM), pl.BlockSpec(memory_space=pl.ANY)],
        out_specs=pl.BlockSpec(memory_space=pl.ANY),
        scratch_shapes=[pltpu.VMEM((2, seq * group, dim), BF16), pltpu.VMEM((2, seq, dim), BF16), pltpu.SemaphoreType.DMA((2,)), pltpu.SemaphoreType.DMA((2,))],
        cost_estimate=pl.CostEstimate(flops=10**9, bytes_accessed=2 * seq * group * dim * 2, transcendentals=0),
        name="gather",
    )(tokens.reshape(n_micro * seq), tokens, emb)


def token_table(row_ref, cut_ref, meta):
    n_tok = row_ref.shape[1]
    n_grp = n_tok // LANES
    lane = lax.broadcasted_iota(jnp.int32, (LANES, LANES), 1).astype(F32)
    sub = lax.broadcasted_iota(jnp.int32, (LANES, LANES), 0)
    row = lambda g: row_ref[:, g * LANES:(g + 1) * LANES].astype(F32)
    zero = jnp.zeros((LANES, LANES), F32)
    fold = lambda acc: jnp.sum(acc, axis=0, keepdims=True)
    cols = [column(row(c)) for c in range(n_grp)]
    firsts = []
    for g in range(n_grp):
        acc = zero
        for c in range(g + 1):
            same = cols[c] == row(g)
            if c == g:
                same = same & (sub < lane.astype(jnp.int32))
            acc = acc + jnp.where(same, 1.0, 0.0)
        firsts.append(column(jnp.where(fold(acc) == 0.0, 1.0, 0.0)))
    ranks = []
    for g in range(n_grp):
        acc = zero
        for c in range(n_grp):
            acc = acc + jnp.where(cols[c] < row(g), firsts[c], 0.0)
        ranks.append(fold(acc))
        meta[g:g + 1, :] = ranks[g].astype(jnp.int32)
    rank_cols = [column(r) for r in ranks]
    for g in range(n_grp):
        acc = zero
        for c in range(n_grp):
            acc = acc + jnp.where(rank_cols[c] == lane + g * LANES, firsts[c] * cols[c], 0.0)
        meta[n_grp + g:n_grp + g + 1, :] = fold(acc).astype(jnp.int32)
    cut = cut_ref[...].astype(F32)
    acc = zero
    for c in range(n_grp):
        acc = acc + jnp.where(cols[c] < cut, firsts[c], 0.0)
    meta[2 * n_grp:3 * n_grp, :] = jnp.broadcast_to(fold(acc), (n_grp, LANES)).astype(jnp.int32)


def logit_grad(e, n_t, shift, lab, first_id, inv_count, scale, dz):
    rows = e.shape[0]
    n_tok = n_t.shape[1]
    blk = 256
    vid = lax.broadcasted_iota(jnp.int32, (rows, blk), 0)
    for j in range(n_tok // blk):
        cols = slice(j * blk, (j + 1) * blk)
        z = (dot(e, n_t[:, cols]) * scale).astype(BF16).astype(F32)
        prob = jnp.exp2(z * LOG2E - shift[:, cols])
        dz[:, cols] = jnp.where(vid == lab[:, cols] - first_id, prob - inv_count, prob).astype(BF16)


def pipe_kernel(n_stage, plan, x0_hbm, emb_hbm, up_hbm, down_hbm, lab_ref, row_ref, cut_ref,
                n_out, xs_out, hid_out, da_out, g_out, dx0_out, stat_out, loss_out, tmp_out, meta_out,
                xbuf, ybuf, abuf, hbuf, nbuf, gbuf, dxbuf, dx0buf, dnbuf, up, down, up_t, down_t,
                emb, zbuf, n_t, dn_acc, dn_send, dn_recv, dn_own, st_send, st_recv, statall, lossall, tops, n_all_t, shift, dz, obuf, z_pair, meta,
                w_sem, e_sem, x_sem, x_send, x_recv, f_send, f_recv, n_send, n_recv, nf_send, ag_send, ag_recv, fw_send,
                st_sems, dp_sems, dn_ssem, dn_rsem, sa_sems, lo_sems, b_send, b_recv, d_send, d_recv, r_sems, out_sem, o_sem, od_send, od_recv, ic_send):
    n_micro, seq, dim = gbuf.shape
    part = xbuf.shape[1]
    n_part = xbuf.shape[0]
    per = seq // part
    n_tok = n_micro * seq
    ffn = up.shape[1]
    vocab = emb_hbm.shape[0]
    me = lax.axis_index("stage")
    core = lax.rem(me, 2)
    chip = me // 2
    mate = me + 1 - 2 * core
    last_id = n_stage - 1
    first = me == 0
    last = me == last_id
    fblk = 512
    n_fblk = ffn // fblk
    base, extra, tile = plan.base, plan.extra, plan.head_tile
    row0 = core * (base + extra)
    n_tiles = base // tile
    wide_tile = plan.grad_tile

    barrier = pltpu.get_barrier_semaphore()
    gives_x = (me >= 1) & (me + 2 < n_micro)

    def here(dev):
        pl.semaphore_signal(barrier, inc=1, device_id={"stage": dev}, device_id_type=MESH)

    pl.when(jnp.logical_not(first))(lambda: here(me - 1))
    pl.when(jnp.logical_not(last))(lambda: here(me + 1))

    @pl.when(first)
    def _():
        for dev in range(2, n_micro - 2):
            here(dev)

    w_copy = [pltpu.make_async_copy(up_hbm, up, w_sem.at[0]), pltpu.make_async_copy(down_hbm, down, w_sem.at[1])]
    for c in w_copy:
        c.start()
    x_slots = x0_hbm.shape[0]
    x_mine = [head_chunk(me, k, n_micro) for k in range(x_slots)]

    def x_rows(m):
        return xbuf.at[pl.ds(m * per, per)]

    def x_local(k):
        return pltpu.make_async_copy(x0_hbm.at[k], x_rows(k), x_sem.at[k])

    @pl.when(first)
    def _():
        for k in range(x_slots):
            x_local(k).start()

    e_parts = plan.e_parts
    e_step = base // e_parts

    def e_copy(i):
        src = emb_hbm.at[pl.ds(pl.multiple_of(row0 + i * e_step, 16), e_step)]
        return pltpu.make_async_copy(src, emb.at[pl.ds(i * e_step, e_step)], e_sem.at[0])

    e_more = pltpu.make_async_copy(emb_hbm.at[pl.ds(base, extra)], emb.at[pl.ds(base, extra)], e_sem.at[1])
    with jax.named_scope("entry"):
        pl.semaphore_wait(barrier, jnp.where(first | last, 1, 2) + jnp.where(gives_x & (me >= 2), 1, 0))

    def x_copy(k):
        return remote(x0_hbm.at[k], x_rows(x_mine[k]), x_send.at[k], x_recv.at[x_mine[k]], 0)

    @pl.when(gives_x)
    def _():
        x_copy(0).start()

        @pl.when(me < 2)
        def _():
            x_copy(1).start()

    with jax.named_scope("w_wait"):
        for c in w_copy:
            c.wait()
        for i in range(e_parts):
            e_copy(i).start()
        pl.when(core == 0)(e_more.start)

    def transpose_weights():
        for j in range(n_fblk):
            up_t[j * fblk:(j + 1) * fblk, :] = up[:, j * fblk:(j + 1) * fblk].T
            down_t[:, j * fblk:(j + 1) * fblk] = down[j * fblk:(j + 1) * fblk, :].T

    def idle_work():
        transpose_weights()
        token_table(row_ref, jnp.where(core == 0, cut_ref[0:1, :], cut_ref[1:2, :]), meta)

    @pl.when(chip >= n_stage // 4)
    def _():
        idle_work()

    def n_start(m):
        remote(nbuf.at[m], nbuf.at[m], n_send, n_recv.at[m], jnp.where(m == last_id, last_id - 1, m)).start()

    def fwd(h, carry):
        m = h // per
        sub = lax.rem(h, per)
        rows = pl.ds(pl.multiple_of(sub * part, part), part)
        with jax.named_scope("fwd_wait"):

            @pl.when(first & (sub == 0))
            def _():
                @pl.when(m < x_slots)
                def _():
                    x_local(m).wait()

                @pl.when(m >= x_slots)
                def _():
                    remote(x_rows(m), x_rows(m), x_send.at[0], x_recv.at[m], me).wait_recv()

            @pl.when(jnp.logical_not(first))
            def _():
                remote(xbuf.at[h], xbuf.at[h], f_send, f_recv.at[h], me).wait_recv()

        with jax.named_scope("fwd_comp"):
            x = xbuf[h]
            for j in range(n_fblk):
                cols = slice(j * fblk, (j + 1) * fblk)
                a = dot(x, up[:, cols]).astype(BF16)
                abuf[m, rows, cols] = a
                hbuf[m, rows, cols] = gelu_fwd(a.astype(F32)).astype(BF16)
            y = (x.astype(F32) + dot(hbuf[m, rows, :], down[...])).astype(BF16)
            ybuf[h] = y

        @pl.when(jnp.logical_not(last))
        def _():
            remote(ybuf.at[h], xbuf.at[h], f_send, f_recv.at[h], me + 1).start()

        @pl.when(last)
        def _():
            yf = y.astype(F32)
            inv = lax.rsqrt(jnp.mean(yf * yf, axis=-1, keepdims=True) + EPS)
            nbuf[m, rows, :] = (yf * inv).astype(BF16)
            pl.when(sub == per - 1)(lambda: n_start(m))

        @pl.when(sub == per - 1)
        def _():
            pltpu.make_async_copy(hbuf.at[m], hid_out.at[m], out_sem.at[0]).start()
            pltpu.make_async_copy(x_rows(m), xs_out.at[pl.ds(m * per, per)], out_sem.at[1]).start()

        return carry

    lax.fori_loop(0, n_part, fwd, 0)

    @pl.when(chip < n_stage // 4)
    def _():
        idle_work()

    n_forward = remote(nbuf.at[me], nbuf.at[me], nf_send, n_recv.at[me], mate)
    with jax.named_scope("n_wait"):

        @pl.when(jnp.logical_not(last))
        def _():
            remote(nbuf.at[me], nbuf.at[me], n_send, n_recv.at[me], me).wait_recv()
            pl.when(mate != last_id)(n_forward.start)
            remote(nbuf.at[mate], nbuf.at[mate], n_send, n_recv.at[mate], me).wait_recv()

        for k in range(2):
            n_t[:, k * seq:(k + 1) * seq] = nbuf[2 * chip + k].T

    peers = [lax.rem(me + 2 * d, n_stage) for d in range(1, n_stage // 2)]
    ag_copies = [remote(nbuf.at[me], nbuf.at[me], ag_send.at[d], ag_recv.at[me], p) for d, p in enumerate(peers)]
    for c, p in zip(ag_copies, peers):
        pl.when(p != last_id)(c.start)
    with jax.named_scope("e_wait"):
        pltpu.make_async_copy(emb_hbm.at[pl.ds(0, base)], emb.at[pl.ds(0, base)], e_sem.at[0]).wait()
        pl.when(core == 0)(e_more.wait)

    pair = 2 * seq
    scale = dim ** -0.5
    inv_count = 1.0 / n_tok
    log_count = math.log2(n_tok)
    lab = lab_ref[:, pl.ds(pl.multiple_of(chip * pair, pair), pair)]

    def logits(rows, size):
        e = emb[rows, :]
        parts = [dot(e[k * size // 2:(k + 1) * size // 2], n_t[...]) for k in range(2)]
        z = jnp.concatenate([(p * scale).astype(BF16) for p in parts], axis=0)
        zbuf[rows, :] = z
        return z

    def peak(z, size, top):
        best = jnp.max(z.reshape(size // 16, 16, pair), axis=0).astype(F32)
        return jnp.maximum(top, jnp.maximum(best[:8], best[8:]))

    def total(z, size, old, top, tot):
        off = top * LOG2E
        return tot * jnp.exp2(old * LOG2E - off) + jnp.sum(jnp.exp2(z.astype(F32).reshape(size // 8, 8, pair) * LOG2E - off[None]), axis=0)

    tops[0] = jnp.full((8, pair), -jnp.inf, F32)
    tops[1] = jnp.zeros((8, pair), F32)

    @pl.when(core == 0)
    def _():
        z = logits(pl.ds(base, extra), extra)
        top = peak(z, extra, tops[0])
        tops[1] = total(z, extra, tops[0], top, tops[1])
        tops[0] = top

    def logits_step(i, slot, old, top, tot):
        z = logits(pl.ds(pl.multiple_of(i * tile, 16), tile), tile)
        tot = total(z_pair[1 - slot], tile, old, top, tot)
        z_pair[slot] = z
        return top, peak(z, tile, top), tot

    with jax.named_scope("logits"):
        z = logits(pl.ds(0, tile), tile)
        z_pair[0] = z
        state = (tops[0], peak(z, tile, tops[0]), tops[1])
        state = lax.fori_loop(0, (n_tiles - 1) // 2, lambda i, c: logits_step(2 * i + 2, 0, *logits_step(2 * i + 1, 1, *c)), state)
        if n_tiles % 2 == 0:
            state = logits_step(n_tiles - 1, 1, *state)
        old, top, tot = state
        tot = total(z_pair[(n_tiles - 1) % 2], tile, old, top, tot)
    row_top = jnp.max(top, axis=0, keepdims=True)
    row_tot = jnp.sum(tot * jnp.exp2((top - row_top) * LOG2E), axis=0, keepdims=True)
    st_send[0:8, :] = jnp.broadcast_to(row_top, (8, pair))
    st_send[8:16, :] = jnp.broadcast_to(row_tot, (8, pair))
    st_copy = remote(st_send, st_recv, st_sems.at[0], st_sems.at[1], mate)
    with jax.named_scope("stat_x"):
        st_copy.start()
        st_copy.wait()
    far_top = st_recv[0:1, :]
    far_tot = st_recv[8:9, :]
    all_top = jnp.maximum(row_top, far_top)
    mine = row_tot * jnp.exp(row_top - all_top)
    other = far_tot * jnp.exp(far_top - all_top)
    lse = all_top + jnp.log(jnp.where(core == 0, mine + other, other + mine))
    my_shift = lse * LOG2E + log_count
    others = [lax.rem(me + d, n_stage) for d in range(1, n_stage)]

    def spread(buf, sems):
        whole = buf.at[pl.ds(0, n_stage - 1)]
        return [remote(buf.at[me], buf.at[me], sems.at[0], sems.at[1], p) for p in others], remote(whole, whole, sems.at[0], sems.at[1], me)

    statall[me] = jnp.broadcast_to(lse, (8, pair))
    sa_copies, sa_all = spread(statall, sa_sems)
    for c in sa_copies:
        c.start()

    def grads(rows, size, first_row, picked):
        zf = zbuf[rows, :].astype(F32)
        prob = jnp.exp2(zf * LOG2E - my_shift)
        hit = lax.broadcasted_iota(jnp.int32, (size, pair), 0) == lab - (row0 + first_row)
        dz_t = jnp.where(hit, prob - inv_count, prob).astype(BF16)
        got = jnp.where(hit, zf, 0.0).reshape(size // 8, 8, pair)
        return dot_t(dz_t, emb[rows, :]), picked + jnp.sum(got, axis=0)

    tops[0] = jnp.zeros((8, pair), F32)
    dn_acc[...] = jnp.zeros_like(dn_acc)

    @pl.when(core == 0)
    def _():
        dn_acc[...], tops[0] = grads(pl.ds(base, extra), extra, base, tops[0])

    def grad_step(i, picked):
        part, picked = grads(pl.ds(pl.multiple_of(i * wide_tile, 16), wide_tile), wide_tile, i * wide_tile, picked)
        dn_acc[...] += part
        return picked

    with jax.named_scope("grads"):
        picked = lax.fori_loop(0, base // wide_tile, grad_step, tops[0])
    far = pl.ds(pl.multiple_of((1 - core) * seq, seq), seq)
    near = pl.ds(pl.multiple_of(core * seq, seq), seq)
    dn_send[...] = dn_acc[far, :]
    dp_copy = remote(dn_send, dn_recv, dp_sems.at[0], dp_sems.at[1], mate)
    dp_copy.start()
    row_loss = jnp.where(core == 0, lse, 0.0) - jnp.sum(picked, axis=0, keepdims=True)
    lossall[me] = jnp.broadcast_to(row_loss, (8, pair))
    lo_copies, lo_all = spread(lossall, lo_sems)
    for c in lo_copies:
        c.start()
    with jax.named_scope("dn_x"):
        dp_copy.wait()
        dn = ((dn_acc[near, :] + dn_recv[...]) * scale).astype(BF16)
    dn_copy = remote(dn_own, dnbuf.at[me], dn_ssem, dn_rsem.at[me], last_id)

    @pl.when(last)
    def _():
        dnbuf[last_id] = dn

    @pl.when(jnp.logical_not(last))
    def _():
        dn_own[...] = dn
        remote(dn_own, dnbuf.at[me], dn_ssem, dn_rsem.at[me], last_id).start()

    with jax.named_scope("ag_wait"):
        for p in peers:
            got = remote(nbuf.at[p], nbuf.at[p], ag_send.at[0], ag_recv.at[p], me)
            pl.when(jnp.logical_not(last))(got.wait_recv)
            pl.when(mate != last_id)(remote(nbuf.at[p], nbuf.at[p], fw_send, ag_recv.at[p], mate).start)

    near_dst = [1, 3, last_id]
    far_dst = n_stage // 2 + 1
    direct = n_micro - 1
    by_prev = n_micro - 3
    hands_on = (core == 1) & (me != 1)

    def dx0_start(m, k, dev):
        remote(dxbuf.at[m], dx0buf.at[m], d_send.at[k], d_recv.at[m], dev).start()

    def relayed(m):
        return (m < direct) & (((me == 3) & (m != by_prev)) | (last & (m == by_prev)))

    def relay_far(m):
        remote(dx0buf.at[m], dx0buf.at[m], r_sems.at[1], d_recv.at[m], far_dst).start()

    def bwd(m):
        with jax.named_scope("bwd_wait"):
            @pl.when(jnp.logical_not(last))
            def _():
                remote(gbuf.at[m], gbuf.at[m], b_send, b_recv.at[m], me).wait_recv()

            @pl.when(last)
            def _():
                @pl.when(m != last_id)
                def _():
                    remote(dnbuf.at[m], dnbuf.at[m], dn_ssem, dn_rsem.at[m], me).wait_recv()

                yf = ybuf[pl.ds(m * per, per)].reshape(seq, dim).astype(F32)
                inv = lax.rsqrt(jnp.mean(yf * yf, axis=-1, keepdims=True) + EPS)
                dnf = dnbuf[m].astype(F32)
                proj = jnp.mean(yf * dnf, axis=-1, keepdims=True)
                gbuf[m] = (dnf * inv - yf * (inv * inv * inv * proj)).astype(BF16)

        with jax.named_scope("bwd_comp"):
            g = gbuf[m]
            for j in range(n_fblk):
                cols = slice(j * fblk, (j + 1) * fblk)
                dh = dot(g, down_t[:, cols]).astype(BF16).astype(F32)
                abuf[m, :, cols] = (dh * gelu_slope(abuf[m, :, cols].astype(F32))).astype(BF16)
            dxbuf[m] = (g.astype(F32) + dot(abuf[m], up_t[...])).astype(BF16)

        @pl.when(jnp.logical_not(first))
        def _():
            remote(dxbuf.at[m], gbuf.at[m], b_send, b_recv.at[m], me - 1).start()

        @pl.when(first)
        def _():
            pl.when(m >= direct)(lambda: dx0_start(m, len(near_dst), far_dst))
            for k, dev in enumerate(near_dst):
                dx0_start(m, k, dev)

        pltpu.make_async_copy(abuf.at[m], da_out.at[m], out_sem.at[2]).start()
        pltpu.make_async_copy(gbuf.at[m], g_out.at[m], out_sem.at[3]).start()

    n_slot = obuf.shape[0]
    busy = chip == last_id // 2
    far_tile = remote(tmp_out.at[core, pl.ds(0, plan.rows)], tmp_out.at[core, pl.ds(0, plan.rows)], ic_send, od_recv, jnp.where(first, last_id, last_id - 1))
    sends_far = first | (me == last_id - 2)

    def tile_copy(k):
        rows = pl.ds(pl.multiple_of(k * plan.rows, plan.rows), plan.rows)
        slot = lax.rem(k, n_slot)
        return pltpu.make_async_copy(obuf.at[slot], tmp_out.at[core, rows], o_sem.at[slot])

    def piece(p):
        k = p // plan.per_tile
        rows = pl.ds(pl.multiple_of(p * plan.piece, plan.piece), plan.piece)
        here = pl.ds(pl.multiple_of(lax.rem(p, plan.per_tile) * plan.piece, plan.piece), plan.piece)
        return remote(obuf.at[lax.rem(k, n_slot), here], tmp_out.at[core, rows], od_send.at[k], od_recv, mate)

    def tile_sent(k):
        slot = lax.rem(k, n_slot)
        return remote(obuf.at[slot], tmp_out.at[core, pl.ds(0, plan.rows)], od_send.at[k], od_recv, mate)

    def emb_tile(k):
        with jax.named_scope("tile_prep"):

            @pl.when(k == 0)
            def _():
                for d in range(1, n_stage // 2):
                    src = lax.rem(mate + 2 * d, n_stage)
                    pl.when(jnp.logical_not(last))(remote(nbuf.at[src], nbuf.at[src], ag_send.at[0], ag_recv.at[src], me).wait_recv)
                for m in range(n_micro):
                    n_all_t[:, m * seq:(m + 1) * seq] = nbuf[m].T
                sa_all.wait_recv()
                for c in range(n_stage // 2):
                    shift[:, c * pair:(c + 1) * pair] = statall[2 * c, 0:1, :] * LOG2E + log_count

        slot = lax.rem(k, n_slot)
        with jax.named_scope("tile_wait"):
            @pl.when(k == 2)
            def _():
                tile_copy(0).wait()
                pl.when(sends_far)(far_tile.start)

            pl.when(k > n_slot)(lambda: tile_copy(k - n_slot).wait())
            pl.when((k >= n_slot) & (k - n_slot < plan.shared) & jnp.logical_not(busy & (k == n_slot)))(lambda: tile_sent(k - n_slot).wait_send())

        with jax.named_scope("tile"):
            rows = pl.ds(pl.multiple_of(k * plan.rows, plan.rows), plan.rows)
            logit_grad(emb[rows, :], n_all_t, shift, lab_ref, row0 + k * plan.rows, inv_count, scale, dz)
            obuf[slot] = dot(dz[...], nbuf[...].reshape(n_tok, dim)) * scale

        tile_copy(k).start()

    def send_pieces(done, until):
        lax.fori_loop(done, until, lambda p, c: (piece(p).start(), c)[1], 0)

    def send_tiles(done, until):
        def one(k, carry):
            rows = pl.ds(pl.multiple_of(k * plan.rows, plan.rows), plan.rows)
            remote(obuf.at[lax.rem(k, n_slot)], tmp_out.at[core, rows], od_send.at[k], od_recv, mate).start()
            return carry

        lax.fori_loop(done, until, one, 0)

    before = sum(jnp.where(me == s, plan.before[s], 0) for s in range(n_stage))

    def pass_dx0(m, carry):
        @pl.when(jnp.logical_not(first))
        def _():
            remote(dx0buf.at[m], dx0buf.at[m], r_sems.at[0], d_recv.at[m], me).wait_recv()

            @pl.when(hands_on)
            def _():
                remote(dx0buf.at[m], dx0buf.at[m], r_sems.at[0], d_recv.at[m], mate).start()

            @pl.when(relayed(m))
            def _():
                relay_far(m)

            pltpu.make_async_copy(dx0buf.at[m], dx0_out.at[m], out_sem.at[4]).start()

        @pl.when(first)
        def _():
            pltpu.make_async_copy(dxbuf.at[m], dx0_out.at[m], out_sem.at[4]).start()

        return carry

    lead = jnp.where(me == 3, -300, jnp.where(last, -1800, jnp.where(me == far_dst, -1600, -10**6)))

    def work(i, carry):
        sent, passed = carry
        chunk = (i >= before) & (i < before + n_micro)
        pl.when(chunk)(lambda: bwd(i - before))
        k = jnp.where(i < before, i, i - n_micro)
        pl.when(jnp.logical_not(chunk))(lambda: emb_tile(k))
        after = i - before - n_micro + 1
        here = jnp.where(after > 0, jnp.clip((after * 264 + lead) // 138, 0, n_micro), 0)
        lax.fori_loop(passed, here, pass_dx0, 0)
        ready = jnp.where(i < before, i + 1, jnp.where(chunk, before, i + 1 - n_micro))
        near_chunks = chunk | ((i < before) & (i + 1 >= before))
        whole = (sent + plan.per_tile - 1) // plan.per_tile
        upto = jnp.minimum(jnp.minimum(ready, plan.shared), whole + 1)
        some = jnp.where(near_chunks, jnp.minimum(sent + 1, jnp.minimum(ready, plan.shared) * plan.per_tile), whole * plan.per_tile)
        send_pieces(sent, some)
        send_tiles(whole, jnp.where(near_chunks, 0, upto))
        now = jnp.where(near_chunks, some, jnp.maximum(some, upto * plan.per_tile))
        return jnp.maximum(sent, now), jnp.maximum(passed, here)

    sent, passed = lax.fori_loop(0, plan.tiles + n_micro, work, (jnp.where(busy, plan.per_tile, 0), 0))
    outs = [pltpu.make_async_copy(nbuf, n_out, out_sem.at[5]), pltpu.make_async_copy(lossall, loss_out, out_sem.at[6]), pltpu.make_async_copy(meta, meta_out, out_sem.at[7])]
    lo_all.wait_recv()
    for c in outs:
        c.start()
    pltpu.make_async_copy(statall, stat_out, out_sem.at[8]).start()
    with jax.named_scope("relay_all"):
        lax.fori_loop(passed, n_micro, pass_dx0, 0)

    with jax.named_scope("drain"):
        send_pieces(sent, plan.shared * plan.per_tile)
        for k in range(max(plan.tiles - n_slot, 0), plan.tiles):
            tile_copy(k).wait()
            if k < plan.shared:
                tile_sent(k).wait_send()
        pl.when(sends_far)(far_tile.wait_send)
        all_rows = pl.ds(0, plan.shared * plan.rows)
        remote(tmp_out.at[1 - core, all_rows], tmp_out.at[1 - core, all_rows], od_send.at[0], od_recv, me).wait_recv()
        sa_all.wait_send()
        lo_all.wait_send()
        pltpu.make_async_copy(statall, stat_out, out_sem.at[8]).wait()
        for c, p in zip(ag_copies, peers):
            pl.when(p != last_id)(c.wait_send)

        @pl.when(jnp.logical_not(last))
        def _():
            dn_copy.wait_send()
            pl.when(mate != last_id)(n_forward.wait_send)
            remote(ybuf, xbuf, f_send, f_recv.at[0], me + 1).wait_send()

        @pl.when(last)
        def _():
            remote(nbuf, nbuf, n_send, n_recv.at[0], me).wait_send()

        @pl.when(mate != last_id)
        def _():
            some = nbuf.at[pl.ds(0, len(peers))]
            remote(some, some, fw_send, ag_recv.at[0], mate).wait_send()

        @pl.when(gives_x)
        def _():
            x_copy(0).wait_send()

            @pl.when(me < 2)
            def _():
                x_copy(1).wait_send()

        @pl.when(jnp.logical_not(first))
        def _():
            remote(dxbuf, gbuf, b_send, b_recv.at[0], me).wait_send()
            pl.when(hands_on)(remote(dx0buf, dx0buf, r_sems.at[0], d_recv.at[0], mate).wait_send)

        @pl.when(first)
        def _():
            for k in range(len(near_dst)):
                remote(dxbuf, dx0buf, d_send.at[k], d_recv.at[0], me).wait_send()
            rest = pl.ds(0, n_micro - direct)
            remote(dxbuf.at[rest], dx0buf.at[rest], d_send.at[len(near_dst)], d_recv.at[0], me).wait_send()

        for dev, kept in ((3, direct - 1), (last_id, 1)):
            some = dx0buf.at[pl.ds(0, kept)]
            pl.when(me == dev)(remote(some, some, r_sems.at[1], d_recv.at[0], me).wait_send)

        pltpu.make_async_copy(hbuf, hid_out, out_sem.at[0]).wait()
        pltpu.make_async_copy(xbuf, xs_out, out_sem.at[1]).wait()
        pltpu.make_async_copy(abuf, da_out, out_sem.at[2]).wait()
        pltpu.make_async_copy(gbuf, g_out, out_sem.at[3]).wait()
        pltpu.make_async_copy(dx0buf, dx0_out, out_sem.at[4]).wait()
        for c in outs:
            c.wait()


class Plan:
    def __init__(self, vocab, n_stage):
        units = vocab // LANES
        self.base = units // 2 * LANES
        self.extra = vocab - 2 * self.base
        self.head_tile = next(t for t in (1600, 1536, 1280, 1024, 768, 640, 512, 256, 128) if self.base % t == 0)
        self.rows = 1024
        self.tiles, self.shared = 11, 9
        self.grad_tile = next(t for t in (4000, 3200, 1600, 1280, 640, 256, 128) if self.base % t == 0)
        self.e_parts = next(k for k in (10, 8, 5, 4, 2, 1) if self.base % (16 * k) == 0)
        self.part = 128
        self.slots = 4
        self.piece = 256
        self.per_tile = self.rows // self.piece
        measured = [10, 9, 6, 5, 3, 2, 0, 0]
        self.before = (measured + [0] * n_stage)[:n_stage]
        mid = self.base + self.extra
        ends = [(0, mid), (mid, vocab)]
        early = (self.tiles * self.rows, self.shared * self.rows)
        self.spans = [[(ends[h][0] + early[0 if h == c else 1], ends[h][1]) for h in (c, 1 - c)] for c in range(2)]
        self.longest = [max(self.spans[c][k][1] - self.spans[c][k][0] for c in range(2)) for k in range(2)]
        best = min(range(16, 1281, 16), key=lambda r: (sum(-(-n // r) for n in self.longest)) * (r + 40))
        self.calc_rows = best
        self.calc_steps = [-(-n // best) for n in self.longest]
        self.steps = sum(self.calc_steps)
        self.copy_rows = self.rows
        self.copies = self.tiles + self.shared
        self.starts = ends

    def calc_start(self, core, s):
        k = 0 if s < self.calc_steps[0] else 1
        lo, hi = self.spans[core][k]
        return min(lo + (s - k * self.calc_steps[0]) * self.calc_rows, hi - self.calc_rows)

    def copy_start(self, core, c):
        own = c < self.tiles
        h = core if own else 1 - core
        return self.starts[h][0] + (c if own else c - self.tiles) * self.copy_rows

    def cuts(self, core):
        firsts = [(self.calc_start(core, s), self.calc_rows) for s in range(self.steps)] + [(self.copy_start(core, c), self.copy_rows) for c in range(self.copies)]
        flat = [v for lo, rows in firsts for v in (lo, lo + rows)]
        return flat + [0] * (LANES - len(flat))


def run_pipe(x0, emb, w_up, w_down, labels, tokens, cuts, n_stage, plan):
    n_micro, seq = labels.shape
    dim, ffn = w_up.shape
    n_tok = n_micro * seq
    base = plan.base
    any_spec = pl.BlockSpec(memory_space=pl.ANY)
    act = (n_micro, seq, dim)
    fine = (n_tok // plan.part, plan.part, dim)
    wide = (n_micro, seq, ffn)
    dma = pltpu.SemaphoreType.DMA
    vm = pltpu.VMEM
    pair = 2 * seq
    return pl.pallas_call(
        functools.partial(pipe_kernel, n_stage, plan),
        out_shape=[
            jax.ShapeDtypeStruct(act, BF16), jax.ShapeDtypeStruct(fine, BF16), jax.ShapeDtypeStruct(wide, BF16),
            jax.ShapeDtypeStruct(wide, BF16), jax.ShapeDtypeStruct(act, BF16), jax.ShapeDtypeStruct(act, BF16),
            jax.ShapeDtypeStruct((n_stage, 8, pair), F32), jax.ShapeDtypeStruct((n_stage, 8, pair), F32), jax.ShapeDtypeStruct((2, plan.tiles * plan.rows, dim), F32),
            jax.ShapeDtypeStruct((3 * n_tok // LANES, LANES), jnp.int32),
        ],
        in_specs=[any_spec] * 4 + [pl.BlockSpec(memory_space=pltpu.VMEM)] * 3,
        out_specs=[any_spec] * 10,
        scratch_shapes=[
            vm(fine, BF16), vm(fine, BF16), vm(wide, BF16), vm(wide, BF16), vm(act, BF16), vm(act, BF16), vm(act, BF16), vm(act, BF16), vm(act, BF16),
            vm((dim, ffn), BF16), vm((ffn, dim), BF16), vm((ffn, dim), BF16), vm((dim, ffn), BF16),
            vm((base + plan.extra, dim), BF16), vm((base + plan.extra, pair), BF16), vm((dim, pair), BF16), vm((pair, dim), F32),
            vm((seq, dim), F32), vm((seq, dim), F32), vm((seq, dim), BF16), vm((16, pair), F32), vm((16, pair), F32), vm((n_stage, 8, pair), F32), vm((n_stage, 8, pair), F32),
            vm((2, 8, pair), F32), vm((dim, n_tok), BF16), vm((1, n_tok), F32), vm((plan.rows, n_tok), BF16), vm((plan.slots, plan.rows, dim), F32),
            vm((2, plan.head_tile, pair), BF16), vm((3 * n_tok // LANES, LANES), jnp.int32),
            dma((2,)), dma((2,)), dma((2,)), dma((2,)), dma((n_micro,)), dma, dma((n_tok // plan.part,)), dma, dma((n_micro,)), dma,
            dma((n_stage // 2,)), dma((n_micro,)), dma,
            dma((2,)), dma((2,)), dma, dma((n_stage,)), dma((2,)), dma((2,)), dma, dma((n_micro,)), dma((4,)), dma((n_micro,)), dma((2,)), dma((9,)),
            dma((plan.slots,)), dma((plan.shared,)), dma, dma,
        ],
        compiler_params=pltpu.CompilerParams(collective_id=0, has_side_effects=True, vmem_limit_bytes=67_000_000),
        cost_estimate=pl.CostEstimate(flops=60 * 10**9, bytes_accessed=100 * 10**6, transcendentals=0),
        name="pipe",
    )(x0.reshape(x0.shape[0], seq // plan.part, plan.part, dim), emb, w_up, w_down, labels.reshape(1, n_tok), tokens.reshape(1, n_tok), cuts)


def fin_kernel(n_stage, n_tok, plan, ids_ref, emb_hbm, tmp_hbm, n_hbm, stat_ref, part_ref, lab_ref, meta_ref, dx0_hbm, xs_hbm, hid_hbm, da_hbm, g_hbm,
               out_hbm, loss_ref, gup_hbm, gdown_hbm,
               n_all, dx0, xs, hid, da, g, n_t, x_t, dx0s, dz, shift, e_in, c_out, cp, gup, gdown,
               ld_sem, e_sem, t_sem, co_sem, po_sem, gu_sem, gd_sem, wi_sem):
    dim, ffn = gup_hbm.shape
    scale = dim ** -0.5
    inv_count = 1.0 / n_tok
    steps, crows, prows = plan.steps, plan.calc_rows, plan.copy_rows
    core = lax.rem(lax.axis_index("stage"), 2)
    early = plan.tiles * prows
    wblk = gup.shape[2]
    n_wblk = ffn // wblk
    turn = plan.calc_steps[0]

    def pick(pair):
        return jnp.where(core == 0, pair[0], pair[1])

    def calc_start(s):
        own = s < turn
        lo, hi = [jnp.where(own, pick([plan.spans[c][0][e] for c in range(2)]), pick([plan.spans[c][1][e] for c in range(2)])) for e in range(2)]
        return pl.multiple_of(jnp.minimum(lo + (s - jnp.where(own, 0, turn)) * crows, hi - crows), 16)

    def copy_start(c):
        own = c < plan.tiles
        first = jnp.where(own, pick([plan.starts[0][0], plan.starts[1][0]]), pick([plan.starts[1][0], plan.starts[0][0]]))
        return pl.multiple_of(first + (c - jnp.where(own, 0, plan.tiles)) * prows, 16)

    def e_copy(s):
        return pltpu.make_async_copy(emb_hbm.at[pl.ds(calc_start(s), crows)], e_in.at[lax.rem(s, 2)], e_sem.at[lax.rem(s, 2)])

    n_slot = cp.shape[0]
    ahead = 6

    def t_copy(c):
        own = c < plan.tiles
        row = jnp.where(own, core, 1 - core) * early + (c - jnp.where(own, 0, plan.tiles)) * prows
        slot = lax.rem(c, n_slot)
        return pltpu.make_async_copy(tmp_hbm.at[pl.ds(pl.multiple_of(row, 16), prows)], cp.at[slot], t_sem.at[slot])

    def p_out(c):
        slot = lax.rem(c, n_slot)
        return pltpu.make_async_copy(cp.at[slot], out_hbm.at[pl.ds(copy_start(c), prows)], po_sem.at[slot])

    def c_outs(s):
        slot = lax.rem(s, 2)
        return pltpu.make_async_copy(c_out.at[slot], out_hbm.at[pl.ds(calc_start(s), crows)], co_sem.at[slot])

    loads = [pltpu.make_async_copy(s, d, ld_sem.at[i]) for i, (s, d) in enumerate(((n_hbm, n_all), (dx0_hbm, dx0), (xs_hbm, xs), (g_hbm, g)))]
    loads[0].start()
    loads[1].start()
    e_copy(0).start()
    for c in range(ahead):
        t_copy(c).start(priority=1)
    pair = stat_ref.shape[2]
    loss = jnp.zeros((1, pair), F32)
    for d in range(n_stage):
        if d % 2 == 0:
            shift[:, (d // 2) * pair:(d // 2 + 1) * pair] = stat_ref[d, 0:1, :] * LOG2E + math.log2(n_tok)
        loss = loss + part_ref[d, 0:1, :]
    loss_ref[0] = jnp.sum(loss) * inv_count
    with jax.named_scope("fin_pre"):
        loads[0].wait()
        n_t[...] = n_all[...].T

    def sum_rows():
        loads[1].wait()
        dense = jnp.concatenate([meta_ref[g:g + 1, :] for g in range(n_tok // LANES)], axis=1)
        order = lax.broadcasted_iota(jnp.int32, (n_tok, n_tok), 0) == dense
        dx0s[...] = dot(jnp.where(order, 1.0, 0.0).astype(BF16), dx0[...])

    def add_rows(k, start, ref):
        lo, hi = ids_ref[2 * n_tok + k], ids_ref[2 * n_tok + k + 1]
        wide = 8

        def some(p, width):
            at = [pl.ds(ids_ref[n_tok + p + u] - start, 1) for u in range(width)]
            new = [ref[at[u], :] + dx0s[pl.ds(p + u, 1), :] for u in range(width)]
            for u in range(width):
                ref[at[u], :] = new[u]

        def group(g, carry):
            some(lo + g * wide, wide)
            return carry

        def single(p, carry):
            some(p, 1)
            return carry

        n_grp = (hi - lo) // wide
        lax.fori_loop(0, n_grp, group, 0)
        lax.fori_loop(lo + n_grp * wide, hi, single, 0)

    def w_ins(w):
        cols = pl.ds(pl.multiple_of(w * wblk, wblk), wblk)
        wslot = lax.rem(w, 2)
        return (pltpu.make_async_copy(da_hbm.at[:, cols], da.at[wslot], wi_sem.at[0, wslot]), pltpu.make_async_copy(hid_hbm.at[:, cols], hid.at[wslot], wi_sem.at[1, wslot]))

    def w_outs(w):
        cols = pl.ds(pl.multiple_of(w * wblk, wblk), wblk)
        wslot = lax.rem(w, 2)
        return (pltpu.make_async_copy(gup.at[wslot], gup_hbm.at[:, cols], gu_sem.at[wslot]), pltpu.make_async_copy(gdown.at[wslot], gdown_hbm.at[cols], gd_sem.at[wslot]))

    def copy_tile(c, carry):
        with jax.named_scope("copy_wait"):
            t_copy(c).wait()
        with jax.named_scope("add_p"):
            add_rows(2 * steps + 2 * c, copy_start(c), cp.at[lax.rem(c, n_slot)])
        p_out(c).start()

        @pl.when(c + ahead < plan.copies)
        def _():
            pl.when(c + ahead >= n_slot)(lambda: p_out(c + ahead - n_slot).wait())
            t_copy(c + ahead).start(priority=1)

        return carry

    w_first = 2
    tails = [turn - 1, steps - 1]

    def tail(s):
        return (s == tails[0]) | (s == tails[1])

    def step(s, carry):
        pl.when(s + 1 < steps)(lambda: e_copy(s + 1).start())
        with jax.named_scope("fin_wait"):
            e_copy(s).wait()

        @pl.when(s == 0)
        def _():
            for c in loads[2:]:
                c.start()

        w = s - w_first

        @pl.when((w + 1 >= 0) & (w + 1 < n_wblk))
        def _():
            for c in w_ins(w + 1):
                c.start()

        pl.when((s >= 2) & jnp.logical_not(tail(s - 1)))(lambda: c_outs(s - 2).wait())
        slot = lax.rem(s, 2)
        start = calc_start(s)
        with jax.named_scope("calc"):
            logit_grad(e_in[slot], n_t, shift, lab_ref, start, inv_count, scale, dz)
            c_out[slot] = dot(dz[...], n_all[...]) * scale
        pl.when(s == 0)(sum_rows)
        with jax.named_scope("add_c"):
            add_rows(2 * s, start, c_out.at[slot])
        pl.when(tail(s))(lambda: c_outs(s - 1).wait())
        c_outs(s).start()
        lax.fori_loop(s * plan.copies // (steps - 1), jnp.minimum((s + 1) * plan.copies // (steps - 1), plan.copies), copy_tile, 0)

        @pl.when(w == 0)
        def _():
            for c in loads[2:]:
                c.wait()
            x_t[...] = xs[...].T

        @pl.when((w >= 0) & (w < n_wblk))
        def _():
            wslot = lax.rem(w, 2)
            with jax.named_scope("dw_wait"):
                for c in w_ins(w):
                    c.wait()

                @pl.when(w >= 2)
                def _():
                    for c in w_outs(w - 2):
                        c.wait()

            with jax.named_scope("dw"):
                gup[wslot] = dot(x_t[...], da[wslot])
                gdown[wslot] = dot_t(hid[wslot], g[...])
            for c in w_outs(w):
                c.start()

        return carry

    lax.fori_loop(0, steps, step, 0)
    with jax.named_scope("fin_drain"):
        for w in range(n_wblk - 2, n_wblk):
            for c in w_outs(w):
                c.wait()
        c_outs(steps - 1).wait()
        for c in range(plan.copies - n_slot, plan.copies):
            p_out(c).wait()


def run_fin(emb, tmp, n_all, stats, losses, labels, meta, dx0, xs, hid, da, g, n_stage, plan):
    vocab, dim = emb.shape
    n_tok, ffn = hid.shape
    vm = pltpu.VMEM
    dma = pltpu.SemaphoreType.DMA
    any_spec = pl.BlockSpec(memory_space=pl.ANY)
    vspec = pl.BlockSpec(memory_space=pltpu.VMEM)
    smem = pl.BlockSpec(memory_space=pltpu.SMEM)
    wblk = 512
    return pl.pallas_call(
        functools.partial(fin_kernel, n_stage, n_tok, plan),
        out_shape=[jax.ShapeDtypeStruct((vocab, dim), F32), jax.ShapeDtypeStruct((1,), F32), jax.ShapeDtypeStruct((dim, ffn), F32), jax.ShapeDtypeStruct((ffn, dim), F32)],
        in_specs=[smem, any_spec, any_spec, any_spec, vspec, vspec, vspec, vspec] + [any_spec] * 5,
        out_specs=[any_spec, smem, any_spec, any_spec],
        scratch_shapes=[
            vm((n_tok, dim), BF16), vm((n_tok, dim), BF16), vm((n_tok, dim), BF16), vm((2, n_tok, wblk), BF16), vm((2, n_tok, wblk), BF16), vm((n_tok, dim), BF16),
            vm((dim, n_tok), BF16), vm((dim, n_tok), BF16), vm((n_tok, dim), F32), vm((plan.calc_rows, n_tok), BF16), vm((1, n_tok), F32),
            vm((2, plan.calc_rows, dim), BF16), vm((2, plan.calc_rows, dim), F32), vm((9, plan.copy_rows, dim), F32),
            vm((2, dim, wblk), F32), vm((2, wblk, dim), F32),
            dma((4,)), dma((2,)), dma((9,)), dma((2,)), dma((9,)), dma((2,)), dma((2,)), dma((2, 2)),
        ],
        compiler_params=pltpu.CompilerParams(vmem_limit_bytes=67_000_000),
        cost_estimate=pl.CostEstimate(flops=2 * n_tok * vocab * dim, bytes_accessed=5 * vocab * dim, transcendentals=0),
        name="fin",
    )(meta.reshape(-1), emb, tmp, n_all, stats, losses, labels.reshape(1, n_tok), meta, dx0, xs, hid, da, g)


def solution(mesh):
    n_stage = mesh.shape["stage"]

    def device_fn(tokens, labels, emb, w_up, w_down):
        n_micro, seq = tokens.shape
        vocab, dim = emb.shape
        w_up, w_down = w_up[0], w_down[0]
        n_tok = n_micro * seq
        plan = Plan(vocab, n_stage)
        cuts = jnp.array([plan.cuts(0), plan.cuts(1)], jnp.int32)
        x0 = run_gather(tokens, emb)
        n_all, xs, hid, da, g, dx0, stats, losses, tmp, meta = run_pipe(x0, emb, w_up, w_down, labels, tokens, cuts, n_stage, plan)
        flat = lambda p: p.reshape(n_tok, -1)
        grad_emb, loss, grad_up, grad_down = run_fin(
            emb, tmp.reshape(-1, dim), flat(n_all), stats, losses, labels, meta, flat(dx0), flat(xs), flat(hid), flat(da), flat(g), n_stage, plan
        )
        return loss, grad_up[None], grad_down[None], grad_emb

    return jax.shard_map(device_fn, mesh=mesh, in_specs=(P("dp", None), P("dp", None), P(None, None), P("stage", None, None), P("stage", None, None)), out_specs=(P("dp"), P(("dp", "stage"), None, None), P(("dp", "stage"), None, None), P("dp", None)), check_vma=False)
```

```python
import functools
import math

import jax
import jax.numpy as jnp
from jax import lax
from jax.experimental import pallas as pl
from jax.experimental.pallas import tpu as pltpu
from jax.sharding import PartitionSpec as P


MESH = pl.DeviceIdType.MESH
LOG2E = math.log2(math.e)
LN2 = math.log(2.0)
GELU_C = math.sqrt(2.0 / math.pi)
GELU_K = 0.044715
EPS = 1e-6
LANES = 128
F32 = jnp.float32
BF16 = jnp.bfloat16


def gelu_fwd(a):
    return (0.5 * a) * (1.0 + jnp.tanh(a * (GELU_C + (GELU_C * GELU_K) * (a * a))))


def gelu_slope(a):
    a2 = a * a
    half = 0.5 * jnp.tanh(a * (GELU_C + (GELU_C * GELU_K) * a2))
    up, down = 0.5 + half, 0.5 - half
    return up + (up * down) * (a * (2.0 * GELU_C + (6.0 * GELU_C * GELU_K) * a2))


def dot(x, y):
    return jnp.dot(x, y, preferred_element_type=F32)


def dot_t(x, y):
    return lax.dot_general(x, y, (((0,), (0,)), ((), ())), preferred_element_type=F32)


def remote(src, dst, send_sem, recv_sem, dev):
    return pltpu.make_async_remote_copy(src_ref=src, dst_ref=dst, send_sem=send_sem, recv_sem=recv_sem, device_id={"stage": dev}, device_id_type=MESH)


def column(row):
    return jnp.broadcast_to(row, (LANES, LANES)).T


def gather_kernel(ids_ref, tok_ref, emb_hbm, x0_hbm, tiles, picked, sem, out_sem):
    n_micro, seq = tok_ref.shape
    me = lax.axis_index("stage")
    group = tiles.shape[1] // seq
    slots = tiles.shape[0]
    owners = [head_chunk(me, k, n_micro) for k in range(slots)]

    def fetch(k):
        def one(i, carry):
            t = ids_ref[owners[k] * seq + i]
            start = pl.multiple_of(t // group * group, group)
            pltpu.make_async_copy(emb_hbm.at[pl.ds(start, group)], tiles.at[k, pl.ds(pl.multiple_of(i * group, group), group)], sem.at[k]).start()
            return carry

        lax.fori_loop(0, seq, one, 0, unroll=8)

    def select(k):
        sub = lax.broadcasted_iota(jnp.int32, (LANES, LANES), 0)
        lane = lax.broadcasted_iota(jnp.int32, (LANES, LANES), 1)
        tok = column(tok_ref[pl.ds(owners[k], 1), :].astype(F32)).astype(jnp.int32)
        want = sub * group + (tok - tok // group * group)
        hot = jnp.concatenate([jnp.where(lane + b * LANES == want, 1.0, 0.0).astype(BF16) for b in range(seq * group // LANES)], axis=1)
        pltpu.make_async_copy(emb_hbm.at[pl.ds(0, seq * group)], tiles.at[k], sem.at[k]).wait()
        picked[k] = dot(hot, tiles[k]).astype(BF16)
        pltpu.make_async_copy(picked.at[k], x0_hbm.at[k], out_sem.at[k]).start()

    def finish(k):
        pltpu.make_async_copy(picked.at[k], x0_hbm.at[k], out_sem.at[k]).wait()

    for work in (fetch, select, finish):
        work(0)
        for k in range(1, slots):
            pl.when(me < slots)(functools.partial(work, k))


def head_chunk(dev, k, n_micro):
    return jnp.minimum(jnp.where(dev < 2, 2 * dev + k, dev + 2), n_micro - 1)


def run_gather(tokens, emb):
    n_micro, seq = tokens.shape
    dim = emb.shape[1]
    group = 16
    return pl.pallas_call(
        gather_kernel,
        out_shape=jax.ShapeDtypeStruct((2, seq, dim), BF16),
        in_specs=[pl.BlockSpec(memory_space=pltpu.SMEM), pl.BlockSpec(memory_space=pltpu.VMEM), pl.BlockSpec(memory_space=pl.ANY)],
        out_specs=pl.BlockSpec(memory_space=pl.ANY),
        scratch_shapes=[pltpu.VMEM((2, seq * group, dim), BF16), pltpu.VMEM((2, seq, dim), BF16), pltpu.SemaphoreType.DMA((2,)), pltpu.SemaphoreType.DMA((2,))],
        cost_estimate=pl.CostEstimate(flops=10**9, bytes_accessed=2 * seq * group * dim * 2, transcendentals=0),
        name="gather",
    )(tokens.reshape(n_micro * seq), tokens, emb)


def token_table(row_ref, cut_ref, meta):
    n_tok = row_ref.shape[1]
    n_grp = n_tok // LANES
    lane = lax.broadcasted_iota(jnp.int32, (LANES, LANES), 1).astype(F32)
    sub = lax.broadcasted_iota(jnp.int32, (LANES, LANES), 0)
    row = lambda g: row_ref[:, g * LANES:(g + 1) * LANES].astype(F32)
    zero = jnp.zeros((LANES, LANES), F32)
    fold = lambda acc: jnp.sum(acc, axis=0, keepdims=True)
    cols = [column(row(c)) for c in range(n_grp)]
    firsts = []
    for g in range(n_grp):
        acc = zero
        for c in range(g + 1):
            same = cols[c] == row(g)
            if c == g:
                same = same & (sub < lane.astype(jnp.int32))
            acc = acc + jnp.where(same, 1.0, 0.0)
        firsts.append(column(jnp.where(fold(acc) == 0.0, 1.0, 0.0)))
    ranks = []
    for g in range(n_grp):
        acc = zero
        for c in range(n_grp):
            acc = acc + jnp.where(cols[c] < row(g), firsts[c], 0.0)
        ranks.append(fold(acc))
        meta[g:g + 1, :] = ranks[g].astype(jnp.int32)
    rank_cols = [column(r) for r in ranks]
    for g in range(n_grp):
        acc = zero
        for c in range(n_grp):
            acc = acc + jnp.where(rank_cols[c] == lane + g * LANES, firsts[c] * cols[c], 0.0)
        meta[n_grp + g:n_grp + g + 1, :] = fold(acc).astype(jnp.int32)
    cut = cut_ref[...].astype(F32)
    acc = zero
    for c in range(n_grp):
        acc = acc + jnp.where(cols[c] < cut, firsts[c], 0.0)
    meta[2 * n_grp:3 * n_grp, :] = jnp.broadcast_to(fold(acc), (n_grp, LANES)).astype(jnp.int32)


def logit_grad(e, n_t, shift, lab, first_id, inv_count, scale, dz):
    rows = e.shape[0]
    n_tok = n_t.shape[1]
    blk = 256
    vid = lax.broadcasted_iota(jnp.int32, (rows, blk), 0)
    for j in range(n_tok // blk):
        cols = slice(j * blk, (j + 1) * blk)
        z = (dot(e, n_t[:, cols]) * scale).astype(BF16).astype(F32)
        prob = jnp.exp2(z * LOG2E - shift[:, cols])
        dz[:, cols] = jnp.where(vid == lab[:, cols] - first_id, prob - inv_count, prob).astype(BF16)


def pipe_kernel(n_stage, plan, x0_hbm, emb_hbm, up_hbm, down_hbm, lab_ref, row_ref, cut_ref,
                n_out, xs_out, hid_out, da_out, g_out, dx0_out, stat_out, loss_out, tmp_out, meta_out,
                xbuf, ybuf, abuf, hbuf, nbuf, gbuf, dxbuf, dx0buf, dnbuf, up, down, up_t, down_t,
                emb, zbuf, n_t, dn_acc, dn_send, dn_recv, dn_own, st_send, st_recv, statall, lossall, tops, n_all_t, shift, dz, obuf, z_pair, meta,
                w_sem, e_sem, x_sem, x_send, x_recv, f_send, f_recv, n_send, n_recv, nf_send, ag_send, ag_recv, fw_send,
                st_sems, dp_sems, dn_ssem, dn_rsem, sa_sems, lo_sems, b_send, b_recv, d_send, d_recv, r_sems, out_sem, o_sem, od_send, od_recv, ic_send):
    n_micro, seq, dim = gbuf.shape
    part = xbuf.shape[1]
    n_part = xbuf.shape[0]
    per = seq // part
    n_tok = n_micro * seq
    ffn = up.shape[1]
    vocab = emb_hbm.shape[0]
    me = lax.axis_index("stage")
    core = lax.rem(me, 2)
    chip = me // 2
    mate = me + 1 - 2 * core
    last_id = n_stage - 1
    first = me == 0
    last = me == last_id
    fblk = 512
    n_fblk = ffn // fblk
    base, extra, tile = plan.base, plan.extra, plan.head_tile
    row0 = core * (base + extra)
    n_tiles = base // tile
    wide_tile = plan.grad_tile

    barrier = pltpu.get_barrier_semaphore()
    gives_x = (me >= 1) & (me + 2 < n_micro)

    def here(dev):
        pl.semaphore_signal(barrier, inc=1, device_id={"stage": dev}, device_id_type=MESH)

    pl.when(jnp.logical_not(first))(lambda: here(me - 1))
    pl.when(jnp.logical_not(last))(lambda: here(me + 1))

    @pl.when(first)
    def _():
        for dev in range(2, n_micro - 2):
            here(dev)

    w_copy = [pltpu.make_async_copy(up_hbm, up, w_sem.at[0]), pltpu.make_async_copy(down_hbm, down, w_sem.at[1])]
    for c in w_copy:
        c.start()
    x_slots = x0_hbm.shape[0]
    x_mine = [head_chunk(me, k, n_micro) for k in range(x_slots)]

    def x_rows(m):
        return xbuf.at[pl.ds(m * per, per)]

    def x_local(k):
        return pltpu.make_async_copy(x0_hbm.at[k], x_rows(k), x_sem.at[k])

    @pl.when(first)
    def _():
        for k in range(x_slots):
            x_local(k).start()

    e_parts = plan.e_parts
    e_step = base // e_parts

    def e_copy(i):
        src = emb_hbm.at[pl.ds(pl.multiple_of(row0 + i * e_step, 16), e_step)]
        return pltpu.make_async_copy(src, emb.at[pl.ds(i * e_step, e_step)], e_sem.at[0])

    e_more = pltpu.make_async_copy(emb_hbm.at[pl.ds(base, extra)], emb.at[pl.ds(base, extra)], e_sem.at[1])
    with jax.named_scope("entry"):
        pl.semaphore_wait(barrier, jnp.where(first | last, 1, 2) + jnp.where(gives_x & (me >= 2), 1, 0))

    def x_copy(k):
        return remote(x0_hbm.at[k], x_rows(x_mine[k]), x_send.at[k], x_recv.at[x_mine[k]], 0)

    @pl.when(gives_x)
    def _():
        x_copy(0).start()

        @pl.when(me < 2)
        def _():
            x_copy(1).start()

    def table_start():
        for i in range(e_parts):
            e_copy(i).start()
        pl.when(core == 0)(e_more.start)

    def transpose_weights():
        for j in range(n_fblk):
            up_t[j * fblk:(j + 1) * fblk, :] = up[:, j * fblk:(j + 1) * fblk].T
            down_t[:, j * fblk:(j + 1) * fblk] = down[j * fblk:(j + 1) * fblk, :].T

    @pl.when(jnp.logical_not(first))
    def _():
        for c in w_copy:
            c.wait()
        table_start()

    def idle_work():
        transpose_weights()
        token_table(row_ref, jnp.where(core == 0, cut_ref[0:1, :], cut_ref[1:2, :]), meta)

    @pl.when(chip >= n_stage // 4)
    def _():
        idle_work()

    def n_start(m):
        remote(nbuf.at[m], nbuf.at[m], n_send, n_recv.at[m], jnp.where(m == last_id, last_id - 1, m)).start()

    def fwd(h, carry, cold=False):
        m = h // per
        sub = lax.rem(h, per)
        rows = pl.ds(pl.multiple_of(sub * part, part), part)
        with jax.named_scope("fwd_wait"):

            @pl.when(first & (sub == 0))
            def _():
                @pl.when(m < x_slots)
                def _():
                    x_local(m).wait()

                @pl.when(m >= x_slots)
                def _():
                    remote(x_rows(m), x_rows(m), x_send.at[0], x_recv.at[m], me).wait_recv()

            @pl.when(jnp.logical_not(first))
            def _():
                remote(xbuf.at[h], xbuf.at[h], f_send, f_recv.at[h], me).wait_recv()

        with jax.named_scope("fwd_comp"):
            x = xbuf[h]
            if cold:
                w_copy[0].wait()
            for j in range(n_fblk):
                cols = slice(j * fblk, (j + 1) * fblk)
                a = dot(x, up[:, cols]).astype(BF16)
                abuf[m, rows, cols] = a
                hbuf[m, rows, cols] = gelu_fwd(a.astype(F32)).astype(BF16)
            if cold:
                w_copy[1].wait()
                table_start()
            y = (x.astype(F32) + dot(hbuf[m, rows, :], down[...])).astype(BF16)
            ybuf[h] = y

        @pl.when(jnp.logical_not(last))
        def _():
            remote(ybuf.at[h], xbuf.at[h], f_send, f_recv.at[h], me + 1).start()

        @pl.when(last)
        def _():
            yf = y.astype(F32)
            inv = lax.rsqrt(jnp.mean(yf * yf, axis=-1, keepdims=True) + EPS)
            nbuf[m, rows, :] = (yf * inv).astype(BF16)
            pl.when(sub == per - 1)(lambda: n_start(m))

        @pl.when(sub == per - 1)
        def _():
            pltpu.make_async_copy(hbuf.at[m], hid_out.at[m], out_sem.at[0]).start()
            pltpu.make_async_copy(x_rows(m), xs_out.at[pl.ds(m * per, per)], out_sem.at[1]).start()

        return carry

    pl.when(first)(lambda: (fwd(0, 0, cold=True), None)[1])
    lax.fori_loop(jnp.where(first, 1, 0), n_part, fwd, 0)

    @pl.when(chip < n_stage // 4)
    def _():
        idle_work()

    n_forward = remote(nbuf.at[me], nbuf.at[me], nf_send, n_recv.at[me], mate)
    with jax.named_scope("n_wait"):

        @pl.when(jnp.logical_not(last))
        def _():
            remote(nbuf.at[me], nbuf.at[me], n_send, n_recv.at[me], me).wait_recv()
            pl.when(mate != last_id)(n_forward.start)
            remote(nbuf.at[mate], nbuf.at[mate], n_send, n_recv.at[mate], me).wait_recv()

        for k in range(2):
            n_t[:, k * seq:(k + 1) * seq] = nbuf[2 * chip + k].T

    peers = [lax.rem(me + 2 * d, n_stage) for d in range(1, n_stage // 2)]
    ag_copies = [remote(nbuf.at[me], nbuf.at[me], ag_send.at[d], ag_recv.at[me], p) for d, p in enumerate(peers)]
    for c, p in zip(ag_copies, peers):
        pl.when(p != last_id)(c.start)
    with jax.named_scope("e_wait"):
        pltpu.make_async_copy(emb_hbm.at[pl.ds(0, base)], emb.at[pl.ds(0, base)], e_sem.at[0]).wait()
        pl.when(core == 0)(e_more.wait)

    pair = 2 * seq
    scale = dim ** -0.5
    inv_count = 1.0 / n_tok
    log_count = math.log2(n_tok)
    lab = lab_ref[:, pl.ds(pl.multiple_of(chip * pair, pair), pair)]

    def logits(rows, size):
        e = emb[rows, :]
        parts = [dot(e[k * size // 2:(k + 1) * size // 2], n_t[...]) for k in range(2)]
        z = jnp.concatenate([(p * scale).astype(BF16) for p in parts], axis=0)
        zbuf[rows, :] = z
        return z

    def peak(z, size, top):
        best = jnp.max(z.reshape(size // 16, 16, pair), axis=0).astype(F32)
        return jnp.maximum(top, jnp.maximum(best[:8], best[8:]))

    def total(z, size, old, top, tot):
        off = top * LOG2E
        return tot * jnp.exp2(old * LOG2E - off) + jnp.sum(jnp.exp2(z.astype(F32).reshape(size // 8, 8, pair) * LOG2E - off[None]), axis=0)

    tops[0] = jnp.full((8, pair), -jnp.inf, F32)
    tops[1] = jnp.zeros((8, pair), F32)

    @pl.when(core == 0)
    def _():
        z = logits(pl.ds(base, extra), extra)
        top = peak(z, extra, tops[0])
        tops[1] = total(z, extra, tops[0], top, tops[1])
        tops[0] = top

    def logits_step(i, slot, old, top, tot):
        z = logits(pl.ds(pl.multiple_of(i * tile, 16), tile), tile)
        tot = total(z_pair[1 - slot], tile, old, top, tot)
        z_pair[slot] = z
        return top, peak(z, tile, top), tot

    with jax.named_scope("logits"):
        z = logits(pl.ds(0, tile), tile)
        z_pair[0] = z
        state = (tops[0], peak(z, tile, tops[0]), tops[1])
        state = lax.fori_loop(0, (n_tiles - 1) // 2, lambda i, c: logits_step(2 * i + 2, 0, *logits_step(2 * i + 1, 1, *c)), state)
        if n_tiles % 2 == 0:
            state = logits_step(n_tiles - 1, 1, *state)
        old, top, tot = state
        tot = total(z_pair[(n_tiles - 1) % 2], tile, old, top, tot)
    row_top = jnp.max(top, axis=0, keepdims=True)
    row_tot = jnp.sum(tot * jnp.exp2((top - row_top) * LOG2E), axis=0, keepdims=True)
    st_send[0:8, :] = jnp.broadcast_to(row_top, (8, pair))
    st_send[8:16, :] = jnp.broadcast_to(row_tot, (8, pair))
    st_copy = remote(st_send, st_recv, st_sems.at[0], st_sems.at[1], mate)
    with jax.named_scope("stat_x"):
        st_copy.start()
        st_copy.wait()
    far_top = st_recv[0:1, :]
    far_tot = st_recv[8:9, :]
    all_top = jnp.maximum(row_top, far_top)
    mine = row_tot * jnp.exp(row_top - all_top)
    other = far_tot * jnp.exp(far_top - all_top)
    lse = all_top + jnp.log(jnp.where(core == 0, mine + other, other + mine))
    my_shift = lse * LOG2E + log_count
    others = [lax.rem(me + d, n_stage) for d in range(1, n_stage)]

    def spread(buf, sems):
        whole = buf.at[pl.ds(0, n_stage - 1)]
        return [remote(buf.at[me], buf.at[me], sems.at[0], sems.at[1], p) for p in others], remote(whole, whole, sems.at[0], sems.at[1], me)

    statall[me] = jnp.broadcast_to(lse, (8, pair))
    sa_copies, sa_all = spread(statall, sa_sems)
    for c in sa_copies:
        c.start()

    def grads(rows, size, first_row, picked):
        zf = zbuf[rows, :].astype(F32)
        prob = jnp.exp2(zf * LOG2E - my_shift)
        hit = lax.broadcasted_iota(jnp.int32, (size, pair), 0) == lab - (row0 + first_row)
        dz_t = jnp.where(hit, prob - inv_count, prob).astype(BF16)
        got = jnp.where(hit, zf, 0.0).reshape(size // 8, 8, pair)
        return dot_t(dz_t, emb[rows, :]), picked + jnp.sum(got, axis=0)

    tops[0] = jnp.zeros((8, pair), F32)
    dn_acc[...] = jnp.zeros_like(dn_acc)

    @pl.when(core == 0)
    def _():
        dn_acc[...], tops[0] = grads(pl.ds(base, extra), extra, base, tops[0])

    def grad_step(i, picked):
        part, picked = grads(pl.ds(pl.multiple_of(i * wide_tile, 16), wide_tile), wide_tile, i * wide_tile, picked)
        dn_acc[...] += part
        return picked

    with jax.named_scope("grads"):
        picked = lax.fori_loop(0, base // wide_tile, grad_step, tops[0])
    far = pl.ds(pl.multiple_of((1 - core) * seq, seq), seq)
    near = pl.ds(pl.multiple_of(core * seq, seq), seq)
    dn_send[...] = dn_acc[far, :]
    dp_copy = remote(dn_send, dn_recv, dp_sems.at[0], dp_sems.at[1], mate)
    dp_copy.start()
    row_loss = jnp.where(core == 0, lse, 0.0) - jnp.sum(picked, axis=0, keepdims=True)
    lossall[me] = jnp.broadcast_to(row_loss, (8, pair))
    lo_copies, lo_all = spread(lossall, lo_sems)
    for c in lo_copies:
        c.start()
    with jax.named_scope("dn_x"):
        dp_copy.wait()
        dn = ((dn_acc[near, :] + dn_recv[...]) * scale).astype(BF16)
    dn_copy = remote(dn_own, dnbuf.at[me], dn_ssem, dn_rsem.at[me], last_id)

    @pl.when(last)
    def _():
        dnbuf[last_id] = dn

    @pl.when(jnp.logical_not(last))
    def _():
        dn_own[...] = dn
        remote(dn_own, dnbuf.at[me], dn_ssem, dn_rsem.at[me], last_id).start()

    with jax.named_scope("ag_wait"):
        for p in peers:
            got = remote(nbuf.at[p], nbuf.at[p], ag_send.at[0], ag_recv.at[p], me)
            pl.when(jnp.logical_not(last))(got.wait_recv)
            pl.when(mate != last_id)(remote(nbuf.at[p], nbuf.at[p], fw_send, ag_recv.at[p], mate).start)

    near_dst = [1, 3, last_id]
    far_dst = n_stage // 2 + 1
    direct = n_micro - 1
    by_prev = n_micro - 3
    hands_on = (core == 1) & (me != 1)

    def dx0_start(m, k, dev):
        remote(dxbuf.at[m], dx0buf.at[m], d_send.at[k], d_recv.at[m], dev).start()

    def relayed(m):
        return (m < direct) & (((me == 3) & (m != by_prev)) | (last & (m == by_prev)))

    def relay_far(m):
        remote(dx0buf.at[m], dx0buf.at[m], r_sems.at[1], d_recv.at[m], far_dst).start()

    def bwd(m):
        with jax.named_scope("bwd_wait"):
            @pl.when(jnp.logical_not(last))
            def _():
                remote(gbuf.at[m], gbuf.at[m], b_send, b_recv.at[m], me).wait_recv()

            @pl.when(last)
            def _():
                @pl.when(m != last_id)
                def _():
                    remote(dnbuf.at[m], dnbuf.at[m], dn_ssem, dn_rsem.at[m], me).wait_recv()

                yf = ybuf[pl.ds(m * per, per)].reshape(seq, dim).astype(F32)
                inv = lax.rsqrt(jnp.mean(yf * yf, axis=-1, keepdims=True) + EPS)
                dnf = dnbuf[m].astype(F32)
                proj = jnp.mean(yf * dnf, axis=-1, keepdims=True)
                gbuf[m] = (dnf * inv - yf * (inv * inv * inv * proj)).astype(BF16)

        with jax.named_scope("bwd_comp"):
            g = gbuf[m]
            for j in range(n_fblk):
                cols = slice(j * fblk, (j + 1) * fblk)
                dh = dot(g, down_t[:, cols]).astype(BF16).astype(F32)
                abuf[m, :, cols] = (dh * gelu_slope(abuf[m, :, cols].astype(F32))).astype(BF16)
            dxbuf[m] = (g.astype(F32) + dot(abuf[m], up_t[...])).astype(BF16)

        @pl.when(jnp.logical_not(first))
        def _():
            remote(dxbuf.at[m], gbuf.at[m], b_send, b_recv.at[m], me - 1).start()

        @pl.when(first)
        def _():
            pl.when(m >= direct)(lambda: dx0_start(m, len(near_dst), far_dst))
            for k, dev in enumerate(near_dst):
                dx0_start(m, k, dev)

        pltpu.make_async_copy(abuf.at[m], da_out.at[m], out_sem.at[2]).start()
        pltpu.make_async_copy(gbuf.at[m], g_out.at[m], out_sem.at[3]).start()

    n_slot = obuf.shape[0]
    busy = chip == last_id // 2
    far_tile = remote(tmp_out.at[core, pl.ds(0, plan.rows)], tmp_out.at[core, pl.ds(0, plan.rows)], ic_send, od_recv, jnp.where(first, last_id, last_id - 1))
    sends_far = first | (me == last_id - 2)

    def tile_copy(k):
        rows = pl.ds(pl.multiple_of(k * plan.rows, plan.rows), plan.rows)
        slot = lax.rem(k, n_slot)
        return pltpu.make_async_copy(obuf.at[slot], tmp_out.at[core, rows], o_sem.at[slot])

    def piece(p):
        k = p // plan.per_tile
        rows = pl.ds(pl.multiple_of(p * plan.piece, plan.piece), plan.piece)
        here = pl.ds(pl.multiple_of(lax.rem(p, plan.per_tile) * plan.piece, plan.piece), plan.piece)
        return remote(obuf.at[lax.rem(k, n_slot), here], tmp_out.at[core, rows], od_send.at[k], od_recv, mate)

    def tile_sent(k):
        slot = lax.rem(k, n_slot)
        return remote(obuf.at[slot], tmp_out.at[core, pl.ds(0, plan.rows)], od_send.at[k], od_recv, mate)

    def emb_tile(k):
        with jax.named_scope("tile_prep"):

            @pl.when(k == 0)
            def _():
                for d in range(1, n_stage // 2):
                    src = lax.rem(mate + 2 * d, n_stage)
                    pl.when(jnp.logical_not(last))(remote(nbuf.at[src], nbuf.at[src], ag_send.at[0], ag_recv.at[src], me).wait_recv)
                for m in range(n_micro):
                    n_all_t[:, m * seq:(m + 1) * seq] = nbuf[m].T
                sa_all.wait_recv()
                for c in range(n_stage // 2):
                    shift[:, c * pair:(c + 1) * pair] = statall[2 * c, 0:1, :] * LOG2E + log_count

        slot = lax.rem(k, n_slot)
        with jax.named_scope("tile_wait"):
            @pl.when(k == 2)
            def _():
                tile_copy(0).wait()
                pl.when(sends_far)(far_tile.start)

            pl.when(k > n_slot)(lambda: tile_copy(k - n_slot).wait())
            pl.when((k >= n_slot) & (k - n_slot < plan.shared) & jnp.logical_not(busy & (k == n_slot)))(lambda: tile_sent(k - n_slot).wait_send())

        with jax.named_scope("tile"):
            rows = pl.ds(pl.multiple_of(k * plan.rows, plan.rows), plan.rows)
            logit_grad(emb[rows, :], n_all_t, shift, lab_ref, row0 + k * plan.rows, inv_count, scale, dz)
            obuf[slot] = dot(dz[...], nbuf[...].reshape(n_tok, dim)) * scale

        tile_copy(k).start()

    def send_pieces(done, until):
        lax.fori_loop(done, until, lambda p, c: (piece(p).start(), c)[1], 0)

    def send_tiles(done, until):
        def one(k, carry):
            rows = pl.ds(pl.multiple_of(k * plan.rows, plan.rows), plan.rows)
            remote(obuf.at[lax.rem(k, n_slot)], tmp_out.at[core, rows], od_send.at[k], od_recv, mate).start()
            return carry

        lax.fori_loop(done, until, one, 0)

    before = sum(jnp.where(me == s, plan.before[s], 0) for s in range(n_stage))

    def pass_dx0(m, carry):
        @pl.when(jnp.logical_not(first))
        def _():
            remote(dx0buf.at[m], dx0buf.at[m], r_sems.at[0], d_recv.at[m], me).wait_recv()

            @pl.when(hands_on)
            def _():
                remote(dx0buf.at[m], dx0buf.at[m], r_sems.at[0], d_recv.at[m], mate).start()

            @pl.when(relayed(m))
            def _():
                relay_far(m)

            pltpu.make_async_copy(dx0buf.at[m], dx0_out.at[m], out_sem.at[4]).start()

        @pl.when(first)
        def _():
            pltpu.make_async_copy(dxbuf.at[m], dx0_out.at[m], out_sem.at[4]).start()

        return carry

    lead = jnp.where(me == 3, -300, jnp.where(last, -1800, jnp.where(me == far_dst, -1600, -10**6)))

    def work(i, carry):
        sent, passed = carry
        chunk = (i >= before) & (i < before + n_micro)
        pl.when(chunk)(lambda: bwd(i - before))
        k = jnp.where(i < before, i, i - n_micro)
        pl.when(jnp.logical_not(chunk))(lambda: emb_tile(k))
        after = i - before - n_micro + 1
        here = jnp.where(after > 0, jnp.clip((after * 264 + lead) // 138, 0, n_micro), 0)
        lax.fori_loop(passed, here, pass_dx0, 0)
        ready = jnp.where(i < before, i + 1, jnp.where(chunk, before, i + 1 - n_micro))
        near_chunks = chunk | ((i < before) & (i + 1 >= before))
        whole = (sent + plan.per_tile - 1) // plan.per_tile
        upto = jnp.minimum(jnp.minimum(ready, plan.shared), whole + 1)
        some = jnp.where(near_chunks, jnp.minimum(sent + 1, jnp.minimum(ready, plan.shared) * plan.per_tile), whole * plan.per_tile)
        send_pieces(sent, some)
        send_tiles(whole, jnp.where(near_chunks, 0, upto))
        now = jnp.where(near_chunks, some, jnp.maximum(some, upto * plan.per_tile))
        return jnp.maximum(sent, now), jnp.maximum(passed, here)

    sent, passed = lax.fori_loop(0, plan.tiles + n_micro, work, (jnp.where(busy, plan.per_tile, 0), 0))
    outs = [pltpu.make_async_copy(nbuf, n_out, out_sem.at[5]), pltpu.make_async_copy(lossall, loss_out, out_sem.at[6]), pltpu.make_async_copy(meta, meta_out, out_sem.at[7])]
    lo_all.wait_recv()
    for c in outs:
        c.start()
    pltpu.make_async_copy(statall, stat_out, out_sem.at[8]).start()
    with jax.named_scope("relay_all"):
        lax.fori_loop(passed, n_micro, pass_dx0, 0)

    with jax.named_scope("drain"):
        send_pieces(sent, plan.shared * plan.per_tile)
        for k in range(max(plan.tiles - n_slot, 0), plan.tiles):
            tile_copy(k).wait()
            if k < plan.shared:
                tile_sent(k).wait_send()
        pl.when(sends_far)(far_tile.wait_send)
        all_rows = pl.ds(0, plan.shared * plan.rows)
        remote(tmp_out.at[1 - core, all_rows], tmp_out.at[1 - core, all_rows], od_send.at[0], od_recv, me).wait_recv()
        sa_all.wait_send()
        lo_all.wait_send()
        pltpu.make_async_copy(statall, stat_out, out_sem.at[8]).wait()
        for c, p in zip(ag_copies, peers):
            pl.when(p != last_id)(c.wait_send)

        @pl.when(jnp.logical_not(last))
        def _():
            dn_copy.wait_send()
            pl.when(mate != last_id)(n_forward.wait_send)
            remote(ybuf, xbuf, f_send, f_recv.at[0], me + 1).wait_send()

        @pl.when(last)
        def _():
            remote(nbuf, nbuf, n_send, n_recv.at[0], me).wait_send()

        @pl.when(mate != last_id)
        def _():
            some = nbuf.at[pl.ds(0, len(peers))]
            remote(some, some, fw_send, ag_recv.at[0], mate).wait_send()

        @pl.when(gives_x)
        def _():
            x_copy(0).wait_send()

            @pl.when(me < 2)
            def _():
                x_copy(1).wait_send()

        @pl.when(jnp.logical_not(first))
        def _():
            remote(dxbuf, gbuf, b_send, b_recv.at[0], me).wait_send()
            pl.when(hands_on)(remote(dx0buf, dx0buf, r_sems.at[0], d_recv.at[0], mate).wait_send)

        @pl.when(first)
        def _():
            for k in range(len(near_dst)):
                remote(dxbuf, dx0buf, d_send.at[k], d_recv.at[0], me).wait_send()
            rest = pl.ds(0, n_micro - direct)
            remote(dxbuf.at[rest], dx0buf.at[rest], d_send.at[len(near_dst)], d_recv.at[0], me).wait_send()

        for dev, kept in ((3, direct - 1), (last_id, 1)):
            some = dx0buf.at[pl.ds(0, kept)]
            pl.when(me == dev)(remote(some, some, r_sems.at[1], d_recv.at[0], me).wait_send)

        pltpu.make_async_copy(hbuf, hid_out, out_sem.at[0]).wait()
        pltpu.make_async_copy(xbuf, xs_out, out_sem.at[1]).wait()
        pltpu.make_async_copy(abuf, da_out, out_sem.at[2]).wait()
        pltpu.make_async_copy(gbuf, g_out, out_sem.at[3]).wait()
        pltpu.make_async_copy(dx0buf, dx0_out, out_sem.at[4]).wait()
        for c in outs:
            c.wait()


class Plan:
    def __init__(self, vocab, n_stage):
        units = vocab // LANES
        self.base = units // 2 * LANES
        self.extra = vocab - 2 * self.base
        self.head_tile = next(t for t in (1600, 1536, 1280, 1024, 768, 640, 512, 256, 128) if self.base % t == 0)
        self.rows = 1024
        self.tiles, self.shared = 11, 9
        self.grad_tile = next(t for t in (4000, 3200, 1600, 1280, 640, 256, 128) if self.base % t == 0)
        self.e_parts = next(k for k in (10, 8, 5, 4, 2, 1) if self.base % (16 * k) == 0)
        self.part = 128
        self.slots = 4
        self.piece = 256
        self.per_tile = self.rows // self.piece
        measured = [10, 9, 6, 5, 3, 2, 0, 0]
        self.before = (measured + [0] * n_stage)[:n_stage]
        mid = self.base + self.extra
        ends = [(0, mid), (mid, vocab)]
        early = (self.tiles * self.rows, self.shared * self.rows)
        self.spans = [[(ends[h][0] + early[0 if h == c else 1], ends[h][1]) for h in (c, 1 - c)] for c in range(2)]
        self.longest = [max(self.spans[c][k][1] - self.spans[c][k][0] for c in range(2)) for k in range(2)]
        best = min(range(16, 1281, 16), key=lambda r: (sum(-(-n // r) for n in self.longest)) * (r + 40))
        self.calc_rows = best
        self.calc_steps = [-(-n // best) for n in self.longest]
        self.steps = sum(self.calc_steps)
        self.copy_rows = self.rows
        self.copies = self.tiles + self.shared
        self.starts = ends

    def calc_start(self, core, s):
        k = 0 if s < self.calc_steps[0] else 1
        lo, hi = self.spans[core][k]
        return min(lo + (s - k * self.calc_steps[0]) * self.calc_rows, hi - self.calc_rows)

    def copy_start(self, core, c):
        own = c < self.tiles
        h = core if own else 1 - core
        return self.starts[h][0] + (c if own else c - self.tiles) * self.copy_rows

    def cuts(self, core):
        firsts = [(self.calc_start(core, s), self.calc_rows) for s in range(self.steps)] + [(self.copy_start(core, c), self.copy_rows) for c in range(self.copies)]
        flat = [v for lo, rows in firsts for v in (lo, lo + rows)]
        return flat + [0] * (LANES - len(flat))


def run_pipe(x0, emb, w_up, w_down, labels, tokens, cuts, n_stage, plan):
    n_micro, seq = labels.shape
    dim, ffn = w_up.shape
    n_tok = n_micro * seq
    base = plan.base
    any_spec = pl.BlockSpec(memory_space=pl.ANY)
    act = (n_micro, seq, dim)
    fine = (n_tok // plan.part, plan.part, dim)
    wide = (n_micro, seq, ffn)
    dma = pltpu.SemaphoreType.DMA
    vm = pltpu.VMEM
    pair = 2 * seq
    return pl.pallas_call(
        functools.partial(pipe_kernel, n_stage, plan),
        out_shape=[
            jax.ShapeDtypeStruct(act, BF16), jax.ShapeDtypeStruct(fine, BF16), jax.ShapeDtypeStruct(wide, BF16),
            jax.ShapeDtypeStruct(wide, BF16), jax.ShapeDtypeStruct(act, BF16), jax.ShapeDtypeStruct(act, BF16),
            jax.ShapeDtypeStruct((n_stage, 8, pair), F32), jax.ShapeDtypeStruct((n_stage, 8, pair), F32), jax.ShapeDtypeStruct((2, plan.tiles * plan.rows, dim), F32),
            jax.ShapeDtypeStruct((3 * n_tok // LANES, LANES), jnp.int32),
        ],
        in_specs=[any_spec] * 4 + [pl.BlockSpec(memory_space=pltpu.VMEM)] * 3,
        out_specs=[any_spec] * 10,
        scratch_shapes=[
            vm(fine, BF16), vm(fine, BF16), vm(wide, BF16), vm(wide, BF16), vm(act, BF16), vm(act, BF16), vm(act, BF16), vm(act, BF16), vm(act, BF16),
            vm((dim, ffn), BF16), vm((ffn, dim), BF16), vm((ffn, dim), BF16), vm((dim, ffn), BF16),
            vm((base + plan.extra, dim), BF16), vm((base + plan.extra, pair), BF16), vm((dim, pair), BF16), vm((pair, dim), F32),
            vm((seq, dim), F32), vm((seq, dim), F32), vm((seq, dim), BF16), vm((16, pair), F32), vm((16, pair), F32), vm((n_stage, 8, pair), F32), vm((n_stage, 8, pair), F32),
            vm((2, 8, pair), F32), vm((dim, n_tok), BF16), vm((1, n_tok), F32), vm((plan.rows, n_tok), BF16), vm((plan.slots, plan.rows, dim), F32),
            vm((2, plan.head_tile, pair), BF16), vm((3 * n_tok // LANES, LANES), jnp.int32),
            dma((2,)), dma((2,)), dma((2,)), dma((2,)), dma((n_micro,)), dma, dma((n_tok // plan.part,)), dma, dma((n_micro,)), dma,
            dma((n_stage // 2,)), dma((n_micro,)), dma,
            dma((2,)), dma((2,)), dma, dma((n_stage,)), dma((2,)), dma((2,)), dma, dma((n_micro,)), dma((4,)), dma((n_micro,)), dma((2,)), dma((9,)),
            dma((plan.slots,)), dma((plan.shared,)), dma, dma,
        ],
        compiler_params=pltpu.CompilerParams(collective_id=0, has_side_effects=True, vmem_limit_bytes=67_000_000),
        cost_estimate=pl.CostEstimate(flops=60 * 10**9, bytes_accessed=100 * 10**6, transcendentals=0),
        name="pipe",
    )(x0.reshape(x0.shape[0], seq // plan.part, plan.part, dim), emb, w_up, w_down, labels.reshape(1, n_tok), tokens.reshape(1, n_tok), cuts)


def fin_kernel(n_stage, n_tok, plan, ids_ref, emb_hbm, tmp_hbm, n_hbm, stat_ref, part_ref, lab_ref, meta_ref, dx0_hbm, xs_hbm, hid_hbm, da_hbm, g_hbm,
               out_hbm, loss_ref, gup_hbm, gdown_hbm,
               n_all, dx0, xs, hid, da, g, n_t, x_t, dx0s, dz, shift, e_in, c_out, cp, gup, gdown,
               ld_sem, e_sem, t_sem, co_sem, po_sem, gu_sem, gd_sem, wi_sem):
    dim, ffn = gup_hbm.shape
    scale = dim ** -0.5
    inv_count = 1.0 / n_tok
    steps, crows, prows = plan.steps, plan.calc_rows, plan.copy_rows
    core = lax.rem(lax.axis_index("stage"), 2)
    early = plan.tiles * prows
    wblk = gup.shape[2]
    n_wblk = ffn // wblk
    turn = plan.calc_steps[0]

    def pick(pair):
        return jnp.where(core == 0, pair[0], pair[1])

    def calc_start(s):
        own = s < turn
        lo, hi = [jnp.where(own, pick([plan.spans[c][0][e] for c in range(2)]), pick([plan.spans[c][1][e] for c in range(2)])) for e in range(2)]
        return pl.multiple_of(jnp.minimum(lo + (s - jnp.where(own, 0, turn)) * crows, hi - crows), 16)

    def copy_start(c):
        own = c < plan.tiles
        first = jnp.where(own, pick([plan.starts[0][0], plan.starts[1][0]]), pick([plan.starts[1][0], plan.starts[0][0]]))
        return pl.multiple_of(first + (c - jnp.where(own, 0, plan.tiles)) * prows, 16)

    def e_copy(s):
        return pltpu.make_async_copy(emb_hbm.at[pl.ds(calc_start(s), crows)], e_in.at[lax.rem(s, 3)], e_sem.at[lax.rem(s, 3)])

    n_slot = cp.shape[0]
    ahead = 6

    def t_copy(c):
        own = c < plan.tiles
        row = jnp.where(own, core, 1 - core) * early + (c - jnp.where(own, 0, plan.tiles)) * prows
        slot = lax.rem(c, n_slot)
        return pltpu.make_async_copy(tmp_hbm.at[pl.ds(pl.multiple_of(row, 16), prows)], cp.at[slot], t_sem.at[slot])

    def p_out(c):
        slot = lax.rem(c, n_slot)
        return pltpu.make_async_copy(cp.at[slot], out_hbm.at[pl.ds(copy_start(c), prows)], po_sem.at[slot])

    def c_outs(s):
        slot = lax.rem(s, 2)
        return pltpu.make_async_copy(c_out.at[slot], out_hbm.at[pl.ds(calc_start(s), crows)], co_sem.at[slot])

    loads = [pltpu.make_async_copy(s, d, ld_sem.at[i]) for i, (s, d) in enumerate(((n_hbm, n_all), (dx0_hbm, dx0), (xs_hbm, xs), (g_hbm, g)))]
    loads[0].start()
    loads[1].start()
    e_copy(0).start()
    e_copy(1).start()
    for c in range(ahead):
        t_copy(c).start(priority=1)
    pair = stat_ref.shape[2]
    loss = jnp.zeros((1, pair), F32)
    for d in range(n_stage):
        if d % 2 == 0:
            shift[:, (d // 2) * pair:(d // 2 + 1) * pair] = stat_ref[d, 0:1, :] * LOG2E + math.log2(n_tok)
        loss = loss + part_ref[d, 0:1, :]
    loss_ref[0] = jnp.sum(loss) * inv_count
    with jax.named_scope("fin_pre"):
        loads[0].wait()
        n_t[...] = n_all[...].T

    def sum_rows():
        loads[1].wait()
        dense = jnp.concatenate([meta_ref[g:g + 1, :] for g in range(n_tok // LANES)], axis=1)
        order = lax.broadcasted_iota(jnp.int32, (n_tok, n_tok), 0) == dense
        dx0s[...] = dot(jnp.where(order, 1.0, 0.0).astype(BF16), dx0[...])

    def add_rows(k, start, ref):
        lo, hi = ids_ref[2 * n_tok + k], ids_ref[2 * n_tok + k + 1]
        wide = 8

        def some(p, width):
            at = [pl.ds(ids_ref[n_tok + p + u] - start, 1) for u in range(width)]
            new = [ref[at[u], :] + dx0s[pl.ds(p + u, 1), :] for u in range(width)]
            for u in range(width):
                ref[at[u], :] = new[u]

        def group(g, carry):
            some(lo + g * wide, wide)
            return carry

        def single(p, carry):
            some(p, 1)
            return carry

        n_grp = (hi - lo) // wide
        lax.fori_loop(0, n_grp, group, 0)
        lax.fori_loop(lo + n_grp * wide, hi, single, 0)

    def w_ins(w):
        cols = pl.ds(pl.multiple_of(w * wblk, wblk), wblk)
        wslot = lax.rem(w, 2)
        return (pltpu.make_async_copy(da_hbm.at[:, cols], da.at[wslot], wi_sem.at[0, wslot]), pltpu.make_async_copy(hid_hbm.at[:, cols], hid.at[wslot], wi_sem.at[1, wslot]))

    def w_outs(w):
        cols = pl.ds(pl.multiple_of(w * wblk, wblk), wblk)
        wslot = lax.rem(w, 2)
        return (pltpu.make_async_copy(gup.at[wslot], gup_hbm.at[:, cols], gu_sem.at[wslot]), pltpu.make_async_copy(gdown.at[wslot], gdown_hbm.at[cols], gd_sem.at[wslot]))

    def copy_tile(c, carry):
        with jax.named_scope("copy_wait"):
            t_copy(c).wait()
        with jax.named_scope("add_p"):
            add_rows(2 * steps + 2 * c, copy_start(c), cp.at[lax.rem(c, n_slot)])
        p_out(c).start()

        @pl.when(c + ahead < plan.copies)
        def _():
            pl.when(c + ahead >= n_slot)(lambda: p_out(c + ahead - n_slot).wait())
            t_copy(c + ahead).start(priority=1)

        return carry

    w_first = 2
    tails = [turn - 1, steps - 1]

    def tail(s):
        return (s == tails[0]) | (s == tails[1])

    def step(s, carry):
        pl.when(s + 2 < steps)(lambda: e_copy(s + 2).start())
        with jax.named_scope("fin_wait"):
            e_copy(s).wait()

        @pl.when(s == 0)
        def _():
            for c in loads[2:]:
                c.start()

        w = s - w_first

        @pl.when((w + 1 >= 0) & (w + 1 < n_wblk))
        def _():
            for c in w_ins(w + 1):
                c.start()

        pl.when((s >= 2) & jnp.logical_not(tail(s - 1)))(lambda: c_outs(s - 2).wait())
        slot = lax.rem(s, 2)
        start = calc_start(s)
        with jax.named_scope("calc"):
            logit_grad(e_in[lax.rem(s, 3)], n_t, shift, lab_ref, start, inv_count, scale, dz)
            c_out[slot] = dot(dz[...], n_all[...]) * scale
        pl.when(s == 0)(sum_rows)
        with jax.named_scope("add_c"):
            add_rows(2 * s, start, c_out.at[slot])
        pl.when(tail(s))(lambda: c_outs(s - 1).wait())
        c_outs(s).start()
        lax.fori_loop(s * plan.copies // (steps - 1), jnp.minimum((s + 1) * plan.copies // (steps - 1), plan.copies), copy_tile, 0)

        @pl.when(w == 0)
        def _():
            for c in loads[2:]:
                c.wait()
            x_t[...] = xs[...].T

        @pl.when((w >= 0) & (w < n_wblk))
        def _():
            wslot = lax.rem(w, 2)
            with jax.named_scope("dw_wait"):
                for c in w_ins(w):
                    c.wait()

                @pl.when(w >= 2)
                def _():
                    for c in w_outs(w - 2):
                        c.wait()

            with jax.named_scope("dw"):
                gup[wslot] = dot(x_t[...], da[wslot])
                gdown[wslot] = dot_t(hid[wslot], g[...])
            for c in w_outs(w):
                c.start()

        return carry

    lax.fori_loop(0, steps, step, 0)
    with jax.named_scope("fin_drain"):
        for w in range(n_wblk - 2, n_wblk):
            for c in w_outs(w):
                c.wait()
        c_outs(steps - 1).wait()
        for c in range(plan.copies - n_slot, plan.copies):
            p_out(c).wait()


def run_fin(emb, tmp, n_all, stats, losses, labels, meta, dx0, xs, hid, da, g, n_stage, plan):
    vocab, dim = emb.shape
    n_tok, ffn = hid.shape
    vm = pltpu.VMEM
    dma = pltpu.SemaphoreType.DMA
    any_spec = pl.BlockSpec(memory_space=pl.ANY)
    vspec = pl.BlockSpec(memory_space=pltpu.VMEM)
    smem = pl.BlockSpec(memory_space=pltpu.SMEM)
    wblk = 512
    return pl.pallas_call(
        functools.partial(fin_kernel, n_stage, n_tok, plan),
        out_shape=[jax.ShapeDtypeStruct((vocab, dim), F32), jax.ShapeDtypeStruct((1,), F32), jax.ShapeDtypeStruct((dim, ffn), F32), jax.ShapeDtypeStruct((ffn, dim), F32)],
        in_specs=[smem, any_spec, any_spec, any_spec, vspec, vspec, vspec, vspec] + [any_spec] * 5,
        out_specs=[any_spec, smem, any_spec, any_spec],
        scratch_shapes=[
            vm((n_tok, dim), BF16), vm((n_tok, dim), BF16), vm((n_tok, dim), BF16), vm((2, n_tok, wblk), BF16), vm((2, n_tok, wblk), BF16), vm((n_tok, dim), BF16),
            vm((dim, n_tok), BF16), vm((dim, n_tok), BF16), vm((n_tok, dim), F32), vm((plan.calc_rows, n_tok), BF16), vm((1, n_tok), F32),
            vm((3, plan.calc_rows, dim), BF16), vm((2, plan.calc_rows, dim), F32), vm((9, plan.copy_rows, dim), F32),
            vm((2, dim, wblk), F32), vm((2, wblk, dim), F32),
            dma((4,)), dma((3,)), dma((9,)), dma((2,)), dma((9,)), dma((2,)), dma((2,)), dma((2, 2)),
        ],
        compiler_params=pltpu.CompilerParams(vmem_limit_bytes=67_000_000),
        cost_estimate=pl.CostEstimate(flops=2 * n_tok * vocab * dim, bytes_accessed=5 * vocab * dim, transcendentals=0),
        name="fin",
    )(meta.reshape(-1), emb, tmp, n_all, stats, losses, labels.reshape(1, n_tok), meta, dx0, xs, hid, da, g)


def solution(mesh):
    n_stage = mesh.shape["stage"]

    def device_fn(tokens, labels, emb, w_up, w_down):
        n_micro, seq = tokens.shape
        vocab, dim = emb.shape
        w_up, w_down = w_up[0], w_down[0]
        n_tok = n_micro * seq
        plan = Plan(vocab, n_stage)
        cuts = jnp.array([plan.cuts(0), plan.cuts(1)], jnp.int32)
        x0 = run_gather(tokens, emb)
        n_all, xs, hid, da, g, dx0, stats, losses, tmp, meta = run_pipe(x0, emb, w_up, w_down, labels, tokens, cuts, n_stage, plan)
        flat = lambda p: p.reshape(n_tok, -1)
        grad_emb, loss, grad_up, grad_down = run_fin(
            emb, tmp.reshape(-1, dim), flat(n_all), stats, losses, labels, meta, flat(dx0), flat(xs), flat(hid), flat(da), flat(g), n_stage, plan
        )
        return loss, grad_up[None], grad_down[None], grad_emb

    return jax.shard_map(device_fn, mesh=mesh, in_specs=(P("dp", None), P("dp", None), P(None, None), P("stage", None, None), P("stage", None, None)), out_specs=(P("dp"), P(("dp", "stage"), None, None), P(("dp", "stage"), None, None), P("dp", None)), check_vma=False)
```

```python
import functools
import math

import jax
import jax.numpy as jnp
from jax import lax
from jax.experimental import pallas as pl
from jax.experimental.pallas import tpu as pltpu
from jax.sharding import PartitionSpec as P


MESH = pl.DeviceIdType.MESH
LOG2E = math.log2(math.e)
LN2 = math.log(2.0)
GELU_C = math.sqrt(2.0 / math.pi)
GELU_K = 0.044715
EPS = 1e-6
LANES = 128
F32 = jnp.float32
BF16 = jnp.bfloat16


def gelu_fwd(a):
    return (0.5 * a) * (1.0 + jnp.tanh(a * (GELU_C + (GELU_C * GELU_K) * (a * a))))


def gelu_slope(a):
    a2 = a * a
    half = 0.5 * jnp.tanh(a * (GELU_C + (GELU_C * GELU_K) * a2))
    up, down = 0.5 + half, 0.5 - half
    return up + (up * down) * (a * (2.0 * GELU_C + (6.0 * GELU_C * GELU_K) * a2))


def dot(x, y):
    return jnp.dot(x, y, preferred_element_type=F32)


def dot_t(x, y):
    return lax.dot_general(x, y, (((0,), (0,)), ((), ())), preferred_element_type=F32)


def remote(src, dst, send_sem, recv_sem, dev):
    return pltpu.make_async_remote_copy(src_ref=src, dst_ref=dst, send_sem=send_sem, recv_sem=recv_sem, device_id={"stage": dev}, device_id_type=MESH)


def column(row):
    return jnp.broadcast_to(row, (LANES, LANES)).T


def gather_kernel(ids_ref, tok_ref, emb_hbm, x0_hbm, tiles, picked, sem, out_sem):
    n_micro, seq = tok_ref.shape
    me = lax.axis_index("stage")
    group = tiles.shape[1] // seq
    slots = tiles.shape[0]
    owners = [head_chunk(me, k, n_micro) for k in range(slots)]

    def fetch(k):
        def one(i, carry):
            t = ids_ref[owners[k] * seq + i]
            start = pl.multiple_of(lax.bitwise_and(t, -group), group)
            pltpu.make_async_copy(emb_hbm.at[pl.ds(start, group)], tiles.at[k, pl.ds(pl.multiple_of(i * group, group), group)], sem.at[k]).start()
            return carry

        lax.fori_loop(0, seq, one, 0, unroll=8)

    def select(k):
        sub = lax.broadcasted_iota(jnp.int32, (LANES, LANES), 0)
        lane = lax.broadcasted_iota(jnp.int32, (LANES, LANES), 1)
        tok = column(tok_ref[pl.ds(owners[k], 1), :].astype(F32)).astype(jnp.int32)
        want = sub * group + lax.bitwise_and(tok, group - 1)
        hot = jnp.concatenate([jnp.where(lane + b * LANES == want, 1.0, 0.0).astype(BF16) for b in range(seq * group // LANES)], axis=1)
        pltpu.make_async_copy(emb_hbm.at[pl.ds(0, seq * group)], tiles.at[k], sem.at[k]).wait()
        picked[k] = dot(hot, tiles[k]).astype(BF16)
        pltpu.make_async_copy(picked.at[k], x0_hbm.at[k], out_sem.at[k]).start()

    def finish(k):
        pltpu.make_async_copy(picked.at[k], x0_hbm.at[k], out_sem.at[k]).wait()

    for work in (fetch, select, finish):
        work(0)
        for k in range(1, slots):
            pl.when(me < slots)(functools.partial(work, k))


def head_chunk(dev, k, n_micro):
    return jnp.minimum(jnp.where(dev < 2, 2 * dev + k, dev + 2), n_micro - 1)


def run_gather(tokens, emb):
    n_micro, seq = tokens.shape
    dim = emb.shape[1]
    group = 16
    return pl.pallas_call(
        gather_kernel,
        out_shape=jax.ShapeDtypeStruct((2, seq, dim), BF16),
        in_specs=[pl.BlockSpec(memory_space=pltpu.SMEM), pl.BlockSpec(memory_space=pltpu.VMEM), pl.BlockSpec(memory_space=pl.ANY)],
        out_specs=pl.BlockSpec(memory_space=pl.ANY),
        scratch_shapes=[pltpu.VMEM((2, seq * group, dim), BF16), pltpu.VMEM((2, seq, dim), BF16), pltpu.SemaphoreType.DMA((2,)), pltpu.SemaphoreType.DMA((2,))],
        cost_estimate=pl.CostEstimate(flops=10**9, bytes_accessed=2 * seq * group * dim * 2, transcendentals=0),
        name="gather",
    )(tokens.reshape(n_micro * seq), tokens, emb)


def token_table(row_ref, cut_ref, meta):
    n_tok = row_ref.shape[1]
    n_grp = n_tok // LANES
    lane = lax.broadcasted_iota(jnp.int32, (LANES, LANES), 1).astype(F32)
    sub = lax.broadcasted_iota(jnp.int32, (LANES, LANES), 0)
    row = lambda g: row_ref[:, g * LANES:(g + 1) * LANES].astype(F32)
    zero = jnp.zeros((LANES, LANES), F32)
    fold = lambda acc: jnp.sum(acc, axis=0, keepdims=True)
    cols = [column(row(c)) for c in range(n_grp)]
    firsts = []
    for g in range(n_grp):
        acc = zero
        for c in range(g + 1):
            same = cols[c] == row(g)
            if c == g:
                same = same & (sub < lane.astype(jnp.int32))
            acc = acc + jnp.where(same, 1.0, 0.0)
        firsts.append(column(jnp.where(fold(acc) == 0.0, 1.0, 0.0)))
    ranks = []
    for g in range(n_grp):
        acc = zero
        for c in range(n_grp):
            acc = acc + jnp.where(cols[c] < row(g), firsts[c], 0.0)
        ranks.append(fold(acc))
        meta[g:g + 1, :] = ranks[g].astype(jnp.int32)
    rank_cols = [column(r) for r in ranks]
    for g in range(n_grp):
        acc = zero
        for c in range(n_grp):
            acc = acc + jnp.where(rank_cols[c] == lane + g * LANES, firsts[c] * cols[c], 0.0)
        meta[n_grp + g:n_grp + g + 1, :] = fold(acc).astype(jnp.int32)
    cut = cut_ref[...].astype(F32)
    acc = zero
    for c in range(n_grp):
        acc = acc + jnp.where(cols[c] < cut, firsts[c], 0.0)
    meta[2 * n_grp:3 * n_grp, :] = jnp.broadcast_to(fold(acc), (n_grp, LANES)).astype(jnp.int32)


def logit_grad(e, n_t, shift, lab, first_id, inv_count, scale, dz):
    rows = e.shape[0]
    n_tok = n_t.shape[1]
    blk = 256
    vid = lax.broadcasted_iota(jnp.int32, (rows, blk), 0)
    for j in range(n_tok // blk):
        cols = slice(j * blk, (j + 1) * blk)
        z = (dot(e, n_t[:, cols]) * scale).astype(BF16).astype(F32)
        prob = jnp.exp2(z * LOG2E - shift[:, cols])
        dz[:, cols] = jnp.where(vid == lab[:, cols] - first_id, prob - inv_count, prob).astype(BF16)


def pipe_kernel(n_stage, plan, x0_hbm, emb_hbm, up_hbm, down_hbm, lab_hbm, row_hbm, cut_hbm,
                n_out, xs_out, hid_out, da_out, g_out, dx0_out, stat_out, loss_out, tmp_out, meta_out,
                xbuf, ybuf, abuf, hbuf, nbuf, gbuf, dxbuf, dx0buf, dnbuf, up, down, up_t, down_t,
                emb, zbuf, n_t, dn_acc, dn_send, dn_recv, dn_own, st_send, st_recv, statall, lossall, tops, n_all_t, shift, dz, obuf, z_pair, meta, lab_ref, row_ref, cut_ref,
                w_sem, e_sem, x_sem, x_send, x_recv, f_send, f_recv, n_send, n_recv, nf_send, ag_send, ag_recv, fw_send,
                st_sems, dp_sems, dn_ssem, dn_rsem, sa_sems, lo_sems, b_send, b_recv, d_send, d_recv, r_sems, out_sem, o_sem, od_send, od_recv, ic_send, in_sem):
    n_micro, seq, dim = gbuf.shape
    part = xbuf.shape[1]
    n_part = xbuf.shape[0]
    per = seq // part
    n_tok = n_micro * seq
    ffn = up.shape[1]
    vocab = emb_hbm.shape[0]
    me = lax.axis_index("stage")
    core = lax.rem(me, 2)
    chip = me // 2
    mate = me + 1 - 2 * core
    last_id = n_stage - 1
    first = me == 0
    last = me == last_id
    fblk = 512
    n_fblk = ffn // fblk
    base, extra, tile = plan.base, plan.extra, plan.head_tile
    row0 = core * (base + extra)
    n_tiles = base // tile
    wide_tile = plan.grad_tile

    barrier = pltpu.get_barrier_semaphore()
    gives_x = (me >= 1) & (me + 2 < n_micro)

    def here(dev):
        pl.semaphore_signal(barrier, inc=1, device_id={"stage": dev}, device_id_type=MESH)

    pl.when(jnp.logical_not(first))(lambda: here(me - 1))
    pl.when(jnp.logical_not(last))(lambda: here(me + 1))

    @pl.when(first)
    def _():
        for dev in range(2, n_micro - 2):
            here(dev)

    w_copy = [pltpu.make_async_copy(up_hbm, up, w_sem.at[0]), pltpu.make_async_copy(down_hbm, down, w_sem.at[1])]
    for c in w_copy:
        c.start()
    in_copy = [pltpu.make_async_copy(src, dst, in_sem.at[k]) for k, (src, dst) in enumerate(((lab_hbm, lab_ref), (row_hbm, row_ref), (cut_hbm, cut_ref)))]
    x_slots = x0_hbm.shape[0]
    x_mine = [head_chunk(me, k, n_micro) for k in range(x_slots)]

    def x_rows(m):
        return xbuf.at[pl.ds(m * per, per)]

    def x_local(k):
        return pltpu.make_async_copy(x0_hbm.at[k], x_rows(k), x_sem.at[k])

    @pl.when(first)
    def _():
        for k in range(x_slots):
            x_local(k).start()

    for c in in_copy:
        c.start()

    e_parts = plan.e_parts
    e_step = base // e_parts

    def e_copy(i):
        src = emb_hbm.at[pl.ds(pl.multiple_of(row0 + i * e_step, 16), e_step)]
        return pltpu.make_async_copy(src, emb.at[pl.ds(i * e_step, e_step)], e_sem.at[0])

    e_more = pltpu.make_async_copy(emb_hbm.at[pl.ds(base, extra)], emb.at[pl.ds(base, extra)], e_sem.at[1])
    with jax.named_scope("entry"):
        pl.semaphore_wait(barrier, jnp.where(first | last, 1, 2) + jnp.where(gives_x & (me >= 2), 1, 0))

    def x_copy(k):
        return remote(x0_hbm.at[k], x_rows(x_mine[k]), x_send.at[k], x_recv.at[x_mine[k]], 0)

    @pl.when(gives_x)
    def _():
        x_copy(0).start()

        @pl.when(me < 2)
        def _():
            x_copy(1).start()

    def table_start():
        for i in range(e_parts):
            e_copy(i).start()
        pl.when(core == 0)(e_more.start)

    def transpose_weights():
        for j in range(n_fblk):
            up_t[j * fblk:(j + 1) * fblk, :] = up[:, j * fblk:(j + 1) * fblk].T
            down_t[:, j * fblk:(j + 1) * fblk] = down[j * fblk:(j + 1) * fblk, :].T

    @pl.when(jnp.logical_not(first))
    def _():
        for c in w_copy:
            c.wait()
        table_start()

    def idle_work():
        transpose_weights()
        in_copy[1].wait()
        in_copy[2].wait()
        token_table(row_ref, jnp.where(core == 0, cut_ref[0:1, :], cut_ref[1:2, :]), meta)

    @pl.when(chip >= n_stage // 4)
    def _():
        idle_work()

    def n_start(m):
        remote(nbuf.at[m], nbuf.at[m], n_send, n_recv.at[m], jnp.where(m == last_id, last_id - 1, m)).start()

    def fwd(h, carry, cold=False):
        m = h // per
        sub = lax.rem(h, per)
        rows = pl.ds(pl.multiple_of(sub * part, part), part)
        with jax.named_scope("fwd_wait"):

            @pl.when(first & (sub == 0))
            def _():
                @pl.when(m < x_slots)
                def _():
                    x_local(m).wait()

                @pl.when(m >= x_slots)
                def _():
                    remote(x_rows(m), x_rows(m), x_send.at[0], x_recv.at[m], me).wait_recv()

            @pl.when(jnp.logical_not(first))
            def _():
                remote(xbuf.at[h], xbuf.at[h], f_send, f_recv.at[h], me).wait_recv()

        with jax.named_scope("fwd_comp"):
            x = xbuf[h]
            if cold:
                w_copy[0].wait()
            for j in range(n_fblk):
                cols = slice(j * fblk, (j + 1) * fblk)
                a = dot(x, up[:, cols]).astype(BF16)
                abuf[m, rows, cols] = a
                hbuf[m, rows, cols] = gelu_fwd(a.astype(F32)).astype(BF16)
            if cold:
                w_copy[1].wait()
                table_start()
            y = (x.astype(F32) + dot(hbuf[m, rows, :], down[...])).astype(BF16)
            ybuf[h] = y

        @pl.when(jnp.logical_not(last))
        def _():
            remote(ybuf.at[h], xbuf.at[h], f_send, f_recv.at[h], me + 1).start()

        @pl.when(last)
        def _():
            yf = y.astype(F32)
            inv = lax.rsqrt(jnp.mean(yf * yf, axis=-1, keepdims=True) + EPS)
            nbuf[m, rows, :] = (yf * inv).astype(BF16)
            pl.when(sub == per - 1)(lambda: n_start(m))

        @pl.when(sub == per - 1)
        def _():
            pltpu.make_async_copy(hbuf.at[m], hid_out.at[m], out_sem.at[0]).start()
            pltpu.make_async_copy(x_rows(m), xs_out.at[pl.ds(m * per, per)], out_sem.at[1]).start()

        return carry

    pl.when(first)(lambda: (fwd(0, 0, cold=True), None)[1])
    lax.fori_loop(jnp.where(first, 1, 0), n_part, fwd, 0)

    @pl.when(chip < n_stage // 4)
    def _():
        idle_work()

    n_forward = remote(nbuf.at[me], nbuf.at[me], nf_send, n_recv.at[me], mate)
    with jax.named_scope("n_wait"):

        @pl.when(jnp.logical_not(last))
        def _():
            remote(nbuf.at[me], nbuf.at[me], n_send, n_recv.at[me], me).wait_recv()
            pl.when(mate != last_id)(n_forward.start)
            remote(nbuf.at[mate], nbuf.at[mate], n_send, n_recv.at[mate], me).wait_recv()

        for k in range(2):
            n_t[:, k * seq:(k + 1) * seq] = nbuf[2 * chip + k].T

    peers = [lax.rem(me + 2 * d, n_stage) for d in range(1, n_stage // 2)]
    ag_copies = [remote(nbuf.at[me], nbuf.at[me], ag_send.at[d], ag_recv.at[me], p) for d, p in enumerate(peers)]
    for c, p in zip(ag_copies, peers):
        pl.when(p != last_id)(c.start)
    with jax.named_scope("e_wait"):
        pltpu.make_async_copy(emb_hbm.at[pl.ds(0, base)], emb.at[pl.ds(0, base)], e_sem.at[0]).wait()
        pl.when(core == 0)(e_more.wait)

    pair = 2 * seq
    scale = dim ** -0.5
    inv_count = 1.0 / n_tok
    log_count = math.log2(n_tok)
    in_copy[0].wait()
    lab = lab_ref[:, pl.ds(pl.multiple_of(chip * pair, pair), pair)]

    def logits(rows, size):
        e = emb[rows, :]
        parts = [dot(e[k * size // 2:(k + 1) * size // 2], n_t[...]) for k in range(2)]
        z = jnp.concatenate([(p * scale).astype(BF16) for p in parts], axis=0)
        zbuf[rows, :] = z
        return z

    def peak(z, size, top):
        best = jnp.max(z.reshape(size // 16, 16, pair), axis=0).astype(F32)
        return jnp.maximum(top, jnp.maximum(best[:8], best[8:]))

    def total(z, size, old, top, tot):
        off = top * LOG2E
        return tot * jnp.exp2(old * LOG2E - off) + jnp.sum(jnp.exp2(z.astype(F32).reshape(size // 8, 8, pair) * LOG2E - off[None]), axis=0)

    tops[0] = jnp.full((8, pair), -jnp.inf, F32)
    tops[1] = jnp.zeros((8, pair), F32)

    @pl.when(core == 0)
    def _():
        z = logits(pl.ds(base, extra), extra)
        top = peak(z, extra, tops[0])
        tops[1] = total(z, extra, tops[0], top, tops[1])
        tops[0] = top

    def logits_step(i, slot, old, top, tot):
        z = logits(pl.ds(pl.multiple_of(i * tile, 16), tile), tile)
        tot = total(z_pair[1 - slot], tile, old, top, tot)
        z_pair[slot] = z
        return top, peak(z, tile, top), tot

    with jax.named_scope("logits"):
        z = logits(pl.ds(0, tile), tile)
        z_pair[0] = z
        state = (tops[0], peak(z, tile, tops[0]), tops[1])
        state = lax.fori_loop(0, (n_tiles - 1) // 2, lambda i, c: logits_step(2 * i + 2, 0, *logits_step(2 * i + 1, 1, *c)), state)
        if n_tiles % 2 == 0:
            state = logits_step(n_tiles - 1, 1, *state)
        old, top, tot = state
        tot = total(z_pair[(n_tiles - 1) % 2], tile, old, top, tot)
    row_top = jnp.max(top, axis=0, keepdims=True)
    row_tot = jnp.sum(tot * jnp.exp2((top - row_top) * LOG2E), axis=0, keepdims=True)
    st_send[0:8, :] = jnp.broadcast_to(row_top, (8, pair))
    st_send[8:16, :] = jnp.broadcast_to(row_tot, (8, pair))
    st_copy = remote(st_send, st_recv, st_sems.at[0], st_sems.at[1], mate)
    with jax.named_scope("stat_x"):
        st_copy.start()
        st_copy.wait()
    far_top = st_recv[0:1, :]
    far_tot = st_recv[8:9, :]
    all_top = jnp.maximum(row_top, far_top)
    mine = row_tot * jnp.exp(row_top - all_top)
    other = far_tot * jnp.exp(far_top - all_top)
    lse = all_top + jnp.log(jnp.where(core == 0, mine + other, other + mine))
    my_shift = lse * LOG2E + log_count
    others = [lax.rem(me + d, n_stage) for d in range(1, n_stage)]

    def spread(buf, sems):
        whole = buf.at[pl.ds(0, n_stage - 1)]
        return [remote(buf.at[me], buf.at[me], sems.at[0], sems.at[1], p) for p in others], remote(whole, whole, sems.at[0], sems.at[1], me)

    statall[me] = jnp.broadcast_to(lse, (8, pair))
    sa_copies, sa_all = spread(statall, sa_sems)
    for c in sa_copies:
        c.start()

    def grads(rows, size, first_row, picked):
        zf = zbuf[rows, :].astype(F32)
        prob = jnp.exp2(zf * LOG2E - my_shift)
        hit = lax.broadcasted_iota(jnp.int32, (size, pair), 0) == lab - (row0 + first_row)
        dz_t = jnp.where(hit, prob - inv_count, prob).astype(BF16)
        got = jnp.where(hit, zf, 0.0).reshape(size // 8, 8, pair)
        return dot_t(dz_t, emb[rows, :]), picked + jnp.sum(got, axis=0)

    tops[0] = jnp.zeros((8, pair), F32)
    dn_acc[...] = jnp.zeros_like(dn_acc)

    @pl.when(core == 0)
    def _():
        dn_acc[...], tops[0] = grads(pl.ds(base, extra), extra, base, tops[0])

    def grad_step(i, picked):
        part, picked = grads(pl.ds(pl.multiple_of(i * wide_tile, 16), wide_tile), wide_tile, i * wide_tile, picked)
        dn_acc[...] += part
        return picked

    with jax.named_scope("grads"):
        picked = lax.fori_loop(0, base // wide_tile, grad_step, tops[0])
    far = pl.ds(pl.multiple_of((1 - core) * seq, seq), seq)
    near = pl.ds(pl.multiple_of(core * seq, seq), seq)
    dn_send[...] = dn_acc[far, :]
    dp_copy = remote(dn_send, dn_recv, dp_sems.at[0], dp_sems.at[1], mate)
    dp_copy.start()
    row_loss = jnp.where(core == 0, lse, 0.0) - jnp.sum(picked, axis=0, keepdims=True)
    lossall[me] = jnp.broadcast_to(row_loss, (8, pair))
    lo_copies, lo_all = spread(lossall, lo_sems)
    for c in lo_copies:
        c.start()
    with jax.named_scope("dn_x"):
        dp_copy.wait()
        dn = ((dn_acc[near, :] + dn_recv[...]) * scale).astype(BF16)
    dn_copy = remote(dn_own, dnbuf.at[me], dn_ssem, dn_rsem.at[me], last_id)

    @pl.when(last)
    def _():
        dnbuf[last_id] = dn

    @pl.when(jnp.logical_not(last))
    def _():
        dn_own[...] = dn
        remote(dn_own, dnbuf.at[me], dn_ssem, dn_rsem.at[me], last_id).start()

    with jax.named_scope("ag_wait"):
        for p in peers:
            got = remote(nbuf.at[p], nbuf.at[p], ag_send.at[0], ag_recv.at[p], me)
            pl.when(jnp.logical_not(last))(got.wait_recv)
            pl.when(mate != last_id)(remote(nbuf.at[p], nbuf.at[p], fw_send, ag_recv.at[p], mate).start)

    near_dst = [1, 3, last_id]
    far_dst = n_stage // 2 + 1
    direct = n_micro - 1
    by_prev = n_micro - 3
    hands_on = (core == 1) & (me != 1)

    def dx0_start(m, k, dev):
        remote(dxbuf.at[m], dx0buf.at[m], d_send.at[k], d_recv.at[m], dev).start()

    def relayed(m):
        return (m < direct) & (((me == 3) & (m != by_prev)) | (last & (m == by_prev)))

    def relay_far(m):
        remote(dx0buf.at[m], dx0buf.at[m], r_sems.at[1], d_recv.at[m], far_dst).start()

    def bwd(m):
        with jax.named_scope("bwd_wait"):
            @pl.when(jnp.logical_not(last))
            def _():
                remote(gbuf.at[m], gbuf.at[m], b_send, b_recv.at[m], me).wait_recv()

            @pl.when(last)
            def _():
                @pl.when(m != last_id)
                def _():
                    remote(dnbuf.at[m], dnbuf.at[m], dn_ssem, dn_rsem.at[m], me).wait_recv()

                yf = ybuf[pl.ds(m * per, per)].reshape(seq, dim).astype(F32)
                inv = lax.rsqrt(jnp.mean(yf * yf, axis=-1, keepdims=True) + EPS)
                dnf = dnbuf[m].astype(F32)
                proj = jnp.mean(yf * dnf, axis=-1, keepdims=True)
                gbuf[m] = (dnf * inv - yf * (inv * inv * inv * proj)).astype(BF16)

        with jax.named_scope("bwd_comp"):
            g = gbuf[m]
            for j in range(n_fblk):
                cols = slice(j * fblk, (j + 1) * fblk)
                dh = dot(g, down_t[:, cols]).astype(BF16).astype(F32)
                abuf[m, :, cols] = (dh * gelu_slope(abuf[m, :, cols].astype(F32))).astype(BF16)
            dxbuf[m] = (g.astype(F32) + dot(abuf[m], up_t[...])).astype(BF16)

        @pl.when(jnp.logical_not(first))
        def _():
            remote(dxbuf.at[m], gbuf.at[m], b_send, b_recv.at[m], me - 1).start()

        @pl.when(first)
        def _():
            pl.when(m >= direct)(lambda: dx0_start(m, len(near_dst), far_dst))
            for k, dev in enumerate(near_dst):
                dx0_start(m, k, dev)

        pltpu.make_async_copy(abuf.at[m], da_out.at[m], out_sem.at[2]).start()
        pltpu.make_async_copy(gbuf.at[m], g_out.at[m], out_sem.at[3]).start()

    n_slot = obuf.shape[0]
    busy = chip == last_id // 2
    far_tile = remote(tmp_out.at[core, pl.ds(0, plan.rows)], tmp_out.at[core, pl.ds(0, plan.rows)], ic_send, od_recv, jnp.where(first, last_id, last_id - 1))
    sends_far = first | (me == last_id - 2)

    def tile_copy(k):
        rows = pl.ds(pl.multiple_of(k * plan.rows, plan.rows), plan.rows)
        slot = lax.rem(k, n_slot)
        return pltpu.make_async_copy(obuf.at[slot], tmp_out.at[core, rows], o_sem.at[slot])

    def piece(p):
        k = p // plan.per_tile
        rows = pl.ds(pl.multiple_of(p * plan.piece, plan.piece), plan.piece)
        here = pl.ds(pl.multiple_of(lax.rem(p, plan.per_tile) * plan.piece, plan.piece), plan.piece)
        return remote(obuf.at[lax.rem(k, n_slot), here], tmp_out.at[core, rows], od_send.at[k], od_recv, mate)

    def tile_sent(k):
        slot = lax.rem(k, n_slot)
        return remote(obuf.at[slot], tmp_out.at[core, pl.ds(0, plan.rows)], od_send.at[k], od_recv, mate)

    def emb_tile(k):
        with jax.named_scope("tile_prep"):

            @pl.when(k == 0)
            def _():
                for d in range(1, n_stage // 2):
                    src = lax.rem(mate + 2 * d, n_stage)
                    pl.when(jnp.logical_not(last))(remote(nbuf.at[src], nbuf.at[src], ag_send.at[0], ag_recv.at[src], me).wait_recv)
                for m in range(n_micro):
                    n_all_t[:, m * seq:(m + 1) * seq] = nbuf[m].T
                sa_all.wait_recv()
                for c in range(n_stage // 2):
                    shift[:, c * pair:(c + 1) * pair] = statall[2 * c, 0:1, :] * LOG2E + log_count

        slot = lax.rem(k, n_slot)
        with jax.named_scope("tile_wait"):
            @pl.when(k == 2)
            def _():
                tile_copy(0).wait()
                pl.when(sends_far)(far_tile.start)

            pl.when(k > n_slot)(lambda: tile_copy(k - n_slot).wait())
            pl.when((k >= n_slot) & (k - n_slot < plan.shared) & jnp.logical_not(busy & (k == n_slot)))(lambda: tile_sent(k - n_slot).wait_send())

        with jax.named_scope("tile"):
            rows = pl.ds(pl.multiple_of(k * plan.rows, plan.rows), plan.rows)
            logit_grad(emb[rows, :], n_all_t, shift, lab_ref, row0 + k * plan.rows, inv_count, scale, dz)
            obuf[slot] = dot(dz[...], nbuf[...].reshape(n_tok, dim)) * scale

        tile_copy(k).start()

    def send_pieces(done, until):
        lax.fori_loop(done, until, lambda p, c: (piece(p).start(), c)[1], 0)

    def send_tiles(done, until):
        def one(k, carry):
            rows = pl.ds(pl.multiple_of(k * plan.rows, plan.rows), plan.rows)
            remote(obuf.at[lax.rem(k, n_slot)], tmp_out.at[core, rows], od_send.at[k], od_recv, mate).start()
            return carry

        lax.fori_loop(done, until, one, 0)

    before = sum(jnp.where(me == s, plan.before[s], 0) for s in range(n_stage))

    def pass_dx0(m, carry):
        @pl.when(jnp.logical_not(first))
        def _():
            remote(dx0buf.at[m], dx0buf.at[m], r_sems.at[0], d_recv.at[m], me).wait_recv()

            @pl.when(hands_on)
            def _():
                remote(dx0buf.at[m], dx0buf.at[m], r_sems.at[0], d_recv.at[m], mate).start()

            @pl.when(relayed(m))
            def _():
                relay_far(m)

            pltpu.make_async_copy(dx0buf.at[m], dx0_out.at[m], out_sem.at[4]).start()

        @pl.when(first)
        def _():
            pltpu.make_async_copy(dxbuf.at[m], dx0_out.at[m], out_sem.at[4]).start()

        return carry

    lead = jnp.where(me == 3, -300, jnp.where(last, -1800, jnp.where(me == far_dst, -1600, -10**6)))

    def work(i, carry):
        sent, passed = carry
        chunk = (i >= before) & (i < before + n_micro)
        pl.when(chunk)(lambda: bwd(i - before))
        k = jnp.where(i < before, i, i - n_micro)
        pl.when(jnp.logical_not(chunk))(lambda: emb_tile(k))
        after = i - before - n_micro + 1
        here = jnp.where(after > 0, jnp.clip((after * 264 + lead) // 138, 0, n_micro), 0)
        lax.fori_loop(passed, here, pass_dx0, 0)
        ready = jnp.where(i < before, i + 1, jnp.where(chunk, before, i + 1 - n_micro))
        near_chunks = chunk | ((i < before) & (i + 1 >= before))
        whole = (sent + plan.per_tile - 1) // plan.per_tile
        upto = jnp.minimum(jnp.minimum(ready, plan.shared), whole + 1)
        some = jnp.where(near_chunks, jnp.minimum(sent + 1, jnp.minimum(ready, plan.shared) * plan.per_tile), whole * plan.per_tile)
        send_pieces(sent, some)
        send_tiles(whole, jnp.where(near_chunks, 0, upto))
        now = jnp.where(near_chunks, some, jnp.maximum(some, upto * plan.per_tile))
        return jnp.maximum(sent, now), jnp.maximum(passed, here)

    sent, passed = lax.fori_loop(0, plan.tiles + n_micro, work, (jnp.where(busy, plan.per_tile, 0), 0))
    outs = [pltpu.make_async_copy(nbuf, n_out, out_sem.at[5]), pltpu.make_async_copy(lossall, loss_out, out_sem.at[6]), pltpu.make_async_copy(meta, meta_out, out_sem.at[7])]
    lo_all.wait_recv()
    for c in outs:
        c.start()
    pltpu.make_async_copy(statall, stat_out, out_sem.at[8]).start()
    with jax.named_scope("relay_all"):
        lax.fori_loop(passed, n_micro, pass_dx0, 0)

    with jax.named_scope("drain"):
        send_pieces(sent, plan.shared * plan.per_tile)
        for k in range(max(plan.tiles - n_slot, 0), plan.tiles):
            tile_copy(k).wait()
            if k < plan.shared:
                tile_sent(k).wait_send()
        pl.when(sends_far)(far_tile.wait_send)
        all_rows = pl.ds(0, plan.shared * plan.rows)
        remote(tmp_out.at[1 - core, all_rows], tmp_out.at[1 - core, all_rows], od_send.at[0], od_recv, me).wait_recv()
        sa_all.wait_send()
        lo_all.wait_send()
        pltpu.make_async_copy(statall, stat_out, out_sem.at[8]).wait()
        for c, p in zip(ag_copies, peers):
            pl.when(p != last_id)(c.wait_send)

        @pl.when(jnp.logical_not(last))
        def _():
            dn_copy.wait_send()
            pl.when(mate != last_id)(n_forward.wait_send)
            remote(ybuf, xbuf, f_send, f_recv.at[0], me + 1).wait_send()

        @pl.when(last)
        def _():
            remote(nbuf, nbuf, n_send, n_recv.at[0], me).wait_send()

        @pl.when(mate != last_id)
        def _():
            some = nbuf.at[pl.ds(0, len(peers))]
            remote(some, some, fw_send, ag_recv.at[0], mate).wait_send()

        @pl.when(gives_x)
        def _():
            x_copy(0).wait_send()

            @pl.when(me < 2)
            def _():
                x_copy(1).wait_send()

        @pl.when(jnp.logical_not(first))
        def _():
            remote(dxbuf, gbuf, b_send, b_recv.at[0], me).wait_send()
            pl.when(hands_on)(remote(dx0buf, dx0buf, r_sems.at[0], d_recv.at[0], mate).wait_send)

        @pl.when(first)
        def _():
            for k in range(len(near_dst)):
                remote(dxbuf, dx0buf, d_send.at[k], d_recv.at[0], me).wait_send()
            rest = pl.ds(0, n_micro - direct)
            remote(dxbuf.at[rest], dx0buf.at[rest], d_send.at[len(near_dst)], d_recv.at[0], me).wait_send()

        for dev, kept in ((3, direct - 1), (last_id, 1)):
            some = dx0buf.at[pl.ds(0, kept)]
            pl.when(me == dev)(remote(some, some, r_sems.at[1], d_recv.at[0], me).wait_send)

        pltpu.make_async_copy(hbuf, hid_out, out_sem.at[0]).wait()
        pltpu.make_async_copy(xbuf, xs_out, out_sem.at[1]).wait()
        pltpu.make_async_copy(abuf, da_out, out_sem.at[2]).wait()
        pltpu.make_async_copy(gbuf, g_out, out_sem.at[3]).wait()
        pltpu.make_async_copy(dx0buf, dx0_out, out_sem.at[4]).wait()
        for c in outs:
            c.wait()


class Plan:
    def __init__(self, vocab, n_stage):
        units = vocab // LANES
        self.base = units // 2 * LANES
        self.extra = vocab - 2 * self.base
        self.head_tile = next(t for t in (1600, 1536, 1280, 1024, 768, 640, 512, 256, 128) if self.base % t == 0)
        self.rows = 1024
        self.tiles, self.shared = 11, 9
        self.grad_tile = next(t for t in (4000, 3200, 1600, 1280, 640, 256, 128) if self.base % t == 0)
        self.e_parts = next(k for k in (10, 8, 5, 4, 2, 1) if self.base % (16 * k) == 0)
        self.part = 128
        self.slots = 4
        self.piece = 256
        self.per_tile = self.rows // self.piece
        measured = [10, 9, 6, 5, 3, 2, 0, 0]
        self.before = (measured + [0] * n_stage)[:n_stage]
        mid = self.base + self.extra
        ends = [(0, mid), (mid, vocab)]
        early = (self.tiles * self.rows, self.shared * self.rows)
        self.spans = [[(ends[h][0] + early[0 if h == c else 1], ends[h][1]) for h in (c, 1 - c)] for c in range(2)]
        self.longest = [max(self.spans[c][k][1] - self.spans[c][k][0] for c in range(2)) for k in range(2)]
        best = min(range(16, 1281, 16), key=lambda r: (sum(-(-n // r) for n in self.longest)) * (r + 40))
        self.calc_rows = best
        self.calc_steps = [-(-n // best) for n in self.longest]
        self.steps = sum(self.calc_steps)
        self.copy_rows = self.rows
        self.copies = self.tiles + self.shared
        self.starts = ends

    def calc_start(self, core, s):
        k = 0 if s < self.calc_steps[0] else 1
        lo, hi = self.spans[core][k]
        return min(lo + (s - k * self.calc_steps[0]) * self.calc_rows, hi - self.calc_rows)

    def copy_start(self, core, c):
        own = c < self.tiles
        h = core if own else 1 - core
        return self.starts[h][0] + (c if own else c - self.tiles) * self.copy_rows

    def cuts(self, core):
        firsts = [(self.calc_start(core, s), self.calc_rows) for s in range(self.steps)] + [(self.copy_start(core, c), self.copy_rows) for c in range(self.copies)]
        flat = [v for lo, rows in firsts for v in (lo, lo + rows)]
        return flat + [0] * (LANES - len(flat))


def run_pipe(x0, emb, w_up, w_down, labels, tokens, cuts, n_stage, plan):
    n_micro, seq = labels.shape
    dim, ffn = w_up.shape
    n_tok = n_micro * seq
    base = plan.base
    any_spec = pl.BlockSpec(memory_space=pl.ANY)
    act = (n_micro, seq, dim)
    fine = (n_tok // plan.part, plan.part, dim)
    wide = (n_micro, seq, ffn)
    dma = pltpu.SemaphoreType.DMA
    vm = pltpu.VMEM
    pair = 2 * seq
    return pl.pallas_call(
        functools.partial(pipe_kernel, n_stage, plan),
        out_shape=[
            jax.ShapeDtypeStruct(act, BF16), jax.ShapeDtypeStruct(fine, BF16), jax.ShapeDtypeStruct(wide, BF16),
            jax.ShapeDtypeStruct(wide, BF16), jax.ShapeDtypeStruct(act, BF16), jax.ShapeDtypeStruct(act, BF16),
            jax.ShapeDtypeStruct((n_stage, 8, pair), F32), jax.ShapeDtypeStruct((n_stage, 8, pair), F32), jax.ShapeDtypeStruct((2, plan.tiles * plan.rows, dim), F32),
            jax.ShapeDtypeStruct((3 * n_tok // LANES, LANES), jnp.int32),
        ],
        in_specs=[any_spec] * 7,
        out_specs=[any_spec] * 10,
        scratch_shapes=[
            vm(fine, BF16), vm(fine, BF16), vm(wide, BF16), vm(wide, BF16), vm(act, BF16), vm(act, BF16), vm(act, BF16), vm(act, BF16), vm(act, BF16),
            vm((dim, ffn), BF16), vm((ffn, dim), BF16), vm((ffn, dim), BF16), vm((dim, ffn), BF16),
            vm((base + plan.extra, dim), BF16), vm((base + plan.extra, pair), BF16), vm((dim, pair), BF16), vm((pair, dim), F32),
            vm((seq, dim), F32), vm((seq, dim), F32), vm((seq, dim), BF16), vm((16, pair), F32), vm((16, pair), F32), vm((n_stage, 8, pair), F32), vm((n_stage, 8, pair), F32),
            vm((2, 8, pair), F32), vm((dim, n_tok), BF16), vm((1, n_tok), F32), vm((plan.rows, n_tok), BF16), vm((plan.slots, plan.rows, dim), F32),
            vm((2, plan.head_tile, pair), BF16), vm((3 * n_tok // LANES, LANES), jnp.int32),
            vm((1, n_tok), jnp.int32), vm((1, n_tok), jnp.int32), vm((2, LANES), jnp.int32),
            dma((2,)), dma((2,)), dma((2,)), dma((2,)), dma((n_micro,)), dma, dma((n_tok // plan.part,)), dma, dma((n_micro,)), dma,
            dma((n_stage // 2,)), dma((n_micro,)), dma,
            dma((2,)), dma((2,)), dma, dma((n_stage,)), dma((2,)), dma((2,)), dma, dma((n_micro,)), dma((4,)), dma((n_micro,)), dma((2,)), dma((9,)),
            dma((plan.slots,)), dma((plan.shared,)), dma, dma, dma((3,)),
        ],
        compiler_params=pltpu.CompilerParams(collective_id=0, has_side_effects=True, vmem_limit_bytes=67_000_000),
        cost_estimate=pl.CostEstimate(flops=60 * 10**9, bytes_accessed=100 * 10**6, transcendentals=0),
        name="pipe",
    )(x0.reshape(x0.shape[0], seq // plan.part, plan.part, dim), emb, w_up, w_down, labels.reshape(1, n_tok), tokens.reshape(1, n_tok), cuts)


def fin_kernel(n_stage, n_tok, plan, ids_hbm, emb_hbm, tmp_hbm, n_hbm, stat_hbm, part_hbm, lab_hbm, meta_hbm, dx0_hbm, xs_hbm, hid_hbm, da_hbm, g_hbm,
               out_hbm, loss_ref, gup_hbm, gdown_hbm,
               n_all, dx0, xs, hid, da, g, n_t, x_t, dx0s, dz, shift, e_in, c_out, cp, gup, gdown,
               ld_sem, e_sem, t_sem, co_sem, po_sem, gu_sem, gd_sem, wi_sem, ids_ref, stat_ref, part_ref, lab_ref, meta_ref, in_sem):
    dim, ffn = gup_hbm.shape
    scale = dim ** -0.5
    inv_count = 1.0 / n_tok
    steps, crows, prows = plan.steps, plan.calc_rows, plan.copy_rows
    core = lax.rem(lax.axis_index("stage"), 2)
    early = plan.tiles * prows
    wblk = gup.shape[2]
    n_wblk = ffn // wblk
    turn = plan.calc_steps[0]

    def pick(pair):
        return jnp.where(core == 0, pair[0], pair[1])

    def calc_start(s):
        own = s < turn
        lo, hi = [jnp.where(own, pick([plan.spans[c][0][e] for c in range(2)]), pick([plan.spans[c][1][e] for c in range(2)])) for e in range(2)]
        return pl.multiple_of(jnp.minimum(lo + (s - jnp.where(own, 0, turn)) * crows, hi - crows), 16)

    def copy_start(c):
        own = c < plan.tiles
        first = jnp.where(own, pick([plan.starts[0][0], plan.starts[1][0]]), pick([plan.starts[1][0], plan.starts[0][0]]))
        return pl.multiple_of(first + (c - jnp.where(own, 0, plan.tiles)) * prows, 16)

    def e_copy(s):
        return pltpu.make_async_copy(emb_hbm.at[pl.ds(calc_start(s), crows)], e_in.at[lax.rem(s, 3)], e_sem.at[lax.rem(s, 3)])

    n_slot = cp.shape[0]
    ahead = 6

    def t_copy(c):
        own = c < plan.tiles
        row = jnp.where(own, core, 1 - core) * early + (c - jnp.where(own, 0, plan.tiles)) * prows
        slot = lax.rem(c, n_slot)
        return pltpu.make_async_copy(tmp_hbm.at[pl.ds(pl.multiple_of(row, 16), prows)], cp.at[slot], t_sem.at[slot])

    def p_out(c):
        slot = lax.rem(c, n_slot)
        return pltpu.make_async_copy(cp.at[slot], out_hbm.at[pl.ds(copy_start(c), prows)], po_sem.at[slot])

    def c_outs(s):
        slot = lax.rem(s, 2)
        return pltpu.make_async_copy(c_out.at[slot], out_hbm.at[pl.ds(calc_start(s), crows)], co_sem.at[slot])

    loads = [pltpu.make_async_copy(s, d, ld_sem.at[i]) for i, (s, d) in enumerate(((n_hbm, n_all), (dx0_hbm, dx0), (xs_hbm, xs), (g_hbm, g)))]
    ins = [pltpu.make_async_copy(s, d, in_sem.at[i]) for i, (s, d) in enumerate(((stat_hbm, stat_ref), (lab_hbm, lab_ref), (part_hbm, part_ref), (meta_hbm, meta_ref), (ids_hbm, ids_ref)))]
    loads[0].start()
    ins[0].start()
    ins[1].start()
    e_copy(0).start()
    loads[1].start()
    for c in ins[2:]:
        c.start()
    e_copy(1).start()
    for c in range(ahead):
        t_copy(c).start(priority=1)
    pair = stat_ref.shape[2]
    with jax.named_scope("fin_pre"):
        ins[0].wait()
        ins[1].wait()
        for c in range(n_stage // 2):
            shift[:, c * pair:(c + 1) * pair] = stat_ref[2 * c, 0:1, :] * LOG2E + math.log2(n_tok)
        loads[0].wait()
        n_t[...] = n_all[...].T

    def sum_rows():
        for c in ins[2:]:
            c.wait()
        loss_ref[0] = jnp.sum(sum(part_ref[d, 0:1, :] for d in range(n_stage))) * inv_count
        loads[1].wait()
        dense = jnp.concatenate([meta_ref[g:g + 1, :] for g in range(n_tok // LANES)], axis=1)
        order = lax.broadcasted_iota(jnp.int32, (n_tok, n_tok), 0) == dense
        dx0s[...] = dot(jnp.where(order, 1.0, 0.0).astype(BF16), dx0[...])

    def add_rows(k, start, ref):
        lo, hi = ids_ref[2 * n_tok + k], ids_ref[2 * n_tok + k + 1]
        wide = 8

        def some(p, width):
            at = [pl.ds(ids_ref[n_tok + p + u] - start, 1) for u in range(width)]
            new = [ref[at[u], :] + dx0s[pl.ds(p + u, 1), :] for u in range(width)]
            for u in range(width):
                ref[at[u], :] = new[u]

        def group(g, carry):
            some(lo + g * wide, wide)
            return carry

        def single(p, carry):
            some(p, 1)
            return carry

        n_grp = (hi - lo) // wide
        lax.fori_loop(0, n_grp, group, 0)
        lax.fori_loop(lo + n_grp * wide, hi, single, 0)

    def w_ins(w):
        cols = pl.ds(pl.multiple_of(w * wblk, wblk), wblk)
        wslot = lax.rem(w, 2)
        return (pltpu.make_async_copy(da_hbm.at[:, cols], da.at[wslot], wi_sem.at[0, wslot]), pltpu.make_async_copy(hid_hbm.at[:, cols], hid.at[wslot], wi_sem.at[1, wslot]))

    def w_outs(w):
        cols = pl.ds(pl.multiple_of(w * wblk, wblk), wblk)
        wslot = lax.rem(w, 2)
        return (pltpu.make_async_copy(gup.at[wslot], gup_hbm.at[:, cols], gu_sem.at[wslot]), pltpu.make_async_copy(gdown.at[wslot], gdown_hbm.at[cols], gd_sem.at[wslot]))

    def copy_tile(c, carry):
        with jax.named_scope("copy_wait"):
            t_copy(c).wait()
        with jax.named_scope("add_p"):
            add_rows(2 * steps + 2 * c, copy_start(c), cp.at[lax.rem(c, n_slot)])
        p_out(c).start()

        @pl.when(c + ahead < plan.copies)
        def _():
            pl.when(c + ahead >= n_slot)(lambda: p_out(c + ahead - n_slot).wait())
            t_copy(c + ahead).start(priority=1)

        return carry

    w_first = 2
    tails = [turn - 1, steps - 1]

    def tail(s):
        return (s == tails[0]) | (s == tails[1])

    def step(s, carry):
        pl.when(s + 2 < steps)(lambda: e_copy(s + 2).start())
        with jax.named_scope("fin_wait"):
            e_copy(s).wait()

        @pl.when(s == 0)
        def _():
            for c in loads[2:]:
                c.start()

        w = s - w_first

        @pl.when((w + 1 >= 0) & (w + 1 < n_wblk))
        def _():
            for c in w_ins(w + 1):
                c.start()

        pl.when((s >= 2) & jnp.logical_not(tail(s - 1)))(lambda: c_outs(s - 2).wait())
        slot = lax.rem(s, 2)
        start = calc_start(s)
        with jax.named_scope("calc"):
            logit_grad(e_in[lax.rem(s, 3)], n_t, shift, lab_ref, start, inv_count, scale, dz)
            c_out[slot] = dot(dz[...], n_all[...]) * scale
        pl.when(s == 0)(sum_rows)
        with jax.named_scope("add_c"):
            add_rows(2 * s, start, c_out.at[slot])
        pl.when(tail(s))(lambda: c_outs(s - 1).wait())
        c_outs(s).start()
        lax.fori_loop(s * plan.copies // (steps - 1), jnp.minimum((s + 1) * plan.copies // (steps - 1), plan.copies), copy_tile, 0)

        @pl.when(w == 0)
        def _():
            for c in loads[2:]:
                c.wait()
            x_t[...] = xs[...].T

        @pl.when((w >= 0) & (w < n_wblk))
        def _():
            wslot = lax.rem(w, 2)
            with jax.named_scope("dw_wait"):
                for c in w_ins(w):
                    c.wait()

                @pl.when(w >= 2)
                def _():
                    for c in w_outs(w - 2):
                        c.wait()

            with jax.named_scope("dw"):
                gup[wslot] = dot(x_t[...], da[wslot])
                gdown[wslot] = dot_t(hid[wslot], g[...])
            for c in w_outs(w):
                c.start()

        return carry

    lax.fori_loop(0, steps, step, 0)
    with jax.named_scope("fin_drain"):
        for w in range(n_wblk - 2, n_wblk):
            for c in w_outs(w):
                c.wait()
        c_outs(steps - 1).wait()
        for c in range(plan.copies - n_slot, plan.copies):
            p_out(c).wait()


def run_fin(emb, tmp, n_all, stats, losses, labels, meta, dx0, xs, hid, da, g, n_stage, plan):
    vocab, dim = emb.shape
    n_tok, ffn = hid.shape
    vm = pltpu.VMEM
    dma = pltpu.SemaphoreType.DMA
    any_spec = pl.BlockSpec(memory_space=pl.ANY)
    smem = pl.BlockSpec(memory_space=pltpu.SMEM)
    wblk = 512
    return pl.pallas_call(
        functools.partial(fin_kernel, n_stage, n_tok, plan),
        out_shape=[jax.ShapeDtypeStruct((vocab, dim), F32), jax.ShapeDtypeStruct((1,), F32), jax.ShapeDtypeStruct((dim, ffn), F32), jax.ShapeDtypeStruct((ffn, dim), F32)],
        in_specs=[any_spec] * 13,
        out_specs=[any_spec, smem, any_spec, any_spec],
        scratch_shapes=[
            vm((n_tok, dim), BF16), vm((n_tok, dim), BF16), vm((n_tok, dim), BF16), vm((2, n_tok, wblk), BF16), vm((2, n_tok, wblk), BF16), vm((n_tok, dim), BF16),
            vm((dim, n_tok), BF16), vm((dim, n_tok), BF16), vm((n_tok, dim), F32), vm((plan.calc_rows, n_tok), BF16), vm((1, n_tok), F32),
            vm((3, plan.calc_rows, dim), BF16), vm((2, plan.calc_rows, dim), F32), vm((9, plan.copy_rows, dim), F32),
            vm((2, dim, wblk), F32), vm((2, wblk, dim), F32),
            dma((4,)), dma((3,)), dma((9,)), dma((2,)), dma((9,)), dma((2,)), dma((2,)), dma((2, 2)),
            pltpu.SMEM((meta.size,), jnp.int32), vm(stats.shape, F32), vm(losses.shape, F32), vm((1, n_tok), jnp.int32), vm(meta.shape, jnp.int32), dma((5,)),
        ],
        compiler_params=pltpu.CompilerParams(vmem_limit_bytes=67_000_000),
        cost_estimate=pl.CostEstimate(flops=2 * n_tok * vocab * dim, bytes_accessed=5 * vocab * dim, transcendentals=0),
        name="fin",
    )(meta.reshape(-1), emb, tmp, n_all, stats, losses, labels.reshape(1, n_tok), meta, dx0, xs, hid, da, g)


def solution(mesh):
    n_stage = mesh.shape["stage"]

    def device_fn(tokens, labels, emb, w_up, w_down):
        n_micro, seq = tokens.shape
        vocab, dim = emb.shape
        w_up, w_down = w_up[0], w_down[0]
        n_tok = n_micro * seq
        plan = Plan(vocab, n_stage)
        cuts = jnp.array([plan.cuts(0), plan.cuts(1)], jnp.int32)
        x0 = run_gather(tokens, emb)
        n_all, xs, hid, da, g, dx0, stats, losses, tmp, meta = run_pipe(x0, emb, w_up, w_down, labels, tokens, cuts, n_stage, plan)
        flat = lambda p: p.reshape(n_tok, -1)
        grad_emb, loss, grad_up, grad_down = run_fin(
            emb, tmp.reshape(-1, dim), flat(n_all), stats, losses, labels, meta, flat(dx0), flat(xs), flat(hid), flat(da), flat(g), n_stage, plan
        )
        return loss, grad_up[None], grad_down[None], grad_emb

    return jax.shard_map(device_fn, mesh=mesh, in_specs=(P("dp", None), P("dp", None), P(None, None), P("stage", None, None), P("stage", None, None)), out_specs=(P("dp"), P(("dp", "stage"), None, None), P(("dp", "stage"), None, None), P("dp", None)), check_vma=False)
```

```python
import functools
import math

import jax
import jax.numpy as jnp
from jax import lax
from jax.experimental import pallas as pl
from jax.experimental.pallas import tpu as pltpu
from jax.sharding import PartitionSpec as P


MESH = pl.DeviceIdType.MESH
LOG2E = math.log2(math.e)
LN2 = math.log(2.0)
GELU_C = math.sqrt(2.0 / math.pi)
GELU_K = 0.044715
EPS = 1e-6
LANES = 128
F32 = jnp.float32
BF16 = jnp.bfloat16


def gelu_fwd(a):
    return (0.5 * a) * (1.0 + jnp.tanh(a * (GELU_C + (GELU_C * GELU_K) * (a * a))))


def gelu_slope(a):
    a2 = a * a
    half = 0.5 * jnp.tanh(a * (GELU_C + (GELU_C * GELU_K) * a2))
    up, down = 0.5 + half, 0.5 - half
    return up + (up * down) * (a * (2.0 * GELU_C + (6.0 * GELU_C * GELU_K) * a2))


def dot(x, y):
    return jnp.dot(x, y, preferred_element_type=F32)


def dot_t(x, y):
    return lax.dot_general(x, y, (((0,), (0,)), ((), ())), preferred_element_type=F32)


def remote(src, dst, send_sem, recv_sem, dev):
    return pltpu.make_async_remote_copy(src_ref=src, dst_ref=dst, send_sem=send_sem, recv_sem=recv_sem, device_id={"stage": dev}, device_id_type=MESH)


def column(row):
    return jnp.broadcast_to(row, (LANES, LANES)).T


def gather_kernel(ids_ref, tok_ref, emb_hbm, x0_hbm, tiles, picked, sem, out_sem):
    n_micro, seq = tok_ref.shape
    me = lax.axis_index("stage")
    group = tiles.shape[1] // seq
    slots = tiles.shape[0]
    owners = [head_chunk(me, k, n_micro) for k in range(slots)]

    def fetch(k):
        def one(i, carry):
            t = ids_ref[owners[k] * seq + i]
            start = pl.multiple_of(lax.bitwise_and(t, -group), group)
            pltpu.make_async_copy(emb_hbm.at[pl.ds(start, group)], tiles.at[k, pl.ds(pl.multiple_of(i * group, group), group)], sem.at[k]).start()
            return carry

        lax.fori_loop(0, seq, one, 0, unroll=8)

    def select(k):
        sub = lax.broadcasted_iota(jnp.int32, (LANES, LANES), 0)
        lane = lax.broadcasted_iota(jnp.int32, (LANES, LANES), 1)
        tok = column(tok_ref[pl.ds(owners[k], 1), :].astype(F32)).astype(jnp.int32)
        want = sub * group + lax.bitwise_and(tok, group - 1)
        hot = jnp.concatenate([jnp.where(lane + b * LANES == want, 1.0, 0.0).astype(BF16) for b in range(seq * group // LANES)], axis=1)
        pltpu.make_async_copy(emb_hbm.at[pl.ds(0, seq * group)], tiles.at[k], sem.at[k]).wait()
        picked[k] = dot(hot, tiles[k]).astype(BF16)
        pltpu.make_async_copy(picked.at[k], x0_hbm.at[k], out_sem.at[k]).start()

    def finish(k):
        pltpu.make_async_copy(picked.at[k], x0_hbm.at[k], out_sem.at[k]).wait()

    for work in (fetch, select, finish):
        work(0)
        for k in range(1, slots):
            pl.when(me < slots)(functools.partial(work, k))


def head_chunk(dev, k, n_micro):
    return jnp.minimum(jnp.where(dev < 2, 2 * dev + k, dev + 2), n_micro - 1)


def run_gather(tokens, emb):
    n_micro, seq = tokens.shape
    dim = emb.shape[1]
    group = 16
    return pl.pallas_call(
        gather_kernel,
        out_shape=jax.ShapeDtypeStruct((2, seq, dim), BF16),
        in_specs=[pl.BlockSpec(memory_space=pltpu.SMEM), pl.BlockSpec(memory_space=pltpu.VMEM), pl.BlockSpec(memory_space=pl.ANY)],
        out_specs=pl.BlockSpec(memory_space=pl.ANY),
        scratch_shapes=[pltpu.VMEM((2, seq * group, dim), BF16), pltpu.VMEM((2, seq, dim), BF16), pltpu.SemaphoreType.DMA((2,)), pltpu.SemaphoreType.DMA((2,))],
        cost_estimate=pl.CostEstimate(flops=10**9, bytes_accessed=2 * seq * group * dim * 2, transcendentals=0),
        name="gather",
    )(tokens.reshape(n_micro * seq), tokens, emb)


def token_table(row_ref, cut_ref, meta):
    n_tok = row_ref.shape[1]
    n_grp = n_tok // LANES
    lane = lax.broadcasted_iota(jnp.int32, (LANES, LANES), 1).astype(F32)
    sub = lax.broadcasted_iota(jnp.int32, (LANES, LANES), 0)
    row = lambda g: row_ref[:, g * LANES:(g + 1) * LANES].astype(F32)
    zero = jnp.zeros((LANES, LANES), F32)
    fold = lambda acc: jnp.sum(acc, axis=0, keepdims=True)
    cols = [column(row(c)) for c in range(n_grp)]
    firsts = []
    for g in range(n_grp):
        acc = zero
        for c in range(g + 1):
            same = cols[c] == row(g)
            if c == g:
                same = same & (sub < lane.astype(jnp.int32))
            acc = acc + jnp.where(same, 1.0, 0.0)
        firsts.append(column(jnp.where(fold(acc) == 0.0, 1.0, 0.0)))
    ranks = []
    for g in range(n_grp):
        acc = zero
        for c in range(n_grp):
            acc = acc + jnp.where(cols[c] < row(g), firsts[c], 0.0)
        ranks.append(fold(acc))
        meta[g:g + 1, :] = ranks[g].astype(jnp.int32)
    rank_cols = [column(r) for r in ranks]
    for g in range(n_grp):
        acc = zero
        for c in range(n_grp):
            acc = acc + jnp.where(rank_cols[c] == lane + g * LANES, firsts[c] * cols[c], 0.0)
        meta[n_grp + g:n_grp + g + 1, :] = fold(acc).astype(jnp.int32)
    cut = cut_ref[...].astype(F32)
    acc = zero
    for c in range(n_grp):
        acc = acc + jnp.where(cols[c] < cut, firsts[c], 0.0)
    meta[2 * n_grp:3 * n_grp, :] = jnp.broadcast_to(fold(acc), (n_grp, LANES)).astype(jnp.int32)


def logit_grad(e, n_t, shift, lab, first_id, inv_count, scale, dz):
    rows = e.shape[0]
    n_tok = n_t.shape[1]
    blk = 256
    vid = lax.broadcasted_iota(jnp.int32, (rows, blk), 0)
    for j in range(n_tok // blk):
        cols = slice(j * blk, (j + 1) * blk)
        z = (dot(e, n_t[:, cols]) * scale).astype(BF16).astype(F32)
        prob = jnp.exp2(z * LOG2E - shift[:, cols])
        dz[:, cols] = jnp.where(vid == lab[:, cols] - first_id, prob - inv_count, prob).astype(BF16)


def pipe_kernel(n_stage, plan, x0_hbm, emb_hbm, up_hbm, down_hbm, lab_hbm, row_hbm, cut_hbm,
                n_out, xs_out, hid_out, da_out, g_out, dx0_out, stat_out, loss_out, tmp_out, meta_out,
                xbuf, ybuf, abuf, hbuf, nbuf, gbuf, dxbuf, dx0buf, dnbuf, up, down, up_t, down_t,
                emb, zbuf, n_t, dn_acc, dn_send, dn_recv, dn_own, st_send, st_recv, statall, lossall, tops, n_all_t, shift, dz, obuf, z_pair, meta, lab_ref, row_ref, cut_ref,
                w_sem, e_sem, x_sem, x_send, x_recv, f_send, f_recv, n_send, n_recv, nf_send, ag_send, ag_recv, fw_send,
                st_sems, dp_sems, dn_ssem, dn_rsem, sa_sems, lo_sems, b_send, b_recv, d_send, d_recv, r_sems, out_sem, o_sem, od_send, od_recv, ic_send, in_sem):
    n_micro, seq, dim = gbuf.shape
    part = xbuf.shape[1]
    n_part = xbuf.shape[0]
    per = seq // part
    n_tok = n_micro * seq
    ffn = up.shape[1]
    vocab = emb_hbm.shape[0]
    me = lax.axis_index("stage")
    core = lax.rem(me, 2)
    chip = me // 2
    mate = me + 1 - 2 * core
    last_id = n_stage - 1
    first = me == 0
    last = me == last_id
    fblk = 512
    n_fblk = ffn // fblk
    base, extra, tile = plan.base, plan.extra, plan.head_tile
    row0 = core * (base + extra)
    n_tiles = base // tile
    wide_tile = plan.grad_tile

    barrier = pltpu.get_barrier_semaphore()
    gives_x = (me >= 1) & (me + 2 < n_micro)

    def here(dev):
        pl.semaphore_signal(barrier, inc=1, device_id={"stage": dev}, device_id_type=MESH)

    pl.when(jnp.logical_not(first))(lambda: here(me - 1))
    pl.when(jnp.logical_not(last))(lambda: here(me + 1))

    @pl.when(first)
    def _():
        for dev in range(2, n_micro - 2):
            here(dev)

    w_copy = [pltpu.make_async_copy(up_hbm, up, w_sem.at[0]), pltpu.make_async_copy(down_hbm, down, w_sem.at[1])]
    for c in w_copy:
        c.start()
    in_copy = [pltpu.make_async_copy(src, dst, in_sem.at[k]) for k, (src, dst) in enumerate(((lab_hbm, lab_ref), (row_hbm, row_ref), (cut_hbm, cut_ref)))]
    x_slots = x0_hbm.shape[0]
    x_mine = [head_chunk(me, k, n_micro) for k in range(x_slots)]

    def x_rows(m):
        return xbuf.at[pl.ds(m * per, per)]

    def x_local(k):
        return pltpu.make_async_copy(x0_hbm.at[k], x_rows(k), x_sem.at[k])

    @pl.when(first)
    def _():
        for k in range(x_slots):
            x_local(k).start()

    for c in in_copy:
        c.start()

    e_parts = plan.e_parts
    e_step = base // e_parts

    def e_copy(i):
        src = emb_hbm.at[pl.ds(pl.multiple_of(row0 + i * e_step, 16), e_step)]
        return pltpu.make_async_copy(src, emb.at[pl.ds(i * e_step, e_step)], e_sem.at[0])

    e_more = pltpu.make_async_copy(emb_hbm.at[pl.ds(base, extra)], emb.at[pl.ds(base, extra)], e_sem.at[1])
    with jax.named_scope("entry"):
        pl.semaphore_wait(barrier, jnp.where(first | last, 1, 2) + jnp.where(gives_x & (me >= 2), 1, 0))

    def x_copy(k):
        return remote(x0_hbm.at[k], x_rows(x_mine[k]), x_send.at[k], x_recv.at[x_mine[k]], 0)

    @pl.when(gives_x)
    def _():
        x_copy(0).start()

        @pl.when(me < 2)
        def _():
            x_copy(1).start()

    def table_start():
        for i in range(e_parts):
            e_copy(i).start()
        pl.when(core == 0)(e_more.start)

    def transpose_weights():
        for j in range(n_fblk):
            up_t[j * fblk:(j + 1) * fblk, :] = up[:, j * fblk:(j + 1) * fblk].T
            down_t[:, j * fblk:(j + 1) * fblk] = down[j * fblk:(j + 1) * fblk, :].T

    @pl.when(jnp.logical_not(first))
    def _():
        for c in w_copy:
            c.wait()
        table_start()

    def idle_work():
        transpose_weights()
        in_copy[1].wait()
        in_copy[2].wait()
        token_table(row_ref, jnp.where(core == 0, cut_ref[0:1, :], cut_ref[1:2, :]), meta)

    @pl.when(chip >= n_stage // 4)
    def _():
        idle_work()

    def n_start(m):
        remote(nbuf.at[m], nbuf.at[m], n_send, n_recv.at[m], jnp.where(m == last_id, last_id - 1, m)).start()

    def fwd(h, carry, cold=False):
        m = h // per
        sub = lax.rem(h, per)
        rows = pl.ds(pl.multiple_of(sub * part, part), part)
        with jax.named_scope("fwd_wait"):

            @pl.when(first & (sub == 0))
            def _():
                @pl.when(m < x_slots)
                def _():
                    x_local(m).wait()

                @pl.when(m >= x_slots)
                def _():
                    remote(x_rows(m), x_rows(m), x_send.at[0], x_recv.at[m], me).wait_recv()

            @pl.when(jnp.logical_not(first))
            def _():
                remote(xbuf.at[h], xbuf.at[h], f_send, f_recv.at[h], me).wait_recv()

        with jax.named_scope("fwd_comp"):
            x = xbuf[h]
            if cold:
                w_copy[0].wait()
            for j in range(n_fblk):
                cols = slice(j * fblk, (j + 1) * fblk)
                a = dot(x, up[:, cols]).astype(BF16)
                abuf[m, rows, cols] = a
                hbuf[m, rows, cols] = gelu_fwd(a.astype(F32)).astype(BF16)
            if cold:
                w_copy[1].wait()
                table_start()
            y = (x.astype(F32) + dot(hbuf[m, rows, :], down[...])).astype(BF16)
            ybuf[h] = y

        @pl.when(jnp.logical_not(last))
        def _():
            remote(ybuf.at[h], xbuf.at[h], f_send, f_recv.at[h], me + 1).start()

        @pl.when(last)
        def _():
            yf = y.astype(F32)
            inv = lax.rsqrt(jnp.mean(yf * yf, axis=-1, keepdims=True) + EPS)
            nbuf[m, rows, :] = (yf * inv).astype(BF16)
            pl.when(sub == per - 1)(lambda: n_start(m))

        @pl.when(sub == per - 1)
        def _():
            pltpu.make_async_copy(hbuf.at[m], hid_out.at[m], out_sem.at[0]).start()
            pltpu.make_async_copy(x_rows(m), xs_out.at[pl.ds(m * per, per)], out_sem.at[1]).start()

        return carry

    pl.when(first)(lambda: (fwd(0, 0, cold=True), None)[1])
    lax.fori_loop(jnp.where(first, 1, 0), n_part, fwd, 0)

    @pl.when(chip < n_stage // 4)
    def _():
        idle_work()

    n_forward = remote(nbuf.at[me], nbuf.at[me], nf_send, n_recv.at[me], mate)
    with jax.named_scope("n_wait"):

        @pl.when(jnp.logical_not(last))
        def _():
            remote(nbuf.at[me], nbuf.at[me], n_send, n_recv.at[me], me).wait_recv()
            pl.when(mate != last_id)(n_forward.start)
            remote(nbuf.at[mate], nbuf.at[mate], n_send, n_recv.at[mate], me).wait_recv()

        for k in range(2):
            n_t[:, k * seq:(k + 1) * seq] = nbuf[2 * chip + k].T

    peers = [lax.rem(me + 2 * d, n_stage) for d in range(1, n_stage // 2)]
    ag_copies = [remote(nbuf.at[me], nbuf.at[me], ag_send.at[d], ag_recv.at[me], p) for d, p in enumerate(peers)]
    for c, p in zip(ag_copies, peers):
        pl.when(p != last_id)(c.start)
    with jax.named_scope("e_wait"):
        pltpu.make_async_copy(emb_hbm.at[pl.ds(0, base)], emb.at[pl.ds(0, base)], e_sem.at[0]).wait()
        pl.when(core == 0)(e_more.wait)

    pair = 2 * seq
    scale = dim ** -0.5
    inv_count = 1.0 / n_tok
    log_count = math.log2(n_tok)
    in_copy[0].wait()
    lab = lab_ref[:, pl.ds(pl.multiple_of(chip * pair, pair), pair)]

    def logits(rows, size):
        e = emb[rows, :]
        parts = [dot(e[k * size // 2:(k + 1) * size // 2], n_t[...]) for k in range(2)]
        z = jnp.concatenate([(p * scale).astype(BF16) for p in parts], axis=0)
        zbuf[rows, :] = z
        return z

    def peak(z, size, top):
        best = jnp.max(z.reshape(size // 16, 16, pair), axis=0).astype(F32)
        return jnp.maximum(top, jnp.maximum(best[:8], best[8:]))

    def total(z, size, old, top, tot):
        off = top * LOG2E
        return tot * jnp.exp2(old * LOG2E - off) + jnp.sum(jnp.exp2(z.astype(F32).reshape(size // 8, 8, pair) * LOG2E - off[None]), axis=0)

    tops[0] = jnp.full((8, pair), -jnp.inf, F32)
    tops[1] = jnp.zeros((8, pair), F32)

    @pl.when(core == 0)
    def _():
        z = logits(pl.ds(base, extra), extra)
        top = peak(z, extra, tops[0])
        tops[1] = total(z, extra, tops[0], top, tops[1])
        tops[0] = top

    def logits_step(i, slot, old, top, tot):
        z = logits(pl.ds(pl.multiple_of(i * tile, 16), tile), tile)
        tot = total(z_pair[1 - slot], tile, old, top, tot)
        z_pair[slot] = z
        return top, peak(z, tile, top), tot

    with jax.named_scope("logits"):
        z = logits(pl.ds(0, tile), tile)
        z_pair[0] = z
        state = (tops[0], peak(z, tile, tops[0]), tops[1])
        state = lax.fori_loop(0, (n_tiles - 1) // 2, lambda i, c: logits_step(2 * i + 2, 0, *logits_step(2 * i + 1, 1, *c)), state)
        if n_tiles % 2 == 0:
            state = logits_step(n_tiles - 1, 1, *state)
        old, top, tot = state
        tot = total(z_pair[(n_tiles - 1) % 2], tile, old, top, tot)
    row_top = jnp.max(top, axis=0, keepdims=True)
    row_tot = jnp.sum(tot * jnp.exp2((top - row_top) * LOG2E), axis=0, keepdims=True)
    st_send[0:8, :] = jnp.broadcast_to(row_top, (8, pair))
    st_send[8:16, :] = jnp.broadcast_to(row_tot, (8, pair))
    st_copy = remote(st_send, st_recv, st_sems.at[0], st_sems.at[1], mate)
    with jax.named_scope("stat_x"):
        st_copy.start()
        st_copy.wait()
    far_top = st_recv[0:1, :]
    far_tot = st_recv[8:9, :]
    all_top = jnp.maximum(row_top, far_top)
    mine = row_tot * jnp.exp(row_top - all_top)
    other = far_tot * jnp.exp(far_top - all_top)
    lse = all_top + jnp.log(jnp.where(core == 0, mine + other, other + mine))
    my_shift = lse * LOG2E + log_count
    others = [lax.rem(me + d, n_stage) for d in range(1, n_stage)]

    def spread(buf, sems):
        whole = buf.at[pl.ds(0, n_stage - 1)]
        return [remote(buf.at[me], buf.at[me], sems.at[0], sems.at[1], p) for p in others], remote(whole, whole, sems.at[0], sems.at[1], me)

    statall[me] = jnp.broadcast_to(lse, (8, pair))
    sa_copies, sa_all = spread(statall, sa_sems)
    for c in sa_copies:
        c.start()

    def grads(rows, size, first_row, picked):
        zf = zbuf[rows, :].astype(F32)
        prob = jnp.exp2(zf * LOG2E - my_shift)
        hit = lax.broadcasted_iota(jnp.int32, (size, pair), 0) == lab - (row0 + first_row)
        dz_t = jnp.where(hit, prob - inv_count, prob).astype(BF16)
        got = jnp.where(hit, zf, 0.0).reshape(size // 8, 8, pair)
        return dot_t(dz_t, emb[rows, :]), picked + jnp.sum(got, axis=0)

    tops[0] = jnp.zeros((8, pair), F32)
    dn_acc[...] = jnp.zeros_like(dn_acc)

    @pl.when(core == 0)
    def _():
        dn_acc[...], tops[0] = grads(pl.ds(base, extra), extra, base, tops[0])

    def grad_step(i, picked):
        part, picked = grads(pl.ds(pl.multiple_of(i * wide_tile, 16), wide_tile), wide_tile, i * wide_tile, picked)
        dn_acc[...] += part
        return picked

    with jax.named_scope("grads"):
        picked = lax.fori_loop(0, base // wide_tile, grad_step, tops[0])
    far = pl.ds(pl.multiple_of((1 - core) * seq, seq), seq)
    near = pl.ds(pl.multiple_of(core * seq, seq), seq)
    dn_send[...] = dn_acc[far, :]
    dp_copy = remote(dn_send, dn_recv, dp_sems.at[0], dp_sems.at[1], mate)
    dp_copy.start()
    row_loss = jnp.where(core == 0, lse, 0.0) - jnp.sum(picked, axis=0, keepdims=True)
    lossall[me] = jnp.broadcast_to(row_loss, (8, pair))
    lo_copies, lo_all = spread(lossall, lo_sems)
    for c in lo_copies:
        c.start()
    with jax.named_scope("dn_x"):
        dp_copy.wait()
        dn = ((dn_acc[near, :] + dn_recv[...]) * scale).astype(BF16)
    dn_copy = remote(dn_own, dnbuf.at[me], dn_ssem, dn_rsem.at[me], last_id)

    @pl.when(last)
    def _():
        dnbuf[last_id] = dn

    @pl.when(jnp.logical_not(last))
    def _():
        dn_own[...] = dn
        remote(dn_own, dnbuf.at[me], dn_ssem, dn_rsem.at[me], last_id).start()

    with jax.named_scope("ag_wait"):
        for p in peers:
            got = remote(nbuf.at[p], nbuf.at[p], ag_send.at[0], ag_recv.at[p], me)
            pl.when(jnp.logical_not(last))(got.wait_recv)
            pl.when(mate != last_id)(remote(nbuf.at[p], nbuf.at[p], fw_send, ag_recv.at[p], mate).start)

    near_dst = [1, 3, last_id]
    far_dst = n_stage // 2 + 1
    direct = n_micro - 1
    by_prev = n_micro - 3
    hands_on = (core == 1) & (me != 1)

    def dx0_start(m, k, dev):
        remote(dxbuf.at[m], dx0buf.at[m], d_send.at[k], d_recv.at[m], dev).start()

    def relayed(m):
        return (m < direct) & (((me == 3) & (m != by_prev)) | (last & (m == by_prev)))

    def relay_far(m):
        remote(dx0buf.at[m], dx0buf.at[m], r_sems.at[1], d_recv.at[m], far_dst).start()

    def bwd(m):
        with jax.named_scope("bwd_wait"):
            @pl.when(jnp.logical_not(last))
            def _():
                remote(gbuf.at[m], gbuf.at[m], b_send, b_recv.at[m], me).wait_recv()

            @pl.when(last)
            def _():
                @pl.when(m != last_id)
                def _():
                    remote(dnbuf.at[m], dnbuf.at[m], dn_ssem, dn_rsem.at[m], me).wait_recv()

                yf = ybuf[pl.ds(m * per, per)].reshape(seq, dim).astype(F32)
                inv = lax.rsqrt(jnp.mean(yf * yf, axis=-1, keepdims=True) + EPS)
                dnf = dnbuf[m].astype(F32)
                proj = jnp.mean(yf * dnf, axis=-1, keepdims=True)
                gbuf[m] = (dnf * inv - yf * (inv * inv * inv * proj)).astype(BF16)

        with jax.named_scope("bwd_comp"):
            g = gbuf[m]
            for j in range(n_fblk):
                cols = slice(j * fblk, (j + 1) * fblk)
                dh = dot(g, down_t[:, cols]).astype(BF16).astype(F32)
                abuf[m, :, cols] = (dh * gelu_slope(abuf[m, :, cols].astype(F32))).astype(BF16)
            dxbuf[m] = (g.astype(F32) + dot(abuf[m], up_t[...])).astype(BF16)

        @pl.when(jnp.logical_not(first))
        def _():
            remote(dxbuf.at[m], gbuf.at[m], b_send, b_recv.at[m], me - 1).start()

        @pl.when(first)
        def _():
            pl.when(m >= direct)(lambda: dx0_start(m, len(near_dst), far_dst))
            for k, dev in enumerate(near_dst):
                dx0_start(m, k, dev)

        pltpu.make_async_copy(abuf.at[m], da_out.at[m], out_sem.at[2]).start()
        pltpu.make_async_copy(gbuf.at[m], g_out.at[m], out_sem.at[3]).start()

    n_slot = obuf.shape[0]
    busy = chip == last_id // 2
    far_tile = remote(tmp_out.at[core, pl.ds(0, plan.rows)], tmp_out.at[core, pl.ds(0, plan.rows)], ic_send, od_recv, jnp.where(first, last_id, last_id - 1))
    sends_far = first | (me == last_id - 2)

    def tile_copy(k):
        rows = pl.ds(pl.multiple_of(k * plan.rows, plan.rows), plan.rows)
        slot = lax.rem(k, n_slot)
        return pltpu.make_async_copy(obuf.at[slot], tmp_out.at[core, rows], o_sem.at[slot])

    def piece(p):
        k = p // plan.per_tile
        rows = pl.ds(pl.multiple_of(p * plan.piece, plan.piece), plan.piece)
        here = pl.ds(pl.multiple_of(lax.rem(p, plan.per_tile) * plan.piece, plan.piece), plan.piece)
        return remote(obuf.at[lax.rem(k, n_slot), here], tmp_out.at[core, rows], od_send.at[k], od_recv, mate)

    def tile_sent(k):
        slot = lax.rem(k, n_slot)
        return remote(obuf.at[slot], tmp_out.at[core, pl.ds(0, plan.rows)], od_send.at[k], od_recv, mate)

    def emb_tile(k):
        with jax.named_scope("tile_prep"):

            @pl.when(k == 0)
            def _():
                for d in range(1, n_stage // 2):
                    src = lax.rem(mate + 2 * d, n_stage)
                    pl.when(jnp.logical_not(last))(remote(nbuf.at[src], nbuf.at[src], ag_send.at[0], ag_recv.at[src], me).wait_recv)
                for m in range(n_micro):
                    n_all_t[:, m * seq:(m + 1) * seq] = nbuf[m].T
                sa_all.wait_recv()
                for c in range(n_stage // 2):
                    shift[:, c * pair:(c + 1) * pair] = statall[2 * c, 0:1, :] * LOG2E + log_count

        slot = lax.rem(k, n_slot)
        with jax.named_scope("tile_wait"):
            @pl.when(k == 2)
            def _():
                tile_copy(0).wait()
                pl.when(sends_far)(far_tile.start)

            pl.when(k > n_slot)(lambda: tile_copy(k - n_slot).wait())
            pl.when((k >= n_slot) & (k - n_slot < plan.shared) & jnp.logical_not(busy & (k == n_slot)))(lambda: tile_sent(k - n_slot).wait_send())

        with jax.named_scope("tile"):
            rows = pl.ds(pl.multiple_of(k * plan.rows, plan.rows), plan.rows)
            logit_grad(emb[rows, :], n_all_t, shift, lab_ref, row0 + k * plan.rows, inv_count, scale, dz)
            obuf[slot] = dot(dz[...], nbuf[...].reshape(n_tok, dim)) * scale

        tile_copy(k).start()

    def send_pieces(done, until):
        lax.fori_loop(done, until, lambda p, c: (piece(p).start(), c)[1], 0)

    def send_tiles(done, until):
        def one(k, carry):
            rows = pl.ds(pl.multiple_of(k * plan.rows, plan.rows), plan.rows)
            remote(obuf.at[lax.rem(k, n_slot)], tmp_out.at[core, rows], od_send.at[k], od_recv, mate).start()
            return carry

        lax.fori_loop(done, until, one, 0)

    before = sum(jnp.where(me == s, plan.before[s], 0) for s in range(n_stage))

    def pass_dx0(m, carry):
        @pl.when(jnp.logical_not(first))
        def _():
            remote(dx0buf.at[m], dx0buf.at[m], r_sems.at[0], d_recv.at[m], me).wait_recv()

            @pl.when(hands_on)
            def _():
                remote(dx0buf.at[m], dx0buf.at[m], r_sems.at[0], d_recv.at[m], mate).start()

            @pl.when(relayed(m))
            def _():
                relay_far(m)

            pltpu.make_async_copy(dx0buf.at[m], dx0_out.at[m], out_sem.at[4]).start()

        @pl.when(first)
        def _():
            pltpu.make_async_copy(dxbuf.at[m], dx0_out.at[m], out_sem.at[4]).start()

        return carry

    lead = jnp.where(me == 3, -300, jnp.where(last, -1800, jnp.where(me == far_dst, -1600, -10**6)))

    def work(i, carry):
        sent, passed = carry
        chunk = (i >= before) & (i < before + n_micro)
        pl.when(chunk)(lambda: bwd(i - before))
        k = jnp.where(i < before, i, i - n_micro)
        pl.when(jnp.logical_not(chunk))(lambda: emb_tile(k))
        after = i - before - n_micro + 1
        here = jnp.where(after > 0, jnp.clip((after * 264 + lead) // 138, 0, n_micro), 0)
        lax.fori_loop(passed, here, pass_dx0, 0)
        ready = jnp.where(i < before, i + 1, jnp.where(chunk, before, i + 1 - n_micro))
        near_chunks = chunk | ((i < before) & (i + 1 >= before))
        whole = (sent + plan.per_tile - 1) // plan.per_tile
        upto = jnp.minimum(jnp.minimum(ready, plan.shared), whole + 1)
        some = jnp.where(near_chunks, jnp.minimum(sent + 1, jnp.minimum(ready, plan.shared) * plan.per_tile), whole * plan.per_tile)
        send_pieces(sent, some)
        send_tiles(whole, jnp.where(near_chunks, 0, upto))
        now = jnp.where(near_chunks, some, jnp.maximum(some, upto * plan.per_tile))
        return jnp.maximum(sent, now), jnp.maximum(passed, here)

    sent, passed = lax.fori_loop(0, plan.tiles + n_micro, work, (jnp.where(busy, plan.per_tile, 0), 0))
    outs = [pltpu.make_async_copy(nbuf, n_out, out_sem.at[5]), pltpu.make_async_copy(lossall, loss_out, out_sem.at[6]), pltpu.make_async_copy(meta, meta_out, out_sem.at[7])]
    lo_all.wait_recv()
    for c in outs:
        c.start()
    pltpu.make_async_copy(statall, stat_out, out_sem.at[8]).start()
    with jax.named_scope("relay_all"):
        lax.fori_loop(passed, n_micro, pass_dx0, 0)

    with jax.named_scope("drain"):
        send_pieces(sent, plan.shared * plan.per_tile)
        for k in range(max(plan.tiles - n_slot, 0), plan.tiles):
            tile_copy(k).wait()
            if k < plan.shared:
                tile_sent(k).wait_send()
        pl.when(sends_far)(far_tile.wait_send)
        all_rows = pl.ds(0, plan.shared * plan.rows)
        remote(tmp_out.at[1 - core, all_rows], tmp_out.at[1 - core, all_rows], od_send.at[0], od_recv, me).wait_recv()
        sa_all.wait_send()
        lo_all.wait_send()
        pltpu.make_async_copy(statall, stat_out, out_sem.at[8]).wait()
        for c, p in zip(ag_copies, peers):
            pl.when(p != last_id)(c.wait_send)

        @pl.when(jnp.logical_not(last))
        def _():
            dn_copy.wait_send()
            pl.when(mate != last_id)(n_forward.wait_send)
            remote(ybuf, xbuf, f_send, f_recv.at[0], me + 1).wait_send()

        @pl.when(last)
        def _():
            remote(nbuf, nbuf, n_send, n_recv.at[0], me).wait_send()

        @pl.when(mate != last_id)
        def _():
            some = nbuf.at[pl.ds(0, len(peers))]
            remote(some, some, fw_send, ag_recv.at[0], mate).wait_send()

        @pl.when(gives_x)
        def _():
            x_copy(0).wait_send()

            @pl.when(me < 2)
            def _():
                x_copy(1).wait_send()

        @pl.when(jnp.logical_not(first))
        def _():
            remote(dxbuf, gbuf, b_send, b_recv.at[0], me).wait_send()
            pl.when(hands_on)(remote(dx0buf, dx0buf, r_sems.at[0], d_recv.at[0], mate).wait_send)

        @pl.when(first)
        def _():
            for k in range(len(near_dst)):
                remote(dxbuf, dx0buf, d_send.at[k], d_recv.at[0], me).wait_send()
            rest = pl.ds(0, n_micro - direct)
            remote(dxbuf.at[rest], dx0buf.at[rest], d_send.at[len(near_dst)], d_recv.at[0], me).wait_send()

        for dev, kept in ((3, direct - 1), (last_id, 1)):
            some = dx0buf.at[pl.ds(0, kept)]
            pl.when(me == dev)(remote(some, some, r_sems.at[1], d_recv.at[0], me).wait_send)

        pltpu.make_async_copy(hbuf, hid_out, out_sem.at[0]).wait()
        pltpu.make_async_copy(xbuf, xs_out, out_sem.at[1]).wait()
        pltpu.make_async_copy(abuf, da_out, out_sem.at[2]).wait()
        pltpu.make_async_copy(gbuf, g_out, out_sem.at[3]).wait()
        pltpu.make_async_copy(dx0buf, dx0_out, out_sem.at[4]).wait()
        for c in outs:
            c.wait()


class Plan:
    def __init__(self, vocab, n_stage):
        units = vocab // LANES
        self.base = units // 2 * LANES
        self.extra = vocab - 2 * self.base
        self.head_tile = next(t for t in (1600, 1536, 1280, 1024, 768, 640, 512, 256, 128) if self.base % t == 0)
        self.rows = 1024
        self.tiles, self.shared = 11, 9
        self.grad_tile = next(t for t in (4000, 3200, 1600, 1280, 640, 256, 128) if self.base % t == 0)
        self.e_parts = next(k for k in (10, 8, 5, 4, 2, 1) if self.base % (16 * k) == 0)
        self.part = 128
        self.slots = 4
        self.piece = 256
        self.per_tile = self.rows // self.piece
        measured = [10, 9, 6, 5, 3, 2, 0, 0]
        self.before = (measured + [0] * n_stage)[:n_stage]
        mid = self.base + self.extra
        ends = [(0, mid), (mid, vocab)]
        early = (self.tiles * self.rows, self.shared * self.rows)
        self.spans = [[(ends[h][0] + early[0 if h == c else 1], ends[h][1]) for h in (c, 1 - c)] for c in range(2)]
        self.longest = [max(self.spans[c][k][1] - self.spans[c][k][0] for c in range(2)) for k in range(2)]
        best = min(range(16, 1281, 16), key=lambda r: (sum(-(-n // r) for n in self.longest)) * (r + 40))
        self.calc_rows = best
        self.calc_steps = [-(-n // best) for n in self.longest]
        self.steps = sum(self.calc_steps)
        self.copy_rows = self.rows
        self.copies = self.tiles + self.shared
        self.starts = ends

    def calc_start(self, core, s):
        k = 0 if s < self.calc_steps[0] else 1
        lo, hi = self.spans[core][k]
        return min(lo + (s - k * self.calc_steps[0]) * self.calc_rows, hi - self.calc_rows)

    def copy_start(self, core, c):
        own = c < self.tiles
        h = core if own else 1 - core
        return self.starts[h][0] + (c if own else c - self.tiles) * self.copy_rows

    def cuts(self, core):
        firsts = [(self.calc_start(core, s), self.calc_rows) for s in range(self.steps)] + [(self.copy_start(core, c), self.copy_rows) for c in range(self.copies)]
        flat = [v for lo, rows in firsts for v in (lo, lo + rows)]
        return flat + [0] * (LANES - len(flat))


def run_pipe(x0, emb, w_up, w_down, labels, tokens, cuts, n_stage, plan):
    n_micro, seq = labels.shape
    dim, ffn = w_up.shape
    n_tok = n_micro * seq
    base = plan.base
    any_spec = pl.BlockSpec(memory_space=pl.ANY)
    act = (n_micro, seq, dim)
    fine = (n_tok // plan.part, plan.part, dim)
    wide = (n_micro, seq, ffn)
    dma = pltpu.SemaphoreType.DMA
    vm = pltpu.VMEM
    pair = 2 * seq
    return pl.pallas_call(
        functools.partial(pipe_kernel, n_stage, plan),
        out_shape=[
            jax.ShapeDtypeStruct(act, BF16), jax.ShapeDtypeStruct(fine, BF16), jax.ShapeDtypeStruct(wide, BF16),
            jax.ShapeDtypeStruct(wide, BF16), jax.ShapeDtypeStruct(act, BF16), jax.ShapeDtypeStruct(act, BF16),
            jax.ShapeDtypeStruct((n_stage, 8, pair), F32), jax.ShapeDtypeStruct((n_stage, 8, pair), F32), jax.ShapeDtypeStruct((2, plan.tiles * plan.rows, dim), F32),
            jax.ShapeDtypeStruct((3 * n_tok // LANES, LANES), jnp.int32),
        ],
        in_specs=[any_spec] * 7,
        out_specs=[any_spec] * 10,
        scratch_shapes=[
            vm(fine, BF16), vm(fine, BF16), vm(wide, BF16), vm(wide, BF16), vm(act, BF16), vm(act, BF16), vm(act, BF16), vm(act, BF16), vm(act, BF16),
            vm((dim, ffn), BF16), vm((ffn, dim), BF16), vm((ffn, dim), BF16), vm((dim, ffn), BF16),
            vm((base + plan.extra, dim), BF16), vm((base + plan.extra, pair), BF16), vm((dim, pair), BF16), vm((pair, dim), F32),
            vm((seq, dim), F32), vm((seq, dim), F32), vm((seq, dim), BF16), vm((16, pair), F32), vm((16, pair), F32), vm((n_stage, 8, pair), F32), vm((n_stage, 8, pair), F32),
            vm((2, 8, pair), F32), vm((dim, n_tok), BF16), vm((1, n_tok), F32), vm((plan.rows, n_tok), BF16), vm((plan.slots, plan.rows, dim), F32),
            vm((2, plan.head_tile, pair), BF16), vm((3 * n_tok // LANES, LANES), jnp.int32),
            vm((1, n_tok), jnp.int32), vm((1, n_tok), jnp.int32), vm((2, LANES), jnp.int32),
            dma((2,)), dma((2,)), dma((2,)), dma((2,)), dma((n_micro,)), dma, dma((n_tok // plan.part,)), dma, dma((n_micro,)), dma,
            dma((n_stage // 2,)), dma((n_micro,)), dma,
            dma((2,)), dma((2,)), dma, dma((n_stage,)), dma((2,)), dma((2,)), dma, dma((n_micro,)), dma((4,)), dma((n_micro,)), dma((2,)), dma((9,)),
            dma((plan.slots,)), dma((plan.shared,)), dma, dma, dma((3,)),
        ],
        compiler_params=pltpu.CompilerParams(collective_id=0, has_side_effects=True, vmem_limit_bytes=67_000_000),
        cost_estimate=pl.CostEstimate(flops=60 * 10**9, bytes_accessed=100 * 10**6, transcendentals=0),
        name="pipe",
    )(x0.reshape(x0.shape[0], seq // plan.part, plan.part, dim), emb, w_up, w_down, labels.reshape(1, n_tok), tokens.reshape(1, n_tok), cuts)


def fin_kernel(n_stage, n_tok, plan, ids_hbm, emb_hbm, tmp_hbm, n_hbm, stat_hbm, part_hbm, lab_hbm, meta_hbm, dx0_hbm, xs_hbm, hid_hbm, da_hbm, g_hbm,
               out_hbm, loss_ref, gup_hbm, gdown_hbm,
               n_all, dx0, xs, hid, da, g, n_t, x_t, dx0s, dz, shift, e_in, c_out, cp, gup, gdown,
               ld_sem, e_sem, t_sem, co_sem, po_sem, gu_sem, gd_sem, wi_sem, ids_ref, stat_ref, part_ref, lab_ref, meta_ref, in_sem):
    dim, ffn = gup_hbm.shape
    scale = dim ** -0.5
    inv_count = 1.0 / n_tok
    steps, crows, prows = plan.steps, plan.calc_rows, plan.copy_rows
    core = lax.rem(lax.axis_index("stage"), 2)
    early = plan.tiles * prows
    wblk = gup.shape[2]
    n_wblk = ffn // wblk
    turn = plan.calc_steps[0]

    def pick(pair):
        return jnp.where(core == 0, pair[0], pair[1])

    def calc_start(s):
        own = s < turn
        lo, hi = [jnp.where(own, pick([plan.spans[c][0][e] for c in range(2)]), pick([plan.spans[c][1][e] for c in range(2)])) for e in range(2)]
        return pl.multiple_of(jnp.minimum(lo + (s - jnp.where(own, 0, turn)) * crows, hi - crows), 16)

    def copy_start(c):
        own = c < plan.tiles
        first = jnp.where(own, pick([plan.starts[0][0], plan.starts[1][0]]), pick([plan.starts[1][0], plan.starts[0][0]]))
        return pl.multiple_of(first + (c - jnp.where(own, 0, plan.tiles)) * prows, 16)

    def e_copy(s):
        return pltpu.make_async_copy(emb_hbm.at[pl.ds(calc_start(s), crows)], e_in.at[lax.rem(s, 3)], e_sem.at[lax.rem(s, 3)])

    n_slot = cp.shape[0]
    ahead = 8

    def t_copy(c):
        own = c < plan.tiles
        row = jnp.where(own, core, 1 - core) * early + (c - jnp.where(own, 0, plan.tiles)) * prows
        slot = lax.rem(c, n_slot)
        return pltpu.make_async_copy(tmp_hbm.at[pl.ds(pl.multiple_of(row, 16), prows)], cp.at[slot], t_sem.at[slot])

    def p_out(c):
        slot = lax.rem(c, n_slot)
        return pltpu.make_async_copy(cp.at[slot], out_hbm.at[pl.ds(copy_start(c), prows)], po_sem.at[slot])

    def c_outs(s):
        slot = lax.rem(s, 2)
        return pltpu.make_async_copy(c_out.at[slot], out_hbm.at[pl.ds(calc_start(s), crows)], co_sem.at[slot])

    loads = [pltpu.make_async_copy(s, d, ld_sem.at[i]) for i, (s, d) in enumerate(((n_hbm, n_all), (dx0_hbm, dx0), (xs_hbm, xs), (g_hbm, g)))]
    ins = [pltpu.make_async_copy(s, d, in_sem.at[i]) for i, (s, d) in enumerate(((stat_hbm, stat_ref), (lab_hbm, lab_ref), (part_hbm, part_ref), (meta_hbm, meta_ref), (ids_hbm, ids_ref)))]
    loads[0].start()
    ins[0].start()
    ins[1].start()
    e_copy(0).start()
    loads[1].start()
    for c in ins[2:]:
        c.start()
    e_copy(1).start()
    for c in range(ahead):
        t_copy(c).start(priority=1)
    pair = stat_ref.shape[2]
    with jax.named_scope("fin_pre"):
        ins[0].wait()
        ins[1].wait()
        for c in range(n_stage // 2):
            shift[:, c * pair:(c + 1) * pair] = stat_ref[2 * c, 0:1, :] * LOG2E + math.log2(n_tok)
        loads[0].wait()
        n_t[...] = n_all[...].T

    def sum_rows():
        for c in ins[2:]:
            c.wait()
        loss_ref[0] = jnp.sum(sum(part_ref[d, 0:1, :] for d in range(n_stage))) * inv_count
        loads[1].wait()
        dense = jnp.concatenate([meta_ref[g:g + 1, :] for g in range(n_tok // LANES)], axis=1)
        order = lax.broadcasted_iota(jnp.int32, (n_tok, n_tok), 0) == dense
        dx0s[...] = dot(jnp.where(order, 1.0, 0.0).astype(BF16), dx0[...])

    def add_rows(k, start, ref):
        lo, hi = ids_ref[2 * n_tok + k], ids_ref[2 * n_tok + k + 1]
        wide = 8

        def some(p, width):
            at = [pl.ds(ids_ref[n_tok + p + u] - start, 1) for u in range(width)]
            new = [ref[at[u], :] + dx0s[pl.ds(p + u, 1), :] for u in range(width)]
            for u in range(width):
                ref[at[u], :] = new[u]

        def group(g, carry):
            some(lo + g * wide, wide)
            return carry

        def single(p, carry):
            some(p, 1)
            return carry

        n_grp = (hi - lo) // wide
        lax.fori_loop(0, n_grp, group, 0)
        lax.fori_loop(lo + n_grp * wide, hi, single, 0)

    def w_ins(w):
        cols = pl.ds(pl.multiple_of(w * wblk, wblk), wblk)
        wslot = lax.rem(w, 2)
        return (pltpu.make_async_copy(da_hbm.at[:, cols], da.at[wslot], wi_sem.at[0, wslot]), pltpu.make_async_copy(hid_hbm.at[:, cols], hid.at[wslot], wi_sem.at[1, wslot]))

    def w_outs(w):
        cols = pl.ds(pl.multiple_of(w * wblk, wblk), wblk)
        wslot = lax.rem(w, 2)
        return (pltpu.make_async_copy(gup.at[wslot], gup_hbm.at[:, cols], gu_sem.at[wslot]), pltpu.make_async_copy(gdown.at[wslot], gdown_hbm.at[cols], gd_sem.at[wslot]))

    def copy_tile(c, carry):
        with jax.named_scope("copy_wait"):
            t_copy(c).wait()
        with jax.named_scope("add_p"):
            add_rows(2 * steps + 2 * c, copy_start(c), cp.at[lax.rem(c, n_slot)])
        p_out(c).start()

        @pl.when(c + ahead < plan.copies)
        def _():
            pl.when(c + ahead >= n_slot)(lambda: p_out(c + ahead - n_slot).wait())
            t_copy(c + ahead).start(priority=1)

        return carry

    w_first = 2
    tails = [turn - 1, steps - 1]

    def tail(s):
        return (s == tails[0]) | (s == tails[1])

    def step(s, carry):
        pl.when(s + 2 < steps)(lambda: e_copy(s + 2).start())
        with jax.named_scope("fin_wait"):
            e_copy(s).wait()

        @pl.when(s == 0)
        def _():
            for c in loads[2:]:
                c.start()

        w = s - w_first

        @pl.when((w + 1 >= 0) & (w + 1 < n_wblk))
        def _():
            for c in w_ins(w + 1):
                c.start()

        pl.when((s >= 2) & jnp.logical_not(tail(s - 1)))(lambda: c_outs(s - 2).wait())
        slot = lax.rem(s, 2)
        start = calc_start(s)
        with jax.named_scope("calc"):
            logit_grad(e_in[lax.rem(s, 3)], n_t, shift, lab_ref, start, inv_count, scale, dz)
            c_out[slot] = dot(dz[...], n_all[...]) * scale
        pl.when(s == 0)(sum_rows)
        with jax.named_scope("add_c"):
            add_rows(2 * s, start, c_out.at[slot])
        pl.when(tail(s))(lambda: c_outs(s - 1).wait())
        c_outs(s).start()
        lax.fori_loop(s * plan.copies // (steps - 1), jnp.minimum((s + 1) * plan.copies // (steps - 1), plan.copies), copy_tile, 0)

        @pl.when(w == 0)
        def _():
            for c in loads[2:]:
                c.wait()
            x_t[...] = xs[...].T

        @pl.when((w >= 0) & (w < n_wblk))
        def _():
            wslot = lax.rem(w, 2)
            with jax.named_scope("dw_wait"):
                for c in w_ins(w):
                    c.wait()

                @pl.when(w >= 2)
                def _():
                    for c in w_outs(w - 2):
                        c.wait()

            with jax.named_scope("dw"):
                gup[wslot] = dot(x_t[...], da[wslot])
                gdown[wslot] = dot_t(hid[wslot], g[...])
            for c in w_outs(w):
                c.start()

        return carry

    lax.fori_loop(0, steps, step, 0)
    with jax.named_scope("fin_drain"):
        for w in range(n_wblk - 2, n_wblk):
            for c in w_outs(w):
                c.wait()
        c_outs(steps - 1).wait()
        for c in range(plan.copies - n_slot, plan.copies):
            p_out(c).wait()


def run_fin(emb, tmp, n_all, stats, losses, labels, meta, dx0, xs, hid, da, g, n_stage, plan):
    vocab, dim = emb.shape
    n_tok, ffn = hid.shape
    vm = pltpu.VMEM
    dma = pltpu.SemaphoreType.DMA
    any_spec = pl.BlockSpec(memory_space=pl.ANY)
    smem = pl.BlockSpec(memory_space=pltpu.SMEM)
    wblk = 512
    return pl.pallas_call(
        functools.partial(fin_kernel, n_stage, n_tok, plan),
        out_shape=[jax.ShapeDtypeStruct((vocab, dim), F32), jax.ShapeDtypeStruct((1,), F32), jax.ShapeDtypeStruct((dim, ffn), F32), jax.ShapeDtypeStruct((ffn, dim), F32)],
        in_specs=[any_spec] * 13,
        out_specs=[any_spec, smem, any_spec, any_spec],
        scratch_shapes=[
            vm((n_tok, dim), BF16), vm((n_tok, dim), BF16), vm((n_tok, dim), BF16), vm((2, n_tok, wblk), BF16), vm((2, n_tok, wblk), BF16), vm((n_tok, dim), BF16),
            vm((dim, n_tok), BF16), vm((dim, n_tok), BF16), vm((n_tok, dim), F32), vm((plan.calc_rows, n_tok), BF16), vm((1, n_tok), F32),
            vm((3, plan.calc_rows, dim), BF16), vm((2, plan.calc_rows, dim), F32), vm((11, plan.copy_rows, dim), F32),
            vm((2, dim, wblk), F32), vm((2, wblk, dim), F32),
            dma((4,)), dma((3,)), dma((11,)), dma((2,)), dma((11,)), dma((2,)), dma((2,)), dma((2, 2)),
            pltpu.SMEM((meta.size,), jnp.int32), vm(stats.shape, F32), vm(losses.shape, F32), vm((1, n_tok), jnp.int32), vm(meta.shape, jnp.int32), dma((5,)),
        ],
        compiler_params=pltpu.CompilerParams(vmem_limit_bytes=67_000_000),
        cost_estimate=pl.CostEstimate(flops=2 * n_tok * vocab * dim, bytes_accessed=5 * vocab * dim, transcendentals=0),
        name="fin",
    )(meta.reshape(-1), emb, tmp, n_all, stats, losses, labels.reshape(1, n_tok), meta, dx0, xs, hid, da, g)


def solution(mesh):
    n_stage = mesh.shape["stage"]

    def device_fn(tokens, labels, emb, w_up, w_down):
        n_micro, seq = tokens.shape
        vocab, dim = emb.shape
        w_up, w_down = w_up[0], w_down[0]
        n_tok = n_micro * seq
        plan = Plan(vocab, n_stage)
        cuts = jnp.array([plan.cuts(0), plan.cuts(1)], jnp.int32)
        x0 = run_gather(tokens, emb)
        n_all, xs, hid, da, g, dx0, stats, losses, tmp, meta = run_pipe(x0, emb, w_up, w_down, labels, tokens, cuts, n_stage, plan)
        flat = lambda p: p.reshape(n_tok, -1)
        grad_emb, loss, grad_up, grad_down = run_fin(
            emb, tmp.reshape(-1, dim), flat(n_all), stats, losses, labels, meta, flat(dx0), flat(xs), flat(hid), flat(da), flat(g), n_stage, plan
        )
        return loss, grad_up[None], grad_down[None], grad_emb

    return jax.shard_map(device_fn, mesh=mesh, in_specs=(P("dp", None), P("dp", None), P(None, None), P("stage", None, None), P("stage", None, None)), out_specs=(P("dp"), P(("dp", "stage"), None, None), P(("dp", "stage"), None, None), P("dp", None)), check_vma=False)
```

```python
import functools
import math

import jax
import jax.numpy as jnp
from jax import lax
from jax.experimental import pallas as pl
from jax.experimental.pallas import tpu as pltpu
from jax.sharding import PartitionSpec as P


MESH = pl.DeviceIdType.MESH
LOG2E = math.log2(math.e)
LN2 = math.log(2.0)
GELU_C = math.sqrt(2.0 / math.pi)
GELU_K = 0.044715
EPS = 1e-6
LANES = 128
F32 = jnp.float32
BF16 = jnp.bfloat16


def gelu_fwd(a):
    return (0.5 * a) * (1.0 + jnp.tanh(a * (GELU_C + (GELU_C * GELU_K) * (a * a))))


def gelu_slope(a):
    a2 = a * a
    half = 0.5 * jnp.tanh(a * (GELU_C + (GELU_C * GELU_K) * a2))
    up, down = 0.5 + half, 0.5 - half
    return up + (up * down) * (a * (2.0 * GELU_C + (6.0 * GELU_C * GELU_K) * a2))


def dot(x, y):
    return jnp.dot(x, y, preferred_element_type=F32)


def dot_t(x, y):
    return lax.dot_general(x, y, (((0,), (0,)), ((), ())), preferred_element_type=F32)


def remote(src, dst, send_sem, recv_sem, dev):
    return pltpu.make_async_remote_copy(src_ref=src, dst_ref=dst, send_sem=send_sem, recv_sem=recv_sem, device_id={"stage": dev}, device_id_type=MESH)


def column(row):
    return jnp.broadcast_to(row, (LANES, LANES)).T


def gather_kernel(ids_ref, tok_ref, emb_hbm, x0_hbm, tiles, picked, sem, out_sem):
    n_micro, seq = tok_ref.shape
    me = lax.axis_index("stage")
    group = tiles.shape[1] // seq
    slots = tiles.shape[0]
    owners = [head_chunk(me, k, n_micro) for k in range(slots)]

    def fetch(k):
        def one(i, carry):
            t = ids_ref[owners[k] * seq + i]
            start = pl.multiple_of(lax.bitwise_and(t, -group), group)
            pltpu.make_async_copy(emb_hbm.at[pl.ds(start, group)], tiles.at[k, pl.ds(pl.multiple_of(i * group, group), group)], sem.at[k]).start()
            return carry

        lax.fori_loop(0, seq, one, 0, unroll=8)

    def select(k):
        sub = lax.broadcasted_iota(jnp.int32, (LANES, LANES), 0)
        lane = lax.broadcasted_iota(jnp.int32, (LANES, LANES), 1)
        tok = column(tok_ref[pl.ds(owners[k], 1), :].astype(F32)).astype(jnp.int32)
        want = sub * group + lax.bitwise_and(tok, group - 1)
        hot = jnp.concatenate([jnp.where(lane + b * LANES == want, 1.0, 0.0).astype(BF16) for b in range(seq * group // LANES)], axis=1)
        pltpu.make_async_copy(emb_hbm.at[pl.ds(0, seq * group)], tiles.at[k], sem.at[k]).wait()
        picked[k] = dot(hot, tiles[k]).astype(BF16)
        pltpu.make_async_copy(picked.at[k], x0_hbm.at[k], out_sem.at[k]).start()

    def finish(k):
        pltpu.make_async_copy(picked.at[k], x0_hbm.at[k], out_sem.at[k]).wait()

    for work in (fetch, select, finish):
        work(0)
        for k in range(1, slots):
            pl.when(me < slots)(functools.partial(work, k))


def head_chunk(dev, k, n_micro):
    return jnp.minimum(jnp.where(dev < 2, 2 * dev + k, dev + 2), n_micro - 1)


def run_gather(tokens, emb):
    n_micro, seq = tokens.shape
    dim = emb.shape[1]
    group = 16
    return pl.pallas_call(
        gather_kernel,
        out_shape=jax.ShapeDtypeStruct((2, seq, dim), BF16),
        in_specs=[pl.BlockSpec(memory_space=pltpu.SMEM), pl.BlockSpec(memory_space=pltpu.VMEM), pl.BlockSpec(memory_space=pl.ANY)],
        out_specs=pl.BlockSpec(memory_space=pl.ANY),
        scratch_shapes=[pltpu.VMEM((2, seq * group, dim), BF16), pltpu.VMEM((2, seq, dim), BF16), pltpu.SemaphoreType.DMA((2,)), pltpu.SemaphoreType.DMA((2,))],
        cost_estimate=pl.CostEstimate(flops=10**9, bytes_accessed=2 * seq * group * dim * 2, transcendentals=0),
        name="gather",
    )(tokens.reshape(n_micro * seq), tokens, emb)


def token_table(row_ref, cut_ref, meta):
    n_tok = row_ref.shape[1]
    n_grp = n_tok // LANES
    lane = lax.broadcasted_iota(jnp.int32, (LANES, LANES), 1).astype(F32)
    sub = lax.broadcasted_iota(jnp.int32, (LANES, LANES), 0)
    row = lambda g: row_ref[:, g * LANES:(g + 1) * LANES].astype(F32)
    zero = jnp.zeros((LANES, LANES), F32)
    fold = lambda acc: jnp.sum(acc, axis=0, keepdims=True)
    cols = [column(row(c)) for c in range(n_grp)]
    firsts = []
    for g in range(n_grp):
        acc = zero
        for c in range(g + 1):
            same = cols[c] == row(g)
            if c == g:
                same = same & (sub < lane.astype(jnp.int32))
            acc = acc + jnp.where(same, 1.0, 0.0)
        firsts.append(column(jnp.where(fold(acc) == 0.0, 1.0, 0.0)))
    ranks = []
    for g in range(n_grp):
        acc = zero
        for c in range(n_grp):
            acc = acc + jnp.where(cols[c] < row(g), firsts[c], 0.0)
        ranks.append(fold(acc))
        meta[g:g + 1, :] = ranks[g].astype(jnp.int32)
    rank_cols = [column(r) for r in ranks]
    for g in range(n_grp):
        acc = zero
        for c in range(n_grp):
            acc = acc + jnp.where(rank_cols[c] == lane + g * LANES, firsts[c] * cols[c], 0.0)
        meta[n_grp + g:n_grp + g + 1, :] = fold(acc).astype(jnp.int32)
    cut = cut_ref[...].astype(F32)
    acc = zero
    for c in range(n_grp):
        acc = acc + jnp.where(cols[c] < cut, firsts[c], 0.0)
    meta[2 * n_grp:3 * n_grp, :] = jnp.broadcast_to(fold(acc), (n_grp, LANES)).astype(jnp.int32)


def logit_grad(e, n_t, shift, lab, first_id, inv_count, scale, dz):
    rows = e.shape[0]
    n_tok = n_t.shape[1]
    blk = 256
    vid = lax.broadcasted_iota(jnp.int32, (rows, blk), 0)
    for j in range(n_tok // blk):
        cols = slice(j * blk, (j + 1) * blk)
        z = (dot(e, n_t[:, cols]) * scale).astype(BF16).astype(F32)
        prob = jnp.exp2(z * LOG2E - shift[:, cols])
        dz[:, cols] = jnp.where(vid == lab[:, cols] - first_id, prob - inv_count, prob).astype(BF16)


def pipe_kernel(n_stage, plan, x0_hbm, emb_hbm, up_hbm, down_hbm, lab_hbm, row_hbm, cut_hbm,
                n_out, xs_out, hid_out, da_out, g_out, dx0_out, stat_out, loss_out, tmp_out, meta_out,
                xbuf, ybuf, abuf, hbuf, nbuf, gbuf, dxbuf, dx0buf, dnbuf, up, down, up_t, down_t,
                emb, zbuf, n_t, dn_acc, dn_send, dn_recv, dn_own, st_send, st_recv, statall, lossall, tops, n_all_t, shift, dz, obuf, z_pair, meta, lab_ref, row_ref, cut_ref,
                w_sem, e_sem, x_sem, x_send, f_send, f_recv, n_send, n_recv, nf_send, ag_send, fw_send,
                st_sems, dp_sems, dn_ssem, dn_rsem, sa_sems, lo_sems, b_send, b_recv, d_send, d_recv, r_sems, out_sem, o_sem, od_send, od_recv, ic_send, in_sem):
    n_micro, seq, dim = gbuf.shape
    part = xbuf.shape[1]
    n_part = xbuf.shape[0]
    per = seq // part
    n_tok = n_micro * seq
    ffn = up.shape[1]
    vocab = emb_hbm.shape[0]
    me = lax.axis_index("stage")
    core = lax.rem(me, 2)
    chip = me // 2
    mate = me + 1 - 2 * core
    last_id = n_stage - 1
    first = me == 0
    last = me == last_id
    fblk = 512
    n_fblk = ffn // fblk
    base, extra, tile = plan.base, plan.extra, plan.head_tile
    row0 = core * base
    n_tiles = base // tile
    wide_tile = plan.grad_tile

    barrier = pltpu.get_barrier_semaphore()
    gives_x = (me >= 1) & (me + 2 < n_micro)

    def here(dev):
        pl.semaphore_signal(barrier, inc=1, device_id={"stage": dev}, device_id_type=MESH)

    pl.when(jnp.logical_not(first))(lambda: here(me - 1))
    pl.when(jnp.logical_not(last))(lambda: here(me + 1))

    @pl.when(first)
    def _():
        for dev in range(2, n_micro - 2):
            here(dev)

    w_copy = [pltpu.make_async_copy(up_hbm, up, w_sem.at[0]), pltpu.make_async_copy(down_hbm, down, w_sem.at[1])]
    for c in w_copy:
        c.start()
    in_copy = [pltpu.make_async_copy(src, dst, in_sem.at[k]) for k, (src, dst) in enumerate(((lab_hbm, lab_ref), (row_hbm, row_ref), (cut_hbm, cut_ref)))]
    x_slots = x0_hbm.shape[0]
    x_mine = [head_chunk(me, k, n_micro) for k in range(x_slots)]

    def x_rows(m):
        return xbuf.at[pl.ds(m * per, per)]

    def x_local(k):
        return pltpu.make_async_copy(x0_hbm.at[k], x_rows(k), x_sem.at[k])

    @pl.when(first)
    def _():
        for k in range(x_slots):
            x_local(k).start()

    for c in in_copy:
        c.start()

    e_parts = plan.e_parts
    e_step = base // e_parts

    def e_copy(i):
        src = emb_hbm.at[pl.ds(pl.multiple_of(row0 + i * e_step, 16), e_step)]
        return pltpu.make_async_copy(src, emb.at[pl.ds(i * e_step, e_step)], e_sem.at[0])

    e_more = pltpu.make_async_copy(emb_hbm.at[pl.ds(2 * base, extra)], emb.at[pl.ds(base, extra)], e_sem.at[1])
    with jax.named_scope("entry"):
        pl.semaphore_wait(barrier, jnp.where(first | last, 1, 2) + jnp.where(gives_x & (me >= 2), 1, 0))

    def x_copy(k):
        return remote(x0_hbm.at[k], x_rows(x_mine[k]), x_send.at[k], f_recv.at[x_mine[k]], 0)

    @pl.when(gives_x)
    def _():
        x_copy(0).start()

        @pl.when(me < 2)
        def _():
            x_copy(1).start()

    def table_start():
        for i in range(e_parts):
            e_copy(i).start()
        pl.when(core == 1)(e_more.start)

    def transpose_weights():
        for j in range(n_fblk):
            up_t[j * fblk:(j + 1) * fblk, :] = up[:, j * fblk:(j + 1) * fblk].T
            down_t[:, j * fblk:(j + 1) * fblk] = down[j * fblk:(j + 1) * fblk, :].T

    @pl.when(jnp.logical_not(first))
    def _():
        for c in w_copy:
            c.wait()
        table_start()

    def idle_work():
        transpose_weights()
        in_copy[1].wait()
        in_copy[2].wait()
        token_table(row_ref, jnp.where(core == 0, cut_ref[0:1, :], cut_ref[1:2, :]), meta)

    @pl.when(chip >= n_stage // 4)
    def _():
        idle_work()

    def n_start(m):
        remote(nbuf.at[m], nbuf.at[m], n_send, n_recv.at[m], jnp.where(m == last_id, last_id - 1, m)).start()

    def fwd(h, carry, cold=False):
        m = h // per
        sub = lax.rem(h, per)
        rows = pl.ds(pl.multiple_of(sub * part, part), part)
        with jax.named_scope("fwd_wait"):

            @pl.when(first & (sub == 0))
            def _():
                @pl.when(m < x_slots)
                def _():
                    x_local(m).wait()

                @pl.when(m >= x_slots)
                def _():
                    remote(x_rows(m), x_rows(m), x_send.at[0], f_recv.at[m], me).wait_recv()

            @pl.when(jnp.logical_not(first))
            def _():
                remote(xbuf.at[h], xbuf.at[h], f_send, f_recv.at[h], me).wait_recv()

        with jax.named_scope("fwd_comp"):
            x = xbuf[h]
            if cold:
                w_copy[0].wait()
            for j in range(n_fblk):
                cols = slice(j * fblk, (j + 1) * fblk)
                a = dot(x, up[:, cols]).astype(BF16)
                abuf[m, rows, cols] = a
                hbuf[m, rows, cols] = gelu_fwd(a.astype(F32)).astype(BF16)
            if cold:
                w_copy[1].wait()
                table_start()
            y = (x.astype(F32) + dot(hbuf[m, rows, :], down[...])).astype(BF16)
            ybuf[h] = y

        @pl.when(jnp.logical_not(last))
        def _():
            remote(ybuf.at[h], xbuf.at[h], f_send, f_recv.at[h], me + 1).start()

        @pl.when(last)
        def _():
            yf = y.astype(F32)
            inv = lax.rsqrt(jnp.mean(yf * yf, axis=-1, keepdims=True) + EPS)
            nbuf[m, rows, :] = (yf * inv).astype(BF16)
            pl.when(sub == per - 1)(lambda: n_start(m))

        @pl.when(sub == per - 1)
        def _():
            pltpu.make_async_copy(hbuf.at[m], hid_out.at[m], out_sem.at[0]).start()
            pltpu.make_async_copy(x_rows(m), xs_out.at[pl.ds(m * per, per)], out_sem.at[1]).start()

        return carry

    pl.when(first)(lambda: (fwd(0, 0, cold=True), None)[1])
    lax.fori_loop(jnp.where(first, 1, 0), n_part, fwd, 0)

    @pl.when(chip < n_stage // 4)
    def _():
        idle_work()

    n_forward = remote(nbuf.at[me], nbuf.at[me], nf_send, n_recv.at[me], mate)
    with jax.named_scope("n_wait"):

        @pl.when(jnp.logical_not(last))
        def _():
            remote(nbuf.at[me], nbuf.at[me], n_send, n_recv.at[me], me).wait_recv()
            pl.when(mate != last_id)(n_forward.start)
            remote(nbuf.at[mate], nbuf.at[mate], n_send, n_recv.at[mate], me).wait_recv()

        for k in range(2):
            n_t[:, k * seq:(k + 1) * seq] = nbuf[2 * chip + k].T

    peers = [lax.rem(me + 2 * d, n_stage) for d in range(1, n_stage // 2)]
    ag_copies = [remote(nbuf.at[me], nbuf.at[me], ag_send.at[d], n_recv.at[me], p) for d, p in enumerate(peers)]
    for c, p in zip(ag_copies, peers):
        pl.when(p != last_id)(c.start)
    with jax.named_scope("e_wait"):
        pltpu.make_async_copy(emb_hbm.at[pl.ds(0, base)], emb.at[pl.ds(0, base)], e_sem.at[0]).wait()
        pl.when(core == 1)(e_more.wait)

    pair = 2 * seq
    scale = dim ** -0.5
    inv_count = 1.0 / n_tok
    log_count = math.log2(n_tok)
    in_copy[0].wait()
    lab = lab_ref[:, pl.ds(pl.multiple_of(chip * pair, pair), pair)]

    def logits(rows, size):
        e = emb[rows, :]
        parts = [dot(e[k * size // 2:(k + 1) * size // 2], n_t[...]) for k in range(2)]
        z = jnp.concatenate([(p * scale).astype(BF16) for p in parts], axis=0)
        zbuf[rows, :] = z
        return z

    def peak(z, size, top):
        best = jnp.max(z.reshape(size // 16, 16, pair), axis=0).astype(F32)
        return jnp.maximum(top, jnp.maximum(best[:8], best[8:]))

    def total(z, size, old, top, tot):
        off = top * LOG2E
        return tot * jnp.exp2(old * LOG2E - off) + jnp.sum(jnp.exp2(z.astype(F32).reshape(size // 8, 8, pair) * LOG2E - off[None]), axis=0)

    tops[0] = jnp.full((8, pair), -jnp.inf, F32)
    tops[1] = jnp.zeros((8, pair), F32)

    @pl.when(core == 1)
    def _():
        z = logits(pl.ds(base, extra), extra)
        top = peak(z, extra, tops[0])
        tops[1] = total(z, extra, tops[0], top, tops[1])
        tops[0] = top

    def logits_step(i, slot, old, top, tot):
        z = logits(pl.ds(pl.multiple_of(i * tile, 16), tile), tile)
        tot = total(z_pair[1 - slot], tile, old, top, tot)
        z_pair[slot] = z
        return top, peak(z, tile, top), tot

    with jax.named_scope("logits"):
        z = logits(pl.ds(0, tile), tile)
        z_pair[0] = z
        state = (tops[0], peak(z, tile, tops[0]), tops[1])
        state = lax.fori_loop(0, (n_tiles - 1) // 2, lambda i, c: logits_step(2 * i + 2, 0, *logits_step(2 * i + 1, 1, *c)), state)
        if n_tiles % 2 == 0:
            state = logits_step(n_tiles - 1, 1, *state)
        old, top, tot = state
        tot = total(z_pair[(n_tiles - 1) % 2], tile, old, top, tot)
    row_top = jnp.max(top, axis=0, keepdims=True)
    row_tot = jnp.sum(tot * jnp.exp2((top - row_top) * LOG2E), axis=0, keepdims=True)
    st_send[0:8, :] = jnp.broadcast_to(row_top, (8, pair))
    st_send[8:16, :] = jnp.broadcast_to(row_tot, (8, pair))
    st_copy = remote(st_send, st_recv, st_sems.at[0], st_sems.at[1], mate)
    with jax.named_scope("stat_x"):
        st_copy.start()
        st_copy.wait()
    far_top = st_recv[0:1, :]
    far_tot = st_recv[8:9, :]
    all_top = jnp.maximum(row_top, far_top)
    mine = row_tot * jnp.exp(row_top - all_top)
    other = far_tot * jnp.exp(far_top - all_top)
    lse = all_top + jnp.log(jnp.where(core == 0, mine + other, other + mine))
    my_shift = lse * LOG2E + log_count
    others = [lax.rem(me + d, n_stage) for d in range(1, n_stage)]

    def spread(buf, sems):
        whole = buf.at[pl.ds(0, n_stage - 1)]
        return [remote(buf.at[me], buf.at[me], sems.at[0], sems.at[1], p) for p in others], remote(whole, whole, sems.at[0], sems.at[1], me)

    statall[me] = jnp.broadcast_to(lse, (8, pair))
    sa_copies, sa_all = spread(statall, sa_sems)
    for c in sa_copies:
        c.start()

    def grads(rows, size, first_row, picked):
        zf = zbuf[rows, :].astype(F32)
        prob = jnp.exp2(zf * LOG2E - my_shift)
        hit = lax.broadcasted_iota(jnp.int32, (size, pair), 0) == lab - (row0 + first_row)
        dz_t = jnp.where(hit, prob - inv_count, prob).astype(BF16)
        got = jnp.where(hit, zf, 0.0).reshape(size // 8, 8, pair)
        return dot_t(dz_t, emb[rows, :]), picked + jnp.sum(got, axis=0)

    tops[0] = jnp.zeros((8, pair), F32)
    dn_acc[...] = jnp.zeros_like(dn_acc)

    @pl.when(core == 1)
    def _():
        dn_acc[...], tops[0] = grads(pl.ds(base, extra), extra, base, tops[0])

    def grad_step(i, picked):
        part, picked = grads(pl.ds(pl.multiple_of(i * wide_tile, 16), wide_tile), wide_tile, i * wide_tile, picked)
        dn_acc[...] += part
        return picked

    with jax.named_scope("grads"):
        picked = lax.fori_loop(0, base // wide_tile, grad_step, tops[0])
    far = pl.ds(pl.multiple_of((1 - core) * seq, seq), seq)
    near = pl.ds(pl.multiple_of(core * seq, seq), seq)
    dn_send[...] = dn_acc[far, :]
    dp_copy = remote(dn_send, dn_recv, dp_sems.at[0], dp_sems.at[1], mate)
    dp_copy.start()
    row_loss = jnp.where(core == 0, lse, 0.0) - jnp.sum(picked, axis=0, keepdims=True)
    lossall[me] = jnp.broadcast_to(row_loss, (8, pair))
    lo_copies, lo_all = spread(lossall, lo_sems)
    for c in lo_copies:
        c.start()
    with jax.named_scope("dn_x"):
        dp_copy.wait()
        dn = ((dn_acc[near, :] + dn_recv[...]) * scale).astype(BF16)
    dn_copy = remote(dn_own, dnbuf.at[me], dn_ssem, dn_rsem.at[me], last_id)

    @pl.when(last)
    def _():
        dnbuf[last_id] = dn

    @pl.when(jnp.logical_not(last))
    def _():
        dn_own[...] = dn
        remote(dn_own, dnbuf.at[me], dn_ssem, dn_rsem.at[me], last_id).start()

    with jax.named_scope("ag_wait"):
        for p in peers:
            got = remote(nbuf.at[p], nbuf.at[p], ag_send.at[0], n_recv.at[p], me)
            pl.when(jnp.logical_not(last))(got.wait_recv)
            pl.when(mate != last_id)(remote(nbuf.at[p], nbuf.at[p], fw_send, n_recv.at[p], mate).start)

    near_dst = [1, 3, last_id]
    far_dst = n_stage // 2 + 1
    direct = n_micro - 2
    by_prev = n_micro - 3
    hands_on = (core == 1) & (me != 1)

    def dx0_start(m, k, dev):
        remote(dxbuf.at[m], dx0buf.at[m], d_send.at[k], d_recv.at[m], dev).start()

    def relayed(m):
        return (m < direct) & (((me == 3) & (m != by_prev)) | (last & (m == by_prev)))

    def relay_far(m):
        remote(dx0buf.at[m], dx0buf.at[m], r_sems.at[1], d_recv.at[m], far_dst).start()

    def bwd(m):
        with jax.named_scope("bwd_wait"):
            @pl.when(jnp.logical_not(last))
            def _():
                remote(gbuf.at[m], gbuf.at[m], b_send, b_recv.at[m], me).wait_recv()

            @pl.when(last)
            def _():
                @pl.when(m != last_id)
                def _():
                    remote(dnbuf.at[m], dnbuf.at[m], dn_ssem, dn_rsem.at[m], me).wait_recv()

                yf = ybuf[pl.ds(m * per, per)].reshape(seq, dim).astype(F32)
                inv = lax.rsqrt(jnp.mean(yf * yf, axis=-1, keepdims=True) + EPS)
                dnf = dnbuf[m].astype(F32)
                proj = jnp.mean(yf * dnf, axis=-1, keepdims=True)
                gbuf[m] = (dnf * inv - yf * (inv * inv * inv * proj)).astype(BF16)

        with jax.named_scope("bwd_comp"):
            g = gbuf[m]
            for j in range(n_fblk):
                cols = slice(j * fblk, (j + 1) * fblk)
                dh = dot(g, down_t[:, cols]).astype(BF16).astype(F32)
                abuf[m, :, cols] = (dh * gelu_slope(abuf[m, :, cols].astype(F32))).astype(BF16)
            dxbuf[m] = (g.astype(F32) + dot(abuf[m], up_t[...])).astype(BF16)

        @pl.when(jnp.logical_not(first))
        def _():
            remote(dxbuf.at[m], gbuf.at[m], b_send, b_recv.at[m], me - 1).start()

        @pl.when(first)
        def _():
            pl.when(m >= direct)(lambda: dx0_start(m, len(near_dst), far_dst))
            for k, dev in enumerate(near_dst):
                dx0_start(m, k, dev)

        pltpu.make_async_copy(abuf.at[m], da_out.at[m], out_sem.at[2]).start()
        pltpu.make_async_copy(gbuf.at[m], g_out.at[m], out_sem.at[3]).start()

    n_slot = obuf.shape[0]
    busy = chip == last_id // 2
    far_tile = remote(tmp_out.at[core, pl.ds(0, plan.rows)], tmp_out.at[core, pl.ds(0, plan.rows)], ic_send, od_recv, jnp.where(first, last_id, last_id - 1))
    sends_far = first | (me == last_id - 2)

    def tile_copy(k):
        rows = pl.ds(pl.multiple_of(k * plan.rows, plan.rows), plan.rows)
        slot = lax.rem(k, n_slot)
        return pltpu.make_async_copy(obuf.at[slot], tmp_out.at[core, rows], o_sem.at[slot])

    def piece(p):
        k = p // plan.per_tile
        rows = pl.ds(pl.multiple_of(p * plan.piece, plan.piece), plan.piece)
        here = pl.ds(pl.multiple_of(lax.rem(p, plan.per_tile) * plan.piece, plan.piece), plan.piece)
        return remote(obuf.at[lax.rem(k, n_slot), here], tmp_out.at[core, rows], od_send.at[k], od_recv, mate)

    def tile_sent(k):
        slot = lax.rem(k, n_slot)
        return remote(obuf.at[slot], tmp_out.at[core, pl.ds(0, plan.rows)], od_send.at[k], od_recv, mate)

    def emb_tile(k):
        with jax.named_scope("tile_prep"):

            @pl.when(k == 0)
            def _():
                for d in range(1, n_stage // 2):
                    src = lax.rem(mate + 2 * d, n_stage)
                    pl.when(jnp.logical_not(last))(remote(nbuf.at[src], nbuf.at[src], ag_send.at[0], n_recv.at[src], me).wait_recv)
                for m in range(n_micro):
                    n_all_t[:, m * seq:(m + 1) * seq] = nbuf[m].T
                sa_all.wait_recv()
                for c in range(n_stage // 2):
                    shift[:, c * pair:(c + 1) * pair] = statall[2 * c, 0:1, :] * LOG2E + log_count

        slot = lax.rem(k, n_slot)
        with jax.named_scope("tile_wait"):
            @pl.when(k == 2)
            def _():
                tile_copy(0).wait()
                pl.when(sends_far)(far_tile.start)

            pl.when(k > n_slot)(lambda: tile_copy(k - n_slot).wait())
            pl.when((k >= n_slot) & (k - n_slot < plan.shared) & jnp.logical_not(busy & (k == n_slot)))(lambda: tile_sent(k - n_slot).wait_send())

        with jax.named_scope("tile"):
            rows = pl.ds(pl.multiple_of(k * plan.rows, plan.rows), plan.rows)
            logit_grad(emb[rows, :], n_all_t, shift, lab_ref, row0 + k * plan.rows, inv_count, scale, dz)
            obuf[slot] = dot(dz[...], nbuf[...].reshape(n_tok, dim)) * scale

        tile_copy(k).start()

    def send_pieces(done, until):
        lax.fori_loop(done, until, lambda p, c: (piece(p).start(), c)[1], 0)

    def send_tiles(done, until):
        def one(k, carry):
            rows = pl.ds(pl.multiple_of(k * plan.rows, plan.rows), plan.rows)
            remote(obuf.at[lax.rem(k, n_slot)], tmp_out.at[core, rows], od_send.at[k], od_recv, mate).start()
            return carry

        lax.fori_loop(done, until, one, 0)

    before = sum(jnp.where(me == s, plan.before[s], 0) for s in range(n_stage))

    def pass_dx0(m, carry):
        @pl.when(jnp.logical_not(first))
        def _():
            remote(dx0buf.at[m], dx0buf.at[m], r_sems.at[0], d_recv.at[m], me).wait_recv()

            @pl.when(hands_on)
            def _():
                remote(dx0buf.at[m], dx0buf.at[m], r_sems.at[0], d_recv.at[m], mate).start()

            @pl.when(relayed(m))
            def _():
                relay_far(m)

            pltpu.make_async_copy(dx0buf.at[m], dx0_out.at[m], out_sem.at[4]).start()

        @pl.when(first)
        def _():
            pltpu.make_async_copy(dxbuf.at[m], dx0_out.at[m], out_sem.at[4]).start()

        return carry

    lead = jnp.where(me == 3, -300, jnp.where(last, -1800, jnp.where(me == far_dst, -1600, -10**6)))

    def work(i, carry):
        sent, passed = carry
        chunk = (i >= before) & (i < before + n_micro)
        pl.when(chunk)(lambda: bwd(i - before))
        k = jnp.where(i < before, i, i - n_micro)
        pl.when(jnp.logical_not(chunk))(lambda: emb_tile(k))
        after = i - before - n_micro + 1
        here = jnp.where(after > 0, jnp.clip((after * 264 + lead) // 138, 0, n_micro), 0)
        lax.fori_loop(passed, here, pass_dx0, 0)
        ready = jnp.where(i < before, i + 1, jnp.where(chunk, before, i + 1 - n_micro))
        near_chunks = chunk | ((i < before) & (i + jnp.where(before >= 6, 2, 1) >= before))
        whole = (sent + plan.per_tile - 1) // plan.per_tile
        upto = jnp.minimum(jnp.minimum(ready, plan.shared), whole + 1)
        some = jnp.where(near_chunks, jnp.minimum(sent + 1, jnp.minimum(ready, plan.shared) * plan.per_tile), whole * plan.per_tile)
        send_pieces(sent, some)
        send_tiles(whole, jnp.where(near_chunks, 0, upto))
        now = jnp.where(near_chunks, some, jnp.maximum(some, upto * plan.per_tile))
        return jnp.maximum(sent, now), jnp.maximum(passed, here)

    sent, passed = lax.fori_loop(0, plan.tiles + n_micro, work, (jnp.where(busy, plan.per_tile, 0), 0))
    outs = [pltpu.make_async_copy(nbuf, n_out, out_sem.at[5]), pltpu.make_async_copy(lossall, loss_out, out_sem.at[6]), pltpu.make_async_copy(meta, meta_out, out_sem.at[7])]
    lo_all.wait_recv()
    for c in outs:
        c.start()
    pltpu.make_async_copy(statall, stat_out, out_sem.at[8]).start()
    with jax.named_scope("relay_all"):
        lax.fori_loop(passed, n_micro, pass_dx0, 0)

    with jax.named_scope("drain"):
        send_pieces(sent, plan.shared * plan.per_tile)
        for k in range(max(plan.tiles - n_slot, 0), plan.tiles):
            tile_copy(k).wait()
            if k < plan.shared:
                tile_sent(k).wait_send()
        pl.when(sends_far)(far_tile.wait_send)
        all_rows = pl.ds(0, plan.shared * plan.rows)
        remote(tmp_out.at[1 - core, all_rows], tmp_out.at[1 - core, all_rows], od_send.at[0], od_recv, me).wait_recv()
        sa_all.wait_send()
        lo_all.wait_send()
        pltpu.make_async_copy(statall, stat_out, out_sem.at[8]).wait()
        for c, p in zip(ag_copies, peers):
            pl.when(p != last_id)(c.wait_send)

        @pl.when(jnp.logical_not(last))
        def _():
            dn_copy.wait_send()
            pl.when(mate != last_id)(n_forward.wait_send)
            remote(ybuf, xbuf, f_send, f_recv.at[0], me + 1).wait_send()

        @pl.when(last)
        def _():
            remote(nbuf, nbuf, n_send, n_recv.at[0], me).wait_send()

        @pl.when(mate != last_id)
        def _():
            some = nbuf.at[pl.ds(0, len(peers))]
            remote(some, some, fw_send, n_recv.at[0], mate).wait_send()

        @pl.when(gives_x)
        def _():
            x_copy(0).wait_send()

            @pl.when(me < 2)
            def _():
                x_copy(1).wait_send()

        @pl.when(jnp.logical_not(first))
        def _():
            remote(dxbuf, gbuf, b_send, b_recv.at[0], me).wait_send()
            pl.when(hands_on)(remote(dx0buf, dx0buf, r_sems.at[0], d_recv.at[0], mate).wait_send)

        @pl.when(first)
        def _():
            for k in range(len(near_dst)):
                remote(dxbuf, dx0buf, d_send.at[k], d_recv.at[0], me).wait_send()
            rest = pl.ds(0, n_micro - direct)
            remote(dxbuf.at[rest], dx0buf.at[rest], d_send.at[len(near_dst)], d_recv.at[0], me).wait_send()

        for dev, kept in ((3, direct - 1), (last_id, 1)):
            some = dx0buf.at[pl.ds(0, kept)]
            pl.when(me == dev)(remote(some, some, r_sems.at[1], d_recv.at[0], me).wait_send)

        pltpu.make_async_copy(hbuf, hid_out, out_sem.at[0]).wait()
        pltpu.make_async_copy(xbuf, xs_out, out_sem.at[1]).wait()
        pltpu.make_async_copy(abuf, da_out, out_sem.at[2]).wait()
        pltpu.make_async_copy(gbuf, g_out, out_sem.at[3]).wait()
        pltpu.make_async_copy(dx0buf, dx0_out, out_sem.at[4]).wait()
        for c in outs:
            c.wait()


class Plan:
    def __init__(self, vocab, n_stage):
        units = vocab // LANES
        self.base = units // 2 * LANES
        self.extra = vocab - 2 * self.base
        self.head_tile = next(t for t in (1600, 1536, 1280, 1024, 768, 640, 512, 256, 128) if self.base % t == 0)
        self.rows = 1024
        self.tiles, self.shared = 11, 9
        self.grad_tile = next(t for t in (4000, 3200, 1600, 1280, 640, 256, 128) if self.base % t == 0)
        self.e_parts = next(k for k in (10, 8, 5, 4, 2, 1) if self.base % (16 * k) == 0)
        self.part = 128
        self.slots = 4
        self.piece = 256
        self.per_tile = self.rows // self.piece
        measured = [10, 9, 6, 5, 3, 2, 0, 0]
        self.before = (measured + [0] * n_stage)[:n_stage]
        mid = self.base
        ends = [(0, mid), (mid, vocab)]
        early = (self.tiles * self.rows, self.shared * self.rows)
        self.spans = [[(ends[h][0] + early[0 if h == c else 1], ends[h][1]) for h in (c, 1 - c)] for c in range(2)]
        self.longest = [max(self.spans[c][k][1] - self.spans[c][k][0] for c in range(2)) for k in range(2)]
        best = min(range(16, 1281, 16), key=lambda r: (sum(-(-n // r) for n in self.longest)) * (r + 40))
        self.calc_rows = best
        self.calc_steps = [-(-n // best) for n in self.longest]
        self.steps = sum(self.calc_steps)
        self.copy_rows = self.rows
        self.copies = self.tiles + self.shared
        self.starts = ends

    def calc_start(self, core, s):
        k = 0 if s < self.calc_steps[0] else 1
        lo, hi = self.spans[core][k]
        return min(lo + (s - k * self.calc_steps[0]) * self.calc_rows, hi - self.calc_rows)

    def copy_start(self, core, c):
        own = c < self.tiles
        h = core if own else 1 - core
        return self.starts[h][0] + (c if own else c - self.tiles) * self.copy_rows

    def cuts(self, core):
        firsts = [(self.calc_start(core, s), self.calc_rows) for s in range(self.steps)] + [(self.copy_start(core, c), self.copy_rows) for c in range(self.copies)]
        flat = [v for lo, rows in firsts for v in (lo, lo + rows)]
        return flat + [0] * (LANES - len(flat))


def run_pipe(x0, emb, w_up, w_down, labels, tokens, cuts, n_stage, plan):
    n_micro, seq = labels.shape
    dim, ffn = w_up.shape
    n_tok = n_micro * seq
    base = plan.base
    any_spec = pl.BlockSpec(memory_space=pl.ANY)
    act = (n_micro, seq, dim)
    fine = (n_tok // plan.part, plan.part, dim)
    wide = (n_micro, seq, ffn)
    dma = pltpu.SemaphoreType.DMA
    vm = pltpu.VMEM
    pair = 2 * seq
    return pl.pallas_call(
        functools.partial(pipe_kernel, n_stage, plan),
        out_shape=[
            jax.ShapeDtypeStruct(act, BF16), jax.ShapeDtypeStruct(fine, BF16), jax.ShapeDtypeStruct(wide, BF16),
            jax.ShapeDtypeStruct(wide, BF16), jax.ShapeDtypeStruct(act, BF16), jax.ShapeDtypeStruct(act, BF16),
            jax.ShapeDtypeStruct((n_stage, 8, pair), F32), jax.ShapeDtypeStruct((n_stage, 8, pair), F32), jax.ShapeDtypeStruct((2, plan.tiles * plan.rows, dim), F32),
            jax.ShapeDtypeStruct((3 * n_tok // LANES, LANES), jnp.int32),
        ],
        in_specs=[any_spec] * 7,
        out_specs=[any_spec] * 10,
        scratch_shapes=[
            vm(fine, BF16), vm(fine, BF16), vm(wide, BF16), vm(wide, BF16), vm(act, BF16), vm(act, BF16), vm(act, BF16), vm(act, BF16), vm(act, BF16),
            vm((dim, ffn), BF16), vm((ffn, dim), BF16), vm((ffn, dim), BF16), vm((dim, ffn), BF16),
            vm((base + plan.extra, dim), BF16), vm((base + plan.extra, pair), BF16), vm((dim, pair), BF16), vm((pair, dim), F32),
            vm((seq, dim), F32), vm((seq, dim), F32), vm((seq, dim), BF16), vm((16, pair), F32), vm((16, pair), F32), vm((n_stage, 8, pair), F32), vm((n_stage, 8, pair), F32),
            vm((2, 8, pair), F32), vm((dim, n_tok), BF16), vm((1, n_tok), F32), vm((plan.rows, n_tok), BF16), vm((plan.slots, plan.rows, dim), F32),
            vm((2, plan.head_tile, pair), BF16), vm((3 * n_tok // LANES, LANES), jnp.int32),
            vm((1, n_tok), jnp.int32), vm((1, n_tok), jnp.int32), vm((2, LANES), jnp.int32),
            dma((2,)), dma((2,)), dma((2,)), dma((2,)), dma, dma((n_tok // plan.part,)), dma, dma((n_micro,)), dma,
            dma((n_stage // 2,)), dma,
            dma((2,)), dma((2,)), dma, dma((n_stage,)), dma((2,)), dma((2,)), dma, dma((n_micro,)), dma((4,)), dma((n_micro,)), dma((2,)), dma((9,)),
            dma((plan.slots,)), dma((plan.shared,)), dma, dma, dma((3,)),
        ],
        compiler_params=pltpu.CompilerParams(collective_id=0, has_side_effects=True, vmem_limit_bytes=67_000_000),
        cost_estimate=pl.CostEstimate(flops=60 * 10**9, bytes_accessed=100 * 10**6, transcendentals=0),
        name="pipe",
    )(x0.reshape(x0.shape[0], seq // plan.part, plan.part, dim), emb, w_up, w_down, labels.reshape(1, n_tok), tokens.reshape(1, n_tok), cuts)


def fin_kernel(n_stage, n_tok, plan, ids_hbm, emb_hbm, tmp_hbm, n_hbm, stat_hbm, part_hbm, lab_hbm, meta_hbm, dx0_hbm, xs_hbm, hid_hbm, da_hbm, g_hbm,
               out_hbm, loss_ref, gup_hbm, gdown_hbm,
               n_all, dx0, xs, hid, da, g, n_t, x_t, dx0s, dz, shift, e_in, c_out, cp, gup, gdown,
               ld_sem, e_sem, t_sem, co_sem, po_sem, gu_sem, gd_sem, wi_sem, ids_ref, stat_ref, part_ref, lab_ref, meta_ref, in_sem):
    dim, ffn = gup_hbm.shape
    scale = dim ** -0.5
    inv_count = 1.0 / n_tok
    steps, crows, prows = plan.steps, plan.calc_rows, plan.copy_rows
    core = lax.rem(lax.axis_index("stage"), 2)
    early = plan.tiles * prows
    wblk = gup.shape[2]
    n_wblk = ffn // wblk
    turn = plan.calc_steps[0]

    def pick(pair):
        return jnp.where(core == 0, pair[0], pair[1])

    def calc_start(s):
        own = s < turn
        lo, hi = [jnp.where(own, pick([plan.spans[c][0][e] for c in range(2)]), pick([plan.spans[c][1][e] for c in range(2)])) for e in range(2)]
        return pl.multiple_of(jnp.minimum(lo + (s - jnp.where(own, 0, turn)) * crows, hi - crows), 16)

    def copy_start(c):
        own = c < plan.tiles
        first = jnp.where(own, pick([plan.starts[0][0], plan.starts[1][0]]), pick([plan.starts[1][0], plan.starts[0][0]]))
        return pl.multiple_of(first + (c - jnp.where(own, 0, plan.tiles)) * prows, 16)

    def e_copy(s):
        return pltpu.make_async_copy(emb_hbm.at[pl.ds(calc_start(s), crows)], e_in.at[lax.rem(s, 3)], e_sem.at[lax.rem(s, 3)])

    n_slot = cp.shape[0]
    ahead = 8

    def t_copy(c):
        own = c < plan.tiles
        row = jnp.where(own, core, 1 - core) * early + (c - jnp.where(own, 0, plan.tiles)) * prows
        slot = lax.rem(c, n_slot)
        return pltpu.make_async_copy(tmp_hbm.at[pl.ds(pl.multiple_of(row, 16), prows)], cp.at[slot], t_sem.at[slot])

    def p_out(c):
        slot = lax.rem(c, n_slot)
        return pltpu.make_async_copy(cp.at[slot], out_hbm.at[pl.ds(copy_start(c), prows)], po_sem.at[slot])

    def c_outs(s):
        slot = lax.rem(s, 2)
        return pltpu.make_async_copy(c_out.at[slot], out_hbm.at[pl.ds(calc_start(s), crows)], co_sem.at[slot])

    loads = [pltpu.make_async_copy(s, d, ld_sem.at[i]) for i, (s, d) in enumerate(((n_hbm, n_all), (dx0_hbm, dx0), (xs_hbm, xs), (g_hbm, g)))]
    ins = [pltpu.make_async_copy(s, d, in_sem.at[i]) for i, (s, d) in enumerate(((stat_hbm, stat_ref), (lab_hbm, lab_ref), (part_hbm, part_ref), (meta_hbm, meta_ref), (ids_hbm, ids_ref)))]
    loads[0].start()
    ins[0].start()
    ins[1].start()
    e_copy(0).start()
    loads[1].start()
    for c in ins[2:]:
        c.start()
    e_copy(1).start()
    for c in range(ahead):
        t_copy(c).start(priority=1)
    pair = stat_ref.shape[2]
    with jax.named_scope("fin_pre"):
        ins[0].wait()
        ins[1].wait()
        for c in range(n_stage // 2):
            shift[:, c * pair:(c + 1) * pair] = stat_ref[2 * c, 0:1, :] * LOG2E + math.log2(n_tok)
        loads[0].wait()
        n_t[...] = n_all[...].T

    def sum_rows():
        for c in ins[2:]:
            c.wait()
        loss_ref[0] = jnp.sum(sum(part_ref[d, 0:1, :] for d in range(n_stage))) * inv_count
        loads[1].wait()
        dense = jnp.concatenate([meta_ref[g:g + 1, :] for g in range(n_tok // LANES)], axis=1)
        order = lax.broadcasted_iota(jnp.int32, (n_tok, n_tok), 0) == dense
        dx0s[...] = dot(jnp.where(order, 1.0, 0.0).astype(BF16), dx0[...])

    def add_rows(k, start, ref):
        lo, hi = ids_ref[2 * n_tok + k], ids_ref[2 * n_tok + k + 1]
        wide = 8

        def some(p, width):
            at = [pl.ds(ids_ref[n_tok + p + u] - start, 1) for u in range(width)]
            new = [ref[at[u], :] + dx0s[pl.ds(p + u, 1), :] for u in range(width)]
            for u in range(width):
                ref[at[u], :] = new[u]

        def group(g, carry):
            some(lo + g * wide, wide)
            return carry

        def single(p, carry):
            some(p, 1)
            return carry

        n_grp = (hi - lo) // wide
        lax.fori_loop(0, n_grp, group, 0)
        lax.fori_loop(lo + n_grp * wide, hi, single, 0)

    def w_ins(w):
        cols = pl.ds(pl.multiple_of(w * wblk, wblk), wblk)
        wslot = lax.rem(w, 2)
        return (pltpu.make_async_copy(da_hbm.at[:, cols], da.at[wslot], wi_sem.at[0, wslot]), pltpu.make_async_copy(hid_hbm.at[:, cols], hid.at[wslot], wi_sem.at[1, wslot]))

    def w_outs(w):
        cols = pl.ds(pl.multiple_of(w * wblk, wblk), wblk)
        wslot = lax.rem(w, 2)
        return (pltpu.make_async_copy(gup.at[wslot], gup_hbm.at[:, cols], gu_sem.at[wslot]), pltpu.make_async_copy(gdown.at[wslot], gdown_hbm.at[cols], gd_sem.at[wslot]))

    def copy_tile(c, carry):
        with jax.named_scope("copy_wait"):
            t_copy(c).wait()
        with jax.named_scope("add_p"):
            add_rows(2 * steps + 2 * c, copy_start(c), cp.at[lax.rem(c, n_slot)])
        p_out(c).start()

        @pl.when(c + ahead < plan.copies)
        def _():
            pl.when(c + ahead >= n_slot)(lambda: p_out(c + ahead - n_slot).wait())
            t_copy(c + ahead).start(priority=1)

        return carry

    w_first = 2
    tails = [turn - 1, steps - 1]

    def tail(s):
        return (s == tails[0]) | (s == tails[1])

    def step(s, carry):
        pl.when(s + 2 < steps)(lambda: e_copy(s + 2).start())
        with jax.named_scope("fin_wait"):
            e_copy(s).wait()

        @pl.when(s == 0)
        def _():
            for c in loads[2:]:
                c.start()

        w = s - w_first

        @pl.when((w + 1 >= 0) & (w + 1 < n_wblk))
        def _():
            for c in w_ins(w + 1):
                c.start()

        pl.when((s >= 2) & jnp.logical_not(tail(s - 1)))(lambda: c_outs(s - 2).wait())
        slot = lax.rem(s, 2)
        start = calc_start(s)
        with jax.named_scope("calc"):
            logit_grad(e_in[lax.rem(s, 3)], n_t, shift, lab_ref, start, inv_count, scale, dz)
            c_out[slot] = dot(dz[...], n_all[...]) * scale
        pl.when(s == 0)(sum_rows)
        with jax.named_scope("add_c"):
            add_rows(2 * s, start, c_out.at[slot])
        pl.when(tail(s))(lambda: c_outs(s - 1).wait())
        c_outs(s).start()
        lax.fori_loop(s * plan.copies // (steps - 1), jnp.minimum((s + 1) * plan.copies // (steps - 1), plan.copies), copy_tile, 0)

        @pl.when(w == 0)
        def _():
            for c in loads[2:]:
                c.wait()
            x_t[...] = xs[...].T

        @pl.when((w >= 0) & (w < n_wblk))
        def _():
            wslot = lax.rem(w, 2)
            with jax.named_scope("dw_wait"):
                for c in w_ins(w):
                    c.wait()

                @pl.when(w >= 2)
                def _():
                    for c in w_outs(w - 2):
                        c.wait()

            with jax.named_scope("dw"):
                gup[wslot] = dot(x_t[...], da[wslot])
                gdown[wslot] = dot_t(hid[wslot], g[...])
            for c in w_outs(w):
                c.start()

        return carry

    lax.fori_loop(0, steps, step, 0)
    with jax.named_scope("fin_drain"):
        for w in range(n_wblk - 2, n_wblk):
            for c in w_outs(w):
                c.wait()
        c_outs(steps - 1).wait()
        for c in range(plan.copies - n_slot, plan.copies):
            p_out(c).wait()


def run_fin(emb, tmp, n_all, stats, losses, labels, meta, dx0, xs, hid, da, g, n_stage, plan):
    vocab, dim = emb.shape
    n_tok, ffn = hid.shape
    vm = pltpu.VMEM
    dma = pltpu.SemaphoreType.DMA
    any_spec = pl.BlockSpec(memory_space=pl.ANY)
    smem = pl.BlockSpec(memory_space=pltpu.SMEM)
    wblk = 512
    return pl.pallas_call(
        functools.partial(fin_kernel, n_stage, n_tok, plan),
        out_shape=[jax.ShapeDtypeStruct((vocab, dim), F32), jax.ShapeDtypeStruct((1,), F32), jax.ShapeDtypeStruct((dim, ffn), F32), jax.ShapeDtypeStruct((ffn, dim), F32)],
        in_specs=[any_spec] * 13,
        out_specs=[any_spec, smem, any_spec, any_spec],
        scratch_shapes=[
            vm((n_tok, dim), BF16), vm((n_tok, dim), BF16), vm((n_tok, dim), BF16), vm((2, n_tok, wblk), BF16), vm((2, n_tok, wblk), BF16), vm((n_tok, dim), BF16),
            vm((dim, n_tok), BF16), vm((dim, n_tok), BF16), vm((n_tok, dim), F32), vm((plan.calc_rows, n_tok), BF16), vm((1, n_tok), F32),
            vm((3, plan.calc_rows, dim), BF16), vm((2, plan.calc_rows, dim), F32), vm((11, plan.copy_rows, dim), F32),
            vm((2, dim, wblk), F32), vm((2, wblk, dim), F32),
            dma((4,)), dma((3,)), dma((11,)), dma((2,)), dma((11,)), dma((2,)), dma((2,)), dma((2, 2)),
            pltpu.SMEM((meta.size,), jnp.int32), vm(stats.shape, F32), vm(losses.shape, F32), vm((1, n_tok), jnp.int32), vm(meta.shape, jnp.int32), dma((5,)),
        ],
        compiler_params=pltpu.CompilerParams(vmem_limit_bytes=67_000_000),
        cost_estimate=pl.CostEstimate(flops=2 * n_tok * vocab * dim, bytes_accessed=5 * vocab * dim, transcendentals=0),
        name="fin",
    )(meta.reshape(-1), emb, tmp, n_all, stats, losses, labels.reshape(1, n_tok), meta, dx0, xs, hid, da, g)


def solution(mesh):
    n_stage = mesh.shape["stage"]

    def device_fn(tokens, labels, emb, w_up, w_down):
        n_micro, seq = tokens.shape
        vocab, dim = emb.shape
        w_up, w_down = w_up[0], w_down[0]
        n_tok = n_micro * seq
        plan = Plan(vocab, n_stage)
        cuts = jnp.array([plan.cuts(0), plan.cuts(1)], jnp.int32)
        x0 = run_gather(tokens, emb)
        n_all, xs, hid, da, g, dx0, stats, losses, tmp, meta = run_pipe(x0, emb, w_up, w_down, labels, tokens, cuts, n_stage, plan)
        flat = lambda p: p.reshape(n_tok, -1)
        grad_emb, loss, grad_up, grad_down = run_fin(
            emb, tmp.reshape(-1, dim), flat(n_all), stats, losses, labels, meta, flat(dx0), flat(xs), flat(hid), flat(da), flat(g), n_stage, plan
        )
        return loss, grad_up[None], grad_down[None], grad_emb

    return jax.shard_map(device_fn, mesh=mesh, in_specs=(P("dp", None), P("dp", None), P(None, None), P("stage", None, None), P("stage", None, None)), out_specs=(P("dp"), P(("dp", "stage"), None, None), P(("dp", "stage"), None, None), P("dp", None)), check_vma=False)
```

```python
import functools
import math

import jax
import jax.numpy as jnp
from jax import lax
from jax.experimental import pallas as pl
from jax.experimental.pallas import tpu as pltpu
from jax.sharding import PartitionSpec as P


MESH = pl.DeviceIdType.MESH
LOG2E = math.log2(math.e)
LN2 = math.log(2.0)
GELU_C = math.sqrt(2.0 / math.pi)
GELU_K = 0.044715
EPS = 1e-6
LANES = 128
F32 = jnp.float32
BF16 = jnp.bfloat16


def gelu_fwd(a):
    return (0.5 * a) * (1.0 + jnp.tanh(a * (GELU_C + (GELU_C * GELU_K) * (a * a))))


def gelu_slope(a):
    a2 = a * a
    half = 0.5 * jnp.tanh(a * (GELU_C + (GELU_C * GELU_K) * a2))
    up, down = 0.5 + half, 0.5 - half
    return up + (up * down) * (a * (2.0 * GELU_C + (6.0 * GELU_C * GELU_K) * a2))


def dot(x, y):
    return jnp.dot(x, y, preferred_element_type=F32)


def dot_t(x, y):
    return lax.dot_general(x, y, (((0,), (0,)), ((), ())), preferred_element_type=F32)


def remote(src, dst, send_sem, recv_sem, dev):
    return pltpu.make_async_remote_copy(src_ref=src, dst_ref=dst, send_sem=send_sem, recv_sem=recv_sem, device_id={"stage": dev}, device_id_type=MESH)


def column(row):
    return jnp.broadcast_to(row, (LANES, LANES)).T


def gather_kernel(ids_ref, tok_ref, emb_hbm, x0_hbm, tiles, picked, sem, out_sem):
    n_micro, seq = tok_ref.shape
    me = lax.axis_index("stage")
    group = tiles.shape[1] // seq
    slots = tiles.shape[0]
    owners = [head_chunk(me, k, n_micro) for k in range(slots)]

    def fetch(k):
        def one(i, carry):
            t = ids_ref[owners[k] * seq + i]
            start = pl.multiple_of(lax.bitwise_and(t, -group), group)
            pltpu.make_async_copy(emb_hbm.at[pl.ds(start, group)], tiles.at[k, pl.ds(pl.multiple_of(i * group, group), group)], sem.at[k]).start()
            return carry

        lax.fori_loop(0, seq, one, 0, unroll=8)

    def select(k):
        sub = lax.broadcasted_iota(jnp.int32, (LANES, LANES), 0)
        lane = lax.broadcasted_iota(jnp.int32, (LANES, LANES), 1)
        tok = column(tok_ref[pl.ds(owners[k], 1), :].astype(F32)).astype(jnp.int32)
        want = sub * group + lax.bitwise_and(tok, group - 1)
        hot = jnp.concatenate([jnp.where(lane + b * LANES == want, 1.0, 0.0).astype(BF16) for b in range(seq * group // LANES)], axis=1)
        pltpu.make_async_copy(emb_hbm.at[pl.ds(0, seq * group)], tiles.at[k], sem.at[k]).wait()
        picked[k] = dot(hot, tiles[k]).astype(BF16)
        pltpu.make_async_copy(picked.at[k], x0_hbm.at[k], out_sem.at[k]).start()

    def finish(k):
        pltpu.make_async_copy(picked.at[k], x0_hbm.at[k], out_sem.at[k]).wait()

    for work in (fetch, select, finish):
        work(0)
        for k in range(1, slots):
            pl.when(me < slots)(functools.partial(work, k))


def head_chunk(dev, k, n_micro):
    return jnp.minimum(jnp.where(dev < 2, 2 * dev + k, dev + 2), n_micro - 1)


def run_gather(tokens, emb):
    n_micro, seq = tokens.shape
    dim = emb.shape[1]
    group = 16
    return pl.pallas_call(
        gather_kernel,
        out_shape=jax.ShapeDtypeStruct((2, seq, dim), BF16),
        in_specs=[pl.BlockSpec(memory_space=pltpu.SMEM), pl.BlockSpec(memory_space=pltpu.VMEM), pl.BlockSpec(memory_space=pl.ANY)],
        out_specs=pl.BlockSpec(memory_space=pl.ANY),
        scratch_shapes=[pltpu.VMEM((2, seq * group, dim), BF16), pltpu.VMEM((2, seq, dim), BF16), pltpu.SemaphoreType.DMA((2,)), pltpu.SemaphoreType.DMA((2,))],
        cost_estimate=pl.CostEstimate(flops=10**9, bytes_accessed=2 * seq * group * dim * 2, transcendentals=0),
        name="gather",
    )(tokens.reshape(n_micro * seq), tokens, emb)


def token_table(row_ref, cut_ref, meta):
    n_tok = row_ref.shape[1]
    n_grp = n_tok // LANES
    lane = lax.broadcasted_iota(jnp.int32, (LANES, LANES), 1).astype(F32)
    sub = lax.broadcasted_iota(jnp.int32, (LANES, LANES), 0)
    row = lambda g: row_ref[:, g * LANES:(g + 1) * LANES].astype(F32)
    zero = jnp.zeros((LANES, LANES), F32)
    fold = lambda acc: jnp.sum(acc, axis=0, keepdims=True)
    cols = [column(row(c)) for c in range(n_grp)]
    firsts = []
    for g in range(n_grp):
        acc = zero
        for c in range(g + 1):
            same = cols[c] == row(g)
            if c == g:
                same = same & (sub < lane.astype(jnp.int32))
            acc = acc + jnp.where(same, 1.0, 0.0)
        firsts.append(column(jnp.where(fold(acc) == 0.0, 1.0, 0.0)))
    ranks = []
    for g in range(n_grp):
        acc = zero
        for c in range(n_grp):
            acc = acc + jnp.where(cols[c] < row(g), firsts[c], 0.0)
        ranks.append(fold(acc))
        meta[g:g + 1, :] = ranks[g].astype(jnp.int32)
    rank_cols = [column(r) for r in ranks]
    for g in range(n_grp):
        acc = zero
        for c in range(n_grp):
            acc = acc + jnp.where(rank_cols[c] == lane + g * LANES, firsts[c] * cols[c], 0.0)
        meta[n_grp + g:n_grp + g + 1, :] = fold(acc).astype(jnp.int32)
    cut = cut_ref[...].astype(F32)
    acc = zero
    for c in range(n_grp):
        acc = acc + jnp.where(cols[c] < cut, firsts[c], 0.0)
    meta[2 * n_grp:3 * n_grp, :] = jnp.broadcast_to(fold(acc), (n_grp, LANES)).astype(jnp.int32)


def logit_grad(e, n_t, shift, lab, first_id, inv_count, scale, dz):
    rows = e.shape[0]
    n_tok = n_t.shape[1]
    blk = 256
    vid = lax.broadcasted_iota(jnp.int32, (rows, blk), 0)
    for j in range(n_tok // blk):
        cols = slice(j * blk, (j + 1) * blk)
        z = (dot(e, n_t[:, cols]) * scale).astype(BF16).astype(F32)
        prob = jnp.exp2(z * LOG2E - shift[:, cols])
        dz[:, cols] = jnp.where(vid == lab[:, cols] - first_id, prob - inv_count, prob).astype(BF16)


def pipe_kernel(n_stage, plan, x0_hbm, emb_hbm, up_hbm, down_hbm, lab_hbm, row_hbm, cut_hbm,
                n_out, xs_out, hid_out, da_out, g_out, dx0_out, stat_out, loss_out, tmp_out, meta_out, nt_out,
                xbuf, ybuf, abuf, hbuf, nbuf, gbuf, dxbuf, dx0buf, dnbuf, up, down, up_t, down_t,
                emb, zbuf, n_t, dn_acc, dn_send, dn_recv, dn_own, st_send, st_recv, statall, lossall, tops, n_all_t, shift, dz, obuf, z_pair, meta, lab_ref, row_ref, cut_ref,
                w_sem, e_sem, x_sem, x_send, f_send, f_recv, n_send, n_recv, nf_send, ag_send, fw_send,
                st_sems, dp_sems, dn_ssem, dn_rsem, sa_sems, lo_sems, b_send, b_recv, d_send, d_recv, r_sems, out_sem, o_sem, od_send, od_recv, ic_send, in_sem):
    n_micro, seq, dim = gbuf.shape
    part = xbuf.shape[1]
    n_part = xbuf.shape[0]
    per = seq // part
    n_tok = n_micro * seq
    ffn = up.shape[1]
    vocab = emb_hbm.shape[0]
    me = lax.axis_index("stage")
    core = lax.rem(me, 2)
    chip = me // 2
    mate = me + 1 - 2 * core
    last_id = n_stage - 1
    first = me == 0
    last = me == last_id
    fblk = 512
    n_fblk = ffn // fblk
    base, extra, tile = plan.base, plan.extra, plan.head_tile
    row0 = core * base
    n_tiles = base // tile
    wide_tile = plan.grad_tile

    barrier = pltpu.get_barrier_semaphore()
    gives_x = (me >= 1) & (me + 2 < n_micro)

    def here(dev):
        pl.semaphore_signal(barrier, inc=1, device_id={"stage": dev}, device_id_type=MESH)

    pl.when(jnp.logical_not(first))(lambda: here(me - 1))
    pl.when(jnp.logical_not(last))(lambda: here(me + 1))

    @pl.when(first)
    def _():
        for dev in range(2, n_micro - 2):
            here(dev)

    w_copy = [pltpu.make_async_copy(up_hbm, up, w_sem.at[0]), pltpu.make_async_copy(down_hbm, down, w_sem.at[1])]
    for c in w_copy:
        c.start()
    in_copy = [pltpu.make_async_copy(src, dst, in_sem.at[k]) for k, (src, dst) in enumerate(((lab_hbm, lab_ref), (row_hbm, row_ref), (cut_hbm, cut_ref)))]
    x_slots = x0_hbm.shape[0]
    x_mine = [head_chunk(me, k, n_micro) for k in range(x_slots)]

    def x_rows(m):
        return xbuf.at[pl.ds(m * per, per)]

    def x_local(k):
        return pltpu.make_async_copy(x0_hbm.at[k], x_rows(k), x_sem.at[k])

    @pl.when(first)
    def _():
        for k in range(x_slots):
            x_local(k).start()

    for c in in_copy:
        c.start()

    e_parts = plan.e_parts
    e_step = base // e_parts

    def e_copy(i):
        src = emb_hbm.at[pl.ds(pl.multiple_of(row0 + i * e_step, 16), e_step)]
        return pltpu.make_async_copy(src, emb.at[pl.ds(i * e_step, e_step)], e_sem.at[0])

    e_more = pltpu.make_async_copy(emb_hbm.at[pl.ds(2 * base, extra)], emb.at[pl.ds(base, extra)], e_sem.at[1])
    with jax.named_scope("entry"):
        pl.semaphore_wait(barrier, jnp.where(first | last, 1, 2) + jnp.where(gives_x & (me >= 2), 1, 0))

    def x_copy(k):
        return remote(x0_hbm.at[k], x_rows(x_mine[k]), x_send.at[k], f_recv.at[x_mine[k]], 0)

    @pl.when(gives_x)
    def _():
        x_copy(0).start()

        @pl.when(me < 2)
        def _():
            x_copy(1).start()

    def table_start():
        for i in range(e_parts):
            e_copy(i).start()
        pl.when(core == 1)(e_more.start)

    def transpose_weights():
        for j in range(n_fblk):
            up_t[j * fblk:(j + 1) * fblk, :] = up[:, j * fblk:(j + 1) * fblk].T
            down_t[:, j * fblk:(j + 1) * fblk] = down[j * fblk:(j + 1) * fblk, :].T

    @pl.when(jnp.logical_not(first))
    def _():
        for c in w_copy:
            c.wait()
        table_start()

    def idle_work():
        transpose_weights()
        in_copy[1].wait()
        in_copy[2].wait()
        token_table(row_ref, jnp.where(core == 0, cut_ref[0:1, :], cut_ref[1:2, :]), meta)

    @pl.when(chip >= n_stage // 4)
    def _():
        idle_work()

    def n_start(m):
        remote(nbuf.at[m], nbuf.at[m], n_send, n_recv.at[m], jnp.where(m == last_id, last_id - 1, m)).start()

    def fwd(h, carry, cold=False):
        m = h // per
        sub = lax.rem(h, per)
        rows = pl.ds(pl.multiple_of(sub * part, part), part)
        with jax.named_scope("fwd_wait"):

            @pl.when(first & (sub == 0))
            def _():
                @pl.when(m < x_slots)
                def _():
                    x_local(m).wait()

                @pl.when(m >= x_slots)
                def _():
                    remote(x_rows(m), x_rows(m), x_send.at[0], f_recv.at[m], me).wait_recv()

            @pl.when(jnp.logical_not(first))
            def _():
                remote(xbuf.at[h], xbuf.at[h], f_send, f_recv.at[h], me).wait_recv()

        with jax.named_scope("fwd_comp"):
            x = xbuf[h]
            if cold:
                w_copy[0].wait()
            for j in range(n_fblk):
                cols = slice(j * fblk, (j + 1) * fblk)
                a = dot(x, up[:, cols]).astype(BF16)
                abuf[m, rows, cols] = a
                hbuf[m, rows, cols] = gelu_fwd(a.astype(F32)).astype(BF16)
            if cold:
                w_copy[1].wait()
                table_start()
            y = (x.astype(F32) + dot(hbuf[m, rows, :], down[...])).astype(BF16)
            ybuf[h] = y

        @pl.when(jnp.logical_not(last))
        def _():
            remote(ybuf.at[h], xbuf.at[h], f_send, f_recv.at[h], me + 1).start()

        @pl.when(last)
        def _():
            yf = y.astype(F32)
            inv = lax.rsqrt(jnp.mean(yf * yf, axis=-1, keepdims=True) + EPS)
            nbuf[m, rows, :] = (yf * inv).astype(BF16)
            pl.when(sub == per - 1)(lambda: n_start(m))

        @pl.when(sub == per - 1)
        def _():
            pltpu.make_async_copy(hbuf.at[m], hid_out.at[m], out_sem.at[0]).start()
            pltpu.make_async_copy(x_rows(m), xs_out.at[pl.ds(m * per, per)], out_sem.at[1]).start()

        return carry

    pl.when(first)(lambda: (fwd(0, 0, cold=True), None)[1])
    lax.fori_loop(jnp.where(first, 1, 0), n_part, fwd, 0)

    @pl.when(chip < n_stage // 4)
    def _():
        idle_work()

    n_forward = remote(nbuf.at[me], nbuf.at[me], nf_send, n_recv.at[me], mate)
    with jax.named_scope("n_wait"):

        @pl.when(jnp.logical_not(last))
        def _():
            remote(nbuf.at[me], nbuf.at[me], n_send, n_recv.at[me], me).wait_recv()
            pl.when(mate != last_id)(n_forward.start)
            remote(nbuf.at[mate], nbuf.at[mate], n_send, n_recv.at[mate], me).wait_recv()

        for k in range(2):
            n_t[:, k * seq:(k + 1) * seq] = nbuf[2 * chip + k].T

    peers = [lax.rem(me + 2 * d, n_stage) for d in range(1, n_stage // 2)]
    ag_copies = [remote(nbuf.at[me], nbuf.at[me], ag_send.at[d], n_recv.at[me], p) for d, p in enumerate(peers)]
    for c, p in zip(ag_copies, peers):
        pl.when(p != last_id)(c.start)
    with jax.named_scope("e_wait"):
        pltpu.make_async_copy(emb_hbm.at[pl.ds(0, base)], emb.at[pl.ds(0, base)], e_sem.at[0]).wait()
        pl.when(core == 1)(e_more.wait)

    pair = 2 * seq
    scale = dim ** -0.5
    inv_count = 1.0 / n_tok
    log_count = math.log2(n_tok)
    in_copy[0].wait()
    lab = lab_ref[:, pl.ds(pl.multiple_of(chip * pair, pair), pair)]

    def logits(rows, size):
        e = emb[rows, :]
        parts = [dot(e[k * size // 2:(k + 1) * size // 2], n_t[...]) for k in range(2)]
        z = jnp.concatenate([(p * scale).astype(BF16) for p in parts], axis=0)
        zbuf[rows, :] = z
        return z

    def peak(z, size, top):
        best = jnp.max(z.reshape(size // 16, 16, pair), axis=0).astype(F32)
        return jnp.maximum(top, jnp.maximum(best[:8], best[8:]))

    def total(z, size, old, top, tot):
        off = top * LOG2E
        return tot * jnp.exp2(old * LOG2E - off) + jnp.sum(jnp.exp2(z.astype(F32).reshape(size // 8, 8, pair) * LOG2E - off[None]), axis=0)

    tops[0] = jnp.full((8, pair), -jnp.inf, F32)
    tops[1] = jnp.zeros((8, pair), F32)

    @pl.when(core == 1)
    def _():
        z = logits(pl.ds(base, extra), extra)
        top = peak(z, extra, tops[0])
        tops[1] = total(z, extra, tops[0], top, tops[1])
        tops[0] = top

    def logits_step(i, slot, old, top, tot):
        z = logits(pl.ds(pl.multiple_of(i * tile, 16), tile), tile)
        tot = total(z_pair[1 - slot], tile, old, top, tot)
        z_pair[slot] = z
        return top, peak(z, tile, top), tot

    with jax.named_scope("logits"):
        z = logits(pl.ds(0, tile), tile)
        z_pair[0] = z
        state = (tops[0], peak(z, tile, tops[0]), tops[1])
        state = lax.fori_loop(0, (n_tiles - 1) // 2, lambda i, c: logits_step(2 * i + 2, 0, *logits_step(2 * i + 1, 1, *c)), state)
        if n_tiles % 2 == 0:
            state = logits_step(n_tiles - 1, 1, *state)
        old, top, tot = state
        tot = total(z_pair[(n_tiles - 1) % 2], tile, old, top, tot)
    row_top = jnp.max(top, axis=0, keepdims=True)
    row_tot = jnp.sum(tot * jnp.exp2((top - row_top) * LOG2E), axis=0, keepdims=True)
    st_send[0:8, :] = jnp.broadcast_to(row_top, (8, pair))
    st_send[8:16, :] = jnp.broadcast_to(row_tot, (8, pair))
    st_copy = remote(st_send, st_recv, st_sems.at[0], st_sems.at[1], mate)
    with jax.named_scope("stat_x"):
        st_copy.start()
        for p in peers:
            got = remote(nbuf.at[p], nbuf.at[p], ag_send.at[0], n_recv.at[p], me)
            pl.when(jnp.logical_not(last))(got.wait_recv)
            pl.when(mate != last_id)(remote(nbuf.at[p], nbuf.at[p], fw_send, n_recv.at[p], mate).start)
        st_copy.wait()
    far_top = st_recv[0:1, :]
    far_tot = st_recv[8:9, :]
    all_top = jnp.maximum(row_top, far_top)
    mine = row_tot * jnp.exp(row_top - all_top)
    other = far_tot * jnp.exp(far_top - all_top)
    lse = all_top + jnp.log(jnp.where(core == 0, mine + other, other + mine))
    my_shift = lse * LOG2E + log_count
    others = [lax.rem(me + d, n_stage) for d in range(1, n_stage)]

    def spread(buf, sems):
        whole = buf.at[pl.ds(0, n_stage - 1)]
        return [remote(buf.at[me], buf.at[me], sems.at[0], sems.at[1], p) for p in others], remote(whole, whole, sems.at[0], sems.at[1], me)

    statall[me] = jnp.broadcast_to(lse, (8, pair))
    sa_copies, sa_all = spread(statall, sa_sems)
    for c in sa_copies:
        c.start()

    def grads(rows, size, first_row, picked):
        zf = zbuf[rows, :].astype(F32)
        prob = jnp.exp2(zf * LOG2E - my_shift)
        hit = lax.broadcasted_iota(jnp.int32, (size, pair), 0) == lab - (row0 + first_row)
        dz_t = jnp.where(hit, prob - inv_count, prob).astype(BF16)
        got = jnp.where(hit, zf, 0.0).reshape(size // 8, 8, pair)
        return dot_t(dz_t, emb[rows, :]), picked + jnp.sum(got, axis=0)

    tops[0] = jnp.zeros((8, pair), F32)
    dn_acc[...] = jnp.zeros_like(dn_acc)

    @pl.when(core == 1)
    def _():
        dn_acc[...], tops[0] = grads(pl.ds(base, extra), extra, base, tops[0])

    def grad_step(i, picked):
        part, picked = grads(pl.ds(pl.multiple_of(i * wide_tile, 16), wide_tile), wide_tile, i * wide_tile, picked)
        dn_acc[...] += part
        return picked

    with jax.named_scope("grads"):
        picked = lax.fori_loop(0, base // wide_tile, grad_step, tops[0])
    far = pl.ds(pl.multiple_of((1 - core) * seq, seq), seq)
    near = pl.ds(pl.multiple_of(core * seq, seq), seq)
    dn_send[...] = dn_acc[far, :]
    dp_copy = remote(dn_send, dn_recv, dp_sems.at[0], dp_sems.at[1], mate)
    dp_copy.start()
    row_loss = jnp.where(core == 0, lse, 0.0) - jnp.sum(picked, axis=0, keepdims=True)
    lossall[me] = jnp.broadcast_to(row_loss, (8, pair))
    lo_copies, lo_all = spread(lossall, lo_sems)
    for c in lo_copies:
        c.start()
    with jax.named_scope("dn_x"):
        for d in range(1, n_stage // 2):
            src = lax.rem(mate + 2 * d, n_stage)
            pl.when(jnp.logical_not(last))(remote(nbuf.at[src], nbuf.at[src], ag_send.at[0], n_recv.at[src], me).wait_recv)
        for m in range(n_micro):
            n_all_t[:, m * seq:(m + 1) * seq] = nbuf[m].T
        nt_copy = pltpu.make_async_copy(n_all_t, nt_out, out_sem.at[9])
        nt_copy.start()
        dp_copy.wait()
        dn = ((dn_acc[near, :] + dn_recv[...]) * scale).astype(BF16)
    dn_copy = remote(dn_own, dnbuf.at[me], dn_ssem, dn_rsem.at[me], last_id)

    @pl.when(last)
    def _():
        dnbuf[last_id] = dn

    @pl.when(jnp.logical_not(last))
    def _():
        dn_own[...] = dn
        remote(dn_own, dnbuf.at[me], dn_ssem, dn_rsem.at[me], last_id).start()

    near_dst = [1, 3, last_id]
    far_dst = n_stage // 2 + 1
    direct = n_micro - 2
    by_prev = n_micro - 3
    hands_on = (core == 1) & (me != 1)

    def dx0_start(m, k, dev):
        remote(dxbuf.at[m], dx0buf.at[m], d_send.at[k], d_recv.at[m], dev).start()

    def relayed(m):
        return (m < direct) & (((me == 3) & (m != by_prev)) | (last & (m == by_prev)))

    def relay_far(m):
        remote(dx0buf.at[m], dx0buf.at[m], r_sems.at[1], d_recv.at[m], far_dst).start()

    def bwd(m):
        with jax.named_scope("bwd_wait"):
            @pl.when(jnp.logical_not(last))
            def _():
                remote(gbuf.at[m], gbuf.at[m], b_send, b_recv.at[m], me).wait_recv()

            @pl.when(last)
            def _():
                @pl.when(m != last_id)
                def _():
                    remote(dnbuf.at[m], dnbuf.at[m], dn_ssem, dn_rsem.at[m], me).wait_recv()

                yf = ybuf[pl.ds(m * per, per)].reshape(seq, dim).astype(F32)
                inv = lax.rsqrt(jnp.mean(yf * yf, axis=-1, keepdims=True) + EPS)
                dnf = dnbuf[m].astype(F32)
                proj = jnp.mean(yf * dnf, axis=-1, keepdims=True)
                gbuf[m] = (dnf * inv - yf * (inv * inv * inv * proj)).astype(BF16)

        with jax.named_scope("bwd_comp"):
            g = gbuf[m]
            for j in range(n_fblk):
                cols = slice(j * fblk, (j + 1) * fblk)
                dh = dot(g, down_t[:, cols]).astype(BF16).astype(F32)
                abuf[m, :, cols] = (dh * gelu_slope(abuf[m, :, cols].astype(F32))).astype(BF16)
            dxbuf[m] = (g.astype(F32) + dot(abuf[m], up_t[...])).astype(BF16)

        @pl.when(jnp.logical_not(first))
        def _():
            remote(dxbuf.at[m], gbuf.at[m], b_send, b_recv.at[m], me - 1).start()

        @pl.when(first)
        def _():
            pl.when(m >= direct)(lambda: dx0_start(m, len(near_dst), far_dst))
            for k, dev in enumerate(near_dst):
                dx0_start(m, k, dev)

        pltpu.make_async_copy(abuf.at[m], da_out.at[m], out_sem.at[2]).start()
        pltpu.make_async_copy(gbuf.at[m], g_out.at[m], out_sem.at[3]).start()

    n_slot = obuf.shape[0]
    busy = chip == last_id // 2
    far_tile = remote(tmp_out.at[core, pl.ds(0, plan.rows)], tmp_out.at[core, pl.ds(0, plan.rows)], ic_send, od_recv, jnp.where(first, last_id, last_id - 1))
    sends_far = first | (me == last_id - 2)

    def tile_copy(k):
        rows = pl.ds(pl.multiple_of(k * plan.rows, plan.rows), plan.rows)
        slot = lax.rem(k, n_slot)
        return pltpu.make_async_copy(obuf.at[slot], tmp_out.at[core, rows], o_sem.at[slot])

    def piece(p):
        k = p // plan.per_tile
        rows = pl.ds(pl.multiple_of(p * plan.piece, plan.piece), plan.piece)
        here = pl.ds(pl.multiple_of(lax.rem(p, plan.per_tile) * plan.piece, plan.piece), plan.piece)
        return remote(obuf.at[lax.rem(k, n_slot), here], tmp_out.at[core, rows], od_send.at[k], od_recv, mate)

    def tile_sent(k):
        slot = lax.rem(k, n_slot)
        return remote(obuf.at[slot], tmp_out.at[core, pl.ds(0, plan.rows)], od_send.at[k], od_recv, mate)

    def emb_tile(k):
        with jax.named_scope("tile_prep"):

            @pl.when(k == 0)
            def _():
                sa_all.wait_recv()
                for c in range(n_stage // 2):
                    shift[:, c * pair:(c + 1) * pair] = statall[2 * c, 0:1, :] * LOG2E + log_count

        slot = lax.rem(k, n_slot)
        with jax.named_scope("tile_wait"):
            @pl.when(k == 2)
            def _():
                tile_copy(0).wait()
                pl.when(sends_far)(far_tile.start)

            pl.when(k > n_slot)(lambda: tile_copy(k - n_slot).wait())
            pl.when((k >= n_slot) & (k - n_slot < plan.shared) & jnp.logical_not(busy & (k == n_slot)))(lambda: tile_sent(k - n_slot).wait_send())

        with jax.named_scope("tile"):
            rows = pl.ds(pl.multiple_of(k * plan.rows, plan.rows), plan.rows)
            logit_grad(emb[rows, :], n_all_t, shift, lab_ref, row0 + k * plan.rows, inv_count, scale, dz)
            obuf[slot] = dot(dz[...], nbuf[...].reshape(n_tok, dim)) * scale

        tile_copy(k).start()

    def send_pieces(done, until):
        lax.fori_loop(done, until, lambda p, c: (piece(p).start(), c)[1], 0)

    def send_tiles(done, until):
        def one(k, carry):
            rows = pl.ds(pl.multiple_of(k * plan.rows, plan.rows), plan.rows)
            remote(obuf.at[lax.rem(k, n_slot)], tmp_out.at[core, rows], od_send.at[k], od_recv, mate).start()
            return carry

        lax.fori_loop(done, until, one, 0)

    before = sum(jnp.where(me == s, plan.before[s], 0) for s in range(n_stage))

    def pass_dx0(m, carry):
        @pl.when(jnp.logical_not(first))
        def _():
            remote(dx0buf.at[m], dx0buf.at[m], r_sems.at[0], d_recv.at[m], me).wait_recv()

            @pl.when(hands_on)
            def _():
                remote(dx0buf.at[m], dx0buf.at[m], r_sems.at[0], d_recv.at[m], mate).start()

            @pl.when(relayed(m))
            def _():
                relay_far(m)

            pltpu.make_async_copy(dx0buf.at[m], dx0_out.at[m], out_sem.at[4]).start()

        @pl.when(first)
        def _():
            pltpu.make_async_copy(dxbuf.at[m], dx0_out.at[m], out_sem.at[4]).start()

        return carry

    lead = jnp.where(me == 3, -300, jnp.where(last, -1800, jnp.where(me == far_dst, -1600, -10**6)))

    def work(i, carry):
        sent, passed = carry
        chunk = (i >= before) & (i < before + n_micro)
        pl.when(chunk)(lambda: bwd(i - before))
        k = jnp.where(i < before, i, i - n_micro)
        pl.when(jnp.logical_not(chunk))(lambda: emb_tile(k))
        after = i - before - n_micro + 1
        here = jnp.where(after > 0, jnp.clip((after * 264 + lead) // 138, 0, n_micro), 0)
        lax.fori_loop(passed, here, pass_dx0, 0)
        ready = jnp.where(i < before, i + 1, jnp.where(chunk, before, i + 1 - n_micro))
        near_chunks = chunk | ((i < before) & (i + jnp.where(before >= 6, 2, 1) >= before))
        whole = (sent + plan.per_tile - 1) // plan.per_tile
        upto = jnp.minimum(jnp.minimum(ready, plan.shared), whole + 1)
        some = jnp.where(near_chunks, jnp.minimum(sent + 1, jnp.minimum(ready, plan.shared) * plan.per_tile), whole * plan.per_tile)
        send_pieces(sent, some)
        send_tiles(whole, jnp.where(near_chunks, 0, upto))
        now = jnp.where(near_chunks, some, jnp.maximum(some, upto * plan.per_tile))
        return jnp.maximum(sent, now), jnp.maximum(passed, here)

    sent, passed = lax.fori_loop(0, plan.tiles + n_micro, work, (jnp.where(busy, plan.per_tile, 0), 0))
    outs = [pltpu.make_async_copy(nbuf, n_out, out_sem.at[5]), pltpu.make_async_copy(lossall, loss_out, out_sem.at[6]), pltpu.make_async_copy(meta, meta_out, out_sem.at[7])]
    lo_all.wait_recv()
    for c in outs:
        c.start()
    pltpu.make_async_copy(statall, stat_out, out_sem.at[8]).start()
    with jax.named_scope("relay_all"):
        lax.fori_loop(passed, n_micro, pass_dx0, 0)

    with jax.named_scope("drain"):
        send_pieces(sent, plan.shared * plan.per_tile)
        for k in range(max(plan.tiles - n_slot, 0), plan.tiles):
            tile_copy(k).wait()
            if k < plan.shared:
                tile_sent(k).wait_send()
        pl.when(sends_far)(far_tile.wait_send)
        all_rows = pl.ds(0, plan.shared * plan.rows)
        remote(tmp_out.at[1 - core, all_rows], tmp_out.at[1 - core, all_rows], od_send.at[0], od_recv, me).wait_recv()
        sa_all.wait_send()
        lo_all.wait_send()
        pltpu.make_async_copy(statall, stat_out, out_sem.at[8]).wait()
        for c, p in zip(ag_copies, peers):
            pl.when(p != last_id)(c.wait_send)

        @pl.when(jnp.logical_not(last))
        def _():
            dn_copy.wait_send()
            pl.when(mate != last_id)(n_forward.wait_send)
            remote(ybuf, xbuf, f_send, f_recv.at[0], me + 1).wait_send()

        @pl.when(last)
        def _():
            remote(nbuf, nbuf, n_send, n_recv.at[0], me).wait_send()

        @pl.when(mate != last_id)
        def _():
            some = nbuf.at[pl.ds(0, len(peers))]
            remote(some, some, fw_send, n_recv.at[0], mate).wait_send()

        @pl.when(gives_x)
        def _():
            x_copy(0).wait_send()

            @pl.when(me < 2)
            def _():
                x_copy(1).wait_send()

        @pl.when(jnp.logical_not(first))
        def _():
            remote(dxbuf, gbuf, b_send, b_recv.at[0], me).wait_send()
            pl.when(hands_on)(remote(dx0buf, dx0buf, r_sems.at[0], d_recv.at[0], mate).wait_send)

        @pl.when(first)
        def _():
            for k in range(len(near_dst)):
                remote(dxbuf, dx0buf, d_send.at[k], d_recv.at[0], me).wait_send()
            rest = pl.ds(0, n_micro - direct)
            remote(dxbuf.at[rest], dx0buf.at[rest], d_send.at[len(near_dst)], d_recv.at[0], me).wait_send()

        for dev, kept in ((3, direct - 1), (last_id, 1)):
            some = dx0buf.at[pl.ds(0, kept)]
            pl.when(me == dev)(remote(some, some, r_sems.at[1], d_recv.at[0], me).wait_send)

        pltpu.make_async_copy(hbuf, hid_out, out_sem.at[0]).wait()
        pltpu.make_async_copy(xbuf, xs_out, out_sem.at[1]).wait()
        pltpu.make_async_copy(abuf, da_out, out_sem.at[2]).wait()
        pltpu.make_async_copy(gbuf, g_out, out_sem.at[3]).wait()
        pltpu.make_async_copy(dx0buf, dx0_out, out_sem.at[4]).wait()
        nt_copy.wait()
        for c in outs:
            c.wait()


class Plan:
    def __init__(self, vocab, n_stage):
        units = vocab // LANES
        self.base = units // 2 * LANES
        self.extra = vocab - 2 * self.base
        self.head_tile = next(t for t in (1600, 1536, 1280, 1024, 768, 640, 512, 256, 128) if self.base % t == 0)
        self.rows = 1024
        self.tiles, self.shared = 11, 9
        self.grad_tile = next(t for t in (4000, 3200, 1600, 1280, 640, 256, 128) if self.base % t == 0)
        self.e_parts = next(k for k in (10, 8, 5, 4, 2, 1) if self.base % (16 * k) == 0)
        self.part = 128
        self.slots = 4
        self.piece = 256
        self.per_tile = self.rows // self.piece
        measured = [10, 9, 6, 5, 3, 2, 0, 0]
        self.before = (measured + [0] * n_stage)[:n_stage]
        mid = self.base
        ends = [(0, mid), (mid, vocab)]
        early = (self.tiles * self.rows, self.shared * self.rows)
        self.spans = [[(ends[h][0] + early[0 if h == c else 1], ends[h][1]) for h in (c, 1 - c)] for c in range(2)]
        self.longest = [max(self.spans[c][k][1] - self.spans[c][k][0] for c in range(2)) for k in range(2)]
        best = min(range(16, 1281, 16), key=lambda r: (sum(-(-n // r) for n in self.longest)) * (r + 40))
        self.calc_rows = best
        self.calc_steps = [-(-n // best) for n in self.longest]
        self.steps = sum(self.calc_steps)
        self.copy_rows = self.rows
        self.copies = self.tiles + self.shared
        self.starts = ends

    def calc_start(self, core, s):
        k = 0 if s < self.calc_steps[0] else 1
        lo, hi = self.spans[core][k]
        return min(lo + (s - k * self.calc_steps[0]) * self.calc_rows, hi - self.calc_rows)

    def copy_start(self, core, c):
        own = c < self.tiles
        h = core if own else 1 - core
        return self.starts[h][0] + (c if own else c - self.tiles) * self.copy_rows

    def cuts(self, core):
        firsts = [(self.calc_start(core, s), self.calc_rows) for s in range(self.steps)] + [(self.copy_start(core, c), self.copy_rows) for c in range(self.copies)]
        flat = [v for lo, rows in firsts for v in (lo, lo + rows)]
        return flat + [0] * (LANES - len(flat))


def run_pipe(x0, emb, w_up, w_down, labels, tokens, cuts, n_stage, plan):
    n_micro, seq = labels.shape
    dim, ffn = w_up.shape
    n_tok = n_micro * seq
    base = plan.base
    any_spec = pl.BlockSpec(memory_space=pl.ANY)
    act = (n_micro, seq, dim)
    fine = (n_tok // plan.part, plan.part, dim)
    wide = (n_micro, seq, ffn)
    dma = pltpu.SemaphoreType.DMA
    vm = pltpu.VMEM
    pair = 2 * seq
    return pl.pallas_call(
        functools.partial(pipe_kernel, n_stage, plan),
        out_shape=[
            jax.ShapeDtypeStruct(act, BF16), jax.ShapeDtypeStruct(fine, BF16), jax.ShapeDtypeStruct(wide, BF16),
            jax.ShapeDtypeStruct(wide, BF16), jax.ShapeDtypeStruct(act, BF16), jax.ShapeDtypeStruct(act, BF16),
            jax.ShapeDtypeStruct((n_stage, 8, pair), F32), jax.ShapeDtypeStruct((n_stage, 8, pair), F32), jax.ShapeDtypeStruct((2, plan.tiles * plan.rows, dim), F32),
            jax.ShapeDtypeStruct((3 * n_tok // LANES, LANES), jnp.int32), jax.ShapeDtypeStruct((dim, n_tok), BF16),
        ],
        in_specs=[any_spec] * 7,
        out_specs=[any_spec] * 11,
        scratch_shapes=[
            vm(fine, BF16), vm(fine, BF16), vm(wide, BF16), vm(wide, BF16), vm(act, BF16), vm(act, BF16), vm(act, BF16), vm(act, BF16), vm(act, BF16),
            vm((dim, ffn), BF16), vm((ffn, dim), BF16), vm((ffn, dim), BF16), vm((dim, ffn), BF16),
            vm((base + plan.extra, dim), BF16), vm((base + plan.extra, pair), BF16), vm((dim, pair), BF16), vm((pair, dim), F32),
            vm((seq, dim), F32), vm((seq, dim), F32), vm((seq, dim), BF16), vm((16, pair), F32), vm((16, pair), F32), vm((n_stage, 8, pair), F32), vm((n_stage, 8, pair), F32),
            vm((2, 8, pair), F32), vm((dim, n_tok), BF16), vm((1, n_tok), F32), vm((plan.rows, n_tok), BF16), vm((plan.slots, plan.rows, dim), F32),
            vm((2, plan.head_tile, pair), BF16), vm((3 * n_tok // LANES, LANES), jnp.int32),
            vm((1, n_tok), jnp.int32), vm((1, n_tok), jnp.int32), vm((2, LANES), jnp.int32),
            dma((2,)), dma((2,)), dma((2,)), dma((2,)), dma, dma((n_tok // plan.part,)), dma, dma((n_micro,)), dma,
            dma((n_stage // 2,)), dma,
            dma((2,)), dma((2,)), dma, dma((n_stage,)), dma((2,)), dma((2,)), dma, dma((n_micro,)), dma((4,)), dma((n_micro,)), dma((2,)), dma((10,)),
            dma((plan.slots,)), dma((plan.shared,)), dma, dma, dma((3,)),
        ],
        compiler_params=pltpu.CompilerParams(collective_id=0, has_side_effects=True, vmem_limit_bytes=67_000_000),
        cost_estimate=pl.CostEstimate(flops=60 * 10**9, bytes_accessed=100 * 10**6, transcendentals=0),
        name="pipe",
    )(x0.reshape(x0.shape[0], seq // plan.part, plan.part, dim), emb, w_up, w_down, labels.reshape(1, n_tok), tokens.reshape(1, n_tok), cuts)


def fin_kernel(n_stage, n_tok, plan, ids_hbm, emb_hbm, tmp_hbm, n_hbm, nt_hbm, stat_hbm, part_hbm, lab_hbm, meta_hbm, dx0_hbm, xs_hbm, hid_hbm, da_hbm, g_hbm,
               out_hbm, loss_ref, gup_hbm, gdown_hbm,
               n_all, dx0, xs, hid, da, g, n_t, x_t, dx0s, dz, shift, e_in, c_out, cp, gup, gdown,
               ld_sem, e_sem, t_sem, co_sem, po_sem, gu_sem, gd_sem, wi_sem, ids_ref, stat_ref, part_ref, lab_ref, meta_ref, in_sem):
    dim, ffn = gup_hbm.shape
    scale = dim ** -0.5
    inv_count = 1.0 / n_tok
    steps, crows, prows = plan.steps, plan.calc_rows, plan.copy_rows
    core = lax.rem(lax.axis_index("stage"), 2)
    early = plan.tiles * prows
    wblk = gup.shape[2]
    n_wblk = ffn // wblk
    turn = plan.calc_steps[0]

    def pick(pair):
        return jnp.where(core == 0, pair[0], pair[1])

    def calc_start(s):
        own = s < turn
        lo, hi = [jnp.where(own, pick([plan.spans[c][0][e] for c in range(2)]), pick([plan.spans[c][1][e] for c in range(2)])) for e in range(2)]
        return pl.multiple_of(jnp.minimum(lo + (s - jnp.where(own, 0, turn)) * crows, hi - crows), 16)

    def copy_start(c):
        own = c < plan.tiles
        first = jnp.where(own, pick([plan.starts[0][0], plan.starts[1][0]]), pick([plan.starts[1][0], plan.starts[0][0]]))
        return pl.multiple_of(first + (c - jnp.where(own, 0, plan.tiles)) * prows, 16)

    def e_copy(s):
        return pltpu.make_async_copy(emb_hbm.at[pl.ds(calc_start(s), crows)], e_in.at[lax.rem(s, 3)], e_sem.at[lax.rem(s, 3)])

    n_slot = cp.shape[0]
    ahead = 8

    def t_copy(c):
        own = c < plan.tiles
        row = jnp.where(own, core, 1 - core) * early + (c - jnp.where(own, 0, plan.tiles)) * prows
        slot = lax.rem(c, n_slot)
        return pltpu.make_async_copy(tmp_hbm.at[pl.ds(pl.multiple_of(row, 16), prows)], cp.at[slot], t_sem.at[slot])

    def p_out(c):
        slot = lax.rem(c, n_slot)
        return pltpu.make_async_copy(cp.at[slot], out_hbm.at[pl.ds(copy_start(c), prows)], po_sem.at[slot])

    def c_outs(s):
        slot = lax.rem(s, 2)
        return pltpu.make_async_copy(c_out.at[slot], out_hbm.at[pl.ds(calc_start(s), crows)], co_sem.at[slot])

    loads = [pltpu.make_async_copy(s, d, ld_sem.at[i]) for i, (s, d) in enumerate(((n_hbm, n_all), (dx0_hbm, dx0), (xs_hbm, xs), (g_hbm, g)))]
    ins = [pltpu.make_async_copy(s, d, in_sem.at[i]) for i, (s, d) in enumerate(((stat_hbm, stat_ref), (lab_hbm, lab_ref), (part_hbm, part_ref), (meta_hbm, meta_ref), (ids_hbm, ids_ref)))]
    nt_load = pltpu.make_async_copy(nt_hbm, n_t, in_sem.at[5])
    nt_load.start()
    ins[0].start()
    ins[1].start()
    e_copy(0).start()
    loads[0].start()
    loads[1].start()
    for c in ins[2:]:
        c.start()
    e_copy(1).start()
    for c in range(ahead):
        t_copy(c).start(priority=1)
    pair = stat_ref.shape[2]
    with jax.named_scope("fin_pre"):
        ins[0].wait()
        ins[1].wait()
        for c in range(n_stage // 2):
            shift[:, c * pair:(c + 1) * pair] = stat_ref[2 * c, 0:1, :] * LOG2E + math.log2(n_tok)
        nt_load.wait()
        loads[0].wait()

    def sum_rows():
        for c in ins[2:]:
            c.wait()
        loss_ref[0] = jnp.sum(sum(part_ref[d, 0:1, :] for d in range(n_stage))) * inv_count
        loads[1].wait()
        dense = jnp.concatenate([meta_ref[g:g + 1, :] for g in range(n_tok // LANES)], axis=1)
        order = lax.broadcasted_iota(jnp.int32, (n_tok, n_tok), 0) == dense
        dx0s[...] = dot(jnp.where(order, 1.0, 0.0).astype(BF16), dx0[...])

    def add_rows(k, start, ref):
        lo, hi = ids_ref[2 * n_tok + k], ids_ref[2 * n_tok + k + 1]
        wide = 8

        def some(p, width):
            at = [pl.ds(ids_ref[n_tok + p + u] - start, 1) for u in range(width)]
            new = [ref[at[u], :] + dx0s[pl.ds(p + u, 1), :] for u in range(width)]
            for u in range(width):
                ref[at[u], :] = new[u]

        def group(g, carry):
            some(lo + g * wide, wide)
            return carry

        def single(p, carry):
            some(p, 1)
            return carry

        n_grp = (hi - lo) // wide
        lax.fori_loop(0, n_grp, group, 0)
        lax.fori_loop(lo + n_grp * wide, hi, single, 0)

    def w_ins(w):
        cols = pl.ds(pl.multiple_of(w * wblk, wblk), wblk)
        wslot = lax.rem(w, 2)
        return (pltpu.make_async_copy(da_hbm.at[:, cols], da.at[wslot], wi_sem.at[0, wslot]), pltpu.make_async_copy(hid_hbm.at[:, cols], hid.at[wslot], wi_sem.at[1, wslot]))

    def w_outs(w):
        cols = pl.ds(pl.multiple_of(w * wblk, wblk), wblk)
        wslot = lax.rem(w, 2)
        return (pltpu.make_async_copy(gup.at[wslot], gup_hbm.at[:, cols], gu_sem.at[wslot]), pltpu.make_async_copy(gdown.at[wslot], gdown_hbm.at[cols], gd_sem.at[wslot]))

    def copy_tile(c, carry):
        with jax.named_scope("copy_wait"):
            t_copy(c).wait()
        with jax.named_scope("add_p"):
            add_rows(2 * steps + 2 * c, copy_start(c), cp.at[lax.rem(c, n_slot)])
        p_out(c).start()

        @pl.when(c + ahead < plan.copies)
        def _():
            pl.when(c + ahead >= n_slot)(lambda: p_out(c + ahead - n_slot).wait())
            t_copy(c + ahead).start(priority=1)

        return carry

    w_first = 2
    tails = [turn - 1, steps - 1]

    def tail(s):
        return (s == tails[0]) | (s == tails[1])

    def step(s, carry):
        pl.when(s + 2 < steps)(lambda: e_copy(s + 2).start())
        with jax.named_scope("fin_wait"):
            e_copy(s).wait()

        @pl.when(s == 0)
        def _():
            for c in loads[2:]:
                c.start()

        w = s - w_first

        @pl.when((w + 1 >= 0) & (w + 1 < n_wblk))
        def _():
            for c in w_ins(w + 1):
                c.start()

        pl.when((s >= 2) & jnp.logical_not(tail(s - 1)))(lambda: c_outs(s - 2).wait())
        slot = lax.rem(s, 2)
        start = calc_start(s)
        with jax.named_scope("calc"):
            logit_grad(e_in[lax.rem(s, 3)], n_t, shift, lab_ref, start, inv_count, scale, dz)
            c_out[slot] = dot(dz[...], n_all[...]) * scale
        pl.when(s == 0)(sum_rows)
        with jax.named_scope("add_c"):
            add_rows(2 * s, start, c_out.at[slot])
        pl.when(tail(s))(lambda: c_outs(s - 1).wait())
        c_outs(s).start()
        lax.fori_loop(s * plan.copies // (steps - 1), jnp.minimum((s + 1) * plan.copies // (steps - 1), plan.copies), copy_tile, 0)

        @pl.when(w == 0)
        def _():
            for c in loads[2:]:
                c.wait()
            x_t[...] = xs[...].T

        @pl.when((w >= 0) & (w < n_wblk))
        def _():
            wslot = lax.rem(w, 2)
            with jax.named_scope("dw_wait"):
                for c in w_ins(w):
                    c.wait()

                @pl.when(w >= 2)
                def _():
                    for c in w_outs(w - 2):
                        c.wait()

            with jax.named_scope("dw"):
                gup[wslot] = dot(x_t[...], da[wslot])
                gdown[wslot] = dot_t(hid[wslot], g[...])
            for c in w_outs(w):
                c.start()

        return carry

    lax.fori_loop(0, steps, step, 0)
    with jax.named_scope("fin_drain"):
        for w in range(n_wblk - 2, n_wblk):
            for c in w_outs(w):
                c.wait()
        c_outs(steps - 1).wait()
        for c in range(plan.copies - n_slot, plan.copies):
            p_out(c).wait()


def run_fin(emb, tmp, n_all, n_all_t, stats, losses, labels, meta, dx0, xs, hid, da, g, n_stage, plan):
    vocab, dim = emb.shape
    n_tok, ffn = hid.shape
    vm = pltpu.VMEM
    dma = pltpu.SemaphoreType.DMA
    any_spec = pl.BlockSpec(memory_space=pl.ANY)
    smem = pl.BlockSpec(memory_space=pltpu.SMEM)
    wblk = 512
    return pl.pallas_call(
        functools.partial(fin_kernel, n_stage, n_tok, plan),
        out_shape=[jax.ShapeDtypeStruct((vocab, dim), F32), jax.ShapeDtypeStruct((1,), F32), jax.ShapeDtypeStruct((dim, ffn), F32), jax.ShapeDtypeStruct((ffn, dim), F32)],
        in_specs=[any_spec] * 14,
        out_specs=[any_spec, smem, any_spec, any_spec],
        scratch_shapes=[
            vm((n_tok, dim), BF16), vm((n_tok, dim), BF16), vm((n_tok, dim), BF16), vm((2, n_tok, wblk), BF16), vm((2, n_tok, wblk), BF16), vm((n_tok, dim), BF16),
            vm((dim, n_tok), BF16), vm((dim, n_tok), BF16), vm((n_tok, dim), F32), vm((plan.calc_rows, n_tok), BF16), vm((1, n_tok), F32),
            vm((3, plan.calc_rows, dim), BF16), vm((2, plan.calc_rows, dim), F32), vm((11, plan.copy_rows, dim), F32),
            vm((2, dim, wblk), F32), vm((2, wblk, dim), F32),
            dma((4,)), dma((3,)), dma((11,)), dma((2,)), dma((11,)), dma((2,)), dma((2,)), dma((2, 2)),
            pltpu.SMEM((meta.size,), jnp.int32), vm(stats.shape, F32), vm(losses.shape, F32), vm((1, n_tok), jnp.int32), vm(meta.shape, jnp.int32), dma((6,)),
        ],
        compiler_params=pltpu.CompilerParams(vmem_limit_bytes=67_000_000),
        cost_estimate=pl.CostEstimate(flops=2 * n_tok * vocab * dim, bytes_accessed=5 * vocab * dim, transcendentals=0),
        name="fin",
    )(meta.reshape(-1), emb, tmp, n_all, n_all_t, stats, losses, labels.reshape(1, n_tok), meta, dx0, xs, hid, da, g)


def solution(mesh):
    n_stage = mesh.shape["stage"]

    def device_fn(tokens, labels, emb, w_up, w_down):
        n_micro, seq = tokens.shape
        vocab, dim = emb.shape
        w_up, w_down = w_up[0], w_down[0]
        n_tok = n_micro * seq
        plan = Plan(vocab, n_stage)
        cuts = jnp.array([plan.cuts(0), plan.cuts(1)], jnp.int32)
        x0 = run_gather(tokens, emb)
        n_all, xs, hid, da, g, dx0, stats, losses, tmp, meta, n_all_t = run_pipe(x0, emb, w_up, w_down, labels, tokens, cuts, n_stage, plan)
        flat = lambda p: p.reshape(n_tok, -1)
        grad_emb, loss, grad_up, grad_down = run_fin(
            emb, tmp.reshape(-1, dim), flat(n_all), n_all_t, stats, losses, labels, meta, flat(dx0), flat(xs), flat(hid), flat(da), flat(g), n_stage, plan
        )
        return loss, grad_up[None], grad_down[None], grad_emb

    return jax.shard_map(device_fn, mesh=mesh, in_specs=(P("dp", None), P("dp", None), P(None, None), P("stage", None, None), P("stage", None, None)), out_specs=(P("dp"), P(("dp", "stage"), None, None), P(("dp", "stage"), None, None), P("dp", None)), check_vma=False)
```

```python
import functools
import math

import jax
import jax.numpy as jnp
from jax import lax
from jax.experimental import pallas as pl
from jax.experimental.pallas import tpu as pltpu
from jax.sharding import PartitionSpec as P


MESH = pl.DeviceIdType.MESH
LOG2E = math.log2(math.e)
LN2 = math.log(2.0)
GELU_C = math.sqrt(2.0 / math.pi)
GELU_K = 0.044715
EPS = 1e-6
LANES = 128
F32 = jnp.float32
BF16 = jnp.bfloat16


def gelu_fwd(a):
    return (0.5 * a) * (1.0 + jnp.tanh(a * (GELU_C + (GELU_C * GELU_K) * (a * a))))


def gelu_slope(a):
    a2 = a * a
    half = 0.5 * jnp.tanh(a * (GELU_C + (GELU_C * GELU_K) * a2))
    up, down = 0.5 + half, 0.5 - half
    return up + (up * down) * (a * (2.0 * GELU_C + (6.0 * GELU_C * GELU_K) * a2))


def dot(x, y):
    return jnp.dot(x, y, preferred_element_type=F32)


def dot_t(x, y):
    return lax.dot_general(x, y, (((0,), (0,)), ((), ())), preferred_element_type=F32)


def remote(src, dst, send_sem, recv_sem, dev):
    return pltpu.make_async_remote_copy(src_ref=src, dst_ref=dst, send_sem=send_sem, recv_sem=recv_sem, device_id={"stage": dev}, device_id_type=MESH)


def column(row):
    return jnp.broadcast_to(row, (LANES, LANES)).T


def gather_kernel(ids_ref, tok_ref, emb_hbm, x0_hbm, tiles, picked, sem, out_sem):
    n_micro, seq = tok_ref.shape
    me = lax.axis_index("stage")
    group = tiles.shape[1] // seq
    slots = tiles.shape[0]
    owners = [head_chunk(me, k, n_micro) for k in range(slots)]

    def fetch(k):
        def one(i, carry):
            t = ids_ref[owners[k] * seq + i]
            start = pl.multiple_of(lax.bitwise_and(t, -group), group)
            pltpu.make_async_copy(emb_hbm.at[pl.ds(start, group)], tiles.at[k, pl.ds(pl.multiple_of(i * group, group), group)], sem.at[k]).start()
            return carry

        lax.fori_loop(0, seq, one, 0, unroll=8)

    def select(k):
        sub = lax.broadcasted_iota(jnp.int32, (LANES, LANES), 0)
        lane = lax.broadcasted_iota(jnp.int32, (LANES, LANES), 1)
        tok = column(tok_ref[pl.ds(owners[k], 1), :].astype(F32)).astype(jnp.int32)
        want = sub * group + lax.bitwise_and(tok, group - 1)
        hot = jnp.concatenate([jnp.where(lane + b * LANES == want, 1.0, 0.0).astype(BF16) for b in range(seq * group // LANES)], axis=1)
        pltpu.make_async_copy(emb_hbm.at[pl.ds(0, seq * group)], tiles.at[k], sem.at[k]).wait()
        picked[k] = dot(hot, tiles[k]).astype(BF16)
        pltpu.make_async_copy(picked.at[k], x0_hbm.at[k], out_sem.at[k]).start()

    def finish(k):
        pltpu.make_async_copy(picked.at[k], x0_hbm.at[k], out_sem.at[k]).wait()

    for work in (fetch, select, finish):
        work(0)
        for k in range(1, slots):
            pl.when(me < slots)(functools.partial(work, k))


def head_chunk(dev, k, n_micro):
    return jnp.minimum(jnp.where(dev < 2, 2 * dev + k, dev + 2), n_micro - 1)


def run_gather(tokens, emb):
    n_micro, seq = tokens.shape
    dim = emb.shape[1]
    group = 16
    return pl.pallas_call(
        gather_kernel,
        out_shape=jax.ShapeDtypeStruct((2, seq, dim), BF16),
        in_specs=[pl.BlockSpec(memory_space=pltpu.SMEM), pl.BlockSpec(memory_space=pltpu.VMEM), pl.BlockSpec(memory_space=pl.ANY)],
        out_specs=pl.BlockSpec(memory_space=pl.ANY),
        scratch_shapes=[pltpu.VMEM((2, seq * group, dim), BF16), pltpu.VMEM((2, seq, dim), BF16), pltpu.SemaphoreType.DMA((2,)), pltpu.SemaphoreType.DMA((2,))],
        cost_estimate=pl.CostEstimate(flops=10**9, bytes_accessed=2 * seq * group * dim * 2, transcendentals=0),
        name="gather",
    )(tokens.reshape(n_micro * seq), tokens, emb)


def token_table(row_ref, cut_ref, meta):
    n_tok = row_ref.shape[1]
    n_grp = n_tok // LANES
    lane = lax.broadcasted_iota(jnp.int32, (LANES, LANES), 1).astype(F32)
    sub = lax.broadcasted_iota(jnp.int32, (LANES, LANES), 0)
    row = lambda g: row_ref[:, g * LANES:(g + 1) * LANES].astype(F32)
    zero = jnp.zeros((LANES, LANES), F32)
    fold = lambda acc: jnp.sum(acc, axis=0, keepdims=True)
    cols = [column(row(c)) for c in range(n_grp)]
    firsts = []
    for g in range(n_grp):
        acc = zero
        for c in range(g + 1):
            same = cols[c] == row(g)
            if c == g:
                same = same & (sub < lane.astype(jnp.int32))
            acc = acc + jnp.where(same, 1.0, 0.0)
        firsts.append(column(jnp.where(fold(acc) == 0.0, 1.0, 0.0)))
    ranks = []
    for g in range(n_grp):
        acc = zero
        for c in range(n_grp):
            acc = acc + jnp.where(cols[c] < row(g), firsts[c], 0.0)
        ranks.append(fold(acc))
        meta[g:g + 1, :] = ranks[g].astype(jnp.int32)
    rank_cols = [column(r) for r in ranks]
    for g in range(n_grp):
        acc = zero
        for c in range(n_grp):
            acc = acc + jnp.where(rank_cols[c] == lane + g * LANES, firsts[c] * cols[c], 0.0)
        meta[n_grp + g:n_grp + g + 1, :] = fold(acc).astype(jnp.int32)
    cut = cut_ref[...].astype(F32)
    acc = zero
    for c in range(n_grp):
        acc = acc + jnp.where(cols[c] < cut, firsts[c], 0.0)
    meta[2 * n_grp:3 * n_grp, :] = jnp.broadcast_to(fold(acc), (n_grp, LANES)).astype(jnp.int32)


def logit_grad(e, n_t, shift, lab, first_id, inv_count, scale, dz):
    rows = e.shape[0]
    n_tok = n_t.shape[1]
    blk = 256
    vid = lax.broadcasted_iota(jnp.int32, (rows, blk), 0)
    for j in range(n_tok // blk):
        cols = slice(j * blk, (j + 1) * blk)
        z = (dot(e, n_t[:, cols]) * scale).astype(BF16).astype(F32)
        prob = jnp.exp2(z * LOG2E - shift[:, cols])
        dz[:, cols] = jnp.where(vid == lab[:, cols] - first_id, prob - inv_count, prob).astype(BF16)


def pipe_kernel(n_stage, plan, x0_hbm, emb_hbm, up_hbm, down_hbm, lab_hbm, row_hbm, cut_hbm,
                n_out, xs_out, hid_out, da_out, g_out, dx0_out, stat_out, loss_out, tmp_out, meta_out,
                xbuf, ybuf, abuf, hbuf, nbuf, gbuf, dxbuf, dx0buf, dnbuf, up, down, up_t, down_t,
                emb, zbuf, n_t, dn_acc, dn_send, dn_recv, dn_own, st_send, st_recv, statall, lossall, tops, n_all_t, shift, dz, obuf, z_pair, meta, lab_ref, row_ref, cut_ref,
                w_sem, e_sem, x_sem, x_send, f_send, f_recv, n_send, n_recv, nf_send, ag_send, fw_send,
                st_sems, dp_sems, dn_ssem, dn_rsem, sa_sems, lo_sems, b_send, b_recv, d_send, d_recv, r_sems, out_sem, o_sem, od_send, od_recv, ic_send, in_sem):
    n_micro, seq, dim = gbuf.shape
    part = xbuf.shape[1]
    n_part = xbuf.shape[0]
    per = seq // part
    n_tok = n_micro * seq
    ffn = up.shape[1]
    vocab = emb_hbm.shape[0]
    me = lax.axis_index("stage")
    core = lax.rem(me, 2)
    chip = me // 2
    mate = me + 1 - 2 * core
    last_id = n_stage - 1
    first = me == 0
    last = me == last_id
    fblk = 512
    n_fblk = ffn // fblk
    base, extra, tile = plan.base, plan.extra, plan.head_tile
    row0 = core * base
    n_tiles = base // tile
    wide_tile = plan.grad_tile

    barrier = pltpu.get_barrier_semaphore()
    gives_x = (me >= 1) & (me + 2 < n_micro)

    def here(dev):
        pl.semaphore_signal(barrier, inc=1, device_id={"stage": dev}, device_id_type=MESH)

    pl.when(jnp.logical_not(first))(lambda: here(me - 1))
    pl.when(jnp.logical_not(last))(lambda: here(me + 1))

    @pl.when(first)
    def _():
        for dev in range(2, n_micro - 2):
            here(dev)

    w_copy = [pltpu.make_async_copy(up_hbm, up, w_sem.at[0]), pltpu.make_async_copy(down_hbm, down, w_sem.at[1])]
    for c in w_copy:
        c.start()
    in_copy = [pltpu.make_async_copy(src, dst, in_sem.at[k]) for k, (src, dst) in enumerate(((lab_hbm, lab_ref), (row_hbm, row_ref), (cut_hbm, cut_ref)))]
    x_slots = x0_hbm.shape[0]
    x_mine = [head_chunk(me, k, n_micro) for k in range(x_slots)]

    def x_rows(m):
        return xbuf.at[pl.ds(m * per, per)]

    def x_local(k):
        return pltpu.make_async_copy(x0_hbm.at[k], x_rows(k), x_sem.at[k])

    @pl.when(first)
    def _():
        for k in range(x_slots):
            x_local(k).start()

    for c in in_copy:
        c.start()

    e_parts = plan.e_parts
    e_step = base // e_parts

    def e_copy(i):
        src = emb_hbm.at[pl.ds(pl.multiple_of(row0 + i * e_step, 16), e_step)]
        return pltpu.make_async_copy(src, emb.at[pl.ds(i * e_step, e_step)], e_sem.at[0])

    e_more = pltpu.make_async_copy(emb_hbm.at[pl.ds(2 * base, extra)], emb.at[pl.ds(base, extra)], e_sem.at[1])
    with jax.named_scope("entry"):
        pl.semaphore_wait(barrier, jnp.where(first | last, 1, 2) + jnp.where(gives_x & (me >= 2), 1, 0))

    def x_copy(k):
        return remote(x0_hbm.at[k], x_rows(x_mine[k]), x_send.at[k], f_recv.at[x_mine[k]], 0)

    @pl.when(gives_x)
    def _():
        x_copy(0).start()

        @pl.when(me < 2)
        def _():
            x_copy(1).start()

    def table_start():
        for i in range(e_parts):
            e_copy(i).start()
        pl.when(core == 1)(e_more.start)

    def transpose_weights():
        for j in range(n_fblk):
            up_t[j * fblk:(j + 1) * fblk, :] = up[:, j * fblk:(j + 1) * fblk].T
            down_t[:, j * fblk:(j + 1) * fblk] = down[j * fblk:(j + 1) * fblk, :].T

    @pl.when(jnp.logical_not(first))
    def _():
        for c in w_copy:
            c.wait()
        table_start()

    def idle_work():
        transpose_weights()
        in_copy[1].wait()
        in_copy[2].wait()
        token_table(row_ref, jnp.where(core == 0, cut_ref[0:1, :], cut_ref[1:2, :]), meta)

    @pl.when(chip >= n_stage // 4)
    def _():
        idle_work()

    def n_start(m):
        remote(nbuf.at[m], nbuf.at[m], n_send, n_recv.at[m], jnp.where(m == last_id, last_id - 1, m)).start()

    def fwd(h, carry, cold=False):
        m = h // per
        sub = lax.rem(h, per)
        rows = pl.ds(pl.multiple_of(sub * part, part), part)
        with jax.named_scope("fwd_wait"):

            @pl.when(first & (sub == 0))
            def _():
                @pl.when(m < x_slots)
                def _():
                    x_local(m).wait()

                @pl.when(m >= x_slots)
                def _():
                    remote(x_rows(m), x_rows(m), x_send.at[0], f_recv.at[m], me).wait_recv()

            @pl.when(jnp.logical_not(first))
            def _():
                remote(xbuf.at[h], xbuf.at[h], f_send, f_recv.at[h], me).wait_recv()

        with jax.named_scope("fwd_comp"):
            x = xbuf[h]
            if cold:
                w_copy[0].wait()
            for j in range(n_fblk):
                cols = slice(j * fblk, (j + 1) * fblk)
                a = dot(x, up[:, cols]).astype(BF16)
                abuf[m, rows, cols] = a
                hbuf[m, rows, cols] = gelu_fwd(a.astype(F32)).astype(BF16)
            if cold:
                w_copy[1].wait()
                table_start()
            y = (x.astype(F32) + dot(hbuf[m, rows, :], down[...])).astype(BF16)
            ybuf[h] = y

        @pl.when(jnp.logical_not(last))
        def _():
            remote(ybuf.at[h], xbuf.at[h], f_send, f_recv.at[h], me + 1).start()

        @pl.when(last)
        def _():
            yf = y.astype(F32)
            inv = lax.rsqrt(jnp.mean(yf * yf, axis=-1, keepdims=True) + EPS)
            nbuf[m, rows, :] = (yf * inv).astype(BF16)
            pl.when(sub == per - 1)(lambda: n_start(m))

        @pl.when(sub == per - 1)
        def _():
            pltpu.make_async_copy(hbuf.at[m], hid_out.at[m], out_sem.at[0]).start()
            pltpu.make_async_copy(x_rows(m), xs_out.at[pl.ds(m * per, per)], out_sem.at[1]).start()

        return carry

    pl.when(first)(lambda: (fwd(0, 0, cold=True), None)[1])
    lax.fori_loop(jnp.where(first, 1, 0), n_part, fwd, 0)

    @pl.when(chip < n_stage // 4)
    def _():
        idle_work()

    n_forward = remote(nbuf.at[me], nbuf.at[me], nf_send, n_recv.at[me], mate)
    with jax.named_scope("n_wait"):

        @pl.when(jnp.logical_not(last))
        def _():
            remote(nbuf.at[me], nbuf.at[me], n_send, n_recv.at[me], me).wait_recv()
            pl.when(mate != last_id)(n_forward.start)
            remote(nbuf.at[mate], nbuf.at[mate], n_send, n_recv.at[mate], me).wait_recv()

        for k in range(2):
            n_t[:, k * seq:(k + 1) * seq] = nbuf[2 * chip + k].T

    peers = [lax.rem(me + 2 * d, n_stage) for d in range(1, n_stage // 2)]
    ag_copies = [remote(nbuf.at[me], nbuf.at[me], ag_send.at[d], n_recv.at[me], p) for d, p in enumerate(peers)]
    for c, p in zip(ag_copies, peers):
        pl.when(p != last_id)(c.start)
    with jax.named_scope("e_wait"):
        pltpu.make_async_copy(emb_hbm.at[pl.ds(0, base)], emb.at[pl.ds(0, base)], e_sem.at[0]).wait()
        pl.when(core == 1)(e_more.wait)

    pair = 2 * seq
    scale = dim ** -0.5
    inv_count = 1.0 / n_tok
    log_count = math.log2(n_tok)
    in_copy[0].wait()
    lab = lab_ref[:, pl.ds(pl.multiple_of(chip * pair, pair), pair)]

    def logits(rows, size):
        e = emb[rows, :]
        parts = [dot(e[k * size // 2:(k + 1) * size // 2], n_t[...]) for k in range(2)]
        z = jnp.concatenate([(p * scale).astype(BF16) for p in parts], axis=0)
        zbuf[rows, :] = z
        return z

    def peak(z, size, top):
        best = jnp.max(z.reshape(size // 16, 16, pair), axis=0).astype(F32)
        return jnp.maximum(top, jnp.maximum(best[:8], best[8:]))

    def total(z, size, old, top, tot):
        off = top * LOG2E
        return tot * jnp.exp2(old * LOG2E - off) + jnp.sum(jnp.exp2(z.astype(F32).reshape(size // 8, 8, pair) * LOG2E - off[None]), axis=0)

    tops[0] = jnp.full((8, pair), -jnp.inf, F32)
    tops[1] = jnp.zeros((8, pair), F32)

    @pl.when(core == 1)
    def _():
        z = logits(pl.ds(base, extra), extra)
        top = peak(z, extra, tops[0])
        tops[1] = total(z, extra, tops[0], top, tops[1])
        tops[0] = top

    def logits_step(i, slot, old, top, tot):
        z = logits(pl.ds(pl.multiple_of(i * tile, 16), tile), tile)
        tot = total(z_pair[1 - slot], tile, old, top, tot)
        z_pair[slot] = z
        return top, peak(z, tile, top), tot

    with jax.named_scope("logits"):
        z = logits(pl.ds(0, tile), tile)
        z_pair[0] = z
        state = (tops[0], peak(z, tile, tops[0]), tops[1])
        state = lax.fori_loop(0, (n_tiles - 1) // 2, lambda i, c: logits_step(2 * i + 2, 0, *logits_step(2 * i + 1, 1, *c)), state)
        if n_tiles % 2 == 0:
            state = logits_step(n_tiles - 1, 1, *state)
        old, top, tot = state
        tot = total(z_pair[(n_tiles - 1) % 2], tile, old, top, tot)
    row_top = jnp.max(top, axis=0, keepdims=True)
    row_tot = jnp.sum(tot * jnp.exp2((top - row_top) * LOG2E), axis=0, keepdims=True)
    st_send[0:8, :] = jnp.broadcast_to(row_top, (8, pair))
    st_send[8:16, :] = jnp.broadcast_to(row_tot, (8, pair))
    st_copy = remote(st_send, st_recv, st_sems.at[0], st_sems.at[1], mate)
    with jax.named_scope("stat_x"):
        st_copy.start()
        st_copy.wait()
    far_top = st_recv[0:1, :]
    far_tot = st_recv[8:9, :]
    all_top = jnp.maximum(row_top, far_top)
    mine = row_tot * jnp.exp(row_top - all_top)
    other = far_tot * jnp.exp(far_top - all_top)
    lse = all_top + jnp.log(jnp.where(core == 0, mine + other, other + mine))
    my_shift = lse * LOG2E + log_count
    others = [lax.rem(me + d, n_stage) for d in range(1, n_stage)]

    def spread(buf, sems):
        whole = buf.at[pl.ds(0, n_stage - 1)]
        return [remote(buf.at[me], buf.at[me], sems.at[0], sems.at[1], p) for p in others], remote(whole, whole, sems.at[0], sems.at[1], me)

    statall[me] = jnp.broadcast_to(lse, (8, pair))
    sa_copies, sa_all = spread(statall, sa_sems)
    for c in sa_copies:
        c.start()

    def grads(rows, size, first_row, picked):
        zf = zbuf[rows, :].astype(F32)
        prob = jnp.exp2(zf * LOG2E - my_shift)
        hit = lax.broadcasted_iota(jnp.int32, (size, pair), 0) == lab - (row0 + first_row)
        dz_t = jnp.where(hit, prob - inv_count, prob).astype(BF16)
        got = jnp.where(hit, zf, 0.0).reshape(size // 8, 8, pair)
        return dot_t(dz_t, emb[rows, :]), picked + jnp.sum(got, axis=0)

    tops[0] = jnp.zeros((8, pair), F32)
    dn_acc[...] = jnp.zeros_like(dn_acc)

    @pl.when(core == 1)
    def _():
        dn_acc[...], tops[0] = grads(pl.ds(base, extra), extra, base, tops[0])

    def grad_step(i, picked):
        part, picked = grads(pl.ds(pl.multiple_of(i * wide_tile, 16), wide_tile), wide_tile, i * wide_tile, picked)
        dn_acc[...] += part
        return picked

    with jax.named_scope("grads"):
        picked = lax.fori_loop(0, base // wide_tile, grad_step, tops[0])
    far = pl.ds(pl.multiple_of((1 - core) * seq, seq), seq)
    near = pl.ds(pl.multiple_of(core * seq, seq), seq)
    dn_send[...] = dn_acc[far, :]
    dp_copy = remote(dn_send, dn_recv, dp_sems.at[0], dp_sems.at[1], mate)
    dp_copy.start()
    row_loss = jnp.where(core == 0, lse, 0.0) - jnp.sum(picked, axis=0, keepdims=True)
    lossall[me] = jnp.broadcast_to(row_loss, (8, pair))
    lo_copies, lo_all = spread(lossall, lo_sems)
    for c in lo_copies:
        c.start()
    with jax.named_scope("dn_x"):
        dp_copy.wait()
        dn = ((dn_acc[near, :] + dn_recv[...]) * scale).astype(BF16)
    dn_copy = remote(dn_own, dnbuf.at[me], dn_ssem, dn_rsem.at[me], last_id)

    @pl.when(last)
    def _():
        dnbuf[last_id] = dn

    @pl.when(jnp.logical_not(last))
    def _():
        dn_own[...] = dn
        remote(dn_own, dnbuf.at[me], dn_ssem, dn_rsem.at[me], last_id).start()

    with jax.named_scope("ag_wait"):
        for p in peers:
            got = remote(nbuf.at[p], nbuf.at[p], ag_send.at[0], n_recv.at[p], me)
            pl.when(jnp.logical_not(last))(got.wait_recv)
            pl.when(mate != last_id)(remote(nbuf.at[p], nbuf.at[p], fw_send, n_recv.at[p], mate).start)

    near_dst = [1, 3, last_id]
    far_dst = n_stage // 2 + 1
    direct = n_micro - 2
    by_prev = n_micro - 3
    hands_on = (core == 1) & (me != 1)

    def dx0_start(m, k, dev):
        remote(dxbuf.at[m], dx0buf.at[m], d_send.at[k], d_recv.at[m], dev).start()

    def relayed(m):
        return (m < direct) & (((me == 3) & (m != by_prev)) | (last & (m == by_prev)))

    def relay_far(m):
        remote(dx0buf.at[m], dx0buf.at[m], r_sems.at[1], d_recv.at[m], far_dst).start()

    def bwd(m):
        with jax.named_scope("bwd_wait"):
            @pl.when(jnp.logical_not(last))
            def _():
                remote(gbuf.at[m], gbuf.at[m], b_send, b_recv.at[m], me).wait_recv()

            @pl.when(last)
            def _():
                @pl.when(m != last_id)
                def _():
                    remote(dnbuf.at[m], dnbuf.at[m], dn_ssem, dn_rsem.at[m], me).wait_recv()

                yf = ybuf[pl.ds(m * per, per)].reshape(seq, dim).astype(F32)
                inv = lax.rsqrt(jnp.mean(yf * yf, axis=-1, keepdims=True) + EPS)
                dnf = dnbuf[m].astype(F32)
                proj = jnp.mean(yf * dnf, axis=-1, keepdims=True)
                gbuf[m] = (dnf * inv - yf * (inv * inv * inv * proj)).astype(BF16)

        with jax.named_scope("bwd_comp"):
            g = gbuf[m]
            for j in range(n_fblk):
                cols = slice(j * fblk, (j + 1) * fblk)
                dh = dot(g, down_t[:, cols]).astype(BF16).astype(F32)
                abuf[m, :, cols] = (dh * gelu_slope(abuf[m, :, cols].astype(F32))).astype(BF16)
            dxbuf[m] = (g.astype(F32) + dot(abuf[m], up_t[...])).astype(BF16)

        @pl.when(jnp.logical_not(first))
        def _():
            remote(dxbuf.at[m], gbuf.at[m], b_send, b_recv.at[m], me - 1).start()

        @pl.when(first)
        def _():
            pl.when(m >= direct)(lambda: dx0_start(m, len(near_dst), far_dst))
            for k, dev in enumerate(near_dst):
                dx0_start(m, k, dev)

        pltpu.make_async_copy(abuf.at[m], da_out.at[m], out_sem.at[2]).start()
        pltpu.make_async_copy(gbuf.at[m], g_out.at[m], out_sem.at[3]).start()

    n_slot = obuf.shape[0]
    busy = chip == last_id // 2
    far_tile = remote(tmp_out.at[core, pl.ds(0, plan.rows)], tmp_out.at[core, pl.ds(0, plan.rows)], ic_send, od_recv, jnp.where(first, last_id, last_id - 1))
    sends_far = first | (me == last_id - 2)

    def tile_copy(k):
        rows = pl.ds(pl.multiple_of(k * plan.rows, plan.rows), plan.rows)
        slot = lax.rem(k, n_slot)
        return pltpu.make_async_copy(obuf.at[slot], tmp_out.at[core, rows], o_sem.at[slot])

    def piece(p):
        k = p // plan.per_tile
        rows = pl.ds(pl.multiple_of(p * plan.piece, plan.piece), plan.piece)
        here = pl.ds(pl.multiple_of(lax.rem(p, plan.per_tile) * plan.piece, plan.piece), plan.piece)
        return remote(obuf.at[lax.rem(k, n_slot), here], tmp_out.at[core, rows], od_send.at[k], od_recv, mate)

    def tile_sent(k):
        slot = lax.rem(k, n_slot)
        return remote(obuf.at[slot], tmp_out.at[core, pl.ds(0, plan.rows)], od_send.at[k], od_recv, mate)

    def emb_tile(k):
        with jax.named_scope("tile_prep"):

            @pl.when(k == 0)
            def _():
                for d in range(1, n_stage // 2):
                    src = lax.rem(mate + 2 * d, n_stage)
                    pl.when(jnp.logical_not(last))(remote(nbuf.at[src], nbuf.at[src], ag_send.at[0], n_recv.at[src], me).wait_recv)
                for m in range(n_micro):
                    n_all_t[:, m * seq:(m + 1) * seq] = nbuf[m].T
                sa_all.wait_recv()
                for c in range(n_stage // 2):
                    shift[:, c * pair:(c + 1) * pair] = statall[2 * c, 0:1, :] * LOG2E + log_count

        slot = lax.rem(k, n_slot)
        with jax.named_scope("tile_wait"):
            @pl.when(k == 2)
            def _():
                tile_copy(0).wait()
                pl.when(sends_far)(far_tile.start)

            pl.when(k > n_slot)(lambda: tile_copy(k - n_slot).wait())
            pl.when((k >= n_slot) & (k - n_slot < plan.shared) & jnp.logical_not(busy & (k == n_slot)))(lambda: tile_sent(k - n_slot).wait_send())

        with jax.named_scope("tile"):
            rows = pl.ds(pl.multiple_of(k * plan.rows, plan.rows), plan.rows)
            logit_grad(emb[rows, :], n_all_t, shift, lab_ref, row0 + k * plan.rows, inv_count, scale, dz)
            obuf[slot] = dot(dz[...], nbuf[...].reshape(n_tok, dim)) * scale

        tile_copy(k).start()

    def send_pieces(done, until):
        lax.fori_loop(done, until, lambda p, c: (piece(p).start(), c)[1], 0)

    def send_tiles(done, until):
        def one(k, carry):
            rows = pl.ds(pl.multiple_of(k * plan.rows, plan.rows), plan.rows)
            remote(obuf.at[lax.rem(k, n_slot)], tmp_out.at[core, rows], od_send.at[k], od_recv, mate).start()
            return carry

        lax.fori_loop(done, until, one, 0)

    before = sum(jnp.where(me == s, plan.before[s], 0) for s in range(n_stage))

    def pass_dx0(m, carry):
        @pl.when(jnp.logical_not(first))
        def _():
            remote(dx0buf.at[m], dx0buf.at[m], r_sems.at[0], d_recv.at[m], me).wait_recv()

            @pl.when(hands_on)
            def _():
                remote(dx0buf.at[m], dx0buf.at[m], r_sems.at[0], d_recv.at[m], mate).start()

            @pl.when(relayed(m))
            def _():
                relay_far(m)

            pltpu.make_async_copy(dx0buf.at[m], dx0_out.at[m], out_sem.at[4]).start()

        @pl.when(first)
        def _():
            pltpu.make_async_copy(dxbuf.at[m], dx0_out.at[m], out_sem.at[4]).start()

        return carry

    lead = jnp.where(me == 3, -300, jnp.where(last, -1800, jnp.where(me == far_dst, -1750, -10**6)))

    def work(i, carry):
        sent, passed = carry
        chunk = (i >= before) & (i < before + n_micro)
        pl.when(chunk)(lambda: bwd(i - before))
        k = jnp.where(i < before, i, i - n_micro)
        pl.when(jnp.logical_not(chunk))(lambda: emb_tile(k))
        after = i - before - n_micro + 1
        here = jnp.where(after > 0, jnp.clip((after * 264 + lead) // 138, 0, n_micro), 0)
        lax.fori_loop(passed, here, pass_dx0, 0)
        ready = jnp.where(i < before, i + 1, jnp.where(chunk, before, i + 1 - n_micro))
        near_chunks = chunk | ((i < before) & (i + jnp.where(before >= 6, 2, 1) >= before))
        whole = (sent + plan.per_tile - 1) // plan.per_tile
        upto = jnp.minimum(jnp.minimum(ready, plan.shared), whole + 1)
        some = jnp.where(near_chunks, jnp.minimum(sent + 1, jnp.minimum(ready, plan.shared) * plan.per_tile), whole * plan.per_tile)
        send_pieces(sent, some)
        send_tiles(whole, jnp.where(near_chunks, 0, upto))
        now = jnp.where(near_chunks, some, jnp.maximum(some, upto * plan.per_tile))
        return jnp.maximum(sent, now), jnp.maximum(passed, here)

    sent, passed = lax.fori_loop(0, plan.tiles + n_micro, work, (jnp.where(busy, plan.per_tile, 0), 0))
    outs = [pltpu.make_async_copy(nbuf, n_out, out_sem.at[5]), pltpu.make_async_copy(lossall, loss_out, out_sem.at[6]), pltpu.make_async_copy(meta, meta_out, out_sem.at[7])]
    lo_all.wait_recv()
    for c in outs:
        c.start()
    pltpu.make_async_copy(statall, stat_out, out_sem.at[8]).start()
    with jax.named_scope("relay_all"):
        lax.fori_loop(passed, n_micro, pass_dx0, 0)

    with jax.named_scope("drain"):
        send_pieces(sent, plan.shared * plan.per_tile)
        for k in range(max(plan.tiles - n_slot, 0), plan.tiles):
            tile_copy(k).wait()
            if k < plan.shared:
                tile_sent(k).wait_send()
        pl.when(sends_far)(far_tile.wait_send)
        all_rows = pl.ds(0, plan.shared * plan.rows)
        remote(tmp_out.at[1 - core, all_rows], tmp_out.at[1 - core, all_rows], od_send.at[0], od_recv, me).wait_recv()
        sa_all.wait_send()
        lo_all.wait_send()
        pltpu.make_async_copy(statall, stat_out, out_sem.at[8]).wait()
        for c, p in zip(ag_copies, peers):
            pl.when(p != last_id)(c.wait_send)

        @pl.when(jnp.logical_not(last))
        def _():
            dn_copy.wait_send()
            pl.when(mate != last_id)(n_forward.wait_send)
            remote(ybuf, xbuf, f_send, f_recv.at[0], me + 1).wait_send()

        @pl.when(last)
        def _():
            remote(nbuf, nbuf, n_send, n_recv.at[0], me).wait_send()

        @pl.when(mate != last_id)
        def _():
            some = nbuf.at[pl.ds(0, len(peers))]
            remote(some, some, fw_send, n_recv.at[0], mate).wait_send()

        @pl.when(gives_x)
        def _():
            x_copy(0).wait_send()

            @pl.when(me < 2)
            def _():
                x_copy(1).wait_send()

        @pl.when(jnp.logical_not(first))
        def _():
            remote(dxbuf, gbuf, b_send, b_recv.at[0], me).wait_send()
            pl.when(hands_on)(remote(dx0buf, dx0buf, r_sems.at[0], d_recv.at[0], mate).wait_send)

        @pl.when(first)
        def _():
            for k in range(len(near_dst)):
                remote(dxbuf, dx0buf, d_send.at[k], d_recv.at[0], me).wait_send()
            rest = pl.ds(0, n_micro - direct)
            remote(dxbuf.at[rest], dx0buf.at[rest], d_send.at[len(near_dst)], d_recv.at[0], me).wait_send()

        for dev, kept in ((3, direct - 1), (last_id, 1)):
            some = dx0buf.at[pl.ds(0, kept)]
            pl.when(me == dev)(remote(some, some, r_sems.at[1], d_recv.at[0], me).wait_send)

        pltpu.make_async_copy(hbuf, hid_out, out_sem.at[0]).wait()
        pltpu.make_async_copy(xbuf, xs_out, out_sem.at[1]).wait()
        pltpu.make_async_copy(abuf, da_out, out_sem.at[2]).wait()
        pltpu.make_async_copy(gbuf, g_out, out_sem.at[3]).wait()
        pltpu.make_async_copy(dx0buf, dx0_out, out_sem.at[4]).wait()
        for c in outs:
            c.wait()


class Plan:
    def __init__(self, vocab, n_stage):
        units = vocab // LANES
        self.base = units // 2 * LANES
        self.extra = vocab - 2 * self.base
        self.head_tile = next(t for t in (1600, 1536, 1280, 1024, 768, 640, 512, 256, 128) if self.base % t == 0)
        self.rows = 1024
        self.tiles, self.shared = 11, 9
        self.grad_tile = next(t for t in (4000, 3200, 1600, 1280, 640, 256, 128) if self.base % t == 0)
        self.e_parts = next(k for k in (10, 8, 5, 4, 2, 1) if self.base % (16 * k) == 0)
        self.part = 128
        self.slots = 4
        self.piece = 256
        self.per_tile = self.rows // self.piece
        measured = [10, 9, 6, 5, 3, 2, 0, 0]
        self.before = (measured + [0] * n_stage)[:n_stage]
        mid = self.base
        ends = [(0, mid), (mid, vocab)]
        early = (self.tiles * self.rows, self.shared * self.rows)
        self.spans = [[(ends[h][0] + early[0 if h == c else 1], ends[h][1]) for h in (c, 1 - c)] for c in range(2)]
        self.longest = [max(self.spans[c][k][1] - self.spans[c][k][0] for c in range(2)) for k in range(2)]
        best = min(range(16, 1281, 16), key=lambda r: (sum(-(-n // r) for n in self.longest)) * (r + 40))
        self.calc_rows = best
        self.calc_steps = [-(-n // best) for n in self.longest]
        self.steps = sum(self.calc_steps)
        self.copy_rows = self.rows
        self.copies = self.tiles + self.shared
        self.starts = ends

    def calc_start(self, core, s):
        k = 0 if s < self.calc_steps[0] else 1
        lo, hi = self.spans[core][k]
        return min(lo + (s - k * self.calc_steps[0]) * self.calc_rows, hi - self.calc_rows)

    def copy_start(self, core, c):
        own = c < self.tiles
        h = core if own else 1 - core
        return self.starts[h][0] + (c if own else c - self.tiles) * self.copy_rows

    def cuts(self, core):
        firsts = [(self.calc_start(core, s), self.calc_rows) for s in range(self.steps)] + [(self.copy_start(core, c), self.copy_rows) for c in range(self.copies)]
        flat = [v for lo, rows in firsts for v in (lo, lo + rows)]
        return flat + [0] * (LANES - len(flat))


def run_pipe(x0, emb, w_up, w_down, labels, tokens, cuts, n_stage, plan):
    n_micro, seq = labels.shape
    dim, ffn = w_up.shape
    n_tok = n_micro * seq
    base = plan.base
    any_spec = pl.BlockSpec(memory_space=pl.ANY)
    act = (n_micro, seq, dim)
    fine = (n_tok // plan.part, plan.part, dim)
    wide = (n_micro, seq, ffn)
    dma = pltpu.SemaphoreType.DMA
    vm = pltpu.VMEM
    pair = 2 * seq
    return pl.pallas_call(
        functools.partial(pipe_kernel, n_stage, plan),
        out_shape=[
            jax.ShapeDtypeStruct(act, BF16), jax.ShapeDtypeStruct(fine, BF16), jax.ShapeDtypeStruct(wide, BF16),
            jax.ShapeDtypeStruct(wide, BF16), jax.ShapeDtypeStruct(act, BF16), jax.ShapeDtypeStruct(act, BF16),
            jax.ShapeDtypeStruct((n_stage, 8, pair), F32), jax.ShapeDtypeStruct((n_stage, 8, pair), F32), jax.ShapeDtypeStruct((2, plan.tiles * plan.rows, dim), F32),
            jax.ShapeDtypeStruct((3 * n_tok // LANES, LANES), jnp.int32),
        ],
        in_specs=[any_spec] * 7,
        out_specs=[any_spec] * 10,
        scratch_shapes=[
            vm(fine, BF16), vm(fine, BF16), vm(wide, BF16), vm(wide, BF16), vm(act, BF16), vm(act, BF16), vm(act, BF16), vm(act, BF16), vm(act, BF16),
            vm((dim, ffn), BF16), vm((ffn, dim), BF16), vm((ffn, dim), BF16), vm((dim, ffn), BF16),
            vm((base + plan.extra, dim), BF16), vm((base + plan.extra, pair), BF16), vm((dim, pair), BF16), vm((pair, dim), F32),
            vm((seq, dim), F32), vm((seq, dim), F32), vm((seq, dim), BF16), vm((16, pair), F32), vm((16, pair), F32), vm((n_stage, 8, pair), F32), vm((n_stage, 8, pair), F32),
            vm((2, 8, pair), F32), vm((dim, n_tok), BF16), vm((1, n_tok), F32), vm((plan.rows, n_tok), BF16), vm((plan.slots, plan.rows, dim), F32),
            vm((2, plan.head_tile, pair), BF16), vm((3 * n_tok // LANES, LANES), jnp.int32),
            vm((1, n_tok), jnp.int32), vm((1, n_tok), jnp.int32), vm((2, LANES), jnp.int32),
            dma((2,)), dma((2,)), dma((2,)), dma((2,)), dma, dma((n_tok // plan.part,)), dma, dma((n_micro,)), dma,
            dma((n_stage // 2,)), dma,
            dma((2,)), dma((2,)), dma, dma((n_stage,)), dma((2,)), dma((2,)), dma, dma((n_micro,)), dma((4,)), dma((n_micro,)), dma((2,)), dma((9,)),
            dma((plan.slots,)), dma((plan.shared,)), dma, dma, dma((3,)),
        ],
        compiler_params=pltpu.CompilerParams(collective_id=0, has_side_effects=True, vmem_limit_bytes=67_000_000),
        cost_estimate=pl.CostEstimate(flops=60 * 10**9, bytes_accessed=100 * 10**6, transcendentals=0),
        name="pipe",
    )(x0.reshape(x0.shape[0], seq // plan.part, plan.part, dim), emb, w_up, w_down, labels.reshape(1, n_tok), tokens.reshape(1, n_tok), cuts)


def fin_kernel(n_stage, n_tok, plan, ids_hbm, emb_hbm, tmp_hbm, n_hbm, stat_hbm, part_hbm, lab_hbm, meta_hbm, dx0_hbm, xs_hbm, hid_hbm, da_hbm, g_hbm,
               out_hbm, loss_ref, gup_hbm, gdown_hbm,
               n_all, dx0, xs, hid, da, g, n_t, x_t, dx0s, dz, shift, e_in, c_out, cp, gup, gdown,
               ld_sem, e_sem, t_sem, co_sem, po_sem, gu_sem, gd_sem, wi_sem, ids_ref, stat_ref, part_ref, lab_ref, meta_ref, in_sem):
    dim, ffn = gup_hbm.shape
    scale = dim ** -0.5
    inv_count = 1.0 / n_tok
    steps, crows, prows = plan.steps, plan.calc_rows, plan.copy_rows
    core = lax.rem(lax.axis_index("stage"), 2)
    early = plan.tiles * prows
    wblk = gup.shape[2]
    n_wblk = ffn // wblk
    turn = plan.calc_steps[0]

    def pick(pair):
        return jnp.where(core == 0, pair[0], pair[1])

    def calc_start(s):
        own = s < turn
        lo, hi = [jnp.where(own, pick([plan.spans[c][0][e] for c in range(2)]), pick([plan.spans[c][1][e] for c in range(2)])) for e in range(2)]
        return pl.multiple_of(jnp.minimum(lo + (s - jnp.where(own, 0, turn)) * crows, hi - crows), 16)

    def copy_start(c):
        own = c < plan.tiles
        first = jnp.where(own, pick([plan.starts[0][0], plan.starts[1][0]]), pick([plan.starts[1][0], plan.starts[0][0]]))
        return pl.multiple_of(first + (c - jnp.where(own, 0, plan.tiles)) * prows, 16)

    def e_copy(s):
        return pltpu.make_async_copy(emb_hbm.at[pl.ds(calc_start(s), crows)], e_in.at[lax.rem(s, 3)], e_sem.at[lax.rem(s, 3)])

    n_slot = cp.shape[0]
    ahead = 8

    def t_copy(c):
        own = c < plan.tiles
        row = jnp.where(own, core, 1 - core) * early + (c - jnp.where(own, 0, plan.tiles)) * prows
        slot = lax.rem(c, n_slot)
        return pltpu.make_async_copy(tmp_hbm.at[pl.ds(pl.multiple_of(row, 16), prows)], cp.at[slot], t_sem.at[slot])

    def p_out(c):
        slot = lax.rem(c, n_slot)
        return pltpu.make_async_copy(cp.at[slot], out_hbm.at[pl.ds(copy_start(c), prows)], po_sem.at[slot])

    def c_outs(s):
        slot = lax.rem(s, 2)
        return pltpu.make_async_copy(c_out.at[slot], out_hbm.at[pl.ds(calc_start(s), crows)], co_sem.at[slot])

    loads = [pltpu.make_async_copy(s, d, ld_sem.at[i]) for i, (s, d) in enumerate(((n_hbm, n_all), (dx0_hbm, dx0), (xs_hbm, xs), (g_hbm, g)))]
    ins = [pltpu.make_async_copy(s, d, in_sem.at[i]) for i, (s, d) in enumerate(((stat_hbm, stat_ref), (lab_hbm, lab_ref), (part_hbm, part_ref), (meta_hbm, meta_ref), (ids_hbm, ids_ref)))]
    loads[0].start()
    ins[0].start()
    ins[1].start()
    e_copy(0).start()
    loads[1].start()
    for c in ins[2:]:
        c.start()
    e_copy(1).start()
    for c in range(ahead):
        t_copy(c).start(priority=1)
    pair = stat_ref.shape[2]
    with jax.named_scope("fin_pre"):
        ins[0].wait()
        ins[1].wait()
        for c in range(n_stage // 2):
            shift[:, c * pair:(c + 1) * pair] = stat_ref[2 * c, 0:1, :] * LOG2E + math.log2(n_tok)
        loads[0].wait()
        n_t[...] = n_all[...].T

    def sum_rows():
        for c in ins[2:]:
            c.wait()
        loss_ref[0] = jnp.sum(sum(part_ref[d, 0:1, :] for d in range(n_stage))) * inv_count
        loads[1].wait()
        dense = jnp.concatenate([meta_ref[g:g + 1, :] for g in range(n_tok // LANES)], axis=1)
        order = lax.broadcasted_iota(jnp.int32, (n_tok, n_tok), 0) == dense
        dx0s[...] = dot(jnp.where(order, 1.0, 0.0).astype(BF16), dx0[...])

    def add_rows(k, start, ref):
        lo, hi = ids_ref[2 * n_tok + k], ids_ref[2 * n_tok + k + 1]
        wide = 8

        def some(p, width):
            at = [pl.ds(ids_ref[n_tok + p + u] - start, 1) for u in range(width)]
            new = [ref[at[u], :] + dx0s[pl.ds(p + u, 1), :] for u in range(width)]
            for u in range(width):
                ref[at[u], :] = new[u]

        def group(g, carry):
            some(lo + g * wide, wide)
            return carry

        def single(p, carry):
            some(p, 1)
            return carry

        n_grp = (hi - lo) // wide
        lax.fori_loop(0, n_grp, group, 0)
        lax.fori_loop(lo + n_grp * wide, hi, single, 0)

    def w_ins(w):
        cols = pl.ds(pl.multiple_of(w * wblk, wblk), wblk)
        wslot = lax.rem(w, 2)
        return (pltpu.make_async_copy(da_hbm.at[:, cols], da.at[wslot], wi_sem.at[0, wslot]), pltpu.make_async_copy(hid_hbm.at[:, cols], hid.at[wslot], wi_sem.at[1, wslot]))

    def w_outs(w):
        cols = pl.ds(pl.multiple_of(w * wblk, wblk), wblk)
        wslot = lax.rem(w, 2)
        return (pltpu.make_async_copy(gup.at[wslot], gup_hbm.at[:, cols], gu_sem.at[wslot]), pltpu.make_async_copy(gdown.at[wslot], gdown_hbm.at[cols], gd_sem.at[wslot]))

    def copy_tile(c, carry):
        with jax.named_scope("copy_wait"):
            t_copy(c).wait()
        with jax.named_scope("add_p"):
            add_rows(2 * steps + 2 * c, copy_start(c), cp.at[lax.rem(c, n_slot)])
        p_out(c).start()

        @pl.when(c + ahead < plan.copies)
        def _():
            pl.when(c + ahead >= n_slot)(lambda: p_out(c + ahead - n_slot).wait())
            t_copy(c + ahead).start(priority=1)

        return carry

    w_first = 2
    tails = [turn - 1, steps - 1]

    def tail(s):
        return (s == tails[0]) | (s == tails[1])

    def step(s, carry):
        pl.when(s + 2 < steps)(lambda: e_copy(s + 2).start())
        with jax.named_scope("fin_wait"):
            e_copy(s).wait()

        @pl.when(s == 0)
        def _():
            for c in loads[2:]:
                c.start()

        w = s - w_first

        @pl.when((w + 1 >= 0) & (w + 1 < n_wblk))
        def _():
            for c in w_ins(w + 1):
                c.start()

        pl.when((s >= 2) & jnp.logical_not(tail(s - 1)))(lambda: c_outs(s - 2).wait())
        slot = lax.rem(s, 2)
        start = calc_start(s)
        with jax.named_scope("calc"):
            logit_grad(e_in[lax.rem(s, 3)], n_t, shift, lab_ref, start, inv_count, scale, dz)
            c_out[slot] = dot(dz[...], n_all[...]) * scale
        pl.when(s == 0)(sum_rows)
        with jax.named_scope("add_c"):
            add_rows(2 * s, start, c_out.at[slot])
        pl.when(tail(s))(lambda: c_outs(s - 1).wait())
        c_outs(s).start()
        lax.fori_loop(s * plan.copies // (steps - 1), jnp.minimum((s + 1) * plan.copies // (steps - 1), plan.copies), copy_tile, 0)

        @pl.when(w == 0)
        def _():
            for c in loads[2:]:
                c.wait()
            x_t[...] = xs[...].T

        @pl.when((w >= 0) & (w < n_wblk))
        def _():
            wslot = lax.rem(w, 2)
            with jax.named_scope("dw_wait"):
                for c in w_ins(w):
                    c.wait()

                @pl.when(w >= 2)
                def _():
                    for c in w_outs(w - 2):
                        c.wait()

            with jax.named_scope("dw"):
                gup[wslot] = dot(x_t[...], da[wslot])
                gdown[wslot] = dot_t(hid[wslot], g[...])
            for c in w_outs(w):
                c.start()

        return carry

    lax.fori_loop(0, steps, step, 0)
    with jax.named_scope("fin_drain"):
        for w in range(n_wblk - 2, n_wblk):
            for c in w_outs(w):
                c.wait()
        c_outs(steps - 1).wait()
        for c in range(plan.copies - n_slot, plan.copies):
            p_out(c).wait()


def run_fin(emb, tmp, n_all, stats, losses, labels, meta, dx0, xs, hid, da, g, n_stage, plan):
    vocab, dim = emb.shape
    n_tok, ffn = hid.shape
    vm = pltpu.VMEM
    dma = pltpu.SemaphoreType.DMA
    any_spec = pl.BlockSpec(memory_space=pl.ANY)
    smem = pl.BlockSpec(memory_space=pltpu.SMEM)
    wblk = 512
    return pl.pallas_call(
        functools.partial(fin_kernel, n_stage, n_tok, plan),
        out_shape=[jax.ShapeDtypeStruct((vocab, dim), F32), jax.ShapeDtypeStruct((1,), F32), jax.ShapeDtypeStruct((dim, ffn), F32), jax.ShapeDtypeStruct((ffn, dim), F32)],
        in_specs=[any_spec] * 13,
        out_specs=[any_spec, smem, any_spec, any_spec],
        scratch_shapes=[
            vm((n_tok, dim), BF16), vm((n_tok, dim), BF16), vm((n_tok, dim), BF16), vm((2, n_tok, wblk), BF16), vm((2, n_tok, wblk), BF16), vm((n_tok, dim), BF16),
            vm((dim, n_tok), BF16), vm((dim, n_tok), BF16), vm((n_tok, dim), F32), vm((plan.calc_rows, n_tok), BF16), vm((1, n_tok), F32),
            vm((3, plan.calc_rows, dim), BF16), vm((2, plan.calc_rows, dim), F32), vm((11, plan.copy_rows, dim), F32),
            vm((2, dim, wblk), F32), vm((2, wblk, dim), F32),
            dma((4,)), dma((3,)), dma((11,)), dma((2,)), dma((11,)), dma((2,)), dma((2,)), dma((2, 2)),
            pltpu.SMEM((meta.size,), jnp.int32), vm(stats.shape, F32), vm(losses.shape, F32), vm((1, n_tok), jnp.int32), vm(meta.shape, jnp.int32), dma((5,)),
        ],
        compiler_params=pltpu.CompilerParams(vmem_limit_bytes=67_000_000),
        cost_estimate=pl.CostEstimate(flops=2 * n_tok * vocab * dim, bytes_accessed=5 * vocab * dim, transcendentals=0),
        name="fin",
    )(meta.reshape(-1), emb, tmp, n_all, stats, losses, labels.reshape(1, n_tok), meta, dx0, xs, hid, da, g)


def solution(mesh):
    n_stage = mesh.shape["stage"]

    def device_fn(tokens, labels, emb, w_up, w_down):
        n_micro, seq = tokens.shape
        vocab, dim = emb.shape
        w_up, w_down = w_up[0], w_down[0]
        n_tok = n_micro * seq
        plan = Plan(vocab, n_stage)
        cuts = jnp.array([plan.cuts(0), plan.cuts(1)], jnp.int32)
        x0 = run_gather(tokens, emb)
        n_all, xs, hid, da, g, dx0, stats, losses, tmp, meta = run_pipe(x0, emb, w_up, w_down, labels, tokens, cuts, n_stage, plan)
        flat = lambda p: p.reshape(n_tok, -1)
        grad_emb, loss, grad_up, grad_down = run_fin(
            emb, tmp.reshape(-1, dim), flat(n_all), stats, losses, labels, meta, flat(dx0), flat(xs), flat(hid), flat(da), flat(g), n_stage, plan
        )
        return loss, grad_up[None], grad_down[None], grad_emb

    return jax.shard_map(device_fn, mesh=mesh, in_specs=(P("dp", None), P("dp", None), P(None, None), P("stage", None, None), P("stage", None, None)), out_specs=(P("dp"), P(("dp", "stage"), None, None), P(("dp", "stage"), None, None), P("dp", None)), check_vma=False)
```
